128 devices in a mesh: tp: 4 (over x), fsdp: 32 (over z, y, core).
Axes of the slice: x: 4, y: 4, z: 4, core: 2. Of those that a mesh axis runs over, the one named last changes fastest.
Arguments:
- patches: bfloat16 [1024, 49, 3072], P('fsdp')
- labels: int32 [1024], P('fsdp')
- w_stem: float32 [3072, 1024], P('fsdp', 'tp')
- b_stem: float32 [1024], P(('tp', 'fsdp'))
- ln1_g: float32 [2, 1024], P(None, ('tp', 'fsdp'))
- ln1_b: float32 [2, 1024], P(None, ('tp', 'fsdp'))
- w_tok1: float32 [2, 49, 512], P(None, None, 'fsdp')
- b_tok1: float32 [2, 512], P(None, 'fsdp')
- w_tok2: float32 [2, 512, 49], P(None, 'fsdp')
- ln2_g: float32 [2, 1024], P(None, ('tp', 'fsdp'))
- ln2_b: float32 [2, 1024], P(None, ('tp', 'fsdp'))
- w_ch1: float32 [2, 1024, 4096], P(None, 'fsdp', 'tp')
- b_ch1: float32 [2, 4096], P(None, ('tp', 'fsdp'))
- w_ch2: float32 [2, 4096, 1024], P(None, ('tp', 'fsdp'))
- b_ch2: float32 [2, 1024], P(None, ('tp', 'fsdp'))
- lnf_g: float32 [1024], P(('tp', 'fsdp'))
- lnf_b: float32 [1024], P(('tp', 'fsdp'))
- w_head: float32 [1024, 1000], P('fsdp', 'tp')
- b_head: float32 [1000], P('tp')
Outputs:
- output 1: float32 [], replicated
- output 2: float32 [3072, 1024], P('fsdp', 'tp')
- output 3: float32 [1024], P(('tp', 'fsdp'))
- output 4: float32 [2, 1024], P(None, ('tp', 'fsdp'))
- output 5: float32 [2, 1024], P(None, ('tp', 'fsdp'))
- output 6: float32 [2, 49, 512], P(None, None, 'fsdp')
- output 7: float32 [2, 512], P(None, 'fsdp')
- output 8: float32 [2, 512, 49], P(None, 'fsdp')
- output 9: float32 [2, 1024], P(None, ('tp', 'fsdp'))
- output 10: float32 [2, 1024], P(None, ('tp', 'fsdp'))
- output 11: float32 [2, 1024, 4096], P(None, 'fsdp', 'tp')
- output 12: float32 [2, 4096], P(None, ('tp', 'fsdp'))
- output 13: float32 [2, 4096, 1024], P(None, ('tp', 'fsdp'))
- output 14: float32 [2, 1024], P(None, ('tp', 'fsdp'))
- output 15: float32 [1024], P(('tp', 'fsdp'))
- output 16: float32 [1024], P(('tp', 'fsdp'))
- output 17: float32 [1024, 1000], P('fsdp', 'tp')
- output 18: float32 [1000], P('tp')
All inputs are finite; a program needn't handle non-finite values.
Results may differ from the reference program's by a relative error of at most 0.014476.
Values are sent between devices in bfloat16 or wider.
A program may use at most 1 GiB of HBM per device.

```python
import jax
import jax.numpy as jnp
from jax import lax

PATCH_SIDE = 32
TOKENS = 49
CHANNELS = 1024
TOKEN_HIDDEN = 512
CHANNEL_HIDDEN = 4096
CLASSES = 1000
LAYERS = 2
IMAGES = 1024
BLOCKS = 32

PATCH_DIM = 3 * PATCH_SIDE * PATCH_SIDE
PER_BLOCK = IMAGES // BLOCKS
EPS = 1e-6
LAYER_NAMES = ('ln1_g', 'ln1_b', 'w_tok1', 'b_tok1', 'w_tok2', 'ln2_g', 'ln2_b', 'w_ch1', 'b_ch1', 'w_ch2', 'b_ch2')


def setup_inputs(seed: int = 0) -> dict:
    key_list = jax.random.split(jax.random.key(seed), 20)

    def normal(index, shape, scale):
        return scale * jax.random.normal(key_list[index], shape, jnp.float32)

    chan_shape = (LAYERS, CHANNELS)
    return {
        'patches': normal(0, (IMAGES, TOKENS, PATCH_DIM), 1.0).astype(jnp.bfloat16),
        'labels': jax.random.randint(key_list[1], (IMAGES,), 0, CLASSES, jnp.int32),
        'w_stem': normal(2, (PATCH_DIM, CHANNELS), PATCH_DIM ** -0.5),
        'b_stem': normal(3, (CHANNELS,), 0.5),
        'ln1_g': 1.0 + normal(4, chan_shape, 0.3),
        'ln1_b': normal(5, chan_shape, 0.3),
        'w_tok1': normal(6, (LAYERS, TOKENS, TOKEN_HIDDEN), TOKENS ** -0.5),
        'b_tok1': normal(7, (LAYERS, TOKEN_HIDDEN), 0.3),
        'w_tok2': normal(8, (LAYERS, TOKEN_HIDDEN, TOKENS), TOKEN_HIDDEN ** -0.5),
        'ln2_g': 1.0 + normal(9, chan_shape, 0.3),
        'ln2_b': normal(10, chan_shape, 0.3),
        'w_ch1': normal(11, (LAYERS, CHANNELS, CHANNEL_HIDDEN), CHANNELS ** -0.5),
        'b_ch1': normal(12, (LAYERS, CHANNEL_HIDDEN), 0.3),
        'w_ch2': normal(13, (LAYERS, CHANNEL_HIDDEN, CHANNELS), CHANNEL_HIDDEN ** -0.5),
        'b_ch2': normal(14, chan_shape, 0.3),
        'lnf_g': 1.0 + normal(15, (CHANNELS,), 0.3),
        'lnf_b': normal(16, (CHANNELS,), 0.3),
        'w_head': normal(17, (CHANNELS, CLASSES), CHANNELS ** -0.5),
        'b_head': normal(18, (CLASSES,), 0.5),
    }


def as_matmul(values):
    return values.astype(jnp.bfloat16).astype(jnp.float32)


def layer_norm(values, gain, shift):
    mean_val = jnp.mean(values, axis=-1, keepdims=True)
    centered = values - mean_val
    var_val = jnp.mean(centered * centered, axis=-1, keepdims=True)
    return centered * lax.rsqrt(var_val + EPS) * gain + shift


def mixer_layer(resid, layer):
    normed = as_matmul(layer_norm(resid, layer['ln1_g'], layer['ln1_b']))
    hidden = jnp.einsum('bsc,sj->bcj', normed, as_matmul(layer['w_tok1'])) + layer['b_tok1']
    mixed = jnp.einsum('bcj,js->bsc', as_matmul(jax.nn.gelu(hidden)), as_matmul(layer['w_tok2']))
    resid = resid + mixed
    normed = as_matmul(layer_norm(resid, layer['ln2_g'], layer['ln2_b']))
    hidden = jnp.einsum('bsc,cd->bsd', normed, as_matmul(layer['w_ch1'])) + layer['b_ch1']
    out_val = jnp.einsum('bsd,dc->bsc', as_matmul(jax.nn.gelu(hidden)), as_matmul(layer['w_ch2']))
    return resid + out_val + layer['b_ch2'], None


def block_loss(weights, patch_blk, label_blk):
    resid = jnp.einsum('bsp,pc->bsc', patch_blk.astype(jnp.float32), as_matmul(weights['w_stem'])) + weights['b_stem']
    layer_weights = {name: weights[name] for name in LAYER_NAMES}
    resid = lax.scan(mixer_layer, resid, layer_weights)[0]
    pooled = jnp.mean(resid, axis=1)
    normed = as_matmul(layer_norm(pooled, weights['lnf_g'], weights['lnf_b']))
    logits = jnp.einsum('bc,ck->bk', normed, as_matmul(weights['w_head'])) + weights['b_head']
    log_norm = jax.nn.logsumexp(logits, axis=-1)
    class_ids = jnp.arange(CLASSES, dtype=jnp.int32)
    picked = jnp.sum(jnp.where(class_ids[None, :] == label_blk[:, None], logits, 0.0), axis=-1)
    return jnp.sum(log_norm - picked)


def reference(patches, labels, w_stem, b_stem, ln1_g, ln1_b, w_tok1, b_tok1, w_tok2,
              ln2_g, ln2_b, w_ch1, b_ch1, w_ch2, b_ch2, lnf_g, lnf_b, w_head, b_head):
    weights = dict(w_stem=w_stem, b_stem=b_stem, ln1_g=ln1_g, ln1_b=ln1_b, w_tok1=w_tok1,
                   b_tok1=b_tok1, w_tok2=w_tok2, ln2_g=ln2_g, ln2_b=ln2_b, w_ch1=w_ch1,
                   b_ch1=b_ch1, w_ch2=w_ch2, b_ch2=b_ch2, lnf_g=lnf_g, lnf_b=lnf_b,
                   w_head=w_head, b_head=b_head)
    patch_blocks = patches.reshape(BLOCKS, PER_BLOCK, TOKENS, PATCH_DIM)
    label_blocks = labels.reshape(BLOCKS, PER_BLOCK)
    loss_grad = jax.value_and_grad(block_loss)

    def accumulate(carry, block):
        loss_sum, grad_sum = carry
        value, grads = loss_grad(weights, block[0], block[1])
        return (loss_sum + value, jax.tree.map(jnp.add, grad_sum, grads)), None

    start_carry = (jnp.zeros((), jnp.float32), jax.tree.map(jnp.zeros_like, weights))
    loss_sum, grad_sum = lax.scan(accumulate, start_carry, (patch_blocks, label_blocks))[0]
    scale = 1.0 / IMAGES
    return (loss_sum * scale, grad_sum['w_stem'] * scale, grad_sum['b_stem'] * scale,
            grad_sum['ln1_g'] * scale, grad_sum['ln1_b'] * scale, grad_sum['w_tok1'] * scale,
            grad_sum['b_tok1'] * scale, grad_sum['w_tok2'] * scale, grad_sum['ln2_g'] * scale,
            grad_sum['ln2_b'] * scale, grad_sum['w_ch1'] * scale, grad_sum['b_ch1'] * scale,
            grad_sum['w_ch2'] * scale, grad_sum['b_ch2'] * scale, grad_sum['lnf_g'] * scale,
            grad_sum['lnf_b'] * scale, grad_sum['w_head'] * scale, grad_sum['b_head'] * scale)
```

```python
import jax
import jax.numpy as jnp
from jax import lax
from jax.sharding import PartitionSpec as P

EPS = 1e-6
CHANNEL_AXES = ('tp', 'fsdp')
ALL_AXES = ('tp', 'fsdp')
RS_DTYPE = jnp.float32


def product(form, left, right):
    return jnp.einsum(form, left, right, preferred_element_type=jnp.float32)


def bf(x):
    return x.astype(jnp.bfloat16)


def gather_all(x):
    g = lax.all_gather(x, ALL_AXES, axis=0, tiled=False)
    return g


def scatter_all(x):
    return lax.psum_scatter(x.astype(RS_DTYPE), ALL_AXES, scatter_dimension=0, tiled=True).astype(jnp.float32)[0]


def norm_forward(values, gain, shift):
    mean_val = jnp.mean(values, axis=-1, keepdims=True)
    cent = values - mean_val
    inv_std = lax.rsqrt(jnp.mean(cent * cent, axis=-1, keepdims=True) + EPS)
    standard = cent * inv_std
    return standard * gain + shift, standard, inv_std


def norm_backward(grad_out, gain, standard, inv_std):
    gs = grad_out * gain
    m0 = jnp.mean(gs, axis=-1, keepdims=True)
    m1 = jnp.mean(gs * standard, axis=-1, keepdims=True)
    return inv_std * (gs - m0 - standard * m1)


def gelu_grad(pre_act, grad_out):
    return jax.vjp(jax.nn.gelu, pre_act)[1](grad_out)[0]


def weight_specs():
    vec_spec = P(CHANNEL_AXES)
    layer_vec = P(None, CHANNEL_AXES)
    return (P('fsdp', 'tp'), vec_spec, layer_vec, layer_vec, P(None, None, 'fsdp'), P(None, 'fsdp'),
            P(None, 'fsdp', None), layer_vec, layer_vec, P(None, 'fsdp', 'tp'), layer_vec,
            P(None, CHANNEL_AXES, None), layer_vec, vec_spec, vec_spec, P('fsdp', 'tp'), P('tp'))


def solution(mesh):
    fs = mesh.shape['fsdp']
    tp = mesh.shape['tp']
    nd = fs * tp

    def step(patches, labels, w_stem, b_stem, ln1_g, ln1_b, w_tok1, b_tok1, w_tok2,
             ln2_g, ln2_b, w_ch1, b_ch1, w_ch2, b_ch2, lnf_g, lnf_b, w_head, b_head):
        t = lax.axis_index('tp')
        nl = w_tok1.shape[0]
        bl = patches.shape[0] // tp
        tokens = patches.shape[1]
        total_images = bl * nd
        pat = lax.dynamic_slice_in_dim(patches, t * bl, bl, 0)
        lab = lax.dynamic_slice_in_dim(labels, t * bl, bl, 0)

        vecs = [b_stem[None], ln1_g, ln1_b, ln2_g, ln2_b, b_ch2, lnf_g[None], lnf_b[None]]
        vec_rows = jnp.concatenate(vecs, axis=0)
        n_rows = vec_rows.shape[0]
        pieces = [vec_rows.reshape(-1), b_ch1.reshape(-1), b_tok1.reshape(-1), b_head.reshape(-1),
                  w_tok1.reshape(-1), w_tok2.reshape(-1)]
        sizes = [p.shape[0] for p in pieces]
        pack = jnp.concatenate(pieces)
        pad = (-pack.shape[0]) % 1024
        pack = jnp.pad(pack, (0, pad))
        small = gather_all(pack).reshape(tp, fs, -1)
        offs = []
        o = 0
        for s in sizes:
            offs.append(small[:, :, o:o + s])
            o += s
        vec_all = offs[0].reshape(tp, fs, n_rows, -1).transpose(2, 0, 1, 3).reshape(n_rows, -1)
        bch1 = offs[1].reshape(tp, fs, nl, -1).transpose(2, 0, 1, 3).reshape(nl, -1)
        btok1 = offs[2][0].reshape(fs, nl, -1).transpose(1, 0, 2).reshape(nl, -1)
        bhead = offs[3][:, 0].reshape(-1)
        wtok1 = bf(offs[4][0].reshape(fs, nl, tokens, -1).transpose(1, 2, 0, 3).reshape(nl, tokens, -1))
        wtok2 = bf(offs[5][0].reshape(fs, nl, -1, tokens).transpose(1, 0, 2, 3).reshape(nl, -1, tokens))
        bstem = vec_all[0]
        l1g, l1b, l2g, l2b, bc2 = [vec_all[1 + nl * i:1 + nl * (i + 1)] for i in range(5)]
        lfg, lfb = vec_all[1 + 5 * nl], vec_all[2 + 5 * nl]

        ws = gather_all(bf(w_stem)).reshape(tp, -1, w_stem.shape[1])
        wc1 = [gather_all(bf(w_ch1[l])).reshape(tp, -1, w_ch1.shape[2]) for l in range(nl)]
        wc2 = [gather_all(bf(w_ch2[l])).reshape(-1, w_ch2.shape[2]) for l in range(nl)]
        wh = gather_all(bf(w_head)).reshape(tp, -1, w_head.shape[1])

        c = w_stem.shape[1] * tp
        resid = product('bsp,tpc->bstc', pat, ws).reshape(bl, tokens, c) + bstem
        saved = []
        for l in range(nl):
            normed, n1s, n1i = norm_forward(resid, l1g[l], l1b[l])
            normed = bf(normed)
            tok_pre = product('bsc,sj->bcj', normed, wtok1[l]) + btok1[l]
            tok_act = bf(jax.nn.gelu(tok_pre))
            resid = resid + product('bcj,js->bsc', tok_act, wtok2[l])
            normed2, n2s, n2i = norm_forward(resid, l2g[l], l2b[l])
            full_in = bf(normed2)
            ch_pre = product('bsc,tcd->bstd', full_in, wc1[l]).reshape(bl, tokens, -1) + bch1[l]
            ch_act = bf(jax.nn.gelu(ch_pre))
            resid = resid + product('bsd,dc->bsc', ch_act, wc2[l]) + bc2[l]
            saved.append((normed, n1s, n1i, tok_pre, tok_act, n2s, n2i, full_in, ch_pre, ch_act))

        pooled = jnp.mean(resid, axis=1)
        head_in, hs, hi = norm_forward(pooled, lfg, lfb)
        head_bf = bf(head_in)
        logits = product('bc,tck->btk', head_bf, wh).reshape(bl, -1) + bhead
        is_label = jnp.arange(logits.shape[1])[None, :] == lab[:, None]
        row_max = jnp.max(logits, axis=1, keepdims=True)
        ex = jnp.exp(logits - row_max)
        es = jnp.sum(ex, axis=1, keepdims=True)
        log_norm = row_max + jnp.log(es)
        loss_loc = jnp.sum(log_norm) - jnp.sum(jnp.where(is_label, logits, 0.0))

        d_logits = (ex / es - is_label.astype(jnp.float32)) / total_images
        dlb = bf(d_logits).reshape(bl, tp, -1)
        g_bhead = jnp.sum(d_logits, axis=0)
        gh_full = product('bc,btk->tck', head_bf, dlb).reshape(nd, -1)
        gh_full = jnp.pad(gh_full, ((0, 0), (0, (-gh_full.shape[1]) % c))).reshape(nd, -1, c)
        gh_full = jnp.pad(gh_full, ((0, 0), (0, 8), (0, 0)))
        d_hin = product('btk,tck->bc', dlb, wh)
        g_lfg = jnp.sum(d_hin * hs, axis=0)
        g_lfb = jnp.sum(d_hin, axis=0)
        d_pooled = norm_backward(d_hin, lfg, hs, hi)
        d_resid = jnp.broadcast_to((d_pooled / tokens)[:, None, :], resid.shape)

        big1, big2 = [None] * nl, [None] * nl
        sm = {}
        for l in reversed(range(nl)):
            normed, n1s, n1i, tok_pre, tok_act, n2s, n2i, full_in, ch_pre, ch_act = saved[l]
            sm['b_ch2', l] = jnp.sum(d_resid, axis=(0, 1))
            dob = bf(d_resid)
            big2[l] = product('bsd,bsc->dc', ch_act, dob).reshape(nd, -1, c)
            d_pre = gelu_grad(ch_pre, product('bsc,dc->bsd', dob, wc2[l]))
            sm['b_ch1', l] = jnp.sum(d_pre, axis=(0, 1))
            dpb = bf(d_pre).reshape(bl, tokens, tp, -1)
            big1[l] = product('bsc,bstd->tcd', full_in, dpb).reshape(nd, -1, w_ch1.shape[2])
            d_n2 = product('bstd,tcd->bsc', dpb, wc1[l])
            sm['ln2_g', l] = jnp.sum(d_n2 * n2s, axis=(0, 1))
            sm['ln2_b', l] = jnp.sum(d_n2, axis=(0, 1))
            d_mid = d_resid + norm_backward(d_n2, l2g[l], n2s, n2i)
            dmb = bf(d_mid)
            sm['w_tok2', l] = product('bcj,bsc->js', tok_act, dmb)
            d_tp = gelu_grad(tok_pre, product('bsc,js->bcj', dmb, wtok2[l]))
            sm['b_tok1', l] = jnp.sum(d_tp, axis=(0, 1))
            dtb = bf(d_tp)
            sm['w_tok1', l] = product('bsc,bcj->sj', normed, dtb)
            d_n1 = product('bcj,sj->bsc', dtb, wtok1[l])
            sm['ln1_g', l] = jnp.sum(d_n1 * n1s, axis=(0, 1))
            sm['ln1_b', l] = jnp.sum(d_n1, axis=(0, 1))
            d_resid = d_mid + norm_backward(d_n1, l1g[l], n1s, n1i)
        g_bstem = jnp.sum(d_resid, axis=(0, 1))
        g_stem = scatter_all(product('bsp,bstc->tpc', pat, bf(d_resid).reshape(bl, tokens, tp, -1)).reshape(nd, -1, w_stem.shape[1]))

        half = w_ch2.shape[1] // 2
        ra = scatter_all(jnp.concatenate([big2[1], gh_full], axis=1))
        rb = scatter_all(jnp.concatenate([big1[1], big2[0][:, :half]], axis=1))
        rc = scatter_all(jnp.concatenate([big1[0], big2[0][:, half:]], axis=1))
        g_ch2 = jnp.stack([jnp.concatenate([rb[2 * half:], rc[2 * half:]], axis=0), ra[:2 * half]])
        g_ch1 = jnp.stack([rc[:2 * half], rb[:2 * half]])
        g_head = ra[2 * half:].reshape(-1)[:w_head.size].reshape(w_head.shape)
        st = lambda k: jnp.stack([sm[k, l] for l in range(nl)])
        parts = [g_bstem, st('ln1_g'), st('ln1_b'), st('ln2_g'), st('ln2_b'), st('b_ch2'), g_lfg, g_lfb,
                 st('b_ch1'), st('b_tok1'), g_bhead, st('w_tok1'), st('w_tok2'), loss_loc[None]]
        flat = jnp.concatenate([p.reshape(-1) for p in parts])
        flat = jnp.pad(flat, (0, (-flat.shape[0]) % 1024))
        tot = lax.psum(flat, ALL_AXES)
        out = []
        o = 0
        for p in parts:
            out.append(tot[o:o + p.size].reshape(p.shape))
            o += p.size
        f = lax.axis_index('fsdp')
        dev = t * fs + f

        def own(x, n, i, ax):
            k = x.shape[ax] // n
            return lax.dynamic_slice_in_dim(x, i * k, k, ax)
        (gb, g1g, g1b, g2g, g2b, gc2, gfg, gfb, gc1, gt1, gbh, gw1, gw2, ls) = out
        loss = ls[0] / total_images
        return (loss, g_stem, own(gb, nd, dev, 0), own(g1g, nd, dev, 1), own(g1b, nd, dev, 1),
                own(gw1, fs, f, 2), own(gt1, fs, f, 1), own(gw2, fs, f, 1),
                own(g2g, nd, dev, 1), own(g2b, nd, dev, 1), g_ch1, own(gc1, nd, dev, 1),
                g_ch2, own(gc2, nd, dev, 1), own(gfg, nd, dev, 0), own(gfb, nd, dev, 0),
                g_head, own(gbh, tp, t, 0))

    specs = weight_specs()
    return jax.shard_map(step, mesh=mesh, in_specs=(P('fsdp', None, None), P('fsdp')) + specs,
                         out_specs=(P(),) + specs, check_vma=False)
```

```python
import functools

import jax
import jax.numpy as jnp
from jax import lax
from jax.experimental import pallas as pl
from jax.experimental.pallas import tpu as pltpu
from jax.sharding import PartitionSpec as P

MESH = pl.DeviceIdType.MESH
ORDERS = (('x', 'y', 'z'), ('y', 'z', 'x'), ('z', 'x', 'y'))
COLS = ((0, 384), (384, 384), (768, 256))
N_CH = 4
STEM, HEAD = 4, 5
bf16, f32 = jnp.bfloat16, jnp.float32


def my_place():
    f = lax.axis_index('fsdp')
    return {'x': lax.axis_index('tp'), 'z': f // 8, 'y': (f // 2) % 4, 'k': f % 2}


def moved(place, dim, step):
    new = dict(place)
    new[dim] = 1 - place['k'] if dim == 'k' else (place[dim] + step) % 4
    return new


def device(place):
    return {'tp': place['x'], 'fsdp': (place['z'] * 4 + place['y']) * 2 + place['k']}


def meet_neighbours(me):
    barrier = pltpu.get_barrier_semaphore()
    for dim in 'xyz':
        for step in (1, 3):
            pl.semaphore_signal(barrier, inc=1, device_id=device(moved(me, dim, step)), device_id_type=MESH)
    pl.semaphore_signal(barrier, inc=1, device_id=device(moved(me, 'k', 1)), device_id_type=MESH)
    pl.semaphore_wait(barrier, 7)


class Sender:
    def __init__(self, send_sems, recv_sems):
        self.send_sems, self.recv_sems, self.count, self.started = send_sems, recv_sems, 0, []

    def start(self, src, dst, target):
        n = self.count
        self.count += 1
        copy = pltpu.make_async_remote_copy(src_ref=src, dst_ref=dst, send_sem=self.send_sems.at[n],
                                            recv_sem=self.recv_sems.at[n], device_id=device(target),
                                            device_id_type=MESH)
        copy.start()
        self.started.append(copy)
        return copy


GATHER_COPIES = 7 * 8 + 16 * 4 + 16 * 4


def gather_kernel(pc, ps, ph, wc, ws, wh, send_sems, recv_sems, local_sems):
    me = my_place()
    other = moved(me, 'k', 1)
    meet_neighbours(me)
    sender = Sender(send_sems, recv_sems)
    every = pl.ds(0, 4)

    def view(kind, colour, block, half=None, group=None, k=None):
        k = me['k'] if k is None else k
        x, z, y = block['x'], block['z'], block['y']
        r0, rn = (0, 32) if half is None else (16 * half, 16)
        if kind == 'ch':
            c0, cn = COLS[colour]
            return wc.at[every if group is None else group, x, z, y, k, pl.ds(r0, rn), pl.ds(c0, cn)]
        cols = pl.ds(0, 1024) if x is every else pl.ds(pl.multiple_of(x * 256, 256), 256)
        if kind == 'stem':
            return ws.at[z, y, k, pl.ds(32 * colour + r0, rn), cols]
        return wh.at[z, y, k, pl.ds(r0, rn), cols]

    def piece(kind, colour):
        if kind == 'ch':
            c0, cn = COLS[colour]
            return pc.at[:, :, pl.ds(c0, cn)]
        if kind == 'stem':
            return ps.at[pl.ds(32 * colour, 32), :]
        return ph.at[:, :]

    early = [('stem', 0), ('stem', 1), ('stem', 2), ('ch', 0), ('ch', 1), ('ch', 2), ('head', 2)]
    late = [('stem', c, None) for c in range(3)] + [('ch', c, g) for g in range(N_CH) for c in range(3)]
    late += [('head', 2, None)]

    own = [pltpu.make_async_copy(piece(kind, c), view(kind, c, me), local_sems.at[i])
           for i, (kind, c) in enumerate(early)]
    for copy in own:
        copy.start()

    def exchange(unit, dim, block, src=None):
        kind, c = unit[:2]
        g = unit[2] if len(unit) > 2 else None
        mine = view(kind, c, block, group=g)
        source = mine if src is None else src
        return [sender.start(source, mine, moved(me, dim, step)) for step in (1, 3)]

    def forward(unit, dim, block):
        kind, c = unit[:2]
        g = unit[2] if len(unit) > 2 else None
        out = []
        for half, (origin, target) in enumerate(((3, 1), (1, 3))):
            part = view(kind, c, {**block, dim: (me[dim] + origin) % 4}, half=half, group=g)
            out.append(sender.start(part, part, moved(me, dim, target)))
        return out

    def arrived(copies):
        for copy in copies:
            copy.wait_recv()

    first, second, third, swaps = {}, {}, {}, []
    for u in early:
        first[u] = exchange(u, ORDERS[u[1]][0], me, piece(*u))
    for copy in own:
        copy.wait()
    for u in early:
        arrived(first[u])
        first[u] = forward(u, ORDERS[u[1]][0], me)
    for u in early:
        d1, d2, _ = ORDERS[u[1]]
        arrived(first[u])
        second[u] = exchange(u, d2, {**me, d1: every})
    for u in early:
        d1, d2, _ = ORDERS[u[1]]
        arrived(second[u])
        second[u] = forward(u, d2, {**me, d1: every})
    done = set()
    for u in late:
        d1, d2, d3 = ORDERS[u[1]]
        if u[:2] not in done:
            arrived(second[u[:2]])
            done.add(u[:2])
        plane = {**me, d1: every, d2: every}
        third[u] = exchange(u, d3, plane)
        mine = view(u[0], u[1], plane, group=u[2])
        swaps.append(sender.start(mine, mine, other))
    for u in late:
        d1, d2, d3 = ORDERS[u[1]]
        plane = {**me, d1: every, d2: every}
        arrived(third[u])
        third[u] = forward(u, d3, plane)
        for step in (1, 3):
            part = view(u[0], u[1], {**plane, d3: (me[d3] + step) % 4}, group=u[2])
            swaps.append(sender.start(part, part, other))
    for u in late:
        d1, d2, d3 = ORDERS[u[1]]
        plane = {**me, d1: every, d2: every}
        arrived(third[u])
        part = view(u[0], u[1], {**plane, d3: (me[d3] + 2) % 4}, group=u[2])
        swaps.append(sender.start(part, part, other))
    arrived(swaps)
    for copy in sender.started:
        copy.wait_send()
    assert sender.count == GATHER_COPIES, sender.count


def gather_weights(pc, ps, ph):
    any_spec = pl.BlockSpec(memory_space=pl.ANY)
    vmem = pl.BlockSpec(memory_space=pltpu.VMEM)
    return pl.pallas_call(
        gather_kernel, name='gather_weights',
        out_shape=[jax.ShapeDtypeStruct((N_CH, 4, 4, 4, 2, 32, 1024), bf16),
                   jax.ShapeDtypeStruct((4, 4, 2, 96, 1024), bf16),
                   jax.ShapeDtypeStruct((4, 4, 2, 32, 1024), bf16)],
        in_specs=[vmem] * 3, out_specs=[any_spec] * 3,
        scratch_shapes=[pltpu.SemaphoreType.DMA((GATHER_COPIES,)), pltpu.SemaphoreType.DMA((GATHER_COPIES,)),
                        pltpu.SemaphoreType.DMA((7,))],
        compiler_params=pltpu.CompilerParams(collective_id=0, has_side_effects=True),
        cost_estimate=pl.CostEstimate(flops=90_000_000_000, bytes_accessed=80_000_000, transcendentals=0),
    )(pc, ps, ph)


GROUPS = (STEM, 3, 2, 1, 0, HEAD)
UNITS = tuple((g, c) for g in GROUPS for c in (2, 0, 1) if g != HEAD or c == 2)
REDUCE_COPIES = 13 * len(UNITS)


def reduce_scratch():
    per = []
    for c in range(3):
        n = COLS[c][1]
        many = sum(1 for u in UNITS if u[1] == c)
        lead = ((4, 4), (4,), ())
        b = {'C': pltpu.VMEM((4, 4, 4, 2, 32, n), bf16), 'D': pltpu.VMEM((4, 4, 4, 32, n), bf16),
             'S1': pltpu.VMEM((4, 4, 32, n), f32), 'S2': pltpu.VMEM((4, 32, n), f32)}
        for ph in range(3):
            for name in ('opp', 'rig', 'lef'):
                b[f'{name}{ph}'] = pltpu.VMEM(lead[ph] + (32, n), bf16)
            for name in ('half0', 'half1'):
                b[f'{name}{ph}'] = pltpu.VMEM((many,) + lead[ph] + (16, n), bf16)
            for name in ('froml', 'fromr'):
                b[f'{name}{ph}'] = pltpu.VMEM((many,) + lead[ph] + (32, n), bf16)
        per.append(b)
    return per


def transposed_product(left, right):
    return lax.dot_general(left, right, (((0,), (0,)), ((), ())), preferred_element_type=f32)


def reduce_kernel(*refs):
    wides, narrows, (head_l, head_r) = refs[:5], refs[5:10], refs[10:12]
    out_c, out_s, out_h = refs[12:15]
    wide, narrow, per, send_sems, recv_sems, load_sems, credit = refs[15:]
    me = my_place()
    other = moved(me, 'k', 1)
    k = me['k']
    loads = {}

    def load(i):
        g = GROUPS[i]
        if g == HEAD:
            return
        cols = 3072 if g == STEM else 4096
        loads[g] = [pltpu.make_async_copy(wides[g], wide.at[i % 2, :, pl.ds(0, cols)], load_sems.at[i % 2, 0]),
                    pltpu.make_async_copy(narrows[g], narrow.at[i % 2], load_sems.at[i % 2, 1])]
        for copy in loads[g]:
            copy.start()

    load(0)
    meet_neighbours(me)
    sender = Sender(send_sems, recv_sems)
    busy = {}

    def free(key):
        for copy in busy.pop(key, ()):
            copy.wait_send()

    def make(g, c):
        i = GROUPS.index(g)
        slot = i % 2
        if g != HEAD and c == 2:
            for copy in loads[g]:
                copy.wait()
            load(i + 1)
        if g == STEM:
            if c != 2:
                return
            for d in range(3):
                free(('C', d))

            @pl.loop(0, 32)
            def _(j):
                b = j // 4
                t = j % 4
                z, y2 = b // 2, b % 2
                left = wide[slot, :, pl.ds(pl.multiple_of(b * 384, 128), 384)]
                right = narrow[slot, :, pl.ds(pl.multiple_of(t * 256, 128), 256)]
                prod = transposed_product(left, right).astype(bf16).reshape(2, 2, 3, 32, 256)
                for d in range(3):
                    per[d]['C'][t, z, pl.ds(y2 * 2, 2), :, :, pl.ds(0, 256)] = prod[:, :, d]
        elif g == HEAD:
            free(('C', c))

            @pl.loop(0, 4)
            def _(t):
                right = head_r[:, pl.ds(pl.multiple_of(t * 256, 128), 256)]
                prod = transposed_product(head_l[...], right)
                per[c]['C'][t] = prod.astype(bf16).reshape(4, 4, 2, 32, 256)
        else:
            free(('C', c))
            c0, n = COLS[c]

            @pl.loop(0, 16)
            def _(j):
                t, z = j // 4, j % 4
                if g % 2 == 0:
                    left = narrow[slot, :, pl.ds(pl.multiple_of(z * 256, 128), 256)]
                    right = wide[slot, :, pl.ds(pl.multiple_of(t * 1024 + c0, 128), n)]
                else:
                    left = wide[slot, :, pl.ds(pl.multiple_of(j * 256, 128), 256)]
                    right = narrow[slot, :, pl.ds(c0, n)]
                per[c]['C'][t, z] = transposed_product(left, right).astype(bf16).reshape(4, 2, 32, n)

    class Unit:
        def __init__(self, g, c):
            self.g, self.c = g, c
            same = [u for u in UNITS if u[1] == c]
            self.index = same.index((g, c))
            self.last = self.index == len(same) - 1
            self.n = COLS[c][1] if g < N_CH else 256
            self.buf = per[c]
            self.dims = ORDERS[c]

        def cut(self, name, *at):
            ref = self.buf[name]
            rest = len(ref.shape) - len(at) - 1
            return ref.at[(*at, *[slice(None)] * rest, pl.ds(0, self.n))]

        def share(self, phase, p, e, rows):
            r = pl.ds(*rows)
            cols = pl.ds(0, self.n)
            if phase == 0:
                at = dict(zip(self.dims, (p, *e)))
                at = (at['x'], at['z'], at['y'])
                return (self.buf['C'][(*at, k, r, cols)].astype(f32) + self.buf['D'][(*at, r, cols)].astype(f32))
            return self.buf[f'S{phase}'][(p, *e, r, cols)]

        def each(self, phase, body):
            if phase == 2:
                body(())
            elif phase == 1:
                pl.loop(0, 4)(lambda i: body((i,)))
            else:
                pl.loop(0, 16)(lambda i: body((i // 4, i % 4)))

        def start(self):
            make(self.g, self.c)
            if self.index:
                pl.semaphore_wait(credit.at[self.c], 1)
            cols = pl.ds(0, self.n)
            src = self.buf['C'].at[:, :, :, 1 - k, :, cols]
            self.swap = sender.start(src, self.buf['D'].at[:, :, :, :, cols], other)
            busy['C', self.c] = [self.swap]

        def opposite(self, phase):
            if phase == 0:
                self.swap.wait_recv()
            p = (me[self.dims[phase]] + 2) % 4
            free((f'opp{phase}', self.c))
            cols = pl.ds(0, self.n)

            def body(e):
                self.buf[f'opp{phase}'][(*e, slice(None), cols)] = self.share(phase, p, e, (0, 32)).astype(bf16)
            self.each(phase, body)
            lead = [slice(None)] * (2 - phase)
            copies = []
            for half, step in ((0, 1), (1, 3)):
                src = self.buf[f'opp{phase}'].at[(*lead, pl.ds(16 * half, 16), cols)]
                dst = self.cut(f'half{half}{phase}', self.index)
                copies.append(sender.start(src, dst, moved(me, self.dims[phase], step)))
            busy[f'opp{phase}', self.c] = copies
            self.halves = copies

        def beside(self, phase):
            copies = []
            for half, step, name, dst in ((0, 1, 'rig', 'froml'), (1, 3, 'lef', 'fromr')):
                self.halves[half].wait_recv()
                free((f'{name}{phase}', self.c))
                p = (me[self.dims[phase]] + step) % 4
                cols = pl.ds(0, self.n)
                whole, got = self.buf[f'{name}{phase}'], self.buf[f'half{half}{phase}']

                def body(e):
                    mine = self.share(phase, p, e, (16 * half, 16)) + got[(self.index, *e, slice(None), cols)].astype(f32)
                    whole[(*e, pl.ds(16 * half, 16), cols)] = mine.astype(bf16)
                    plain = self.share(phase, p, e, (16 - 16 * half, 16))
                    whole[(*e, pl.ds(16 - 16 * half, 16), cols)] = plain.astype(bf16)
                self.each(phase, body)
                copy = sender.start(self.cut(f'{name}{phase}'), self.cut(f'{dst}{phase}', self.index),
                                    moved(me, self.dims[phase], step))
                busy[f'{name}{phase}', self.c] = [copy]
                copies.append(copy)
            self.wholes = copies

        def total(self, phase):
            for copy in self.wholes:
                copy.wait_recv()
            p = me[self.dims[phase]]
            cols = pl.ds(0, self.n)

            def body(e):
                got = [self.buf[f'{name}{phase}'][(self.index, *e, slice(None), cols)].astype(f32)
                       for name in ('froml', 'fromr')]
                value = self.share(phase, p, e, (0, 32)) + got[0] + got[1]
                if phase < 2:
                    self.buf[f'S{phase + 1}'][(*e, slice(None), cols)] = value
                elif self.g == STEM:
                    out_s[pl.ds(32 * self.c, 32), :] = value
                elif self.g == HEAD:
                    out_h[...] = value
                else:
                    out_c[self.g, :, pl.ds(*COLS[self.c])] = value
            self.each(phase, body)
            if phase == 0 and not self.last:
                pl.semaphore_signal(credit.at[self.c], inc=1, device_id=device(other), device_id_type=MESH)

        def run(self, stage):
            if stage == 0:
                self.start()
            elif stage == 7:
                self.total(2)
            elif stage % 2 == 0:
                self.beside(stage // 2 - 1)
            else:
                if stage > 1:
                    self.total(stage // 2 - 1)
                self.opposite(stage // 2)

    units = [Unit(g, c) for g, c in UNITS]
    for slot in range(len(units) + 7):
        for stage in range(7, -1, -1):
            if 0 <= slot - stage < len(units):
                units[slot - stage].run(stage)
    for key in list(busy):
        free(key)
    assert sender.count == REDUCE_COPIES, sender.count


def reduce_gradients(wides, narrows, head_l, head_r):
    any_spec = pl.BlockSpec(memory_space=pl.ANY)
    vmem = pl.BlockSpec(memory_space=pltpu.VMEM)
    rows = narrows[0].shape[0]
    return pl.pallas_call(
        reduce_kernel, name='reduce_gradients',
        out_shape=[jax.ShapeDtypeStruct((N_CH, 32, 1024), f32), jax.ShapeDtypeStruct((96, 256), f32),
                   jax.ShapeDtypeStruct((32, 256), f32)],
        in_specs=[any_spec] * 10 + [vmem] * 2, out_specs=[vmem] * 3,
        scratch_shapes=[pltpu.VMEM((2, rows, 4096), bf16), pltpu.VMEM((2, rows, 1024), bf16), reduce_scratch(),
                        pltpu.SemaphoreType.DMA((REDUCE_COPIES,)), pltpu.SemaphoreType.DMA((REDUCE_COPIES,)),
                        pltpu.SemaphoreType.DMA((2, 2)), pltpu.SemaphoreType.REGULAR((3,))],
        compiler_params=pltpu.CompilerParams(collective_id=1, has_side_effects=True, vmem_limit_bytes=64 * 1024 * 1024 - 65536),
        cost_estimate=pl.CostEstimate(flops=100_000_000_000, bytes_accessed=80_000_000, transcendentals=0),
    )(*wides, *narrows, head_l, head_r)


EPS = 1e-6
CHANNEL_AXES = ('tp', 'fsdp')


def product(form, left, right):
    return jnp.einsum(form, left, right, preferred_element_type=f32)


def bf(x):
    return x.astype(bf16)


def norm_forward(values, gain, shift):
    mean_val = jnp.mean(values, axis=-1, keepdims=True)
    cent = values - mean_val
    inv_std = lax.rsqrt(jnp.mean(cent * cent, axis=-1, keepdims=True) + EPS)
    standard = cent * inv_std
    return standard * gain + shift, standard, inv_std


def norm_backward(grad_out, gain, standard, inv_std):
    gs = grad_out * gain
    m0 = jnp.mean(gs, axis=-1, keepdims=True)
    m1 = jnp.mean(gs * standard, axis=-1, keepdims=True)
    return inv_std * (gs - m0 - standard * m1)


def gelu_grad(pre_act, grad_out):
    return jax.vjp(jax.nn.gelu, pre_act)[1](grad_out)[0]


def weight_specs():
    vec_spec = P(CHANNEL_AXES)
    layer_vec = P(None, CHANNEL_AXES)
    return (P('fsdp', 'tp'), vec_spec, layer_vec, layer_vec, P(None, None, 'fsdp'), P(None, 'fsdp'),
            P(None, 'fsdp', None), layer_vec, layer_vec, P(None, 'fsdp', 'tp'), layer_vec,
            P(None, CHANNEL_AXES, None), layer_vec, vec_spec, vec_spec, P('fsdp', 'tp'), P('tp'))


def solution(mesh):
    fs = mesh.shape['fsdp']
    tp = mesh.shape['tp']
    nd = fs * tp

    def step(patches, labels, w_stem, b_stem, ln1_g, ln1_b, w_tok1, b_tok1, w_tok2,
             ln2_g, ln2_b, w_ch1, b_ch1, w_ch2, b_ch2, lnf_g, lnf_b, w_head, b_head):
        t = lax.axis_index('tp')
        nl = w_tok1.shape[0]
        bl = patches.shape[0] // tp
        tokens = patches.shape[1]
        rows = bl * tokens
        total_images = bl * nd
        pat = lax.dynamic_slice_in_dim(patches, t * bl, bl, 0)
        pat = pat.transpose(1, 0, 2).reshape(rows, -1)
        lab = lax.dynamic_slice_in_dim(labels, t * bl, bl, 0)

        vecs = [b_stem[None], ln1_g, ln1_b, ln2_g, ln2_b, b_ch2, lnf_g[None], lnf_b[None]]
        vec_rows = jnp.concatenate(vecs, axis=0)
        n_rows = vec_rows.shape[0]
        pieces = [vec_rows.reshape(-1), b_ch1.reshape(-1), b_tok1.reshape(-1), b_head.reshape(-1),
                  w_tok1.reshape(-1), w_tok2.reshape(-1)]
        pack = jnp.concatenate(pieces)
        pack = jnp.pad(pack, (0, (-pack.shape[0]) % 1024))
        small = lax.all_gather(pack, CHANNEL_AXES, axis=0, tiled=False).reshape(tp, fs, -1)
        offs = []
        o = 0
        for p in pieces:
            offs.append(small[:, :, o:o + p.shape[0]])
            o += p.shape[0]
        vec_all = offs[0].reshape(tp, fs, n_rows, -1).transpose(2, 0, 1, 3).reshape(n_rows, -1)
        bch1 = offs[1].reshape(tp, fs, nl, -1).transpose(2, 0, 1, 3).reshape(nl, -1)
        btok1 = offs[2][0].reshape(fs, nl, -1).transpose(1, 0, 2).reshape(nl, -1)
        bhead = offs[3][:, 0]
        wtok1 = bf(offs[4][0].reshape(fs, nl, tokens, -1).transpose(1, 2, 0, 3).reshape(nl, tokens, -1))
        wtok2 = bf(offs[5][0].reshape(fs, nl, -1, tokens).transpose(1, 0, 2, 3).reshape(nl, -1, tokens))
        bstem = vec_all[0]
        l1g, l1b, l2g, l2b, bc2 = [vec_all[1 + nl * i:1 + nl * (i + 1)] for i in range(5)]
        lfg, lfb = vec_all[1 + 5 * nl], vec_all[2 + 5 * nl]

        classes = w_head.shape[1]
        pad_cls = 256 - classes
        pc = jnp.stack([bf(w_ch1[0]), bf(w_ch2[0]), bf(w_ch1[1]), bf(w_ch2[1])])
        ph = jnp.pad(bf(w_head), ((0, 0), (0, pad_cls)))
        wc, ws, wh = gather_weights(pc, bf(w_stem), ph)
        c = w_stem.shape[1] * tp
        ws = ws.reshape(-1, c)
        wh = wh.reshape(c, -1)
        wc = wc.reshape(2 * nl, tp, c, c)
        bhead = jnp.pad(bhead, ((0, 0), (0, pad_cls)), constant_values=-1e30).reshape(-1)
        col = lab // classes * 256 + lab % classes

        resid = product('rp,pc->rc', pat, ws) + bstem
        saved = []
        for l in range(nl):
            normed, n1s, n1i = norm_forward(resid, l1g[l], l1b[l])
            normed = bf(normed).reshape(tokens, bl, c)
            tok_pre = product('sbc,sj->bcj', normed, wtok1[l]) + btok1[l]
            tok_act = bf(jax.nn.gelu(tok_pre))
            resid = resid + product('bcj,js->sbc', tok_act, wtok2[l]).reshape(rows, c)
            normed2, n2s, n2i = norm_forward(resid, l2g[l], l2b[l])
            full_in = bf(normed2)
            ch_pre = [product('rc,cd->rd', full_in, wc[2 * l, i]) + bch1[l, i * c:(i + 1) * c] for i in range(tp)]
            ch_act = [bf(jax.nn.gelu(p)) for p in ch_pre]
            for i in range(tp):
                resid = resid + product('rd,dc->rc', ch_act[i], wc[2 * l + 1, i])
            resid = resid + bc2[l]
            saved.append((normed, n1s, n1i, tok_pre, tok_act, n2s, n2i, full_in, ch_pre, ch_act))

        pooled = jnp.mean(resid.reshape(tokens, bl, c), axis=0)
        head_in, hs, hi = norm_forward(pooled, lfg, lfb)
        head_bf = bf(head_in)
        logits = product('bc,ck->bk', head_bf, wh) + bhead
        is_label = jnp.arange(logits.shape[1])[None, :] == col[:, None]
        row_max = jnp.max(logits, axis=1, keepdims=True)
        ex = jnp.exp(logits - row_max)
        es = jnp.sum(ex, axis=1, keepdims=True)
        log_norm = row_max + jnp.log(es)
        loss_loc = jnp.sum(log_norm) - jnp.sum(jnp.where(is_label, logits, 0.0))

        d_logits = (ex / es - is_label.astype(f32)) / total_images
        dlb = bf(d_logits)
        g_bhead = jnp.sum(d_logits, axis=0)
        d_hin = product('bk,ck->bc', dlb, wh)
        g_lfg = jnp.sum(d_hin * hs, axis=0)
        g_lfb = jnp.sum(d_hin, axis=0)
        d_pooled = norm_backward(d_hin, lfg, hs, hi)
        d_resid = jnp.broadcast_to((d_pooled / tokens)[None], (tokens, bl, c)).reshape(rows, c)

        wides, narrows = [None] * 5, [None] * 5
        sm = {}
        for l in reversed(range(nl)):
            normed, n1s, n1i, tok_pre, tok_act, n2s, n2i, full_in, ch_pre, ch_act = saved[l]
            sm['b_ch2', l] = jnp.sum(d_resid, axis=0)
            dob = bf(d_resid)
            wides[2 * l + 1], narrows[2 * l + 1] = jnp.concatenate(ch_act, axis=1), dob
            d_pre = [gelu_grad(ch_pre[i], product('rc,dc->rd', dob, wc[2 * l + 1, i])) for i in range(tp)]
            sm['b_ch1', l] = jnp.concatenate([jnp.sum(d, axis=0) for d in d_pre])
            dpb = [bf(d) for d in d_pre]
            wides[2 * l], narrows[2 * l] = jnp.concatenate(dpb, axis=1), full_in
            d_n2 = sum(product('rd,cd->rc', dpb[i], wc[2 * l, i]) for i in range(tp))
            sm['ln2_g', l] = jnp.sum(d_n2 * n2s, axis=0)
            sm['ln2_b', l] = jnp.sum(d_n2, axis=0)
            d_mid = d_resid + norm_backward(d_n2, l2g[l], n2s, n2i)
            dmb = bf(d_mid).reshape(tokens, bl, c)
            sm['w_tok2', l] = product('bcj,sbc->js', tok_act, dmb)
            d_tp = gelu_grad(tok_pre, product('sbc,js->bcj', dmb, wtok2[l]))
            sm['b_tok1', l] = jnp.sum(d_tp, axis=(0, 1))
            dtb = bf(d_tp)
            sm['w_tok1', l] = product('sbc,bcj->sj', normed, dtb)
            d_n1 = product('bcj,sj->sbc', dtb, wtok1[l]).reshape(rows, c)
            sm['ln1_g', l] = jnp.sum(d_n1 * n1s, axis=0)
            sm['ln1_b', l] = jnp.sum(d_n1, axis=0)
            d_resid = d_mid + norm_backward(d_n1, l1g[l], n1s, n1i)
        g_bstem = jnp.sum(d_resid, axis=0)
        wides[4], narrows[4] = pat, bf(d_resid)

        def st(key):
            return jnp.stack([sm[key, l] for l in range(nl)])
        parts = [g_bstem, st('ln1_g'), st('ln1_b'), st('ln2_g'), st('ln2_b'), st('b_ch2'), g_lfg, g_lfb,
                 st('b_ch1'), st('b_tok1'), g_bhead, st('w_tok1'), st('w_tok2'), loss_loc[None]]
        flat = jnp.concatenate([p.reshape(-1) for p in parts])
        flat = jnp.pad(flat, (0, (-flat.shape[0]) % 1024))
        tot = lax.psum(flat, CHANNEL_AXES)

        g_c, g_s, g_h = reduce_gradients(wides, narrows, head_bf, dlb)
        g_ch1, g_ch2 = g_c[0::2], g_c[1::2]
        g_head = g_h[:, :classes]

        out = []
        o = 0
        for p in parts:
            out.append(tot[o:o + p.size].reshape(p.shape))
            o += p.size
        f = lax.axis_index('fsdp')
        dev = t * fs + f

        def own(x, n, i, ax):
            size = x.shape[ax] // n
            return lax.dynamic_slice_in_dim(x, i * size, size, ax)
        (gb, g1g, g1b, g2g, g2b, gc2, gfg, gfb, gc1, gt1, gbh, gw1, gw2, ls) = out
        loss = ls[0] / total_images
        return (loss, g_s, own(gb, nd, dev, 0), own(g1g, nd, dev, 1), own(g1b, nd, dev, 1),
                own(gw1, fs, f, 2), own(gt1, fs, f, 1), own(gw2, fs, f, 1),
                own(g2g, nd, dev, 1), own(g2b, nd, dev, 1), g_ch1, own(gc1, nd, dev, 1),
                g_ch2, own(gc2, nd, dev, 1), own(gfg, nd, dev, 0), own(gfb, nd, dev, 0),
                g_head, own(gbh.reshape(tp, 256), tp, t, 0)[0, :classes])

    specs = weight_specs()
    return jax.shard_map(step, mesh=mesh, in_specs=(P('fsdp', None, None), P('fsdp')) + specs,
                         out_specs=(P(),) + specs, check_vma=False)
```

```python
import functools

import jax
import jax.numpy as jnp
from jax import lax
from jax.experimental import pallas as pl
from jax.experimental.pallas import tpu as pltpu
from jax.sharding import PartitionSpec as P

MESH = pl.DeviceIdType.MESH
ORDERS = (('x', 'y', 'z'), ('y', 'z', 'x'), ('z', 'x', 'y'))
COLS = ((0, 384), (384, 384), (768, 256))
N_CH = 4
STEM, HEAD = 4, 5
bf16, f32 = jnp.bfloat16, jnp.float32


def my_place():
    f = lax.axis_index('fsdp')
    return {'x': lax.axis_index('tp'), 'z': f // 8, 'y': (f // 2) % 4, 'k': f % 2}


def moved(place, dim, step):
    new = dict(place)
    new[dim] = 1 - place['k'] if dim == 'k' else (place[dim] + step) % 4
    return new


def device(place):
    return {'tp': place['x'], 'fsdp': (place['z'] * 4 + place['y']) * 2 + place['k']}


def meet_neighbours(me):
    barrier = pltpu.get_barrier_semaphore()
    for dim in 'xyz':
        for step in (1, 3):
            pl.semaphore_signal(barrier, inc=1, device_id=device(moved(me, dim, step)), device_id_type=MESH)
    pl.semaphore_signal(barrier, inc=1, device_id=device(moved(me, 'k', 1)), device_id_type=MESH)
    pl.semaphore_wait(barrier, 7)


class Sender:
    def __init__(self, send_sems, recv_sems):
        self.send_sems, self.recv_sems, self.count, self.started = send_sems, recv_sems, 0, []

    def start(self, src, dst, target):
        n = self.count
        self.count += 1
        copy = pltpu.make_async_remote_copy(src_ref=src, dst_ref=dst, send_sem=self.send_sems.at[n],
                                            recv_sem=self.recv_sems.at[n], device_id=device(target),
                                            device_id_type=MESH)
        copy.start()
        self.started.append(copy)
        return copy


GATHER_COPIES = 7 * 8 + 16 * 4 + 16 * 4


def gather_kernel(pc, ps, ph, wc, ws, wh, send_sems, recv_sems, local_sems):
    me = my_place()
    other = moved(me, 'k', 1)
    meet_neighbours(me)
    sender = Sender(send_sems, recv_sems)
    every = pl.ds(0, 4)

    def view(kind, colour, block, half=None, group=None, k=None):
        k = me['k'] if k is None else k
        x, z, y = block['x'], block['z'], block['y']
        r0, rn = (0, 32) if half is None else (16 * half, 16)
        if kind == 'ch':
            c0, cn = COLS[colour]
            return wc.at[every if group is None else group, x, z, y, k, pl.ds(r0, rn), pl.ds(c0, cn)]
        cols = pl.ds(0, 1024) if x is every else pl.ds(pl.multiple_of(x * 256, 256), 256)
        if kind == 'stem':
            return ws.at[z, y, k, pl.ds(32 * colour + r0, rn), cols]
        return wh.at[z, y, k, pl.ds(r0, rn), cols]

    def piece(kind, colour):
        if kind == 'ch':
            c0, cn = COLS[colour]
            return pc.at[:, :, pl.ds(c0, cn)]
        if kind == 'stem':
            return ps.at[pl.ds(32 * colour, 32), :]
        return ph.at[:, :]

    early = [('stem', 0), ('stem', 1), ('stem', 2), ('ch', 0), ('ch', 1), ('ch', 2), ('head', 2)]
    late = [('stem', c, None) for c in range(3)] + [('ch', c, g) for g in range(N_CH) for c in range(3)]
    late += [('head', 2, None)]

    own = [pltpu.make_async_copy(piece(kind, c), view(kind, c, me), local_sems.at[i])
           for i, (kind, c) in enumerate(early)]
    for copy in own:
        copy.start()

    def exchange(unit, dim, block, src=None):
        kind, c = unit[:2]
        g = unit[2] if len(unit) > 2 else None
        mine = view(kind, c, block, group=g)
        source = mine if src is None else src
        return [sender.start(source, mine, moved(me, dim, step)) for step in (1, 3)]

    def forward(unit, dim, block):
        kind, c = unit[:2]
        g = unit[2] if len(unit) > 2 else None
        out = []
        for half, (origin, target) in enumerate(((3, 1), (1, 3))):
            part = view(kind, c, {**block, dim: (me[dim] + origin) % 4}, half=half, group=g)
            out.append(sender.start(part, part, moved(me, dim, target)))
        return out

    def arrived(copies):
        for copy in copies:
            copy.wait_recv()

    first, second, third, swaps = {}, {}, {}, []
    for u in early:
        first[u] = exchange(u, ORDERS[u[1]][0], me, piece(*u))
    for copy in own:
        copy.wait()
    for u in early:
        arrived(first[u])
        first[u] = forward(u, ORDERS[u[1]][0], me)
    for u in early:
        d1, d2, _ = ORDERS[u[1]]
        arrived(first[u])
        second[u] = exchange(u, d2, {**me, d1: every})
    for u in early:
        d1, d2, _ = ORDERS[u[1]]
        arrived(second[u])
        second[u] = forward(u, d2, {**me, d1: every})
    done = set()
    for u in late:
        d1, d2, d3 = ORDERS[u[1]]
        if u[:2] not in done:
            arrived(second[u[:2]])
            done.add(u[:2])
        plane = {**me, d1: every, d2: every}
        third[u] = exchange(u, d3, plane)
        mine = view(u[0], u[1], plane, group=u[2])
        swaps.append(sender.start(mine, mine, other))
    for u in late:
        d1, d2, d3 = ORDERS[u[1]]
        plane = {**me, d1: every, d2: every}
        arrived(third[u])
        third[u] = forward(u, d3, plane)
        for step in (1, 3):
            part = view(u[0], u[1], {**plane, d3: (me[d3] + step) % 4}, group=u[2])
            swaps.append(sender.start(part, part, other))
    for u in late:
        d1, d2, d3 = ORDERS[u[1]]
        plane = {**me, d1: every, d2: every}
        arrived(third[u])
        part = view(u[0], u[1], {**plane, d3: (me[d3] + 2) % 4}, group=u[2])
        swaps.append(sender.start(part, part, other))
    arrived(swaps)
    for copy in sender.started:
        copy.wait_send()
    assert sender.count == GATHER_COPIES, sender.count


def gather_weights(pc, ps, ph):
    any_spec = pl.BlockSpec(memory_space=pl.ANY)
    vmem = pl.BlockSpec(memory_space=pltpu.VMEM)
    return pl.pallas_call(
        gather_kernel, name='gather_weights',
        out_shape=[jax.ShapeDtypeStruct((N_CH, 4, 4, 4, 2, 32, 1024), bf16),
                   jax.ShapeDtypeStruct((4, 4, 2, 96, 1024), bf16),
                   jax.ShapeDtypeStruct((4, 4, 2, 32, 1024), bf16)],
        in_specs=[vmem] * 3, out_specs=[any_spec] * 3,
        scratch_shapes=[pltpu.SemaphoreType.DMA((GATHER_COPIES,)), pltpu.SemaphoreType.DMA((GATHER_COPIES,)),
                        pltpu.SemaphoreType.DMA((7,))],
        compiler_params=pltpu.CompilerParams(collective_id=0, has_side_effects=True),
        cost_estimate=pl.CostEstimate(flops=90_000_000_000, bytes_accessed=80_000_000, transcendentals=0),
    )(pc, ps, ph)


GROUPS = (STEM, 3, 2, 1, 0, HEAD)
UNITS = tuple((g, c) for g in GROUPS for c in (2, 0, 1) if g != HEAD or c == 2)
REDUCE_COPIES = 13 * len(UNITS)
ORDER = (0, 1, 2, 3, 4, 0, 5, 1, 2, 0, 3, 1, 2, 0, 4, 6, 3, 1, 7, 5, 0, 6, 4, 1, 2, 8, 0, 6, 7, 5, 2, 3, 1, 9, 0, 8, 4, 10, 7, 9, 1, 2,
         3, 0, 5, 11, 8, 9, 10, 1, 4, 5, 2, 11, 3, 6, 12, 10, 2, 5, 8, 6, 4, 7, 13, 11, 12, 3, 4, 7, 8, 14, 5, 12, 6, 13, 4, 9,
         15, 5, 8, 11, 3, 14, 13, 6, 7, 8, 9, 10, 11, 15, 7, 14, 6, 11, 10, 15, 7, 8, 9, 12, 11, 12, 14, 11, 10, 9, 13, 12, 15,
         14, 10, 9, 13, 12, 15, 14, 10, 13, 15, 12, 14, 13, 15, 14, 15, 13)


def reduce_scratch():
    per = []
    for c in range(3):
        n = COLS[c][1]
        many = sum(1 for u in UNITS if u[1] == c)
        lead = ((4, 4), (4,), ())
        b = {'C': pltpu.VMEM((2, 4, 4, 4, 2, 32, n), bf16), 'D': pltpu.VMEM((2, 4, 4, 4, 32, n), bf16),
             'S1': pltpu.VMEM((4, 4, 32, n), f32), 'S2': pltpu.VMEM((3, 4, 32, n), f32)}
        for ph in range(3):
            for name in ('opp', 'rig', 'lef'):
                b[f'{name}{ph}'] = pltpu.VMEM(lead[ph] + (32, n), bf16)
            for name in ('half0', 'half1'):
                b[f'{name}{ph}'] = pltpu.VMEM((many,) + lead[ph] + (16, n), bf16)
            for name in ('froml', 'fromr'):
                b[f'{name}{ph}'] = pltpu.VMEM((many,) + lead[ph] + (32, n), bf16)
        per.append(b)
    return per


def transposed_product(left, right):
    return lax.dot_general(left, right, (((0,), (0,)), ((), ())), preferred_element_type=f32)


def reduce_kernel(*refs):
    wides, narrows, (head_l, head_r) = refs[:5], refs[5:10], refs[10:12]
    out_c, out_s, out_h = refs[12:15]
    wide, narrow, per, send_sems, recv_sems, load_sems, credit = refs[15:]
    me = my_place()
    other = moved(me, 'k', 1)
    k = me['k']
    loads = {}

    def load(i):
        g = GROUPS[i]
        if g == HEAD:
            return
        cols = 3072 if g == STEM else 4096
        loads[g] = [pltpu.make_async_copy(wides[g], wide.at[i % 2, :, pl.ds(0, cols)], load_sems.at[i % 2, 0]),
                    pltpu.make_async_copy(narrows[g], narrow.at[i % 2], load_sems.at[i % 2, 1])]
        for copy in loads[g]:
            copy.start()

    load(0)
    meet_neighbours(me)
    sender = Sender(send_sems, recv_sems)
    busy = {}

    def free(key):
        for copy in busy.pop(key, ()):
            copy.wait_send()

    def make(g, c, cslot):
        i = GROUPS.index(g)
        slot = i % 2
        if g != HEAD and c == 2:
            for copy in loads[g]:
                copy.wait()
            load(i + 1)
        if g == STEM:
            if c != 2:
                return
            @pl.loop(0, 32)
            def _(j):
                b = j // 4
                t = j % 4
                z, y2 = b // 2, b % 2
                left = wide[slot, :, pl.ds(pl.multiple_of(b * 384, 128), 384)]
                right = narrow[slot, :, pl.ds(pl.multiple_of(t * 256, 128), 256)]
                prod = transposed_product(left, right).astype(bf16).reshape(2, 2, 3, 32, 256)
                for d in range(3):
                    per[d]['C'][0, t, z, pl.ds(y2 * 2, 2), :, :, pl.ds(0, 256)] = prod[:, :, d]
        elif g == HEAD:

            @pl.loop(0, 4)
            def _(t):
                right = head_r[:, pl.ds(pl.multiple_of(t * 256, 128), 256)]
                prod = transposed_product(head_l[...], right)
                per[c]['C'][cslot, t] = prod.astype(bf16).reshape(4, 4, 2, 32, 256)
        else:
            c0, n = COLS[c]

            @pl.loop(0, 16)
            def _(j):
                t, z = j // 4, j % 4
                if g % 2 == 0:
                    left = narrow[slot, :, pl.ds(pl.multiple_of(z * 256, 128), 256)]
                    right = wide[slot, :, pl.ds(pl.multiple_of(t * 1024 + c0, 128), n)]
                else:
                    left = wide[slot, :, pl.ds(pl.multiple_of(j * 256, 128), 256)]
                    right = narrow[slot, :, pl.ds(c0, n)]
                per[c]['C'][cslot, t, z] = transposed_product(left, right).astype(bf16).reshape(4, 2, 32, n)

    class Unit:
        def __init__(self, g, c):
            self.g, self.c = g, c
            same = [u for u in UNITS if u[1] == c]
            self.index = same.index((g, c))
            self.slot = self.index % 2
            self.last = self.index >= len(same) - 2
            self.n = COLS[c][1] if g < N_CH else 256
            self.buf = per[c]
            self.dims = ORDERS[c]

        def cut(self, name, *at):
            ref = self.buf[name]
            rest = len(ref.shape) - len(at) - 1
            return ref.at[(*at, *[slice(None)] * rest, pl.ds(0, self.n))]

        def share(self, phase, p, e, rows):
            r = pl.ds(*rows)
            cols = pl.ds(0, self.n)
            if phase == 0:
                at = dict(zip(self.dims, (p, *e)))
                at = (at['x'], at['z'], at['y'])
                return (self.buf['C'][(self.slot, *at, k, r, cols)].astype(f32)
                        + self.buf['D'][(self.slot, *at, r, cols)].astype(f32))
            lead = () if phase == 1 else (self.index % 3,)
            return self.buf[f'S{phase}'][(*lead, p, *e, r, cols)]

        def each(self, phase, body):
            if phase == 2:
                body(())
            elif phase == 1:
                pl.loop(0, 4)(lambda i: body((i,)))
            else:
                pl.loop(0, 16)(lambda i: body((i // 4, i % 4)))

        def start(self):
            free(('C', self.c, self.slot))
            make(self.g, self.c, self.slot)
            if self.index > 1:
                pl.semaphore_wait(credit.at[self.c], 1)
            cols = pl.ds(0, self.n)
            src = self.buf['C'].at[self.slot, :, :, :, 1 - k, :, cols]
            self.swap = sender.start(src, self.buf['D'].at[self.slot, :, :, :, :, cols], other)
            busy['C', self.c, self.slot] = [self.swap]

        def opposite(self, phase):
            if phase == 0:
                self.swap.wait_recv()
            p = (me[self.dims[phase]] + 2) % 4
            free((f'opp{phase}', self.c))
            cols = pl.ds(0, self.n)

            def body(e):
                self.buf[f'opp{phase}'][(*e, slice(None), cols)] = self.share(phase, p, e, (0, 32)).astype(bf16)
            self.each(phase, body)
            lead = [slice(None)] * (2 - phase)
            copies = []
            for half, step in ((0, 1), (1, 3)):
                src = self.buf[f'opp{phase}'].at[(*lead, pl.ds(16 * half, 16), cols)]
                dst = self.cut(f'half{half}{phase}', self.index)
                copies.append(sender.start(src, dst, moved(me, self.dims[phase], step)))
            busy[f'opp{phase}', self.c] = copies
            self.halves = copies

        def beside(self, phase):
            copies = []
            for half, step, name, dst in ((0, 1, 'rig', 'froml'), (1, 3, 'lef', 'fromr')):
                self.halves[half].wait_recv()
                free((f'{name}{phase}', self.c))
                p = (me[self.dims[phase]] + step) % 4
                cols = pl.ds(0, self.n)
                whole, got = self.buf[f'{name}{phase}'], self.buf[f'half{half}{phase}']

                def body(e):
                    mine = self.share(phase, p, e, (16 * half, 16)) + got[(self.index, *e, slice(None), cols)].astype(f32)
                    whole[(*e, pl.ds(16 * half, 16), cols)] = mine.astype(bf16)
                    plain = self.share(phase, p, e, (16 - 16 * half, 16))
                    whole[(*e, pl.ds(16 - 16 * half, 16), cols)] = plain.astype(bf16)
                self.each(phase, body)
                copy = sender.start(self.cut(f'{name}{phase}'), self.cut(f'{dst}{phase}', self.index),
                                    moved(me, self.dims[phase], step))
                busy[f'{name}{phase}', self.c] = [copy]
                copies.append(copy)
            self.wholes = copies

        def total(self, phase):
            for copy in self.wholes:
                copy.wait_recv()
            p = me[self.dims[phase]]
            cols = pl.ds(0, self.n)

            def body(e):
                got = [self.buf[f'{name}{phase}'][(self.index, *e, slice(None), cols)].astype(f32)
                       for name in ('froml', 'fromr')]
                value = self.share(phase, p, e, (0, 32)) + got[0] + got[1]
                if phase == 0:
                    self.buf['S1'][(*e, slice(None), cols)] = value
                elif phase == 1:
                    self.buf['S2'][(self.index % 3, *e, slice(None), cols)] = value
                elif self.g == STEM:
                    out_s[pl.ds(32 * self.c, 32), :] = value
                elif self.g == HEAD:
                    out_h[...] = value
                else:
                    out_c[self.g, :, pl.ds(*COLS[self.c])] = value
            self.each(phase, body)
            if phase == 0 and not self.last:
                pl.semaphore_signal(credit.at[self.c], inc=1, device_id=device(other), device_id_type=MESH)

        def run(self, stage):
            if stage == 0:
                self.start()
            elif stage == 7:
                self.total(2)
            elif stage % 2 == 0:
                self.beside(stage // 2 - 1)
            else:
                if stage > 1:
                    self.total(stage // 2 - 1)
                self.opposite(stage // 2)

    units = [Unit(g, c) for g, c in UNITS]
    stage_of = [0] * len(units)
    for u in ORDER:
        units[u].run(stage_of[u])
        stage_of[u] += 1
    assert stage_of == [8] * len(units)
    for key in list(busy):
        free(key)
    assert sender.count == REDUCE_COPIES, sender.count


def reduce_gradients(wides, narrows, head_l, head_r):
    any_spec = pl.BlockSpec(memory_space=pl.ANY)
    vmem = pl.BlockSpec(memory_space=pltpu.VMEM)
    rows = narrows[0].shape[0]
    return pl.pallas_call(
        reduce_kernel, name='reduce_gradients',
        out_shape=[jax.ShapeDtypeStruct((N_CH, 32, 1024), f32), jax.ShapeDtypeStruct((96, 256), f32),
                   jax.ShapeDtypeStruct((32, 256), f32)],
        in_specs=[any_spec] * 10 + [vmem] * 2, out_specs=[vmem] * 3,
        scratch_shapes=[pltpu.VMEM((2, rows, 4096), bf16), pltpu.VMEM((2, rows, 1024), bf16), reduce_scratch(),
                        pltpu.SemaphoreType.DMA((REDUCE_COPIES,)), pltpu.SemaphoreType.DMA((REDUCE_COPIES,)),
                        pltpu.SemaphoreType.DMA((2, 2)), pltpu.SemaphoreType.REGULAR((3,))],
        compiler_params=pltpu.CompilerParams(collective_id=1, has_side_effects=True, vmem_limit_bytes=64 * 1024 * 1024 - 65536),
        cost_estimate=pl.CostEstimate(flops=100_000_000_000, bytes_accessed=80_000_000, transcendentals=0),
    )(*wides, *narrows, head_l, head_r)


EPS = 1e-6
CHANNEL_AXES = ('tp', 'fsdp')


def product(form, left, right):
    return jnp.einsum(form, left, right, preferred_element_type=f32)


def bf(x):
    return x.astype(bf16)


def norm_forward(values, gain, shift):
    mean_val = jnp.mean(values, axis=-1, keepdims=True)
    cent = values - mean_val
    inv_std = lax.rsqrt(jnp.mean(cent * cent, axis=-1, keepdims=True) + EPS)
    standard = cent * inv_std
    return standard * gain + shift, standard, inv_std


def norm_backward(grad_out, gain, standard, inv_std):
    gs = grad_out * gain
    m0 = jnp.mean(gs, axis=-1, keepdims=True)
    m1 = jnp.mean(gs * standard, axis=-1, keepdims=True)
    return inv_std * (gs - m0 - standard * m1)


def gelu_grad(pre_act, grad_out):
    return jax.vjp(jax.nn.gelu, pre_act)[1](grad_out)[0]


def weight_specs():
    vec_spec = P(CHANNEL_AXES)
    layer_vec = P(None, CHANNEL_AXES)
    return (P('fsdp', 'tp'), vec_spec, layer_vec, layer_vec, P(None, None, 'fsdp'), P(None, 'fsdp'),
            P(None, 'fsdp', None), layer_vec, layer_vec, P(None, 'fsdp', 'tp'), layer_vec,
            P(None, CHANNEL_AXES, None), layer_vec, vec_spec, vec_spec, P('fsdp', 'tp'), P('tp'))


def solution(mesh):
    fs = mesh.shape['fsdp']
    tp = mesh.shape['tp']
    nd = fs * tp

    def step(patches, labels, w_stem, b_stem, ln1_g, ln1_b, w_tok1, b_tok1, w_tok2,
             ln2_g, ln2_b, w_ch1, b_ch1, w_ch2, b_ch2, lnf_g, lnf_b, w_head, b_head):
        t = lax.axis_index('tp')
        nl = w_tok1.shape[0]
        bl = patches.shape[0] // tp
        tokens = patches.shape[1]
        rows = bl * tokens
        total_images = bl * nd
        pat = lax.dynamic_slice_in_dim(patches, t * bl, bl, 0)
        pat = pat.transpose(1, 0, 2).reshape(rows, -1)
        lab = lax.dynamic_slice_in_dim(labels, t * bl, bl, 0)

        vecs = [b_stem[None], ln1_g, ln1_b, ln2_g, ln2_b, b_ch2, lnf_g[None], lnf_b[None]]
        vec_rows = jnp.concatenate(vecs, axis=0)
        n_rows = vec_rows.shape[0]
        pieces = [vec_rows.reshape(-1), b_ch1.reshape(-1), b_tok1.reshape(-1), b_head.reshape(-1),
                  w_tok1.reshape(-1), w_tok2.reshape(-1)]
        pack = jnp.concatenate(pieces)
        pack = jnp.pad(pack, (0, (-pack.shape[0]) % 1024))
        small = lax.all_gather(pack, CHANNEL_AXES, axis=0, tiled=False).reshape(tp, fs, -1)
        offs = []
        o = 0
        for p in pieces:
            offs.append(small[:, :, o:o + p.shape[0]])
            o += p.shape[0]
        vec_all = offs[0].reshape(tp, fs, n_rows, -1).transpose(2, 0, 1, 3).reshape(n_rows, -1)
        bch1 = offs[1].reshape(tp, fs, nl, -1).transpose(2, 0, 1, 3).reshape(nl, -1)
        btok1 = offs[2][0].reshape(fs, nl, -1).transpose(1, 0, 2).reshape(nl, -1)
        bhead = offs[3][:, 0]
        wtok1 = bf(offs[4][0].reshape(fs, nl, tokens, -1).transpose(1, 2, 0, 3).reshape(nl, tokens, -1))
        wtok2 = bf(offs[5][0].reshape(fs, nl, -1, tokens).transpose(1, 0, 2, 3).reshape(nl, -1, tokens))
        bstem = vec_all[0]
        l1g, l1b, l2g, l2b, bc2 = [vec_all[1 + nl * i:1 + nl * (i + 1)] for i in range(5)]
        lfg, lfb = vec_all[1 + 5 * nl], vec_all[2 + 5 * nl]

        classes = w_head.shape[1]
        pad_cls = 256 - classes
        pc = jnp.stack([bf(w_ch1[0]), bf(w_ch2[0]), bf(w_ch1[1]), bf(w_ch2[1])])
        ph = jnp.pad(bf(w_head), ((0, 0), (0, pad_cls)))
        wc, ws, wh = gather_weights(pc, bf(w_stem), ph)
        c = w_stem.shape[1] * tp
        ws = ws.reshape(-1, c)
        wh = wh.reshape(c, -1)
        wc = wc.reshape(2 * nl, tp, c, c)
        bhead = jnp.pad(bhead, ((0, 0), (0, pad_cls)), constant_values=-1e30).reshape(-1)
        col = lab // classes * 256 + lab % classes

        resid = product('rp,pc->rc', pat, ws) + bstem
        saved = []
        for l in range(nl):
            normed, n1s, n1i = norm_forward(resid, l1g[l], l1b[l])
            normed = bf(normed).reshape(tokens, bl, c)
            tok_pre = product('sbc,sj->bcj', normed, wtok1[l]) + btok1[l]
            tok_act = bf(jax.nn.gelu(tok_pre))
            resid = resid + product('bcj,js->sbc', tok_act, wtok2[l]).reshape(rows, c)
            normed2, n2s, n2i = norm_forward(resid, l2g[l], l2b[l])
            full_in = bf(normed2)
            ch_pre = [product('rc,cd->rd', full_in, wc[2 * l, i]) + bch1[l, i * c:(i + 1) * c] for i in range(tp)]
            ch_act = [bf(jax.nn.gelu(p)) for p in ch_pre]
            for i in range(tp):
                resid = resid + product('rd,dc->rc', ch_act[i], wc[2 * l + 1, i])
            resid = resid + bc2[l]
            saved.append((normed, n1s, n1i, tok_pre, tok_act, n2s, n2i, full_in, ch_pre, ch_act))

        pooled = jnp.mean(resid.reshape(tokens, bl, c), axis=0)
        head_in, hs, hi = norm_forward(pooled, lfg, lfb)
        head_bf = bf(head_in)
        logits = product('bc,ck->bk', head_bf, wh) + bhead
        is_label = jnp.arange(logits.shape[1])[None, :] == col[:, None]
        row_max = jnp.max(logits, axis=1, keepdims=True)
        ex = jnp.exp(logits - row_max)
        es = jnp.sum(ex, axis=1, keepdims=True)
        log_norm = row_max + jnp.log(es)
        loss_loc = jnp.sum(log_norm) - jnp.sum(jnp.where(is_label, logits, 0.0))

        d_logits = (ex / es - is_label.astype(f32)) / total_images
        dlb = bf(d_logits)
        g_bhead = jnp.sum(d_logits, axis=0)
        d_hin = product('bk,ck->bc', dlb, wh)
        g_lfg = jnp.sum(d_hin * hs, axis=0)
        g_lfb = jnp.sum(d_hin, axis=0)
        d_pooled = norm_backward(d_hin, lfg, hs, hi)
        d_resid = jnp.broadcast_to((d_pooled / tokens)[None], (tokens, bl, c)).reshape(rows, c)

        wides, narrows = [None] * 5, [None] * 5
        sm = {}
        for l in reversed(range(nl)):
            normed, n1s, n1i, tok_pre, tok_act, n2s, n2i, full_in, ch_pre, ch_act = saved[l]
            sm['b_ch2', l] = jnp.sum(d_resid, axis=0)
            dob = bf(d_resid)
            wides[2 * l + 1], narrows[2 * l + 1] = jnp.concatenate(ch_act, axis=1), dob
            d_pre = [gelu_grad(ch_pre[i], product('rc,dc->rd', dob, wc[2 * l + 1, i])) for i in range(tp)]
            sm['b_ch1', l] = jnp.concatenate([jnp.sum(d, axis=0) for d in d_pre])
            dpb = [bf(d) for d in d_pre]
            wides[2 * l], narrows[2 * l] = jnp.concatenate(dpb, axis=1), full_in
            d_n2 = sum(product('rd,cd->rc', dpb[i], wc[2 * l, i]) for i in range(tp))
            sm['ln2_g', l] = jnp.sum(d_n2 * n2s, axis=0)
            sm['ln2_b', l] = jnp.sum(d_n2, axis=0)
            d_mid = d_resid + norm_backward(d_n2, l2g[l], n2s, n2i)
            dmb = bf(d_mid).reshape(tokens, bl, c)
            sm['w_tok2', l] = product('bcj,sbc->js', tok_act, dmb)
            d_tp = gelu_grad(tok_pre, product('sbc,js->bcj', dmb, wtok2[l]))
            sm['b_tok1', l] = jnp.sum(d_tp, axis=(0, 1))
            dtb = bf(d_tp)
            sm['w_tok1', l] = product('sbc,bcj->sj', normed, dtb)
            d_n1 = product('bcj,sj->sbc', dtb, wtok1[l]).reshape(rows, c)
            sm['ln1_g', l] = jnp.sum(d_n1 * n1s, axis=0)
            sm['ln1_b', l] = jnp.sum(d_n1, axis=0)
            d_resid = d_mid + norm_backward(d_n1, l1g[l], n1s, n1i)
        g_bstem = jnp.sum(d_resid, axis=0)
        wides[4], narrows[4] = pat, bf(d_resid)

        def st(key):
            return jnp.stack([sm[key, l] for l in range(nl)])
        parts = [g_bstem, st('ln1_g'), st('ln1_b'), st('ln2_g'), st('ln2_b'), st('b_ch2'), g_lfg, g_lfb,
                 st('b_ch1'), st('b_tok1'), g_bhead, st('w_tok1'), st('w_tok2'), loss_loc[None]]
        flat = jnp.concatenate([p.reshape(-1) for p in parts])
        flat = jnp.pad(flat, (0, (-flat.shape[0]) % 1024))
        tot = lax.psum(flat, CHANNEL_AXES)

        g_c, g_s, g_h = reduce_gradients(wides, narrows, head_bf, dlb)
        g_ch1, g_ch2 = g_c[0::2], g_c[1::2]
        g_head = g_h[:, :classes]

        out = []
        o = 0
        for p in parts:
            out.append(tot[o:o + p.size].reshape(p.shape))
            o += p.size
        f = lax.axis_index('fsdp')
        dev = t * fs + f

        def own(x, n, i, ax):
            size = x.shape[ax] // n
            return lax.dynamic_slice_in_dim(x, i * size, size, ax)
        (gb, g1g, g1b, g2g, g2b, gc2, gfg, gfb, gc1, gt1, gbh, gw1, gw2, ls) = out
        loss = ls[0] / total_images
        return (loss, g_s, own(gb, nd, dev, 0), own(g1g, nd, dev, 1), own(g1b, nd, dev, 1),
                own(gw1, fs, f, 2), own(gt1, fs, f, 1), own(gw2, fs, f, 1),
                own(g2g, nd, dev, 1), own(g2b, nd, dev, 1), g_ch1, own(gc1, nd, dev, 1),
                g_ch2, own(gc2, nd, dev, 1), own(gfg, nd, dev, 0), own(gfb, nd, dev, 0),
                g_head, own(gbh.reshape(tp, 256), tp, t, 0)[0, :classes])

    specs = weight_specs()
    return jax.shard_map(step, mesh=mesh, in_specs=(P('fsdp', None, None), P('fsdp')) + specs,
                         out_specs=(P(),) + specs, check_vma=False)
```

```python
import functools

import jax
import jax.numpy as jnp
from jax import lax
from jax.experimental import pallas as pl
from jax.experimental.pallas import tpu as pltpu
from jax.sharding import PartitionSpec as P

MESH = pl.DeviceIdType.MESH
ORDERS = (('x', 'y', 'z'), ('y', 'z', 'x'), ('z', 'x', 'y'))
COLS = ((0, 384), (384, 384), (768, 256))
N_CH = 4
STEM, HEAD = 4, 5
bf16, f32 = jnp.bfloat16, jnp.float32


def my_place():
    f = lax.axis_index('fsdp')
    return {'x': lax.axis_index('tp'), 'z': f // 8, 'y': (f // 2) % 4, 'k': f % 2}


def moved(place, dim, step):
    new = dict(place)
    new[dim] = 1 - place['k'] if dim == 'k' else (place[dim] + step) % 4
    return new


def device(place):
    return {'tp': place['x'], 'fsdp': (place['z'] * 4 + place['y']) * 2 + place['k']}


def meet_neighbours(me):
    barrier = pltpu.get_barrier_semaphore()
    for dim in 'xyz':
        for step in (1, 3):
            pl.semaphore_signal(barrier, inc=1, device_id=device(moved(me, dim, step)), device_id_type=MESH)
    pl.semaphore_signal(barrier, inc=1, device_id=device(moved(me, 'k', 1)), device_id_type=MESH)
    pl.semaphore_wait(barrier, 7)


class Sender:
    def __init__(self, send_sems, recv_sems):
        self.send_sems, self.recv_sems, self.count, self.started = send_sems, recv_sems, 0, []

    def start(self, src, dst, target):
        n = self.count
        self.count += 1
        copy = pltpu.make_async_remote_copy(src_ref=src, dst_ref=dst, send_sem=self.send_sems.at[n],
                                            recv_sem=self.recv_sems.at[n], device_id=device(target),
                                            device_id_type=MESH)
        copy.start()
        self.started.append(copy)
        return copy


GATHER_COPIES = 7 * 8 + 16 * 4 + 16 * 4


def gather_kernel(pc, ps, ph, wc, ws, wh, send_sems, recv_sems, local_sems):
    me = my_place()
    other = moved(me, 'k', 1)
    meet_neighbours(me)
    sender = Sender(send_sems, recv_sems)
    every = pl.ds(0, 4)

    def view(kind, colour, block, half=None, group=None, k=None):
        k = me['k'] if k is None else k
        x, z, y = block['x'], block['z'], block['y']
        r0, rn = (0, 32) if half is None else (16 * half, 16)
        if kind == 'ch':
            c0, cn = COLS[colour]
            return wc.at[every if group is None else group, x, z, y, k, pl.ds(r0, rn), pl.ds(c0, cn)]
        cols = pl.ds(0, 1024) if x is every else pl.ds(pl.multiple_of(x * 256, 256), 256)
        if kind == 'stem':
            return ws.at[z, y, k, pl.ds(32 * colour + r0, rn), cols]
        return wh.at[z, y, k, pl.ds(r0, rn), cols]

    def piece(kind, colour):
        if kind == 'ch':
            c0, cn = COLS[colour]
            return pc.at[:, :, pl.ds(c0, cn)]
        if kind == 'stem':
            return ps.at[pl.ds(32 * colour, 32), :]
        return ph.at[:, :]

    early = [('stem', 0), ('stem', 1), ('stem', 2), ('ch', 0), ('ch', 1), ('ch', 2), ('head', 2)]
    late = [('stem', c, None) for c in range(3)] + [('ch', c, g) for g in range(N_CH) for c in range(3)]
    late += [('head', 2, None)]

    own = [pltpu.make_async_copy(piece(kind, c), view(kind, c, me), local_sems.at[i])
           for i, (kind, c) in enumerate(early)]
    for copy in own:
        copy.start()

    def exchange(unit, dim, block, src=None):
        kind, c = unit[:2]
        g = unit[2] if len(unit) > 2 else None
        mine = view(kind, c, block, group=g)
        source = mine if src is None else src
        return [sender.start(source, mine, moved(me, dim, step)) for step in (1, 3)]

    def forward(unit, dim, block):
        kind, c = unit[:2]
        g = unit[2] if len(unit) > 2 else None
        out = []
        for half, (origin, target) in enumerate(((3, 1), (1, 3))):
            part = view(kind, c, {**block, dim: (me[dim] + origin) % 4}, half=half, group=g)
            out.append(sender.start(part, part, moved(me, dim, target)))
        return out

    def arrived(copies):
        for copy in copies:
            copy.wait_recv()

    first, second, third, swaps = {}, {}, {}, []
    for u in early:
        first[u] = exchange(u, ORDERS[u[1]][0], me, piece(*u))
    for copy in own:
        copy.wait()
    for u in early:
        arrived(first[u])
        first[u] = forward(u, ORDERS[u[1]][0], me)
    for u in early:
        d1, d2, _ = ORDERS[u[1]]
        arrived(first[u])
        second[u] = exchange(u, d2, {**me, d1: every})
    for u in early:
        d1, d2, _ = ORDERS[u[1]]
        arrived(second[u])
        second[u] = forward(u, d2, {**me, d1: every})
    done = set()
    for u in late:
        d1, d2, d3 = ORDERS[u[1]]
        if u[:2] not in done:
            arrived(second[u[:2]])
            done.add(u[:2])
        plane = {**me, d1: every, d2: every}
        third[u] = exchange(u, d3, plane)
        mine = view(u[0], u[1], plane, group=u[2])
        swaps.append(sender.start(mine, mine, other))
    for u in late:
        d1, d2, d3 = ORDERS[u[1]]
        plane = {**me, d1: every, d2: every}
        arrived(third[u])
        third[u] = forward(u, d3, plane)
        for step in (1, 3):
            part = view(u[0], u[1], {**plane, d3: (me[d3] + step) % 4}, group=u[2])
            swaps.append(sender.start(part, part, other))
    for u in late:
        d1, d2, d3 = ORDERS[u[1]]
        plane = {**me, d1: every, d2: every}
        arrived(third[u])
        part = view(u[0], u[1], {**plane, d3: (me[d3] + 2) % 4}, group=u[2])
        swaps.append(sender.start(part, part, other))
    arrived(swaps)
    for copy in sender.started:
        copy.wait_send()
    assert sender.count == GATHER_COPIES, sender.count


def gather_weights(pc, ps, ph):
    any_spec = pl.BlockSpec(memory_space=pl.ANY)
    vmem = pl.BlockSpec(memory_space=pltpu.VMEM)
    return pl.pallas_call(
        gather_kernel, name='gather_weights',
        out_shape=[jax.ShapeDtypeStruct((N_CH, 4, 4, 4, 2, 32, 1024), bf16),
                   jax.ShapeDtypeStruct((4, 4, 2, 96, 1024), bf16),
                   jax.ShapeDtypeStruct((4, 4, 2, 32, 1024), bf16)],
        in_specs=[vmem] * 3, out_specs=[any_spec] * 3,
        scratch_shapes=[pltpu.SemaphoreType.DMA((GATHER_COPIES,)), pltpu.SemaphoreType.DMA((GATHER_COPIES,)),
                        pltpu.SemaphoreType.DMA((7,))],
        compiler_params=pltpu.CompilerParams(collective_id=0, has_side_effects=True),
        cost_estimate=pl.CostEstimate(flops=90_000_000_000, bytes_accessed=80_000_000, transcendentals=0),
    )(pc, ps, ph)


GROUPS = (STEM, 3, 2, 1, 0, HEAD)
UNITS = tuple((g, c) for g in GROUPS for c in (2, 0, 1) if g != HEAD or c == 2)
REDUCE_COPIES = 13 * len(UNITS)
ORDER = (0, 1, 2, 3, 4, 0, 5, 1, 2, 0, 3, 1, 2, 0, 4, 6, 3, 1, 7, 5, 0, 6, 4, 1, 2, 8, 0, 6, 7, 5, 2, 3, 1, 9, 0, 8, 4, 10, 7, 9, 1, 2,
         3, 0, 5, 11, 8, 9, 10, 1, 4, 5, 2, 11, 3, 6, 12, 10, 2, 5, 8, 6, 4, 7, 13, 11, 12, 3, 4, 7, 8, 14, 5, 12, 6, 13, 4, 9,
         15, 5, 8, 11, 3, 14, 13, 6, 7, 8, 9, 10, 11, 15, 7, 14, 6, 11, 10, 15, 7, 8, 9, 12, 11, 12, 14, 11, 10, 9, 13, 12, 15,
         14, 10, 9, 13, 12, 15, 14, 10, 13, 15, 12, 14, 13, 15, 14, 15, 13)


def reduce_scratch():
    per = []
    for c in range(3):
        n = COLS[c][1]
        many = sum(1 for u in UNITS if u[1] == c)
        lead = ((4, 4), (4,), ())
        b = {'C': pltpu.VMEM((2, 4, 4, 4, 2, 32, n), bf16), 'D': pltpu.VMEM((2, 4, 4, 4, 32, n), bf16),
             'S1': pltpu.VMEM((4, 4, 32, n), f32), 'S2': pltpu.VMEM((3, 4, 32, n), f32)}
        for ph in range(3):
            for name in ('opp', 'rig', 'lef'):
                b[f'{name}{ph}'] = pltpu.VMEM(lead[ph] + (32, n), bf16)
            for name in ('half0', 'half1'):
                b[f'{name}{ph}'] = pltpu.VMEM((many,) + lead[ph] + (16, n), bf16)
            for name in ('froml', 'fromr'):
                b[f'{name}{ph}'] = pltpu.VMEM((many,) + lead[ph] + (32, n), bf16)
        per.append(b)
    return per


def transposed_product(left, right):
    return lax.dot_general(left, right, (((0,), (0,)), ((), ())), preferred_element_type=f32)


def reduce_kernel(*refs):
    dpre, act, pat, vin, dout, dstem, head_l, head_r = refs[:8]
    wides = [dpre.at[0], act.at[0], dpre.at[1], act.at[1], pat]
    narrows = [vin.at[0], dout.at[0], vin.at[1], dout.at[1], dstem]
    out_c, out_s, out_h = refs[8:11]
    wide, narrow, per, send_sems, recv_sems, load_sems, credit = refs[11:]
    me = my_place()
    other = moved(me, 'k', 1)
    k = me['k']
    loads = {}

    def load(i):
        g = GROUPS[i]
        if g == HEAD:
            return
        cols = 3072 if g == STEM else 4096
        loads[g] = [pltpu.make_async_copy(wides[g], wide.at[i % 2, :, pl.ds(0, cols)], load_sems.at[i % 2, 0]),
                    pltpu.make_async_copy(narrows[g], narrow.at[i % 2], load_sems.at[i % 2, 1])]
        for copy in loads[g]:
            copy.start()

    load(0)
    meet_neighbours(me)
    sender = Sender(send_sems, recv_sems)
    busy = {}

    def free(key):
        for copy in busy.pop(key, ()):
            copy.wait_send()

    def make(g, c, cslot):
        i = GROUPS.index(g)
        slot = i % 2
        if g != HEAD and c == 2:
            for copy in loads[g]:
                copy.wait()
            load(i + 1)
        if g == STEM:
            if c != 2:
                return
            @pl.loop(0, 32)
            def _(j):
                b = j // 4
                t = j % 4
                z, y2 = b // 2, b % 2
                left = wide[slot, :, pl.ds(pl.multiple_of(b * 384, 128), 384)]
                right = narrow[slot, :, pl.ds(pl.multiple_of(t * 256, 128), 256)]
                prod = transposed_product(left, right).astype(bf16).reshape(2, 2, 3, 32, 256)
                for d in range(3):
                    per[d]['C'][0, t, z, pl.ds(y2 * 2, 2), :, :, pl.ds(0, 256)] = prod[:, :, d]
        elif g == HEAD:

            @pl.loop(0, 4)
            def _(t):
                right = head_r[:, pl.ds(pl.multiple_of(t * 256, 128), 256)]
                prod = transposed_product(head_l[...], right)
                per[c]['C'][cslot, t] = prod.astype(bf16).reshape(4, 4, 2, 32, 256)
        else:
            c0, n = COLS[c]

            @pl.loop(0, 16)
            def _(j):
                t, z = j // 4, j % 4
                if g % 2 == 0:
                    left = narrow[slot, :, pl.ds(pl.multiple_of(z * 256, 128), 256)]
                    right = wide[slot, :, pl.ds(pl.multiple_of(t * 1024 + c0, 128), n)]
                else:
                    left = wide[slot, :, pl.ds(pl.multiple_of(j * 256, 128), 256)]
                    right = narrow[slot, :, pl.ds(c0, n)]
                per[c]['C'][cslot, t, z] = transposed_product(left, right).astype(bf16).reshape(4, 2, 32, n)

    class Unit:
        def __init__(self, g, c):
            self.g, self.c = g, c
            same = [u for u in UNITS if u[1] == c]
            self.index = same.index((g, c))
            self.slot = self.index % 2
            self.last = self.index >= len(same) - 2
            self.n = COLS[c][1] if g < N_CH else 256
            self.buf = per[c]
            self.dims = ORDERS[c]

        def cut(self, name, *at):
            ref = self.buf[name]
            rest = len(ref.shape) - len(at) - 1
            return ref.at[(*at, *[slice(None)] * rest, pl.ds(0, self.n))]

        def share(self, phase, p, e, rows):
            r = pl.ds(*rows)
            cols = pl.ds(0, self.n)
            if phase == 0:
                at = dict(zip(self.dims, (p, *e)))
                at = (at['x'], at['z'], at['y'])
                return (self.buf['C'][(self.slot, *at, k, r, cols)].astype(f32)
                        + self.buf['D'][(self.slot, *at, r, cols)].astype(f32))
            lead = () if phase == 1 else (self.index % 3,)
            return self.buf[f'S{phase}'][(*lead, p, *e, r, cols)]

        def each(self, phase, body):
            if phase == 2:
                body(())
            elif phase == 1:
                pl.loop(0, 4)(lambda i: body((i,)))
            else:
                pl.loop(0, 16)(lambda i: body((i // 4, i % 4)))

        def start(self):
            free(('C', self.c, self.slot))
            make(self.g, self.c, self.slot)
            if self.index > 1:
                pl.semaphore_wait(credit.at[self.c], 1)
            cols = pl.ds(0, self.n)
            src = self.buf['C'].at[self.slot, :, :, :, 1 - k, :, cols]
            self.swap = sender.start(src, self.buf['D'].at[self.slot, :, :, :, :, cols], other)
            busy['C', self.c, self.slot] = [self.swap]

        def opposite(self, phase):
            if phase == 0:
                self.swap.wait_recv()
            p = (me[self.dims[phase]] + 2) % 4
            free((f'opp{phase}', self.c))
            cols = pl.ds(0, self.n)

            def body(e):
                self.buf[f'opp{phase}'][(*e, slice(None), cols)] = self.share(phase, p, e, (0, 32)).astype(bf16)
            self.each(phase, body)
            lead = [slice(None)] * (2 - phase)
            copies = []
            for half, step in ((0, 1), (1, 3)):
                src = self.buf[f'opp{phase}'].at[(*lead, pl.ds(16 * half, 16), cols)]
                dst = self.cut(f'half{half}{phase}', self.index)
                copies.append(sender.start(src, dst, moved(me, self.dims[phase], step)))
            busy[f'opp{phase}', self.c] = copies
            self.halves = copies

        def beside(self, phase):
            copies = []
            for half, step, name, dst in ((0, 1, 'rig', 'froml'), (1, 3, 'lef', 'fromr')):
                self.halves[half].wait_recv()
                free((f'{name}{phase}', self.c))
                p = (me[self.dims[phase]] + step) % 4
                cols = pl.ds(0, self.n)
                whole, got = self.buf[f'{name}{phase}'], self.buf[f'half{half}{phase}']

                def body(e):
                    mine = self.share(phase, p, e, (16 * half, 16)) + got[(self.index, *e, slice(None), cols)].astype(f32)
                    whole[(*e, pl.ds(16 * half, 16), cols)] = mine.astype(bf16)
                    plain = self.share(phase, p, e, (16 - 16 * half, 16))
                    whole[(*e, pl.ds(16 - 16 * half, 16), cols)] = plain.astype(bf16)
                self.each(phase, body)
                copy = sender.start(self.cut(f'{name}{phase}'), self.cut(f'{dst}{phase}', self.index),
                                    moved(me, self.dims[phase], step))
                busy[f'{name}{phase}', self.c] = [copy]
                copies.append(copy)
            self.wholes = copies

        def total(self, phase):
            for copy in self.wholes:
                copy.wait_recv()
            p = me[self.dims[phase]]
            cols = pl.ds(0, self.n)

            def body(e):
                got = [self.buf[f'{name}{phase}'][(self.index, *e, slice(None), cols)].astype(f32)
                       for name in ('froml', 'fromr')]
                value = self.share(phase, p, e, (0, 32)) + got[0] + got[1]
                if phase == 0:
                    self.buf['S1'][(*e, slice(None), cols)] = value
                elif phase == 1:
                    self.buf['S2'][(self.index % 3, *e, slice(None), cols)] = value
                elif self.g == STEM:
                    out_s[pl.ds(32 * self.c, 32), :] = value
                elif self.g == HEAD:
                    out_h[...] = value
                else:
                    out_c[self.g, :, pl.ds(*COLS[self.c])] = value
            self.each(phase, body)
            if phase == 0 and not self.last:
                pl.semaphore_signal(credit.at[self.c], inc=1, device_id=device(other), device_id_type=MESH)

        def run(self, stage):
            if stage == 0:
                self.start()
            elif stage == 7:
                self.total(2)
            elif stage % 2 == 0:
                self.beside(stage // 2 - 1)
            else:
                if stage > 1:
                    self.total(stage // 2 - 1)
                self.opposite(stage // 2)

    units = [Unit(g, c) for g, c in UNITS]
    stage_of = [0] * len(units)
    for u in ORDER:
        units[u].run(stage_of[u])
        stage_of[u] += 1
    assert stage_of == [8] * len(units)
    for key in list(busy):
        free(key)
    assert sender.count == REDUCE_COPIES, sender.count


def reduce_gradients(*operands):
    any_spec = pl.BlockSpec(memory_space=pl.ANY)
    vmem = pl.BlockSpec(memory_space=pltpu.VMEM)
    rows = operands[2].shape[0]
    return pl.pallas_call(
        reduce_kernel, name='reduce_gradients',
        out_shape=[jax.ShapeDtypeStruct((N_CH, 32, 1024), f32), jax.ShapeDtypeStruct((96, 256), f32),
                   jax.ShapeDtypeStruct((32, 256), f32)],
        in_specs=[any_spec] * 6 + [vmem] * 2, out_specs=[vmem] * 3,
        scratch_shapes=[pltpu.VMEM((2, rows, 4096), bf16), pltpu.VMEM((2, rows, 1024), bf16), reduce_scratch(),
                        pltpu.SemaphoreType.DMA((REDUCE_COPIES,)), pltpu.SemaphoreType.DMA((REDUCE_COPIES,)),
                        pltpu.SemaphoreType.DMA((2, 2)), pltpu.SemaphoreType.REGULAR((3,))],
        compiler_params=pltpu.CompilerParams(collective_id=1, has_side_effects=True, vmem_limit_bytes=64 * 1024 * 1024 - 65536),
        cost_estimate=pl.CostEstimate(flops=100_000_000_000, bytes_accessed=80_000_000, transcendentals=0),
    )(*operands)


EPS = 1e-6
TOK, TPAD = 49, 56
IMG = 8
ROWS = IMG * TPAD
CH, TOKH, CHH = 1024, 512, 4096
BLK = 512
NBLK = CHH // BLK
GELU_C, GELU_A = 0.7978845608028654, 0.044715


def dot_nn(a, b):
    return lax.dot_general(a, b, (((1,), (0,)), ((), ())), preferred_element_type=f32)


def dot_nt(a, b):
    return lax.dot_general(a, b, (((1,), (1,)), ((), ())), preferred_element_type=f32)


def dot_tn(a, b):
    return lax.dot_general(a, b, (((0,), (0,)), ((), ())), preferred_element_type=f32)


def gelu(x):
    half = 0.5 * x
    return half + half * jnp.tanh(x * (GELU_C + (GELU_C * GELU_A) * (x * x)))


def gelu_both(x):
    sq = x * x
    th = jnp.tanh(x * (GELU_C + (GELU_C * GELU_A) * sq))
    half = 0.5 * x
    rise = 0.5 + 0.5 * th
    slope = (1.0 - th * th) * (GELU_C + (3.0 * GELU_C * GELU_A) * sq)
    return x * rise, rise + half * slope


def standardize(x):
    mean = jnp.mean(x, axis=-1, keepdims=True)
    cent = x - mean
    inv = lax.rsqrt(jnp.mean(cent * cent, axis=-1, keepdims=True) + EPS)
    return cent * inv, inv


def norm_grad(d, gain, std, inv):
    gs = d * gain
    m0 = jnp.mean(gs, axis=-1, keepdims=True)
    m1 = jnp.mean(gs * std, axis=-1, keepdims=True)
    return inv * (gs - m0 - std * m1)


def row_mask(rows=TPAD):
    return lax.broadcasted_iota(jnp.int32, (rows, 1), 0) < TOK


def image(b):
    return pl.ds(pl.multiple_of(b * TPAD, 8), TPAD)


def pair(p):
    return pl.ds(pl.multiple_of(p * 2 * TPAD, 16), 2 * TPAD)


class Stream:
    def __init__(self, sem, copies, count):
        self.sem, self.copies, self.count = sem, copies, count

    def make(self, i, slot):
        return [pltpu.make_async_copy(src, dst, self.sem.at[slot, n]) for n, (src, dst) in enumerate(self.copies(i, slot))]

    def start(self, i, slot):
        for copy in self.make(i, slot):
            copy.start()

    def wait(self, i, slot):
        for copy in self.make(i, slot):
            copy.wait()


def for_blocks(stream, body, out=None):
    n = stream.count
    stream.start(0, 0)

    @pl.loop(0, n)
    def _(i):
        slot = i % 2
        stream.wait(i, slot)

        @pl.when(i + 1 < n)
        def _():
            stream.start(i + 1, 1 - slot)
        if out is not None:
            @pl.when(i >= 2)
            def _():
                out.wait(i - 2, slot)
        body(i, slot)
        if out is not None:
            out.start(i, slot)
    if out is not None:
        out.wait(n - 2, n % 2)
        out.wait(n - 1, 1 - n % 2)


def forward_kernel(pat, ws, wc, wh, wt1, wt2, bt1, vec, bch1, bhead, label,
                   xin, xmid, vout, pre_out, act_out, hl, hr, dx0, hstat, gbh,
                   p_v, x_v, v_v, w1_v, w2_v, ws_v, wh_v, pre_v, act_v, g_v, sem, sem_w, sem_o, sem_x):
    load_p = pltpu.make_async_copy(pat, p_v, sem.at[0])
    load_p.start()
    load_h = pltpu.make_async_copy(wh, wh_v, sem.at[1])
    load_h.start()
    load_p.wait()

    def stem_copies(i, slot):
        return [(ws.at[:, pl.ds(pl.multiple_of(i * 256, 256), 256)], ws_v.at[slot])]

    def stem(i, slot):
        cols = pl.ds(pl.multiple_of(i * 256, 256), 256)
        mask = (lax.broadcasted_iota(jnp.int32, (ROWS, 1), 0) % TPAD) < TOK
        x_v[:, cols] = jnp.where(mask, dot_nn(p_v[...], ws_v[slot]) + vec[0:1, cols], 0.0)
    for_blocks(Stream(sem_w, stem_copies, 4), stem)

    saves = []

    def save(src, dst, n):
        copy = pltpu.make_async_copy(src, dst, sem_x.at[n])
        copy.start()
        saves.append(copy)

    for l in range(2):
        r = 1 + 5 * l
        for copy in saves:
            copy.wait()
        saves.clear()
        first = pltpu.make_async_copy(x_v, xin.at[l], sem_x.at[0])
        first.start()
        first.wait()

        @pl.loop(0, IMG)
        def _(b):
            x = x_v[image(b), :]
            std, _ = standardize(x)
            a = (std * vec[r:r + 1, :] + vec[r + 1:r + 2, :]).astype(bf16)
            h = dot_nn(wt1[l], a) + bt1[l]
            g_v[...] = gelu(h).astype(bf16)
            x_v[image(b), :] = x + dot_tn(wt2[l], g_v[...])
        save(x_v, xmid.at[l], 0)

        @pl.loop(0, IMG // 2)
        def _(p):
            std, _ = standardize(x_v[pair(p), :])
            v_v[pair(p), :] = (std * vec[r + 2:r + 3, :] + vec[r + 3:r + 4, :]).astype(bf16)
        save(v_v, vout.at[l], 1)
        saves[0].wait()
        saves.pop(0)

        def blocks(i, slot):
            t, h = i // 2, i % 2
            part = pl.ds(pl.multiple_of(h * BLK, BLK), BLK)
            return [(wc.at[2 * l, t, :, part], w1_v.at[slot]), (wc.at[2 * l + 1, t, part, :], w2_v.at[slot])]

        def outs(i, slot):
            part = pl.ds(pl.multiple_of(i * BLK, BLK), BLK)
            return [(pre_v.at[slot], pre_out.at[l, :, part]), (act_v.at[slot], act_out.at[l, :, part])]

        def channel(i, slot):
            part = pl.ds(pl.multiple_of(i * BLK, BLK), BLK)
            h = dot_nn(v_v[...], w1_v[slot]) + bch1[l:l + 1, part]
            pre_v[slot] = h
            act_v[slot] = gelu(h).astype(bf16)
            x_v[...] += dot_nn(act_v[slot], w2_v[slot])
        for_blocks(Stream(sem_w, blocks, NBLK), channel, Stream(sem_o, outs, NBLK))
        x_v[...] += vec[r + 4:r + 5, :]
    for copy in saves:
        copy.wait()

    load_h.wait()
    last = 11
    mask = row_mask()
    pooled = jnp.concatenate([jnp.sum(jnp.where(mask, x_v[b * TPAD:(b + 1) * TPAD, :], 0.0), axis=0, keepdims=True)
                              for b in range(IMG)], axis=0) * (1.0 / TOK)
    std, inv = standardize(pooled)
    head_in = (std * vec[last:last + 1, :] + vec[last + 1:last + 2, :]).astype(bf16)
    hl[...] = head_in
    logits = dot_nn(head_in, wh_v[...]) + bhead[...]
    is_label = lax.broadcasted_iota(jnp.int32, logits.shape, 1) == label[...]
    top = jnp.max(logits, axis=-1, keepdims=True)
    ex = jnp.exp(logits - top)
    es = jnp.sum(ex, axis=-1, keepdims=True)
    nll = top + jnp.log(es) - jnp.sum(jnp.where(is_label, logits, 0.0), axis=-1, keepdims=True)
    d_logits = (ex / es - jnp.where(is_label, 1.0, 0.0)) * (1.0 / 1024)
    gbh[...] = jnp.sum(d_logits, axis=0, keepdims=True)
    d_bf = d_logits.astype(bf16)
    hr[...] = d_bf
    d_in = dot_nt(d_bf, wh_v[...])
    hstat[0:1, :] = jnp.sum(d_in * std, axis=0, keepdims=True)
    hstat[1:2, :] = jnp.sum(d_in, axis=0, keepdims=True)
    hstat[2:3, :] = jnp.broadcast_to(jnp.sum(nll, axis=0, keepdims=True), (1, CH))
    dx0[...] = norm_grad(d_in, vec[last:last + 1, :], std, inv) * (1.0 / TOK)


def forward(pat, ws, wc, wh, wt1, wt2, bt1, vec, bch1, bhead, label):
    a, v = pl.BlockSpec(memory_space=pl.ANY), pl.BlockSpec(memory_space=pltpu.VMEM)
    S = jax.ShapeDtypeStruct
    return pl.pallas_call(
        forward_kernel, name='forward',
        in_specs=[a, a, a, a] + [v] * 7,
        out_specs=[a] * 5 + [v] * 5,
        out_shape=[S((2, ROWS, CH), f32), S((2, ROWS, CH), f32), S((2, ROWS, CH), bf16), S((2, ROWS, CHH), f32),
                   S((2, ROWS, CHH), bf16), S((IMG, CH), bf16), S((IMG, CH), bf16), S((IMG, CH), f32), S((8, CH), f32),
                   S((1, CH), f32)],
        scratch_shapes=[pltpu.VMEM((ROWS, 3072), bf16), pltpu.VMEM((ROWS, CH), f32), pltpu.VMEM((ROWS, CH), bf16),
                        pltpu.VMEM((2, CH, BLK), bf16), pltpu.VMEM((2, BLK, CH), bf16), pltpu.VMEM((2, 3072, 256), bf16),
                        pltpu.VMEM((CH, CH), bf16), pltpu.VMEM((2, ROWS, BLK), f32), pltpu.VMEM((2, ROWS, BLK), bf16),
                        pltpu.VMEM((TOKH, CH), bf16), pltpu.SemaphoreType.DMA((2,)), pltpu.SemaphoreType.DMA((2, 2)),
                        pltpu.SemaphoreType.DMA((2, 2)), pltpu.SemaphoreType.DMA((2,))],
        compiler_params=pltpu.CompilerParams(vmem_limit_bytes=60 * 1024 * 1024),
        cost_estimate=pl.CostEstimate(flops=50_000_000_000, bytes_accessed=100_000_000, transcendentals=0),
    )(pat, ws, wc, wh, wt1, wt2, bt1, vec, bch1, bhead, label)


def backward_kernel(xin, xmid, pre_in, wc, wt1, wt2, bt1, vec, dx0,
                    dpre, dout, dstem, gvec, gbch1, gt1, gt2, gbt,
                    x_v, d_v, dv_v, do_v, w1_v, w2_v, pre_v, dp_v, g_v, dh_v, sem, sem_w, sem_o):
    mask = row_mask()
    for b in range(IMG):
        d_v[b * TPAD:(b + 1) * TPAD, :] = jnp.where(mask, jnp.broadcast_to(dx0[b:b + 1, :], (TPAD, CH)), 0.0)
    gvec[...] = jnp.zeros_like(gvec)
    gt1[...] = jnp.zeros_like(gt1)
    gt2[...] = jnp.zeros_like(gt2)
    gbt[...] = jnp.zeros_like(gbt)

    def add(row, value):
        gvec[row:row + 1, :] += jnp.sum(value, axis=0, keepdims=True)

    for l in (1, 0):
        r = 1 + 5 * l
        load = pltpu.make_async_copy(xmid.at[l], x_v, sem.at[0])
        load.start()

        @pl.loop(0, IMG // 2)
        def _(p):
            d = d_v[pair(p), :]
            add(r + 4, d)
            do_v[pair(p), :] = d.astype(bf16)
        send = pltpu.make_async_copy(do_v, dout.at[l], sem.at[1])
        send.start()

        def blocks(i, slot):
            t, h = i // 2, i % 2
            part = pl.ds(pl.multiple_of(h * BLK, BLK), BLK)
            whole = pl.ds(pl.multiple_of(i * BLK, BLK), BLK)
            return [(wc.at[2 * l, t, :, part], w1_v.at[slot]), (wc.at[2 * l + 1, t, part, :], w2_v.at[slot]),
                    (pre_in.at[l, :, whole], pre_v.at[slot])]

        def outs(i, slot):
            return [(dp_v.at[slot], dpre.at[l, :, pl.ds(pl.multiple_of(i * BLK, BLK), BLK)])]

        def channel(i, slot):
            _, slope = gelu_both(pre_v[slot])
            d = dot_nt(do_v[...], w2_v[slot]) * slope
            gbch1[l:l + 1, pl.ds(pl.multiple_of(i * BLK, BLK), BLK)] = jnp.sum(d, axis=0, keepdims=True)
            dp_v[slot] = d.astype(bf16)
            part = dot_nt(dp_v[slot], w1_v[slot])

            @pl.when(i == 0)
            def _():
                dv_v[...] = part

            @pl.when(i > 0)
            def _():
                dv_v[...] += part
        for_blocks(Stream(sem_w, blocks, NBLK), channel, Stream(sem_o, outs, NBLK))
        load.wait()
        send.wait()

        @pl.loop(0, IMG)
        def _(b):
            std, inv = standardize(x_v[image(b), :])
            d = dv_v[image(b), :]
            add(r + 2, d * std)
            add(r + 3, d)
            d_v[image(b), :] += norm_grad(d, vec[r + 2:r + 3, :], std, inv)
        load = pltpu.make_async_copy(xin.at[l], x_v, sem.at[0])
        load.start()
        load.wait()

        @pl.loop(0, IMG)
        def _(b):
            std, inv = standardize(x_v[image(b), :])
            a = (std * vec[r:r + 1, :] + vec[r + 1:r + 2, :]).astype(bf16)
            d_mid = d_v[image(b), :]
            dm = d_mid.astype(bf16)
            act, slope = gelu_both(dot_nn(wt1[l], a) + bt1[l])
            g_v[...] = act.astype(bf16)
            dh = dot_nn(wt2[l], dm) * slope
            gbt[l] += jnp.sum(dh, axis=-1, keepdims=True)
            dh_v[...] = dh.astype(bf16)
            gt2[l] += dot_nt(g_v[...], dm)
            gt1[l] += dot_nt(dh_v[...], a)
            d = dot_tn(wt1[l], dh_v[...])
            add(r, d * std)
            add(r + 1, d)
            d_v[image(b), :] = d_mid + norm_grad(d, vec[r:r + 1, :], std, inv)

    @pl.loop(0, IMG // 2)
    def _(p):
        d = d_v[pair(p), :]
        add(0, d)
        do_v[pair(p), :] = d.astype(bf16)
    send = pltpu.make_async_copy(do_v, dstem, sem.at[1])
    send.start()
    send.wait()


def backward(xin, xmid, pre, wc, wt1, wt2, bt1, vec, dx0):
    a, v = pl.BlockSpec(memory_space=pl.ANY), pl.BlockSpec(memory_space=pltpu.VMEM)
    S = jax.ShapeDtypeStruct
    return pl.pallas_call(
        backward_kernel, name='backward',
        in_specs=[a] * 4 + [v] * 5,
        out_specs=[a] * 3 + [v] * 5,
        out_shape=[S((2, ROWS, CHH), bf16), S((2, ROWS, CH), bf16), S((ROWS, CH), bf16), S((16, CH), f32), S((2, CHH), f32),
                   S((2, TOKH, TPAD), f32), S((2, TOKH, TPAD), f32), S((2, TOKH, 1), f32)],
        scratch_shapes=[pltpu.VMEM((ROWS, CH), f32), pltpu.VMEM((ROWS, CH), f32), pltpu.VMEM((ROWS, CH), f32),
                        pltpu.VMEM((ROWS, CH), bf16), pltpu.VMEM((2, CH, BLK), bf16), pltpu.VMEM((2, BLK, CH), bf16),
                        pltpu.VMEM((2, ROWS, BLK), f32), pltpu.VMEM((2, ROWS, BLK), bf16), pltpu.VMEM((TOKH, CH), bf16),
                        pltpu.VMEM((TOKH, CH), bf16), pltpu.SemaphoreType.DMA((2,)), pltpu.SemaphoreType.DMA((2, 3)),
                        pltpu.SemaphoreType.DMA((2, 1))],
        compiler_params=pltpu.CompilerParams(vmem_limit_bytes=60 * 1024 * 1024),
        cost_estimate=pl.CostEstimate(flops=50_000_000_000, bytes_accessed=100_000_000, transcendentals=0),
    )(xin, xmid, pre, wc, wt1, wt2, bt1, vec, dx0)

CHANNEL_AXES = ('tp', 'fsdp')


def weight_specs():
    vec_spec = P(CHANNEL_AXES)
    layer_vec = P(None, CHANNEL_AXES)
    return (P('fsdp', 'tp'), vec_spec, layer_vec, layer_vec, P(None, None, 'fsdp'), P(None, 'fsdp'),
            P(None, 'fsdp', None), layer_vec, layer_vec, P(None, 'fsdp', 'tp'), layer_vec,
            P(None, CHANNEL_AXES, None), layer_vec, vec_spec, vec_spec, P('fsdp', 'tp'), P('tp'))


def solution(mesh):
    fs = mesh.shape['fsdp']
    tp = mesh.shape['tp']
    nd = fs * tp

    def step(patches, labels, w_stem, b_stem, ln1_g, ln1_b, w_tok1, b_tok1, w_tok2,
             ln2_g, ln2_b, w_ch1, b_ch1, w_ch2, b_ch2, lnf_g, lnf_b, w_head, b_head):
        t = lax.axis_index('tp')
        nl = w_tok1.shape[0]
        total_images = IMG * nd
        pat = lax.dynamic_slice_in_dim(patches, t * IMG, IMG, 0)
        pat = jnp.pad(pat, ((0, 0), (0, TPAD - TOK), (0, 0))).reshape(ROWS, -1)
        lab = lax.dynamic_slice_in_dim(labels, t * IMG, IMG, 0)

        vecs = [b_stem[None]]
        for l in range(nl):
            vecs += [a[l:l + 1] for a in (ln1_g, ln1_b, ln2_g, ln2_b, b_ch2)]
        vec_rows = jnp.concatenate(vecs + [lnf_g[None], lnf_b[None]], axis=0)
        n_rows = vec_rows.shape[0]
        toks = jnp.pad(jnp.concatenate([w_tok1.transpose(0, 2, 1), w_tok2], axis=0), ((0, 0), (0, 0), (0, TPAD - TOK)))
        pieces = [vec_rows.reshape(-1), b_ch1.reshape(-1), b_tok1.reshape(-1), b_head.reshape(-1), toks.reshape(-1)]
        pack = jnp.concatenate(pieces)
        pack = jnp.pad(pack, (0, (-pack.shape[0]) % 1024))
        small = lax.all_gather(pack, CHANNEL_AXES, axis=0, tiled=False).reshape(tp, fs, -1)
        offs = []
        o = 0
        for p in pieces:
            offs.append(small[:, :, o:o + p.shape[0]])
            o += p.shape[0]
        vec = offs[0].reshape(tp, fs, n_rows, -1).transpose(2, 0, 1, 3).reshape(n_rows, -1)
        bch1 = offs[1].reshape(tp, fs, nl, -1).transpose(2, 0, 1, 3).reshape(nl, -1)
        bt1 = offs[2][0].reshape(fs, nl, -1).transpose(1, 0, 2).reshape(nl, -1)[:, :, None]
        bhead = offs[3][:, 0]
        wt = offs[4][0].reshape(fs, 2 * nl, -1, TPAD).transpose(1, 0, 2, 3).reshape(2 * nl, TOKH, TPAD).astype(bf16)

        classes = w_head.shape[1]
        pad_cls = 256 - classes
        pc = jnp.stack([w_ch1[0], w_ch2[0], w_ch1[1], w_ch2[1]]).astype(bf16)
        ph = jnp.pad(w_head.astype(bf16), ((0, 0), (0, pad_cls)))
        wc, ws, wh = gather_weights(pc, w_stem.astype(bf16), ph)
        ws = ws.reshape(-1, CH)
        wh = wh.reshape(CH, -1)
        wc = wc.reshape(2 * nl, tp, CH, CH)
        bhead = jnp.pad(bhead, ((0, 0), (0, pad_cls)), constant_values=-1e30).reshape(1, -1)
        label = (lab // classes * 256 + lab % classes).reshape(IMG, 1)

        xin, xmid, vin, pre, act, hl, hr, dx0, hstat, gbh = forward(pat, ws, wc, wh, wt[:nl], wt[nl:], bt1, vec, bch1,
                                                                    bhead, label)
        dpre, dout, dstem, gvec, gbch1, gt1, gt2, gbt = backward(xin, xmid, pre, wc, wt[:nl], wt[nl:], bt1, vec, dx0)

        gvec = jnp.concatenate([gvec[:11], hstat[:2]], axis=0)
        parts = [gvec, gbch1, gbt[:, :, 0], gbh, gt1, gt2, hstat[2, :1]]
        flat = jnp.concatenate([p.reshape(-1) for p in parts])
        flat = jnp.pad(flat, (0, (-flat.shape[0]) % 1024))
        tot = lax.psum(flat, CHANNEL_AXES)

        g_c, g_s, g_h = reduce_gradients(dpre, act, pat, vin, dout, dstem, hl, hr)

        out = []
        o = 0
        for p in parts:
            out.append(tot[o:o + p.size].reshape(p.shape))
            o += p.size
        f = lax.axis_index('fsdp')

        def own(x, n, i, ax):
            size = x.shape[ax] // n
            return lax.dynamic_slice_in_dim(x, i * size, size, ax)
        dev = t * fs + f
        gv = own(out[0], nd, dev, 1)
        gc1 = own(out[1], nd, dev, 1)
        gtb = own(out[2], fs, f, 1)
        gbh = own(out[3].reshape(tp, 256), tp, t, 0)[0, :classes]
        gw1 = own(out[4], fs, f, 1)[:, :, :TOK].transpose(0, 2, 1)
        gw2 = own(out[5], fs, f, 1)[:, :, :TOK]
        loss = out[6][0] / total_images
        per = [jnp.stack([gv[1 + i], gv[6 + i]]) for i in range(5)]
        return (loss, g_s, gv[0], per[0], per[1], gw1, gtb, gw2, per[2], per[3], g_c[0::2], gc1, g_c[1::2], per[4],
                gv[11], gv[12], g_h[:, :classes], gbh)

    specs = weight_specs()
    return jax.shard_map(step, mesh=mesh, in_specs=(P('fsdp', None, None), P('fsdp')) + specs,
                         out_specs=(P(),) + specs, check_vma=False)
```

```python
import functools

import jax
import jax.numpy as jnp
from jax import lax
from jax.experimental import pallas as pl
from jax.experimental.pallas import tpu as pltpu
from jax.sharding import PartitionSpec as P

MESH = pl.DeviceIdType.MESH
ORDERS = (('x', 'y', 'z'), ('y', 'z', 'x'), ('z', 'x', 'y'))
COLS = ((0, 384), (384, 384), (768, 256))
N_CH = 4
STEM, HEAD = 4, 5
bf16, f32 = jnp.bfloat16, jnp.float32


def my_place():
    f = lax.axis_index('fsdp')
    return {'x': lax.axis_index('tp'), 'z': f // 8, 'y': (f // 2) % 4, 'k': f % 2}


def moved(place, dim, step):
    new = dict(place)
    new[dim] = 1 - place['k'] if dim == 'k' else (place[dim] + step) % 4
    return new


def device(place):
    return {'tp': place['x'], 'fsdp': (place['z'] * 4 + place['y']) * 2 + place['k']}


def meet_neighbours(me):
    barrier = pltpu.get_barrier_semaphore()
    for dim in 'xyz':
        for step in (1, 3):
            pl.semaphore_signal(barrier, inc=1, device_id=device(moved(me, dim, step)), device_id_type=MESH)
    pl.semaphore_signal(barrier, inc=1, device_id=device(moved(me, 'k', 1)), device_id_type=MESH)
    pl.semaphore_wait(barrier, 7)


class Sender:
    def __init__(self, send_sems, recv_sems):
        self.send_sems, self.recv_sems, self.count, self.started = send_sems, recv_sems, 0, []

    def start(self, src, dst, target):
        n = self.count
        self.count += 1
        copy = pltpu.make_async_remote_copy(src_ref=src, dst_ref=dst, send_sem=self.send_sems.at[n],
                                            recv_sem=self.recv_sems.at[n], device_id=device(target),
                                            device_id_type=MESH)
        copy.start()
        self.started.append(copy)
        return copy


GROUPS = (STEM, 3, 2, 1, 0, HEAD)
UNITS = tuple((g, c) for g in GROUPS for c in (2, 0, 1) if g != HEAD or c == 2)
REDUCE_COPIES = 13 * len(UNITS)
ORDER = (0, 1, 2, 3, 4, 0, 5, 1, 2, 0, 3, 1, 2, 0, 4, 6, 3, 1, 7, 5, 0, 6, 4, 1, 2, 8, 0, 6, 7, 5, 2, 3, 1, 9, 0, 8, 4, 10, 7, 9, 1, 2,
         3, 0, 5, 11, 8, 9, 10, 1, 4, 5, 2, 11, 3, 6, 12, 10, 2, 5, 8, 6, 4, 7, 13, 11, 12, 3, 4, 7, 8, 14, 5, 12, 6, 13, 4, 9,
         15, 5, 8, 11, 3, 14, 13, 6, 7, 8, 9, 10, 11, 15, 7, 14, 6, 11, 10, 15, 7, 8, 9, 12, 11, 12, 14, 11, 10, 9, 13, 12, 15,
         14, 10, 9, 13, 12, 15, 14, 10, 13, 15, 12, 14, 13, 15, 14, 15, 13)


def reduce_scratch():
    per = []
    for c in range(3):
        n = COLS[c][1]
        many = sum(1 for u in UNITS if u[1] == c)
        lead = ((4, 4), (4,), ())
        b = {'C': pltpu.VMEM((2, 4, 4, 4, 2, 32, n), bf16), 'D': pltpu.VMEM((2, 4, 4, 4, 32, n), bf16),
             'S1': pltpu.VMEM((4, 4, 32, n), f32), 'S2': pltpu.VMEM((3, 4, 32, n), f32)}
        for ph in range(3):
            for name in ('opp', 'rig', 'lef'):
                b[f'{name}{ph}'] = pltpu.VMEM(lead[ph] + (32, n), bf16)
            for name in ('half0', 'half1'):
                b[f'{name}{ph}'] = pltpu.VMEM((many,) + lead[ph] + (16, n), bf16)
            for name in ('froml', 'fromr'):
                b[f'{name}{ph}'] = pltpu.VMEM((many,) + lead[ph] + (32, n), bf16)
        per.append(b)
    return per


def transposed_product(left, right):
    return lax.dot_general(left, right, (((0,), (0,)), ((), ())), preferred_element_type=f32)


def reduce_kernel(*refs):
    dpre, act, pat, vin, dout, dstem, head_l, head_r = refs[:8]
    wides = [dpre.at[0], act.at[0], dpre.at[1], act.at[1], pat]
    narrows = [vin.at[0], dout.at[0], vin.at[1], dout.at[1], dstem]
    out_c, out_s, out_h = refs[8:11]
    wide, narrow, per, send_sems, recv_sems, load_sems, credit = refs[11:]
    me = my_place()
    other = moved(me, 'k', 1)
    k = me['k']
    loads = {}

    def load(i):
        g = GROUPS[i]
        if g == HEAD:
            return
        cols = 3072 if g == STEM else 4096
        loads[g] = [pltpu.make_async_copy(wides[g], wide.at[i % 2, :, pl.ds(0, cols)], load_sems.at[i % 2, 0]),
                    pltpu.make_async_copy(narrows[g], narrow.at[i % 2], load_sems.at[i % 2, 1])]
        for copy in loads[g]:
            copy.start()

    load(0)
    meet_neighbours(me)
    sender = Sender(send_sems, recv_sems)
    busy = {}

    def free(key):
        for copy in busy.pop(key, ()):
            copy.wait_send()

    def make(g, c, cslot):
        i = GROUPS.index(g)
        slot = i % 2
        if g != HEAD and c == 2:
            for copy in loads[g]:
                copy.wait()
            load(i + 1)
        if g == STEM:
            if c != 2:
                return
            @pl.loop(0, 32)
            def _(j):
                b = j // 4
                t = j % 4
                z, y2 = b // 2, b % 2
                left = wide[slot, :, pl.ds(pl.multiple_of(b * 384, 128), 384)]
                right = narrow[slot, :, pl.ds(pl.multiple_of(t * 256, 128), 256)]
                prod = transposed_product(left, right).astype(bf16).reshape(2, 2, 3, 32, 256)
                for d in range(3):
                    per[d]['C'][0, t, z, pl.ds(y2 * 2, 2), :, :, pl.ds(0, 256)] = prod[:, :, d]
        elif g == HEAD:

            @pl.loop(0, 4)
            def _(t):
                right = head_r[:, pl.ds(pl.multiple_of(t * 256, 128), 256)]
                prod = transposed_product(head_l[...], right)
                per[c]['C'][cslot, t] = prod.astype(bf16).reshape(4, 4, 2, 32, 256)
        else:
            c0, n = COLS[c]

            @pl.loop(0, 16)
            def _(j):
                t, z = j // 4, j % 4
                if g % 2 == 0:
                    left = narrow[slot, :, pl.ds(pl.multiple_of(z * 256, 128), 256)]
                    right = wide[slot, :, pl.ds(pl.multiple_of(t * 1024 + c0, 128), n)]
                else:
                    left = wide[slot, :, pl.ds(pl.multiple_of(j * 256, 128), 256)]
                    right = narrow[slot, :, pl.ds(c0, n)]
                per[c]['C'][cslot, t, z] = transposed_product(left, right).astype(bf16).reshape(4, 2, 32, n)

    class Unit:
        def __init__(self, g, c):
            self.g, self.c = g, c
            same = [u for u in UNITS if u[1] == c]
            self.index = same.index((g, c))
            self.slot = self.index % 2
            self.last = self.index >= len(same) - 2
            self.n = COLS[c][1] if g < N_CH else 256
            self.buf = per[c]
            self.dims = ORDERS[c]

        def cut(self, name, *at):
            ref = self.buf[name]
            rest = len(ref.shape) - len(at) - 1
            return ref.at[(*at, *[slice(None)] * rest, pl.ds(0, self.n))]

        def share(self, phase, p, e, rows):
            r = pl.ds(*rows)
            cols = pl.ds(0, self.n)
            if phase == 0:
                at = dict(zip(self.dims, (p, *e)))
                at = (at['x'], at['z'], at['y'])
                return (self.buf['C'][(self.slot, *at, k, r, cols)].astype(f32)
                        + self.buf['D'][(self.slot, *at, r, cols)].astype(f32))
            lead = () if phase == 1 else (self.index % 3,)
            return self.buf[f'S{phase}'][(*lead, p, *e, r, cols)]

        def each(self, phase, body):
            if phase == 2:
                body(())
            elif phase == 1:
                pl.loop(0, 4)(lambda i: body((i,)))
            else:
                pl.loop(0, 16)(lambda i: body((i // 4, i % 4)))

        def start(self):
            free(('C', self.c, self.slot))
            make(self.g, self.c, self.slot)
            if self.index > 1:
                pl.semaphore_wait(credit.at[self.c], 1)
            cols = pl.ds(0, self.n)
            src = self.buf['C'].at[self.slot, :, :, :, 1 - k, :, cols]
            self.swap = sender.start(src, self.buf['D'].at[self.slot, :, :, :, :, cols], other)
            busy['C', self.c, self.slot] = [self.swap]

        def opposite(self, phase):
            if phase == 0:
                self.swap.wait_recv()
            p = (me[self.dims[phase]] + 2) % 4
            free((f'opp{phase}', self.c))
            cols = pl.ds(0, self.n)

            def body(e):
                self.buf[f'opp{phase}'][(*e, slice(None), cols)] = self.share(phase, p, e, (0, 32)).astype(bf16)
            self.each(phase, body)
            lead = [slice(None)] * (2 - phase)
            copies = []
            for half, step in ((0, 1), (1, 3)):
                src = self.buf[f'opp{phase}'].at[(*lead, pl.ds(16 * half, 16), cols)]
                dst = self.cut(f'half{half}{phase}', self.index)
                copies.append(sender.start(src, dst, moved(me, self.dims[phase], step)))
            busy[f'opp{phase}', self.c] = copies
            self.halves = copies

        def beside(self, phase):
            copies = []
            for half, step, name, dst in ((0, 1, 'rig', 'froml'), (1, 3, 'lef', 'fromr')):
                self.halves[half].wait_recv()
                free((f'{name}{phase}', self.c))
                p = (me[self.dims[phase]] + step) % 4
                cols = pl.ds(0, self.n)
                whole, got = self.buf[f'{name}{phase}'], self.buf[f'half{half}{phase}']

                def body(e):
                    mine = self.share(phase, p, e, (16 * half, 16)) + got[(self.index, *e, slice(None), cols)].astype(f32)
                    whole[(*e, pl.ds(16 * half, 16), cols)] = mine.astype(bf16)
                    plain = self.share(phase, p, e, (16 - 16 * half, 16))
                    whole[(*e, pl.ds(16 - 16 * half, 16), cols)] = plain.astype(bf16)
                self.each(phase, body)
                copy = sender.start(self.cut(f'{name}{phase}'), self.cut(f'{dst}{phase}', self.index),
                                    moved(me, self.dims[phase], step))
                busy[f'{name}{phase}', self.c] = [copy]
                copies.append(copy)
            self.wholes = copies

        def total(self, phase):
            for copy in self.wholes:
                copy.wait_recv()
            p = me[self.dims[phase]]
            cols = pl.ds(0, self.n)

            def body(e):
                got = [self.buf[f'{name}{phase}'][(self.index, *e, slice(None), cols)].astype(f32)
                       for name in ('froml', 'fromr')]
                value = self.share(phase, p, e, (0, 32)) + got[0] + got[1]
                if phase == 0:
                    self.buf['S1'][(*e, slice(None), cols)] = value
                elif phase == 1:
                    self.buf['S2'][(self.index % 3, *e, slice(None), cols)] = value
                elif self.g == STEM:
                    out_s[pl.ds(32 * self.c, 32), :] = value
                elif self.g == HEAD:
                    out_h[...] = value
                else:
                    out_c[self.g, :, pl.ds(*COLS[self.c])] = value
            self.each(phase, body)
            if phase == 0 and not self.last:
                pl.semaphore_signal(credit.at[self.c], inc=1, device_id=device(other), device_id_type=MESH)

        def run(self, stage):
            if stage == 0:
                self.start()
            elif stage == 7:
                self.total(2)
            elif stage % 2 == 0:
                self.beside(stage // 2 - 1)
            else:
                if stage > 1:
                    self.total(stage // 2 - 1)
                self.opposite(stage // 2)

    units = [Unit(g, c) for g, c in UNITS]
    stage_of = [0] * len(units)
    for u in ORDER:
        units[u].run(stage_of[u])
        stage_of[u] += 1
    assert stage_of == [8] * len(units)
    for key in list(busy):
        free(key)
    assert sender.count == REDUCE_COPIES, sender.count


def reduce_gradients(*operands):
    any_spec = pl.BlockSpec(memory_space=pl.ANY)
    vmem = pl.BlockSpec(memory_space=pltpu.VMEM)
    rows = operands[2].shape[0]
    return pl.pallas_call(
        reduce_kernel, name='reduce_gradients',
        out_shape=[jax.ShapeDtypeStruct((N_CH, 32, 1024), f32), jax.ShapeDtypeStruct((96, 256), f32),
                   jax.ShapeDtypeStruct((32, 256), f32)],
        in_specs=[any_spec] * 6 + [vmem] * 2, out_specs=[vmem] * 3,
        scratch_shapes=[pltpu.VMEM((2, rows, 4096), bf16), pltpu.VMEM((2, rows, 1024), bf16), reduce_scratch(),
                        pltpu.SemaphoreType.DMA((REDUCE_COPIES,)), pltpu.SemaphoreType.DMA((REDUCE_COPIES,)),
                        pltpu.SemaphoreType.DMA((2, 2)), pltpu.SemaphoreType.REGULAR((3,))],
        compiler_params=pltpu.CompilerParams(collective_id=1, has_side_effects=True, vmem_limit_bytes=64 * 1024 * 1024 - 65536),
        cost_estimate=pl.CostEstimate(flops=100_000_000_000, bytes_accessed=80_000_000, transcendentals=0),
    )(*operands)


EPS = 1e-6
TOK, TPAD = 49, 56
IMG = 8
ROWS = IMG * TPAD
CH, TOKH, CHH = 1024, 512, 4096
BLK = 512
NBLK = CHH // BLK
GELU_C, GELU_A = 0.7978845608028654, 0.044715


def dot_nn(a, b):
    return lax.dot_general(a, b, (((1,), (0,)), ((), ())), preferred_element_type=f32)


def dot_nt(a, b):
    return lax.dot_general(a, b, (((1,), (1,)), ((), ())), preferred_element_type=f32)


def dot_tn(a, b):
    return lax.dot_general(a, b, (((0,), (0,)), ((), ())), preferred_element_type=f32)


def gelu(x):
    half = 0.5 * x
    return half + half * jnp.tanh(x * (GELU_C + (GELU_C * GELU_A) * (x * x)))


def gelu_both(x):
    sq = x * x
    th = jnp.tanh(x * (GELU_C + (GELU_C * GELU_A) * sq))
    half = 0.5 * x
    rise = 0.5 + 0.5 * th
    slope = (1.0 - th * th) * (GELU_C + (3.0 * GELU_C * GELU_A) * sq)
    return x * rise, rise + half * slope


def standardize(x):
    mean = jnp.mean(x, axis=-1, keepdims=True)
    cent = x - mean
    inv = lax.rsqrt(jnp.mean(cent * cent, axis=-1, keepdims=True) + EPS)
    return cent * inv, inv


def norm_grad(d, gain, std, inv):
    gs = d * gain
    m0 = jnp.mean(gs, axis=-1, keepdims=True)
    m1 = jnp.mean(gs * std, axis=-1, keepdims=True)
    return inv * (gs - m0 - std * m1)


def row_mask(rows=TPAD):
    return lax.broadcasted_iota(jnp.int32, (rows, 1), 0) < TOK


def image(b):
    return pl.ds(pl.multiple_of(b * TPAD, 8), TPAD)


def pair(p):
    return pl.ds(pl.multiple_of(p * 2 * TPAD, 16), 2 * TPAD)


class Stream:
    def __init__(self, sem, copies, count):
        self.sem, self.copies, self.count = sem, copies, count

    def make(self, i, slot):
        return [pltpu.make_async_copy(src, dst, self.sem.at[slot, n]) for n, (src, dst) in enumerate(self.copies(i, slot))]

    def start(self, i, slot):
        for copy in self.make(i, slot):
            copy.start()

    def wait(self, i, slot):
        for copy in self.make(i, slot):
            copy.wait()


def for_blocks(stream, body, out=None):
    n = stream.count
    stream.start(0, 0)

    @pl.loop(0, n)
    def _(i):
        slot = i % 2
        stream.wait(i, slot)

        @pl.when(i + 1 < n)
        def _():
            stream.start(i + 1, 1 - slot)
        if out is not None:
            @pl.when(i >= 2)
            def _():
                out.wait(i - 2, slot)
        body(i, slot)
        if out is not None:
            out.start(i, slot)
    if out is not None:
        out.wait(n - 2, n % 2)
        out.wait(n - 1, 1 - n % 2)


def backward_kernel(xin, xmid, pre_in, wc, wt, vec, dx0,
                    dpre, dout, dstem, gvec, gbch1, gt1, gt2, gbt,
                    x_v, d_v, dv_v, do_v, w1_v, w2_v, pre_v, dp_v, g_v, dh_v, sem, sem_w, sem_o):
    mask = row_mask()
    for b in range(IMG):
        d_v[b * TPAD:(b + 1) * TPAD, :] = jnp.where(mask, jnp.broadcast_to(dx0[b:b + 1, :], (TPAD, CH)), 0.0)
    gvec[...] = jnp.zeros_like(gvec)
    gt1[...] = jnp.zeros_like(gt1)
    gt2[...] = jnp.zeros_like(gt2)
    gbt[...] = jnp.zeros_like(gbt)

    def add(row, value):
        gvec[row:row + 1, :] += jnp.sum(value, axis=0, keepdims=True)

    for l in (1, 0):
        r = 1 + 5 * l
        load = pltpu.make_async_copy(xmid.at[l], x_v, sem.at[0])
        load.start()

        @pl.loop(0, IMG // 2)
        def _(p):
            d = d_v[pair(p), :]
            add(r + 4, d)
            do_v[pair(p), :] = d.astype(bf16)
        send = pltpu.make_async_copy(do_v, dout.at[l], sem.at[1])
        send.start()

        def blocks(i, slot):
            t, h = i // 2, i % 2
            part = pl.ds(pl.multiple_of(h * BLK, BLK), BLK)
            whole = pl.ds(pl.multiple_of(i * BLK, BLK), BLK)
            return [(wc.at[2 * l, t, :, :, :, :, part], w1_v.at[slot]),
                    (wc.at[2 * l + 1, t, pl.ds(pl.multiple_of(h * 2, 2), 2)], w2_v.at[slot]),
                    (pre_in.at[l, :, whole], pre_v.at[slot])]

        def outs(i, slot):
            return [(dp_v.at[slot], dpre.at[l, :, pl.ds(pl.multiple_of(i * BLK, BLK), BLK)])]

        def channel(i, slot):
            _, slope = gelu_both(pre_v[slot])
            d = dot_nt(do_v[...], w2_v[slot].reshape(BLK, CH)) * slope
            gbch1[l:l + 1, pl.ds(pl.multiple_of(i * BLK, BLK), BLK)] = jnp.sum(d, axis=0, keepdims=True)
            dp_v[slot] = d.astype(bf16)
            part = dot_nt(dp_v[slot], w1_v[slot].reshape(CH, BLK))

            @pl.when(i == 0)
            def _():
                dv_v[...] = part

            @pl.when(i > 0)
            def _():
                dv_v[...] += part
        for_blocks(Stream(sem_w, blocks, NBLK), channel, Stream(sem_o, outs, NBLK))
        load.wait()
        send.wait()

        @pl.loop(0, IMG)
        def _(b):
            std, inv = standardize(x_v[image(b), :])
            d = dv_v[image(b), :]
            add(r + 2, d * std)
            add(r + 3, d)
            d_v[image(b), :] += norm_grad(d, vec[r + 2:r + 3, :], std, inv)
        load = pltpu.make_async_copy(xin.at[l], x_v, sem.at[0])
        load.start()
        load.wait()

        @pl.loop(0, IMG)
        def _(b):
            std, inv = standardize(x_v[image(b), :])
            a = with_bias_rows(std * vec[r:r + 1, :] + vec[r + 1:r + 2, :])
            d_mid = d_v[image(b), :]
            dm = d_mid.astype(bf16)
            act, slope = gelu_both(dot_nn(wt[l, :, 0:TPAD], a))
            g_v[...] = act.astype(bf16)
            dh = dot_nn(wt[2 + l, :, 0:TPAD], dm) * slope
            gbt[l] += jnp.sum(dh, axis=-1, keepdims=True)
            dh_v[...] = dh.astype(bf16)
            gt2[l] += dot_nt(g_v[...], dm)
            gt1[l] += dot_nt(dh_v[...], a)
            d = jnp.where(mask, dot_tn(wt[l, :, 0:TPAD], dh_v[...]), 0.0)
            add(r, d * std)
            add(r + 1, d)
            d_v[image(b), :] = d_mid + norm_grad(d, vec[r:r + 1, :], std, inv)

    @pl.loop(0, IMG // 2)
    def _(p):
        d = d_v[pair(p), :]
        add(0, d)
        do_v[pair(p), :] = d.astype(bf16)
    send = pltpu.make_async_copy(do_v, dstem, sem.at[1])
    send.start()
    send.wait()


def backward(*operands):
    a, v = pl.BlockSpec(memory_space=pl.ANY), pl.BlockSpec(memory_space=pltpu.VMEM)
    S = jax.ShapeDtypeStruct
    return pl.pallas_call(
        backward_kernel, name='backward',
        in_specs=[a] * 4 + [v] * 3,
        out_specs=[a] * 3 + [v] * 5,
        out_shape=[S((2, ROWS, CHH), bf16), S((2, ROWS, CH), bf16), S((ROWS, CH), bf16), S((16, CH), f32), S((2, CHH), f32),
                   S((2, TOKH, TPAD), f32), S((2, TOKH, TPAD), f32), S((2, TOKH, 1), f32)],
        scratch_shapes=[pltpu.VMEM((ROWS, CH), f32), pltpu.VMEM((ROWS, CH), f32), pltpu.VMEM((ROWS, CH), f32),
                        pltpu.VMEM((ROWS, CH), bf16), pltpu.VMEM((2, 4, 4, 2, 32, BLK), bf16),
                        pltpu.VMEM((2, 2, 4, 2, 32, CH), bf16),
                        pltpu.VMEM((2, ROWS, BLK), f32), pltpu.VMEM((2, ROWS, BLK), bf16), pltpu.VMEM((TOKH, CH), bf16),
                        pltpu.VMEM((TOKH, CH), bf16), pltpu.SemaphoreType.DMA((2,)), pltpu.SemaphoreType.DMA((2, 3)),
                        pltpu.SemaphoreType.DMA((2, 1))],
        compiler_params=pltpu.CompilerParams(vmem_limit_bytes=60 * 1024 * 1024),
        cost_estimate=pl.CostEstimate(flops=50_000_000_000, bytes_accessed=100_000_000, transcendentals=0),
    )(*operands)


FRONT_COPIES = 240
EARLY = [('stem', 0), ('stem', 1), ('stem', 2), ('ch', 0), ('ch', 1), ('ch', 2), ('head', 2)]
LATE = [('stem', c, None) for c in range(3)] + [('ch', c, g) for g in range(N_CH) for c in range(3)] + [('head', 2, None)]
UNIT_GROUP = {('stem', None): 0, ('ch', 0): 1, ('ch', 1): 2, ('ch', 2): 3, ('ch', 3): 4, ('head', None): 5}
EVERY = pl.ds(0, 4)
FRONT_ORDER = (
    ('prep', (('M0', ('sm',)), ('M0', ('tk',)), ('A0', ('stem', 0)), ('A0', ('stem', 1)), ('A0', ('stem', 2)),
        ('A0', ('ch', 0)), ('A0', ('ch', 1)), ('A0', ('ch', 2)), ('A0', ('head', 2)),)),
    ('unpack', (('M1', ('sm',)), ('M1', ('tk',)), ('A', ('stem', 0)), ('A', ('stem', 1)), ('A', ('stem', 2)),
        ('A', ('head', 2)), ('A', ('ch', 2)), ('A', ('ch', 0)), ('A', ('ch', 1)), ('B', ('stem', 0)), ('M2', ('sm',)),
        ('B', ('stem', 1)), ('M2', ('tk',)), ('B', ('stem', 2)), ('B', ('ch', 0)), ('B', ('head', 2)), ('B', ('ch', 1)),
        ('C', ('stem', 0)), ('B', ('ch', 2)), ('M3', ('sm',)), ('C', ('stem', 2)), ('C', ('stem', 1)), ('C', ('head', 2)),)),
    ('stem0', (('D', ('stem', 2, None)), ('D', ('stem', 0, None)), ('C', ('ch', 2)), ('C', ('ch', 0)),
        ('D', ('stem', 1, None)), ('C', ('ch', 1)), ('D', ('ch', 2, 0)), ('D', ('ch', 2, 1)), ('E', ('stem', 2, None)),
        ('E', ('stem', 0, None)), ('E', ('stem', 1, None)), ('D', ('ch', 0, 0)), ('D', ('ch', 0, 1)), ('D', ('ch', 1, 0)),
        ('D', ('ch', 1, 1)), ('F', ('stem', 0, None)), ('F', ('stem', 1, None)), ('E', ('ch', 2, 0)), ('E', ('ch', 2, 1)),
        ('E', ('ch', 0, 0)), ('E', ('ch', 1, 0)), ('F', ('stem', 2, None)), ('F', ('ch', 2, 0)),)),
    ('stem1', (('F', ('ch', 2, 1)), ('E', ('ch', 0, 1)), ('E', ('ch', 1, 1)), ('D', ('ch', 0, 2)), ('D', ('ch', 1, 2)),
        ('D', ('ch', 2, 2)), ('D', ('ch', 0, 3)), ('D', ('ch', 1, 3)), ('D', ('ch', 2, 3)),)),
    ('stem3', (('F', ('ch', 0, 0)),)),
    ('tok0_0', (('F', ('ch', 1, 0)),)),
    ('tok0_3', (('F', ('ch', 0, 1)),)),
    ('tok0_4', (('F', ('ch', 1, 1)),)),
    ('tok0_5', (('E', ('ch', 2, 2)),)),
    ('ch0_0', (('E', ('ch', 2, 3)), ('E', ('ch', 0, 2)), ('E', ('ch', 1, 2)), ('F', ('ch', 2, 2)),)),
    ('ch0_3', (('F', ('ch', 2, 3)),)),
    ('ch0_5', (('E', ('ch', 0, 3)), ('E', ('ch', 1, 3)), ('D', ('head', 2, None)),)),
    ('ch0_7', (('F', ('ch', 0, 2)), ('F', ('ch', 1, 2)),)),
    ('tok1_2', (('F', ('ch', 0, 3)),)),
    ('tok1_3', (('F', ('ch', 1, 3)), ('E', ('head', 2, None)),)),
    ('ln1', (('F', ('head', 2, None)),)),
)


class Net:
    def __init__(self, send_sems, recv_sems):
        self.send_sems, self.recv_sems, self.names, self.builds = send_sems, recv_sems, {}, []

    def copy(self, name):
        n = self.names[name]
        src, dst, target = self.builds[n]()
        return pltpu.make_async_remote_copy(src_ref=src, dst_ref=dst, send_sem=self.send_sems.at[n],
                                            recv_sem=self.recv_sems.at[n], device_id=target, device_id_type=MESH)

    def start(self, name, build):
        self.names[name] = len(self.builds)
        self.builds.append(build)
        self.copy(name).start()

    def arrived(self, *names):
        for name in names:
            self.copy(name).wait_recv()

    def finish(self):
        for name in self.names:
            self.copy(name).wait_send()


def three_parts(x):
    hi = x.astype(bf16)
    rest = x - hi.astype(f32)
    mid = rest.astype(bf16)
    return hi, mid, (rest - mid.astype(f32)).astype(bf16)


def with_bias_rows(a):
    row = lax.broadcasted_iota(jnp.int32, (TPAD, 1), 0)
    return jnp.where(row < TOK, a, jnp.where(row < TOK + 3, 1.0, 0.0)).astype(bf16)


def front_kernel(labels, patches, w_stem, w_ch1, w_ch2, w_head, w_tok1, w_tok2, b_tok1, b_ch1, b_head, vecs,
                 wc, pat_out, xin, xmid, vout, pre_out, act_out, hl, hr, dx0, hstat, gbh, vec, wt,
                 pc, ps, ph, tk_f, tk_p, sm_p, bh_p, ws, wh, tk_v, sm_v, sm_2, bh_v, bch1,
                 stage_v, pair_v, p_v, x_v, v_v, w1_v, w2_v, pre_v, act_v, g_v,
                 send_sems, recv_sems, sem, sem_w, sem_o, sem_x):
    me = my_place()
    other = moved(me, 'k', 1)
    load_p = pltpu.make_async_copy(patches.at[pl.ds(me['x'] * IMG, IMG)], stage_v, sem.at[0])
    load_p.start()

    for l in range(2):
        pc[2 * l] = w_ch1[l].astype(bf16)
        pc[2 * l + 1] = w_ch2[l].astype(bf16)
    ps[...] = w_stem[...].astype(bf16)
    ph[...] = jnp.zeros_like(ph)
    ph[:, pl.ds(0, 250)] = w_head[...].astype(bf16)
    tk_f[...] = jnp.zeros_like(tk_f)
    for l in range(2):
        tk_f[l, :, pl.ds(0, TOK)] = w_tok1[l]
        tk_f[2 + l, :, pl.ds(0, TOK)] = w_tok2[l]
        for n, part in enumerate(three_parts(b_tok1[l])):
            tk_f[l, :, pl.ds(TOK + n, 1)] = part.astype(f32)
    tk_p[...] = tk_f[...].astype(bf16)
    sm_p[...] = jnp.zeros_like(sm_p)
    sm_p[:, pl.ds(0, 13)] = vecs[...]
    sm_p[pl.ds(0, 2), pl.ds(32, 32)] = b_ch1[...]
    bh_p[...] = jnp.full_like(bh_p, -1e30)
    bh_p[pl.ds(0, 1), pl.ds(0, 250)] = b_head[...]

    barrier = pltpu.get_barrier_semaphore()
    for dim in 'xyz':
        for step in (1, 2, 3):
            pl.semaphore_signal(barrier, inc=1, device_id=device(moved(me, dim, step)), device_id_type=MESH)
    pl.semaphore_signal(barrier, inc=1, device_id=device(other), device_id_type=MESH)
    net = Net(send_sems, recv_sems)
    core = me['k']
    ring = {d: [moved(me, d, n)[d] for n in range(4)] for d in 'xyz'}
    columns = [pl.ds(pl.multiple_of(x * 256, 256), 256) for x in ring['x']]
    peers = {(d, n): device(moved(me, d, n)) for d in 'xyz' for n in (1, 2, 3)}
    partner = device(other)
    here = {'x': 0, 'y': 0, 'z': 0}

    def view(unit, block, half=None):
        kind, colour = unit[:2]
        x, z, y = (EVERY if block[d] is None else ring[d][block[d]] for d in 'xzy')
        r0, rn = (0, 32) if half is None else (16 * half, 16)
        if kind == 'ch':
            c0, cn = COLS[colour]
            g = EVERY if len(unit) == 2 else unit[2]
            return wc.at[g, x, z, y, core, pl.ds(r0, rn), pl.ds(c0, cn)]
        cols = pl.ds(0, CH) if x is EVERY else columns[block['x']]
        if kind == 'stem':
            return ws.at[z, y, core, pl.ds(32 * colour + r0, rn), cols]
        return wh.at[z, y, core, pl.ds(r0, rn), cols]

    def piece(unit):
        kind, colour = unit
        if kind == 'ch':
            return pc.at[:, :, pl.ds(*COLS[colour])]
        return ps.at[pl.ds(32 * colour, 32), :] if kind == 'stem' else ph.at[:, :]

    def exchange(unit, tag, dim, block):
        for side, step in (('l', 1), ('r', 3)):
            def build(step=step):
                part = view(unit, block)
                return (piece(unit) if tag == '1' else part), part, peers[dim, step]
            net.start((unit, tag, side), build)

    def forward_half(unit, tag, dim, block):
        for half, (origin, target, side) in enumerate(((3, 1, 'l'), (1, 3, 'r'))):
            def build(half=half, origin=origin, target=target):
                part = view(unit, {**block, dim: origin}, half)
                return part, part, peers[dim, target]
            net.start((unit, tag, side), build)

    def swap(unit, tag, block):
        def build():
            part = view(unit, block)
            return part, part, partner
        net.start((unit, tag), build)

    own = pltpu.make_async_copy(pc, wc.at[:, me['x'], me['z'], me['y'], me['k']], sem.at[1])
    own.start()
    mine = pl.ds(pl.multiple_of(me['x'] * 256, 256), 256)
    ws[me['z'], me['y'], me['k'], :, mine] = ps[...]
    wh[me['z'], me['y'], me['k'], :, mine] = ph[...]
    sm_v[me['x'], me['z'], me['y'], me['k']] = sm_p[...]
    tk_v[:, me['z'], me['y'], me['k']] = tk_p[...]
    bh_v[:, mine] = bh_p[...]
    own.wait()
    pl.semaphore_wait(barrier, 10)

    def small(kind, n):
        dims = 'xyz' if kind == 'sm' else 'yz'
        at = {d: EVERY if d in dims[:n] else ring[d][0] for d in 'xyz'}

        def part():
            if kind == 'sm':
                return sm_v.at[at['x'], at['z'], at['y'], core]
            return tk_v.at[:, at['z'], at['y'], core]
        if n > 0:
            net.arrived(*[(kind, n - 1, s) for s in (1, 2, 3)])
        if n < len(dims):
            for s in (1, 2, 3):
                net.start((kind, n, s), lambda s=s: (part(), part(), peers[dims[n], s]))
            if kind == 'sm' and n == 0:
                def head_bias():
                    return bh_v.at[:, columns[0]]
                for s in (1, 2, 3):
                    net.start(('bh', s), lambda s=s: (head_bias(), head_bias(), peers['x', s]))
        else:
            net.start((kind, 'k'), lambda: (part(), part(), partner))

    def step(name, unit):
        if name[0] == 'M':
            small(unit[0], int(name[1]))
            return
        d1, d2, d3 = ORDERS[unit[1]]
        early = unit[:2]
        plane = {**here, d1: None, d2: None}
        if name == 'A0':
            exchange(unit, '1', d1, here)
        elif name == 'A':
            net.arrived((unit, '1', 'l'), (unit, '1', 'r'))
            forward_half(unit, '1h', d1, here)
        elif name == 'B':
            net.arrived((unit, '1h', 'l'), (unit, '1h', 'r'))
            exchange(unit, '2', d2, {**here, d1: None})
        elif name == 'C':
            net.arrived((unit, '2', 'l'), (unit, '2', 'r'))
            forward_half(unit, '2h', d2, {**here, d1: None})
        elif name == 'D':
            if early not in planes:
                planes.add(early)
                net.arrived((early, '2h', 'l'), (early, '2h', 'r'))
            exchange(unit, '3', d3, plane)
            swap(unit, 'k0', plane)
        elif name == 'E':
            net.arrived((unit, '3', 'l'), (unit, '3', 'r'))
            forward_half(unit, '3h', d3, plane)
            for n in (1, 3):
                swap(unit, f'k{n}', {**plane, d3: n})
        else:
            net.arrived((unit, '3h', 'l'), (unit, '3h', 'r'))
            swap(unit, 'k2', {**plane, d3: 2})

    planes = set()
    awaited = set()

    def need(group):
        for u in LATE:
            if UNIT_GROUP[u[0], u[2]] <= group and u not in awaited:
                awaited.add(u)
                net.arrived(*[(u, f'k{n}') for n in range(4)])

    bursts = {name: steps for name, steps in FRONT_ORDER}

    def burst(name):
        for s in bursts.get(name, ()):
            step(*s)

    def during(name, count):
        def run(i):
            for n in range(1, count):
                if bursts.get(f'{name}{n}'):
                    pl.when(i == n)(functools.partial(burst, f'{name}{n}'))
        return run

    burst('prep')
    load_p.wait()
    pair_v[...] = jnp.zeros_like(pair_v)

    @pl.loop(0, IMG // 2)
    def _(p):
        for n in range(2):
            pair_v[pl.ds(TPAD * n, TOK), :] = stage_v[2 * p + n].astype(f32)
        p_v[pair(p), :] = pair_v[...].astype(bf16)
    keep_p = pltpu.make_async_copy(p_v, pat_out, sem.at[0])
    keep_p.start()

    burst('unpack')
    net.arrived(('sm', 'k'), ('tk', 'k'), ('bh', 1), ('bh', 2), ('bh', 3))
    sm_2[...] = sm_v[...].reshape(1024, 128)
    for n in range(8):
        vec[:, pl.ds(128 * n, 128)] = sm_2[pl.ds(128 * n, 128), :].T[0:16, :]
    wt[...] = tk_v[...].reshape(4, TOKH, 128)
    for l in range(2):
        rows = jnp.concatenate(three_parts(sm_2[pl.ds(l, 128, stride=8), :]), axis=0)

        @pl.loop(0, 8)
        def _(n):
            lane = lax.broadcasted_iota(jnp.int32, (128, 512), 0)
            col = lax.broadcasted_iota(jnp.int32, (128, 512), 1)
            pick = jnp.where(lane == 32 + col % 32, 1.0, 0.0).astype(bf16)
            spread = dot_nn(rows, pick)
            value = spread[0:128] + spread[128:256] + spread[256:384]
            mine = lane == n * 16 + col // 32
            bch1[l:l + 1, pl.ds(pl.multiple_of(n * 512, 512), 512)] = jnp.sum(jnp.where(mine, value, 0.0), axis=0, keepdims=True)

    burst('stem0')
    need(0)
    mask_all = (lax.broadcasted_iota(jnp.int32, (ROWS, 1), 0) % TPAD) < TOK
    run = during('stem', 4)

    @pl.loop(0, 4)
    def _(i):
        run(i)
        cols = pl.ds(pl.multiple_of(i * 256, 256), 256)
        w = ws[:, :, :, :, cols].reshape(3072, 256)
        x_v[:, cols] = jnp.where(mask_all, dot_nn(p_v[...], w) + vec[0:1, cols], 0.0)

    wc_all = wc
    for l in range(2):
        r = 1 + 5 * l
        burst(f'tok{l}_0')
        run = during(f'tok{l}_', IMG)
        save_in = pltpu.make_async_copy(x_v, xin.at[l], sem_x.at[0])
        save_in.start()
        save_in.wait()

        @pl.loop(0, IMG)
        def _(b):
            run(b)
            x = x_v[image(b), :]
            std, _ = standardize(x)
            a = with_bias_rows(std * vec[r:r + 1, :] + vec[r + 1:r + 2, :])
            g_v[...] = gelu(dot_nn(wt[l, :, 0:TPAD], a)).astype(bf16)
            x_v[image(b), :] = x + dot_tn(wt[2 + l, :, 0:TPAD], g_v[...])
        save_mid = pltpu.make_async_copy(x_v, xmid.at[l], sem_x.at[0])
        save_mid.start()
        burst(f'ln{l}')

        @pl.loop(0, IMG // 2)
        def _(p):
            std, _ = standardize(x_v[pair(p), :])
            v_v[pair(p), :] = (std * vec[r + 2:r + 3, :] + vec[r + 3:r + 4, :]).astype(bf16)
        save_v = pltpu.make_async_copy(v_v, vout.at[l], sem_x.at[1])
        save_v.start()
        burst(f'ch{l}_0')
        need(2 + 2 * l)
        save_mid.wait()

        def blocks(i, slot):
            t, h = i // 2, i % 2
            part = pl.ds(pl.multiple_of(h * BLK, BLK), BLK)
            half = [pl.ds(pl.multiple_of(h * 2, 2), 2)]
            return [(wc_all.at[2 * l, t, :, :, :, :, part], w1_v.at[slot]), (wc_all.at[2 * l + 1, t, *half], w2_v.at[slot])]

        def outs(i, slot):
            part = pl.ds(pl.multiple_of(i * BLK, BLK), BLK)
            return [(pre_v.at[slot], pre_out.at[l, :, part]), (act_v.at[slot], act_out.at[l, :, part])]
        run = during(f'ch{l}_', NBLK)

        def channel(i, slot):
            run(i)
            part = pl.ds(pl.multiple_of(i * BLK, BLK), BLK)
            h = dot_nn(v_v[...], w1_v[slot].reshape(CH, BLK)) + bch1[l:l + 1, part]
            pre_v[slot] = h
            act_v[slot] = gelu(h).astype(bf16)
            x_v[...] += dot_nn(act_v[slot], w2_v[slot].reshape(BLK, CH))
        for_blocks(Stream(sem_w, blocks, NBLK), channel, Stream(sem_o, outs, NBLK))
        x_v[...] += vec[r + 4:r + 5, :]
        save_v.wait()

    burst('head')
    need(5)
    keep_p.wait()
    last = 11
    mask = row_mask()
    pooled = jnp.concatenate([jnp.sum(jnp.where(mask, x_v[b * TPAD:(b + 1) * TPAD, :], 0.0), axis=0, keepdims=True)
                              for b in range(IMG)], axis=0) * (1.0 / TOK)
    std, inv = standardize(pooled)
    head_in = (std * vec[last:last + 1, :] + vec[last + 1:last + 2, :]).astype(bf16)
    hl[...] = head_in
    w_h = wh[...].reshape(CH, CH)
    logits = dot_nn(head_in, w_h) + bh_v[0:1, :]
    row = lax.broadcasted_iota(jnp.int32, (IMG, 1), 0)
    label = jnp.zeros((IMG, 1), jnp.int32)
    for b in range(IMG):
        value = labels[me['x'] * IMG + b]
        label = jnp.where(row == b, value, label)
    label = label + 6 * sum(jnp.where(label >= edge, 1, 0) for edge in (250, 500, 750))
    is_label = lax.broadcasted_iota(jnp.int32, logits.shape, 1) == label
    top = jnp.max(logits, axis=-1, keepdims=True)
    ex = jnp.exp(logits - top)
    es = jnp.sum(ex, axis=-1, keepdims=True)
    nll = top + jnp.log(es) - jnp.sum(jnp.where(is_label, logits, 0.0), axis=-1, keepdims=True)
    d_logits = (ex / es - jnp.where(is_label, 1.0, 0.0)) * (1.0 / 1024)
    gbh[...] = jnp.sum(d_logits, axis=0, keepdims=True)
    d_bf = d_logits.astype(bf16)
    hr[...] = d_bf
    d_in = dot_nt(d_bf, w_h)
    hstat[0:1, :] = jnp.sum(d_in * std, axis=0, keepdims=True)
    hstat[1:2, :] = jnp.sum(d_in, axis=0, keepdims=True)
    hstat[2:3, :] = jnp.broadcast_to(jnp.sum(nll, axis=0, keepdims=True), (1, CH))
    dx0[...] = norm_grad(d_in, vec[last:last + 1, :], std, inv) * (1.0 / TOK)
    burst('end')
    net.finish()
    assert len(net.builds) <= FRONT_COPIES, len(net.builds)


def front(*operands):
    a, v = pl.BlockSpec(memory_space=pl.ANY), pl.BlockSpec(memory_space=pltpu.VMEM)
    S, V, DMA = jax.ShapeDtypeStruct, pltpu.VMEM, pltpu.SemaphoreType.DMA
    return pl.pallas_call(
        front_kernel, name='front',
        in_specs=[pl.BlockSpec(memory_space=pltpu.SMEM), a] + [v] * 10,
        out_specs=[a] * 7 + [v] * 7,
        out_shape=[S((N_CH, 4, 4, 4, 2, 32, 1024), bf16), S((ROWS, 3072), bf16), S((2, ROWS, CH), f32), S((2, ROWS, CH), f32),
                   S((2, ROWS, CH), bf16), S((2, ROWS, CHH), f32), S((2, ROWS, CHH), bf16), S((IMG, CH), bf16),
                   S((IMG, CH), bf16), S((IMG, CH), f32), S((8, CH), f32), S((1, CH), f32), S((16, CH), f32),
                   S((4, TOKH, 128), bf16)],
        scratch_shapes=[V((N_CH, 32, 1024), bf16), V((96, 256), bf16), V((32, 256), bf16), V((4, 16, 128), f32),
                        V((4, 16, 128), bf16), V((8, 128), f32), V((8, 256), f32), V((4, 4, 2, 96, CH), bf16),
                        V((4, 4, 2, 32, CH), bf16), V((4, 4, 4, 2, 16, 128), bf16), V((4, 4, 4, 2, 8, 128), f32),
                        V((1024, 128), f32), V((8, CH), f32), V((2, CHH), f32),
                        V((IMG, TOK, 3072), bf16), V((2 * TPAD, 3072), f32), V((ROWS, 3072), bf16), V((ROWS, CH), f32),
                        V((ROWS, CH), bf16), V((2, 4, 4, 2, 32, BLK), bf16), V((2, 2, 4, 2, 32, CH), bf16),
                        V((2, ROWS, BLK), f32), V((2, ROWS, BLK), bf16), V((TOKH, CH), bf16),
                        DMA((FRONT_COPIES,)), DMA((FRONT_COPIES,)), DMA((2,)), DMA((2, 2)), DMA((2, 2)), DMA((2,))],
        compiler_params=pltpu.CompilerParams(collective_id=0, has_side_effects=True, vmem_limit_bytes=62 * 1024 * 1024),
        cost_estimate=pl.CostEstimate(flops=90_000_000_000, bytes_accessed=180_000_000, transcendentals=0),
    )(*operands)

CHANNEL_AXES = ('tp', 'fsdp')


def weight_specs():
    vec_spec = P(CHANNEL_AXES)
    layer_vec = P(None, CHANNEL_AXES)
    return (P('fsdp', 'tp'), vec_spec, layer_vec, layer_vec, P(None, None, 'fsdp'), P(None, 'fsdp'),
            P(None, 'fsdp', None), layer_vec, layer_vec, P(None, 'fsdp', 'tp'), layer_vec,
            P(None, CHANNEL_AXES, None), layer_vec, vec_spec, vec_spec, P('fsdp', 'tp'), P('tp'))


def solution(mesh):
    fs = mesh.shape['fsdp']
    tp = mesh.shape['tp']
    nd = fs * tp

    def step(patches, labels, w_stem, b_stem, ln1_g, ln1_b, w_tok1, b_tok1, w_tok2,
             ln2_g, ln2_b, w_ch1, b_ch1, w_ch2, b_ch2, lnf_g, lnf_b, w_head, b_head):
        t = lax.axis_index('tp')
        nl = w_tok1.shape[0]
        total_images = IMG * nd
        vecs = [b_stem[None]]
        for l in range(nl):
            vecs += [a[l:l + 1] for a in (ln1_g, ln1_b, ln2_g, ln2_b, b_ch2)]
        vecs = jnp.concatenate(vecs + [lnf_g[None], lnf_b[None]], axis=0).T
        classes = w_head.shape[1]
        wc, pat, xin, xmid, vin, pre, act, hl, hr, dx0, hstat, gbh, vec, wt = front(
            labels, patches, w_stem, w_ch1, w_ch2, w_head, w_tok1.transpose(0, 2, 1), w_tok2, b_tok1[:, :, None], b_ch1,
            b_head[None], vecs)
        dpre, dout, dstem, gvec, gbch1, gt1, gt2, gbt = backward(xin, xmid, pre, wc, wt, vec, dx0)

        gvec = jnp.concatenate([gvec[:11], hstat[:2]], axis=0)
        parts = [gvec, gbch1, gbt[:, :, 0], gbh, gt1, gt2, hstat[2, :1]]
        flat = jnp.concatenate([p.reshape(-1) for p in parts])
        flat = jnp.pad(flat, (0, (-flat.shape[0]) % 1024))
        tot = lax.psum(flat, CHANNEL_AXES)

        g_c, g_s, g_h = reduce_gradients(dpre, act, pat, vin, dout, dstem, hl, hr)

        out = []
        o = 0
        for p in parts:
            out.append(tot[o:o + p.size].reshape(p.shape))
            o += p.size
        f = lax.axis_index('fsdp')

        def own(x, n, i, ax):
            size = x.shape[ax] // n
            return lax.dynamic_slice_in_dim(x, i * size, size, ax)
        dev = t * fs + f
        gv = own(out[0], nd, dev, 1)
        gc1 = own(out[1], nd, dev, 1)
        gtb = own(out[2], fs, f, 1)
        gbh = own(out[3].reshape(tp, 256), tp, t, 0)[0, :classes]
        gw1 = own(out[4], fs, f, 1)[:, :, :TOK].transpose(0, 2, 1)
        gw2 = own(out[5], fs, f, 1)[:, :, :TOK]
        loss = out[6][0] / total_images
        per = [jnp.stack([gv[1 + i], gv[6 + i]]) for i in range(5)]
        return (loss, g_s, gv[0], per[0], per[1], gw1, gtb, gw2, per[2], per[3], g_c[0::2], gc1, g_c[1::2], per[4],
                gv[11], gv[12], g_h[:, :classes], gbh)

    specs = weight_specs()
    return jax.shard_map(step, mesh=mesh, in_specs=(P('fsdp', None, None), P('fsdp')) + specs,
                         out_specs=(P(),) + specs, check_vma=False)
```

```python
import functools

import jax
import jax.numpy as jnp
from jax import lax
from jax.experimental import pallas as pl
from jax.experimental.pallas import tpu as pltpu
from jax.sharding import PartitionSpec as P

MESH = pl.DeviceIdType.MESH
ORDERS = (('x', 'y', 'z'), ('y', 'z', 'x'), ('z', 'x', 'y'))
COLS = ((0, 384), (384, 384), (768, 256))
N_CH = 4
STEM, HEAD = 4, 5
bf16, f32 = jnp.bfloat16, jnp.float32


def my_place():
    f = lax.axis_index('fsdp')
    return {'x': lax.axis_index('tp'), 'z': f // 8, 'y': (f // 2) % 4, 'k': f % 2}


def moved(place, dim, step):
    new = dict(place)
    new[dim] = 1 - place['k'] if dim == 'k' else (place[dim] + step) % 4
    return new


def device(place):
    return {'tp': place['x'], 'fsdp': (place['z'] * 4 + place['y']) * 2 + place['k']}


def meet_neighbours(me):
    barrier = pltpu.get_barrier_semaphore()
    for dim in 'xyz':
        for step in (1, 3):
            pl.semaphore_signal(barrier, inc=1, device_id=device(moved(me, dim, step)), device_id_type=MESH)
    pl.semaphore_signal(barrier, inc=1, device_id=device(moved(me, 'k', 1)), device_id_type=MESH)
    pl.semaphore_wait(barrier, 7)


class Sender:
    def __init__(self, send_sems, recv_sems):
        self.send_sems, self.recv_sems, self.count, self.started = send_sems, recv_sems, 0, []

    def start(self, src, dst, target):
        n = self.count
        self.count += 1
        copy = pltpu.make_async_remote_copy(src_ref=src, dst_ref=dst, send_sem=self.send_sems.at[n],
                                            recv_sem=self.recv_sems.at[n], device_id=device(target),
                                            device_id_type=MESH)
        copy.start()
        self.started.append(copy)
        return copy


GROUPS = (STEM, 3, 2, 1, 0, HEAD)
UNITS = tuple((g, c) for g in GROUPS for c in (2, 0, 1) if g != HEAD or c == 2)
REDUCE_COPIES = 13 * len(UNITS)
ORDER = (0, 1, 2, 3, 4, 0, 5, 1, 2, 0, 3, 1, 2, 0, 4, 6, 3, 1, 7, 5, 0, 6, 4, 1, 2, 8, 0, 6, 7, 5, 2, 3, 1, 9, 0, 8, 4, 10, 7, 9, 1, 2,
         3, 0, 5, 11, 8, 9, 10, 1, 4, 5, 2, 11, 3, 6, 12, 10, 2, 5, 8, 6, 4, 7, 13, 11, 12, 3, 4, 7, 8, 14, 5, 12, 6, 13, 4, 9,
         15, 5, 8, 11, 3, 14, 13, 6, 7, 8, 9, 10, 11, 15, 7, 14, 6, 11, 10, 15, 7, 8, 9, 12, 11, 12, 14, 11, 10, 9, 13, 12, 15,
         14, 10, 9, 13, 12, 15, 14, 10, 13, 15, 12, 14, 13, 15, 14, 15, 13)


def reduce_scratch():
    per = []
    for c in range(3):
        n = COLS[c][1]
        many = sum(1 for u in UNITS if u[1] == c)
        lead = ((4, 4), (4,), ())
        b = {'C': pltpu.VMEM((2, 4, 4, 4, 2, 32, n), bf16), 'D': pltpu.VMEM((2, 4, 4, 4, 32, n), bf16),
             'S1': pltpu.VMEM((4, 4, 32, n), f32), 'S2': pltpu.VMEM((3, 4, 32, n), f32)}
        for ph in range(3):
            for name in ('opp', 'rig', 'lef'):
                b[f'{name}{ph}'] = pltpu.VMEM(lead[ph] + (32, n), bf16)
            for name in ('half0', 'half1'):
                b[f'{name}{ph}'] = pltpu.VMEM((many,) + lead[ph] + (16, n), bf16)
            for name in ('froml', 'fromr'):
                b[f'{name}{ph}'] = pltpu.VMEM((many,) + lead[ph] + (32, n), bf16)
        per.append(b)
    return per


def transposed_product(left, right):
    return lax.dot_general(left, right, (((0,), (0,)), ((), ())), preferred_element_type=f32)


def reduce_kernel(*refs):
    dpre, act, pat, vin, dout, dstem, head_l, head_r = refs[:8]
    wides = [dpre.at[0], act.at[0], dpre.at[1], act.at[1], pat]
    narrows = [vin.at[0], dout.at[0], vin.at[1], dout.at[1], dstem]
    out_c, out_s, out_h = refs[8:11]
    wide, narrow, per, send_sems, recv_sems, load_sems, credit = refs[11:]
    me = my_place()
    other = moved(me, 'k', 1)
    k = me['k']
    loads = {}

    def load(i):
        g = GROUPS[i]
        if g == HEAD:
            return
        cols = 3072 if g == STEM else 4096
        loads[g] = [pltpu.make_async_copy(wides[g], wide.at[i % 2, :, pl.ds(0, cols)], load_sems.at[i % 2, 0]),
                    pltpu.make_async_copy(narrows[g], narrow.at[i % 2], load_sems.at[i % 2, 1])]
        for copy in loads[g]:
            copy.start()

    load(0)
    meet_neighbours(me)
    sender = Sender(send_sems, recv_sems)
    busy = {}

    def free(key):
        for copy in busy.pop(key, ()):
            copy.wait_send()

    def make(g, c, cslot):
        i = GROUPS.index(g)
        slot = i % 2
        if g != HEAD and c == 2:
            for copy in loads[g]:
                copy.wait()
            load(i + 1)
        if g == STEM:
            if c != 2:
                return
            @pl.loop(0, 32)
            def _(j):
                b = j // 4
                t = j % 4
                z, y2 = b // 2, b % 2
                left = wide[slot, :, pl.ds(pl.multiple_of(b * 384, 128), 384)]
                right = narrow[slot, :, pl.ds(pl.multiple_of(t * 256, 128), 256)]
                prod = transposed_product(left, right).astype(bf16).reshape(2, 2, 3, 32, 256)
                for d in range(3):
                    per[d]['C'][0, t, z, pl.ds(y2 * 2, 2), :, :, pl.ds(0, 256)] = prod[:, :, d]
        elif g == HEAD:

            @pl.loop(0, 4)
            def _(t):
                right = head_r[:, pl.ds(pl.multiple_of(t * 256, 128), 256)]
                prod = transposed_product(head_l[...], right)
                per[c]['C'][cslot, t] = prod.astype(bf16).reshape(4, 4, 2, 32, 256)
        else:
            c0, n = COLS[c]

            @pl.loop(0, 16)
            def _(j):
                t, z = j // 4, j % 4
                if g % 2 == 0:
                    left = narrow[slot, :, pl.ds(pl.multiple_of(z * 256, 128), 256)]
                    right = wide[slot, :, pl.ds(pl.multiple_of(t * 1024 + c0, 128), n)]
                else:
                    left = wide[slot, :, pl.ds(pl.multiple_of(j * 256, 128), 256)]
                    right = narrow[slot, :, pl.ds(c0, n)]
                per[c]['C'][cslot, t, z] = transposed_product(left, right).astype(bf16).reshape(4, 2, 32, n)

    class Unit:
        def __init__(self, g, c):
            self.g, self.c = g, c
            same = [u for u in UNITS if u[1] == c]
            self.index = same.index((g, c))
            self.slot = self.index % 2
            self.last = self.index >= len(same) - 2
            self.n = COLS[c][1] if g < N_CH else 256
            self.buf = per[c]
            self.dims = ORDERS[c]

        def cut(self, name, *at):
            ref = self.buf[name]
            rest = len(ref.shape) - len(at) - 1
            return ref.at[(*at, *[slice(None)] * rest, pl.ds(0, self.n))]

        def share(self, phase, p, e, rows):
            r = pl.ds(*rows)
            cols = pl.ds(0, self.n)
            if phase == 0:
                at = dict(zip(self.dims, (p, *e)))
                at = (at['x'], at['z'], at['y'])
                return (self.buf['C'][(self.slot, *at, k, r, cols)].astype(f32)
                        + self.buf['D'][(self.slot, *at, r, cols)].astype(f32))
            lead = () if phase == 1 else (self.index % 3,)
            return self.buf[f'S{phase}'][(*lead, p, *e, r, cols)]

        def each(self, phase, body):
            if phase == 2:
                body(())
            elif phase == 1:
                pl.loop(0, 4)(lambda i: body((i,)))
            else:
                pl.loop(0, 16)(lambda i: body((i // 4, i % 4)))

        def start(self):
            free(('C', self.c, self.slot))
            make(self.g, self.c, self.slot)
            if self.index > 1:
                pl.semaphore_wait(credit.at[self.c], 1)
            cols = pl.ds(0, self.n)
            src = self.buf['C'].at[self.slot, :, :, :, 1 - k, :, cols]
            self.swap = sender.start(src, self.buf['D'].at[self.slot, :, :, :, :, cols], other)
            busy['C', self.c, self.slot] = [self.swap]

        def opposite(self, phase):
            if phase == 0:
                self.swap.wait_recv()
            p = (me[self.dims[phase]] + 2) % 4
            free((f'opp{phase}', self.c))
            cols = pl.ds(0, self.n)

            def body(e):
                self.buf[f'opp{phase}'][(*e, slice(None), cols)] = self.share(phase, p, e, (0, 32)).astype(bf16)
            self.each(phase, body)
            lead = [slice(None)] * (2 - phase)
            copies = []
            for half, step in ((0, 1), (1, 3)):
                src = self.buf[f'opp{phase}'].at[(*lead, pl.ds(16 * half, 16), cols)]
                dst = self.cut(f'half{half}{phase}', self.index)
                copies.append(sender.start(src, dst, moved(me, self.dims[phase], step)))
            busy[f'opp{phase}', self.c] = copies
            self.halves = copies

        def beside(self, phase):
            copies = []
            for half, step, name, dst in ((0, 1, 'rig', 'froml'), (1, 3, 'lef', 'fromr')):
                self.halves[half].wait_recv()
                free((f'{name}{phase}', self.c))
                p = (me[self.dims[phase]] + step) % 4
                cols = pl.ds(0, self.n)
                whole, got = self.buf[f'{name}{phase}'], self.buf[f'half{half}{phase}']

                def body(e):
                    mine = self.share(phase, p, e, (16 * half, 16)) + got[(self.index, *e, slice(None), cols)].astype(f32)
                    whole[(*e, pl.ds(16 * half, 16), cols)] = mine.astype(bf16)
                    plain = self.share(phase, p, e, (16 - 16 * half, 16))
                    whole[(*e, pl.ds(16 - 16 * half, 16), cols)] = plain.astype(bf16)
                self.each(phase, body)
                copy = sender.start(self.cut(f'{name}{phase}'), self.cut(f'{dst}{phase}', self.index),
                                    moved(me, self.dims[phase], step))
                busy[f'{name}{phase}', self.c] = [copy]
                copies.append(copy)
            self.wholes = copies

        def total(self, phase):
            for copy in self.wholes:
                copy.wait_recv()
            p = me[self.dims[phase]]
            cols = pl.ds(0, self.n)

            def body(e):
                got = [self.buf[f'{name}{phase}'][(self.index, *e, slice(None), cols)].astype(f32)
                       for name in ('froml', 'fromr')]
                value = self.share(phase, p, e, (0, 32)) + got[0] + got[1]
                if phase == 0:
                    self.buf['S1'][(*e, slice(None), cols)] = value
                elif phase == 1:
                    self.buf['S2'][(self.index % 3, *e, slice(None), cols)] = value
                elif self.g == STEM:
                    out_s[pl.ds(32 * self.c, 32), :] = value
                elif self.g == HEAD:
                    out_h[...] = value
                else:
                    out_c[self.g, :, pl.ds(*COLS[self.c])] = value
            self.each(phase, body)
            if phase == 0 and not self.last:
                pl.semaphore_signal(credit.at[self.c], inc=1, device_id=device(other), device_id_type=MESH)

        def run(self, stage):
            if stage == 0:
                self.start()
            elif stage == 7:
                self.total(2)
            elif stage % 2 == 0:
                self.beside(stage // 2 - 1)
            else:
                if stage > 1:
                    self.total(stage // 2 - 1)
                self.opposite(stage // 2)

    units = [Unit(g, c) for g, c in UNITS]
    stage_of = [0] * len(units)
    for u in ORDER:
        units[u].run(stage_of[u])
        stage_of[u] += 1
    assert stage_of == [8] * len(units)
    for key in list(busy):
        free(key)
    assert sender.count == REDUCE_COPIES, sender.count


def reduce_gradients(*operands):
    any_spec = pl.BlockSpec(memory_space=pl.ANY)
    vmem = pl.BlockSpec(memory_space=pltpu.VMEM)
    rows = operands[2].shape[0]
    return pl.pallas_call(
        reduce_kernel, name='reduce_gradients',
        out_shape=[jax.ShapeDtypeStruct((N_CH, 32, 1024), f32), jax.ShapeDtypeStruct((96, 256), f32),
                   jax.ShapeDtypeStruct((32, 256), f32)],
        in_specs=[any_spec] * 6 + [vmem] * 2, out_specs=[vmem] * 3,
        scratch_shapes=[pltpu.VMEM((2, rows, 4096), bf16), pltpu.VMEM((2, rows, 1024), bf16), reduce_scratch(),
                        pltpu.SemaphoreType.DMA((REDUCE_COPIES,)), pltpu.SemaphoreType.DMA((REDUCE_COPIES,)),
                        pltpu.SemaphoreType.DMA((2, 2)), pltpu.SemaphoreType.REGULAR((3,))],
        compiler_params=pltpu.CompilerParams(collective_id=1, has_side_effects=True, vmem_limit_bytes=64 * 1024 * 1024 - 65536),
        cost_estimate=pl.CostEstimate(flops=100_000_000_000, bytes_accessed=80_000_000, transcendentals=0),
    )(*operands)


EPS = 1e-6
TOK, TPAD = 49, 56
IMG = 8
ROWS, XROWS = IMG * TOK, IMG * TPAD
CHUNKS = ((0, 112), (112, 112), (224, 112), (336, 56))
CH, TOKH, CHH = 1024, 512, 4096
BLK = 512
NBLK = CHH // BLK
GELU_C, GELU_A = 0.7978845608028654, 0.044715


def dot_nn(a, b):
    return lax.dot_general(a, b, (((1,), (0,)), ((), ())), preferred_element_type=f32)


def dot_nt(a, b):
    return lax.dot_general(a, b, (((1,), (1,)), ((), ())), preferred_element_type=f32)


def dot_tn(a, b):
    return lax.dot_general(a, b, (((0,), (0,)), ((), ())), preferred_element_type=f32)


def gelu(x):
    half = 0.5 * x
    return half + half * jnp.tanh(x * (GELU_C + (GELU_C * GELU_A) * (x * x)))


def gelu_both(x):
    sq = x * x
    th = jnp.tanh(x * (GELU_C + (GELU_C * GELU_A) * sq))
    half = 0.5 * x
    rise = 0.5 + 0.5 * th
    slope = (1.0 - th * th) * (GELU_C + (3.0 * GELU_C * GELU_A) * sq)
    return x * rise, rise + half * slope


def standardize(x):
    mean = jnp.mean(x, axis=-1, keepdims=True)
    cent = x - mean
    inv = lax.rsqrt(jnp.mean(cent * cent, axis=-1, keepdims=True) + EPS)
    return cent * inv, inv


def norm_grad(d, gain, std, inv):
    gs = d * gain
    m0 = jnp.mean(gs, axis=-1, keepdims=True)
    m1 = jnp.mean(gs * std, axis=-1, keepdims=True)
    return inv * (gs - m0 - std * m1)


def row_mask(rows=TPAD):
    return lax.broadcasted_iota(jnp.int32, (rows, 1), 0) < TOK


def image(b):
    return pl.ds(b, TPAD, stride=IMG)


def get(ref, rows):
    return jnp.concatenate([ref[n, rows, :] for n in range(CH // 128)], axis=1)


def put(ref, rows, value):
    for n in range(CH // 128):
        ref[n, rows, :] = value[:, 128 * n:128 * (n + 1)]


class Stream:
    def __init__(self, sem, copies, count):
        self.sem, self.copies, self.count = sem, copies, count

    def make(self, i, slot):
        return [pltpu.make_async_copy(src, dst, self.sem.at[slot, n]) for n, (src, dst) in enumerate(self.copies(i, slot))]

    def start(self, i, slot):
        for copy in self.make(i, slot):
            copy.start()

    def wait(self, i, slot):
        for copy in self.make(i, slot):
            copy.wait()


def for_blocks(stream, body, out=None):
    n = stream.count
    stream.start(0, 0)

    @pl.loop(0, n)
    def _(i):
        slot = i % 2
        stream.wait(i, slot)

        @pl.when(i + 1 < n)
        def _():
            stream.start(i + 1, 1 - slot)
        if out is not None:
            @pl.when(i >= 2)
            def _():
                out.wait(i - 2, slot)
        body(i, slot)
        if out is not None:
            out.start(i, slot)
    if out is not None:
        out.wait(n - 2, n % 2)
        out.wait(n - 1, 1 - n % 2)


def backward_kernel(xin, xmid, pre_in, wc, wt, vec, dx0,
                    dpre, dout, dstem, gvec, gbch1, gt1, gt2, gbt,
                    x_v, d_v, dv_v, do_v, w1_v, w2_v, pre_v, dp_v, g_v, dh_v, sem, sem_w, sem_o):
    mask = row_mask()
    rest = pl.ds(ROWS, XROWS - ROWS)
    put(d_v, rest, jnp.zeros((XROWS - ROWS, CH), f32))
    put(x_v, rest, jnp.zeros((XROWS - ROWS, CH), f32))

    @pl.loop(0, TOK)
    def _(s):
        put(d_v, pl.ds(pl.multiple_of(s * IMG, IMG), IMG), dx0[...])
    gvec[...] = jnp.zeros_like(gvec)
    gt1[...] = jnp.zeros_like(gt1)
    gt2[...] = jnp.zeros_like(gt2)
    gbt[...] = jnp.zeros_like(gbt)

    def add(row, value):
        gvec[row:row + 1, :] += jnp.sum(value, axis=0, keepdims=True)

    for l in (1, 0):
        r = 1 + 5 * l
        load = pltpu.make_async_copy(xmid.at[l], x_v.at[:, pl.ds(0, ROWS)], sem.at[0])
        load.start()

        for at, size in CHUNKS:
            d = get(d_v, pl.ds(at, size))
            add(r + 4, d)
            do_v[pl.ds(at, size), :] = d.astype(bf16)
        send = pltpu.make_async_copy(do_v, dout.at[l], sem.at[1])
        send.start()

        def blocks(i, slot):
            t, h = i // 2, i % 2
            part = pl.ds(pl.multiple_of(h * BLK, BLK), BLK)
            whole = pl.ds(pl.multiple_of(i * BLK, BLK), BLK)
            return [(wc.at[2 * l, t, :, :, :, :, part], w1_v.at[slot]),
                    (wc.at[2 * l + 1, t, pl.ds(pl.multiple_of(h * 2, 2), 2)], w2_v.at[slot]),
                    (pre_in.at[l, :, whole], pre_v.at[slot])]

        def outs(i, slot):
            return [(dp_v.at[slot], dpre.at[l, :, pl.ds(pl.multiple_of(i * BLK, BLK), BLK)])]

        def channel(i, slot):
            _, slope = gelu_both(pre_v[slot])
            d = dot_nt(do_v[...], w2_v[slot].reshape(BLK, CH)) * slope
            gbch1[l:l + 1, pl.ds(pl.multiple_of(i * BLK, BLK), BLK)] = jnp.sum(d, axis=0, keepdims=True)
            dp_v[slot] = d.astype(bf16)
            part = dot_nt(dp_v[slot], w1_v[slot].reshape(CH, BLK))

            @pl.when(i == 0)
            def _():
                dv_v[...] = part

            @pl.when(i > 0)
            def _():
                dv_v[...] += part
        for_blocks(Stream(sem_w, blocks, NBLK), channel, Stream(sem_o, outs, NBLK))
        load.wait()
        send.wait()

        @pl.loop(0, ROWS // TPAD)
        def _(n):
            rows = pl.ds(pl.multiple_of(n * TPAD, TPAD), TPAD)
            std, inv = standardize(get(x_v, rows))
            d = dv_v[rows, :]
            add(r + 2, d * std)
            add(r + 3, d)
            put(d_v, rows, get(d_v, rows) + norm_grad(d, vec[r + 2:r + 3, :], std, inv))
        load = pltpu.make_async_copy(xin.at[l], x_v.at[:, pl.ds(0, ROWS)], sem.at[0])
        load.start()
        load.wait()

        @pl.loop(0, IMG)
        def _(b):
            std, inv = standardize(get(x_v, image(b)))
            a = with_bias_rows(std * vec[r:r + 1, :] + vec[r + 1:r + 2, :])
            d_mid = get(d_v, image(b))
            dm = d_mid.astype(bf16)
            act, slope = gelu_both(dot_nn(wt[l, :, 0:TPAD], a))
            g_v[...] = act.astype(bf16)
            dh = dot_nn(wt[2 + l, :, 0:TPAD], dm) * slope
            gbt[l] += jnp.sum(dh, axis=-1, keepdims=True)
            dh_v[...] = dh.astype(bf16)
            gt2[l] += dot_nt(g_v[...], dm)
            gt1[l] += dot_nt(dh_v[...], a)
            d = jnp.where(mask, dot_tn(wt[l, :, 0:TPAD], dh_v[...]), 0.0)
            add(r, d * std)
            add(r + 1, d)
            put(d_v, image(b), d_mid + norm_grad(d, vec[r:r + 1, :], std, inv))

    for at, size in CHUNKS:
        d = get(d_v, pl.ds(at, size))
        add(0, d)
        do_v[pl.ds(at, size), :] = d.astype(bf16)
    send = pltpu.make_async_copy(do_v, dstem, sem.at[1])
    send.start()
    send.wait()


def backward(*operands):
    a, v = pl.BlockSpec(memory_space=pl.ANY), pl.BlockSpec(memory_space=pltpu.VMEM)
    S = jax.ShapeDtypeStruct
    return pl.pallas_call(
        backward_kernel, name='backward',
        in_specs=[a] * 4 + [v] * 3,
        out_specs=[a] * 3 + [v] * 5,
        out_shape=[S((2, ROWS, CHH), bf16), S((2, ROWS, CH), bf16), S((ROWS, CH), bf16), S((16, CH), f32), S((2, CHH), f32),
                   S((2, TOKH, TPAD), f32), S((2, TOKH, TPAD), f32), S((2, TOKH, 1), f32)],
        scratch_shapes=[pltpu.VMEM((CH // 128, XROWS, 128), f32), pltpu.VMEM((CH // 128, XROWS, 128), f32), pltpu.VMEM((ROWS, CH), f32),
                        pltpu.VMEM((ROWS, CH), bf16), pltpu.VMEM((2, 4, 4, 2, 32, BLK), bf16),
                        pltpu.VMEM((2, 2, 4, 2, 32, CH), bf16),
                        pltpu.VMEM((2, ROWS, BLK), f32), pltpu.VMEM((2, ROWS, BLK), bf16), pltpu.VMEM((TOKH, CH), bf16),
                        pltpu.VMEM((TOKH, CH), bf16), pltpu.SemaphoreType.DMA((2,)), pltpu.SemaphoreType.DMA((2, 3)),
                        pltpu.SemaphoreType.DMA((2, 1))],
        compiler_params=pltpu.CompilerParams(vmem_limit_bytes=60 * 1024 * 1024),
        cost_estimate=pl.CostEstimate(flops=50_000_000_000, bytes_accessed=100_000_000, transcendentals=0),
    )(*operands)


FRONT_COPIES = 240
EARLY = [('stem', 0), ('stem', 1), ('stem', 2), ('ch', 0), ('ch', 1), ('ch', 2), ('head', 2)]
LATE = [('stem', c, None) for c in range(3)] + [('ch', c, g) for g in range(N_CH) for c in range(3)] + [('head', 2, None)]
UNIT_GROUP = {('stem', None): 0, ('ch', 0): 1, ('ch', 1): 2, ('ch', 2): 3, ('ch', 3): 4, ('head', None): 5}
EVERY = pl.ds(0, 4)
FRONT_ORDER = (
    ('prep', (('M0', ('sm',)), ('M0', ('tk',)), ('A0', ('stem', 0)), ('A0', ('stem', 1)), ('A0', ('stem', 2)),
        ('A0', ('ch', 0)), ('A0', ('ch', 1)), ('A0', ('ch', 2)), ('A0', ('head', 2)),)),
    ('unpack', (('M1', ('sm',)), ('M1', ('tk',)), ('A', ('stem', 0)), ('A', ('stem', 1)), ('A', ('stem', 2)),
        ('A', ('head', 2)), ('A', ('ch', 2)), ('A', ('ch', 0)), ('A', ('ch', 1)), ('B', ('stem', 0)), ('M2', ('sm',)),
        ('B', ('stem', 1)), ('M2', ('tk',)), ('B', ('stem', 2)), ('B', ('ch', 0)), ('B', ('head', 2)), ('B', ('ch', 1)),
        ('C', ('stem', 0)), ('B', ('ch', 2)), ('M3', ('sm',)), ('C', ('stem', 2)), ('C', ('stem', 1)), ('C', ('head', 2)),)),
    ('stem0', (('D', ('stem', 2, None)), ('D', ('stem', 0, None)), ('C', ('ch', 2)), ('C', ('ch', 0)),
        ('D', ('stem', 1, None)), ('C', ('ch', 1)), ('D', ('ch', 2, 0)), ('D', ('ch', 2, 1)), ('E', ('stem', 2, None)),
        ('E', ('stem', 0, None)), ('E', ('stem', 1, None)), ('D', ('ch', 0, 0)), ('D', ('ch', 0, 1)), ('D', ('ch', 1, 0)),
        ('D', ('ch', 1, 1)), ('F', ('stem', 0, None)), ('F', ('stem', 1, None)), ('E', ('ch', 2, 0)), ('E', ('ch', 2, 1)),
        ('E', ('ch', 0, 0)), ('E', ('ch', 1, 0)), ('F', ('stem', 2, None)), ('F', ('ch', 2, 0)),)),
    ('stem1', (('F', ('ch', 2, 1)), ('E', ('ch', 0, 1)), ('E', ('ch', 1, 1)), ('D', ('ch', 0, 2)), ('D', ('ch', 1, 2)),
        ('D', ('ch', 2, 2)), ('D', ('ch', 0, 3)), ('D', ('ch', 1, 3)), ('D', ('ch', 2, 3)),)),
    ('stem3', (('F', ('ch', 0, 0)),)),
    ('tok0_0', (('F', ('ch', 1, 0)),)),
    ('tok0_3', (('F', ('ch', 0, 1)),)),
    ('tok0_4', (('F', ('ch', 1, 1)),)),
    ('tok0_5', (('E', ('ch', 2, 2)),)),
    ('ch0_0', (('E', ('ch', 2, 3)), ('E', ('ch', 0, 2)), ('E', ('ch', 1, 2)), ('F', ('ch', 2, 2)),)),
    ('ch0_3', (('F', ('ch', 2, 3)),)),
    ('ch0_5', (('E', ('ch', 0, 3)), ('E', ('ch', 1, 3)), ('D', ('head', 2, None)),)),
    ('ch0_7', (('F', ('ch', 0, 2)), ('F', ('ch', 1, 2)),)),
    ('tok1_2', (('F', ('ch', 0, 3)),)),
    ('tok1_3', (('F', ('ch', 1, 3)), ('E', ('head', 2, None)),)),
    ('ln1', (('F', ('head', 2, None)),)),
)


class Net:
    def __init__(self, send_sems, recv_sems):
        self.send_sems, self.recv_sems, self.names, self.builds = send_sems, recv_sems, {}, []

    def copy(self, name):
        n = self.names[name]
        src, dst, target = self.builds[n]()
        return pltpu.make_async_remote_copy(src_ref=src, dst_ref=dst, send_sem=self.send_sems.at[n],
                                            recv_sem=self.recv_sems.at[n], device_id=target, device_id_type=MESH)

    def start(self, name, build):
        self.names[name] = len(self.builds)
        self.builds.append(build)
        self.copy(name).start()

    def arrived(self, *names):
        for name in names:
            self.copy(name).wait_recv()

    def finish(self):
        for name in self.names:
            self.copy(name).wait_send()


def three_parts(x):
    hi = x.astype(bf16)
    rest = x - hi.astype(f32)
    mid = rest.astype(bf16)
    return hi, mid, (rest - mid.astype(f32)).astype(bf16)


def with_bias_rows(a):
    row = lax.broadcasted_iota(jnp.int32, (TPAD, 1), 0)
    return jnp.where(row < TOK, a, jnp.where(row < TOK + 3, 1.0, 0.0)).astype(bf16)


def front_kernel(labels, patches, w_stem, w_ch1, w_ch2, w_head, w_tok1, w_tok2, b_tok1, b_ch1, b_head, b_stem, ln1_g, ln1_b,
                 ln2_g, ln2_b, b_ch2, lnf_g, lnf_b,
                 wc, pat_out, xin, xmid, vout, pre_out, act_out, hl, hr, dx0, hstat, gbh, vec, wt,
                 pc, ps, ph, tk_f, tk_p, sm_p, bh_p, ws, wh, tk_v, sm_v, sm_2, bh_v, bch1,
                 turn, p_v, x_v, v_v, w1_v, w2_v, pre_v, act_v, g_v,
                 send_sems, recv_sems, sem, sem_w, sem_o, sem_x):
    me = my_place()
    other = moved(me, 'k', 1)
    load_p = pltpu.make_async_copy(patches.at[:, pl.ds(pl.multiple_of(me['x'] * IMG, IMG), IMG)], p_v, sem.at[0])
    load_p.start()

    for l in range(2):
        pc[2 * l] = w_ch1[l].astype(bf16)
        pc[2 * l + 1] = w_ch2[l].astype(bf16)
    ps[...] = w_stem[...].astype(bf16)
    ph[...] = jnp.zeros_like(ph)
    ph[:, pl.ds(0, 250)] = w_head[...].astype(bf16)
    turn[...] = jnp.zeros_like(turn)
    for n, ref in ((0, b_stem), (11, lnf_g), (12, lnf_b)):
        turn[n, pl.ds(0, 8)] = ref[...]
    for n, ref in enumerate((ln1_g, ln1_b, ln2_g, ln2_b, b_ch2)):
        for l in range(2):
            turn[pl.ds(1 + 5 * l + n, 1), pl.ds(0, 8)] = ref[pl.ds(l, 1), :]
    turn[pl.ds(16, 2), pl.ds(0, 16)] = b_tok1[...]
    turned = turn[...].T
    tk_f[...] = jnp.zeros_like(tk_f)
    for l in range(2):
        tk_f[l, :, pl.ds(0, TOK)] = w_tok1[l]
        tk_f[2 + l, :, pl.ds(0, TOK)] = w_tok2[l]
        for n, part in enumerate(three_parts(turned[0:16, 16 + l:17 + l])):
            tk_f[l, :, pl.ds(TOK + n, 1)] = part.astype(f32)
    tk_p[...] = tk_f[...].astype(bf16)
    sm_p[...] = jnp.zeros_like(sm_p)
    sm_p[:, pl.ds(0, 16)] = turned[0:8, 0:16]
    sm_p[pl.ds(0, 2), pl.ds(32, 32)] = b_ch1[...]
    bh_p[...] = jnp.full_like(bh_p, -1e30)
    bh_p[0, pl.ds(0, 250)] = b_head[...]

    barrier = pltpu.get_barrier_semaphore()
    for dim in 'xyz':
        for step in (1, 2, 3):
            pl.semaphore_signal(barrier, inc=1, device_id=device(moved(me, dim, step)), device_id_type=MESH)
    pl.semaphore_signal(barrier, inc=1, device_id=device(other), device_id_type=MESH)
    net = Net(send_sems, recv_sems)
    core = me['k']
    ring = {d: [moved(me, d, n)[d] for n in range(4)] for d in 'xyz'}
    columns = [pl.ds(pl.multiple_of(x * 256, 256), 256) for x in ring['x']]
    peers = {(d, n): device(moved(me, d, n)) for d in 'xyz' for n in (1, 2, 3)}
    partner = device(other)
    here = {'x': 0, 'y': 0, 'z': 0}

    def view(unit, block, half=None):
        kind, colour = unit[:2]
        x, z, y = (EVERY if block[d] is None else ring[d][block[d]] for d in 'xzy')
        r0, rn = (0, 32) if half is None else (16 * half, 16)
        if kind == 'ch':
            c0, cn = COLS[colour]
            g = EVERY if len(unit) == 2 else unit[2]
            return wc.at[g, x, z, y, core, pl.ds(r0, rn), pl.ds(c0, cn)]
        cols = pl.ds(0, CH) if x is EVERY else columns[block['x']]
        if kind == 'stem':
            return ws.at[z, y, core, pl.ds(32 * colour + r0, rn), cols]
        return wh.at[z, y, core, pl.ds(r0, rn), cols]

    def piece(unit):
        kind, colour = unit
        if kind == 'ch':
            return pc.at[:, :, pl.ds(*COLS[colour])]
        return ps.at[pl.ds(32 * colour, 32), :] if kind == 'stem' else ph.at[:, :]

    def exchange(unit, tag, dim, block):
        for side, step in (('l', 1), ('r', 3)):
            def build(step=step):
                part = view(unit, block)
                return (piece(unit) if tag == '1' else part), part, peers[dim, step]
            net.start((unit, tag, side), build)

    def forward_half(unit, tag, dim, block):
        for half, (origin, target, side) in enumerate(((3, 1, 'l'), (1, 3, 'r'))):
            def build(half=half, origin=origin, target=target):
                part = view(unit, {**block, dim: origin}, half)
                return part, part, peers[dim, target]
            net.start((unit, tag, side), build)

    def swap(unit, tag, block):
        def build():
            part = view(unit, block)
            return part, part, partner
        net.start((unit, tag), build)

    own = pltpu.make_async_copy(pc, wc.at[:, me['x'], me['z'], me['y'], me['k']], sem.at[1])
    own.start()
    mine = pl.ds(pl.multiple_of(me['x'] * 256, 256), 256)
    ws[me['z'], me['y'], me['k'], :, mine] = ps[...]
    wh[me['z'], me['y'], me['k'], :, mine] = ph[...]
    sm_v[me['x'], me['z'], me['y'], me['k']] = sm_p[...]
    tk_v[:, me['z'], me['y'], me['k']] = tk_p[...]
    bh_v[:, mine] = bh_p[...]
    own.wait()
    pl.semaphore_wait(barrier, 10)

    def small(kind, n):
        dims = 'xyz' if kind == 'sm' else 'yz'
        at = {d: EVERY if d in dims[:n] else ring[d][0] for d in 'xyz'}

        def part():
            if kind == 'sm':
                return sm_v.at[at['x'], at['z'], at['y'], core]
            return tk_v.at[:, at['z'], at['y'], core]
        if n > 0:
            net.arrived(*[(kind, n - 1, s) for s in (1, 2, 3)])
        if n < len(dims):
            for s in (1, 2, 3):
                net.start((kind, n, s), lambda s=s: (part(), part(), peers[dims[n], s]))
            if kind == 'sm' and n == 0:
                def head_bias():
                    return bh_v.at[:, columns[0]]
                for s in (1, 2, 3):
                    net.start(('bh', s), lambda s=s: (head_bias(), head_bias(), peers['x', s]))
        else:
            net.start((kind, 'k'), lambda: (part(), part(), partner))

    def step(name, unit):
        if name[0] == 'M':
            small(unit[0], int(name[1]))
            return
        d1, d2, d3 = ORDERS[unit[1]]
        early = unit[:2]
        plane = {**here, d1: None, d2: None}
        if name == 'A0':
            exchange(unit, '1', d1, here)
        elif name == 'A':
            net.arrived((unit, '1', 'l'), (unit, '1', 'r'))
            forward_half(unit, '1h', d1, here)
        elif name == 'B':
            net.arrived((unit, '1h', 'l'), (unit, '1h', 'r'))
            exchange(unit, '2', d2, {**here, d1: None})
        elif name == 'C':
            net.arrived((unit, '2', 'l'), (unit, '2', 'r'))
            forward_half(unit, '2h', d2, {**here, d1: None})
        elif name == 'D':
            if early not in planes:
                planes.add(early)
                net.arrived((early, '2h', 'l'), (early, '2h', 'r'))
            exchange(unit, '3', d3, plane)
            swap(unit, 'k0', plane)
        elif name == 'E':
            net.arrived((unit, '3', 'l'), (unit, '3', 'r'))
            forward_half(unit, '3h', d3, plane)
            for n in (1, 3):
                swap(unit, f'k{n}', {**plane, d3: n})
        else:
            net.arrived((unit, '3h', 'l'), (unit, '3h', 'r'))
            swap(unit, 'k2', {**plane, d3: 2})

    planes = set()
    awaited = set()

    def need(group):
        for u in LATE:
            if UNIT_GROUP[u[0], u[2]] <= group and u not in awaited:
                awaited.add(u)
                net.arrived(*[(u, f'k{n}') for n in range(4)])

    bursts = {name: steps for name, steps in FRONT_ORDER}

    def burst(name):
        for s in bursts.get(name, ()):
            step(*s)

    def during(name, count):
        def run(i):
            for n in range(1, count):
                if bursts.get(f'{name}{n}'):
                    pl.when(i == n)(functools.partial(burst, f'{name}{n}'))
        return run

    burst('prep')
    load_p.wait()
    keep_p = pltpu.make_async_copy(p_v, pat_out, sem.at[0])
    keep_p.start()

    burst('unpack')
    net.arrived(('sm', 'k'), ('tk', 'k'), ('bh', 1), ('bh', 2), ('bh', 3))
    sm_2[...] = sm_v[...].reshape(1024, 128)
    for n in range(8):
        vec[:, pl.ds(128 * n, 128)] = sm_2[pl.ds(128 * n, 128), :].T[0:16, :]
    wt[...] = tk_v[...].reshape(4, TOKH, 128)
    for l in range(2):
        rows = jnp.concatenate(three_parts(sm_2[pl.ds(l, 128, stride=8), :]), axis=0)

        @pl.loop(0, 8)
        def _(n):
            lane = lax.broadcasted_iota(jnp.int32, (128, 512), 0)
            col = lax.broadcasted_iota(jnp.int32, (128, 512), 1)
            pick = jnp.where(lane == 32 + col % 32, 1.0, 0.0).astype(bf16)
            spread = dot_nn(rows, pick)
            value = spread[0:128] + spread[128:256] + spread[256:384]
            mine = lane == n * 16 + col // 32
            bch1[l:l + 1, pl.ds(pl.multiple_of(n * 512, 512), 512)] = jnp.sum(jnp.where(mine, value, 0.0), axis=0, keepdims=True)

    burst('stem0')
    need(0)
    run = during('stem', 4)
    put(x_v, pl.ds(ROWS, XROWS - ROWS), jnp.zeros((XROWS - ROWS, CH), f32))

    @pl.loop(0, 4)
    def _(i):
        run(i)
        cols = pl.ds(pl.multiple_of(i * 256, 256), 256)
        w = ws[:, :, :, :, cols].reshape(3072, 256)
        value = dot_nn(p_v[...].reshape(ROWS, 3072), w) + vec[0:1, cols]
        for n in range(2):
            x_v[2 * i + n, pl.ds(0, ROWS), :] = value[:, 128 * n:128 * (n + 1)]

    wc_all = wc

    def add_rows(value):
        for n in range(CH // 128):
            x_v[n, pl.ds(0, ROWS), :] += value[:, 128 * n:128 * (n + 1)]

    for l in range(2):
        r = 1 + 5 * l
        burst(f'tok{l}_0')
        run = during(f'tok{l}_', IMG)
        save_in = pltpu.make_async_copy(x_v.at[:, pl.ds(0, ROWS)], xin.at[l], sem_x.at[0])
        save_in.start()
        save_in.wait()

        @pl.loop(0, IMG)
        def _(b):
            run(b)
            x = get(x_v, image(b))
            std, _ = standardize(x)
            a = with_bias_rows(std * vec[r:r + 1, :] + vec[r + 1:r + 2, :])
            g_v[...] = gelu(dot_nn(wt[l, :, 0:TPAD], a)).astype(bf16)
            put(x_v, image(b), x + dot_tn(wt[2 + l, :, 0:TPAD], g_v[...]))
        save_mid = pltpu.make_async_copy(x_v.at[:, pl.ds(0, ROWS)], xmid.at[l], sem_x.at[0])
        save_mid.start()
        burst(f'ln{l}')

        for at, size in CHUNKS:
            std, _ = standardize(get(x_v, pl.ds(at, size)))
            v_v[pl.ds(at, size), :] = (std * vec[r + 2:r + 3, :] + vec[r + 3:r + 4, :]).astype(bf16)
        save_v = pltpu.make_async_copy(v_v, vout.at[l], sem_x.at[1])
        save_v.start()
        burst(f'ch{l}_0')
        need(2 + 2 * l)
        save_mid.wait()

        def blocks(i, slot):
            t, h = i // 2, i % 2
            part = pl.ds(pl.multiple_of(h * BLK, BLK), BLK)
            half = [pl.ds(pl.multiple_of(h * 2, 2), 2)]
            return [(wc_all.at[2 * l, t, :, :, :, :, part], w1_v.at[slot]), (wc_all.at[2 * l + 1, t, *half], w2_v.at[slot])]

        def outs(i, slot):
            part = pl.ds(pl.multiple_of(i * BLK, BLK), BLK)
            return [(pre_v.at[slot], pre_out.at[l, :, part]), (act_v.at[slot], act_out.at[l, :, part])]
        run = during(f'ch{l}_', NBLK)

        def channel(i, slot):
            run(i)
            part = pl.ds(pl.multiple_of(i * BLK, BLK), BLK)
            h = dot_nn(v_v[...], w1_v[slot].reshape(CH, BLK)) + bch1[l:l + 1, part]
            pre_v[slot] = h
            act_v[slot] = gelu(h).astype(bf16)
            add_rows(dot_nn(act_v[slot], w2_v[slot].reshape(BLK, CH)))
        for_blocks(Stream(sem_w, blocks, NBLK), channel, Stream(sem_o, outs, NBLK))
        add_rows(jnp.broadcast_to(vec[r + 4:r + 5, :], (ROWS, CH)))
        save_v.wait()

    burst('head')
    need(5)
    keep_p.wait()
    last = 11
    pooled = jnp.sum(get(x_v, pl.ds(0, ROWS)).reshape(TOK, IMG, CH), axis=0) * (1.0 / TOK)
    std, inv = standardize(pooled)
    head_in = (std * vec[last:last + 1, :] + vec[last + 1:last + 2, :]).astype(bf16)
    hl[...] = head_in
    w_h = wh[...].reshape(CH, CH)
    logits = dot_nn(head_in, w_h) + bh_v[0:1, :]
    row = lax.broadcasted_iota(jnp.int32, (IMG, 1), 0)
    label = jnp.zeros((IMG, 1), jnp.int32)
    for b in range(IMG):
        value = labels[me['x'] * IMG + b]
        label = jnp.where(row == b, value, label)
    label = label + 6 * sum(jnp.where(label >= edge, 1, 0) for edge in (250, 500, 750))
    is_label = lax.broadcasted_iota(jnp.int32, logits.shape, 1) == label
    top = jnp.max(logits, axis=-1, keepdims=True)
    ex = jnp.exp(logits - top)
    es = jnp.sum(ex, axis=-1, keepdims=True)
    nll = top + jnp.log(es) - jnp.sum(jnp.where(is_label, logits, 0.0), axis=-1, keepdims=True)
    d_logits = (ex / es - jnp.where(is_label, 1.0, 0.0)) * (1.0 / 1024)
    gbh[...] = jnp.sum(d_logits, axis=0, keepdims=True)
    d_bf = d_logits.astype(bf16)
    hr[...] = d_bf
    d_in = dot_nt(d_bf, w_h)
    hstat[0:1, :] = jnp.sum(d_in * std, axis=0, keepdims=True)
    hstat[1:2, :] = jnp.sum(d_in, axis=0, keepdims=True)
    hstat[2:3, :] = jnp.broadcast_to(jnp.sum(nll, axis=0, keepdims=True), (1, CH))
    dx0[...] = norm_grad(d_in, vec[last:last + 1, :], std, inv) * (1.0 / TOK)
    burst('end')
    net.finish()
    assert len(net.builds) <= FRONT_COPIES, len(net.builds)


def front(*operands):
    a, v = pl.BlockSpec(memory_space=pl.ANY), pl.BlockSpec(memory_space=pltpu.VMEM)
    S, V, DMA = jax.ShapeDtypeStruct, pltpu.VMEM, pltpu.SemaphoreType.DMA
    return pl.pallas_call(
        front_kernel, name='front',
        in_specs=[pl.BlockSpec(memory_space=pltpu.SMEM), a] + [v] * 17,
        out_specs=[a] * 7 + [v] * 7,
        out_shape=[S((N_CH, 4, 4, 4, 2, 32, 1024), bf16), S((TOK, IMG, 3072), bf16), S((2, CH // 128, ROWS, 128), f32),
                   S((2, CH // 128, ROWS, 128), f32),
                   S((2, ROWS, CH), bf16), S((2, ROWS, CHH), f32), S((2, ROWS, CHH), bf16), S((IMG, CH), bf16),
                   S((IMG, CH), bf16), S((IMG, CH), f32), S((8, CH), f32), S((1, CH), f32), S((16, CH), f32),
                   S((4, TOKH, 128), bf16)],
        scratch_shapes=[V((N_CH, 32, 1024), bf16), V((96, 256), bf16), V((32, 256), bf16), V((4, 16, 128), f32),
                        V((4, 16, 128), bf16), V((8, 128), f32), V((8, 256), f32), V((4, 4, 2, 96, CH), bf16),
                        V((4, 4, 2, 32, CH), bf16), V((4, 4, 4, 2, 16, 128), bf16), V((4, 4, 4, 2, 8, 128), f32),
                        V((1024, 128), f32), V((8, CH), f32), V((2, CHH), f32),
                        V((128, 128), f32), V((TOK, IMG, 3072), bf16), V((CH // 128, XROWS, 128), f32),
                        V((ROWS, CH), bf16), V((2, 4, 4, 2, 32, BLK), bf16), V((2, 2, 4, 2, 32, CH), bf16),
                        V((2, ROWS, BLK), f32), V((2, ROWS, BLK), bf16), V((TOKH, CH), bf16),
                        DMA((FRONT_COPIES,)), DMA((FRONT_COPIES,)), DMA((2,)), DMA((2, 2)), DMA((2, 2)), DMA((2,))],
        compiler_params=pltpu.CompilerParams(collective_id=0, has_side_effects=True, vmem_limit_bytes=62 * 1024 * 1024),
        cost_estimate=pl.CostEstimate(flops=90_000_000_000, bytes_accessed=180_000_000, transcendentals=0),
    )(*operands)

CHANNEL_AXES = ('tp', 'fsdp')


def weight_specs():
    vec_spec = P(CHANNEL_AXES)
    layer_vec = P(None, CHANNEL_AXES)
    return (P('fsdp', 'tp'), vec_spec, layer_vec, layer_vec, P(None, None, 'fsdp'), P(None, 'fsdp'),
            P(None, 'fsdp', None), layer_vec, layer_vec, P(None, 'fsdp', 'tp'), layer_vec,
            P(None, CHANNEL_AXES, None), layer_vec, vec_spec, vec_spec, P('fsdp', 'tp'), P('tp'))


def solution(mesh):
    fs = mesh.shape['fsdp']
    tp = mesh.shape['tp']
    nd = fs * tp

    def step(patches, labels, w_stem, b_stem, ln1_g, ln1_b, w_tok1, b_tok1, w_tok2,
             ln2_g, ln2_b, w_ch1, b_ch1, w_ch2, b_ch2, lnf_g, lnf_b, w_head, b_head):
        t = lax.axis_index('tp')
        nl = w_tok1.shape[0]
        total_images = IMG * nd
        classes = w_head.shape[1]
        wc, pat, xin, xmid, vin, pre, act, hl, hr, dx0, hstat, gbh, vec, wt = front(
            labels, patches.transpose(1, 0, 2), w_stem, w_ch1, w_ch2, w_head, w_tok1.transpose(0, 2, 1), w_tok2, b_tok1, b_ch1,
            b_head, b_stem, ln1_g, ln1_b, ln2_g, ln2_b, b_ch2, lnf_g, lnf_b)
        pat = pat.reshape(ROWS, -1)
        dpre, dout, dstem, gvec, gbch1, gt1, gt2, gbt = backward(xin, xmid, pre, wc, wt, vec, dx0)

        gvec = jnp.concatenate([gvec[:11], hstat[:2]], axis=0)
        parts = [gvec, gbch1, gbt[:, :, 0], gbh, gt1, gt2, hstat[2, :1]]
        flat = jnp.concatenate([p.reshape(-1) for p in parts])
        flat = jnp.pad(flat, (0, (-flat.shape[0]) % 1024))
        tot = lax.psum(flat, CHANNEL_AXES)

        g_c, g_s, g_h = reduce_gradients(dpre, act, pat, vin, dout, dstem, hl, hr)

        out = []
        o = 0
        for p in parts:
            out.append(tot[o:o + p.size].reshape(p.shape))
            o += p.size
        f = lax.axis_index('fsdp')

        def own(x, n, i, ax):
            size = x.shape[ax] // n
            return lax.dynamic_slice_in_dim(x, i * size, size, ax)
        dev = t * fs + f
        gv = own(out[0], nd, dev, 1)
        gc1 = own(out[1], nd, dev, 1)
        gtb = own(out[2], fs, f, 1)
        gbh = own(out[3].reshape(tp, 256), tp, t, 0)[0, :classes]
        gw1 = own(out[4], fs, f, 1)[:, :, :TOK].transpose(0, 2, 1)
        gw2 = own(out[5], fs, f, 1)[:, :, :TOK]
        loss = out[6][0] / total_images
        per = [jnp.stack([gv[1 + i], gv[6 + i]]) for i in range(5)]
        return (loss, g_s, gv[0], per[0], per[1], gw1, gtb, gw2, per[2], per[3], g_c[0::2], gc1, g_c[1::2], per[4],
                gv[11], gv[12], g_h[:, :classes], gbh)

    specs = weight_specs()
    return jax.shard_map(step, mesh=mesh, in_specs=(P('fsdp', None, None), P('fsdp')) + specs,
                         out_specs=(P(),) + specs, check_vma=False)
```

```python
import functools

import jax
import jax.numpy as jnp
from jax import lax
from jax.experimental import pallas as pl
from jax.experimental.pallas import tpu as pltpu
from jax.sharding import PartitionSpec as P

MESH = pl.DeviceIdType.MESH
ORDERS = (('x', 'y', 'z'), ('y', 'z', 'x'), ('z', 'x', 'y'))
COLS = ((0, 384), (384, 384), (768, 256))
N_CH = 4
STEM, HEAD = 4, 5
bf16, f32 = jnp.bfloat16, jnp.float32


def my_place():
    f = lax.axis_index('fsdp')
    return {'x': lax.axis_index('tp'), 'z': f // 8, 'y': (f // 2) % 4, 'k': f % 2}


def moved(place, dim, step):
    new = dict(place)
    new[dim] = 1 - place['k'] if dim == 'k' else (place[dim] + step) % 4
    return new


def device(place):
    return {'tp': place['x'], 'fsdp': (place['z'] * 4 + place['y']) * 2 + place['k']}


class Sender:
    def __init__(self, send_sems, recv_sems):
        self.send_sems, self.recv_sems, self.count, self.started = send_sems, recv_sems, 0, []

    def start(self, src, dst, target):
        n = self.count
        self.count += 1
        copy = pltpu.make_async_remote_copy(src_ref=src, dst_ref=dst, send_sem=self.send_sems.at[n],
                                            recv_sem=self.recv_sems.at[n], device_id=device(target),
                                            device_id_type=MESH)
        copy.start()
        self.started.append(copy)
        return copy


GROUPS = (STEM, 3, 2, 1, 0, HEAD)
UNITS = tuple((g, c) for g in GROUPS for c in (2, 0, 1) if g != HEAD or c == 2)
REDUCE_COPIES = 13 * len(UNITS) + 20
SMALL_AT = (2, 10, 20, 32, 44, 56)
ORDER = (0, 1, 2, 3, 4, 0, 5, 1, 2, 0, 3, 1, 2, 0, 4, 6, 3, 1, 7, 5, 0, 6, 4, 1, 2, 8, 0, 6, 7, 5, 2, 3, 1, 9, 0, 8, 4, 10, 7, 9, 1, 2,
         3, 0, 5, 11, 8, 9, 10, 1, 4, 5, 2, 11, 3, 6, 12, 10, 2, 5, 8, 6, 4, 7, 13, 11, 12, 3, 4, 7, 8, 14, 5, 12, 6, 13, 4, 9,
         15, 5, 8, 11, 3, 14, 13, 6, 7, 8, 9, 10, 11, 15, 7, 14, 6, 11, 10, 15, 7, 8, 9, 12, 11, 12, 14, 11, 10, 9, 13, 12, 15,
         14, 10, 9, 13, 12, 15, 14, 10, 13, 15, 12, 14, 13, 15, 14, 15, 13)


def reduce_scratch():
    per = []
    for c in range(3):
        n = COLS[c][1]
        many = sum(1 for u in UNITS if u[1] == c)
        lead = ((4, 4), (4,), ())
        b = {'C': pltpu.VMEM((2, 4, 4, 4, 2, 32, n), bf16), 'D': pltpu.VMEM((2, 4, 4, 4, 32, n), bf16),
             'S1': pltpu.VMEM((4, 4, 32, n), f32), 'S2': pltpu.VMEM((2, 4, 32, n), f32)}
        for ph in range(3):
            for name in ('opp', 'rig', 'lef'):
                b[f'{name}{ph}'] = pltpu.VMEM(lead[ph] + (32, n), bf16)
            for name in ('half0', 'half1'):
                b[f'{name}{ph}'] = pltpu.VMEM((many,) + lead[ph] + (16, n), bf16)
            for name in ('froml', 'fromr'):
                b[f'{name}{ph}'] = pltpu.VMEM((many,) + lead[ph] + (32, n), bf16)
        per.append(b)
    return per


def transposed_product(left, right):
    return lax.dot_general(left, right, (((0,), (0,)), ((), ())), preferred_element_type=f32)


def reduce_kernel(*refs):
    dpre, act, pat, vin, dout, dstem, head_l, head_r = refs[:8]
    sm_in, tk_in, refs = refs[8], refs[9], refs[:8] + refs[10:]
    wides = [dpre.at[0], act.at[0], dpre.at[1], act.at[1], pat]
    narrows = [vin.at[0], dout.at[0], vin.at[1], dout.at[1], dstem]
    (loss, out_s, o_bstem, o_ln1g, o_ln1b, o_wt1, o_bt1, o_wt2, o_ln2g, o_ln2b, out_c1, o_bch1, out_c2, o_bch2, o_lnfg, o_lnfb,
     out_h, o_bhead) = refs[8:26]
    wide, narrow, per, small, send_sems, recv_sems, load_sems, credit = refs[26:]
    out_c = (out_c1, out_c2)
    me = my_place()
    other = moved(me, 'k', 1)
    k = me['k']
    loads = {}

    def load(i):
        g = GROUPS[i]
        if g == HEAD:
            return
        cols = 3072 if g == STEM else 4096
        loads[g] = [pltpu.make_async_copy(wides[g], wide.at[i % 2, :, pl.ds(0, cols)], load_sems.at[i % 2, 0]),
                    pltpu.make_async_copy(narrows[g], narrow.at[i % 2], load_sems.at[i % 2, 1])]
        for copy in loads[g]:
            copy.start()

    load(0)
    barrier = pltpu.get_barrier_semaphore()
    for dim in 'xyz':
        for step in (1, 2, 3):
            pl.semaphore_signal(barrier, inc=1, device_id=device(moved(me, dim, step)), device_id_type=MESH)
    pl.semaphore_signal(barrier, inc=1, device_id=device(other), device_id_type=MESH)
    mine = [pltpu.make_async_copy(sm_in.at[:, :, :, k], small['sm0'], load_sems.at[2, 0]),
            pltpu.make_async_copy(tk_in.at[:, :, :, k], small['tk0'], load_sems.at[2, 1])]
    for copy in mine:
        copy.start()
    pl.semaphore_wait(barrier, 10)
    sender = Sender(send_sems, recv_sems)
    busy = {}

    def free(key):
        for copy in busy.pop(key, ()):
            copy.wait_send()

    def make(g, c, cslot):
        i = GROUPS.index(g)
        slot = i % 2
        if g != HEAD and c == 2:
            for copy in loads[g]:
                copy.wait()
            load(i + 1)
        if g == STEM:
            if c != 2:
                return
            @pl.loop(0, 32)
            def _(j):
                b = j // 4
                t = j % 4
                z, y2 = b // 2, b % 2
                left = wide[slot, :, pl.ds(pl.multiple_of(b * 384, 128), 384)]
                right = narrow[slot, :, pl.ds(pl.multiple_of(t * 256, 128), 256)]
                prod = transposed_product(left, right).astype(bf16).reshape(2, 2, 3, 32, 256)
                for d in range(3):
                    per[d]['C'][0, t, z, pl.ds(y2 * 2, 2), :, :, pl.ds(0, 256)] = prod[:, :, d]
        elif g == HEAD:

            @pl.loop(0, 4)
            def _(t):
                right = head_r[:, pl.ds(pl.multiple_of(t * 256, 128), 256)]
                prod = transposed_product(head_l[...], right)
                per[c]['C'][cslot, t] = prod.astype(bf16).reshape(4, 4, 2, 32, 256)
        else:
            c0, n = COLS[c]

            @pl.loop(0, 16)
            def _(j):
                t, z = j // 4, j % 4
                if g % 2 == 0:
                    left = narrow[slot, :, pl.ds(pl.multiple_of(z * 256, 128), 256)]
                    right = wide[slot, :, pl.ds(pl.multiple_of(t * 1024 + c0, 128), n)]
                else:
                    left = wide[slot, :, pl.ds(pl.multiple_of(j * 256, 128), 256)]
                    right = narrow[slot, :, pl.ds(c0, n)]
                per[c]['C'][cslot, t, z] = transposed_product(left, right).astype(bf16).reshape(4, 2, 32, n)

    class Unit:
        def __init__(self, g, c):
            self.g, self.c = g, c
            same = [u for u in UNITS if u[1] == c]
            self.index = same.index((g, c))
            self.slot = self.index % 2
            self.last = self.index >= len(same) - 2
            self.n = COLS[c][1] if g < N_CH else 256
            self.buf = per[c]
            self.dims = ORDERS[c]

        def cut(self, name, *at):
            ref = self.buf[name]
            rest = len(ref.shape) - len(at) - 1
            return ref.at[(*at, *[slice(None)] * rest, pl.ds(0, self.n))]

        def share(self, phase, p, e, rows):
            r = pl.ds(*rows)
            cols = pl.ds(0, self.n)
            if phase == 0:
                at = dict(zip(self.dims, (p, *e)))
                at = (at['x'], at['z'], at['y'])
                return (self.buf['C'][(self.slot, *at, k, r, cols)].astype(f32)
                        + self.buf['D'][(self.slot, *at, r, cols)].astype(f32))
            lead = () if phase == 1 else (self.index % 2,)
            return self.buf[f'S{phase}'][(*lead, p, *e, r, cols)]

        def each(self, phase, body):
            if phase == 2:
                body(())
            elif phase == 1:
                pl.loop(0, 4)(lambda i: body((i,)))
            else:
                pl.loop(0, 16)(lambda i: body((i // 4, i % 4)))

        def start(self):
            free(('C', self.c, self.slot))
            make(self.g, self.c, self.slot)
            if self.index > 1:
                pl.semaphore_wait(credit.at[self.c], 1)
            cols = pl.ds(0, self.n)
            src = self.buf['C'].at[self.slot, :, :, :, 1 - k, :, cols]
            self.swap = sender.start(src, self.buf['D'].at[self.slot, :, :, :, :, cols], other)
            busy['C', self.c, self.slot] = [self.swap]

        def opposite(self, phase):
            if phase == 0:
                self.swap.wait_recv()
            p = (me[self.dims[phase]] + 2) % 4
            free((f'opp{phase}', self.c))
            cols = pl.ds(0, self.n)

            def body(e):
                self.buf[f'opp{phase}'][(*e, slice(None), cols)] = self.share(phase, p, e, (0, 32)).astype(bf16)
            self.each(phase, body)
            lead = [slice(None)] * (2 - phase)
            copies = []
            for half, step in ((0, 1), (1, 3)):
                src = self.buf[f'opp{phase}'].at[(*lead, pl.ds(16 * half, 16), cols)]
                dst = self.cut(f'half{half}{phase}', self.index)
                copies.append(sender.start(src, dst, moved(me, self.dims[phase], step)))
            busy[f'opp{phase}', self.c] = copies
            self.halves = copies

        def beside(self, phase):
            copies = []
            for half, step, name, dst in ((0, 1, 'rig', 'froml'), (1, 3, 'lef', 'fromr')):
                self.halves[half].wait_recv()
                free((f'{name}{phase}', self.c))
                p = (me[self.dims[phase]] + step) % 4
                cols = pl.ds(0, self.n)
                whole, got = self.buf[f'{name}{phase}'], self.buf[f'half{half}{phase}']

                def body(e):
                    mine = self.share(phase, p, e, (16 * half, 16)) + got[(self.index, *e, slice(None), cols)].astype(f32)
                    whole[(*e, pl.ds(16 * half, 16), cols)] = mine.astype(bf16)
                    plain = self.share(phase, p, e, (16 - 16 * half, 16))
                    whole[(*e, pl.ds(16 - 16 * half, 16), cols)] = plain.astype(bf16)
                self.each(phase, body)
                copy = sender.start(self.cut(f'{name}{phase}'), self.cut(f'{dst}{phase}', self.index),
                                    moved(me, self.dims[phase], step))
                busy[f'{name}{phase}', self.c] = [copy]
                copies.append(copy)
            self.wholes = copies

        def total(self, phase):
            for copy in self.wholes:
                copy.wait_recv()
            p = me[self.dims[phase]]
            cols = pl.ds(0, self.n)

            def body(e):
                got = [self.buf[f'{name}{phase}'][(self.index, *e, slice(None), cols)].astype(f32)
                       for name in ('froml', 'fromr')]
                value = self.share(phase, p, e, (0, 32)) + got[0] + got[1]
                if phase == 0:
                    self.buf['S1'][(*e, slice(None), cols)] = value
                elif phase == 1:
                    self.buf['S2'][(self.index % 2, *e, slice(None), cols)] = value
                elif self.g == STEM:
                    out_s[pl.ds(32 * self.c, 32), :] = value
                elif self.g == HEAD:
                    out_h[...] = value[:, 0:250]
                else:
                    out_c[self.g % 2][self.g // 2, :, pl.ds(*COLS[self.c])] = value
            self.each(phase, body)
            if phase == 0 and not self.last:
                pl.semaphore_signal(credit.at[self.c], inc=1, device_id=device(other), device_id_type=MESH)

        def run(self, stage):
            if stage == 0:
                self.start()
            elif stage == 7:
                self.total(2)
            elif stage % 2 == 0:
                self.beside(stage // 2 - 1)
            else:
                if stage > 1:
                    self.total(stage // 2 - 1)
                self.opposite(stage // 2)

    units = [Unit(g, c) for g, c in UNITS]
    stage_of = [0] * len(units)
    for copy in mine:
        copy.wait()
    sums = SmallSums(me, sender, small, sm_in, tk_in)
    for n, u in enumerate(ORDER):
        if n in SMALL_AT:
            sums.step(SMALL_AT.index(n))
        units[u].run(stage_of[u])
        stage_of[u] += 1
    assert stage_of == [8] * len(units)
    sums.wait_sent()
    small_unpack(small, loss, (o_bstem, o_lnfg, o_lnfb), (o_ln1g, o_ln1b, o_ln2g, o_ln2b, o_bch2), o_bch1, o_bhead, o_wt1,
                 o_wt2, o_bt1)
    for key in list(busy):
        free(key)
    assert sender.count == REDUCE_COPIES, sender.count


SMALL = dict(sm=((4, 4, 4, 8, 128), (4, 4, 4, 8, 128), (3, 4, 4, 8, 128), (3, 4, 8, 128), (3, 8, 128)),
             tk=((4, 4, 4, 16, 128), (4, 4, 4, 16, 128), (3, 4, 4, 16, 128), (3, 4, 16, 128), (3, 4, 16, 128)))


def small_scratch():
    b = {f'{kind}{n}': pltpu.VMEM(shape, f32) for kind, shapes in SMALL.items() for n, shape in enumerate(shapes)}
    b.update(sm_s1=pltpu.VMEM((4, 4, 8, 128), f32), sm_s2=pltpu.VMEM((4, 8, 128), f32), sm_own=pltpu.VMEM((8, 128), f32),
             tk_s1=pltpu.VMEM((4, 4, 16, 128), f32), tk_s2=pltpu.VMEM((4, 16, 128), f32), tk_own=pltpu.VMEM((4, 16, 128), f32))
    return b


class SmallSums:
    def __init__(self, me, sender, b, sm_in, tk_in):
        self.me, self.sender, self.b, self.sent, self.last = me, sender, b, [], []
        self.sm_in, self.tk_in = sm_in, tk_in

    def send(self, src, dst, target):
        copy = self.sender.start(src, dst, target)
        self.sent.append(copy)
        self.last.append(copy)

    def wait_sent(self):
        for copy in self.sent:
            copy.wait_send()

    def arrived(self):
        for copy in self.last:
            copy.wait_recv()
        self.last = []

    def step(self, n):
        me, b = self.me, self.b
        x, z, y, k = me['x'], me['z'], me['y'], me['k']
        self.arrived()
        if n == 0:
            self.send(self.sm_in.at[:, :, :, 1 - k], b['sm1'], moved(me, 'k', 1))
            self.send(self.tk_in.at[:, :, :, 1 - k], b['tk1'], moved(me, 'k', 1))
        elif n == 1:
            b['sm1'][...] += b['sm0'][...]
            b['tk1'][...] += b['tk0'][...]
            for s in (1, 2, 3):
                self.send(b['sm1'].at[(x + s) % 4], b['sm2'].at[s - 1], moved(me, 'x', s))
                self.send(b['tk1'].at[:, (z + s) % 4], b['tk2'].at[s - 1], moved(me, 'z', s))
        elif n == 2:
            b['sm_s1'][...] = b['sm1'][x] + b['sm2'][0] + b['sm2'][1] + b['sm2'][2]
            b['tk_s1'][...] = b['tk1'][:, z] + b['tk2'][0] + b['tk2'][1] + b['tk2'][2]
            for s in (1, 2, 3):
                self.send(b['sm_s1'].at[(z + s) % 4], b['sm3'].at[s - 1], moved(me, 'z', s))
                self.send(b['tk_s1'].at[:, (y + s) % 4], b['tk3'].at[s - 1], moved(me, 'y', s))
        elif n == 3:
            b['sm_s2'][...] = b['sm_s1'][z] + b['sm3'][0] + b['sm3'][1] + b['sm3'][2]
            b['tk_s2'][...] = b['tk_s1'][:, y] + b['tk3'][0] + b['tk3'][1] + b['tk3'][2]
            for s in (1, 2, 3):
                self.send(b['sm_s2'].at[(y + s) % 4], b['sm4'].at[s - 1], moved(me, 'y', s))
                self.send(b['tk_s2'], b['tk4'].at[s - 1], moved(me, 'x', s))
        elif n == 4:
            b['sm_own'][...] = b['sm_s2'][y] + b['sm4'][0] + b['sm4'][1] + b['sm4'][2]
            parts = [b['tk_s2'][...]] + [b['tk4'][s] for s in range(3)]
            ordered = []
            for place in range(4):
                value = parts[0]
                for s in (1, 2, 3):
                    value = jnp.where((x + 4 - s) % 4 == place, parts[s], value)
                ordered.append(value)
            b['tk_own'][...] = (ordered[0] + ordered[1]) + (ordered[2] + ordered[3])


def small_unpack(b, loss, singles, pairs, o_bch1, o_bhead, o_wt1, o_wt2, o_bt1):
    own = b['sm_own'][...]
    turned = jnp.concatenate([own, jnp.zeros((120, 128), f32)], axis=0).T
    for ref, n in zip(singles, (0, 11, 12)):
        ref[...] = turned[n, 0:8]
    for n, ref in enumerate(pairs):
        for l in range(2):
            ref[pl.ds(l, 1), :] = turned[1 + 5 * l + n:2 + 5 * l + n, 0:8]
    o_bch1[...] = own[0:2, 32:64]
    classes = jnp.concatenate([own[2 + q:3 + q, 64:128] for q in range(4)], axis=1)
    o_bhead[...] = classes[0, 0:250]
    loss[...] = own[6:7, 64:65] * (1.0 / 1024)
    tk = b['tk_own'][...]
    for l in range(2):
        o_wt1[l] = tk[l, :, 0:TOK]
        o_wt2[l] = tk[2 + l, :, 0:TOK]
        tall = jnp.concatenate([tk[l], jnp.zeros((112, 128), f32)], axis=0).T
        o_bt1[pl.ds(l, 1), :] = tall[64:65, 0:16]


def reduce_gradients(*operands):
    any_spec = pl.BlockSpec(memory_space=pl.ANY)
    vmem = pl.BlockSpec(memory_space=pltpu.VMEM)
    rows = operands[2].shape[0]
    S = jax.ShapeDtypeStruct
    return pl.pallas_call(
        reduce_kernel, name='reduce_gradients',
        out_shape=[S((1, 1), f32), S((96, 256), f32), S((8,), f32), S((2, 8), f32), S((2, 8), f32), S((2, 16, TOK), f32),
                   S((2, 16), f32), S((2, 16, TOK), f32), S((2, 8), f32), S((2, 8), f32), S((2, 32, 1024), f32), S((2, 32), f32),
                   S((2, 32, 1024), f32), S((2, 8), f32), S((8,), f32), S((8,), f32), S((32, 250), f32), S((250,), f32)],
        in_specs=[any_spec] * 6 + [vmem] * 2 + [any_spec] * 2, out_specs=[vmem] * 18,
        scratch_shapes=[pltpu.VMEM((2, rows, 4096), bf16), pltpu.VMEM((2, rows, 1024), bf16), reduce_scratch(), small_scratch(),
                        pltpu.SemaphoreType.DMA((REDUCE_COPIES,)), pltpu.SemaphoreType.DMA((REDUCE_COPIES,)),
                        pltpu.SemaphoreType.DMA((3, 2)), pltpu.SemaphoreType.REGULAR((3,))],
        compiler_params=pltpu.CompilerParams(collective_id=1, has_side_effects=True, vmem_limit_bytes=64 * 1024 * 1024 - 65536),
        cost_estimate=pl.CostEstimate(flops=100_000_000_000, bytes_accessed=80_000_000, transcendentals=0),
    )(*operands)


EPS = 1e-6
TOK, TPAD = 49, 56
IMG = 8
ROWS, XROWS = IMG * TOK, IMG * TPAD
CHUNKS = ((0, 112), (112, 112), (224, 112), (336, 56))
CH, TOKH, CHH = 1024, 512, 4096
BLK = 512
NBLK = CHH // BLK
GELU_C, GELU_A = 0.7978845608028654, 0.044715


def dot_nn(a, b):
    return lax.dot_general(a, b, (((1,), (0,)), ((), ())), preferred_element_type=f32)


def dot_nt(a, b):
    return lax.dot_general(a, b, (((1,), (1,)), ((), ())), preferred_element_type=f32)


def dot_tn(a, b):
    return lax.dot_general(a, b, (((0,), (0,)), ((), ())), preferred_element_type=f32)


def gelu(x):
    half = 0.5 * x
    return half + half * jnp.tanh(x * (GELU_C + (GELU_C * GELU_A) * (x * x)))


def gelu_both(x):
    sq = x * x
    th = jnp.tanh(x * (GELU_C + (GELU_C * GELU_A) * sq))
    half = 0.5 * x
    rise = 0.5 + 0.5 * th
    slope = (1.0 - th * th) * (GELU_C + (3.0 * GELU_C * GELU_A) * sq)
    return x * rise, rise + half * slope


def standardize(x):
    mean = jnp.mean(x, axis=-1, keepdims=True)
    cent = x - mean
    inv = lax.rsqrt(jnp.mean(cent * cent, axis=-1, keepdims=True) + EPS)
    return cent * inv, inv


def norm_grad(d, gain, std, inv):
    gs = d * gain
    m0 = jnp.mean(gs, axis=-1, keepdims=True)
    m1 = jnp.mean(gs * std, axis=-1, keepdims=True)
    return inv * (gs - m0 - std * m1)


def row_mask(rows=TPAD):
    return lax.broadcasted_iota(jnp.int32, (rows, 1), 0) < TOK


def image(b):
    return pl.ds(b, TPAD, stride=IMG)


def get(ref, rows):
    return jnp.concatenate([ref[n, rows, :] for n in range(CH // 128)], axis=1)


def put(ref, rows, value):
    for n in range(CH // 128):
        ref[n, rows, :] = value[:, 128 * n:128 * (n + 1)]


class Stream:
    def __init__(self, sem, copies, count):
        self.sem, self.copies, self.count = sem, copies, count

    def make(self, i, slot):
        return [pltpu.make_async_copy(src, dst, self.sem.at[slot, n]) for n, (src, dst) in enumerate(self.copies(i, slot))]

    def start(self, i, slot):
        for copy in self.make(i, slot):
            copy.start()

    def wait(self, i, slot):
        for copy in self.make(i, slot):
            copy.wait()


def for_blocks(stream, body, out=None):
    n = stream.count
    stream.start(0, 0)

    @pl.loop(0, n)
    def _(i):
        slot = i % 2
        stream.wait(i, slot)

        @pl.when(i + 1 < n)
        def _():
            stream.start(i + 1, 1 - slot)
        if out is not None:
            @pl.when(i >= 2)
            def _():
                out.wait(i - 2, slot)
        body(i, slot)
        if out is not None:
            out.start(i, slot)
    if out is not None:
        out.wait(n - 2, n % 2)
        out.wait(n - 1, 1 - n % 2)


def small_pack(flat, turn, gvec, hstat, gbch1, gbh):
    turn[...] = jnp.zeros_like(turn)
    turn[pl.ds(0, 16), :] = gvec[...]
    turn[pl.ds(11, 2), :] = hstat[pl.ds(0, 2), :]
    for n in range(8):
        flat[pl.ds(128 * n, 128), :] = turn[:, pl.ds(128 * n, 128)].T
    for l in range(2):
        total = jnp.zeros((384, 128), f32)
        for n in range(8):
            lane = lax.broadcasted_iota(jnp.int32, (128, 512), 0)
            col = lax.broadcasted_iota(jnp.int32, (128, 512), 1)
            mine = jnp.where(lane == n * 16 + col // 32, gbch1[l:l + 1, 512 * n:512 * (n + 1)], 0.0)
            pick = jnp.where(lane == 32 + col % 32, 1.0, 0.0).astype(bf16)
            total += lax.dot_general(jnp.concatenate(three_parts(mine), axis=0), pick, (((1,), (1,)), ((), ())),
                                     preferred_element_type=f32)
        flat[pl.ds(l, 128, stride=8), :] += total[0:128] + total[128:256] + total[256:384]
    high = lax.broadcasted_iota(jnp.int32, (1, 128), 1) >= 64
    for t in range(4):
        for q in range(4):
            tile = gbh[0:1, t * 256 + q // 2 * 128:t * 256 + q // 2 * 128 + 128]
            if q % 2 == 0:
                tile = jnp.concatenate([tile[:, 64:], tile[:, :64]], axis=1)
            flat[pl.ds(t * 256 + 2 + q, 32, stride=8), :] += jnp.where(high, tile, 0.0)
    at64 = lax.broadcasted_iota(jnp.int32, (1, 128), 1) == 64
    flat[pl.ds(6, 128, stride=8), :] += jnp.where(at64, hstat[2:3, 0:128], 0.0)


def backward_kernel(xin, xmid, pre_in, wc, wt, vec, dx0, hstat, gbh,
                    dpre, dout, dstem, flat, tk, gvec, gbch1, turn, x_v, d_v, dv_v, do_v, w1_v, w2_v, pre_v, dp_v, g_v, dh_v, sem, sem_w, sem_o):
    mask = row_mask()
    rest = pl.ds(ROWS, XROWS - ROWS)
    put(d_v, rest, jnp.zeros((XROWS - ROWS, CH), f32))
    put(x_v, rest, jnp.zeros((XROWS - ROWS, CH), f32))

    @pl.loop(0, TOK)
    def _(s):
        put(d_v, pl.ds(pl.multiple_of(s * IMG, IMG), IMG), dx0[...])
    gvec[...] = jnp.zeros_like(gvec)
    tk[...] = jnp.zeros_like(tk)

    def add(row, value):
        gvec[row:row + 1, :] += jnp.sum(value, axis=0, keepdims=True)

    for l in (1, 0):
        r = 1 + 5 * l
        load = pltpu.make_async_copy(xmid.at[l], x_v.at[:, pl.ds(0, ROWS)], sem.at[0])
        load.start()

        for at, size in CHUNKS:
            d = get(d_v, pl.ds(at, size))
            add(r + 4, d)
            do_v[pl.ds(at, size), :] = d.astype(bf16)
        send = pltpu.make_async_copy(do_v, dout.at[l], sem.at[1])
        send.start()

        def blocks(i, slot):
            t, h = i // 2, i % 2
            part = pl.ds(pl.multiple_of(h * BLK, BLK), BLK)
            whole = pl.ds(pl.multiple_of(i * BLK, BLK), BLK)
            return [(wc.at[2 * l, t, :, :, :, :, part], w1_v.at[slot]),
                    (wc.at[2 * l + 1, t, pl.ds(pl.multiple_of(h * 2, 2), 2)], w2_v.at[slot]),
                    (pre_in.at[l, :, whole], pre_v.at[slot])]

        def outs(i, slot):
            return [(dp_v.at[slot], dpre.at[l, :, pl.ds(pl.multiple_of(i * BLK, BLK), BLK)])]

        def channel(i, slot):
            _, slope = gelu_both(pre_v[slot])
            d = dot_nt(do_v[...], w2_v[slot].reshape(BLK, CH)) * slope
            gbch1[l:l + 1, pl.ds(pl.multiple_of(i * BLK, BLK), BLK)] = jnp.sum(d, axis=0, keepdims=True)
            dp_v[slot] = d.astype(bf16)
            part = dot_nt(dp_v[slot], w1_v[slot].reshape(CH, BLK))

            @pl.when(i == 0)
            def _():
                dv_v[...] = part

            @pl.when(i > 0)
            def _():
                dv_v[...] += part
        for_blocks(Stream(sem_w, blocks, NBLK), channel, Stream(sem_o, outs, NBLK))
        load.wait()
        send.wait()

        @pl.loop(0, ROWS // TPAD)
        def _(n):
            rows = pl.ds(pl.multiple_of(n * TPAD, TPAD), TPAD)
            std, inv = standardize(get(x_v, rows))
            d = dv_v[rows, :]
            add(r + 2, d * std)
            add(r + 3, d)
            put(d_v, rows, get(d_v, rows) + norm_grad(d, vec[r + 2:r + 3, :], std, inv))
        load = pltpu.make_async_copy(xin.at[l], x_v.at[:, pl.ds(0, ROWS)], sem.at[0])
        load.start()
        load.wait()

        @pl.loop(0, IMG)
        def _(b):
            std, inv = standardize(get(x_v, image(b)))
            a = with_bias_rows(std * vec[r:r + 1, :] + vec[r + 1:r + 2, :])
            d_mid = get(d_v, image(b))
            dm = d_mid.astype(bf16)
            act, slope = gelu_both(dot_nn(wt[l, :, 0:TPAD], a))
            g_v[...] = act.astype(bf16)
            dh = dot_nn(wt[2 + l, :, 0:TPAD], dm) * slope
            tk[l, :, pl.ds(64, 1)] += jnp.sum(dh, axis=-1, keepdims=True)
            dh_v[...] = dh.astype(bf16)
            tk[2 + l, :, pl.ds(0, TPAD)] += dot_nt(g_v[...], dm)
            tk[l, :, pl.ds(0, TPAD)] += dot_nt(dh_v[...], a)
            d = jnp.where(mask, dot_tn(wt[l, :, 0:TPAD], dh_v[...]), 0.0)
            add(r, d * std)
            add(r + 1, d)
            put(d_v, image(b), d_mid + norm_grad(d, vec[r:r + 1, :], std, inv))

    for at, size in CHUNKS:
        d = get(d_v, pl.ds(at, size))
        add(0, d)
        do_v[pl.ds(at, size), :] = d.astype(bf16)
    send = pltpu.make_async_copy(do_v, dstem, sem.at[1])
    send.start()
    small_pack(flat, turn, gvec, hstat, gbch1, gbh)
    send.wait()


def backward(*operands):
    a, v = pl.BlockSpec(memory_space=pl.ANY), pl.BlockSpec(memory_space=pltpu.VMEM)
    S = jax.ShapeDtypeStruct
    return pl.pallas_call(
        backward_kernel, name='backward',
        in_specs=[a] * 4 + [v] * 5,
        out_specs=[a] * 3 + [v] * 2,
        out_shape=[S((2, ROWS, CHH), bf16), S((2, ROWS, CH), bf16), S((ROWS, CH), bf16), S((1024, 128), f32),
                   S((4, TOKH, 128), f32)],
        scratch_shapes=[pltpu.VMEM((16, CH), f32), pltpu.VMEM((2, CHH), f32), pltpu.VMEM((128, 1024), f32),
                        pltpu.VMEM((CH // 128, XROWS, 128), f32), pltpu.VMEM((CH // 128, XROWS, 128), f32), pltpu.VMEM((ROWS, CH), f32),
                        pltpu.VMEM((ROWS, CH), bf16), pltpu.VMEM((2, 4, 4, 2, 32, BLK), bf16),
                        pltpu.VMEM((2, 2, 4, 2, 32, CH), bf16),
                        pltpu.VMEM((2, ROWS, BLK), f32), pltpu.VMEM((2, ROWS, BLK), bf16), pltpu.VMEM((TOKH, CH), bf16),
                        pltpu.VMEM((TOKH, CH), bf16), pltpu.SemaphoreType.DMA((2,)), pltpu.SemaphoreType.DMA((2, 3)),
                        pltpu.SemaphoreType.DMA((2, 1))],
        compiler_params=pltpu.CompilerParams(vmem_limit_bytes=60 * 1024 * 1024),
        cost_estimate=pl.CostEstimate(flops=50_000_000_000, bytes_accessed=100_000_000, transcendentals=0),
    )(*operands)


FRONT_COPIES = 240
EARLY = [('stem', 0), ('stem', 1), ('stem', 2), ('ch', 0), ('ch', 1), ('ch', 2), ('head', 2)]
LATE = [('stem', c, None) for c in range(3)] + [('ch', c, g) for g in range(N_CH) for c in range(3)] + [('head', 2, None)]
UNIT_GROUP = {('stem', None): 0, ('ch', 0): 1, ('ch', 1): 2, ('ch', 2): 3, ('ch', 3): 4, ('head', None): 5}
EVERY = pl.ds(0, 4)
FRONT_ORDER = (
    ('prep', (('M0', ('sm',)), ('M0', ('tk',)), ('A0', ('stem', 0)), ('A0', ('stem', 1)), ('A0', ('stem', 2)),
        ('A0', ('ch', 0)), ('A0', ('ch', 1)), ('A0', ('ch', 2)), ('A0', ('head', 2)),)),
    ('unpack', (('M1', ('sm',)), ('M1', ('tk',)), ('A', ('stem', 0)), ('A', ('stem', 1)), ('A', ('stem', 2)),
        ('A', ('head', 2)), ('A', ('ch', 2)), ('A', ('ch', 0)), ('A', ('ch', 1)), ('B', ('stem', 0)), ('M2', ('sm',)),
        ('B', ('stem', 1)), ('M2', ('tk',)), ('B', ('stem', 2)), ('B', ('ch', 0)), ('B', ('head', 2)), ('B', ('ch', 1)),
        ('C', ('stem', 0)), ('B', ('ch', 2)), ('M3', ('sm',)), ('C', ('stem', 2)), ('C', ('stem', 1)), ('C', ('head', 2)),)),
    ('stem0', (('D', ('stem', 2, None)), ('D', ('stem', 0, None)), ('C', ('ch', 2)), ('C', ('ch', 0)),
        ('D', ('stem', 1, None)), ('C', ('ch', 1)), ('D', ('ch', 2, 0)), ('D', ('ch', 2, 1)), ('E', ('stem', 2, None)),
        ('E', ('stem', 0, None)), ('E', ('stem', 1, None)), ('D', ('ch', 0, 0)), ('D', ('ch', 0, 1)), ('D', ('ch', 1, 0)),
        ('D', ('ch', 1, 1)), ('F', ('stem', 0, None)), ('F', ('stem', 1, None)), ('E', ('ch', 2, 0)), ('E', ('ch', 2, 1)),
        ('E', ('ch', 0, 0)), ('E', ('ch', 1, 0)), ('F', ('stem', 2, None)), ('F', ('ch', 2, 0)),)),
    ('stem1', (('F', ('ch', 2, 1)), ('E', ('ch', 0, 1)), ('E', ('ch', 1, 1)), ('D', ('ch', 0, 2)), ('D', ('ch', 1, 2)),
        ('D', ('ch', 2, 2)), ('D', ('ch', 0, 3)), ('D', ('ch', 1, 3)), ('D', ('ch', 2, 3)),)),
    ('stem3', (('F', ('ch', 0, 0)),)),
    ('tok0_0', (('F', ('ch', 1, 0)),)),
    ('tok0_3', (('F', ('ch', 0, 1)),)),
    ('tok0_4', (('F', ('ch', 1, 1)),)),
    ('tok0_5', (('E', ('ch', 2, 2)),)),
    ('ch0_0', (('E', ('ch', 2, 3)), ('E', ('ch', 0, 2)), ('E', ('ch', 1, 2)), ('F', ('ch', 2, 2)),)),
    ('ch0_3', (('F', ('ch', 2, 3)),)),
    ('ch0_5', (('E', ('ch', 0, 3)), ('E', ('ch', 1, 3)), ('D', ('head', 2, None)),)),
    ('ch0_7', (('F', ('ch', 0, 2)), ('F', ('ch', 1, 2)),)),
    ('tok1_2', (('F', ('ch', 0, 3)),)),
    ('tok1_3', (('F', ('ch', 1, 3)), ('E', ('head', 2, None)),)),
    ('ln1', (('F', ('head', 2, None)),)),
)


class Net:
    def __init__(self, send_sems, recv_sems):
        self.send_sems, self.recv_sems, self.names, self.builds = send_sems, recv_sems, {}, []

    def copy(self, name):
        n = self.names[name]
        src, dst, target = self.builds[n]()
        return pltpu.make_async_remote_copy(src_ref=src, dst_ref=dst, send_sem=self.send_sems.at[n],
                                            recv_sem=self.recv_sems.at[n], device_id=target, device_id_type=MESH)

    def start(self, name, build):
        self.names[name] = len(self.builds)
        self.builds.append(build)
        self.copy(name).start()

    def arrived(self, *names):
        for name in names:
            self.copy(name).wait_recv()

    def finish(self):
        for name in self.names:
            self.copy(name).wait_send()


def three_parts(x):
    hi = x.astype(bf16)
    rest = x - hi.astype(f32)
    mid = rest.astype(bf16)
    return hi, mid, (rest - mid.astype(f32)).astype(bf16)


def with_bias_rows(a):
    row = lax.broadcasted_iota(jnp.int32, (TPAD, 1), 0)
    return jnp.where(row < TOK, a, jnp.where(row < TOK + 3, 1.0, 0.0)).astype(bf16)


def front_kernel(labels, patches, w_stem, w_ch1, w_ch2, w_head, w_tok1, w_tok2, b_tok1, b_ch1, b_head, b_stem, ln1_g, ln1_b,
                 ln2_g, ln2_b, b_ch2, lnf_g, lnf_b,
                 wc, pat_out, xin, xmid, vout, pre_out, act_out, hl, hr, dx0, hstat, gbh, vec, wt,
                 pc, ps, ph, tk_f, tk_p, sm_p, bh_p, ws, wh, tk_v, sm_v, sm_2, bh_v, bch1,
                 turn, p_v, x_v, v_v, w1_v, w2_v, pre_v, act_v, g_v,
                 send_sems, recv_sems, sem, sem_w, sem_o, sem_x):
    me = my_place()
    other = moved(me, 'k', 1)
    load_p = pltpu.make_async_copy(patches.at[:, pl.ds(pl.multiple_of(me['x'] * IMG, IMG), IMG)], p_v, sem.at[0])
    load_p.start()

    for l in range(2):
        pc[2 * l] = w_ch1[l].astype(bf16)
        pc[2 * l + 1] = w_ch2[l].astype(bf16)
    ps[...] = w_stem[...].astype(bf16)
    ph[...] = jnp.zeros_like(ph)
    ph[:, pl.ds(0, 250)] = w_head[...].astype(bf16)
    turn[...] = jnp.zeros_like(turn)
    for n, ref in ((0, b_stem), (11, lnf_g), (12, lnf_b)):
        turn[n, pl.ds(0, 8)] = ref[...]
    for n, ref in enumerate((ln1_g, ln1_b, ln2_g, ln2_b, b_ch2)):
        for l in range(2):
            turn[pl.ds(1 + 5 * l + n, 1), pl.ds(0, 8)] = ref[pl.ds(l, 1), :]
    turn[pl.ds(16, 2), pl.ds(0, 16)] = b_tok1[...]
    turned = turn[...].T
    tk_f[...] = jnp.zeros_like(tk_f)
    for l in range(2):
        tk_f[l, :, pl.ds(0, TOK)] = w_tok1[l]
        tk_f[2 + l, :, pl.ds(0, TOK)] = w_tok2[l]
        for n, part in enumerate(three_parts(turned[0:16, 16 + l:17 + l])):
            tk_f[l, :, pl.ds(TOK + n, 1)] = part.astype(f32)
    tk_p[...] = tk_f[...].astype(bf16)
    sm_p[...] = jnp.zeros_like(sm_p)
    sm_p[:, pl.ds(0, 16)] = turned[0:8, 0:16]
    sm_p[pl.ds(0, 2), pl.ds(32, 32)] = b_ch1[...]
    bh_p[...] = jnp.full_like(bh_p, -1e30)
    bh_p[0, pl.ds(0, 250)] = b_head[...]

    barrier = pltpu.get_barrier_semaphore()
    for dim in 'xyz':
        for step in (1, 2, 3):
            pl.semaphore_signal(barrier, inc=1, device_id=device(moved(me, dim, step)), device_id_type=MESH)
    pl.semaphore_signal(barrier, inc=1, device_id=device(other), device_id_type=MESH)
    net = Net(send_sems, recv_sems)
    core = me['k']
    ring = {d: [moved(me, d, n)[d] for n in range(4)] for d in 'xyz'}
    columns = [pl.ds(pl.multiple_of(x * 256, 256), 256) for x in ring['x']]
    peers = {(d, n): device(moved(me, d, n)) for d in 'xyz' for n in (1, 2, 3)}
    partner = device(other)
    here = {'x': 0, 'y': 0, 'z': 0}

    def view(unit, block, half=None):
        kind, colour = unit[:2]
        x, z, y = (EVERY if block[d] is None else ring[d][block[d]] for d in 'xzy')
        r0, rn = (0, 32) if half is None else (16 * half, 16)
        if kind == 'ch':
            c0, cn = COLS[colour]
            g = EVERY if len(unit) == 2 else unit[2]
            return wc.at[g, x, z, y, core, pl.ds(r0, rn), pl.ds(c0, cn)]
        cols = pl.ds(0, CH) if x is EVERY else columns[block['x']]
        if kind == 'stem':
            return ws.at[z, y, core, pl.ds(32 * colour + r0, rn), cols]
        return wh.at[z, y, core, pl.ds(r0, rn), cols]

    def piece(unit):
        kind, colour = unit
        if kind == 'ch':
            return pc.at[:, :, pl.ds(*COLS[colour])]
        return ps.at[pl.ds(32 * colour, 32), :] if kind == 'stem' else ph.at[:, :]

    def exchange(unit, tag, dim, block):
        for side, step in (('l', 1), ('r', 3)):
            def build(step=step):
                part = view(unit, block)
                return (piece(unit) if tag == '1' else part), part, peers[dim, step]
            net.start((unit, tag, side), build)

    def forward_half(unit, tag, dim, block):
        for half, (origin, target, side) in enumerate(((3, 1, 'l'), (1, 3, 'r'))):
            def build(half=half, origin=origin, target=target):
                part = view(unit, {**block, dim: origin}, half)
                return part, part, peers[dim, target]
            net.start((unit, tag, side), build)

    def swap(unit, tag, block):
        def build():
            part = view(unit, block)
            return part, part, partner
        net.start((unit, tag), build)

    own = pltpu.make_async_copy(pc, wc.at[:, me['x'], me['z'], me['y'], me['k']], sem.at[1])
    own.start()
    mine = pl.ds(pl.multiple_of(me['x'] * 256, 256), 256)
    ws[me['z'], me['y'], me['k'], :, mine] = ps[...]
    wh[me['z'], me['y'], me['k'], :, mine] = ph[...]
    sm_v[me['x'], me['z'], me['y'], me['k']] = sm_p[...]
    tk_v[:, me['z'], me['y'], me['k']] = tk_p[...]
    bh_v[:, mine] = bh_p[...]
    own.wait()
    pl.semaphore_wait(barrier, 10)

    def small(kind, n):
        dims = 'xyz' if kind == 'sm' else 'yz'
        at = {d: EVERY if d in dims[:n] else ring[d][0] for d in 'xyz'}

        def part():
            if kind == 'sm':
                return sm_v.at[at['x'], at['z'], at['y'], core]
            return tk_v.at[:, at['z'], at['y'], core]
        if n > 0:
            net.arrived(*[(kind, n - 1, s) for s in (1, 2, 3)])
        if n < len(dims):
            for s in (1, 2, 3):
                net.start((kind, n, s), lambda s=s: (part(), part(), peers[dims[n], s]))
            if kind == 'sm' and n == 0:
                def head_bias():
                    return bh_v.at[:, columns[0]]
                for s in (1, 2, 3):
                    net.start(('bh', s), lambda s=s: (head_bias(), head_bias(), peers['x', s]))
        else:
            net.start((kind, 'k'), lambda: (part(), part(), partner))

    def step(name, unit):
        if name[0] == 'M':
            small(unit[0], int(name[1]))
            return
        d1, d2, d3 = ORDERS[unit[1]]
        early = unit[:2]
        plane = {**here, d1: None, d2: None}
        if name == 'A0':
            exchange(unit, '1', d1, here)
        elif name == 'A':
            net.arrived((unit, '1', 'l'), (unit, '1', 'r'))
            forward_half(unit, '1h', d1, here)
        elif name == 'B':
            net.arrived((unit, '1h', 'l'), (unit, '1h', 'r'))
            exchange(unit, '2', d2, {**here, d1: None})
        elif name == 'C':
            net.arrived((unit, '2', 'l'), (unit, '2', 'r'))
            forward_half(unit, '2h', d2, {**here, d1: None})
        elif name == 'D':
            if early not in planes:
                planes.add(early)
                net.arrived((early, '2h', 'l'), (early, '2h', 'r'))
            exchange(unit, '3', d3, plane)
            swap(unit, 'k0', plane)
        elif name == 'E':
            net.arrived((unit, '3', 'l'), (unit, '3', 'r'))
            forward_half(unit, '3h', d3, plane)
            for n in (1, 3):
                swap(unit, f'k{n}', {**plane, d3: n})
        else:
            net.arrived((unit, '3h', 'l'), (unit, '3h', 'r'))
            swap(unit, 'k2', {**plane, d3: 2})

    planes = set()
    awaited = set()

    def need(group):
        for u in LATE:
            if UNIT_GROUP[u[0], u[2]] <= group and u not in awaited:
                awaited.add(u)
                net.arrived(*[(u, f'k{n}') for n in range(4)])

    bursts = {name: steps for name, steps in FRONT_ORDER}

    def burst(name):
        for s in bursts.get(name, ()):
            step(*s)

    def during(name, count):
        def run(i):
            for n in range(1, count):
                if bursts.get(f'{name}{n}'):
                    pl.when(i == n)(functools.partial(burst, f'{name}{n}'))
        return run

    burst('prep')
    load_p.wait()
    keep_p = pltpu.make_async_copy(p_v, pat_out, sem.at[0])
    keep_p.start()

    burst('unpack')
    net.arrived(('sm', 'k'), ('tk', 'k'), ('bh', 1), ('bh', 2), ('bh', 3))
    sm_2[...] = sm_v[...].reshape(1024, 128)
    for n in range(8):
        vec[:, pl.ds(128 * n, 128)] = sm_2[pl.ds(128 * n, 128), :].T[0:16, :]
    wt[...] = tk_v[...].reshape(4, TOKH, 128)
    for l in range(2):
        rows = jnp.concatenate(three_parts(sm_2[pl.ds(l, 128, stride=8), :]), axis=0)

        @pl.loop(0, 8)
        def _(n):
            lane = lax.broadcasted_iota(jnp.int32, (128, 512), 0)
            col = lax.broadcasted_iota(jnp.int32, (128, 512), 1)
            pick = jnp.where(lane == 32 + col % 32, 1.0, 0.0).astype(bf16)
            spread = dot_nn(rows, pick)
            value = spread[0:128] + spread[128:256] + spread[256:384]
            mine = lane == n * 16 + col // 32
            bch1[l:l + 1, pl.ds(pl.multiple_of(n * 512, 512), 512)] = jnp.sum(jnp.where(mine, value, 0.0), axis=0, keepdims=True)

    burst('stem0')
    need(0)
    run = during('stem', 4)
    put(x_v, pl.ds(ROWS, XROWS - ROWS), jnp.zeros((XROWS - ROWS, CH), f32))

    @pl.loop(0, 4)
    def _(i):
        run(i)
        cols = pl.ds(pl.multiple_of(i * 256, 256), 256)
        w = ws[:, :, :, :, cols].reshape(3072, 256)
        value = dot_nn(p_v[...].reshape(ROWS, 3072), w) + vec[0:1, cols]
        for n in range(2):
            x_v[2 * i + n, pl.ds(0, ROWS), :] = value[:, 128 * n:128 * (n + 1)]

    wc_all = wc

    def add_rows(value):
        for n in range(CH // 128):
            x_v[n, pl.ds(0, ROWS), :] += value[:, 128 * n:128 * (n + 1)]

    for l in range(2):
        r = 1 + 5 * l
        burst(f'tok{l}_0')
        run = during(f'tok{l}_', IMG)
        save_in = pltpu.make_async_copy(x_v.at[:, pl.ds(0, ROWS)], xin.at[l], sem_x.at[0])
        save_in.start()
        save_in.wait()

        @pl.loop(0, IMG)
        def _(b):
            run(b)
            x = get(x_v, image(b))
            std, _ = standardize(x)
            a = with_bias_rows(std * vec[r:r + 1, :] + vec[r + 1:r + 2, :])
            g_v[...] = gelu(dot_nn(wt[l, :, 0:TPAD], a)).astype(bf16)
            put(x_v, image(b), x + dot_tn(wt[2 + l, :, 0:TPAD], g_v[...]))
        save_mid = pltpu.make_async_copy(x_v.at[:, pl.ds(0, ROWS)], xmid.at[l], sem_x.at[0])
        save_mid.start()
        burst(f'ln{l}')

        for at, size in CHUNKS:
            std, _ = standardize(get(x_v, pl.ds(at, size)))
            v_v[pl.ds(at, size), :] = (std * vec[r + 2:r + 3, :] + vec[r + 3:r + 4, :]).astype(bf16)
        save_v = pltpu.make_async_copy(v_v, vout.at[l], sem_x.at[1])
        save_v.start()
        burst(f'ch{l}_0')
        need(2 + 2 * l)
        save_mid.wait()

        def blocks(i, slot):
            t, h = i // 2, i % 2
            part = pl.ds(pl.multiple_of(h * BLK, BLK), BLK)
            half = [pl.ds(pl.multiple_of(h * 2, 2), 2)]
            return [(wc_all.at[2 * l, t, :, :, :, :, part], w1_v.at[slot]), (wc_all.at[2 * l + 1, t, *half], w2_v.at[slot])]

        def outs(i, slot):
            part = pl.ds(pl.multiple_of(i * BLK, BLK), BLK)
            return [(pre_v.at[slot], pre_out.at[l, :, part]), (act_v.at[slot], act_out.at[l, :, part])]
        run = during(f'ch{l}_', NBLK)

        def channel(i, slot):
            run(i)
            part = pl.ds(pl.multiple_of(i * BLK, BLK), BLK)
            h = dot_nn(v_v[...], w1_v[slot].reshape(CH, BLK)) + bch1[l:l + 1, part]
            pre_v[slot] = h
            act_v[slot] = gelu(h).astype(bf16)
            add_rows(dot_nn(act_v[slot], w2_v[slot].reshape(BLK, CH)))
        for_blocks(Stream(sem_w, blocks, NBLK), channel, Stream(sem_o, outs, NBLK))
        add_rows(jnp.broadcast_to(vec[r + 4:r + 5, :], (ROWS, CH)))
        save_v.wait()

    burst('head')
    need(5)
    keep_p.wait()
    last = 11
    pooled = jnp.sum(get(x_v, pl.ds(0, ROWS)).reshape(TOK, IMG, CH), axis=0) * (1.0 / TOK)
    std, inv = standardize(pooled)
    head_in = (std * vec[last:last + 1, :] + vec[last + 1:last + 2, :]).astype(bf16)
    hl[...] = head_in
    w_h = wh[...].reshape(CH, CH)
    logits = dot_nn(head_in, w_h) + bh_v[0:1, :]
    row = lax.broadcasted_iota(jnp.int32, (IMG, 1), 0)
    label = jnp.zeros((IMG, 1), jnp.int32)
    for b in range(IMG):
        value = labels[me['x'] * IMG + b]
        label = jnp.where(row == b, value, label)
    label = label + 6 * sum(jnp.where(label >= edge, 1, 0) for edge in (250, 500, 750))
    is_label = lax.broadcasted_iota(jnp.int32, logits.shape, 1) == label
    top = jnp.max(logits, axis=-1, keepdims=True)
    ex = jnp.exp(logits - top)
    es = jnp.sum(ex, axis=-1, keepdims=True)
    nll = top + jnp.log(es) - jnp.sum(jnp.where(is_label, logits, 0.0), axis=-1, keepdims=True)
    d_logits = (ex / es - jnp.where(is_label, 1.0, 0.0)) * (1.0 / 1024)
    gbh[...] = jnp.sum(d_logits, axis=0, keepdims=True)
    d_bf = d_logits.astype(bf16)
    hr[...] = d_bf
    d_in = dot_nt(d_bf, w_h)
    hstat[0:1, :] = jnp.sum(d_in * std, axis=0, keepdims=True)
    hstat[1:2, :] = jnp.sum(d_in, axis=0, keepdims=True)
    hstat[2:3, :] = jnp.broadcast_to(jnp.sum(nll, axis=0, keepdims=True), (1, CH))
    dx0[...] = norm_grad(d_in, vec[last:last + 1, :], std, inv) * (1.0 / TOK)
    burst('end')
    net.finish()
    assert len(net.builds) <= FRONT_COPIES, len(net.builds)


def front(*operands):
    a, v = pl.BlockSpec(memory_space=pl.ANY), pl.BlockSpec(memory_space=pltpu.VMEM)
    S, V, DMA = jax.ShapeDtypeStruct, pltpu.VMEM, pltpu.SemaphoreType.DMA
    return pl.pallas_call(
        front_kernel, name='front',
        in_specs=[pl.BlockSpec(memory_space=pltpu.SMEM), a] + [v] * 17,
        out_specs=[a] * 7 + [v] * 7,
        out_shape=[S((N_CH, 4, 4, 4, 2, 32, 1024), bf16), S((TOK, IMG, 3072), bf16), S((2, CH // 128, ROWS, 128), f32),
                   S((2, CH // 128, ROWS, 128), f32),
                   S((2, ROWS, CH), bf16), S((2, ROWS, CHH), f32), S((2, ROWS, CHH), bf16), S((IMG, CH), bf16),
                   S((IMG, CH), bf16), S((IMG, CH), f32), S((8, CH), f32), S((1, CH), f32), S((16, CH), f32),
                   S((4, TOKH, 128), bf16)],
        scratch_shapes=[V((N_CH, 32, 1024), bf16), V((96, 256), bf16), V((32, 256), bf16), V((4, 16, 128), f32),
                        V((4, 16, 128), bf16), V((8, 128), f32), V((8, 256), f32), V((4, 4, 2, 96, CH), bf16),
                        V((4, 4, 2, 32, CH), bf16), V((4, 4, 4, 2, 16, 128), bf16), V((4, 4, 4, 2, 8, 128), f32),
                        V((1024, 128), f32), V((8, CH), f32), V((2, CHH), f32),
                        V((128, 128), f32), V((TOK, IMG, 3072), bf16), V((CH // 128, XROWS, 128), f32),
                        V((ROWS, CH), bf16), V((2, 4, 4, 2, 32, BLK), bf16), V((2, 2, 4, 2, 32, CH), bf16),
                        V((2, ROWS, BLK), f32), V((2, ROWS, BLK), bf16), V((TOKH, CH), bf16),
                        DMA((FRONT_COPIES,)), DMA((FRONT_COPIES,)), DMA((2,)), DMA((2, 2)), DMA((2, 2)), DMA((2,))],
        compiler_params=pltpu.CompilerParams(collective_id=0, has_side_effects=True, vmem_limit_bytes=62 * 1024 * 1024),
        cost_estimate=pl.CostEstimate(flops=90_000_000_000, bytes_accessed=180_000_000, transcendentals=0),
    )(*operands)

CHANNEL_AXES = ('tp', 'fsdp')


def weight_specs():
    vec_spec = P(CHANNEL_AXES)
    layer_vec = P(None, CHANNEL_AXES)
    return (P('fsdp', 'tp'), vec_spec, layer_vec, layer_vec, P(None, None, 'fsdp'), P(None, 'fsdp'),
            P(None, 'fsdp', None), layer_vec, layer_vec, P(None, 'fsdp', 'tp'), layer_vec,
            P(None, CHANNEL_AXES, None), layer_vec, vec_spec, vec_spec, P('fsdp', 'tp'), P('tp'))


def solution(mesh):
    def step(patches, labels, w_stem, b_stem, ln1_g, ln1_b, w_tok1, b_tok1, w_tok2,
             ln2_g, ln2_b, w_ch1, b_ch1, w_ch2, b_ch2, lnf_g, lnf_b, w_head, b_head):
        wc, pat, xin, xmid, vin, pre, act, hl, hr, dx0, hstat, gbh, vec, wt = front(
            labels, patches.transpose(1, 0, 2), w_stem, w_ch1, w_ch2, w_head, w_tok1.transpose(0, 2, 1), w_tok2, b_tok1, b_ch1,
            b_head, b_stem, ln1_g, ln1_b, ln2_g, ln2_b, b_ch2, lnf_g, lnf_b)
        pat = pat.reshape(ROWS, -1)
        dpre, dout, dstem, sm, tk = backward(xin, xmid, pre, wc, wt, vec, dx0, hstat, gbh)

        loss, g_s, g_bs, g_1g, g_1b, g_t1, g_bt, g_t2, g_2g, g_2b, g_c1, g_b1, g_c2, g_b2, g_fg, g_fb, g_h, g_bh = reduce_gradients(
            dpre, act, pat, vin, dout, dstem, hl, hr, sm.reshape(4, 4, 4, 2, 8, 128), tk.reshape(4, 4, 4, 2, 16, 128))
        return (loss.reshape(()), g_s, g_bs, g_1g, g_1b, g_t1.transpose(0, 2, 1), g_bt, g_t2, g_2g, g_2b, g_c1, g_b1, g_c2, g_b2,
                g_fg, g_fb, g_h, g_bh)

    specs = weight_specs()
    return jax.shard_map(step, mesh=mesh, in_specs=(P('fsdp', None, None), P('fsdp')) + specs,
                         out_specs=(P(),) + specs, check_vma=False)
```

```python
import functools

import jax
import jax.numpy as jnp
from jax import lax
from jax.experimental import pallas as pl
from jax.experimental.pallas import tpu as pltpu
from jax.sharding import PartitionSpec as P

MESH = pl.DeviceIdType.MESH
ORDERS = (('x', 'y', 'z'), ('y', 'z', 'x'), ('z', 'x', 'y'))
COLS = ((0, 384), (384, 384), (768, 256))
N_CH = 4
STEM, HEAD = 4, 5
bf16, f32 = jnp.bfloat16, jnp.float32


def my_place():
    f = lax.axis_index('fsdp')
    return {'x': lax.axis_index('tp'), 'z': f // 8, 'y': (f // 2) % 4, 'k': f % 2}


def moved(place, dim, step):
    new = dict(place)
    new[dim] = 1 - place['k'] if dim == 'k' else (place[dim] + step) % 4
    return new


def device(place):
    return {'tp': place['x'], 'fsdp': (place['z'] * 4 + place['y']) * 2 + place['k']}


class Sender:
    def __init__(self, send_sems, recv_sems):
        self.send_sems, self.recv_sems, self.count, self.started = send_sems, recv_sems, 0, []

    def start(self, src, dst, target):
        n = self.count
        self.count += 1
        copy = pltpu.make_async_remote_copy(src_ref=src, dst_ref=dst, send_sem=self.send_sems.at[n],
                                            recv_sem=self.recv_sems.at[n], device_id=device(target),
                                            device_id_type=MESH)
        copy.start()
        self.started.append(copy)
        return copy


GROUPS = (STEM, 3, 2, 1, 0, HEAD)
UNITS = tuple((g, c) for g in GROUPS for c in (2, 0, 1) if g != HEAD or c == 2)
REDUCE_COPIES = 13 * len(UNITS) + 20
SMALL_AT = (2, 10, 20, 32, 44, 56)
ORDER = (0, 1, 2, 3, 4, 0, 5, 1, 2, 0, 3, 1, 2, 0, 4, 6, 3, 1, 7, 5, 0, 6, 4, 1, 2, 8, 0, 6, 7, 5, 2, 3, 1, 9, 0, 8, 4, 10, 7, 9, 1, 2,
         3, 0, 5, 11, 8, 9, 10, 1, 4, 5, 2, 11, 3, 6, 12, 10, 2, 5, 8, 6, 4, 7, 13, 11, 12, 3, 4, 7, 8, 14, 5, 12, 6, 13, 4, 9,
         15, 5, 8, 11, 3, 14, 13, 6, 7, 8, 9, 10, 11, 15, 7, 14, 6, 11, 10, 15, 7, 8, 9, 12, 11, 12, 14, 11, 10, 9, 13, 12, 15,
         14, 10, 9, 13, 12, 15, 14, 10, 13, 15, 12, 14, 13, 15, 14, 15, 13)


def reduce_scratch():
    per = []
    for c in range(3):
        n = COLS[c][1]
        many = sum(1 for u in UNITS if u[1] == c)
        lead = ((4, 4), (4,), ())
        b = {'C': pltpu.VMEM((2, 4, 4, 4, 2, 32, n), bf16), 'D': pltpu.VMEM((2, 4, 4, 4, 32, n), bf16),
             'S1': pltpu.VMEM((4, 4, 32, n), f32), 'S2': pltpu.VMEM((2, 4, 32, n), f32)}
        for ph in range(3):
            for name in ('opp', 'rig', 'lef'):
                b[f'{name}{ph}'] = pltpu.VMEM(lead[ph] + (32, n), bf16)
            for name in ('half0', 'half1'):
                b[f'{name}{ph}'] = pltpu.VMEM((many,) + lead[ph] + (16, n), bf16)
            for name in ('froml', 'fromr'):
                b[f'{name}{ph}'] = pltpu.VMEM((many,) + lead[ph] + (32, n), bf16)
        per.append(b)
    return per


def transposed_product(left, right):
    return lax.dot_general(left, right, (((0,), (0,)), ((), ())), preferred_element_type=f32)


def reduce_kernel(*refs):
    dpre, act, pat, vin, dout, dstem, head_l, head_r = refs[:8]
    sm_in, tk_in, refs = refs[8], refs[9], refs[:8] + refs[10:]
    wides = [dpre.at[0], act.at[0], dpre.at[1], act.at[1], pat]
    narrows = [vin.at[0], dout.at[0], vin.at[1], dout.at[1], dstem]
    out_c, out_s, out_h, sm_own, tk_own = refs[8:13]
    wide, narrow, per, small, send_sems, recv_sems, load_sems, credit = refs[13:]
    small.update(sm_own=sm_own, tk_own=tk_own)
    me = my_place()
    other = moved(me, 'k', 1)
    k = me['k']
    loads = {}

    def load(i):
        g = GROUPS[i]
        if g == HEAD:
            return
        cols = 3072 if g == STEM else 4096
        loads[g] = [pltpu.make_async_copy(wides[g], wide.at[i % 2, :, pl.ds(0, cols)], load_sems.at[i % 2, 0]),
                    pltpu.make_async_copy(narrows[g], narrow.at[i % 2], load_sems.at[i % 2, 1])]
        for copy in loads[g]:
            copy.start()

    load(0)
    barrier = pltpu.get_barrier_semaphore()
    for dim in 'xyz':
        for step in (1, 2, 3):
            pl.semaphore_signal(barrier, inc=1, device_id=device(moved(me, dim, step)), device_id_type=MESH)
    pl.semaphore_signal(barrier, inc=1, device_id=device(other), device_id_type=MESH)
    mine = [pltpu.make_async_copy(sm_in.at[:, :, :, k], small['sm0'], load_sems.at[2, 0]),
            pltpu.make_async_copy(tk_in.at[:, :, :, k], small['tk0'], load_sems.at[2, 1])]
    for copy in mine:
        copy.start()
    pl.semaphore_wait(barrier, 10)
    sender = Sender(send_sems, recv_sems)
    busy = {}

    def free(key):
        for copy in busy.pop(key, ()):
            copy.wait_send()

    def make(g, c, cslot):
        i = GROUPS.index(g)
        slot = i % 2
        if g != HEAD and c == 2:
            for copy in loads[g]:
                copy.wait()
            load(i + 1)
        if g == STEM:
            if c != 2:
                return
            @pl.loop(0, 32)
            def _(j):
                b = j // 4
                t = j % 4
                z, y2 = b // 2, b % 2
                left = wide[slot, :, pl.ds(pl.multiple_of(b * 384, 128), 384)]
                right = narrow[slot, :, pl.ds(pl.multiple_of(t * 256, 128), 256)]
                prod = transposed_product(left, right).astype(bf16).reshape(2, 2, 3, 32, 256)
                for d in range(3):
                    per[d]['C'][0, t, z, pl.ds(y2 * 2, 2), :, :, pl.ds(0, 256)] = prod[:, :, d]
        elif g == HEAD:

            @pl.loop(0, 4)
            def _(t):
                right = head_r[:, pl.ds(pl.multiple_of(t * 256, 128), 256)]
                prod = transposed_product(head_l[...], right)
                per[c]['C'][cslot, t] = prod.astype(bf16).reshape(4, 4, 2, 32, 256)
        else:
            c0, n = COLS[c]

            @pl.loop(0, 16)
            def _(j):
                t, z = j // 4, j % 4
                if g % 2 == 0:
                    left = narrow[slot, :, pl.ds(pl.multiple_of(z * 256, 128), 256)]
                    right = wide[slot, :, pl.ds(pl.multiple_of(t * 1024 + c0, 128), n)]
                else:
                    left = wide[slot, :, pl.ds(pl.multiple_of(j * 256, 128), 256)]
                    right = narrow[slot, :, pl.ds(c0, n)]
                per[c]['C'][cslot, t, z] = transposed_product(left, right).astype(bf16).reshape(4, 2, 32, n)

    class Unit:
        def __init__(self, g, c):
            self.g, self.c = g, c
            same = [u for u in UNITS if u[1] == c]
            self.index = same.index((g, c))
            self.slot = self.index % 2
            self.last = self.index >= len(same) - 2
            self.n = COLS[c][1] if g < N_CH else 256
            self.buf = per[c]
            self.dims = ORDERS[c]

        def cut(self, name, *at):
            ref = self.buf[name]
            rest = len(ref.shape) - len(at) - 1
            return ref.at[(*at, *[slice(None)] * rest, pl.ds(0, self.n))]

        def share(self, phase, p, e, rows):
            r = pl.ds(*rows)
            cols = pl.ds(0, self.n)
            if phase == 0:
                at = dict(zip(self.dims, (p, *e)))
                at = (at['x'], at['z'], at['y'])
                return (self.buf['C'][(self.slot, *at, k, r, cols)].astype(f32)
                        + self.buf['D'][(self.slot, *at, r, cols)].astype(f32))
            lead = () if phase == 1 else (self.index % 2,)
            return self.buf[f'S{phase}'][(*lead, p, *e, r, cols)]

        def each(self, phase, body):
            if phase == 2:
                body(())
            elif phase == 1:
                pl.loop(0, 4)(lambda i: body((i,)))
            else:
                pl.loop(0, 16)(lambda i: body((i // 4, i % 4)))

        def start(self):
            free(('C', self.c, self.slot))
            make(self.g, self.c, self.slot)
            if self.index > 1:
                pl.semaphore_wait(credit.at[self.c], 1)
            cols = pl.ds(0, self.n)
            src = self.buf['C'].at[self.slot, :, :, :, 1 - k, :, cols]
            self.swap = sender.start(src, self.buf['D'].at[self.slot, :, :, :, :, cols], other)
            busy['C', self.c, self.slot] = [self.swap]

        def opposite(self, phase):
            if phase == 0:
                self.swap.wait_recv()
            p = (me[self.dims[phase]] + 2) % 4
            free((f'opp{phase}', self.c))
            cols = pl.ds(0, self.n)

            def body(e):
                self.buf[f'opp{phase}'][(*e, slice(None), cols)] = self.share(phase, p, e, (0, 32)).astype(bf16)
            self.each(phase, body)
            lead = [slice(None)] * (2 - phase)
            copies = []
            for half, step in ((0, 1), (1, 3)):
                src = self.buf[f'opp{phase}'].at[(*lead, pl.ds(16 * half, 16), cols)]
                dst = self.cut(f'half{half}{phase}', self.index)
                copies.append(sender.start(src, dst, moved(me, self.dims[phase], step)))
            busy[f'opp{phase}', self.c] = copies
            self.halves = copies

        def beside(self, phase):
            copies = []
            for half, step, name, dst in ((0, 1, 'rig', 'froml'), (1, 3, 'lef', 'fromr')):
                self.halves[half].wait_recv()
                free((f'{name}{phase}', self.c))
                p = (me[self.dims[phase]] + step) % 4
                cols = pl.ds(0, self.n)
                whole, got = self.buf[f'{name}{phase}'], self.buf[f'half{half}{phase}']

                def body(e):
                    mine = self.share(phase, p, e, (16 * half, 16)) + got[(self.index, *e, slice(None), cols)].astype(f32)
                    whole[(*e, pl.ds(16 * half, 16), cols)] = mine.astype(bf16)
                    plain = self.share(phase, p, e, (16 - 16 * half, 16))
                    whole[(*e, pl.ds(16 - 16 * half, 16), cols)] = plain.astype(bf16)
                self.each(phase, body)
                copy = sender.start(self.cut(f'{name}{phase}'), self.cut(f'{dst}{phase}', self.index),
                                    moved(me, self.dims[phase], step))
                busy[f'{name}{phase}', self.c] = [copy]
                copies.append(copy)
            self.wholes = copies

        def total(self, phase):
            for copy in self.wholes:
                copy.wait_recv()
            p = me[self.dims[phase]]
            cols = pl.ds(0, self.n)

            def body(e):
                got = [self.buf[f'{name}{phase}'][(self.index, *e, slice(None), cols)].astype(f32)
                       for name in ('froml', 'fromr')]
                value = self.share(phase, p, e, (0, 32)) + got[0] + got[1]
                if phase == 0:
                    self.buf['S1'][(*e, slice(None), cols)] = value
                elif phase == 1:
                    self.buf['S2'][(self.index % 2, *e, slice(None), cols)] = value
                elif self.g == STEM:
                    out_s[pl.ds(32 * self.c, 32), :] = value
                elif self.g == HEAD:
                    out_h[...] = value
                else:
                    out_c[self.g, :, pl.ds(*COLS[self.c])] = value
            self.each(phase, body)
            if phase == 0 and not self.last:
                pl.semaphore_signal(credit.at[self.c], inc=1, device_id=device(other), device_id_type=MESH)

        def run(self, stage):
            if stage == 0:
                self.start()
            elif stage == 7:
                self.total(2)
            elif stage % 2 == 0:
                self.beside(stage // 2 - 1)
            else:
                if stage > 1:
                    self.total(stage // 2 - 1)
                self.opposite(stage // 2)

    units = [Unit(g, c) for g, c in UNITS]
    stage_of = [0] * len(units)
    for copy in mine:
        copy.wait()
    sums = SmallSums(me, sender, small, sm_in, tk_in)
    for n, u in enumerate(ORDER):
        if n in SMALL_AT:
            sums.step(SMALL_AT.index(n))
        units[u].run(stage_of[u])
        stage_of[u] += 1
    assert stage_of == [8] * len(units)
    sums.wait_sent()
    for key in list(busy):
        free(key)
    assert sender.count == REDUCE_COPIES, sender.count


SMALL = dict(sm=((4, 4, 4, 8, 128), (4, 4, 4, 8, 128), (3, 4, 4, 8, 128), (3, 4, 8, 128), (3, 8, 128)),
             tk=((4, 4, 4, 16, 128), (4, 4, 4, 16, 128), (3, 4, 4, 16, 128), (3, 4, 16, 128), (3, 4, 16, 128)))


def small_scratch():
    b = {f'{kind}{n}': pltpu.VMEM(shape, f32) for kind, shapes in SMALL.items() for n, shape in enumerate(shapes)}
    b.update(sm_s1=pltpu.VMEM((4, 4, 8, 128), f32), sm_s2=pltpu.VMEM((4, 8, 128), f32),
             tk_s1=pltpu.VMEM((4, 4, 16, 128), f32), tk_s2=pltpu.VMEM((4, 16, 128), f32))
    return b


class SmallSums:
    def __init__(self, me, sender, b, sm_in, tk_in):
        self.me, self.sender, self.b, self.sent, self.last = me, sender, b, [], []
        self.sm_in, self.tk_in = sm_in, tk_in

    def send(self, src, dst, target):
        copy = self.sender.start(src, dst, target)
        self.sent.append(copy)
        self.last.append(copy)

    def wait_sent(self):
        for copy in self.sent:
            copy.wait_send()

    def arrived(self):
        for copy in self.last:
            copy.wait_recv()
        self.last = []

    def step(self, n):
        me, b = self.me, self.b
        x, z, y, k = me['x'], me['z'], me['y'], me['k']
        self.arrived()
        if n == 0:
            self.send(self.sm_in.at[:, :, :, 1 - k], b['sm1'], moved(me, 'k', 1))
            self.send(self.tk_in.at[:, :, :, 1 - k], b['tk1'], moved(me, 'k', 1))
        elif n == 1:
            b['sm1'][...] += b['sm0'][...]
            b['tk1'][...] += b['tk0'][...]
            for s in (1, 2, 3):
                self.send(b['sm1'].at[(x + s) % 4], b['sm2'].at[s - 1], moved(me, 'x', s))
                self.send(b['tk1'].at[:, (z + s) % 4], b['tk2'].at[s - 1], moved(me, 'z', s))
        elif n == 2:
            b['sm_s1'][...] = b['sm1'][x] + b['sm2'][0] + b['sm2'][1] + b['sm2'][2]
            b['tk_s1'][...] = b['tk1'][:, z] + b['tk2'][0] + b['tk2'][1] + b['tk2'][2]
            for s in (1, 2, 3):
                self.send(b['sm_s1'].at[(z + s) % 4], b['sm3'].at[s - 1], moved(me, 'z', s))
                self.send(b['tk_s1'].at[:, (y + s) % 4], b['tk3'].at[s - 1], moved(me, 'y', s))
        elif n == 3:
            b['sm_s2'][...] = b['sm_s1'][z] + b['sm3'][0] + b['sm3'][1] + b['sm3'][2]
            b['tk_s2'][...] = b['tk_s1'][:, y] + b['tk3'][0] + b['tk3'][1] + b['tk3'][2]
            for s in (1, 2, 3):
                self.send(b['sm_s2'].at[(y + s) % 4], b['sm4'].at[s - 1], moved(me, 'y', s))
                self.send(b['tk_s2'], b['tk4'].at[s - 1], moved(me, 'x', s))
        elif n == 4:
            b['sm_own'][...] = b['sm_s2'][y] + b['sm4'][0] + b['sm4'][1] + b['sm4'][2]
            parts = [b['tk_s2'][...]] + [b['tk4'][s] for s in range(3)]
            ordered = []
            for place in range(4):
                value = parts[0]
                for s in (1, 2, 3):
                    value = jnp.where((x + 4 - s) % 4 == place, parts[s], value)
                ordered.append(value)
            b['tk_own'][...] = (ordered[0] + ordered[1]) + (ordered[2] + ordered[3])


def finish_kernel(c, stem, head, sm, tk, loss, o_stem, o_bstem, o_ln1g, o_ln1b, o_wt1, o_bt1, o_wt2, o_ln2g, o_ln2b, o_ch1,
                  o_bch1, o_ch2, o_bch2, o_lnfg, o_lnfb, o_head, o_bhead):
    for l in range(2):
        o_ch1[l] = c[2 * l]
        o_ch2[l] = c[2 * l + 1]
    o_stem[...] = stem[...]
    o_head[...] = head[:, 0:250]
    own = sm[...]
    turned = jnp.concatenate([own, jnp.zeros((120, 128), f32)], axis=0).T
    for ref, n in ((o_bstem, 0), (o_lnfg, 11), (o_lnfb, 12)):
        ref[...] = turned[n, 0:8]
    for n, ref in enumerate((o_ln1g, o_ln1b, o_ln2g, o_ln2b, o_bch2)):
        for l in range(2):
            ref[pl.ds(l, 1), :] = turned[1 + 5 * l + n:2 + 5 * l + n, 0:8]
    o_bch1[...] = own[0:2, 32:64]
    classes = jnp.concatenate([own[2 + q:3 + q, 64:128] for q in range(4)], axis=1)
    o_bhead[...] = classes[0, 0:250]
    loss[...] = own[6:7, 64:65] * (1.0 / 1024)
    for l in range(2):
        o_wt1[l] = tk[l, :, 0:TOK]
        o_wt2[l] = tk[2 + l, :, 0:TOK]
        tall = jnp.concatenate([tk[l], jnp.zeros((112, 128), f32)], axis=0).T
        o_bt1[pl.ds(l, 1), :] = tall[64:65, 0:16]


def finish(*operands):
    S = jax.ShapeDtypeStruct
    v = pl.BlockSpec(memory_space=pltpu.VMEM)
    return pl.pallas_call(
        finish_kernel, name='finish', in_specs=[v] * 5, out_specs=[v] * 18,
        out_shape=[S((1, 1), f32), S((96, 256), f32), S((8,), f32), S((2, 8), f32), S((2, 8), f32), S((2, 16, TOK), f32),
                   S((2, 16), f32), S((2, 16, TOK), f32), S((2, 8), f32), S((2, 8), f32), S((2, 32, 1024), f32), S((2, 32), f32),
                   S((2, 32, 1024), f32), S((2, 8), f32), S((8,), f32), S((8,), f32), S((32, 250), f32), S((250,), f32)],
    )(*operands)


def reduce_gradients(*operands):
    any_spec = pl.BlockSpec(memory_space=pl.ANY)
    vmem = pl.BlockSpec(memory_space=pltpu.VMEM)
    rows = operands[2].shape[0]
    S = jax.ShapeDtypeStruct
    return pl.pallas_call(
        reduce_kernel, name='reduce_gradients',
        out_shape=[S((N_CH, 32, 1024), f32), S((96, 256), f32), S((32, 256), f32), S((8, 128), f32), S((4, 16, 128), f32)],
        in_specs=[any_spec] * 6 + [vmem] * 2 + [any_spec] * 2, out_specs=[vmem] * 5,
        scratch_shapes=[pltpu.VMEM((2, rows, 4096), bf16), pltpu.VMEM((2, rows, 1024), bf16), reduce_scratch(), small_scratch(),
                        pltpu.SemaphoreType.DMA((REDUCE_COPIES,)), pltpu.SemaphoreType.DMA((REDUCE_COPIES,)),
                        pltpu.SemaphoreType.DMA((3, 2)), pltpu.SemaphoreType.REGULAR((3,))],
        compiler_params=pltpu.CompilerParams(collective_id=1, has_side_effects=True, vmem_limit_bytes=64 * 1024 * 1024 - 65536),
        cost_estimate=pl.CostEstimate(flops=100_000_000_000, bytes_accessed=80_000_000, transcendentals=0),
    )(*operands)


EPS = 1e-6
TOK, TPAD = 49, 56
IMG = 8
ROWS, XROWS = IMG * TOK, IMG * TPAD
CHUNKS = ((0, 112), (112, 112), (224, 112), (336, 56))
CH, TOKH, CHH = 1024, 512, 4096
BLK = 512
NBLK = CHH // BLK
GELU_C, GELU_A = 0.7978845608028654, 0.044715


def dot_nn(a, b):
    return lax.dot_general(a, b, (((1,), (0,)), ((), ())), preferred_element_type=f32)


def dot_nt(a, b):
    return lax.dot_general(a, b, (((1,), (1,)), ((), ())), preferred_element_type=f32)


def dot_tn(a, b):
    return lax.dot_general(a, b, (((0,), (0,)), ((), ())), preferred_element_type=f32)


def gelu(x):
    half = 0.5 * x
    return half + half * jnp.tanh(x * (GELU_C + (GELU_C * GELU_A) * (x * x)))


def gelu_both(x):
    sq = x * x
    th = jnp.tanh(x * (GELU_C + (GELU_C * GELU_A) * sq))
    half = 0.5 * x
    rise = 0.5 + 0.5 * th
    slope = (1.0 - th * th) * (GELU_C + (3.0 * GELU_C * GELU_A) * sq)
    return x * rise, rise + half * slope


def standardize(x):
    mean = jnp.mean(x, axis=-1, keepdims=True)
    cent = x - mean
    inv = lax.rsqrt(jnp.mean(cent * cent, axis=-1, keepdims=True) + EPS)
    return cent * inv, inv


def norm_grad(d, gain, std, inv):
    gs = d * gain
    m0 = jnp.mean(gs, axis=-1, keepdims=True)
    m1 = jnp.mean(gs * std, axis=-1, keepdims=True)
    return inv * (gs - m0 - std * m1)


def row_mask(rows=TPAD):
    return lax.broadcasted_iota(jnp.int32, (rows, 1), 0) < TOK


def image(b):
    return pl.ds(b, TPAD, stride=IMG)


def get(ref, rows):
    return jnp.concatenate([ref[n, rows, :] for n in range(CH // 128)], axis=1)


def put(ref, rows, value):
    for n in range(CH // 128):
        ref[n, rows, :] = value[:, 128 * n:128 * (n + 1)]


class Stream:
    def __init__(self, sem, copies, count):
        self.sem, self.copies, self.count = sem, copies, count

    def make(self, i, slot):
        return [pltpu.make_async_copy(src, dst, self.sem.at[slot, n]) for n, (src, dst) in enumerate(self.copies(i, slot))]

    def start(self, i, slot):
        for copy in self.make(i, slot):
            copy.start()

    def wait(self, i, slot):
        for copy in self.make(i, slot):
            copy.wait()


def for_blocks(stream, body, out=None):
    n = stream.count
    stream.start(0, 0)

    @pl.loop(0, n)
    def _(i):
        slot = i % 2
        stream.wait(i, slot)

        @pl.when(i + 1 < n)
        def _():
            stream.start(i + 1, 1 - slot)
        if out is not None:
            @pl.when(i >= 2)
            def _():
                out.wait(i - 2, slot)
        body(i, slot)
        if out is not None:
            out.start(i, slot)
    if out is not None:
        out.wait(n - 2, n % 2)
        out.wait(n - 1, 1 - n % 2)


def small_pack(flat, turn, gvec, hstat, gbch1, gbh):
    turn[...] = jnp.zeros_like(turn)
    turn[pl.ds(0, 16), :] = gvec[...]
    turn[pl.ds(11, 2), :] = hstat[pl.ds(0, 2), :]
    for n in range(8):
        flat[pl.ds(128 * n, 128), :] = turn[:, pl.ds(128 * n, 128)].T
    for l in range(2):
        total = jnp.zeros((384, 128), f32)
        for n in range(8):
            lane = lax.broadcasted_iota(jnp.int32, (128, 512), 0)
            col = lax.broadcasted_iota(jnp.int32, (128, 512), 1)
            mine = jnp.where(lane == n * 16 + col // 32, gbch1[l:l + 1, 512 * n:512 * (n + 1)], 0.0)
            pick = jnp.where(lane == 32 + col % 32, 1.0, 0.0).astype(bf16)
            total += lax.dot_general(jnp.concatenate(three_parts(mine), axis=0), pick, (((1,), (1,)), ((), ())),
                                     preferred_element_type=f32)
        flat[pl.ds(l, 128, stride=8), :] += total[0:128] + total[128:256] + total[256:384]
    high = lax.broadcasted_iota(jnp.int32, (1, 128), 1) >= 64
    for t in range(4):
        for q in range(4):
            tile = gbh[0:1, t * 256 + q // 2 * 128:t * 256 + q // 2 * 128 + 128]
            if q % 2 == 0:
                tile = jnp.concatenate([tile[:, 64:], tile[:, :64]], axis=1)
            flat[pl.ds(t * 256 + 2 + q, 32, stride=8), :] += jnp.where(high, tile, 0.0)
    at64 = lax.broadcasted_iota(jnp.int32, (1, 128), 1) == 64
    flat[pl.ds(6, 128, stride=8), :] += jnp.where(at64, hstat[2:3, 0:128], 0.0)


def backward_kernel(xin, xmid, pre_in, wc, wt, vec, dx0, hstat, gbh,
                    dpre, dout, dstem, flat, tk, gvec, gbch1, turn, x_v, d_v, dv_v, do_v, w1_v, w2_v, pre_v, dp_v, g_v, dh_v, sem, sem_w, sem_o):
    mask = row_mask()
    rest = pl.ds(ROWS, XROWS - ROWS)
    put(d_v, rest, jnp.zeros((XROWS - ROWS, CH), f32))
    put(x_v, rest, jnp.zeros((XROWS - ROWS, CH), f32))

    @pl.loop(0, TOK)
    def _(s):
        put(d_v, pl.ds(pl.multiple_of(s * IMG, IMG), IMG), dx0[...])
    gvec[...] = jnp.zeros_like(gvec)
    tk[...] = jnp.zeros_like(tk)

    def add(row, value):
        gvec[row:row + 1, :] += jnp.sum(value, axis=0, keepdims=True)

    for l in (1, 0):
        r = 1 + 5 * l
        load = pltpu.make_async_copy(xmid.at[l], x_v.at[:, pl.ds(0, ROWS)], sem.at[0])
        load.start()

        for at, size in CHUNKS:
            d = get(d_v, pl.ds(at, size))
            add(r + 4, d)
            do_v[pl.ds(at, size), :] = d.astype(bf16)
        send = pltpu.make_async_copy(do_v, dout.at[l], sem.at[1])
        send.start()

        def blocks(i, slot):
            t, h = i // 2, i % 2
            part = pl.ds(pl.multiple_of(h * BLK, BLK), BLK)
            whole = pl.ds(pl.multiple_of(i * BLK, BLK), BLK)
            return [(wc.at[2 * l, t, :, :, :, :, part], w1_v.at[slot]),
                    (wc.at[2 * l + 1, t, pl.ds(pl.multiple_of(h * 2, 2), 2)], w2_v.at[slot]),
                    (pre_in.at[l, :, whole], pre_v.at[slot])]

        def outs(i, slot):
            return [(dp_v.at[slot], dpre.at[l, :, pl.ds(pl.multiple_of(i * BLK, BLK), BLK)])]

        def channel(i, slot):
            _, slope = gelu_both(pre_v[slot])
            d = dot_nt(do_v[...], w2_v[slot].reshape(BLK, CH)) * slope
            gbch1[l:l + 1, pl.ds(pl.multiple_of(i * BLK, BLK), BLK)] = jnp.sum(d, axis=0, keepdims=True)
            dp_v[slot] = d.astype(bf16)
            part = dot_nt(dp_v[slot], w1_v[slot].reshape(CH, BLK))

            @pl.when(i == 0)
            def _():
                dv_v[...] = part

            @pl.when(i > 0)
            def _():
                dv_v[...] += part
        for_blocks(Stream(sem_w, blocks, NBLK), channel, Stream(sem_o, outs, NBLK))
        load.wait()
        send.wait()

        @pl.loop(0, ROWS // TPAD)
        def _(n):
            rows = pl.ds(pl.multiple_of(n * TPAD, TPAD), TPAD)
            std, inv = standardize(get(x_v, rows))
            d = dv_v[rows, :]
            add(r + 2, d * std)
            add(r + 3, d)
            put(d_v, rows, get(d_v, rows) + norm_grad(d, vec[r + 2:r + 3, :], std, inv))
        load = pltpu.make_async_copy(xin.at[l], x_v.at[:, pl.ds(0, ROWS)], sem.at[0])
        load.start()
        load.wait()

        @pl.loop(0, IMG)
        def _(b):
            std, inv = standardize(get(x_v, image(b)))
            a = with_bias_rows(std * vec[r:r + 1, :] + vec[r + 1:r + 2, :])
            d_mid = get(d_v, image(b))
            dm = d_mid.astype(bf16)
            act, slope = gelu_both(dot_nn(wt[l, :, 0:TPAD], a))
            g_v[...] = act.astype(bf16)
            dh = dot_nn(wt[2 + l, :, 0:TPAD], dm) * slope
            tk[l, :, pl.ds(64, 1)] += jnp.sum(dh, axis=-1, keepdims=True)
            dh_v[...] = dh.astype(bf16)
            tk[2 + l, :, pl.ds(0, TPAD)] += dot_nt(g_v[...], dm)
            tk[l, :, pl.ds(0, TPAD)] += dot_nt(dh_v[...], a)
            d = jnp.where(mask, dot_tn(wt[l, :, 0:TPAD], dh_v[...]), 0.0)
            add(r, d * std)
            add(r + 1, d)
            put(d_v, image(b), d_mid + norm_grad(d, vec[r:r + 1, :], std, inv))

    for at, size in CHUNKS:
        d = get(d_v, pl.ds(at, size))
        add(0, d)
        do_v[pl.ds(at, size), :] = d.astype(bf16)
    send = pltpu.make_async_copy(do_v, dstem, sem.at[1])
    send.start()
    small_pack(flat, turn, gvec, hstat, gbch1, gbh)
    send.wait()


def backward(*operands):
    a, v = pl.BlockSpec(memory_space=pl.ANY), pl.BlockSpec(memory_space=pltpu.VMEM)
    S = jax.ShapeDtypeStruct
    return pl.pallas_call(
        backward_kernel, name='backward',
        in_specs=[a] * 4 + [v] * 5,
        out_specs=[a] * 3 + [v] * 2,
        out_shape=[S((2, ROWS, CHH), bf16), S((2, ROWS, CH), bf16), S((ROWS, CH), bf16), S((1024, 128), f32),
                   S((4, TOKH, 128), f32)],
        scratch_shapes=[pltpu.VMEM((16, CH), f32), pltpu.VMEM((2, CHH), f32), pltpu.VMEM((128, 1024), f32),
                        pltpu.VMEM((CH // 128, XROWS, 128), f32), pltpu.VMEM((CH // 128, XROWS, 128), f32), pltpu.VMEM((ROWS, CH), f32),
                        pltpu.VMEM((ROWS, CH), bf16), pltpu.VMEM((2, 4, 4, 2, 32, BLK), bf16),
                        pltpu.VMEM((2, 2, 4, 2, 32, CH), bf16),
                        pltpu.VMEM((2, ROWS, BLK), f32), pltpu.VMEM((2, ROWS, BLK), bf16), pltpu.VMEM((TOKH, CH), bf16),
                        pltpu.VMEM((TOKH, CH), bf16), pltpu.SemaphoreType.DMA((2,)), pltpu.SemaphoreType.DMA((2, 3)),
                        pltpu.SemaphoreType.DMA((2, 1))],
        compiler_params=pltpu.CompilerParams(vmem_limit_bytes=60 * 1024 * 1024),
        cost_estimate=pl.CostEstimate(flops=50_000_000_000, bytes_accessed=100_000_000, transcendentals=0),
    )(*operands)


FRONT_COPIES = 240
EARLY = [('stem', 0), ('stem', 1), ('stem', 2), ('ch', 0), ('ch', 1), ('ch', 2), ('head', 2)]
LATE = [('stem', c, None) for c in range(3)] + [('ch', c, g) for g in range(N_CH) for c in range(3)] + [('head', 2, None)]
UNIT_GROUP = {('stem', None): 0, ('ch', 0): 1, ('ch', 1): 2, ('ch', 2): 3, ('ch', 3): 4, ('head', None): 5}
EVERY = pl.ds(0, 4)
FRONT_ORDER = (
    ('prep', (('M0', ('sm',)), ('M0', ('tk',)), ('A0', ('stem', 0)), ('A0', ('stem', 1)), ('A0', ('stem', 2)),
        ('A0', ('ch', 0)), ('A0', ('ch', 1)), ('A0', ('ch', 2)), ('A0', ('head', 2)),)),
    ('unpack', (('M1', ('sm',)), ('M1', ('tk',)), ('A', ('stem', 0)), ('A', ('stem', 1)), ('A', ('stem', 2)),
        ('A', ('head', 2)), ('A', ('ch', 2)), ('A', ('ch', 0)), ('A', ('ch', 1)), ('B', ('stem', 0)), ('M2', ('sm',)),
        ('B', ('stem', 1)), ('M2', ('tk',)), ('B', ('stem', 2)), ('B', ('ch', 0)), ('B', ('head', 2)), ('B', ('ch', 1)),
        ('C', ('stem', 0)), ('B', ('ch', 2)), ('M3', ('sm',)), ('C', ('stem', 2)), ('C', ('stem', 1)), ('C', ('head', 2)),)),
    ('stem0', (('D', ('stem', 2, None)), ('D', ('stem', 0, None)), ('C', ('ch', 2)), ('C', ('ch', 0)),
        ('D', ('stem', 1, None)), ('C', ('ch', 1)), ('D', ('ch', 2, 0)), ('D', ('ch', 2, 1)), ('E', ('stem', 2, None)),
        ('E', ('stem', 0, None)), ('E', ('stem', 1, None)), ('D', ('ch', 0, 0)), ('D', ('ch', 0, 1)), ('D', ('ch', 1, 0)),
        ('D', ('ch', 1, 1)), ('F', ('stem', 0, None)), ('F', ('stem', 1, None)), ('E', ('ch', 2, 0)), ('E', ('ch', 2, 1)),
        ('E', ('ch', 0, 0)), ('E', ('ch', 1, 0)), ('F', ('stem', 2, None)), ('F', ('ch', 2, 0)),)),
    ('stem1', (('F', ('ch', 2, 1)), ('E', ('ch', 0, 1)), ('E', ('ch', 1, 1)), ('D', ('ch', 0, 2)), ('D', ('ch', 1, 2)),
        ('D', ('ch', 2, 2)), ('D', ('ch', 0, 3)), ('D', ('ch', 1, 3)), ('D', ('ch', 2, 3)),)),
    ('stem3', (('F', ('ch', 0, 0)),)),
    ('tok0_0', (('F', ('ch', 1, 0)),)),
    ('tok0_3', (('F', ('ch', 0, 1)),)),
    ('tok0_4', (('F', ('ch', 1, 1)),)),
    ('tok0_5', (('E', ('ch', 2, 2)),)),
    ('ch0_0', (('E', ('ch', 2, 3)), ('E', ('ch', 0, 2)), ('E', ('ch', 1, 2)), ('F', ('ch', 2, 2)),)),
    ('ch0_3', (('F', ('ch', 2, 3)),)),
    ('ch0_5', (('E', ('ch', 0, 3)), ('E', ('ch', 1, 3)), ('D', ('head', 2, None)),)),
    ('ch0_7', (('F', ('ch', 0, 2)), ('F', ('ch', 1, 2)),)),
    ('tok1_2', (('F', ('ch', 0, 3)),)),
    ('tok1_3', (('F', ('ch', 1, 3)), ('E', ('head', 2, None)),)),
    ('ln1', (('F', ('head', 2, None)),)),
)


class Net:
    def __init__(self, send_sems, recv_sems):
        self.send_sems, self.recv_sems, self.names, self.builds = send_sems, recv_sems, {}, []

    def copy(self, name):
        n = self.names[name]
        src, dst, target = self.builds[n]()
        return pltpu.make_async_remote_copy(src_ref=src, dst_ref=dst, send_sem=self.send_sems.at[n],
                                            recv_sem=self.recv_sems.at[n], device_id=target, device_id_type=MESH)

    def start(self, name, build):
        self.names[name] = len(self.builds)
        self.builds.append(build)
        self.copy(name).start()

    def arrived(self, *names):
        for name in names:
            self.copy(name).wait_recv()

    def finish(self):
        for name in self.names:
            self.copy(name).wait_send()


def three_parts(x):
    hi = x.astype(bf16)
    rest = x - hi.astype(f32)
    mid = rest.astype(bf16)
    return hi, mid, (rest - mid.astype(f32)).astype(bf16)


def with_bias_rows(a):
    row = lax.broadcasted_iota(jnp.int32, (TPAD, 1), 0)
    return jnp.where(row < TOK, a, jnp.where(row < TOK + 3, 1.0, 0.0)).astype(bf16)


def front_kernel(labels, patches, w_stem, w_ch1, w_ch2, w_head, w_tok1, w_tok2, b_tok1, b_ch1, b_head, b_stem, ln1_g, ln1_b,
                 ln2_g, ln2_b, b_ch2, lnf_g, lnf_b,
                 wc, pat_out, xin, xmid, vout, pre_out, act_out, hl, hr, dx0, hstat, gbh, vec, wt,
                 pc, ps, ph, tk_f, tk_p, sm_p, bh_p, ws, wh, tk_v, sm_v, sm_2, bh_v, bch1,
                 turn, p_v, x_v, v_v, w1_v, w2_v, pre_v, act_v, g_v,
                 send_sems, recv_sems, sem, sem_w, sem_o, sem_x):
    me = my_place()
    other = moved(me, 'k', 1)
    load_p = pltpu.make_async_copy(patches.at[:, pl.ds(pl.multiple_of(me['x'] * IMG, IMG), IMG)], p_v, sem.at[0])
    load_p.start()

    for l in range(2):
        pc[2 * l] = w_ch1[l].astype(bf16)
        pc[2 * l + 1] = w_ch2[l].astype(bf16)
    ps[...] = w_stem[...].astype(bf16)
    ph[...] = jnp.zeros_like(ph)
    ph[:, pl.ds(0, 250)] = w_head[...].astype(bf16)
    turn[...] = jnp.zeros_like(turn)
    for n, ref in ((0, b_stem), (11, lnf_g), (12, lnf_b)):
        turn[n, pl.ds(0, 8)] = ref[...]
    for n, ref in enumerate((ln1_g, ln1_b, ln2_g, ln2_b, b_ch2)):
        for l in range(2):
            turn[pl.ds(1 + 5 * l + n, 1), pl.ds(0, 8)] = ref[pl.ds(l, 1), :]
    turn[pl.ds(16, 2), pl.ds(0, 16)] = b_tok1[...]
    turned = turn[...].T
    tk_f[...] = jnp.zeros_like(tk_f)
    for l in range(2):
        tk_f[l, :, pl.ds(0, TOK)] = w_tok1[l]
        tk_f[2 + l, :, pl.ds(0, TOK)] = w_tok2[l]
        for n, part in enumerate(three_parts(turned[0:16, 16 + l:17 + l])):
            tk_f[l, :, pl.ds(TOK + n, 1)] = part.astype(f32)
    tk_p[...] = tk_f[...].astype(bf16)
    sm_p[...] = jnp.zeros_like(sm_p)
    sm_p[:, pl.ds(0, 16)] = turned[0:8, 0:16]
    sm_p[pl.ds(0, 2), pl.ds(32, 32)] = b_ch1[...]
    bh_p[...] = jnp.full_like(bh_p, -1e30)
    bh_p[0, pl.ds(0, 250)] = b_head[...]

    barrier = pltpu.get_barrier_semaphore()
    for dim in 'xyz':
        for step in (1, 2, 3):
            pl.semaphore_signal(barrier, inc=1, device_id=device(moved(me, dim, step)), device_id_type=MESH)
    pl.semaphore_signal(barrier, inc=1, device_id=device(other), device_id_type=MESH)
    net = Net(send_sems, recv_sems)
    core = me['k']
    ring = {d: [moved(me, d, n)[d] for n in range(4)] for d in 'xyz'}
    columns = [pl.ds(pl.multiple_of(x * 256, 256), 256) for x in ring['x']]
    peers = {(d, n): device(moved(me, d, n)) for d in 'xyz' for n in (1, 2, 3)}
    partner = device(other)
    here = {'x': 0, 'y': 0, 'z': 0}

    def view(unit, block, half=None):
        kind, colour = unit[:2]
        x, z, y = (EVERY if block[d] is None else ring[d][block[d]] for d in 'xzy')
        r0, rn = (0, 32) if half is None else (16 * half, 16)
        if kind == 'ch':
            c0, cn = COLS[colour]
            g = EVERY if len(unit) == 2 else unit[2]
            return wc.at[g, x, z, y, core, pl.ds(r0, rn), pl.ds(c0, cn)]
        cols = pl.ds(0, CH) if x is EVERY else columns[block['x']]
        if kind == 'stem':
            return ws.at[z, y, core, pl.ds(32 * colour + r0, rn), cols]
        return wh.at[z, y, core, pl.ds(r0, rn), cols]

    def piece(unit):
        kind, colour = unit
        if kind == 'ch':
            return pc.at[:, :, pl.ds(*COLS[colour])]
        return ps.at[pl.ds(32 * colour, 32), :] if kind == 'stem' else ph.at[:, :]

    def exchange(unit, tag, dim, block):
        for side, step in (('l', 1), ('r', 3)):
            def build(step=step):
                part = view(unit, block)
                return (piece(unit) if tag == '1' else part), part, peers[dim, step]
            net.start((unit, tag, side), build)

    def forward_half(unit, tag, dim, block):
        for half, (origin, target, side) in enumerate(((3, 1, 'l'), (1, 3, 'r'))):
            def build(half=half, origin=origin, target=target):
                part = view(unit, {**block, dim: origin}, half)
                return part, part, peers[dim, target]
            net.start((unit, tag, side), build)

    def swap(unit, tag, block):
        def build():
            part = view(unit, block)
            return part, part, partner
        net.start((unit, tag), build)

    own = pltpu.make_async_copy(pc, wc.at[:, me['x'], me['z'], me['y'], me['k']], sem.at[1])
    own.start()
    mine = pl.ds(pl.multiple_of(me['x'] * 256, 256), 256)
    ws[me['z'], me['y'], me['k'], :, mine] = ps[...]
    wh[me['z'], me['y'], me['k'], :, mine] = ph[...]
    sm_v[me['x'], me['z'], me['y'], me['k']] = sm_p[...]
    tk_v[:, me['z'], me['y'], me['k']] = tk_p[...]
    bh_v[:, mine] = bh_p[...]
    own.wait()
    pl.semaphore_wait(barrier, 10)

    def small(kind, n):
        dims = 'xyz' if kind == 'sm' else 'yz'
        at = {d: EVERY if d in dims[:n] else ring[d][0] for d in 'xyz'}

        def part():
            if kind == 'sm':
                return sm_v.at[at['x'], at['z'], at['y'], core]
            return tk_v.at[:, at['z'], at['y'], core]
        if n > 0:
            net.arrived(*[(kind, n - 1, s) for s in (1, 2, 3)])
        if n < len(dims):
            for s in (1, 2, 3):
                net.start((kind, n, s), lambda s=s: (part(), part(), peers[dims[n], s]))
            if kind == 'sm' and n == 0:
                def head_bias():
                    return bh_v.at[:, columns[0]]
                for s in (1, 2, 3):
                    net.start(('bh', s), lambda s=s: (head_bias(), head_bias(), peers['x', s]))
        else:
            net.start((kind, 'k'), lambda: (part(), part(), partner))

    def step(name, unit):
        if name[0] == 'M':
            small(unit[0], int(name[1]))
            return
        d1, d2, d3 = ORDERS[unit[1]]
        early = unit[:2]
        plane = {**here, d1: None, d2: None}
        if name == 'A0':
            exchange(unit, '1', d1, here)
        elif name == 'A':
            net.arrived((unit, '1', 'l'), (unit, '1', 'r'))
            forward_half(unit, '1h', d1, here)
        elif name == 'B':
            net.arrived((unit, '1h', 'l'), (unit, '1h', 'r'))
            exchange(unit, '2', d2, {**here, d1: None})
        elif name == 'C':
            net.arrived((unit, '2', 'l'), (unit, '2', 'r'))
            forward_half(unit, '2h', d2, {**here, d1: None})
        elif name == 'D':
            if early not in planes:
                planes.add(early)
                net.arrived((early, '2h', 'l'), (early, '2h', 'r'))
            exchange(unit, '3', d3, plane)
            swap(unit, 'k0', plane)
        elif name == 'E':
            net.arrived((unit, '3', 'l'), (unit, '3', 'r'))
            forward_half(unit, '3h', d3, plane)
            for n in (1, 3):
                swap(unit, f'k{n}', {**plane, d3: n})
        else:
            net.arrived((unit, '3h', 'l'), (unit, '3h', 'r'))
            swap(unit, 'k2', {**plane, d3: 2})

    planes = set()
    awaited = set()

    def need(group):
        for u in LATE:
            if UNIT_GROUP[u[0], u[2]] <= group and u not in awaited:
                awaited.add(u)
                net.arrived(*[(u, f'k{n}') for n in range(4)])

    bursts = {name: steps for name, steps in FRONT_ORDER}

    def burst(name):
        for s in bursts.get(name, ()):
            step(*s)

    def during(name, count):
        def run(i):
            for n in range(1, count):
                if bursts.get(f'{name}{n}'):
                    pl.when(i == n)(functools.partial(burst, f'{name}{n}'))
        return run

    burst('prep')
    load_p.wait()
    keep_p = pltpu.make_async_copy(p_v, pat_out, sem.at[0])
    keep_p.start()

    burst('unpack')
    net.arrived(('sm', 'k'), ('tk', 'k'), ('bh', 1), ('bh', 2), ('bh', 3))
    sm_2[...] = sm_v[...].reshape(1024, 128)
    for n in range(8):
        vec[:, pl.ds(128 * n, 128)] = sm_2[pl.ds(128 * n, 128), :].T[0:16, :]
    wt[...] = tk_v[...].reshape(4, TOKH, 128)
    for l in range(2):
        rows = jnp.concatenate(three_parts(sm_2[pl.ds(l, 128, stride=8), :]), axis=0)

        @pl.loop(0, 8)
        def _(n):
            lane = lax.broadcasted_iota(jnp.int32, (128, 512), 0)
            col = lax.broadcasted_iota(jnp.int32, (128, 512), 1)
            pick = jnp.where(lane == 32 + col % 32, 1.0, 0.0).astype(bf16)
            spread = dot_nn(rows, pick)
            value = spread[0:128] + spread[128:256] + spread[256:384]
            mine = lane == n * 16 + col // 32
            bch1[l:l + 1, pl.ds(pl.multiple_of(n * 512, 512), 512)] = jnp.sum(jnp.where(mine, value, 0.0), axis=0, keepdims=True)

    burst('stem0')
    need(0)
    run = during('stem', 4)
    put(x_v, pl.ds(ROWS, XROWS - ROWS), jnp.zeros((XROWS - ROWS, CH), f32))

    @pl.loop(0, 4)
    def _(i):
        run(i)
        cols = pl.ds(pl.multiple_of(i * 256, 256), 256)
        w = ws[:, :, :, :, cols].reshape(3072, 256)
        value = dot_nn(p_v[...].reshape(ROWS, 3072), w) + vec[0:1, cols]
        for n in range(2):
            x_v[2 * i + n, pl.ds(0, ROWS), :] = value[:, 128 * n:128 * (n + 1)]

    wc_all = wc

    def add_rows(value):
        for n in range(CH // 128):
            x_v[n, pl.ds(0, ROWS), :] += value[:, 128 * n:128 * (n + 1)]

    for l in range(2):
        r = 1 + 5 * l
        burst(f'tok{l}_0')
        run = during(f'tok{l}_', IMG)
        save_in = pltpu.make_async_copy(x_v.at[:, pl.ds(0, ROWS)], xin.at[l], sem_x.at[0])
        save_in.start()
        save_in.wait()

        @pl.loop(0, IMG)
        def _(b):
            run(b)
            x = get(x_v, image(b))
            std, _ = standardize(x)
            a = with_bias_rows(std * vec[r:r + 1, :] + vec[r + 1:r + 2, :])
            g_v[...] = gelu(dot_nn(wt[l, :, 0:TPAD], a)).astype(bf16)
            put(x_v, image(b), x + dot_tn(wt[2 + l, :, 0:TPAD], g_v[...]))
        save_mid = pltpu.make_async_copy(x_v.at[:, pl.ds(0, ROWS)], xmid.at[l], sem_x.at[0])
        save_mid.start()
        burst(f'ln{l}')

        for at, size in CHUNKS:
            std, _ = standardize(get(x_v, pl.ds(at, size)))
            v_v[pl.ds(at, size), :] = (std * vec[r + 2:r + 3, :] + vec[r + 3:r + 4, :]).astype(bf16)
        save_v = pltpu.make_async_copy(v_v, vout.at[l], sem_x.at[1])
        save_v.start()
        burst(f'ch{l}_0')
        need(2 + 2 * l)
        save_mid.wait()

        def blocks(i, slot):
            t, h = i // 2, i % 2
            part = pl.ds(pl.multiple_of(h * BLK, BLK), BLK)
            half = [pl.ds(pl.multiple_of(h * 2, 2), 2)]
            return [(wc_all.at[2 * l, t, :, :, :, :, part], w1_v.at[slot]), (wc_all.at[2 * l + 1, t, *half], w2_v.at[slot])]

        def outs(i, slot):
            part = pl.ds(pl.multiple_of(i * BLK, BLK), BLK)
            return [(pre_v.at[slot], pre_out.at[l, :, part]), (act_v.at[slot], act_out.at[l, :, part])]
        run = during(f'ch{l}_', NBLK)

        def channel(i, slot):
            run(i)
            part = pl.ds(pl.multiple_of(i * BLK, BLK), BLK)
            h = dot_nn(v_v[...], w1_v[slot].reshape(CH, BLK)) + bch1[l:l + 1, part]
            pre_v[slot] = h
            act_v[slot] = gelu(h).astype(bf16)
            add_rows(dot_nn(act_v[slot], w2_v[slot].reshape(BLK, CH)))
        for_blocks(Stream(sem_w, blocks, NBLK), channel, Stream(sem_o, outs, NBLK))
        add_rows(jnp.broadcast_to(vec[r + 4:r + 5, :], (ROWS, CH)))
        save_v.wait()

    burst('head')
    need(5)
    keep_p.wait()
    last = 11
    pooled = jnp.sum(get(x_v, pl.ds(0, ROWS)).reshape(TOK, IMG, CH), axis=0) * (1.0 / TOK)
    std, inv = standardize(pooled)
    head_in = (std * vec[last:last + 1, :] + vec[last + 1:last + 2, :]).astype(bf16)
    hl[...] = head_in
    w_h = wh[...].reshape(CH, CH)
    logits = dot_nn(head_in, w_h) + bh_v[0:1, :]
    row = lax.broadcasted_iota(jnp.int32, (IMG, 1), 0)
    label = jnp.zeros((IMG, 1), jnp.int32)
    for b in range(IMG):
        value = labels[me['x'] * IMG + b]
        label = jnp.where(row == b, value, label)
    label = label + 6 * sum(jnp.where(label >= edge, 1, 0) for edge in (250, 500, 750))
    is_label = lax.broadcasted_iota(jnp.int32, logits.shape, 1) == label
    top = jnp.max(logits, axis=-1, keepdims=True)
    ex = jnp.exp(logits - top)
    es = jnp.sum(ex, axis=-1, keepdims=True)
    nll = top + jnp.log(es) - jnp.sum(jnp.where(is_label, logits, 0.0), axis=-1, keepdims=True)
    d_logits = (ex / es - jnp.where(is_label, 1.0, 0.0)) * (1.0 / 1024)
    gbh[...] = jnp.sum(d_logits, axis=0, keepdims=True)
    d_bf = d_logits.astype(bf16)
    hr[...] = d_bf
    d_in = dot_nt(d_bf, w_h)
    hstat[0:1, :] = jnp.sum(d_in * std, axis=0, keepdims=True)
    hstat[1:2, :] = jnp.sum(d_in, axis=0, keepdims=True)
    hstat[2:3, :] = jnp.broadcast_to(jnp.sum(nll, axis=0, keepdims=True), (1, CH))
    dx0[...] = norm_grad(d_in, vec[last:last + 1, :], std, inv) * (1.0 / TOK)
    burst('end')
    net.finish()
    assert len(net.builds) <= FRONT_COPIES, len(net.builds)


def front(*operands):
    a, v = pl.BlockSpec(memory_space=pl.ANY), pl.BlockSpec(memory_space=pltpu.VMEM)
    S, V, DMA = jax.ShapeDtypeStruct, pltpu.VMEM, pltpu.SemaphoreType.DMA
    return pl.pallas_call(
        front_kernel, name='front',
        in_specs=[pl.BlockSpec(memory_space=pltpu.SMEM), a] + [v] * 17,
        out_specs=[a] * 7 + [v] * 7,
        out_shape=[S((N_CH, 4, 4, 4, 2, 32, 1024), bf16), S((TOK, IMG, 3072), bf16), S((2, CH // 128, ROWS, 128), f32),
                   S((2, CH // 128, ROWS, 128), f32),
                   S((2, ROWS, CH), bf16), S((2, ROWS, CHH), f32), S((2, ROWS, CHH), bf16), S((IMG, CH), bf16),
                   S((IMG, CH), bf16), S((IMG, CH), f32), S((8, CH), f32), S((1, CH), f32), S((16, CH), f32),
                   S((4, TOKH, 128), bf16)],
        scratch_shapes=[V((N_CH, 32, 1024), bf16), V((96, 256), bf16), V((32, 256), bf16), V((4, 16, 128), f32),
                        V((4, 16, 128), bf16), V((8, 128), f32), V((8, 256), f32), V((4, 4, 2, 96, CH), bf16),
                        V((4, 4, 2, 32, CH), bf16), V((4, 4, 4, 2, 16, 128), bf16), V((4, 4, 4, 2, 8, 128), f32),
                        V((1024, 128), f32), V((8, CH), f32), V((2, CHH), f32),
                        V((128, 128), f32), V((TOK, IMG, 3072), bf16), V((CH // 128, XROWS, 128), f32),
                        V((ROWS, CH), bf16), V((2, 4, 4, 2, 32, BLK), bf16), V((2, 2, 4, 2, 32, CH), bf16),
                        V((2, ROWS, BLK), f32), V((2, ROWS, BLK), bf16), V((TOKH, CH), bf16),
                        DMA((FRONT_COPIES,)), DMA((FRONT_COPIES,)), DMA((2,)), DMA((2, 2)), DMA((2, 2)), DMA((2,))],
        compiler_params=pltpu.CompilerParams(collective_id=0, has_side_effects=True, vmem_limit_bytes=62 * 1024 * 1024),
        cost_estimate=pl.CostEstimate(flops=90_000_000_000, bytes_accessed=180_000_000, transcendentals=0),
    )(*operands)

CHANNEL_AXES = ('tp', 'fsdp')


def weight_specs():
    vec_spec = P(CHANNEL_AXES)
    layer_vec = P(None, CHANNEL_AXES)
    return (P('fsdp', 'tp'), vec_spec, layer_vec, layer_vec, P(None, None, 'fsdp'), P(None, 'fsdp'),
            P(None, 'fsdp', None), layer_vec, layer_vec, P(None, 'fsdp', 'tp'), layer_vec,
            P(None, CHANNEL_AXES, None), layer_vec, vec_spec, vec_spec, P('fsdp', 'tp'), P('tp'))


def solution(mesh):
    def step(patches, labels, w_stem, b_stem, ln1_g, ln1_b, w_tok1, b_tok1, w_tok2,
             ln2_g, ln2_b, w_ch1, b_ch1, w_ch2, b_ch2, lnf_g, lnf_b, w_head, b_head):
        wc, pat, xin, xmid, vin, pre, act, hl, hr, dx0, hstat, gbh, vec, wt = front(
            labels, patches.transpose(1, 0, 2), w_stem, w_ch1, w_ch2, w_head, w_tok1.transpose(0, 2, 1), w_tok2, b_tok1, b_ch1,
            b_head, b_stem, ln1_g, ln1_b, ln2_g, ln2_b, b_ch2, lnf_g, lnf_b)
        pat = pat.reshape(ROWS, -1)
        dpre, dout, dstem, sm, tk = backward(xin, xmid, pre, wc, wt, vec, dx0, hstat, gbh)

        loss, g_s, g_bs, g_1g, g_1b, g_t1, g_bt, g_t2, g_2g, g_2b, g_c1, g_b1, g_c2, g_b2, g_fg, g_fb, g_h, g_bh = finish(*reduce_gradients(
            dpre, act, pat, vin, dout, dstem, hl, hr, sm.reshape(4, 4, 4, 2, 8, 128), tk.reshape(4, 4, 4, 2, 16, 128)))
        return (loss.reshape(()), g_s, g_bs, g_1g, g_1b, g_t1.transpose(0, 2, 1), g_bt, g_t2, g_2g, g_2b, g_c1, g_b1, g_c2, g_b2,
                g_fg, g_fb, g_h, g_bh)

    specs = weight_specs()
    return jax.shard_map(step, mesh=mesh, in_specs=(P('fsdp', None, None), P('fsdp')) + specs,
                         out_specs=(P(),) + specs, check_vma=False)
```

```python
import functools

import jax
import jax.numpy as jnp
from jax import lax
from jax.experimental import pallas as pl
from jax.experimental.pallas import tpu as pltpu
from jax.sharding import PartitionSpec as P

MESH = pl.DeviceIdType.MESH
ORDERS = (('x', 'y', 'z'), ('y', 'z', 'x'), ('z', 'x', 'y'))
COLS = ((0, 384), (384, 384), (768, 256))
N_CH = 4
STEM, HEAD = 4, 5
bf16, f32 = jnp.bfloat16, jnp.float32


def my_place():
    f = lax.axis_index('fsdp')
    return {'x': lax.axis_index('tp'), 'z': f // 8, 'y': (f // 2) % 4, 'k': f % 2}


def moved(place, dim, step):
    new = dict(place)
    new[dim] = 1 - place['k'] if dim == 'k' else (place[dim] + step) % 4
    return new


def device(place):
    return {'tp': place['x'], 'fsdp': (place['z'] * 4 + place['y']) * 2 + place['k']}


EPS = 1e-6
TOK, TPAD = 49, 56
IMG = 8
ROWS, XROWS = IMG * TOK, IMG * TPAD
CHUNKS = ((0, 112), (112, 112), (224, 112), (336, 56))
CH, TOKH, CHH = 1024, 512, 4096
BLK = 512
NBLK = CHH // BLK
GELU_C, GELU_A = 0.7978845608028654, 0.044715


def dot_nn(a, b):
    return lax.dot_general(a, b, (((1,), (0,)), ((), ())), preferred_element_type=f32)


def dot_nt(a, b):
    return lax.dot_general(a, b, (((1,), (1,)), ((), ())), preferred_element_type=f32)


def dot_tn(a, b):
    return lax.dot_general(a, b, (((0,), (0,)), ((), ())), preferred_element_type=f32)


def gelu(x):
    half = 0.5 * x
    return half + half * jnp.tanh(x * (GELU_C + (GELU_C * GELU_A) * (x * x)))


def gelu_both(x):
    sq = x * x
    th = jnp.tanh(x * (GELU_C + (GELU_C * GELU_A) * sq))
    half = 0.5 * x
    rise = 0.5 + 0.5 * th
    slope = (1.0 - th * th) * (GELU_C + (3.0 * GELU_C * GELU_A) * sq)
    return x * rise, rise + half * slope


def standardize(x):
    mean = jnp.mean(x, axis=-1, keepdims=True)
    cent = x - mean
    inv = lax.rsqrt(jnp.mean(cent * cent, axis=-1, keepdims=True) + EPS)
    return cent * inv, inv


def norm_grad(d, gain, std, inv):
    gs = d * gain
    m0 = jnp.mean(gs, axis=-1, keepdims=True)
    m1 = jnp.mean(gs * std, axis=-1, keepdims=True)
    return inv * (gs - m0 - std * m1)


def row_mask(rows=TPAD):
    return lax.broadcasted_iota(jnp.int32, (rows, 1), 0) < TOK


def image(b):
    return pl.ds(b, TPAD, stride=IMG)


def get(ref, rows):
    return jnp.concatenate([ref[n, rows, :] for n in range(CH // 128)], axis=1)


def put(ref, rows, value):
    for n in range(CH // 128):
        ref[n, rows, :] = value[:, 128 * n:128 * (n + 1)]


class Stream:
    def __init__(self, sem, copies, count):
        self.sem, self.copies, self.count = sem, copies, count

    def make(self, i, slot):
        return [pltpu.make_async_copy(src, dst, self.sem.at[slot, n]) for n, (src, dst) in enumerate(self.copies(i, slot))]

    def start(self, i, slot):
        for copy in self.make(i, slot):
            copy.start()

    def wait(self, i, slot):
        for copy in self.make(i, slot):
            copy.wait()


def for_blocks(stream, body, out=None):
    n = stream.count
    stream.start(0, 0)

    @pl.loop(0, n)
    def _(i):
        slot = i % 2
        stream.wait(i, slot)

        @pl.when(i + 1 < n)
        def _():
            stream.start(i + 1, 1 - slot)
        if out is not None:
            @pl.when(i >= 2)
            def _():
                out.wait(i - 2, slot)
        body(i, slot)
        if out is not None:
            out.start(i, slot)
    if out is not None:
        out.wait(n - 2, n % 2)
        out.wait(n - 1, 1 - n % 2)


FRONT_COPIES = 240
EARLY = [('stem', 0), ('stem', 1), ('stem', 2), ('ch', 0), ('ch', 1), ('ch', 2), ('head', 2)]
LATE = [('stem', c, None) for c in range(3)] + [('ch', c, g) for g in range(N_CH) for c in range(3)] + [('head', 2, None)]
UNIT_GROUP = {('stem', None): 0, ('ch', 0): 1, ('ch', 1): 2, ('ch', 2): 3, ('ch', 3): 4, ('head', None): 5}
EVERY = pl.ds(0, 4)
FRONT_ORDER = (
    ('prep', (('M0', ('sm',)), ('M0', ('tk',)), ('A0', ('stem', 0)), ('A0', ('stem', 1)), ('A0', ('stem', 2)),
        ('A0', ('ch', 0)), ('A0', ('ch', 1)), ('A0', ('ch', 2)), ('A0', ('head', 2)),)),
    ('unpack', (('M1', ('sm',)), ('M1', ('tk',)), ('A', ('stem', 0)), ('A', ('stem', 1)), ('A', ('stem', 2)),
        ('A', ('head', 2)), ('A', ('ch', 2)), ('A', ('ch', 0)), ('A', ('ch', 1)), ('B', ('stem', 0)), ('M2', ('sm',)),
        ('B', ('stem', 1)), ('M2', ('tk',)), ('B', ('stem', 2)), ('B', ('ch', 0)), ('B', ('head', 2)), ('B', ('ch', 1)),
        ('C', ('stem', 0)), ('B', ('ch', 2)), ('M3', ('sm',)), ('C', ('stem', 2)), ('C', ('stem', 1)), ('C', ('head', 2)),)),
    ('stem0', (('D', ('stem', 2, None)), ('D', ('stem', 0, None)), ('C', ('ch', 2)), ('C', ('ch', 0)),
        ('D', ('stem', 1, None)), ('C', ('ch', 1)), ('D', ('ch', 2, 0)), ('D', ('ch', 2, 1)), ('E', ('stem', 2, None)),
        ('E', ('stem', 0, None)), ('E', ('stem', 1, None)), ('D', ('ch', 0, 0)), ('D', ('ch', 0, 1)), ('D', ('ch', 1, 0)),
        ('D', ('ch', 1, 1)), ('F', ('stem', 0, None)), ('F', ('stem', 1, None)), ('E', ('ch', 2, 0)), ('E', ('ch', 2, 1)),
        ('E', ('ch', 0, 0)), ('E', ('ch', 1, 0)), ('F', ('stem', 2, None)), ('F', ('ch', 2, 0)),)),
    ('stem1', (('F', ('ch', 2, 1)), ('E', ('ch', 0, 1)), ('E', ('ch', 1, 1)), ('D', ('ch', 0, 2)), ('D', ('ch', 1, 2)),
        ('D', ('ch', 2, 2)), ('D', ('ch', 0, 3)), ('D', ('ch', 1, 3)), ('D', ('ch', 2, 3)),)),
    ('stem3', (('F', ('ch', 0, 0)),)),
    ('tok0_0', (('F', ('ch', 1, 0)),)),
    ('tok0_3', (('F', ('ch', 0, 1)),)),
    ('tok0_4', (('F', ('ch', 1, 1)),)),
    ('tok0_5', (('E', ('ch', 2, 2)),)),
    ('ch0_0', (('E', ('ch', 2, 3)), ('E', ('ch', 0, 2)), ('E', ('ch', 1, 2)), ('F', ('ch', 2, 2)),)),
    ('ch0_3', (('F', ('ch', 2, 3)),)),
    ('ch0_5', (('E', ('ch', 0, 3)), ('E', ('ch', 1, 3)), ('D', ('head', 2, None)),)),
    ('ch0_7', (('F', ('ch', 0, 2)), ('F', ('ch', 1, 2)),)),
    ('tok1_2', (('F', ('ch', 0, 3)),)),
    ('tok1_3', (('F', ('ch', 1, 3)), ('E', ('head', 2, None)),)),
    ('ln1', (('F', ('head', 2, None)),)),
)


class Net:
    def __init__(self, send_sems, recv_sems):
        self.send_sems, self.recv_sems, self.names, self.builds, self.done = send_sems, recv_sems, {}, [], set()

    def copy(self, name):
        n = self.names[name]
        src, dst, target = self.builds[n]()
        return pltpu.make_async_remote_copy(src_ref=src, dst_ref=dst, send_sem=self.send_sems.at[n],
                                            recv_sem=self.recv_sems.at[n], device_id=target, device_id_type=MESH)

    def start(self, name, build):
        self.names[name] = len(self.builds)
        self.builds.append(build)
        self.copy(name).start()

    def arrived(self, *names):
        for name in names:
            self.copy(name).wait_recv()

    def finish(self):
        for name in self.names:
            if name not in self.done:
                self.copy(name).wait_send()


def core_first(size, cols, each):
    half = cols // 2
    row = lax.broadcasted_iota(jnp.int32, (size, size), 0)
    col = lax.broadcasted_iota(jnp.int32, (size, size), 1)
    source = col % half // each * (2 * each) + col // half * each + col % each
    return jnp.where(row == source, 1.0, 0.0).astype(bf16)


def three_parts(x):
    hi = x.astype(bf16)
    rest = x - hi.astype(f32)
    mid = rest.astype(bf16)
    return hi, mid, (rest - mid.astype(f32)).astype(bf16)


def with_bias_rows(a):
    row = lax.broadcasted_iota(jnp.int32, (TPAD, 1), 0)
    return jnp.where(row < TOK, a, jnp.where(row < TOK + 3, 1.0, 0.0)).astype(bf16)


def front_kernel(labels, patches, w_stem, w_ch1, w_ch2, w_head, w_tok1, w_tok2, b_tok1, b_ch1, b_head, b_stem, ln1_g, ln1_b,
                 ln2_g, ln2_b, b_ch2, lnf_g, lnf_b,
                 wc, pat_out, xin, xmid, vout, pre_out, act_out, hl, hr, dx0, hstat, gbh, vec, wt,
                 pc, ps, ph, tk_f, tk_p, sm_p, bh_p, ws, wh, tk_v, sm_v, sm_2, bh_v, bch1,
                 turn, p_v, pk_v, x_v, v_v, w1_v, w2_v, pre_v, act_v, g_v,
                 send_sems, recv_sems, sem, sem_w, sem_o, sem_x):
    me = my_place()
    other = moved(me, 'k', 1)
    load_p = pltpu.make_async_copy(patches.at[:, pl.ds(pl.multiple_of(me['x'] * IMG, IMG), IMG)], p_v, sem.at[0])
    load_p.start()

    barrier = pltpu.get_barrier_semaphore()
    for dim in 'xyz':
        for step in (1, 2, 3):
            pl.semaphore_signal(barrier, inc=1, device_id=device(moved(me, dim, step)), device_id_type=MESH)
    pl.semaphore_signal(barrier, inc=1, device_id=device(other), device_id_type=MESH)

    stem = dot_nn(w_stem[...].astype(bf16), core_first(256, 256, 32)).astype(bf16)
    ps[0], ps[1] = stem[:, 0:128], stem[:, 128:256]
    pick = core_first(1024, 1024, 32)
    for l in range(2):
        pc[2 * l] = dot_nn(w_ch1[l].astype(bf16), pick).astype(bf16)
        pc[2 * l + 1] = dot_nn(w_ch2[l].astype(bf16), pick).astype(bf16)
    ph[...] = jnp.zeros_like(ph)
    ph[:, pl.ds(0, 250)] = w_head[...].astype(bf16)
    turn[...] = jnp.zeros_like(turn)
    for n, ref in ((0, b_stem), (11, lnf_g), (12, lnf_b)):
        turn[n, pl.ds(0, 8)] = ref[...]
    for n, ref in enumerate((ln1_g, ln1_b, ln2_g, ln2_b, b_ch2)):
        for l in range(2):
            turn[pl.ds(1 + 5 * l + n, 1), pl.ds(0, 8)] = ref[pl.ds(l, 1), :]
    turn[pl.ds(16, 2), pl.ds(0, 16)] = b_tok1[...]
    turned = turn[...].T
    tk_f[...] = jnp.zeros_like(tk_f)
    for l in range(2):
        tk_f[l, :, pl.ds(0, TOK)] = w_tok1[l]
        tk_f[2 + l, :, pl.ds(0, TOK)] = w_tok2[l]
        for n, part in enumerate(three_parts(turned[0:16, 16 + l:17 + l])):
            tk_f[l, :, pl.ds(TOK + n, 1)] = part.astype(f32)
    tk_p[...] = tk_f[...].astype(bf16)
    sm_p[...] = jnp.zeros_like(sm_p)
    sm_p[:, pl.ds(0, 16)] = turned[0:8, 0:16]
    sm_p[pl.ds(0, 2), pl.ds(32, 32)] = b_ch1[...]
    bh_p[...] = jnp.full_like(bh_p, -1e30)
    bh_p[0, pl.ds(0, 250)] = b_head[...]

    net = Net(send_sems, recv_sems)
    core = me['k']
    ring = {d: [moved(me, d, n)[d] for n in range(4)] for d in 'xyz'}
    columns = [pl.ds(pl.multiple_of(x * 256, 256), 256) for x in ring['x']]
    stem_columns = [pl.ds(pl.multiple_of(x * 128, 128), 128) for x in ring['x']]
    peers = {(d, n): device(moved(me, d, n)) for d in 'xyz' for n in (1, 2, 3)}
    partner = device(other)
    here = {'x': 0, 'y': 0, 'z': 0}

    def view(unit, block, half=None):
        kind, colour = unit[:2]
        x, z, y = (EVERY if block[d] is None else ring[d][block[d]] for d in 'xzy')
        r0, rn = (0, 32) if half is None else (16 * half, 16)
        if kind == 'ch':
            c0, cn = COLS[colour]
            g = EVERY if len(unit) == 2 else unit[2]
            return wc.at[g, x, core, z, y, pl.ds(r0, rn), pl.ds(c0, cn)]
        if kind == 'stem':
            cols = pl.ds(0, 512) if x is EVERY else stem_columns[block['x']]
            return ws.at[:, z, y, core, pl.ds(32 * colour + r0, rn), cols]
        cols = pl.ds(0, CH) if x is EVERY else columns[block['x']]
        return wh.at[core, z, y, pl.ds(r0, rn), cols]

    def piece(unit):
        kind, colour = unit
        if kind == 'ch':
            return pc.at[:, :, pl.ds(*COLS[colour])]
        return ps.at[:, pl.ds(32 * colour, 32), :] if kind == 'stem' else ph.at[:, :]

    def exchange(unit, tag, dim, block):
        for side, step in (('l', 1), ('r', 3)):
            def build(step=step):
                part = view(unit, block)
                return (piece(unit) if tag == '1' else part), part, peers[dim, step]
            net.start((unit, tag, side), build)

    def forward_half(unit, tag, dim, block):
        for half, (origin, target, side) in enumerate(((3, 1, 'l'), (1, 3, 'r'))):
            def build(half=half, origin=origin, target=target):
                part = view(unit, {**block, dim: origin}, half)
                return part, part, peers[dim, target]
            net.start((unit, tag, side), build)

    def swap(unit, tag, block):
        def build():
            part = view(unit, block)
            return part, part, partner
        net.start((unit, tag), build)

    own = pltpu.make_async_copy(pc, wc.at[:, me['x'], me['k'], me['z'], me['y']], sem.at[1])
    own.start()
    mine = pl.ds(pl.multiple_of(me['x'] * 256, 256), 256)
    for n in range(2):
        ws[n, me['z'], me['y'], me['k'], :, stem_columns[0]] = ps[n]
    wh[me['k'], me['z'], me['y'], :, mine] = ph[...]
    sm_v[me['x'], me['z'], me['y'], me['k']] = sm_p[...]
    tk_v[:, me['z'], me['y'], me['k']] = tk_p[...]
    bh_v[:, mine] = bh_p[...]
    own.wait()
    pl.semaphore_wait(barrier, 10)

    def small(kind, n):
        dims = 'xyz' if kind == 'sm' else 'yz'
        at = {d: EVERY if d in dims[:n] else ring[d][0] for d in 'xyz'}

        def part():
            if kind == 'sm':
                return sm_v.at[at['x'], at['z'], at['y'], core]
            return tk_v.at[:, at['z'], at['y'], core]
        if n > 0:
            net.arrived(*[(kind, n - 1, s) for s in (1, 2, 3)])
        if n < len(dims):
            for s in (1, 2, 3):
                net.start((kind, n, s), lambda s=s: (part(), part(), peers[dims[n], s]))
            if kind == 'sm' and n == 0:
                def head_bias():
                    return bh_v.at[:, columns[0]]
                for s in (1, 2, 3):
                    net.start(('bh', s), lambda s=s: (head_bias(), head_bias(), peers['x', s]))
        else:
            net.start((kind, 'k'), lambda: (part(), part(), partner))

    def step(name, unit):
        if name[0] == 'M':
            small(unit[0], int(name[1]))
            return
        d1, d2, d3 = ORDERS[unit[1]]
        early = unit[:2]
        plane = {**here, d1: None, d2: None}
        if name == 'A0':
            exchange(unit, '1', d1, here)
        elif name == 'A':
            net.arrived((unit, '1', 'l'), (unit, '1', 'r'))
            forward_half(unit, '1h', d1, here)
        elif name == 'B':
            net.arrived((unit, '1h', 'l'), (unit, '1h', 'r'))
            exchange(unit, '2', d2, {**here, d1: None})
        elif name == 'C':
            net.arrived((unit, '2', 'l'), (unit, '2', 'r'))
            forward_half(unit, '2h', d2, {**here, d1: None})
        elif name == 'D':
            if early not in planes:
                planes.add(early)
                net.arrived((early, '2h', 'l'), (early, '2h', 'r'))
            exchange(unit, '3', d3, plane)
            swap(unit, 'k0', plane)
        elif name == 'E':
            net.arrived((unit, '3', 'l'), (unit, '3', 'r'))
            forward_half(unit, '3h', d3, plane)
            for n in (1, 3):
                swap(unit, f'k{n}', {**plane, d3: n})
        else:
            net.arrived((unit, '3h', 'l'), (unit, '3h', 'r'))
            swap(unit, 'k2', {**plane, d3: 2})

    planes = set()
    awaited = set()

    def need(group):
        for u in LATE:
            if UNIT_GROUP[u[0], u[2]] <= group and u not in awaited:
                awaited.add(u)
                net.arrived(*[(u, f'k{n}') for n in range(4)])

    bursts = {name: steps for name, steps in FRONT_ORDER}

    def burst(name):
        for s in bursts.get(name, ()):
            step(*s)

    def during(name, count):
        def run(i):
            for n in range(1, count):
                if bursts.get(f'{name}{n}'):
                    pl.when(i == n)(functools.partial(burst, f'{name}{n}'))
        return run

    burst('prep')
    load_p.wait()
    pick = core_first(768, 768, 96)
    for g in range(4):
        part = dot_nn(p_v[:, :, pl.ds(768 * g, 768)].reshape(ROWS, 768), pick).astype(bf16)
        for n in range(2):
            pk_v[n, :, pl.ds(384 * g, 384)] = part[:, 384 * n:384 * n + 384]
    keep_p = pltpu.make_async_copy(pk_v, pat_out, sem.at[0])
    keep_p.start()

    burst('unpack')
    net.arrived(('sm', 'k'), ('tk', 'k'), ('bh', 1), ('bh', 2), ('bh', 3))
    sm_2[...] = sm_v[...].reshape(1024, 128)
    for n in range(8):
        tile = jnp.concatenate([sm_2[pl.ds((n % 4 * 4 + i) * 64 + n // 4 * 32, 32), :] for i in range(4)], axis=0)
        vec[:, pl.ds(128 * n, 128)] = tile.T[0:16, :]
    wt[...] = tk_v[...].reshape(4, TOKH, 128)
    for l in range(2):
        rows = jnp.concatenate(three_parts(sm_2[pl.ds(l, 128, stride=8), :]), axis=0)

        @pl.loop(0, 8)
        def _(n):
            lane = lax.broadcasted_iota(jnp.int32, (128, 512), 0)
            col = lax.broadcasted_iota(jnp.int32, (128, 512), 1)
            pick = jnp.where(lane == 32 + col % 32, 1.0, 0.0).astype(bf16)
            spread = dot_nn(rows, pick)
            value = spread[0:128] + spread[128:256] + spread[256:384]
            mine = lane == n // 2 * 32 + col // 32 * 2 + n % 2
            bch1[l:l + 1, pl.ds(pl.multiple_of(n * 512, 512), 512)] = jnp.sum(jnp.where(mine, value, 0.0), axis=0, keepdims=True)

    burst('stem0')
    need(0)
    run = during('stem', 4)
    put(x_v, pl.ds(ROWS, XROWS - ROWS), jnp.zeros((XROWS - ROWS, CH), f32))

    @pl.loop(0, 4)
    def _(i):
        run(i)
        cols = pl.ds(pl.multiple_of(i * 256, 256), 256)
        w = ws[i // 2, :, :, :, :, pl.ds(pl.multiple_of(i % 2 * 256, 256), 256)].reshape(3072, 256)
        value = dot_nn(p_v[...].reshape(ROWS, 3072), w) + vec[0:1, cols]
        for n in range(2):
            x_v[2 * i + n, pl.ds(0, ROWS), :] = value[:, 128 * n:128 * (n + 1)]

    wc_all = wc

    def add_rows(value):
        for n in range(CH // 128):
            x_v[n, pl.ds(0, ROWS), :] += value[:, 128 * n:128 * (n + 1)]

    for l in range(2):
        r = 1 + 5 * l
        burst(f'tok{l}_0')
        run = during(f'tok{l}_', IMG)
        save_in = pltpu.make_async_copy(x_v.at[:, pl.ds(0, ROWS)], xin.at[l], sem_x.at[0])
        save_in.start()
        save_in.wait()

        @pl.loop(0, IMG)
        def _(b):
            run(b)
            x = get(x_v, image(b))
            std, _ = standardize(x)
            a = with_bias_rows(std * vec[r:r + 1, :] + vec[r + 1:r + 2, :])
            g_v[...] = gelu(dot_nn(wt[l, :, 0:TPAD], a)).astype(bf16)
            put(x_v, image(b), x + dot_tn(wt[2 + l, :, 0:TPAD], g_v[...]))
        save_mid = pltpu.make_async_copy(x_v.at[:, pl.ds(0, ROWS)], xmid.at[l], sem_x.at[0])
        save_mid.start()
        burst(f'ln{l}')

        for at, size in CHUNKS:
            std, _ = standardize(get(x_v, pl.ds(at, size)))
            v_v[pl.ds(at, size), :] = (std * vec[r + 2:r + 3, :] + vec[r + 3:r + 4, :]).astype(bf16)
        save_v = [pltpu.make_async_copy(v_v.at[:, pl.ds(512 * n, 512)], vout.at[l, n], sem_x.at[1 + n]) for n in range(2)]
        for copy in save_v:
            copy.start()
        burst(f'ch{l}_0')
        need(2 + 2 * l)
        save_mid.wait()

        def blocks(i, slot):
            t, h = i // 2, i % 2
            part = pl.ds(pl.multiple_of(h * BLK, BLK), BLK)
            return [(wc_all.at[2 * l, t, :, :, :, :, part], w1_v.at[slot]), (wc_all.at[2 * l + 1, t, h], w2_v.at[slot])]

        def outs(i, slot):
            part = pl.ds(pl.multiple_of(i * BLK, BLK), BLK)
            half = pl.ds(pl.multiple_of(i // 2 * BLK, BLK), BLK)
            return [(pre_v.at[slot], pre_out.at[l, :, part]), (act_v.at[slot], act_out.at[l, i % 2, :, half])]
        run = during(f'ch{l}_', NBLK)

        def channel(i, slot):
            run(i)
            part = pl.ds(pl.multiple_of(i * BLK, BLK), BLK)
            h = dot_nn(v_v[...], w1_v[slot].reshape(CH, BLK)) + bch1[l:l + 1, part]
            pre_v[slot] = h
            act_v[slot] = gelu(h).astype(bf16)
            add_rows(dot_nn(act_v[slot], w2_v[slot].reshape(BLK, CH)))
        for_blocks(Stream(sem_w, blocks, NBLK), channel, Stream(sem_o, outs, NBLK))
        add_rows(jnp.broadcast_to(vec[r + 4:r + 5, :], (ROWS, CH)))
        for copy in save_v:
            copy.wait()

    burst('head')
    need(5)
    keep_p.wait()
    last = 11
    pooled = jnp.sum(get(x_v, pl.ds(0, ROWS)).reshape(TOK, IMG, CH), axis=0) * (1.0 / TOK)
    std, inv = standardize(pooled)
    head_in = (std * vec[last:last + 1, :] + vec[last + 1:last + 2, :]).astype(bf16)
    hl[...] = head_in
    w_h = wh[...].reshape(CH, CH)
    logits = dot_nn(head_in, w_h) + bh_v[0:1, :]
    row = lax.broadcasted_iota(jnp.int32, (IMG, 1), 0)
    label = jnp.zeros((IMG, 1), jnp.int32)
    for b in range(IMG):
        value = labels[me['x'] * IMG + b]
        label = jnp.where(row == b, value, label)
    label = label + 6 * sum(jnp.where(label >= edge, 1, 0) for edge in (250, 500, 750))
    is_label = lax.broadcasted_iota(jnp.int32, logits.shape, 1) == label
    top = jnp.max(logits, axis=-1, keepdims=True)
    ex = jnp.exp(logits - top)
    es = jnp.sum(ex, axis=-1, keepdims=True)
    nll = top + jnp.log(es) - jnp.sum(jnp.where(is_label, logits, 0.0), axis=-1, keepdims=True)
    d_logits = (ex / es - jnp.where(is_label, 1.0, 0.0)) * (1.0 / 1024)
    gbh[...] = jnp.sum(d_logits, axis=0, keepdims=True)
    d_bf = d_logits.astype(bf16)
    hr[...] = d_bf
    d_in = dot_nt(d_bf, w_h)
    hstat[0:1, :] = jnp.sum(d_in * std, axis=0, keepdims=True)
    hstat[1:2, :] = jnp.sum(d_in, axis=0, keepdims=True)
    hstat[2:3, :] = jnp.broadcast_to(jnp.sum(nll, axis=0, keepdims=True), (1, CH))
    dx0[...] = norm_grad(d_in, vec[last:last + 1, :], std, inv) * (1.0 / TOK)
    burst('end')
    net.finish()
    assert len(net.builds) <= FRONT_COPIES, len(net.builds)


def front(*operands):
    a, v = pl.BlockSpec(memory_space=pl.ANY), pl.BlockSpec(memory_space=pltpu.VMEM)
    S, V, DMA = jax.ShapeDtypeStruct, pltpu.VMEM, pltpu.SemaphoreType.DMA
    return pl.pallas_call(
        front_kernel, name='front',
        in_specs=[pl.BlockSpec(memory_space=pltpu.SMEM), a] + [v] * 17,
        out_specs=[a] * 7 + [v] * 7,
        out_shape=[S((N_CH, 4, 2, 4, 4, 32, 1024), bf16), S((2, ROWS, 1536), bf16), S((2, CH // 128, ROWS, 128), f32),
                   S((2, CH // 128, ROWS, 128), f32),
                   S((2, 2, ROWS, 512), bf16), S((2, ROWS, CHH), f32), S((2, 2, ROWS, 2048), bf16), S((IMG, CH), bf16),
                   S((IMG, CH), bf16), S((IMG, CH), f32), S((8, CH), f32), S((1, CH), f32), S((16, CH), f32),
                   S((4, TOKH, 128), bf16)],
        scratch_shapes=[V((N_CH, 32, 1024), bf16), V((2, 96, 128), bf16), V((32, 256), bf16), V((4, 16, 128), f32),
                        V((4, 16, 128), bf16), V((8, 128), f32), V((8, 256), f32), V((2, 4, 4, 2, 96, 512), bf16),
                        V((2, 4, 4, 32, CH), bf16), V((4, 4, 4, 2, 16, 128), bf16), V((4, 4, 4, 2, 8, 128), f32),
                        V((1024, 128), f32), V((8, CH), f32), V((2, CHH), f32),
                        V((128, 128), f32), V((TOK, IMG, 3072), bf16), V((2, ROWS, 1536), bf16), V((CH // 128, XROWS, 128), f32),
                        V((ROWS, CH), bf16), V((2, 2, 4, 4, 32, BLK), bf16), V((2, 4, 4, 32, CH), bf16),
                        V((2, ROWS, BLK), f32), V((2, ROWS, BLK), bf16), V((TOKH, CH), bf16),
                        DMA((FRONT_COPIES,)), DMA((FRONT_COPIES,)), DMA((2,)), DMA((2, 2)), DMA((2, 2)), DMA((3,))],
        compiler_params=pltpu.CompilerParams(collective_id=0, has_side_effects=True, vmem_limit_bytes=62 * 1024 * 1024),
        cost_estimate=pl.CostEstimate(flops=90_000_000_000, bytes_accessed=180_000_000, transcendentals=0),
    )(*operands)


TOK_CUTS = 4
GROUPS = (HEAD, 3, 2, 1, 0, STEM)
UNITS = tuple((g, c) for g in GROUPS for c in (2, 0, 1) if g != HEAD or c == 2)
BACK_COPIES = 18 * len(UNITS) + 40
NEEDS = {3: ('act1', 'dout1'), 2: ('vin1', 'dpre1'), 1: ('act0', 'dout0'), 0: ('vin0', 'dpre0'), STEM: ('pat', 'dres'),
         HEAD: ('hl', 'hr')}
BACK_ORDER = (
    ('c1_7', ((3, 'L'), (0, 0), (0, 1),)),
    ('l1', ((1, 0), (1, 1),)),
    ('t1_0', ((0, 2),)),
    ('t1_3', ((1, 2),)),
    ('t1_4', ((0, 3), (2, 0), (2, 1), (0, 4),)),
    ('t1_7', ((2, 2),)),
    ('c0_0', ((0, 5), (1, 3), (3, 0), (2, 'L'), (3, 1), (0, 6), (2, 3), (1, 4),)),
    ('c0_1', ((4, 0), (4, 1), (1, 5),)),
    ('c0_2', ((3, 2),)),
    ('c0_4', ((4, 2), (0, 7),)),
    ('c0_5', ((2, 4),)),
    ('c0_6', ((1, 6),)),
    ('c0_7', ((4, 3), (5, 0), (5, 1), (1, 7), (2, 5), (3, 3), (4, 4), (6, 0), (1, 'L'), (6, 1), (2, 6), (3, 4),)),
    ('l0', ((5, 2),)),
    ('t0_0', ((2, 7), (3, 5),)),
    ('t0_1', ((6, 2), (4, 5),)),
    ('t0_3', ((3, 6), (5, 3), (7, 0), (7, 1), (3, 7), (4, 6), (6, 3), (5, 4), (8, 0), (8, 1), (4, 7), (5, 5), (7, 2),)),
    ('t0_5', ((5, 6), (6, 4),)),
    ('t0_6', ((8, 2), (5, 7), (7, 3), (9, 0), (0, 'L'), (9, 1), (6, 5),)),
    ('t0_7', ((8, 3), (7, 4), (10, 0), (10, 1), (6, 6),)),
    ('fin', ((9, 2), (6, 7), (7, 5),)),
    ('end', ((11, 0), (10, 2), (11, 1), (8, 4), (12, 0), (4, 'L'), (12, 1), (7, 6), (8, 5), (9, 3), (10, 3), (13, 0),
        (11, 2), (12, 2), (13, 1), (7, 7), (8, 6), (9, 4), (10, 4), (14, 0), (14, 1), (15, 0), (15, 1), (13, 2), (11, 3),
        (10, 5), (8, 7), (9, 5), (15, 2), (14, 2), (12, 3), (13, 3), (9, 6), (11, 4), (12, 4), (10, 6), (13, 4), (9, 7),
        (12, 5), (15, 3), (11, 5), (10, 7), (14, 3), (13, 5), (12, 6), (15, 4), (14, 4), (11, 6), (13, 6), (12, 7), (15, 5),
        (11, 7), (14, 5), (13, 7), (15, 6), (14, 6), (15, 7), (14, 7),)),
)
SMALL = dict(sm=((4, 4, 4, 8, 128), (3, 4, 4, 8, 128), (3, 4, 8, 128), (3, 8, 128)),
             tk=((4, 4, 4, 16, 128), (3, 4, 4, 16, 128), (3, 4, 16, 128), (3, 4, 16, 128)))


def reduce_scratch():
    per = []
    for c in range(3):
        n = COLS[c][1]
        many = sum(1 for u in UNITS if u[1] == c)
        lead = ((4, 4), (4,), ())
        b = {'C': pltpu.VMEM((2, 4, 4, 4, 32, n), bf16), 'S1': pltpu.VMEM((4, 4, 32, n), f32), 'S2': pltpu.VMEM((2, 4, 32, n), f32)}
        for ph in range(3):
            if ph:
                b[f'opp{ph}'] = pltpu.VMEM(lead[ph] + (32, n), bf16)
                b[f'pr{ph}'] = pltpu.VMEM(lead[ph] + (16, n), bf16)
                b[f'pl{ph}'] = pltpu.VMEM(lead[ph] + (16, n), bf16)
            for name in ('rig', 'lef'):
                b[f'{name}{ph}'] = pltpu.VMEM(lead[ph] + (16, n), bf16)
            for name in ('half0', 'half1'):
                b[f'{name}{ph}'] = pltpu.VMEM((many,) + lead[ph] + (16, n), bf16)
            for name in ('froml', 'fromr'):
                b[f'{name}{ph}'] = pltpu.VMEM((many,) + lead[ph] + (32, n), bf16)
        per.append(b)
    return per


def small_scratch():
    b = {f'{kind}{n + 1}': pltpu.VMEM(shape, f32) for kind, shapes in SMALL.items() for n, shape in enumerate(shapes)}
    b.update(sm=pltpu.VMEM((4, 4, 4, 2, 8, 128), f32), tk=pltpu.VMEM((4, 4, 4, 2, 16, 128), f32),
             sm_s1=pltpu.VMEM((4, 4, 8, 128), f32), sm_s2=pltpu.VMEM((4, 8, 128), f32),
             tk_s1=pltpu.VMEM((4, 4, 16, 128), f32), tk_s2=pltpu.VMEM((4, 16, 128), f32))
    return b


def small_pack(b, flat, turn, gvec, hstat, gbch1, gbh):
    for n in range(8):
        cols = pl.ds(128 * n, 128)
        turn[n, pl.ds(0, 128), :] = jnp.zeros((128, 128), f32)
        turn[n, pl.ds(0, 16), :] = gvec[:, cols]
        turn[n, pl.ds(11, 2), :] = hstat[pl.ds(0, 2), cols]
    for n in range(8):
        tile = turn[n, pl.ds(0, 128), :].T
        for i in range(4):
            a = n % 4 * 4 + i
            flat[a // 2, pl.ds(a % 2 * 64 + n // 4 * 32, 32), :] = tile[32 * i:32 * i + 32]
    for l in range(2):
        def gather(n, total):
            lane = lax.broadcasted_iota(jnp.int32, (128, 512), 0)
            col = lax.broadcasted_iota(jnp.int32, (128, 512), 1)
            sums = gbch1[l:l + 1, pl.ds(pl.multiple_of(512 * n, 512), 512)]
            mine = jnp.where(lane == n // 2 * 32 + col // 32 * 2 + n % 2, sums, 0.0)
            pick = jnp.where(lane == 32 + col % 32, 1.0, 0.0).astype(bf16)
            return total + dot_nt(jnp.concatenate(three_parts(mine), axis=0), pick)
        total = lax.fori_loop(0, 8, gather, jnp.zeros((384, 128), f32))
        total = total[0:128] + total[128:256] + total[256:384]
        for n in range(8):
            flat[n, pl.ds(l, 16, stride=8), :] += total[16 * n:16 * n + 16]
    lane = lax.broadcasted_iota(jnp.int32, (1, 128), 1)
    for t in range(4):
        for q in range(4):
            tile = gbh[0:1, t * 256 + q // 2 * 128:t * 256 + q // 2 * 128 + 128]
            if q % 2 == 0:
                tile = jnp.concatenate([tile[:, 64:], tile[:, :64]], axis=1)
            tile = jnp.where(lane >= 64, tile, 0.0)
            for n in (2 * t, 2 * t + 1):
                flat[n, pl.ds(2 + q, 16, stride=8), :] += tile
    for n in range(8):
        flat[n, pl.ds(6, 16, stride=8), :] += jnp.where(lane == 64, hstat[2:3, 0:128], 0.0)
        b['sm'][n // 2, pl.ds(n % 2 * 2, 2)] = flat[n, pl.ds(0, 128), :].reshape(2, 4, 2, 8, 128)


def back_kernel(*refs):
    xin, xmid, pre_in, wc, act, vin, pat = refs[:7]
    hl, hr, dx0, hstat, gbh, wt, vec = refs[7:14]
    out_c, out_s, out_h, sm_own, tk_own = refs[14:19]
    dpre, dout, dres, x_act, x_vin, x_pat, x_dpre, x_dout, x_dres = refs[19:28]
    (per, b, big, little, x_hl, x_hr, gvec, gbch1, x_v, d_v, dv_v, do_v, w1_v, w2_v, pre_v, dp_v,
     send_sems, recv_sems, load_sems, sem, sem_w, sem_o) = refs[28:]
    me = my_place()
    other = moved(me, 'k', 1)
    k, k2 = me['k'], 1 - me['k']
    barrier = pltpu.get_barrier_semaphore()
    for dim in 'xyz':
        for step in (1, 2, 3):
            pl.semaphore_signal(barrier, inc=1, device_id=device(moved(me, dim, step)), device_id_type=MESH)
    pl.semaphore_signal(barrier, inc=1, device_id=device(other), device_id_type=MESH)
    net = Net(send_sems, recv_sems)
    ring = {d: [moved(me, d, n)[d] for n in range(4)] for d in 'xyz'}
    peers = {(d, n): device(moved(me, d, n)) for d in 'xyz' for n in (1, 2, 3)}
    partner = device(other)
    half_at = pl.ds(pl.multiple_of(k * 512, 512), 512)
    half_to = pl.ds(pl.multiple_of(k2 * 512, 512), 512)
    swaps = {'act1': (act.at[1, k2], x_act.at[1]), 'act0': (act.at[0, k2], x_act.at[0]), 'vin1': (vin.at[1, k2], x_vin.at[1]),
             'vin0': (vin.at[0, k2], x_vin.at[0]), 'pat': (pat.at[k2], x_pat), 'dpre1': (dpre.at[1], x_dpre.at[1]),
             'dpre0': (dpre.at[0], x_dpre.at[0]), 'dout1': (dout.at[1], x_dout.at[1]), 'dout0': (dout.at[0], x_dout.at[0]),
             'dres': (dres, x_dres), 'hl': (hl.at[:, half_to], x_hl), 'hr': (hr, x_hr)}

    def swap(*names):
        for name in names:
            net.start(name, lambda name=name: (*swaps[name], partner))
    busy = {}

    def free(key):
        for name in busy.pop(key, ()):
            net.copy(name).wait_send()
            net.done.add(name)

    def loads(g):
        l = g // 2
        if g == STEM:
            wide, tall = (pat.at[k], x_pat, 1536), (dres, x_dres, CH)
        elif g % 2:
            wide, tall = (act.at[l, k], x_act.at[l], 2048), (dout.at[l], x_dout.at[l], CH)
        else:
            wide, tall = (dpre.at[l], x_dpre.at[l], CHH), (vin.at[l, k], x_vin.at[l], 512)
        out = []
        for n, (buf, (own, far, cols)) in enumerate(((big, wide), (little, tall))):
            out += [pltpu.make_async_copy(own, buf.at[0, :, pl.ds(0, cols)], load_sems.at[2 * n]),
                    pltpu.make_async_copy(far, buf.at[1, :, pl.ds(0, cols)], load_sems.at[2 * n + 1])]
        return out

    def product(u):
        g, c, slot = u.g, u.c, u.slot
        first = c == 2
        if first and g != HEAD:
            for copy in loads(g):
                copy.wait()
        if g == STEM and not first:
            return
        for v in (units if g == STEM else (u,)):
            if v.g == g:
                free(('C', v.c, v.slot))
        if g == HEAD:
            net.arrived(*NEEDS[g])
            for t in range(4):
                cols = pl.ds(256 * t, 256)
                prod = dot_tn(hl[:, half_at], hr[:, cols]) + dot_tn(x_hl[...], x_hr[:, cols])
                per[c]['C'][slot, t] = prod.astype(bf16).reshape(4, 4, 32, 256)
        elif g == STEM:
            slots = {v.c: v.slot for v in units if v.g == STEM}

            @pl.loop(0, 4)
            def _(z):
                rows = pl.ds(pl.multiple_of(z * 384, 384), 384)
                for t in range(4):
                    def right(s):
                        return jnp.concatenate([little[s, :, 128 * t:128 * t + 128], little[s, :, 512 + 128 * t:640 + 128 * t]], axis=1)
                    prod = dot_tn(big[0, :, rows], right(0)) + dot_tn(big[1, :, rows], right(1))
                    prod = prod.astype(bf16).reshape(4, 3, 32, 256)
                    for d in range(3):
                        per[d]['C'][slots[d], t, z, :, :, pl.ds(0, 256)] = prod[:, d]
        else:
            c0, n = COLS[c]

            @pl.loop(0, 4)
            def _(t):
                for h in range(2):
                    if g % 2:
                        left = pl.ds(pl.multiple_of(t * 512 + h * 256, 256), 256)
                        prod = dot_tn(big[0, :, left], little[0, :, c0:c0 + n]) + dot_tn(big[1, :, left], little[1, :, c0:c0 + n])
                    else:
                        right = pl.ds(pl.multiple_of(t * 1024 + c0, 128), n)
                        rows = slice(256 * h, 256 * h + 256)
                        prod = dot_tn(little[0, :, rows], big[0, :, right]) + dot_tn(little[1, :, rows], big[1, :, right])
                    per[c]['C'][slot, t, 2 * h:2 * h + 2] = prod.astype(bf16).reshape(2, 4, 32, n)

    class Unit:
        def __init__(self, g, c):
            self.g, self.c = g, c
            self.index = [u for u in UNITS if u[1] == c].index((g, c))
            self.slot = self.index % 2
            self.n = COLS[c][1] if g < N_CH else 256
            self.cols = pl.ds(0, self.n)
            self.buf = per[c]
            self.dims = ORDERS[c]
            self.rest = [d for d in 'xzy' if d != self.dims[0]]

        def cut(self, name, *at, rows=slice(None)):
            ref = self.buf[name]
            inner = [slice(None)] * (len(ref.shape) - len(at) - 2)
            return ref.at[(*at, *inner, rows, self.cols)]

        def block(self, p, rows):
            at = {d: EVERY for d in 'xzy'}
            at[self.dims[0]] = p
            return self.buf['C'].at[self.slot, at['x'], at['z'], at['y'], rows, self.cols]

        def share(self, phase, p, e, rows):
            if phase == 0:
                at = dict(zip(self.rest, e))
                at[self.dims[0]] = p
                return self.buf['C'][self.slot, at['x'], at['z'], at['y'], rows, self.cols].astype(f32)
            if phase == 1:
                at = (p, e[0]) if self.dims[1] == self.rest[0] else (e[0], p)
                return self.buf['S1'][(*at, rows, self.cols)]
            return self.buf['S2'][self.slot, p, rows, self.cols]

        def each(self, phase, body):
            if phase == 2:
                body(())
            elif phase == 1:
                pl.loop(0, 4)(lambda i: body((i,)))
            else:
                @pl.loop(0, 4)
                def _(i):
                    pl.loop(0, 4)(lambda j: body((i, j)))

        def send(self, tag, phase, src, dst, step):
            name = (self.g, self.c, tag, phase)
            net.start(name, lambda: (src(), dst(), peers[self.dims[phase], step]))
            return name

        def arrived(self, phase, *tags):
            net.arrived(*[(self.g, self.c, tag, phase) for tag in tags])

        def opposite(self, phase):
            places = ring[self.dims[phase]]
            low, high = pl.ds(0, 16), pl.ds(16, 16)
            if phase == 0:
                sources = [lambda: self.block(places[2], low), lambda: self.block(places[2], high),
                           lambda: self.block(places[1], high), lambda: self.block(places[3], low)]
            else:
                names = (f'opp{phase}', f'pr{phase}', f'pl{phase}')
                for name in names:
                    free((name, self.c))
                opp, right, left = (self.buf[name] for name in names)

                def body(e):
                    opp[(*e, slice(None), self.cols)] = self.share(phase, places[2], e, pl.ds(0, 32)).astype(bf16)
                    right[(*e, slice(None), self.cols)] = self.share(phase, places[1], e, high).astype(bf16)
                    left[(*e, slice(None), self.cols)] = self.share(phase, places[3], e, low).astype(bf16)
                self.each(phase, body)
                sources = [lambda: self.cut(names[0], rows=low), lambda: self.cut(names[0], rows=high),
                           lambda: self.cut(names[1]), lambda: self.cut(names[2])]
            targets = [lambda: self.cut(f'half0{phase}', self.index), lambda: self.cut(f'half1{phase}', self.index),
                       lambda: self.cut(f'froml{phase}', self.index, rows=high),
                       lambda: self.cut(f'fromr{phase}', self.index, rows=low)]
            sent = [self.send(tag, phase, src, dst, step)
                    for tag, src, dst, step in zip(('h0', 'h1', 'p0', 'p1'), sources, targets, (1, 3, 1, 3))]
            if phase == 0:
                busy['C', self.c, self.slot] = sent
            else:
                busy[names[0], self.c] = sent[:2]
                busy[names[1], self.c] = sent[2:3]
                busy[names[2], self.c] = sent[3:]

        def beside(self, phase):
            places = ring[self.dims[phase]]
            for half, step, name, dst in ((0, 1, 'rig', 'froml'), (1, 3, 'lef', 'fromr')):
                self.arrived(phase, f'h{half}')
                key = f'{name}{phase}'
                free((key, self.c))
                out, got = self.buf[key], self.buf[f'half{half}{phase}']
                rows = pl.ds(16 * half, 16)

                def body(e):
                    value = self.share(phase, places[step], e, rows) + got[(self.index, *e, slice(None), self.cols)].astype(f32)
                    out[(*e, slice(None), self.cols)] = value.astype(bf16)
                self.each(phase, body)
                busy[key, self.c] = [self.send(f'f{half}', phase, lambda key=key: self.cut(key),
                                               lambda dst=dst, rows=rows: self.cut(f'{dst}{phase}', self.index, rows=rows), step)]

        def total(self, phase):
            self.arrived(phase, 'p0', 'p1', 'f0', 'f1')
            p = ring[self.dims[phase]][0]

            def body(e):
                got = [self.buf[f'{name}{phase}'][(self.index, *e, slice(None), self.cols)].astype(f32)
                       for name in ('froml', 'fromr')]
                value = self.share(phase, p, e, pl.ds(0, 32)) + got[0] + got[1]
                if phase == 0:
                    self.buf['S1'][(*e, slice(None), self.cols)] = value
                elif phase == 1:
                    self.buf['S2'][(self.slot, *e, slice(None), self.cols)] = value
                elif self.g == STEM:
                    out_s[pl.ds(32 * self.c, 32), :] = value
                elif self.g == HEAD:
                    out_h[...] = value
                else:
                    out_c[self.g, :, pl.ds(*COLS[self.c])] = value
            self.each(phase, body)

        def run(self, stage):
            if stage == 0:
                product(self)
            elif stage == 7:
                self.total(2)
            elif stage % 2 == 0:
                self.beside(stage // 2 - 1)
            else:
                if stage > 1:
                    self.total(stage // 2 - 1)
                self.opposite(stage // 2)

    units = [Unit(g, c) for g, c in UNITS]
    bursts = dict(BACK_ORDER)

    def step(which, stage):
        if stage == 'L':
            net.arrived(*NEEDS[which])
            for copy in loads(which):
                copy.start()
        else:
            units[which].run(stage)

    def burst(name):
        for s in bursts.get(name, ()):
            step(*s)

    def during(name, count):
        def run(i):
            for n in range(1, count):
                if bursts.get(f'{name}{n}'):
                    pl.when(i == n)(functools.partial(burst, f'{name}{n}'))
        return run

    load = pltpu.make_async_copy(xmid.at[1], x_v.at[:, pl.ds(0, ROWS)], sem.at[0])
    load.start()
    mask = row_mask()
    rest = pl.ds(ROWS, XROWS - ROWS)
    put(d_v, rest, jnp.zeros((XROWS - ROWS, CH), f32))
    put(x_v, rest, jnp.zeros((XROWS - ROWS, CH), f32))
    gvec[...] = jnp.zeros_like(gvec)
    tk = b['tk']
    tk[...] = jnp.zeros_like(tk)

    @pl.loop(0, TOK)
    def _(s):
        put(d_v, pl.ds(pl.multiple_of(s * IMG, IMG), IMG), dx0[...])

    def add(row, value):
        gvec[row:row + 1, :] += jnp.sum(value, axis=0, keepdims=True)

    def add_token(n, value, start=0):
        tk[n, :, :, :, :, pl.ds(start, value.shape[1])] += value.reshape(4, 4, 2, 16, value.shape[1])

    for l in (1, 0):
        r = 1 + 5 * l
        for at, size in CHUNKS:
            d = get(d_v, pl.ds(at, size))
            add(r + 4, d)
            do_v[pl.ds(at, size), :] = d.astype(bf16)
        keep = pltpu.make_async_copy(do_v, dout.at[l], sem.at[1])
        keep.start()
        keep.wait()
        if l == 1:
            pl.semaphore_wait(barrier, 10)
            swap('hl', 'hr', 'dout1', 'act1', 'vin1', 'act0', 'vin0', 'pat')
        else:
            swap('dout0')
        burst(f'c{l}_0')
        run = during(f'c{l}_', NBLK)

        def blocks(i, slot):
            t, h = i // 2, i % 2
            part = pl.ds(pl.multiple_of(h * BLK, BLK), BLK)
            whole = pl.ds(pl.multiple_of(i * BLK, BLK), BLK)
            return [(wc.at[2 * l, t, :, :, :, :, part], w1_v.at[slot]), (wc.at[2 * l + 1, t, h], w2_v.at[slot]),
                    (pre_in.at[l, :, whole], pre_v.at[slot])]

        def outs(i, slot):
            return [(dp_v.at[slot], dpre.at[l, :, pl.ds(pl.multiple_of(i * BLK, BLK), BLK)])]

        def channel(i, slot):
            run(i)
            for n in range(2):
                cols = slice(256 * n, 256 * n + 256)
                _, slope = gelu_both(pre_v[slot, :, cols])
                d = dot_nt(do_v[...], w2_v[slot, 2 * n:2 * n + 2].reshape(256, CH)) * slope
                gbch1[l:l + 1, pl.ds(pl.multiple_of(i * BLK + 256 * n, 256), 256)] = jnp.sum(d, axis=0, keepdims=True)
                dp_v[slot, :, cols] = d.astype(bf16)

            @pl.when(i == 0)
            def _():
                dv_v[...] = jnp.zeros_like(dv_v)
            for n in range(2):
                cols = slice(512 * n, 512 * n + 512)
                dv_v[:, cols] += dot_nt(dp_v[slot], w1_v[slot, n].reshape(512, BLK))
        for_blocks(Stream(sem_w, blocks, NBLK), channel, Stream(sem_o, outs, NBLK))
        swap(f'dpre{l}')
        burst(f'l{l}')
        load.wait()

        @pl.loop(0, ROWS // TPAD)
        def _(n):
            rows = pl.ds(pl.multiple_of(n * TPAD, TPAD), TPAD)
            std, inv = standardize(get(x_v, rows))
            d = dv_v[rows, :]
            add(r + 2, d * std)
            add(r + 3, d)
            put(d_v, rows, get(d_v, rows) + norm_grad(d, vec[r + 2:r + 3, :], std, inv))
        load = pltpu.make_async_copy(xin.at[l], x_v.at[:, pl.ds(0, ROWS)], sem.at[0])
        load.start()
        burst(f't{l}_0')
        load.wait()
        run = during(f't{l}_', IMG)

        @pl.loop(0, IMG)
        def _(m):
            run(m)
            std, inv = standardize(get(x_v, image(m)))
            a = with_bias_rows(std * vec[r:r + 1, :] + vec[r + 1:r + 2, :])
            d_mid = get(d_v, image(m))
            dm = d_mid.astype(bf16)
            parts = []
            for n in range(TOK_CUTS):
                cols = slice(CH // TOK_CUTS * n, CH // TOK_CUTS * (n + 1))
                value, slope = gelu_both(dot_nn(wt[l, :, 0:TPAD], a[:, cols]))
                add_token(2 + l, dot_nt(value.astype(bf16), dm[:, cols]))
                dh = dot_nn(wt[2 + l, :, 0:TPAD], dm[:, cols]) * slope
                add_token(l, jnp.sum(dh, axis=-1, keepdims=True), 64)
                dh = dh.astype(bf16)
                add_token(l, dot_nt(dh, a[:, cols]))
                parts.append(dot_tn(wt[l, :, 0:TPAD], dh))
            d = jnp.where(mask, jnp.concatenate(parts, axis=1), 0.0)
            add(r, d * std)
            add(r + 1, d)
            put(d_v, image(m), d_mid + norm_grad(d, vec[r:r + 1, :], std, inv))
        if l == 1:
            load = pltpu.make_async_copy(xmid.at[0], x_v.at[:, pl.ds(0, ROWS)], sem.at[0])
            load.start()
            burst('d0')

    burst('fin')
    for at, size in CHUNKS:
        d = get(d_v, pl.ds(at, size))
        add(0, d)
        do_v[pl.ds(at, size), :] = d.astype(bf16)
    keep = pltpu.make_async_copy(do_v, dres, sem.at[1])
    keep.start()
    keep.wait()
    swap('dres')
    small_pack(b, x_v, d_v, gvec, hstat, gbch1, gbh)

    last = []

    def put_small(name, src, dst, target):
        last.append(name)
        net.start(name, lambda: (src, dst, target))

    def small(n):
        x, z, y = (ring[d][0] for d in 'xzy')
        net.arrived(*last)
        last.clear()
        if n == 0:
            put_small(('sm', 0), b['sm'].at[:, :, :, k2], b['sm1'], partner)
            put_small(('tk', 0), b['tk'].at[:, :, :, k2], b['tk1'], partner)
        elif n == 1:
            b['sm1'][...] += b['sm'][:, :, :, k]
            b['tk1'][...] += b['tk'][:, :, :, k]
            for s in (1, 2, 3):
                put_small(('sm', 1, s), b['sm1'].at[ring['x'][s]], b['sm2'].at[s - 1], peers['x', s])
                put_small(('tk', 1, s), b['tk1'].at[:, ring['z'][s]], b['tk2'].at[s - 1], peers['z', s])
        elif n == 2:
            b['sm_s1'][...] = b['sm1'][x] + b['sm2'][0] + b['sm2'][1] + b['sm2'][2]
            b['tk_s1'][...] = b['tk1'][:, z] + b['tk2'][0] + b['tk2'][1] + b['tk2'][2]
            for s in (1, 2, 3):
                put_small(('sm', 2, s), b['sm_s1'].at[ring['z'][s]], b['sm3'].at[s - 1], peers['z', s])
                put_small(('tk', 2, s), b['tk_s1'].at[:, ring['y'][s]], b['tk3'].at[s - 1], peers['y', s])
        elif n == 3:
            b['sm_s2'][...] = b['sm_s1'][z] + b['sm3'][0] + b['sm3'][1] + b['sm3'][2]
            b['tk_s2'][...] = b['tk_s1'][:, y] + b['tk3'][0] + b['tk3'][1] + b['tk3'][2]
            for s in (1, 2, 3):
                put_small(('sm', 3, s), b['sm_s2'].at[ring['y'][s]], b['sm4'].at[s - 1], peers['y', s])
                put_small(('tk', 3, s), b['tk_s2'], b['tk4'].at[s - 1], peers['x', s])
        else:
            sm_own[...] = b['sm_s2'][y] + b['sm4'][0] + b['sm4'][1] + b['sm4'][2]
            ordered = []
            for place in range(4):
                value = b['tk_s2'][...]
                for s in (1, 2, 3):
                    value = jnp.where(ring['x'][4 - s] == place, b['tk4'][s - 1], value)
                ordered.append(value)
            tk_own[...] = (ordered[0] + ordered[1]) + (ordered[2] + ordered[3])

    tail = bursts.get('end', ())
    small(0)
    for n, s in enumerate(tail):
        step(*s)
        if n in (8, 18, 28, 38):
            small(1 + (8, 18, 28, 38).index(n))
    net.finish()
    assert len(net.builds) <= BACK_COPIES, len(net.builds)


def back(*operands):
    a, v = pl.BlockSpec(memory_space=pl.ANY), pl.BlockSpec(memory_space=pltpu.VMEM)
    S, V, DMA = jax.ShapeDtypeStruct, pltpu.VMEM, pltpu.SemaphoreType.DMA
    return pl.pallas_call(
        back_kernel, name='back',
        in_specs=[a] * 7 + [v] * 7, out_specs=[v] * 5 + [a] * 9,
        out_shape=[S((N_CH, 32, 1024), f32), S((96, 256), f32), S((32, 256), f32), S((8, 128), f32), S((4, 16, 128), f32),
                   S((2, ROWS, CHH), bf16), S((2, ROWS, CH), bf16), S((ROWS, CH), bf16), S((2, ROWS, 2048), bf16),
                   S((2, ROWS, 512), bf16), S((ROWS, 1536), bf16), S((2, ROWS, CHH), bf16), S((2, ROWS, CH), bf16),
                   S((ROWS, CH), bf16)],
        scratch_shapes=[reduce_scratch(), small_scratch(), V((2, ROWS, CHH), bf16), V((2, ROWS, CH), bf16), V((IMG, 512), bf16),
                        V((IMG, CH), bf16), V((16, CH), f32), V((2, CHH), f32), V((CH // 128, XROWS, 128), f32),
                        V((CH // 128, XROWS, 128), f32), V((ROWS, CH), f32), V((ROWS, CH), bf16), V((2, 2, 4, 4, 32, BLK), bf16),
                        V((2, 4, 4, 32, CH), bf16), V((2, ROWS, BLK), f32), V((2, ROWS, BLK), bf16), DMA((BACK_COPIES,)), DMA((BACK_COPIES,)), DMA((4,)), DMA((2,)), DMA((2, 3)),
                        DMA((2, 1))],
        compiler_params=pltpu.CompilerParams(collective_id=1, has_side_effects=True, vmem_limit_bytes=64 * 1024 * 1024 - 65536),
        cost_estimate=pl.CostEstimate(flops=120_000_000_000, bytes_accessed=200_000_000, transcendentals=0),
    )(*operands)


def finish_kernel(c, stem, head, sm, tk, loss, o_stem, o_bstem, o_ln1g, o_ln1b, o_wt1, o_bt1, o_wt2, o_ln2g, o_ln2b, o_ch1,
                  o_bch1, o_ch2, o_bch2, o_lnfg, o_lnfb, o_head, o_bhead):
    def core_last(value, pick):
        got = dot_nt(jnp.concatenate(three_parts(value), axis=0), pick)
        n = value.shape[0]
        return got[0:n] + got[n:2 * n] + got[2 * n:3 * n]
    pick = core_first(1024, 1024, 32)
    for l in range(2):
        o_ch1[l] = core_last(c[2 * l], pick)
        o_ch2[l] = core_last(c[2 * l + 1], pick)
    o_stem[...] = core_last(stem[...], core_first(256, 256, 32))
    o_head[...] = head[:, 0:250]
    own = sm[...]
    turned = jnp.concatenate([own, jnp.zeros((120, 128), f32)], axis=0).T
    for ref, n in ((o_bstem, 0), (o_lnfg, 11), (o_lnfb, 12)):
        ref[...] = turned[n, 0:8]
    for n, ref in enumerate((o_ln1g, o_ln1b, o_ln2g, o_ln2b, o_bch2)):
        for l in range(2):
            ref[pl.ds(l, 1), :] = turned[1 + 5 * l + n:2 + 5 * l + n, 0:8]
    o_bch1[...] = own[0:2, 32:64]
    classes = jnp.concatenate([own[2 + q:3 + q, 64:128] for q in range(4)], axis=1)
    o_bhead[...] = classes[0, 0:250]
    loss[...] = own[6:7, 64:65] * (1.0 / 1024)
    for l in range(2):
        o_wt1[l] = tk[l, :, 0:TOK]
        o_wt2[l] = tk[2 + l, :, 0:TOK]
        tall = jnp.concatenate([tk[l], jnp.zeros((112, 128), f32)], axis=0).T
        o_bt1[pl.ds(l, 1), :] = tall[64:65, 0:16]


def finish(*operands):
    S = jax.ShapeDtypeStruct
    v = pl.BlockSpec(memory_space=pltpu.VMEM)
    return pl.pallas_call(
        finish_kernel, name='finish', in_specs=[v] * 5, out_specs=[v] * 18,
        out_shape=[S((1, 1), f32), S((96, 256), f32), S((8,), f32), S((2, 8), f32), S((2, 8), f32), S((2, 16, TOK), f32),
                   S((2, 16), f32), S((2, 16, TOK), f32), S((2, 8), f32), S((2, 8), f32), S((2, 32, 1024), f32), S((2, 32), f32),
                   S((2, 32, 1024), f32), S((2, 8), f32), S((8,), f32), S((8,), f32), S((32, 250), f32), S((250,), f32)],
    )(*operands)

CHANNEL_AXES = ('tp', 'fsdp')


def weight_specs():
    vec_spec = P(CHANNEL_AXES)
    layer_vec = P(None, CHANNEL_AXES)
    return (P('fsdp', 'tp'), vec_spec, layer_vec, layer_vec, P(None, None, 'fsdp'), P(None, 'fsdp'),
            P(None, 'fsdp', None), layer_vec, layer_vec, P(None, 'fsdp', 'tp'), layer_vec,
            P(None, CHANNEL_AXES, None), layer_vec, vec_spec, vec_spec, P('fsdp', 'tp'), P('tp'))


def solution(mesh):
    def step(patches, labels, w_stem, b_stem, ln1_g, ln1_b, w_tok1, b_tok1, w_tok2,
             ln2_g, ln2_b, w_ch1, b_ch1, w_ch2, b_ch2, lnf_g, lnf_b, w_head, b_head):
        wc, pat, xin, xmid, vin, pre, act, hl, hr, dx0, hstat, gbh, vec, wt = front(
            labels, patches.transpose(1, 0, 2), w_stem, w_ch1, w_ch2, w_head, w_tok1.transpose(0, 2, 1), w_tok2, b_tok1, b_ch1,
            b_head, b_stem, ln1_g, ln1_b, ln2_g, ln2_b, b_ch2, lnf_g, lnf_b)
        sums = back(xin, xmid, pre, wc, act, vin, pat, hl, hr, dx0, hstat, gbh, wt, vec)[:5]
        loss, g_s, g_bs, g_1g, g_1b, g_t1, g_bt, g_t2, g_2g, g_2b, g_c1, g_b1, g_c2, g_b2, g_fg, g_fb, g_h, g_bh = finish(*sums)
        return (loss.reshape(()), g_s, g_bs, g_1g, g_1b, g_t1.transpose(0, 2, 1), g_bt, g_t2, g_2g, g_2b, g_c1, g_b1, g_c2, g_b2,
                g_fg, g_fb, g_h, g_bh)

    specs = weight_specs()
    return jax.shard_map(step, mesh=mesh, in_specs=(P('fsdp', None, None), P('fsdp')) + specs,
                         out_specs=(P(),) + specs, check_vma=False)
```

```python
import functools

import jax
import jax.numpy as jnp
from jax import lax
from jax.experimental import pallas as pl
from jax.experimental.pallas import tpu as pltpu
from jax.sharding import PartitionSpec as P

MESH = pl.DeviceIdType.MESH
ORDERS = (('x', 'y', 'z'), ('y', 'z', 'x'), ('z', 'x', 'y'))
COLS = ((0, 384), (384, 384), (768, 256))
N_CH = 4
STEM, HEAD = 4, 5
bf16, f32 = jnp.bfloat16, jnp.float32


def my_place():
    f = lax.axis_index('fsdp')
    return {'x': lax.axis_index('tp'), 'z': f // 8, 'y': (f // 2) % 4, 'k': f % 2}


def moved(place, dim, step):
    new = dict(place)
    new[dim] = 1 - place['k'] if dim == 'k' else (place[dim] + step) % 4
    return new


def device(place):
    return {'tp': place['x'], 'fsdp': (place['z'] * 4 + place['y']) * 2 + place['k']}


EPS = 1e-6
TOK, TPAD = 49, 56
IMG = 8
ROWS, XROWS = IMG * TOK, IMG * TPAD
CHUNKS = ((0, 112), (112, 112), (224, 112), (336, 56))
CH, TOKH, CHH = 1024, 512, 4096
BLK = 512
NBLK = CHH // BLK
GELU_C, GELU_A = 0.7978845608028654, 0.044715


def dot_nn(a, b):
    return lax.dot_general(a, b, (((1,), (0,)), ((), ())), preferred_element_type=f32)


def dot_nt(a, b):
    return lax.dot_general(a, b, (((1,), (1,)), ((), ())), preferred_element_type=f32)


def dot_tn(a, b):
    return lax.dot_general(a, b, (((0,), (0,)), ((), ())), preferred_element_type=f32)


def gelu_both(x):
    sq = x * x
    half = 0.5 * jnp.tanh(x * (GELU_C + (GELU_C * GELU_A) * sq))
    rise = 0.5 + half
    value = x * rise
    return value, rise + value * (0.5 - half) * (2.0 * GELU_C + (6.0 * GELU_C * GELU_A) * sq)


def standardize(x):
    mean = jnp.mean(x, axis=-1, keepdims=True)
    cent = x - mean
    inv = lax.rsqrt(jnp.mean(cent * cent, axis=-1, keepdims=True) + EPS)
    return cent * inv, inv


def norm_grad(d, gain, std, inv):
    gs = d * gain
    m0 = jnp.mean(gs, axis=-1, keepdims=True)
    m1 = jnp.mean(gs * std, axis=-1, keepdims=True)
    return inv * (gs - m0 - std * m1)


def row_mask(rows=TPAD):
    return lax.broadcasted_iota(jnp.int32, (rows, 1), 0) < TOK


def image(b):
    return pl.ds(b, TPAD, stride=IMG)


def get(ref, rows):
    return jnp.concatenate([ref[n, rows, :] for n in range(CH // 128)], axis=1)


def put(ref, rows, value):
    for n in range(CH // 128):
        ref[n, rows, :] = value[:, 128 * n:128 * (n + 1)]


class Stream:
    def __init__(self, sem, copies, count):
        self.sem, self.copies, self.count = sem, copies, count

    def make(self, i, slot):
        return [pltpu.make_async_copy(src, dst, self.sem.at[slot, n]) for n, (src, dst) in enumerate(self.copies(i, slot))]

    def start(self, i, slot):
        for copy in self.make(i, slot):
            copy.start()

    def wait(self, i, slot):
        for copy in self.make(i, slot):
            copy.wait()


def for_blocks(stream, body, out=None):
    n = stream.count
    stream.start(0, 0)

    @pl.loop(0, n)
    def _(i):
        slot = i % 2
        stream.wait(i, slot)

        @pl.when(i + 1 < n)
        def _():
            stream.start(i + 1, 1 - slot)
        if out is not None:
            @pl.when(i >= 2)
            def _():
                out.wait(i - 2, slot)
        body(i, slot)
        if out is not None:
            out.start(i, slot)
    if out is not None:
        out.wait(n - 2, n % 2)
        out.wait(n - 1, 1 - n % 2)


TOK_CUTS = 4
FRONT_COPIES = 270
EARLY = [('stem', c) for c in range(3)] + [('ch', c, p) for p in 'ab' for c in range(3)] + [('head', 2)]
PARTS = {'a': pl.ds(0, 2), 'b': pl.ds(2, 2)}
LATE = [('stem', c, None) for c in range(3)] + [('ch', c, g) for g in range(N_CH) for c in range(3)] + [('head', 2, None)]
UNIT_GROUP = {('stem', None): 0, ('ch', 0): 1, ('ch', 1): 2, ('ch', 2): 3, ('ch', 3): 4, ('head', None): 5}
EVERY = pl.ds(0, 4)
FRONT_ORDER = (
    ('prep', (('M0', ('sm',)), ('M0', ('tk',)), ('A0', ('stem', 0)), ('A0', ('stem', 1)), ('A0', ('stem', 2)),
        ('A0', ('ch', 0, 'a')), ('A0', ('ch', 0, 'b')), ('A0', ('ch', 1, 'a')), ('A0', ('ch', 1, 'b')),
        ('A0', ('ch', 2, 'a')), ('A0', ('ch', 2, 'b')), ('A0', ('head', 2)),)),
    ('unpack', (('M1', ('sm',)), ('M1', ('tk',)), ('A', ('stem', 0)), ('A', ('stem', 1)), ('A', ('stem', 2)),
        ('A', ('ch', 0, 'a')), ('A', ('ch', 1, 'a')), ('A', ('ch', 2, 'a')), ('B', ('stem', 0)), ('M2', ('sm',)),
        ('B', ('stem', 1)), ('M2', ('tk',)), ('B', ('stem', 2)), ('C', ('stem', 0)), ('M3', ('sm',)), ('C', ('stem', 2)),
        ('D', ('stem', 0, None)), ('B', ('ch', 0, 'a')), ('C', ('stem', 1)), ('B', ('ch', 1, 'a')), ('B', ('ch', 2, 'a')),
        ('A', ('head', 2)),)),
    ('stem0', (('D', ('stem', 2, None)), ('C', ('ch', 2, 'a')), ('C', ('ch', 0, 'a')), ('E', ('stem', 0, None)),
        ('D', ('stem', 1, None)), ('B', ('head', 2)), ('C', ('ch', 1, 'a')), ('E', ('stem', 2, None)),
        ('F', ('stem', 0, None)), ('A', ('ch', 0, 'b')), ('A', ('ch', 1, 'b')), ('A', ('ch', 2, 'b')),
        ('E', ('stem', 1, None)), ('D', ('ch', 2, 0)), ('D', ('ch', 0, 0)), ('D', ('ch', 0, 1)), ('D', ('ch', 2, 1)),
        ('D', ('ch', 1, 0)), ('F', ('stem', 2, None)), ('D', ('ch', 1, 1)), ('B', ('ch', 0, 'b')), ('B', ('ch', 2, 'b')),
        ('B', ('ch', 1, 'b')), ('F', ('stem', 1, None)), ('E', ('ch', 2, 0)),)),
    ('stem2', (('E', ('ch', 0, 0)), ('C', ('head', 2)),)),
    ('tok0_0', (('E', ('ch', 1, 0)), ('E', ('ch', 2, 1)),)),
    ('tok0_2', (('C', ('ch', 0, 'b')),)),
    ('tok0_3', (('E', ('ch', 0, 1)),)),
    ('tok0_4', (('F', ('ch', 2, 0)), ('E', ('ch', 1, 1)),)),
    ('tok0_5', (('C', ('ch', 1, 'b')), ('F', ('ch', 2, 1)),)),
    ('tok0_6', (('C', ('ch', 2, 'b')), ('D', ('head', 2, None)), ('D', ('ch', 0, 2)), ('D', ('ch', 0, 3)),)),
    ('tok0_7', (('F', ('ch', 0, 0)),)),
    ('ln0', (('F', ('ch', 1, 0)),)),
    ('ch0_0', (('F', ('ch', 0, 1)), ('F', ('ch', 1, 1)), ('E', ('head', 2, None)), ('D', ('ch', 1, 2)), ('D', ('ch', 1, 3)),
        ('D', ('ch', 2, 2)), ('D', ('ch', 2, 3)),)),
    ('ch0_2', (('F', ('head', 2, None)),)),
    ('ch0_4', (('E', ('ch', 0, 2)),)),
    ('ch0_6', (('E', ('ch', 1, 2)), ('E', ('ch', 2, 2)),)),
    ('tok1_1', (('E', ('ch', 0, 3)), ('E', ('ch', 2, 3)),)),
    ('tok1_2', (('F', ('ch', 2, 2)), ('E', ('ch', 1, 3)),)),
    ('tok1_3', (('F', ('ch', 0, 2)),)),
    ('tok1_5', (('F', ('ch', 1, 2)), ('F', ('ch', 2, 3)), ('F', ('ch', 0, 3)),)),
    ('tok1_7', (('F', ('ch', 1, 3)),)),
)


class Net:
    def __init__(self, send_sems, recv_sems):
        self.send_sems, self.recv_sems, self.names, self.builds, self.done = send_sems, recv_sems, {}, [], set()

    def copy(self, name):
        n = self.names[name]
        src, dst, target = self.builds[n]()
        return pltpu.make_async_remote_copy(src_ref=src, dst_ref=dst, send_sem=self.send_sems.at[n],
                                            recv_sem=self.recv_sems.at[n], device_id=target, device_id_type=MESH)

    def start(self, name, build):
        self.names[name] = len(self.builds)
        self.builds.append(build)
        self.copy(name).start()

    def arrived(self, *names):
        for name in names:
            self.copy(name).wait_recv()

    def finish(self):
        for name in self.names:
            if name not in self.done:
                self.copy(name).wait_send()


def core_first(size, cols, each):
    half = cols // 2
    row = lax.broadcasted_iota(jnp.int32, (size, size), 0)
    col = lax.broadcasted_iota(jnp.int32, (size, size), 1)
    source = col % half // each * (2 * each) + col // half * each + col % each
    return jnp.where(row == source, 1.0, 0.0).astype(bf16)


def three_parts(x):
    hi = x.astype(bf16)
    rest = x - hi.astype(f32)
    mid = rest.astype(bf16)
    return hi, mid, (rest - mid.astype(f32)).astype(bf16)


def with_bias_rows(a):
    row = lax.broadcasted_iota(jnp.int32, (TPAD, 1), 0)
    return jnp.where(row < TOK, a, jnp.where(row < TOK + 3, 1.0, 0.0)).astype(bf16)


def front_kernel(labels, patches, w_stem, w_ch1, w_ch2, w_head, w_tok1, w_tok2, b_tok1, b_ch1, b_head, b_stem, ln1_g, ln1_b,
                 ln2_g, ln2_b, b_ch2, lnf_g, lnf_b,
                 wc, pat_out, xin, xmid, vout, pre_out, act_out, tok_act, tok_slope, hl, hr, dx0, hstat, gbh, vec, wt, wt_t,
                 pc, ps, ph, tk_f, tk_p, sm_p, bh_p, ws, wh, tk_v, sm_v, sm_2, bh_v, bch1,
                 turn, p_v, pk_v, x_v, v_v, w1_v, w2_v, pre_v, act_v, g_v, s_v,
                 send_sems, recv_sems, sem, sem_w, sem_o, sem_x, sem_t):
    me = my_place()
    other = moved(me, 'k', 1)
    load_p = pltpu.make_async_copy(patches.at[:, pl.ds(pl.multiple_of(me['x'] * IMG, IMG), IMG)], p_v, sem.at[0])
    load_p.start()

    barrier = pltpu.get_barrier_semaphore()
    for dim in 'xyz':
        for step in (1, 2, 3):
            pl.semaphore_signal(barrier, inc=1, device_id=device(moved(me, dim, step)), device_id_type=MESH)
    pl.semaphore_signal(barrier, inc=1, device_id=device(other), device_id_type=MESH)

    stem = dot_nn(w_stem[...].astype(bf16), core_first(256, 256, 32)).astype(bf16)
    ps[0], ps[1] = stem[:, 0:128], stem[:, 128:256]
    pick = core_first(1024, 1024, 32)
    for l in range(2):
        pc[2 * l] = dot_nn(w_ch1[l].astype(bf16), pick).astype(bf16)
        pc[2 * l + 1] = dot_nn(w_ch2[l].astype(bf16), pick).astype(bf16)
    ph[...] = jnp.zeros_like(ph)
    ph[:, pl.ds(0, 250)] = w_head[...].astype(bf16)
    turn[...] = jnp.zeros_like(turn)
    for n, ref in ((0, b_stem), (11, lnf_g), (12, lnf_b)):
        turn[n, pl.ds(0, 8)] = ref[...]
    for n, ref in enumerate((ln1_g, ln1_b, ln2_g, ln2_b, b_ch2)):
        for l in range(2):
            turn[pl.ds(1 + 5 * l + n, 1), pl.ds(0, 8)] = ref[pl.ds(l, 1), :]
    turn[pl.ds(16, 2), pl.ds(0, 16)] = b_tok1[...]
    turned = turn[...].T
    tk_f[...] = jnp.zeros_like(tk_f)
    for l in range(2):
        tk_f[l, :, pl.ds(0, TOK)] = w_tok1[l]
        tk_f[2 + l, :, pl.ds(0, TOK)] = w_tok2[l]
        for n, part in enumerate(three_parts(turned[0:16, 16 + l:17 + l])):
            tk_f[l, :, pl.ds(TOK + n, 1)] = part.astype(f32)
    tk_p[...] = tk_f[...].astype(bf16)
    sm_p[...] = jnp.zeros_like(sm_p)
    sm_p[:, pl.ds(0, 16)] = turned[0:8, 0:16]
    sm_p[pl.ds(0, 2), pl.ds(32, 32)] = b_ch1[...]
    bh_p[...] = jnp.full_like(bh_p, -1e30)
    bh_p[0, pl.ds(0, 250)] = b_head[...]

    net = Net(send_sems, recv_sems)
    core = me['k']
    ring = {d: [moved(me, d, n)[d] for n in range(4)] for d in 'xyz'}
    columns = [pl.ds(pl.multiple_of(x * 256, 256), 256) for x in ring['x']]
    stem_columns = [pl.ds(pl.multiple_of(x * 128, 128), 128) for x in ring['x']]
    peers = {(d, n): device(moved(me, d, n)) for d in 'xyz' for n in (1, 2, 3)}
    partner = device(other)
    here = {'x': 0, 'y': 0, 'z': 0}

    def view(unit, block, half=None):
        kind, colour = unit[:2]
        x, z, y = (EVERY if block[d] is None else ring[d][block[d]] for d in 'xzy')
        r0, rn = (0, 32) if half is None else (16 * half, 16)
        if kind == 'ch':
            c0, cn = COLS[colour]
            g = PARTS.get(unit[2], unit[2])
            return wc.at[g, x, core, z, y, pl.ds(r0, rn), pl.ds(c0, cn)]
        if kind == 'stem':
            cols = pl.ds(0, 512) if x is EVERY else stem_columns[block['x']]
            return ws.at[:, z, y, core, pl.ds(32 * colour + r0, rn), cols]
        cols = pl.ds(0, CH) if x is EVERY else columns[block['x']]
        return wh.at[core, z, y, pl.ds(r0, rn), cols]

    def piece(unit):
        kind, colour = unit[:2]
        if kind == 'ch':
            return pc.at[PARTS[unit[2]], :, pl.ds(*COLS[colour])]
        return ps.at[:, pl.ds(32 * colour, 32), :] if kind == 'stem' else ph.at[:, :]

    def exchange(unit, tag, dim, block):
        for side, step in (('l', 1), ('r', 3)):
            def build(step=step):
                part = view(unit, block)
                return (piece(unit) if tag == '1' else part), part, peers[dim, step]
            net.start((unit, tag, side), build)

    def forward_half(unit, tag, dim, block):
        for half, (origin, target, side) in enumerate(((3, 1, 'l'), (1, 3, 'r'))):
            def build(half=half, origin=origin, target=target):
                part = view(unit, {**block, dim: origin}, half)
                return part, part, peers[dim, target]
            net.start((unit, tag, side), build)

    def swap(unit, tag, block):
        def build():
            part = view(unit, block)
            return part, part, partner
        net.start((unit, tag), build)

    own = pltpu.make_async_copy(pc, wc.at[:, me['x'], me['k'], me['z'], me['y']], sem.at[1])
    own.start()
    mine = pl.ds(pl.multiple_of(me['x'] * 256, 256), 256)
    for n in range(2):
        ws[n, me['z'], me['y'], me['k'], :, stem_columns[0]] = ps[n]
    wh[me['k'], me['z'], me['y'], :, mine] = ph[...]
    sm_v[me['x'], me['z'], me['y'], me['k']] = sm_p[...]
    tk_v[:, me['z'], me['y'], me['k']] = tk_p[...]
    bh_v[:, mine] = bh_p[...]
    own.wait()
    pl.semaphore_wait(barrier, 10)

    def small(kind, n):
        dims = 'xyz' if kind == 'sm' else 'yz'
        at = {d: EVERY if d in dims[:n] else ring[d][0] for d in 'xyz'}

        def part():
            if kind == 'sm':
                return sm_v.at[at['x'], at['z'], at['y'], core]
            return tk_v.at[:, at['z'], at['y'], core]
        if n > 0:
            net.arrived(*[(kind, n - 1, s) for s in (1, 2, 3)])
        if n < len(dims):
            for s in (1, 2, 3):
                net.start((kind, n, s), lambda s=s: (part(), part(), peers[dims[n], s]))
            if kind == 'sm' and n == 0:
                def head_bias():
                    return bh_v.at[:, columns[0]]
                for s in (1, 2, 3):
                    net.start(('bh', s), lambda s=s: (head_bias(), head_bias(), peers['x', s]))
        else:
            net.start((kind, 'k'), lambda: (part(), part(), partner))

    def step(name, unit):
        if name[0] == 'M':
            small(unit[0], int(name[1]))
            return
        d1, d2, d3 = ORDERS[unit[1]]
        early = unit[:2] if unit[0] != 'ch' or unit[2] in PARTS else ('ch', unit[1], 'a' if unit[2] < 2 else 'b')
        plane = {**here, d1: None, d2: None}
        if name == 'A0':
            exchange(unit, '1', d1, here)
        elif name == 'A':
            net.arrived((unit, '1', 'l'), (unit, '1', 'r'))
            forward_half(unit, '1h', d1, here)
        elif name == 'B':
            net.arrived((unit, '1h', 'l'), (unit, '1h', 'r'))
            exchange(unit, '2', d2, {**here, d1: None})
        elif name == 'C':
            net.arrived((unit, '2', 'l'), (unit, '2', 'r'))
            forward_half(unit, '2h', d2, {**here, d1: None})
        elif name == 'D':
            if early not in planes:
                planes.add(early)
                net.arrived((early, '2h', 'l'), (early, '2h', 'r'))
            exchange(unit, '3', d3, plane)
            swap(unit, 'k0', plane)
        elif name == 'E':
            net.arrived((unit, '3', 'l'), (unit, '3', 'r'))
            forward_half(unit, '3h', d3, plane)
            for n in (1, 3):
                swap(unit, f'k{n}', {**plane, d3: n})
        else:
            net.arrived((unit, '3h', 'l'), (unit, '3h', 'r'))
            swap(unit, 'k2', {**plane, d3: 2})

    planes = set()
    awaited = set()

    def need(group):
        for u in LATE:
            if UNIT_GROUP[u[0], u[2]] <= group and u not in awaited:
                awaited.add(u)
                net.arrived(*[(u, f'k{n}') for n in range(4)])

    bursts = {name: steps for name, steps in FRONT_ORDER}

    def burst(name):
        for s in bursts.get(name, ()):
            step(*s)

    def during(name, count):
        def run(i):
            for n in range(1, count):
                if bursts.get(f'{name}{n}'):
                    pl.when(i == n)(functools.partial(burst, f'{name}{n}'))
        return run

    burst('prep')
    load_p.wait()
    pick = core_first(768, 768, 96)
    for g in range(4):
        part = dot_nn(p_v[:, :, pl.ds(768 * g, 768)].reshape(ROWS, 768), pick).astype(bf16)
        for n in range(2):
            pk_v[n, :, pl.ds(384 * g, 384)] = part[:, 384 * n:384 * n + 384]
    keep_p = pltpu.make_async_copy(pk_v, pat_out, sem.at[0])
    keep_p.start()

    burst('unpack')
    net.arrived(('sm', 'k'), ('tk', 'k'), ('bh', 1), ('bh', 2), ('bh', 3))
    sm_2[...] = sm_v[...].reshape(1024, 128)
    for n in range(8):
        tile = jnp.concatenate([sm_2[pl.ds((n % 4 * 4 + i) * 64 + n // 4 * 32, 32), :] for i in range(4)], axis=0)
        vec[:, pl.ds(128 * n, 128)] = tile.T[0:16, :]
    wt[...] = tk_v[...].reshape(4, TOKH, 128)
    for n in range(4):
        wt_t[n] = wt[n].astype(f32).T[0:TPAD].astype(bf16)
    for l in range(2):
        rows = jnp.concatenate(three_parts(sm_2[pl.ds(l, 128, stride=8), :]), axis=0)

        @pl.loop(0, 8)
        def _(n):
            lane = lax.broadcasted_iota(jnp.int32, (128, 512), 0)
            col = lax.broadcasted_iota(jnp.int32, (128, 512), 1)
            pick = jnp.where(lane == 32 + col % 32, 1.0, 0.0).astype(bf16)
            spread = dot_nn(rows, pick)
            value = spread[0:128] + spread[128:256] + spread[256:384]
            mine = lane == n // 2 * 32 + col // 32 * 2 + n % 2
            bch1[l:l + 1, pl.ds(pl.multiple_of(n * 512, 512), 512)] = jnp.sum(jnp.where(mine, value, 0.0), axis=0, keepdims=True)

    burst('stem0')
    need(0)
    run = during('stem', 4)
    put(x_v, pl.ds(ROWS, XROWS - ROWS), jnp.zeros((XROWS - ROWS, CH), f32))

    @pl.loop(0, 4)
    def _(i):
        run(i)
        cols = pl.ds(pl.multiple_of(i * 256, 256), 256)
        w = ws[i // 2, :, :, :, :, pl.ds(pl.multiple_of(i % 2 * 256, 256), 256)].reshape(3072, 256)
        value = dot_nn(p_v[...].reshape(ROWS, 3072), w) + vec[0:1, cols]
        for n in range(2):
            x_v[2 * i + n, pl.ds(0, ROWS), :] = value[:, 128 * n:128 * (n + 1)]

    wc_all = wc

    def add_rows(value):
        for n in range(CH // 128):
            x_v[n, pl.ds(0, ROWS), :] += value[:, 128 * n:128 * (n + 1)]

    for l in range(2):
        r = 1 + 5 * l
        burst(f'tok{l}_0')
        run = during(f'tok{l}_', IMG)
        save_in = pltpu.make_async_copy(x_v.at[:, pl.ds(0, ROWS)], xin.at[l], sem_x.at[0])
        save_in.start()
        save_in.wait()
        hidden = Stream(sem_t, lambda i, slot: [(g_v.at[slot], tok_act.at[l, pl.ds(i * TOK_CUTS, TOK_CUTS)]),
                                                (s_v.at[slot], tok_slope.at[l, pl.ds(i * TOK_CUTS, TOK_CUTS)])], IMG)

        @pl.loop(0, IMG)
        def _(b):
            run(b)
            x = get(x_v, image(b))
            std, _ = standardize(x)
            a = with_bias_rows(std * vec[r:r + 1, :] + vec[r + 1:r + 2, :])
            spare = b % 2

            @pl.when(b >= 2)
            def _():
                hidden.wait(b - 2, spare)
            width = CH // TOK_CUTS
            parts = []
            for n in range(TOK_CUTS):
                value, slope = gelu_both(dot_nn(wt[l, :, 0:TPAD], a[:, width * n:width * (n + 1)]))
                g_v[spare, n] = value.astype(bf16)
                s_v[spare, n] = slope
                parts.append(dot_nn(wt_t[2 + l], g_v[spare, n]))
            hidden.start(b, spare)
            put(x_v, image(b), x + jnp.concatenate(parts, axis=1))
        hidden.wait(IMG - 2, 0)
        hidden.wait(IMG - 1, 1)
        save_mid = pltpu.make_async_copy(x_v.at[:, pl.ds(0, ROWS)], xmid.at[l], sem_x.at[0])
        save_mid.start()
        burst(f'ln{l}')

        for at, size in CHUNKS:
            std, _ = standardize(get(x_v, pl.ds(at, size)))
            v_v[pl.ds(at, size), :] = (std * vec[r + 2:r + 3, :] + vec[r + 3:r + 4, :]).astype(bf16)
        save_v = [pltpu.make_async_copy(v_v.at[:, pl.ds(512 * n, 512)], vout.at[l, n], sem_x.at[1 + n]) for n in range(2)]
        for copy in save_v:
            copy.start()
        burst(f'ch{l}_0')
        need(2 + 2 * l)
        save_mid.wait()

        def blocks(i, slot):
            t, h = i // 2, i % 2
            part = pl.ds(pl.multiple_of(h * BLK, BLK), BLK)
            return [(wc_all.at[2 * l, t, :, :, :, :, part], w1_v.at[slot]), (wc_all.at[2 * l + 1, t, h], w2_v.at[slot])]

        def outs(i, slot):
            part = pl.ds(pl.multiple_of(i * BLK, BLK), BLK)
            half = pl.ds(pl.multiple_of(i // 2 * BLK, BLK), BLK)
            return [(pre_v.at[slot], pre_out.at[l, :, part]), (act_v.at[slot], act_out.at[l, i % 2, :, half])]
        run = during(f'ch{l}_', NBLK)

        def channel(i, slot):
            run(i)
            part = pl.ds(pl.multiple_of(i * BLK, BLK), BLK)
            h = dot_nn(v_v[...], w1_v[slot].reshape(CH, BLK)) + bch1[l:l + 1, part]
            value, pre_v[slot] = gelu_both(h)
            act_v[slot] = value.astype(bf16)
            add_rows(dot_nn(act_v[slot], w2_v[slot].reshape(BLK, CH)))
        for_blocks(Stream(sem_w, blocks, NBLK), channel, Stream(sem_o, outs, NBLK))
        add_rows(jnp.broadcast_to(vec[r + 4:r + 5, :], (ROWS, CH)))
        for copy in save_v:
            copy.wait()

    burst('head')
    need(5)
    keep_p.wait()
    last = 11
    pooled = jnp.sum(get(x_v, pl.ds(0, ROWS)).reshape(TOK, IMG, CH), axis=0) * (1.0 / TOK)
    std, inv = standardize(pooled)
    head_in = (std * vec[last:last + 1, :] + vec[last + 1:last + 2, :]).astype(bf16)
    hl[...] = head_in
    w_h = wh[...].reshape(CH, CH)
    logits = dot_nn(head_in, w_h) + bh_v[0:1, :]
    row = lax.broadcasted_iota(jnp.int32, (IMG, 1), 0)
    label = jnp.zeros((IMG, 1), jnp.int32)
    for b in range(IMG):
        value = labels[me['x'] * IMG + b]
        label = jnp.where(row == b, value, label)
    label = label + 6 * sum(jnp.where(label >= edge, 1, 0) for edge in (250, 500, 750))
    is_label = lax.broadcasted_iota(jnp.int32, logits.shape, 1) == label
    top = jnp.max(logits, axis=-1, keepdims=True)
    ex = jnp.exp(logits - top)
    es = jnp.sum(ex, axis=-1, keepdims=True)
    nll = top + jnp.log(es) - jnp.sum(jnp.where(is_label, logits, 0.0), axis=-1, keepdims=True)
    d_logits = (ex / es - jnp.where(is_label, 1.0, 0.0)) * (1.0 / 1024)
    gbh[...] = jnp.sum(d_logits, axis=0, keepdims=True)
    d_bf = d_logits.astype(bf16)
    hr[...] = d_bf
    d_in = dot_nt(d_bf, w_h)
    hstat[0:1, :] = jnp.sum(d_in * std, axis=0, keepdims=True)
    hstat[1:2, :] = jnp.sum(d_in, axis=0, keepdims=True)
    hstat[2:3, :] = jnp.broadcast_to(jnp.sum(nll, axis=0, keepdims=True), (1, CH))
    dx0[...] = norm_grad(d_in, vec[last:last + 1, :], std, inv) * (1.0 / TOK)
    burst('end')
    net.finish()
    assert len(net.builds) <= FRONT_COPIES, len(net.builds)


def front(*operands):
    a, v = pl.BlockSpec(memory_space=pl.ANY), pl.BlockSpec(memory_space=pltpu.VMEM)
    S, V, DMA = jax.ShapeDtypeStruct, pltpu.VMEM, pltpu.SemaphoreType.DMA
    return pl.pallas_call(
        front_kernel, name='front',
        in_specs=[pl.BlockSpec(memory_space=pltpu.SMEM), a] + [v] * 17,
        out_specs=[a] * 9 + [v] * 8,
        out_shape=[S((N_CH, 4, 2, 4, 4, 32, 1024), bf16), S((2, ROWS, 1536), bf16), S((2, CH // 128, ROWS, 128), f32),
                   S((2, CH // 128, ROWS, 128), f32),
                   S((2, 2, ROWS, 512), bf16), S((2, ROWS, CHH), f32), S((2, 2, ROWS, 2048), bf16),
                   S((2, IMG * TOK_CUTS, TOKH, CH // TOK_CUTS), bf16), S((2, IMG * TOK_CUTS, TOKH, CH // TOK_CUTS), f32), S((IMG, CH), bf16),
                   S((IMG, CH), bf16), S((IMG, CH), f32), S((8, CH), f32), S((1, CH), f32), S((16, CH), f32),
                   S((4, TOKH, 128), bf16), S((4, TPAD, TOKH), bf16)],
        scratch_shapes=[V((N_CH, 32, 1024), bf16), V((2, 96, 128), bf16), V((32, 256), bf16), V((4, 16, 128), f32),
                        V((4, 16, 128), bf16), V((8, 128), f32), V((8, 256), f32), V((2, 4, 4, 2, 96, 512), bf16),
                        V((2, 4, 4, 32, CH), bf16), V((4, 4, 4, 2, 16, 128), bf16), V((4, 4, 4, 2, 8, 128), f32),
                        V((1024, 128), f32), V((8, CH), f32), V((2, CHH), f32),
                        V((128, 128), f32), V((TOK, IMG, 3072), bf16), V((2, ROWS, 1536), bf16), V((CH // 128, XROWS, 128), f32),
                        V((ROWS, CH), bf16), V((2, 2, 4, 4, 32, BLK), bf16), V((2, 4, 4, 32, CH), bf16),
                        V((2, ROWS, BLK), f32), V((2, ROWS, BLK), bf16),
                        V((2, TOK_CUTS, TOKH, CH // TOK_CUTS), bf16), V((2, TOK_CUTS, TOKH, CH // TOK_CUTS), f32),
                        DMA((FRONT_COPIES,)), DMA((FRONT_COPIES,)), DMA((2,)), DMA((2, 2)), DMA((2, 2)), DMA((3,)), DMA((2, 2))],
        compiler_params=pltpu.CompilerParams(collective_id=0, has_side_effects=True, vmem_limit_bytes=62 * 1024 * 1024),
        cost_estimate=pl.CostEstimate(flops=90_000_000_000, bytes_accessed=180_000_000, transcendentals=0),
    )(*operands)


GROUPS = (3, 2, 1, 0, HEAD, STEM)
UNITS = tuple((g, c) for g in GROUPS for c in (2, 0, 1) if g != HEAD or c == 2)
BACK_COPIES = 18 * len(UNITS) + 40
NEEDS = {3: ('act1', 'dout1'), 2: ('vin1', 'dpre1'), 1: ('act0', 'dout0'), 0: ('vin0', 'dpre0'), STEM: ('pat', 'dres'),
         HEAD: ('hl', 'hr')}
BACK_ORDER = (
    ('l1', ((3, 'L'),)),
    ('t1_5', ((0, 0), (0, 1), (1, 0), (1, 1),)),
    ('t1_7', ((0, 2),)),
    ('c0_1', ((1, 2),)),
    ('c0_2', ((0, 3), (2, 0), (2, 'L'), (2, 1),)),
    ('c0_4', ((1, 3), (0, 4),)),
    ('c0_7', ((2, 2), (0, 5),)),
    ('t0_1', ((1, 4),)),
    ('t0_3', ((3, 0), (3, 1), (2, 3), (1, 5), (0, 6), (4, 0), (4, 1), (0, 7), (5, 0), (1, 'L'), (5, 1), (3, 2),)),
    ('t0_4', ((2, 4),)),
    ('t0_5', ((4, 2), (1, 6),)),
    ('t0_6', ((3, 3), (6, 0), (6, 1), (5, 2), (2, 5), (1, 7), (7, 0), (7, 1), (4, 3), (3, 4), (2, 6), (8, 0), (0, 'L'),
        (8, 1), (6, 2), (5, 3), (4, 4),)),
    ('t0_7', ((7, 2),)),
    ('fin', ((9, 0), (9, 1), (8, 2), (5, 4), (3, 5), (6, 3), (2, 7),)),
    ('end', ((9, 2), (6, 4), (4, 5), (7, 3), (10, 0), (10, 1), (5, 5), (8, 3), (7, 4), (6, 5), (3, 6), (11, 0), (4, 'L'),
        (11, 1), (9, 3), (8, 4), (7, 5), (4, 6), (6, 6), (3, 7), (12, 0), (12, 1), (10, 2), (13, 0), (13, 1), (11, 2),
        (12, 2), (9, 4), (8, 5), (5, 6), (7, 6), (4, 7), (14, 0), (14, 1), (15, 0), (15, 1), (6, 7), (10, 3), (9, 5), (8, 6),
        (5, 7), (11, 3), (13, 2), (14, 2), (15, 2), (12, 3), (7, 7), (8, 7), (11, 4), (10, 4), (9, 6), (12, 4), (11, 5),
        (15, 3), (12, 5), (13, 3), (10, 5), (14, 3), (9, 7), (11, 6), (12, 6), (15, 4), (13, 4), (10, 6), (14, 4), (11, 7),
        (12, 7), (15, 5), (10, 7), (13, 5), (14, 5), (15, 6), (13, 6), (14, 6), (15, 7), (13, 7), (14, 7),)),
)
SMALL = dict(sm=((4, 4, 4, 8, 128), (3, 4, 4, 8, 128), (3, 4, 8, 128), (3, 8, 128)),
             tk=((4, 4, 4, 16, 128), (3, 4, 4, 16, 128), (3, 4, 16, 128), (3, 4, 16, 128)))


def reduce_scratch():
    per = []
    for c in range(3):
        n = COLS[c][1]
        many = sum(1 for u in UNITS if u[1] == c)
        lead = ((4, 4), (4,), ())
        b = {'C': pltpu.VMEM((2, 4, 4, 4, 32, n), bf16), 'S1': pltpu.VMEM((4, 4, 32, n), f32), 'S2': pltpu.VMEM((2, 4, 32, n), f32)}
        for ph in range(3):
            if ph:
                b[f'opp{ph}'] = pltpu.VMEM(lead[ph] + (32, n), bf16)
                b[f'pr{ph}'] = pltpu.VMEM(lead[ph] + (16, n), bf16)
                b[f'pl{ph}'] = pltpu.VMEM(lead[ph] + (16, n), bf16)
            for name in ('rig', 'lef'):
                b[f'{name}{ph}'] = pltpu.VMEM(lead[ph] + (16, n), bf16)
            for name in ('half0', 'half1'):
                b[f'{name}{ph}'] = pltpu.VMEM((many,) + lead[ph] + (16, n), bf16)
            for name in ('froml', 'fromr'):
                b[f'{name}{ph}'] = pltpu.VMEM((many,) + lead[ph] + (32, n), bf16)
        per.append(b)
    return per


def small_scratch():
    b = {f'{kind}{n + 1}': pltpu.VMEM(shape, f32) for kind, shapes in SMALL.items() for n, shape in enumerate(shapes)}
    b.update(sm=pltpu.VMEM((4, 4, 4, 2, 8, 128), f32), tk=pltpu.VMEM((4, 4, 4, 2, 16, 128), f32),
             sm_s1=pltpu.VMEM((4, 4, 8, 128), f32), sm_s2=pltpu.VMEM((4, 8, 128), f32),
             tk_s1=pltpu.VMEM((4, 4, 16, 128), f32), tk_s2=pltpu.VMEM((4, 16, 128), f32))
    return b


def small_pack(b, flat, turn, gvec, hstat, gbch1, gbh):
    for n in range(8):
        cols = pl.ds(128 * n, 128)
        turn[n, pl.ds(0, 128), :] = jnp.zeros((128, 128), f32)
        turn[n, pl.ds(0, 16), :] = gvec[:, cols]
        turn[n, pl.ds(11, 2), :] = hstat[pl.ds(0, 2), cols]
    for n in range(8):
        tile = turn[n, pl.ds(0, 128), :].T
        for i in range(4):
            a = n % 4 * 4 + i
            flat[a // 2, pl.ds(a % 2 * 64 + n // 4 * 32, 32), :] = tile[32 * i:32 * i + 32]
    for l in range(2):
        def gather(n, total):
            lane = lax.broadcasted_iota(jnp.int32, (128, 512), 0)
            col = lax.broadcasted_iota(jnp.int32, (128, 512), 1)
            sums = gbch1[l:l + 1, pl.ds(pl.multiple_of(512 * n, 512), 512)]
            mine = jnp.where(lane == n // 2 * 32 + col // 32 * 2 + n % 2, sums, 0.0)
            pick = jnp.where(lane == 32 + col % 32, 1.0, 0.0).astype(bf16)
            return total + dot_nt(jnp.concatenate(three_parts(mine), axis=0), pick)
        total = lax.fori_loop(0, 8, gather, jnp.zeros((384, 128), f32))
        total = total[0:128] + total[128:256] + total[256:384]
        for n in range(8):
            flat[n, pl.ds(l, 16, stride=8), :] += total[16 * n:16 * n + 16]
    lane = lax.broadcasted_iota(jnp.int32, (1, 128), 1)
    for t in range(4):
        for q in range(4):
            tile = gbh[0:1, t * 256 + q // 2 * 128:t * 256 + q // 2 * 128 + 128]
            if q % 2 == 0:
                tile = jnp.concatenate([tile[:, 64:], tile[:, :64]], axis=1)
            tile = jnp.where(lane >= 64, tile, 0.0)
            for n in (2 * t, 2 * t + 1):
                flat[n, pl.ds(2 + q, 16, stride=8), :] += tile
    for n in range(8):
        flat[n, pl.ds(6, 16, stride=8), :] += jnp.where(lane == 64, hstat[2:3, 0:128], 0.0)
        b['sm'][n // 2, pl.ds(n % 2 * 2, 2)] = flat[n, pl.ds(0, 128), :].reshape(2, 4, 2, 8, 128)


def back_kernel(*refs):
    xin, xmid, pre_in, wc, act, vin, pat, tok_act, tok_slope = refs[:9]
    hl, hr, dx0, hstat, gbh, wt, wt_t, vec = refs[9:17]
    out_c, out_s, out_h, sm_own, tk_own = refs[17:22]
    dpre, dout, dres, x_act, x_vin, x_pat, x_dpre, x_dout, x_dres = refs[22:31]
    (per, b, big, little, x_hl, x_hr, gvec, gbch1, x_v, d_v, dv_v, do_v, w1_v, w2_v, pre_v, dp_v,
     ta_v, ts_v, send_sems, recv_sems, load_sems, sem, sem_w, sem_o, sem_t) = refs[31:]
    me = my_place()
    other = moved(me, 'k', 1)
    k, k2 = me['k'], 1 - me['k']
    barrier = pltpu.get_barrier_semaphore()
    for dim in 'xyz':
        for step in (1, 2, 3):
            pl.semaphore_signal(barrier, inc=1, device_id=device(moved(me, dim, step)), device_id_type=MESH)
    pl.semaphore_signal(barrier, inc=1, device_id=device(other), device_id_type=MESH)
    net = Net(send_sems, recv_sems)
    ring = {d: [moved(me, d, n)[d] for n in range(4)] for d in 'xyz'}
    peers = {(d, n): device(moved(me, d, n)) for d in 'xyz' for n in (1, 2, 3)}
    partner = device(other)
    half_at = pl.ds(pl.multiple_of(k * 512, 512), 512)
    half_to = pl.ds(pl.multiple_of(k2 * 512, 512), 512)
    swaps = {'act1': (act.at[1, k2], x_act.at[1]), 'act0': (act.at[0, k2], x_act.at[0]), 'vin1': (vin.at[1, k2], x_vin.at[1]),
             'vin0': (vin.at[0, k2], x_vin.at[0]), 'pat': (pat.at[k2], x_pat), 'dpre1': (dpre.at[1], x_dpre.at[1]),
             'dpre0': (dpre.at[0], x_dpre.at[0]), 'dout1': (dout.at[1], x_dout.at[1]), 'dout0': (dout.at[0], x_dout.at[0]),
             'dres': (dres, x_dres), 'hl': (hl.at[:, half_to], x_hl), 'hr': (hr, x_hr)}

    def swap(*names):
        for name in names:
            net.start(name, lambda name=name: (*swaps[name], partner))
    busy = {}

    def free(key):
        for name in busy.pop(key, ()):
            net.copy(name).wait_send()
            net.done.add(name)

    def loads(g):
        l = g // 2
        if g == STEM:
            wide, tall = (pat.at[k], x_pat, 1536), (dres, x_dres, CH)
        elif g % 2:
            wide, tall = (act.at[l, k], x_act.at[l], 2048), (dout.at[l], x_dout.at[l], CH)
        else:
            wide, tall = (dpre.at[l], x_dpre.at[l], CHH), (vin.at[l, k], x_vin.at[l], 512)
        out = []
        for n, (buf, (own, far, cols)) in enumerate(((big, wide), (little, tall))):
            out += [pltpu.make_async_copy(own, buf.at[0, :, pl.ds(0, cols)], load_sems.at[2 * n]),
                    pltpu.make_async_copy(far, buf.at[1, :, pl.ds(0, cols)], load_sems.at[2 * n + 1])]
        return out

    def product(u):
        g, c, slot = u.g, u.c, u.slot
        first = c == 2
        if first and g != HEAD:
            for copy in loads(g):
                copy.wait()
        if g == STEM and not first:
            return
        for v in (units if g == STEM else (u,)):
            if v.g == g:
                free(('C', v.c, v.slot))
        if g == HEAD:
            net.arrived(*NEEDS[g])
            for t in range(4):
                cols = pl.ds(256 * t, 256)
                prod = dot_tn(hl[:, half_at], hr[:, cols]) + dot_tn(x_hl[...], x_hr[:, cols])
                per[c]['C'][slot, t] = prod.astype(bf16).reshape(4, 4, 32, 256)
        elif g == STEM:
            slots = {v.c: v.slot for v in units if v.g == STEM}

            @pl.loop(0, 4)
            def _(z):
                rows = pl.ds(pl.multiple_of(z * 384, 384), 384)
                for t in range(4):
                    def right(s):
                        return jnp.concatenate([little[s, :, 128 * t:128 * t + 128], little[s, :, 512 + 128 * t:640 + 128 * t]], axis=1)
                    prod = dot_tn(big[0, :, rows], right(0)) + dot_tn(big[1, :, rows], right(1))
                    prod = prod.astype(bf16).reshape(4, 3, 32, 256)
                    for d in range(3):
                        per[d]['C'][slots[d], t, z, :, :, pl.ds(0, 256)] = prod[:, d]
        else:
            c0, n = COLS[c]

            @pl.loop(0, 4)
            def _(t):
                for h in range(2):
                    if g % 2:
                        left = pl.ds(pl.multiple_of(t * 512 + h * 256, 256), 256)
                        prod = dot_tn(big[0, :, left], little[0, :, c0:c0 + n]) + dot_tn(big[1, :, left], little[1, :, c0:c0 + n])
                    else:
                        right = pl.ds(pl.multiple_of(t * 1024 + c0, 128), n)
                        rows = slice(256 * h, 256 * h + 256)
                        prod = dot_tn(little[0, :, rows], big[0, :, right]) + dot_tn(little[1, :, rows], big[1, :, right])
                    per[c]['C'][slot, t, 2 * h:2 * h + 2] = prod.astype(bf16).reshape(2, 4, 32, n)

    class Unit:
        def __init__(self, g, c):
            self.g, self.c = g, c
            self.index = [u for u in UNITS if u[1] == c].index((g, c))
            self.slot = self.index % 2
            self.n = COLS[c][1] if g < N_CH else 256
            self.cols = pl.ds(0, self.n)
            self.buf = per[c]
            self.dims = ORDERS[c]
            self.rest = [d for d in 'xzy' if d != self.dims[0]]

        def cut(self, name, *at, rows=slice(None)):
            ref = self.buf[name]
            inner = [slice(None)] * (len(ref.shape) - len(at) - 2)
            return ref.at[(*at, *inner, rows, self.cols)]

        def block(self, p, rows):
            at = {d: EVERY for d in 'xzy'}
            at[self.dims[0]] = p
            return self.buf['C'].at[self.slot, at['x'], at['z'], at['y'], rows, self.cols]

        def share(self, phase, p, e, rows):
            if phase == 0:
                at = dict(zip(self.rest, e))
                at[self.dims[0]] = p
                return self.buf['C'][self.slot, at['x'], at['z'], at['y'], rows, self.cols].astype(f32)
            if phase == 1:
                at = (p, e[0]) if self.dims[1] == self.rest[0] else (e[0], p)
                return self.buf['S1'][(*at, rows, self.cols)]
            return self.buf['S2'][self.slot, p, rows, self.cols]

        def each(self, phase, body):
            if phase == 2:
                body(())
            elif phase == 1:
                pl.loop(0, 4)(lambda i: body((i,)))
            else:
                @pl.loop(0, 4)
                def _(i):
                    pl.loop(0, 4)(lambda j: body((i, j)))

        def send(self, tag, phase, src, dst, step):
            name = (self.g, self.c, tag, phase)
            net.start(name, lambda: (src(), dst(), peers[self.dims[phase], step]))
            return name

        def arrived(self, phase, *tags):
            net.arrived(*[(self.g, self.c, tag, phase) for tag in tags])

        def opposite(self, phase):
            places = ring[self.dims[phase]]
            low, high = pl.ds(0, 16), pl.ds(16, 16)
            if phase == 0:
                sources = [lambda: self.block(places[2], low), lambda: self.block(places[2], high),
                           lambda: self.block(places[1], high), lambda: self.block(places[3], low)]
            else:
                names = (f'opp{phase}', f'pr{phase}', f'pl{phase}')
                for name in names:
                    free((name, self.c))
                opp, right, left = (self.buf[name] for name in names)

                def body(e):
                    opp[(*e, slice(None), self.cols)] = self.share(phase, places[2], e, pl.ds(0, 32)).astype(bf16)
                    right[(*e, slice(None), self.cols)] = self.share(phase, places[1], e, high).astype(bf16)
                    left[(*e, slice(None), self.cols)] = self.share(phase, places[3], e, low).astype(bf16)
                self.each(phase, body)
                sources = [lambda: self.cut(names[0], rows=low), lambda: self.cut(names[0], rows=high),
                           lambda: self.cut(names[1]), lambda: self.cut(names[2])]
            targets = [lambda: self.cut(f'half0{phase}', self.index), lambda: self.cut(f'half1{phase}', self.index),
                       lambda: self.cut(f'froml{phase}', self.index, rows=high),
                       lambda: self.cut(f'fromr{phase}', self.index, rows=low)]
            sent = [self.send(tag, phase, src, dst, step)
                    for tag, src, dst, step in zip(('h0', 'h1', 'p0', 'p1'), sources, targets, (1, 3, 1, 3))]
            if phase == 0:
                busy['C', self.c, self.slot] = sent
            else:
                busy[names[0], self.c] = sent[:2]
                busy[names[1], self.c] = sent[2:3]
                busy[names[2], self.c] = sent[3:]

        def beside(self, phase):
            places = ring[self.dims[phase]]
            for half, step, name, dst in ((0, 1, 'rig', 'froml'), (1, 3, 'lef', 'fromr')):
                self.arrived(phase, f'h{half}')
                key = f'{name}{phase}'
                free((key, self.c))
                out, got = self.buf[key], self.buf[f'half{half}{phase}']
                rows = pl.ds(16 * half, 16)

                def body(e):
                    value = self.share(phase, places[step], e, rows) + got[(self.index, *e, slice(None), self.cols)].astype(f32)
                    out[(*e, slice(None), self.cols)] = value.astype(bf16)
                self.each(phase, body)
                busy[key, self.c] = [self.send(f'f{half}', phase, lambda key=key: self.cut(key),
                                               lambda dst=dst, rows=rows: self.cut(f'{dst}{phase}', self.index, rows=rows), step)]

        def total(self, phase):
            self.arrived(phase, 'p0', 'p1', 'f0', 'f1')
            p = ring[self.dims[phase]][0]

            def body(e):
                got = [self.buf[f'{name}{phase}'][(self.index, *e, slice(None), self.cols)].astype(f32)
                       for name in ('froml', 'fromr')]
                value = self.share(phase, p, e, pl.ds(0, 32)) + got[0] + got[1]
                if phase == 0:
                    self.buf['S1'][(*e, slice(None), self.cols)] = value
                elif phase == 1:
                    self.buf['S2'][(self.slot, *e, slice(None), self.cols)] = value
                elif self.g == STEM:
                    out_s[pl.ds(32 * self.c, 32), :] = value
                elif self.g == HEAD:
                    out_h[...] = value
                else:
                    out_c[self.g, :, pl.ds(*COLS[self.c])] = value
            self.each(phase, body)

        def run(self, stage):
            if stage == 0:
                product(self)
            elif stage == 7:
                self.total(2)
            elif stage % 2 == 0:
                self.beside(stage // 2 - 1)
            else:
                if stage > 1:
                    self.total(stage // 2 - 1)
                self.opposite(stage // 2)

    units = [Unit(g, c) for g, c in UNITS]
    bursts = dict(BACK_ORDER)

    def step(which, stage):
        if stage == 'L':
            net.arrived(*NEEDS[which])
            for copy in loads(which):
                copy.start()
        else:
            units[which].run(stage)

    def burst(name):
        for s in bursts.get(name, ()):
            step(*s)

    def during(name, count):
        def run(i):
            for n in range(1, count):
                if bursts.get(f'{name}{n}'):
                    pl.when(i == n)(functools.partial(burst, f'{name}{n}'))
        return run

    load = pltpu.make_async_copy(xmid.at[1], x_v.at[:, pl.ds(0, ROWS)], sem.at[0])
    load.start()
    mask = row_mask()
    rest = pl.ds(ROWS, XROWS - ROWS)
    put(d_v, rest, jnp.zeros((XROWS - ROWS, CH), f32))
    put(x_v, rest, jnp.zeros((XROWS - ROWS, CH), f32))
    gvec[...] = jnp.zeros_like(gvec)
    tk = b['tk']
    tk[...] = jnp.zeros_like(tk)

    @pl.loop(0, TOK)
    def _(s):
        put(d_v, pl.ds(pl.multiple_of(s * IMG, IMG), IMG), dx0[...])

    def add(row, value):
        gvec[row:row + 1, :] += jnp.sum(value, axis=0, keepdims=True)

    def add_token(n, value, start=0):
        tk[n, :, :, :, :, pl.ds(start, value.shape[1])] += value.reshape(4, 4, 2, 16, value.shape[1])

    for l in (1, 0):
        r = 1 + 5 * l
        for at, size in CHUNKS:
            d = get(d_v, pl.ds(at, size))
            add(r + 4, d)
            do_v[pl.ds(at, size), :] = d.astype(bf16)
        keep = pltpu.make_async_copy(do_v, dout.at[l], sem.at[1])
        keep.start()
        keep.wait()
        if l == 1:
            pl.semaphore_wait(barrier, 10)
            swap('hl', 'hr', 'dout1', 'act1', 'vin1', 'act0', 'vin0', 'pat')
        else:
            swap('dout0')
        burst(f'c{l}_0')
        run = during(f'c{l}_', NBLK)

        def blocks(i, slot):
            t, h = i // 2, i % 2
            part = pl.ds(pl.multiple_of(h * BLK, BLK), BLK)
            whole = pl.ds(pl.multiple_of(i * BLK, BLK), BLK)
            return [(wc.at[2 * l, t, :, :, :, :, part], w1_v.at[slot]), (wc.at[2 * l + 1, t, h], w2_v.at[slot]),
                    (pre_in.at[l, :, whole], pre_v.at[slot])]

        def outs(i, slot):
            return [(dp_v.at[slot], dpre.at[l, :, pl.ds(pl.multiple_of(i * BLK, BLK), BLK)])]

        def channel(i, slot):
            run(i)
            for n in range(2):
                cols = slice(256 * n, 256 * n + 256)
                d = dot_nt(do_v[...], w2_v[slot, 2 * n:2 * n + 2].reshape(256, CH)) * pre_v[slot, :, cols]
                gbch1[l:l + 1, pl.ds(pl.multiple_of(i * BLK + 256 * n, 256), 256)] = jnp.sum(d, axis=0, keepdims=True)
                dp_v[slot, :, cols] = d.astype(bf16)

            @pl.when(i == 0)
            def _():
                dv_v[...] = jnp.zeros_like(dv_v)
            for n in range(2):
                cols = slice(512 * n, 512 * n + 512)
                dv_v[:, cols] += dot_nt(dp_v[slot], w1_v[slot, n].reshape(512, BLK))
        for_blocks(Stream(sem_w, blocks, NBLK), channel, Stream(sem_o, outs, NBLK))
        swap(f'dpre{l}')
        burst(f'l{l}')
        load.wait()

        @pl.loop(0, ROWS // TPAD)
        def _(n):
            rows = pl.ds(pl.multiple_of(n * TPAD, TPAD), TPAD)
            std, inv = standardize(get(x_v, rows))
            d = dv_v[rows, :]
            add(r + 2, d * std)
            add(r + 3, d)
            put(d_v, rows, get(d_v, rows) + norm_grad(d, vec[r + 2:r + 3, :], std, inv))
        load = pltpu.make_async_copy(xin.at[l], x_v.at[:, pl.ds(0, ROWS)], sem.at[0])
        load.start()
        hidden = Stream(sem_t, lambda i, slot: [(tok_act.at[l, i], ta_v.at[slot]), (tok_slope.at[l, i], ts_v.at[slot])],
                        IMG * TOK_CUTS)
        hidden.start(0, 0)
        burst(f't{l}_0')
        load.wait()
        run = during(f't{l}_', IMG)

        @pl.loop(0, IMG)
        def _(m):
            run(m)
            std, inv = standardize(get(x_v, image(m)))
            a = with_bias_rows(std * vec[r:r + 1, :] + vec[r + 1:r + 2, :])
            d_mid = get(d_v, image(m))
            dm = d_mid.astype(bf16)
            parts = []
            for n in range(TOK_CUTS):
                cut, slot = m * TOK_CUTS + n, n % 2
                hidden.wait(cut, slot)
                if n + 1 < TOK_CUTS:
                    hidden.start(cut + 1, 1 - slot)
                else:
                    @pl.when(m + 1 < IMG)
                    def _():
                        hidden.start(cut + 1, 1 - slot)
                cols = slice(CH // TOK_CUTS * n, CH // TOK_CUTS * (n + 1))
                add_token(2 + l, dot_nt(ta_v[slot], dm[:, cols]))
                dh = dot_nn(wt[2 + l, :, 0:TPAD], dm[:, cols]) * ts_v[slot]
                add_token(l, jnp.sum(dh, axis=-1, keepdims=True), 64)
                dh = dh.astype(bf16)
                add_token(l, dot_nt(dh, a[:, cols]))
                parts.append(dot_nn(wt_t[l], dh))
            d = jnp.where(mask, jnp.concatenate(parts, axis=1), 0.0)
            add(r, d * std)
            add(r + 1, d)
            put(d_v, image(m), d_mid + norm_grad(d, vec[r:r + 1, :], std, inv))
        if l == 1:
            load = pltpu.make_async_copy(xmid.at[0], x_v.at[:, pl.ds(0, ROWS)], sem.at[0])
            load.start()
            burst('d0')

    burst('fin')
    for at, size in CHUNKS:
        d = get(d_v, pl.ds(at, size))
        add(0, d)
        do_v[pl.ds(at, size), :] = d.astype(bf16)
    keep = pltpu.make_async_copy(do_v, dres, sem.at[1])
    keep.start()
    keep.wait()
    swap('dres')
    small_pack(b, x_v, d_v, gvec, hstat, gbch1, gbh)

    last = []

    def put_small(name, src, dst, target):
        last.append(name)
        net.start(name, lambda: (src, dst, target))

    def small(n):
        x, z, y = (ring[d][0] for d in 'xzy')
        net.arrived(*last)
        last.clear()
        if n == 0:
            put_small(('sm', 0), b['sm'].at[:, :, :, k2], b['sm1'], partner)
            put_small(('tk', 0), b['tk'].at[:, :, :, k2], b['tk1'], partner)
        elif n == 1:
            b['sm1'][...] += b['sm'][:, :, :, k]
            b['tk1'][...] += b['tk'][:, :, :, k]
            for s in (1, 2, 3):
                put_small(('sm', 1, s), b['sm1'].at[ring['x'][s]], b['sm2'].at[s - 1], peers['x', s])
                put_small(('tk', 1, s), b['tk1'].at[:, ring['z'][s]], b['tk2'].at[s - 1], peers['z', s])
        elif n == 2:
            b['sm_s1'][...] = b['sm1'][x] + b['sm2'][0] + b['sm2'][1] + b['sm2'][2]
            b['tk_s1'][...] = b['tk1'][:, z] + b['tk2'][0] + b['tk2'][1] + b['tk2'][2]
            for s in (1, 2, 3):
                put_small(('sm', 2, s), b['sm_s1'].at[ring['z'][s]], b['sm3'].at[s - 1], peers['z', s])
                put_small(('tk', 2, s), b['tk_s1'].at[:, ring['y'][s]], b['tk3'].at[s - 1], peers['y', s])
        elif n == 3:
            b['sm_s2'][...] = b['sm_s1'][z] + b['sm3'][0] + b['sm3'][1] + b['sm3'][2]
            b['tk_s2'][...] = b['tk_s1'][:, y] + b['tk3'][0] + b['tk3'][1] + b['tk3'][2]
            for s in (1, 2, 3):
                put_small(('sm', 3, s), b['sm_s2'].at[ring['y'][s]], b['sm4'].at[s - 1], peers['y', s])
                put_small(('tk', 3, s), b['tk_s2'], b['tk4'].at[s - 1], peers['x', s])
        else:
            sm_own[...] = b['sm_s2'][y] + b['sm4'][0] + b['sm4'][1] + b['sm4'][2]
            ordered = []
            for place in range(4):
                value = b['tk_s2'][...]
                for s in (1, 2, 3):
                    value = jnp.where(ring['x'][4 - s] == place, b['tk4'][s - 1], value)
                ordered.append(value)
            tk_own[...] = (ordered[0] + ordered[1]) + (ordered[2] + ordered[3])

    tail = bursts.get('end', ())
    small(0)
    for n, s in enumerate(tail):
        step(*s)
        if n in (8, 18, 28, 38):
            small(1 + (8, 18, 28, 38).index(n))
    net.finish()
    assert len(net.builds) <= BACK_COPIES, len(net.builds)


def back(*operands):
    a, v = pl.BlockSpec(memory_space=pl.ANY), pl.BlockSpec(memory_space=pltpu.VMEM)
    S, V, DMA = jax.ShapeDtypeStruct, pltpu.VMEM, pltpu.SemaphoreType.DMA
    return pl.pallas_call(
        back_kernel, name='back',
        in_specs=[a] * 9 + [v] * 8, out_specs=[v] * 5 + [a] * 9,
        out_shape=[S((N_CH, 32, 1024), f32), S((96, 256), f32), S((32, 256), f32), S((8, 128), f32), S((4, 16, 128), f32),
                   S((2, ROWS, CHH), bf16), S((2, ROWS, CH), bf16), S((ROWS, CH), bf16), S((2, ROWS, 2048), bf16),
                   S((2, ROWS, 512), bf16), S((ROWS, 1536), bf16), S((2, ROWS, CHH), bf16), S((2, ROWS, CH), bf16),
                   S((ROWS, CH), bf16)],
        scratch_shapes=[reduce_scratch(), small_scratch(), V((2, ROWS, CHH), bf16), V((2, ROWS, CH), bf16), V((IMG, 512), bf16),
                        V((IMG, CH), bf16), V((16, CH), f32), V((2, CHH), f32), V((CH // 128, XROWS, 128), f32),
                        V((CH // 128, XROWS, 128), f32), V((ROWS, CH), f32), V((ROWS, CH), bf16), V((2, 2, 4, 4, 32, BLK), bf16),
                        V((2, 4, 4, 32, CH), bf16), V((2, ROWS, BLK), f32), V((2, ROWS, BLK), bf16), V((2, TOKH, CH // TOK_CUTS), bf16),
                        V((2, TOKH, CH // TOK_CUTS), f32), DMA((BACK_COPIES,)), DMA((BACK_COPIES,)), DMA((4,)), DMA((2,)), DMA((2, 3)),
                        DMA((2, 1)), DMA((2, 2))],
        compiler_params=pltpu.CompilerParams(collective_id=1, has_side_effects=True, vmem_limit_bytes=64 * 1024 * 1024 - 65536),
        cost_estimate=pl.CostEstimate(flops=120_000_000_000, bytes_accessed=200_000_000, transcendentals=0),
    )(*operands)


def finish_kernel(c, stem, head, sm, tk, loss, o_stem, o_bstem, o_ln1g, o_ln1b, o_wt1, o_bt1, o_wt2, o_ln2g, o_ln2b, o_ch1,
                  o_bch1, o_ch2, o_bch2, o_lnfg, o_lnfb, o_head, o_bhead):
    def core_last(value, pick):
        got = dot_nt(jnp.concatenate(three_parts(value), axis=0), pick)
        n = value.shape[0]
        return got[0:n] + got[n:2 * n] + got[2 * n:3 * n]
    pick = core_first(1024, 1024, 32)
    for l in range(2):
        o_ch1[l] = core_last(c[2 * l], pick)
        o_ch2[l] = core_last(c[2 * l + 1], pick)
    o_stem[...] = core_last(stem[...], core_first(256, 256, 32))
    o_head[...] = head[:, 0:250]
    own = sm[...]
    turned = jnp.concatenate([own, jnp.zeros((120, 128), f32)], axis=0).T
    for ref, n in ((o_bstem, 0), (o_lnfg, 11), (o_lnfb, 12)):
        ref[...] = turned[n, 0:8]
    for n, ref in enumerate((o_ln1g, o_ln1b, o_ln2g, o_ln2b, o_bch2)):
        for l in range(2):
            ref[pl.ds(l, 1), :] = turned[1 + 5 * l + n:2 + 5 * l + n, 0:8]
    o_bch1[...] = own[0:2, 32:64]
    classes = jnp.concatenate([own[2 + q:3 + q, 64:128] for q in range(4)], axis=1)
    o_bhead[...] = classes[0, 0:250]
    loss[...] = own[6:7, 64:65] * (1.0 / 1024)
    for l in range(2):
        o_wt1[l] = tk[l, :, 0:TOK]
        o_wt2[l] = tk[2 + l, :, 0:TOK]
        tall = jnp.concatenate([tk[l], jnp.zeros((112, 128), f32)], axis=0).T
        o_bt1[pl.ds(l, 1), :] = tall[64:65, 0:16]


def finish(*operands):
    S = jax.ShapeDtypeStruct
    v = pl.BlockSpec(memory_space=pltpu.VMEM)
    return pl.pallas_call(
        finish_kernel, name='finish', in_specs=[v] * 5, out_specs=[v] * 18,
        out_shape=[S((1, 1), f32), S((96, 256), f32), S((8,), f32), S((2, 8), f32), S((2, 8), f32), S((2, 16, TOK), f32),
                   S((2, 16), f32), S((2, 16, TOK), f32), S((2, 8), f32), S((2, 8), f32), S((2, 32, 1024), f32), S((2, 32), f32),
                   S((2, 32, 1024), f32), S((2, 8), f32), S((8,), f32), S((8,), f32), S((32, 250), f32), S((250,), f32)],
    )(*operands)

CHANNEL_AXES = ('tp', 'fsdp')


def weight_specs():
    vec_spec = P(CHANNEL_AXES)
    layer_vec = P(None, CHANNEL_AXES)
    return (P('fsdp', 'tp'), vec_spec, layer_vec, layer_vec, P(None, None, 'fsdp'), P(None, 'fsdp'),
            P(None, 'fsdp', None), layer_vec, layer_vec, P(None, 'fsdp', 'tp'), layer_vec,
            P(None, CHANNEL_AXES, None), layer_vec, vec_spec, vec_spec, P('fsdp', 'tp'), P('tp'))


def solution(mesh):
    def step(patches, labels, w_stem, b_stem, ln1_g, ln1_b, w_tok1, b_tok1, w_tok2,
             ln2_g, ln2_b, w_ch1, b_ch1, w_ch2, b_ch2, lnf_g, lnf_b, w_head, b_head):
        wc, pat, xin, xmid, vin, pre, act, tok_act, tok_slope, hl, hr, dx0, hstat, gbh, vec, wt, wt_t = front(
            labels, patches.transpose(1, 0, 2), w_stem, w_ch1, w_ch2, w_head, w_tok1.transpose(0, 2, 1), w_tok2, b_tok1, b_ch1,
            b_head, b_stem, ln1_g, ln1_b, ln2_g, ln2_b, b_ch2, lnf_g, lnf_b)
        sums = back(xin, xmid, pre, wc, act, vin, pat, tok_act, tok_slope, hl, hr, dx0, hstat, gbh, wt, wt_t, vec)[:5]
        loss, g_s, g_bs, g_1g, g_1b, g_t1, g_bt, g_t2, g_2g, g_2b, g_c1, g_b1, g_c2, g_b2, g_fg, g_fb, g_h, g_bh = finish(*sums)
        return (loss.reshape(()), g_s, g_bs, g_1g, g_1b, g_t1.transpose(0, 2, 1), g_bt, g_t2, g_2g, g_2b, g_c1, g_b1, g_c2, g_b2,
                g_fg, g_fb, g_h, g_bh)

    specs = weight_specs()
    return jax.shard_map(step, mesh=mesh, in_specs=(P('fsdp', None, None), P('fsdp')) + specs,
                         out_specs=(P(),) + specs, check_vma=False)
```

```python
import functools

import jax
import jax.numpy as jnp
from jax import lax
from jax.experimental import pallas as pl
from jax.experimental.pallas import tpu as pltpu
from jax.sharding import PartitionSpec as P

MESH = pl.DeviceIdType.MESH
ORDERS = (('x', 'y', 'z'), ('y', 'z', 'x'), ('z', 'x', 'y'))
COLS = ((0, 384), (384, 384), (768, 256))
N_CH = 4
STEM, HEAD = 4, 5
bf16, f32 = jnp.bfloat16, jnp.float32


def my_place():
    f = lax.axis_index('fsdp')
    return {'x': lax.axis_index('tp'), 'z': f // 8, 'y': (f // 2) % 4, 'k': f % 2}


def moved(place, dim, step):
    new = dict(place)
    new[dim] = 1 - place['k'] if dim == 'k' else (place[dim] + step) % 4
    return new


def device(place):
    return {'tp': place['x'], 'fsdp': (place['z'] * 4 + place['y']) * 2 + place['k']}


EPS = 1e-6
TOK, TPAD = 49, 56
IMG = 8
ROWS, XROWS = IMG * TOK, IMG * TPAD
CHUNKS = ((0, 112), (112, 112), (224, 112), (336, 56))
CH, TOKH, CHH = 1024, 512, 4096
BLK = 512
NBLK = CHH // BLK
GELU_C, GELU_A = 0.7978845608028654, 0.044715


def dot_nn(a, b):
    return lax.dot_general(a, b, (((1,), (0,)), ((), ())), preferred_element_type=f32)


def dot_nt(a, b):
    return lax.dot_general(a, b, (((1,), (1,)), ((), ())), preferred_element_type=f32)


def dot_tn(a, b):
    return lax.dot_general(a, b, (((0,), (0,)), ((), ())), preferred_element_type=f32)


def gelu_both(x):
    sq = x * x
    half = 0.5 * jnp.tanh(x * (GELU_C + (GELU_C * GELU_A) * sq))
    rise = 0.5 + half
    value = x * rise
    return value, rise + value * (0.5 - half) * (2.0 * GELU_C + (6.0 * GELU_C * GELU_A) * sq)


def standardize(x):
    mean = jnp.mean(x, axis=-1, keepdims=True)
    cent = x - mean
    inv = lax.rsqrt(jnp.mean(cent * cent, axis=-1, keepdims=True) + EPS)
    return cent * inv, inv


def norm_grad(d, gain, std, inv):
    gs = d * gain
    m0 = jnp.mean(gs, axis=-1, keepdims=True)
    m1 = jnp.mean(gs * std, axis=-1, keepdims=True)
    return inv * (gs - m0 - std * m1)


def row_mask(rows=TPAD):
    return lax.broadcasted_iota(jnp.int32, (rows, 1), 0) < TOK


def image(b):
    return pl.ds(b, TPAD, stride=IMG)


def get(ref, rows):
    return jnp.concatenate([ref[n, rows, :] for n in range(CH // 128)], axis=1)


def put(ref, rows, value):
    for n in range(CH // 128):
        ref[n, rows, :] = value[:, 128 * n:128 * (n + 1)]


class Stream:
    def __init__(self, sem, copies, count):
        self.sem, self.copies, self.count = sem, copies, count

    def make(self, i, slot):
        return [pltpu.make_async_copy(src, dst, self.sem.at[slot, n]) for n, (src, dst) in enumerate(self.copies(i, slot))]

    def start(self, i, slot):
        for copy in self.make(i, slot):
            copy.start()

    def wait(self, i, slot):
        for copy in self.make(i, slot):
            copy.wait()


def for_blocks(stream, body, out=None):
    n = stream.count
    stream.start(0, 0)

    @pl.loop(0, n)
    def _(i):
        slot = i % 2
        stream.wait(i, slot)

        @pl.when(i + 1 < n)
        def _():
            stream.start(i + 1, 1 - slot)
        if out is not None:
            @pl.when(i >= 2)
            def _():
                out.wait(i - 2, slot)
        body(i, slot)
        if out is not None:
            out.start(i, slot)
    if out is not None:
        out.wait(n - 2, n % 2)
        out.wait(n - 1, 1 - n % 2)


TOK_CUTS = 4
FRONT_COPIES = 270
EARLY = [('stem', c) for c in range(3)] + [('ch', c, p) for p in 'ab' for c in range(3)] + [('head', 2)]
PARTS = {'a': pl.ds(0, 2), 'b': pl.ds(2, 2)}
LATE = [('stem', c, None) for c in range(3)] + [('ch', c, g) for g in range(N_CH) for c in range(3)] + [('head', 2, None)]
UNIT_GROUP = {('stem', None): 0, ('ch', 0): 1, ('ch', 1): 2, ('ch', 2): 3, ('ch', 3): 4, ('head', None): 5}
EVERY = pl.ds(0, 4)
FRONT_ORDER = (
    ('prep', (('M0', ('sm',)), ('M0', ('tk',)), ('A0', ('stem', 0)), ('A0', ('stem', 1)), ('A0', ('stem', 2)),
        ('A0', ('ch', 0, 'a')), ('A0', ('ch', 0, 'b')), ('A0', ('ch', 1, 'a')), ('A0', ('ch', 1, 'b')),
        ('A0', ('ch', 2, 'a')), ('A0', ('ch', 2, 'b')), ('A0', ('head', 2)),)),
    ('unpack', (('M1', ('sm',)), ('M1', ('tk',)), ('A', ('stem', 0)), ('A', ('stem', 1)), ('A', ('stem', 2)),
        ('A', ('ch', 0, 'a')), ('A', ('ch', 1, 'a')), ('A', ('ch', 2, 'a')), ('B', ('stem', 0)), ('M2', ('sm',)),
        ('B', ('stem', 1)), ('M2', ('tk',)), ('B', ('stem', 2)), ('C', ('stem', 0)), ('M3', ('sm',)), ('C', ('stem', 2)),
        ('D', ('stem', 0, None)), ('B', ('ch', 0, 'a')), ('C', ('stem', 1)), ('B', ('ch', 1, 'a')), ('B', ('ch', 2, 'a')),
        ('A', ('head', 2)),)),
    ('stem0', (('D', ('stem', 2, None)), ('C', ('ch', 2, 'a')), ('C', ('ch', 0, 'a')), ('E', ('stem', 0, None)),
        ('D', ('stem', 1, None)), ('B', ('head', 2)), ('C', ('ch', 1, 'a')), ('E', ('stem', 2, None)),
        ('F', ('stem', 0, None)), ('A', ('ch', 0, 'b')), ('A', ('ch', 1, 'b')), ('A', ('ch', 2, 'b')),
        ('E', ('stem', 1, None)), ('D', ('ch', 2, 0)), ('D', ('ch', 0, 0)), ('D', ('ch', 0, 1)), ('D', ('ch', 2, 1)),
        ('D', ('ch', 1, 0)), ('F', ('stem', 2, None)), ('D', ('ch', 1, 1)), ('B', ('ch', 0, 'b')), ('B', ('ch', 2, 'b')),
        ('B', ('ch', 1, 'b')), ('F', ('stem', 1, None)), ('E', ('ch', 2, 0)),)),
    ('stem2', (('E', ('ch', 0, 0)), ('C', ('head', 2)),)),
    ('tok0_0', (('E', ('ch', 1, 0)), ('E', ('ch', 2, 1)),)),
    ('tok0_2', (('C', ('ch', 0, 'b')),)),
    ('tok0_3', (('E', ('ch', 0, 1)),)),
    ('tok0_4', (('F', ('ch', 2, 0)), ('E', ('ch', 1, 1)),)),
    ('tok0_5', (('C', ('ch', 1, 'b')), ('F', ('ch', 2, 1)),)),
    ('tok0_6', (('C', ('ch', 2, 'b')), ('D', ('head', 2, None)), ('D', ('ch', 0, 2)), ('D', ('ch', 0, 3)),)),
    ('tok0_7', (('F', ('ch', 0, 0)),)),
    ('ln0', (('F', ('ch', 1, 0)),)),
    ('ch0_0', (('F', ('ch', 0, 1)), ('F', ('ch', 1, 1)), ('E', ('head', 2, None)), ('D', ('ch', 1, 2)), ('D', ('ch', 1, 3)),
        ('D', ('ch', 2, 2)), ('D', ('ch', 2, 3)),)),
    ('ch0_2', (('F', ('head', 2, None)),)),
    ('ch0_4', (('E', ('ch', 0, 2)),)),
    ('ch0_6', (('E', ('ch', 1, 2)), ('E', ('ch', 2, 2)),)),
    ('tok1_1', (('E', ('ch', 0, 3)), ('E', ('ch', 2, 3)),)),
    ('tok1_2', (('F', ('ch', 2, 2)), ('E', ('ch', 1, 3)),)),
    ('tok1_3', (('F', ('ch', 0, 2)),)),
    ('tok1_5', (('F', ('ch', 1, 2)), ('F', ('ch', 2, 3)), ('F', ('ch', 0, 3)),)),
    ('tok1_7', (('F', ('ch', 1, 3)),)),
)


class Net:
    def __init__(self, send_sems, recv_sems):
        self.send_sems, self.recv_sems, self.names, self.builds, self.done = send_sems, recv_sems, {}, [], set()

    def copy(self, name):
        n = self.names[name]
        src, dst, target = self.builds[n]()
        return pltpu.make_async_remote_copy(src_ref=src, dst_ref=dst, send_sem=self.send_sems.at[n],
                                            recv_sem=self.recv_sems.at[n], device_id=target, device_id_type=MESH)

    def start(self, name, build):
        self.names[name] = len(self.builds)
        self.builds.append(build)
        self.copy(name).start()

    def arrived(self, *names):
        for name in names:
            self.copy(name).wait_recv()

    def finish(self):
        for name in self.names:
            if name not in self.done:
                self.copy(name).wait_send()


def core_first(size, cols, each):
    half = cols // 2
    row = lax.broadcasted_iota(jnp.int32, (size, size), 0)
    col = lax.broadcasted_iota(jnp.int32, (size, size), 1)
    source = col % half // each * (2 * each) + col // half * each + col % each
    return jnp.where(row == source, 1.0, 0.0).astype(bf16)


def three_parts(x):
    hi = x.astype(bf16)
    rest = x - hi.astype(f32)
    mid = rest.astype(bf16)
    return hi, mid, (rest - mid.astype(f32)).astype(bf16)


def with_bias_rows(a):
    row = lax.broadcasted_iota(jnp.int32, (TPAD, 1), 0)
    return jnp.where(row < TOK, a, jnp.where(row < TOK + 3, 1.0, 0.0)).astype(bf16)


def front_kernel(labels, patches, w_stem, w_ch1, w_ch2, w_head, w_tok1, w_tok2, b_tok1, b_ch1, b_head, b_stem, ln1_g, ln1_b,
                 ln2_g, ln2_b, b_ch2, lnf_g, lnf_b,
                 wc, pat_out, xin, xmid, vout, pre_out, act_out, tok_act, tok_slope, hl, hr, dx0, hstat, gbh, vec, wt, wt_t,
                 pc, ps, ph, tk_f, tk_p, sm_p, bh_p, ws, wh, tk_v, sm_v, sm_2, bh_v, bch1,
                 turn, p_v, pk_v, x_v, v_v, w1_v, w2_v, pre_v, act_v, g_v, s_v,
                 send_sems, recv_sems, sem, sem_w, sem_o, sem_x, sem_t):
    me = my_place()
    other = moved(me, 'k', 1)
    load_p = pltpu.make_async_copy(patches.at[:, pl.ds(pl.multiple_of(me['x'] * IMG, IMG), IMG)], p_v, sem.at[0])
    load_p.start()

    barrier = pltpu.get_barrier_semaphore()
    for dim in 'xyz':
        for step in (1, 2, 3):
            pl.semaphore_signal(barrier, inc=1, device_id=device(moved(me, dim, step)), device_id_type=MESH)
    pl.semaphore_signal(barrier, inc=1, device_id=device(other), device_id_type=MESH)

    stem = dot_nn(w_stem[...].astype(bf16), core_first(256, 256, 32)).astype(bf16)
    ps[0], ps[1] = stem[:, 0:128], stem[:, 128:256]
    pick = core_first(1024, 1024, 32)
    for l in range(2):
        pc[2 * l] = dot_nn(w_ch1[l].astype(bf16), pick).astype(bf16)
        pc[2 * l + 1] = dot_nn(w_ch2[l].astype(bf16), pick).astype(bf16)
    ph[...] = jnp.zeros_like(ph)
    ph[:, pl.ds(0, 250)] = w_head[...].astype(bf16)
    turn[...] = jnp.zeros_like(turn)
    for n, ref in ((0, b_stem), (11, lnf_g), (12, lnf_b)):
        turn[n, pl.ds(0, 8)] = ref[...]
    for n, ref in enumerate((ln1_g, ln1_b, ln2_g, ln2_b, b_ch2)):
        for l in range(2):
            turn[pl.ds(1 + 5 * l + n, 1), pl.ds(0, 8)] = ref[pl.ds(l, 1), :]
    turn[pl.ds(16, 2), pl.ds(0, 16)] = b_tok1[...]
    turned = turn[...].T
    tk_f[...] = jnp.zeros_like(tk_f)
    for l in range(2):
        tk_f[l, :, pl.ds(0, TOK)] = w_tok1[l]
        tk_f[2 + l, :, pl.ds(0, TOK)] = w_tok2[l]
        for n, part in enumerate(three_parts(turned[0:16, 16 + l:17 + l])):
            tk_f[l, :, pl.ds(TOK + n, 1)] = part.astype(f32)
    tk_p[...] = tk_f[...].astype(bf16)
    sm_p[...] = jnp.zeros_like(sm_p)
    sm_p[:, pl.ds(0, 16)] = turned[0:8, 0:16]
    sm_p[pl.ds(0, 2), pl.ds(32, 32)] = b_ch1[...]
    bh_p[...] = jnp.full_like(bh_p, -1e30)
    bh_p[0, pl.ds(0, 250)] = b_head[...]

    net = Net(send_sems, recv_sems)
    core = me['k']
    ring = {d: [moved(me, d, n)[d] for n in range(4)] for d in 'xyz'}
    columns = [pl.ds(pl.multiple_of(x * 256, 256), 256) for x in ring['x']]
    stem_columns = [pl.ds(pl.multiple_of(x * 128, 128), 128) for x in ring['x']]
    peers = {(d, n): device(moved(me, d, n)) for d in 'xyz' for n in (1, 2, 3)}
    partner = device(other)
    here = {'x': 0, 'y': 0, 'z': 0}

    def view(unit, block, half=None):
        kind, colour = unit[:2]
        x, z, y = (EVERY if block[d] is None else ring[d][block[d]] for d in 'xzy')
        r0, rn = (0, 32) if half is None else (16 * half, 16)
        if kind == 'ch':
            c0, cn = COLS[colour]
            g = PARTS.get(unit[2], unit[2])
            return wc.at[g, x, core, z, y, pl.ds(r0, rn), pl.ds(c0, cn)]
        if kind == 'stem':
            cols = pl.ds(0, 512) if x is EVERY else stem_columns[block['x']]
            return ws.at[:, z, y, core, pl.ds(32 * colour + r0, rn), cols]
        cols = pl.ds(0, CH) if x is EVERY else columns[block['x']]
        return wh.at[core, z, y, pl.ds(r0, rn), cols]

    def piece(unit):
        kind, colour = unit[:2]
        if kind == 'ch':
            return pc.at[PARTS[unit[2]], :, pl.ds(*COLS[colour])]
        return ps.at[:, pl.ds(32 * colour, 32), :] if kind == 'stem' else ph.at[:, :]

    def exchange(unit, tag, dim, block):
        for side, step in (('l', 1), ('r', 3)):
            def build(step=step):
                part = view(unit, block)
                return (piece(unit) if tag == '1' else part), part, peers[dim, step]
            net.start((unit, tag, side), build)

    def forward_half(unit, tag, dim, block):
        for half, (origin, target, side) in enumerate(((3, 1, 'l'), (1, 3, 'r'))):
            def build(half=half, origin=origin, target=target):
                part = view(unit, {**block, dim: origin}, half)
                return part, part, peers[dim, target]
            net.start((unit, tag, side), build)

    def swap(unit, tag, block):
        def build():
            part = view(unit, block)
            return part, part, partner
        net.start((unit, tag), build)

    own = pltpu.make_async_copy(pc, wc.at[:, me['x'], me['k'], me['z'], me['y']], sem.at[1])
    own.start()
    mine = pl.ds(pl.multiple_of(me['x'] * 256, 256), 256)
    for n in range(2):
        ws[n, me['z'], me['y'], me['k'], :, stem_columns[0]] = ps[n]
    wh[me['k'], me['z'], me['y'], :, mine] = ph[...]
    sm_v[me['x'], me['z'], me['y'], me['k']] = sm_p[...]
    tk_v[:, me['z'], me['y'], me['k']] = tk_p[...]
    bh_v[:, mine] = bh_p[...]
    own.wait()
    pl.semaphore_wait(barrier, 10)

    def small(kind, n):
        dims = 'xyz' if kind == 'sm' else 'yz'
        at = {d: EVERY if d in dims[:n] else ring[d][0] for d in 'xyz'}

        def part():
            if kind == 'sm':
                return sm_v.at[at['x'], at['z'], at['y'], core]
            return tk_v.at[:, at['z'], at['y'], core]
        if n > 0:
            net.arrived(*[(kind, n - 1, s) for s in (1, 2, 3)])
        if n < len(dims):
            for s in (1, 2, 3):
                net.start((kind, n, s), lambda s=s: (part(), part(), peers[dims[n], s]))
            if kind == 'sm' and n == 0:
                def head_bias():
                    return bh_v.at[:, columns[0]]
                for s in (1, 2, 3):
                    net.start(('bh', s), lambda s=s: (head_bias(), head_bias(), peers['x', s]))
        else:
            net.start((kind, 'k'), lambda: (part(), part(), partner))

    def step(name, unit):
        if name[0] == 'M':
            small(unit[0], int(name[1]))
            return
        d1, d2, d3 = ORDERS[unit[1]]
        early = unit[:2] if unit[0] != 'ch' or unit[2] in PARTS else ('ch', unit[1], 'a' if unit[2] < 2 else 'b')
        plane = {**here, d1: None, d2: None}
        if name == 'A0':
            exchange(unit, '1', d1, here)
        elif name == 'A':
            net.arrived((unit, '1', 'l'), (unit, '1', 'r'))
            forward_half(unit, '1h', d1, here)
        elif name == 'B':
            net.arrived((unit, '1h', 'l'), (unit, '1h', 'r'))
            exchange(unit, '2', d2, {**here, d1: None})
        elif name == 'C':
            net.arrived((unit, '2', 'l'), (unit, '2', 'r'))
            forward_half(unit, '2h', d2, {**here, d1: None})
        elif name == 'D':
            if early not in planes:
                planes.add(early)
                net.arrived((early, '2h', 'l'), (early, '2h', 'r'))
            exchange(unit, '3', d3, plane)
            swap(unit, 'k0', plane)
        elif name == 'E':
            net.arrived((unit, '3', 'l'), (unit, '3', 'r'))
            forward_half(unit, '3h', d3, plane)
            for n in (1, 3):
                swap(unit, f'k{n}', {**plane, d3: n})
        else:
            net.arrived((unit, '3h', 'l'), (unit, '3h', 'r'))
            swap(unit, 'k2', {**plane, d3: 2})

    planes = set()
    awaited = set()

    def need(group):
        for u in LATE:
            if UNIT_GROUP[u[0], u[2]] <= group and u not in awaited:
                awaited.add(u)
                net.arrived(*[(u, f'k{n}') for n in range(4)])

    bursts = {name: steps for name, steps in FRONT_ORDER}

    def burst(name):
        for s in bursts.get(name, ()):
            step(*s)

    def during(name, count):
        def run(i):
            for n in range(1, count):
                if bursts.get(f'{name}{n}'):
                    pl.when(i == n)(functools.partial(burst, f'{name}{n}'))
        return run

    burst('prep')
    load_p.wait()
    pick = core_first(768, 768, 96)
    for g in range(4):
        part = dot_nn(p_v[:, :, pl.ds(768 * g, 768)].reshape(ROWS, 768), pick).astype(bf16)
        for n in range(2):
            pk_v[n, :, pl.ds(384 * g, 384)] = part[:, 384 * n:384 * n + 384]
    keep_p = pltpu.make_async_copy(pk_v, pat_out, sem.at[0])
    keep_p.start()

    burst('unpack')
    net.arrived(('sm', 'k'), ('tk', 'k'), ('bh', 1), ('bh', 2), ('bh', 3))
    sm_2[...] = sm_v[...].reshape(1024, 128)
    for n in range(8):
        tile = jnp.concatenate([sm_2[pl.ds((n % 4 * 4 + i) * 64 + n // 4 * 32, 32), :] for i in range(4)], axis=0)
        vec[:, pl.ds(128 * n, 128)] = tile.T[0:16, :]
    wt[...] = tk_v[...].reshape(4, TOKH, 128)
    for n in range(4):
        wt_t[n] = wt[n].astype(f32).T[0:TPAD].astype(bf16)
    for l in range(2):
        rows = jnp.concatenate(three_parts(sm_2[pl.ds(l, 128, stride=8), :]), axis=0)

        @pl.loop(0, 8)
        def _(n):
            lane = lax.broadcasted_iota(jnp.int32, (128, 512), 0)
            col = lax.broadcasted_iota(jnp.int32, (128, 512), 1)
            pick = jnp.where(lane == 32 + col % 32, 1.0, 0.0).astype(bf16)
            spread = dot_nn(rows, pick)
            value = spread[0:128] + spread[128:256] + spread[256:384]
            mine = lane == n // 2 * 32 + col // 32 * 2 + n % 2
            bch1[l:l + 1, pl.ds(pl.multiple_of(n * 512, 512), 512)] = jnp.sum(jnp.where(mine, value, 0.0), axis=0, keepdims=True)

    burst('stem0')
    need(0)
    run = during('stem', 4)
    put(x_v, pl.ds(ROWS, XROWS - ROWS), jnp.zeros((XROWS - ROWS, CH), f32))

    @pl.loop(0, 4)
    def _(i):
        run(i)
        cols = pl.ds(pl.multiple_of(i * 256, 256), 256)
        w = ws[i // 2, :, :, :, :, pl.ds(pl.multiple_of(i % 2 * 256, 256), 256)].reshape(3072, 256)
        value = dot_nn(p_v[...].reshape(ROWS, 3072), w) + vec[0:1, cols]
        for n in range(2):
            x_v[2 * i + n, pl.ds(0, ROWS), :] = value[:, 128 * n:128 * (n + 1)]

    wc_all = wc

    def add_rows(value):
        for n in range(CH // 128):
            x_v[n, pl.ds(0, ROWS), :] += value[:, 128 * n:128 * (n + 1)]

    for l in range(2):
        r = 1 + 5 * l
        burst(f'tok{l}_0')
        run = during(f'tok{l}_', IMG)
        save_in = pltpu.make_async_copy(x_v.at[:, pl.ds(0, ROWS)], xin.at[l], sem_x.at[0])
        save_in.start()
        save_in.wait()
        hidden = Stream(sem_t, lambda i, slot: [(g_v.at[slot], tok_act.at[l, pl.ds(i * TOK_CUTS, TOK_CUTS)]),
                                                (s_v.at[slot], tok_slope.at[l, pl.ds(i * TOK_CUTS, TOK_CUTS)])], IMG)

        @pl.loop(0, IMG)
        def _(b):
            run(b)
            x = get(x_v, image(b))
            std, _ = standardize(x)
            a = with_bias_rows(std * vec[r:r + 1, :] + vec[r + 1:r + 2, :])
            spare = b % 2

            @pl.when(b >= 2)
            def _():
                hidden.wait(b - 2, spare)
            width = CH // TOK_CUTS
            parts = []
            for n in range(TOK_CUTS):
                value, slope = gelu_both(dot_nn(wt[l, :, 0:TPAD], a[:, width * n:width * (n + 1)]))
                g_v[spare, n] = value.astype(bf16)
                s_v[spare, n] = slope
                parts.append(dot_nn(wt_t[2 + l], g_v[spare, n]))
            hidden.start(b, spare)
            put(x_v, image(b), x + jnp.concatenate(parts, axis=1))
        hidden.wait(IMG - 2, 0)
        hidden.wait(IMG - 1, 1)
        save_mid = pltpu.make_async_copy(x_v.at[:, pl.ds(0, ROWS)], xmid.at[l], sem_x.at[0])
        save_mid.start()
        burst(f'ln{l}')

        for at, size in CHUNKS:
            std, _ = standardize(get(x_v, pl.ds(at, size)))
            v_v[pl.ds(at, size), :] = (std * vec[r + 2:r + 3, :] + vec[r + 3:r + 4, :]).astype(bf16)
        save_v = [pltpu.make_async_copy(v_v.at[:, pl.ds(512 * n, 512)], vout.at[l, n], sem_x.at[1 + n]) for n in range(2)]
        for copy in save_v:
            copy.start()
        burst(f'ch{l}_0')
        need(2 + 2 * l)
        save_mid.wait()

        def blocks(i, slot):
            t, h = i // 2, i % 2
            part = pl.ds(pl.multiple_of(h * BLK, BLK), BLK)
            return [(wc_all.at[2 * l, t, :, :, :, :, part], w1_v.at[slot]), (wc_all.at[2 * l + 1, t, h], w2_v.at[slot])]

        def outs(i, slot):
            part = pl.ds(pl.multiple_of(i * BLK, BLK), BLK)
            half = pl.ds(pl.multiple_of(i // 2 * BLK, BLK), BLK)
            return [(pre_v.at[slot], pre_out.at[l, :, part]), (act_v.at[slot], act_out.at[l, i % 2, :, half])]
        run = during(f'ch{l}_', NBLK)

        def channel(i, slot):
            run(i)
            part = pl.ds(pl.multiple_of(i * BLK, BLK), BLK)
            h = dot_nn(v_v[...], w1_v[slot].reshape(CH, BLK)) + bch1[l:l + 1, part]
            value, pre_v[slot] = gelu_both(h)
            act_v[slot] = value.astype(bf16)
            add_rows(dot_nn(act_v[slot], w2_v[slot].reshape(BLK, CH)))
        for_blocks(Stream(sem_w, blocks, NBLK), channel, Stream(sem_o, outs, NBLK))
        add_rows(jnp.broadcast_to(vec[r + 4:r + 5, :], (ROWS, CH)))
        for copy in save_v:
            copy.wait()

    burst('head')
    need(5)
    keep_p.wait()
    last = 11
    pooled = jnp.sum(get(x_v, pl.ds(0, ROWS)).reshape(TOK, IMG, CH), axis=0) * (1.0 / TOK)
    std, inv = standardize(pooled)
    head_in = (std * vec[last:last + 1, :] + vec[last + 1:last + 2, :]).astype(bf16)
    hl[...] = head_in
    w_h = wh[...].reshape(CH, CH)
    logits = dot_nn(head_in, w_h) + bh_v[0:1, :]
    row = lax.broadcasted_iota(jnp.int32, (IMG, 1), 0)
    label = jnp.zeros((IMG, 1), jnp.int32)
    for b in range(IMG):
        value = labels[me['x'] * IMG + b]
        label = jnp.where(row == b, value, label)
    label = label + 6 * sum(jnp.where(label >= edge, 1, 0) for edge in (250, 500, 750))
    is_label = lax.broadcasted_iota(jnp.int32, logits.shape, 1) == label
    top = jnp.max(logits, axis=-1, keepdims=True)
    ex = jnp.exp(logits - top)
    es = jnp.sum(ex, axis=-1, keepdims=True)
    nll = top + jnp.log(es) - jnp.sum(jnp.where(is_label, logits, 0.0), axis=-1, keepdims=True)
    d_logits = (ex / es - jnp.where(is_label, 1.0, 0.0)) * (1.0 / 1024)
    gbh[...] = jnp.sum(d_logits, axis=0, keepdims=True)
    d_bf = d_logits.astype(bf16)
    hr[...] = d_bf
    d_in = dot_nt(d_bf, w_h)
    hstat[0:1, :] = jnp.sum(d_in * std, axis=0, keepdims=True)
    hstat[1:2, :] = jnp.sum(d_in, axis=0, keepdims=True)
    hstat[2:3, :] = jnp.broadcast_to(jnp.sum(nll, axis=0, keepdims=True), (1, CH))
    dx0[...] = norm_grad(d_in, vec[last:last + 1, :], std, inv) * (1.0 / TOK)
    burst('end')
    net.finish()
    assert len(net.builds) <= FRONT_COPIES, len(net.builds)


def front(*operands):
    a, v = pl.BlockSpec(memory_space=pl.ANY), pl.BlockSpec(memory_space=pltpu.VMEM)
    S, V, DMA = jax.ShapeDtypeStruct, pltpu.VMEM, pltpu.SemaphoreType.DMA
    return pl.pallas_call(
        front_kernel, name='front',
        in_specs=[pl.BlockSpec(memory_space=pltpu.SMEM), a] + [v] * 17,
        out_specs=[a] * 9 + [v] * 8,
        out_shape=[S((N_CH, 4, 2, 4, 4, 32, 1024), bf16), S((2, ROWS, 1536), bf16), S((2, CH // 128, ROWS, 128), f32),
                   S((2, CH // 128, ROWS, 128), f32),
                   S((2, 2, ROWS, 512), bf16), S((2, ROWS, CHH), f32), S((2, 2, ROWS, 2048), bf16),
                   S((2, IMG * TOK_CUTS, TOKH, CH // TOK_CUTS), bf16), S((2, IMG * TOK_CUTS, TOKH, CH // TOK_CUTS), f32), S((IMG, CH), bf16),
                   S((IMG, CH), bf16), S((IMG, CH), f32), S((8, CH), f32), S((1, CH), f32), S((16, CH), f32),
                   S((4, TOKH, 128), bf16), S((4, TPAD, TOKH), bf16)],
        scratch_shapes=[V((N_CH, 32, 1024), bf16), V((2, 96, 128), bf16), V((32, 256), bf16), V((4, 16, 128), f32),
                        V((4, 16, 128), bf16), V((8, 128), f32), V((8, 256), f32), V((2, 4, 4, 2, 96, 512), bf16),
                        V((2, 4, 4, 32, CH), bf16), V((4, 4, 4, 2, 16, 128), bf16), V((4, 4, 4, 2, 8, 128), f32),
                        V((1024, 128), f32), V((8, CH), f32), V((2, CHH), f32),
                        V((128, 128), f32), V((TOK, IMG, 3072), bf16), V((2, ROWS, 1536), bf16), V((CH // 128, XROWS, 128), f32),
                        V((ROWS, CH), bf16), V((2, 2, 4, 4, 32, BLK), bf16), V((2, 4, 4, 32, CH), bf16),
                        V((2, ROWS, BLK), f32), V((2, ROWS, BLK), bf16),
                        V((2, TOK_CUTS, TOKH, CH // TOK_CUTS), bf16), V((2, TOK_CUTS, TOKH, CH // TOK_CUTS), f32),
                        DMA((FRONT_COPIES,)), DMA((FRONT_COPIES,)), DMA((2,)), DMA((2, 2)), DMA((2, 2)), DMA((3,)), DMA((2, 2))],
        compiler_params=pltpu.CompilerParams(collective_id=0, has_side_effects=True, vmem_limit_bytes=62 * 1024 * 1024),
        cost_estimate=pl.CostEstimate(flops=90_000_000_000, bytes_accessed=180_000_000, transcendentals=0),
    )(*operands)


GROUPS = (3, 2, 1, 0, HEAD, STEM)
UNITS = tuple((g, c) for g in GROUPS for c in (2, 0, 1) if g != HEAD or c == 2)
BACK_COPIES = 18 * len(UNITS) + 40
NEEDS = {3: ('act1', 'dout1'), 2: ('vin1', 'dpre1'), 1: ('act0', 'dout0'), 0: ('vin0', 'dpre0'), STEM: ('pat', 'dres'),
         HEAD: ('hl', 'hr')}
BACK_ORDER = (
    ('l1', ((3, 'L'),)),
    ('t1_5', ((0, 0), (0, 1), (1, 0), (1, 1),)),
    ('t1_7', ((0, 2),)),
    ('c0_1', ((1, 2),)),
    ('c0_2', ((0, 3), (2, 0), (2, 'L'), (2, 1),)),
    ('c0_4', ((1, 3), (0, 4),)),
    ('c0_7', ((2, 2), (0, 5),)),
    ('t0_1', ((1, 4),)),
    ('t0_3', ((3, 0), (3, 1), (2, 3), (1, 5), (0, 6), (4, 0), (4, 1), (0, 7), (5, 0), (1, 'L'), (5, 1), (3, 2),)),
    ('t0_4', ((2, 4),)),
    ('t0_5', ((4, 2), (1, 6),)),
    ('t0_6', ((3, 3), (6, 0), (6, 1), (5, 2), (2, 5), (1, 7), (7, 0), (7, 1), (4, 3), (3, 4), (2, 6), (8, 0), (0, 'L'),
        (8, 1), (6, 2), (5, 3), (4, 4),)),
    ('t0_7', ((7, 2),)),
    ('fin', ((9, 0), (9, 1), (8, 2), (5, 4), (3, 5), (6, 3), (2, 7),)),
    ('end', ((9, 2), (6, 4), (4, 5), (7, 3), (10, 0), (10, 1), (5, 5), (8, 3), (7, 4), (6, 5), (3, 6), (11, 0), (4, 'L'),
        (11, 1), (9, 3), (8, 4), (7, 5), (4, 6), (6, 6), (3, 7), (12, 0), (12, 1), (10, 2), (13, 0), (13, 1), (11, 2),
        (12, 2), (9, 4), (8, 5), (5, 6), (7, 6), (4, 7), (14, 0), (14, 1), (15, 0), (15, 1), (6, 7), (10, 3), (9, 5), (8, 6),
        (5, 7), (11, 3), (13, 2), (14, 2), (15, 2), (12, 3), (7, 7), (8, 7), (11, 4), (10, 4), (9, 6), (12, 4), (11, 5),
        (15, 3), (12, 5), (13, 3), (10, 5), (14, 3), (9, 7), (11, 6), (12, 6), (15, 4), (13, 4), (10, 6), (14, 4), (11, 7),
        (12, 7), (15, 5), (10, 7), (13, 5), (14, 5), (15, 6), (13, 6), (14, 6), (15, 7), (13, 7), (14, 7),)),
)
SMALL = dict(sm=((4, 4, 4, 8, 128), (3, 4, 4, 8, 128), (3, 4, 8, 128), (3, 8, 128)),
             tk=((4, 4, 4, 16, 128), (3, 4, 4, 16, 128), (3, 4, 16, 128), (3, 4, 16, 128)))


def reduce_scratch():
    per = []
    for c in range(3):
        n = COLS[c][1]
        many = sum(1 for u in UNITS if u[1] == c)
        lead = ((4, 4), (4,), ())
        b = {'C': pltpu.VMEM((2, 4, 4, 4, 32, n), bf16), 'S1': pltpu.VMEM((4, 4, 32, n), f32), 'S2': pltpu.VMEM((2, 4, 32, n), f32)}
        for ph in range(3):
            if ph:
                b[f'opp{ph}'] = pltpu.VMEM(lead[ph] + (32, n), bf16)
                b[f'pr{ph}'] = pltpu.VMEM(lead[ph] + (16, n), bf16)
                b[f'pl{ph}'] = pltpu.VMEM(lead[ph] + (16, n), bf16)
            for name in ('rig', 'lef'):
                b[f'{name}{ph}'] = pltpu.VMEM(lead[ph] + (16, n), bf16)
            for name in ('half0', 'half1'):
                b[f'{name}{ph}'] = pltpu.VMEM((many,) + lead[ph] + (16, n), bf16)
            for name in ('froml', 'fromr'):
                b[f'{name}{ph}'] = pltpu.VMEM((many,) + lead[ph] + (32, n), bf16)
        per.append(b)
    return per


def small_scratch():
    b = {f'{kind}{n + 1}': pltpu.VMEM(shape, f32) for kind, shapes in SMALL.items() for n, shape in enumerate(shapes)}
    b.update(sm=pltpu.VMEM((4, 4, 4, 2, 8, 128), f32), tk=pltpu.VMEM((4, 4, 4, 2, 16, 128), f32),
             sm_s1=pltpu.VMEM((4, 4, 8, 128), f32), sm_s2=pltpu.VMEM((4, 8, 128), f32),
             tk_s1=pltpu.VMEM((4, 4, 16, 128), f32), tk_s2=pltpu.VMEM((4, 16, 128), f32))
    return b


def small_pack(b, flat, turn, gvec, hstat, gbch1, gbh):
    for n in range(8):
        cols = pl.ds(128 * n, 128)
        turn[n, pl.ds(0, 128), :] = jnp.zeros((128, 128), f32)
        turn[n, pl.ds(0, 16), :] = gvec[:, cols]
        turn[n, pl.ds(11, 2), :] = hstat[pl.ds(0, 2), cols]
    for n in range(8):
        tile = turn[n, pl.ds(0, 128), :].T
        for i in range(4):
            a = n % 4 * 4 + i
            flat[a // 2, pl.ds(a % 2 * 64 + n // 4 * 32, 32), :] = tile[32 * i:32 * i + 32]
    for l in range(2):
        def gather(n, total):
            lane = lax.broadcasted_iota(jnp.int32, (128, 512), 0)
            col = lax.broadcasted_iota(jnp.int32, (128, 512), 1)
            sums = gbch1[l:l + 1, pl.ds(pl.multiple_of(512 * n, 512), 512)]
            mine = jnp.where(lane == n // 2 * 32 + col // 32 * 2 + n % 2, sums, 0.0)
            pick = jnp.where(lane == 32 + col % 32, 1.0, 0.0).astype(bf16)
            return total + dot_nt(jnp.concatenate(three_parts(mine), axis=0), pick)
        total = lax.fori_loop(0, 8, gather, jnp.zeros((384, 128), f32))
        total = total[0:128] + total[128:256] + total[256:384]
        for n in range(8):
            flat[n, pl.ds(l, 16, stride=8), :] += total[16 * n:16 * n + 16]
    lane = lax.broadcasted_iota(jnp.int32, (1, 128), 1)
    for t in range(4):
        for q in range(4):
            tile = gbh[0:1, t * 256 + q // 2 * 128:t * 256 + q // 2 * 128 + 128]
            if q % 2 == 0:
                tile = jnp.concatenate([tile[:, 64:], tile[:, :64]], axis=1)
            tile = jnp.where(lane >= 64, tile, 0.0)
            for n in (2 * t, 2 * t + 1):
                flat[n, pl.ds(2 + q, 16, stride=8), :] += tile
    for n in range(8):
        flat[n, pl.ds(6, 16, stride=8), :] += jnp.where(lane == 64, hstat[2:3, 0:128], 0.0)
        b['sm'][n // 2, pl.ds(n % 2 * 2, 2)] = flat[n, pl.ds(0, 128), :].reshape(2, 4, 2, 8, 128)


def back_kernel(*refs):
    xin, xmid, pre_in, wc, act, vin, pat, tok_act, tok_slope = refs[:9]
    hl, hr, dx0, hstat, gbh, wt, wt_t, vec = refs[9:17]
    out_c, out_s, out_h, sm_own, tk_own = refs[17:22]
    dpre, dout, dres, x_act, x_vin, x_pat, x_dpre, x_dout, x_dres = refs[22:31]
    (per, b, big, little, x_hl, x_hr, gvec, gbch1, x_v, d_v, dv_v, do_v, w1_v, w2_v, pre_v, dp_v,
     ta_v, ts_v, send_sems, recv_sems, load_sems, sem, sem_w, sem_o, sem_t) = refs[31:]
    me = my_place()
    other = moved(me, 'k', 1)
    k, k2 = me['k'], 1 - me['k']
    barrier = pltpu.get_barrier_semaphore()
    for dim in 'xyz':
        for step in (1, 2, 3):
            pl.semaphore_signal(barrier, inc=1, device_id=device(moved(me, dim, step)), device_id_type=MESH)
    pl.semaphore_signal(barrier, inc=1, device_id=device(other), device_id_type=MESH)
    net = Net(send_sems, recv_sems)
    ring = {d: [moved(me, d, n)[d] for n in range(4)] for d in 'xyz'}
    peers = {(d, n): device(moved(me, d, n)) for d in 'xyz' for n in (1, 2, 3)}
    partner = device(other)
    half_at = pl.ds(pl.multiple_of(k * 512, 512), 512)
    half_to = pl.ds(pl.multiple_of(k2 * 512, 512), 512)
    swaps = {'act1': (act.at[1, k2], x_act.at[1]), 'act0': (act.at[0, k2], x_act.at[0]), 'vin1': (vin.at[1, k2], x_vin.at[1]),
             'vin0': (vin.at[0, k2], x_vin.at[0]), 'pat': (pat.at[k2], x_pat), 'dpre1': (dpre.at[1], x_dpre.at[1]),
             'dpre0': (dpre.at[0], x_dpre.at[0]), 'dout1': (dout.at[1], x_dout.at[1]), 'dout0': (dout.at[0], x_dout.at[0]),
             'dres': (dres, x_dres), 'hl': (hl.at[:, half_to], x_hl), 'hr': (hr, x_hr)}

    def swap(*names):
        for name in names:
            net.start(name, lambda name=name: (*swaps[name], partner))
    busy = {}

    def free(key):
        for name in busy.pop(key, ()):
            net.copy(name).wait_send()
            net.done.add(name)

    def loads(g):
        l = g // 2
        if g == STEM:
            wide, tall = (pat.at[k], x_pat, 1536), (dres, x_dres, CH)
        elif g % 2:
            wide, tall = (act.at[l, k], x_act.at[l], 2048), (dout.at[l], x_dout.at[l], CH)
        else:
            wide, tall = (dpre.at[l], x_dpre.at[l], CHH), (vin.at[l, k], x_vin.at[l], 512)
        out = []
        for n, (buf, (own, far, cols)) in enumerate(((big, wide), (little, tall))):
            out += [pltpu.make_async_copy(own, buf.at[0, :, pl.ds(0, cols)], load_sems.at[2 * n]),
                    pltpu.make_async_copy(far, buf.at[1, :, pl.ds(0, cols)], load_sems.at[2 * n + 1])]
        return out

    def product(u):
        g, c, slot = u.g, u.c, u.slot
        first = c == 2
        if first and g != HEAD:
            for copy in loads(g):
                copy.wait()
        if g == STEM and not first:
            return
        for v in (units if g == STEM else (u,)):
            if v.g == g:
                free(('C', v.c, v.slot))
        if g == HEAD:
            net.arrived(*NEEDS[g])
            for t in range(4):
                cols = pl.ds(256 * t, 256)
                prod = dot_tn(hl[:, half_at], hr[:, cols]) + dot_tn(x_hl[...], x_hr[:, cols])
                per[c]['C'][slot, t] = prod.astype(bf16).reshape(4, 4, 32, 256)
        elif g == STEM:
            slots = {v.c: v.slot for v in units if v.g == STEM}

            @pl.loop(0, 4)
            def _(z):
                rows = pl.ds(pl.multiple_of(z * 384, 384), 384)
                for t in range(4):
                    def right(s):
                        return jnp.concatenate([little[s, :, 128 * t:128 * t + 128], little[s, :, 512 + 128 * t:640 + 128 * t]], axis=1)
                    prod = dot_tn(big[0, :, rows], right(0)) + dot_tn(big[1, :, rows], right(1))
                    prod = prod.astype(bf16).reshape(4, 3, 32, 256)
                    for d in range(3):
                        per[d]['C'][slots[d], t, z, :, :, pl.ds(0, 256)] = prod[:, d]
        else:
            c0, n = COLS[c]

            @pl.loop(0, 4)
            def _(t):
                for h in range(2):
                    if g % 2:
                        left = pl.ds(pl.multiple_of(t * 512 + h * 256, 256), 256)
                        prod = dot_tn(big[0, :, left], little[0, :, c0:c0 + n]) + dot_tn(big[1, :, left], little[1, :, c0:c0 + n])
                    else:
                        right = pl.ds(pl.multiple_of(t * 1024 + c0, 128), n)
                        rows = slice(256 * h, 256 * h + 256)
                        prod = dot_tn(little[0, :, rows], big[0, :, right]) + dot_tn(little[1, :, rows], big[1, :, right])
                    per[c]['C'][slot, t, 2 * h:2 * h + 2] = prod.astype(bf16).reshape(2, 4, 32, n)

    class Unit:
        def __init__(self, g, c):
            self.g, self.c = g, c
            self.index = [u for u in UNITS if u[1] == c].index((g, c))
            self.slot = self.index % 2
            self.n = COLS[c][1] if g < N_CH else 256
            self.cols = pl.ds(0, self.n)
            self.buf = per[c]
            self.dims = ORDERS[c]
            self.rest = [d for d in 'xzy' if d != self.dims[0]]

        def cut(self, name, *at, rows=slice(None)):
            ref = self.buf[name]
            inner = [slice(None)] * (len(ref.shape) - len(at) - 2)
            return ref.at[(*at, *inner, rows, self.cols)]

        def block(self, p, rows):
            at = {d: EVERY for d in 'xzy'}
            at[self.dims[0]] = p
            return self.buf['C'].at[self.slot, at['x'], at['z'], at['y'], rows, self.cols]

        def share(self, phase, p, e, rows):
            if phase == 0:
                at = dict(zip(self.rest, e))
                at[self.dims[0]] = p
                return self.buf['C'][self.slot, at['x'], at['z'], at['y'], rows, self.cols].astype(f32)
            if phase == 1:
                at = (p, e[0]) if self.dims[1] == self.rest[0] else (e[0], p)
                return self.buf['S1'][(*at, rows, self.cols)]
            return self.buf['S2'][self.slot, p, rows, self.cols]

        def each(self, phase, body):
            if phase == 2:
                body(())
            elif phase == 1:
                pl.loop(0, 4)(lambda i: body((i,)))
            else:
                @pl.loop(0, 4)
                def _(i):
                    pl.loop(0, 4)(lambda j: body((i, j)))

        def send(self, tag, phase, src, dst, step):
            name = (self.g, self.c, tag, phase)
            net.start(name, lambda: (src(), dst(), peers[self.dims[phase], step]))
            return name

        def arrived(self, phase, *tags):
            net.arrived(*[(self.g, self.c, tag, phase) for tag in tags])

        def opposite(self, phase):
            places = ring[self.dims[phase]]
            low, high = pl.ds(0, 16), pl.ds(16, 16)
            if phase == 0:
                sources = [lambda: self.block(places[2], low), lambda: self.block(places[2], high),
                           lambda: self.block(places[1], high), lambda: self.block(places[3], low)]
            else:
                names = (f'opp{phase}', f'pr{phase}', f'pl{phase}')
                for name in names:
                    free((name, self.c))
                opp, right, left = (self.buf[name] for name in names)

                def body(e):
                    opp[(*e, slice(None), self.cols)] = self.share(phase, places[2], e, pl.ds(0, 32)).astype(bf16)
                    right[(*e, slice(None), self.cols)] = self.share(phase, places[1], e, high).astype(bf16)
                    left[(*e, slice(None), self.cols)] = self.share(phase, places[3], e, low).astype(bf16)
                self.each(phase, body)
                sources = [lambda: self.cut(names[0], rows=low), lambda: self.cut(names[0], rows=high),
                           lambda: self.cut(names[1]), lambda: self.cut(names[2])]
            targets = [lambda: self.cut(f'half0{phase}', self.index), lambda: self.cut(f'half1{phase}', self.index),
                       lambda: self.cut(f'froml{phase}', self.index, rows=high),
                       lambda: self.cut(f'fromr{phase}', self.index, rows=low)]
            sent = [self.send(tag, phase, src, dst, step)
                    for tag, src, dst, step in zip(('h0', 'h1', 'p0', 'p1'), sources, targets, (1, 3, 1, 3))]
            if phase == 0:
                busy['C', self.c, self.slot] = sent
            else:
                busy[names[0], self.c] = sent[:2]
                busy[names[1], self.c] = sent[2:3]
                busy[names[2], self.c] = sent[3:]

        def beside(self, phase):
            places = ring[self.dims[phase]]
            for half, step, name, dst in ((0, 1, 'rig', 'froml'), (1, 3, 'lef', 'fromr')):
                self.arrived(phase, f'h{half}')
                key = f'{name}{phase}'
                free((key, self.c))
                out, got = self.buf[key], self.buf[f'half{half}{phase}']
                rows = pl.ds(16 * half, 16)

                def body(e):
                    value = self.share(phase, places[step], e, rows) + got[(self.index, *e, slice(None), self.cols)].astype(f32)
                    out[(*e, slice(None), self.cols)] = value.astype(bf16)
                self.each(phase, body)
                busy[key, self.c] = [self.send(f'f{half}', phase, lambda key=key: self.cut(key),
                                               lambda dst=dst, rows=rows: self.cut(f'{dst}{phase}', self.index, rows=rows), step)]

        def total(self, phase):
            self.arrived(phase, 'p0', 'p1', 'f0', 'f1')
            p = ring[self.dims[phase]][0]

            def body(e):
                got = [self.buf[f'{name}{phase}'][(self.index, *e, slice(None), self.cols)].astype(f32)
                       for name in ('froml', 'fromr')]
                value = self.share(phase, p, e, pl.ds(0, 32)) + got[0] + got[1]
                if phase == 0:
                    self.buf['S1'][(*e, slice(None), self.cols)] = value
                elif phase == 1:
                    self.buf['S2'][(self.slot, *e, slice(None), self.cols)] = value
                elif self.g == STEM:
                    out_s[pl.ds(32 * self.c, 32), :] = value
                elif self.g == HEAD:
                    out_h[...] = value
                else:
                    out_c[self.g, :, pl.ds(*COLS[self.c])] = value
            self.each(phase, body)

        def run(self, stage):
            if stage == 0:
                product(self)
            elif stage == 7:
                self.total(2)
            elif stage % 2 == 0:
                self.beside(stage // 2 - 1)
            else:
                if stage > 1:
                    self.total(stage // 2 - 1)
                self.opposite(stage // 2)

    units = [Unit(g, c) for g, c in UNITS]
    bursts = dict(BACK_ORDER)

    def step(which, stage):
        if stage == 'L':
            net.arrived(*NEEDS[which])
            for copy in loads(which):
                copy.start()
        else:
            units[which].run(stage)

    def burst(name):
        for s in bursts.get(name, ()):
            step(*s)

    def during(name, count):
        def run(i):
            for n in range(1, count):
                if bursts.get(f'{name}{n}'):
                    pl.when(i == n)(functools.partial(burst, f'{name}{n}'))
        return run

    load = pltpu.make_async_copy(xmid.at[1], x_v.at[:, pl.ds(0, ROWS)], sem.at[0])
    load.start()
    mask = row_mask()
    rest = pl.ds(ROWS, XROWS - ROWS)
    put(d_v, rest, jnp.zeros((XROWS - ROWS, CH), f32))
    put(x_v, rest, jnp.zeros((XROWS - ROWS, CH), f32))
    gvec[...] = jnp.zeros_like(gvec)
    tk = b['tk']
    tk[...] = jnp.zeros_like(tk)

    @pl.loop(0, TOK)
    def _(s):
        put(d_v, pl.ds(pl.multiple_of(s * IMG, IMG), IMG), dx0[...])

    def add(row, value):
        gvec[row:row + 1, :] += jnp.sum(value, axis=0, keepdims=True)

    def add_token(n, value, start=0):
        tk[n, :, :, :, :, pl.ds(start, value.shape[1])] += value.reshape(4, 4, 2, 16, value.shape[1])

    for l in (1, 0):
        r = 1 + 5 * l
        for at, size in CHUNKS:
            d = get(d_v, pl.ds(at, size))
            add(r + 4, d)
            do_v[pl.ds(at, size), :] = d.astype(bf16)
        keep = pltpu.make_async_copy(do_v, dout.at[l], sem.at[1])
        keep.start()
        keep.wait()
        if l == 1:
            pl.semaphore_wait(barrier, 10)
            swap('hl', 'hr', 'dout1', 'act1', 'vin1', 'act0', 'vin0', 'pat')
        else:
            swap('dout0')
        burst(f'c{l}_0')
        run = during(f'c{l}_', NBLK)

        def blocks(i, slot):
            t, h = i // 2, i % 2
            part = pl.ds(pl.multiple_of(h * BLK, BLK), BLK)
            whole = pl.ds(pl.multiple_of(i * BLK, BLK), BLK)
            return [(wc.at[2 * l, t, :, :, :, :, part], w1_v.at[slot]), (wc.at[2 * l + 1, t, h], w2_v.at[slot]),
                    (pre_in.at[l, :, whole], pre_v.at[slot])]

        def outs(i, slot):
            return [(dp_v.at[slot], dpre.at[l, :, pl.ds(pl.multiple_of(i * BLK, BLK), BLK)])]

        def channel(i, slot):
            run(i)
            for n in range(2):
                cols = slice(256 * n, 256 * n + 256)
                d = dot_nt(do_v[...], w2_v[slot, 2 * n:2 * n + 2].reshape(256, CH)) * pre_v[slot, :, cols]
                gbch1[l:l + 1, pl.ds(pl.multiple_of(i * BLK + 256 * n, 256), 256)] = jnp.sum(d, axis=0, keepdims=True)
                dp_v[slot, :, cols] = d.astype(bf16)

            @pl.when(i == 0)
            def _():
                dv_v[...] = jnp.zeros_like(dv_v)
            for n in range(2):
                cols = slice(512 * n, 512 * n + 512)
                dv_v[:, cols] += dot_nt(dp_v[slot], w1_v[slot, n].reshape(512, BLK))
        for_blocks(Stream(sem_w, blocks, NBLK), channel, Stream(sem_o, outs, NBLK))
        swap(f'dpre{l}')
        burst(f'l{l}')
        load.wait()

        @pl.loop(0, ROWS // TPAD)
        def _(n):
            rows = pl.ds(pl.multiple_of(n * TPAD, TPAD), TPAD)
            std, inv = standardize(get(x_v, rows))
            d = dv_v[rows, :]
            add(r + 2, d * std)
            add(r + 3, d)
            put(d_v, rows, get(d_v, rows) + norm_grad(d, vec[r + 2:r + 3, :], std, inv))
        load = pltpu.make_async_copy(xin.at[l], x_v.at[:, pl.ds(0, ROWS)], sem.at[0])
        load.start()
        hidden = Stream(sem_t, lambda i, slot: [(tok_act.at[l, i], ta_v.at[slot]), (tok_slope.at[l, i], ts_v.at[slot])],
                        IMG * TOK_CUTS)
        for n in range(TOK_CUTS):
            hidden.start(n, n)
        burst(f't{l}_0')
        load.wait()
        run = during(f't{l}_', IMG)

        @pl.loop(0, IMG)
        def _(m):
            run(m)
            std, inv = standardize(get(x_v, image(m)))
            a = with_bias_rows(std * vec[r:r + 1, :] + vec[r + 1:r + 2, :])
            d_mid = get(d_v, image(m))
            dm = d_mid.astype(bf16)
            parts = []
            for n in range(TOK_CUTS):
                slot = n
                hidden.wait(m * TOK_CUTS + n, slot)
                cols = slice(CH // TOK_CUTS * n, CH // TOK_CUTS * (n + 1))
                add_token(2 + l, dot_nt(ta_v[slot], dm[:, cols]))
                dh = dot_nn(wt[2 + l, :, 0:TPAD], dm[:, cols]) * ts_v[slot]
                add_token(l, jnp.sum(dh, axis=-1, keepdims=True), 64)
                dh = dh.astype(bf16)
                add_token(l, dot_nt(dh, a[:, cols]))
                parts.append(dot_nn(wt_t[l], dh))

                @pl.when(m + 1 < IMG)
                def _():
                    hidden.start((m + 1) * TOK_CUTS + n, slot)
            d = jnp.where(mask, jnp.concatenate(parts, axis=1), 0.0)
            add(r, d * std)
            add(r + 1, d)
            put(d_v, image(m), d_mid + norm_grad(d, vec[r:r + 1, :], std, inv))
        if l == 1:
            load = pltpu.make_async_copy(xmid.at[0], x_v.at[:, pl.ds(0, ROWS)], sem.at[0])
            load.start()
            burst('d0')

    burst('fin')
    for at, size in CHUNKS:
        d = get(d_v, pl.ds(at, size))
        add(0, d)
        do_v[pl.ds(at, size), :] = d.astype(bf16)
    keep = pltpu.make_async_copy(do_v, dres, sem.at[1])
    keep.start()
    keep.wait()
    swap('dres')
    small_pack(b, x_v, d_v, gvec, hstat, gbch1, gbh)

    last = []

    def put_small(name, src, dst, target):
        last.append(name)
        net.start(name, lambda: (src, dst, target))

    def small(n):
        x, z, y = (ring[d][0] for d in 'xzy')
        net.arrived(*last)
        last.clear()
        if n == 0:
            put_small(('sm', 0), b['sm'].at[:, :, :, k2], b['sm1'], partner)
            put_small(('tk', 0), b['tk'].at[:, :, :, k2], b['tk1'], partner)
        elif n == 1:
            b['sm1'][...] += b['sm'][:, :, :, k]
            b['tk1'][...] += b['tk'][:, :, :, k]
            for s in (1, 2, 3):
                put_small(('sm', 1, s), b['sm1'].at[ring['x'][s]], b['sm2'].at[s - 1], peers['x', s])
                put_small(('tk', 1, s), b['tk1'].at[:, ring['z'][s]], b['tk2'].at[s - 1], peers['z', s])
        elif n == 2:
            b['sm_s1'][...] = b['sm1'][x] + b['sm2'][0] + b['sm2'][1] + b['sm2'][2]
            b['tk_s1'][...] = b['tk1'][:, z] + b['tk2'][0] + b['tk2'][1] + b['tk2'][2]
            for s in (1, 2, 3):
                put_small(('sm', 2, s), b['sm_s1'].at[ring['z'][s]], b['sm3'].at[s - 1], peers['z', s])
                put_small(('tk', 2, s), b['tk_s1'].at[:, ring['y'][s]], b['tk3'].at[s - 1], peers['y', s])
        elif n == 3:
            b['sm_s2'][...] = b['sm_s1'][z] + b['sm3'][0] + b['sm3'][1] + b['sm3'][2]
            b['tk_s2'][...] = b['tk_s1'][:, y] + b['tk3'][0] + b['tk3'][1] + b['tk3'][2]
            for s in (1, 2, 3):
                put_small(('sm', 3, s), b['sm_s2'].at[ring['y'][s]], b['sm4'].at[s - 1], peers['y', s])
                put_small(('tk', 3, s), b['tk_s2'], b['tk4'].at[s - 1], peers['x', s])
        else:
            sm_own[...] = b['sm_s2'][y] + b['sm4'][0] + b['sm4'][1] + b['sm4'][2]
            ordered = []
            for place in range(4):
                value = b['tk_s2'][...]
                for s in (1, 2, 3):
                    value = jnp.where(ring['x'][4 - s] == place, b['tk4'][s - 1], value)
                ordered.append(value)
            tk_own[...] = (ordered[0] + ordered[1]) + (ordered[2] + ordered[3])

    tail = bursts.get('end', ())
    small(0)
    for n, s in enumerate(tail):
        step(*s)
        if n in (8, 18, 28, 38):
            small(1 + (8, 18, 28, 38).index(n))
    net.finish()
    assert len(net.builds) <= BACK_COPIES, len(net.builds)


def back(*operands):
    a, v = pl.BlockSpec(memory_space=pl.ANY), pl.BlockSpec(memory_space=pltpu.VMEM)
    S, V, DMA = jax.ShapeDtypeStruct, pltpu.VMEM, pltpu.SemaphoreType.DMA
    return pl.pallas_call(
        back_kernel, name='back',
        in_specs=[a] * 9 + [v] * 8, out_specs=[v] * 5 + [a] * 9,
        out_shape=[S((N_CH, 32, 1024), f32), S((96, 256), f32), S((32, 256), f32), S((8, 128), f32), S((4, 16, 128), f32),
                   S((2, ROWS, CHH), bf16), S((2, ROWS, CH), bf16), S((ROWS, CH), bf16), S((2, ROWS, 2048), bf16),
                   S((2, ROWS, 512), bf16), S((ROWS, 1536), bf16), S((2, ROWS, CHH), bf16), S((2, ROWS, CH), bf16),
                   S((ROWS, CH), bf16)],
        scratch_shapes=[reduce_scratch(), small_scratch(), V((2, ROWS, CHH), bf16), V((2, ROWS, CH), bf16), V((IMG, 512), bf16),
                        V((IMG, CH), bf16), V((16, CH), f32), V((2, CHH), f32), V((CH // 128, XROWS, 128), f32),
                        V((CH // 128, XROWS, 128), f32), V((ROWS, CH), f32), V((ROWS, CH), bf16), V((2, 2, 4, 4, 32, BLK), bf16),
                        V((2, 4, 4, 32, CH), bf16), V((2, ROWS, BLK), f32), V((2, ROWS, BLK), bf16), V((TOK_CUTS, TOKH, CH // TOK_CUTS), bf16),
                        V((TOK_CUTS, TOKH, CH // TOK_CUTS), f32), DMA((BACK_COPIES,)), DMA((BACK_COPIES,)), DMA((4,)), DMA((2,)), DMA((2, 3)),
                        DMA((2, 1)), DMA((TOK_CUTS, 2))],
        compiler_params=pltpu.CompilerParams(collective_id=1, has_side_effects=True, vmem_limit_bytes=64 * 1024 * 1024 - 65536),
        cost_estimate=pl.CostEstimate(flops=120_000_000_000, bytes_accessed=200_000_000, transcendentals=0),
    )(*operands)


def finish_kernel(c, stem, head, sm, tk, loss, o_stem, o_bstem, o_ln1g, o_ln1b, o_wt1, o_bt1, o_wt2, o_ln2g, o_ln2b, o_ch1,
                  o_bch1, o_ch2, o_bch2, o_lnfg, o_lnfb, o_head, o_bhead):
    def core_last(value, pick):
        got = dot_nt(jnp.concatenate(three_parts(value), axis=0), pick)
        n = value.shape[0]
        return got[0:n] + got[n:2 * n] + got[2 * n:3 * n]
    pick = core_first(1024, 1024, 32)
    for l in range(2):
        o_ch1[l] = core_last(c[2 * l], pick)
        o_ch2[l] = core_last(c[2 * l + 1], pick)
    o_stem[...] = core_last(stem[...], core_first(256, 256, 32))
    o_head[...] = head[:, 0:250]
    own = sm[...]
    turned = jnp.concatenate([own, jnp.zeros((120, 128), f32)], axis=0).T
    for ref, n in ((o_bstem, 0), (o_lnfg, 11), (o_lnfb, 12)):
        ref[...] = turned[n, 0:8]
    for n, ref in enumerate((o_ln1g, o_ln1b, o_ln2g, o_ln2b, o_bch2)):
        for l in range(2):
            ref[pl.ds(l, 1), :] = turned[1 + 5 * l + n:2 + 5 * l + n, 0:8]
    o_bch1[...] = own[0:2, 32:64]
    classes = jnp.concatenate([own[2 + q:3 + q, 64:128] for q in range(4)], axis=1)
    o_bhead[...] = classes[0, 0:250]
    loss[...] = own[6:7, 64:65] * (1.0 / 1024)
    for l in range(2):
        o_wt1[l] = tk[l, :, 0:TOK]
        o_wt2[l] = tk[2 + l, :, 0:TOK]
        tall = jnp.concatenate([tk[l], jnp.zeros((112, 128), f32)], axis=0).T
        o_bt1[pl.ds(l, 1), :] = tall[64:65, 0:16]


def finish(*operands):
    S = jax.ShapeDtypeStruct
    v = pl.BlockSpec(memory_space=pltpu.VMEM)
    return pl.pallas_call(
        finish_kernel, name='finish', in_specs=[v] * 5, out_specs=[v] * 18,
        out_shape=[S((1, 1), f32), S((96, 256), f32), S((8,), f32), S((2, 8), f32), S((2, 8), f32), S((2, 16, TOK), f32),
                   S((2, 16), f32), S((2, 16, TOK), f32), S((2, 8), f32), S((2, 8), f32), S((2, 32, 1024), f32), S((2, 32), f32),
                   S((2, 32, 1024), f32), S((2, 8), f32), S((8,), f32), S((8,), f32), S((32, 250), f32), S((250,), f32)],
    )(*operands)

CHANNEL_AXES = ('tp', 'fsdp')


def weight_specs():
    vec_spec = P(CHANNEL_AXES)
    layer_vec = P(None, CHANNEL_AXES)
    return (P('fsdp', 'tp'), vec_spec, layer_vec, layer_vec, P(None, None, 'fsdp'), P(None, 'fsdp'),
            P(None, 'fsdp', None), layer_vec, layer_vec, P(None, 'fsdp', 'tp'), layer_vec,
            P(None, CHANNEL_AXES, None), layer_vec, vec_spec, vec_spec, P('fsdp', 'tp'), P('tp'))


def solution(mesh):
    def step(patches, labels, w_stem, b_stem, ln1_g, ln1_b, w_tok1, b_tok1, w_tok2,
             ln2_g, ln2_b, w_ch1, b_ch1, w_ch2, b_ch2, lnf_g, lnf_b, w_head, b_head):
        wc, pat, xin, xmid, vin, pre, act, tok_act, tok_slope, hl, hr, dx0, hstat, gbh, vec, wt, wt_t = front(
            labels, patches.transpose(1, 0, 2), w_stem, w_ch1, w_ch2, w_head, w_tok1.transpose(0, 2, 1), w_tok2, b_tok1, b_ch1,
            b_head, b_stem, ln1_g, ln1_b, ln2_g, ln2_b, b_ch2, lnf_g, lnf_b)
        sums = back(xin, xmid, pre, wc, act, vin, pat, tok_act, tok_slope, hl, hr, dx0, hstat, gbh, wt, wt_t, vec)[:5]
        loss, g_s, g_bs, g_1g, g_1b, g_t1, g_bt, g_t2, g_2g, g_2b, g_c1, g_b1, g_c2, g_b2, g_fg, g_fb, g_h, g_bh = finish(*sums)
        return (loss.reshape(()), g_s, g_bs, g_1g, g_1b, g_t1.transpose(0, 2, 1), g_bt, g_t2, g_2g, g_2b, g_c1, g_b1, g_c2, g_b2,
                g_fg, g_fb, g_h, g_bh)

    specs = weight_specs()
    return jax.shard_map(step, mesh=mesh, in_specs=(P('fsdp', None, None), P('fsdp')) + specs,
                         out_specs=(P(),) + specs, check_vma=False)
```

```python
import functools

import jax
import jax.numpy as jnp
from jax import lax
from jax.experimental import pallas as pl
from jax.experimental.pallas import tpu as pltpu
from jax.sharding import PartitionSpec as P

MESH = pl.DeviceIdType.MESH
ORDERS = (('x', 'y', 'z'), ('y', 'z', 'x'), ('z', 'x', 'y'))
COLS = ((0, 384), (384, 384), (768, 256))
N_CH = 4
STEM, HEAD = 4, 5
bf16, f32 = jnp.bfloat16, jnp.float32


def my_place():
    f = lax.axis_index('fsdp')
    return {'x': lax.axis_index('tp'), 'z': f // 8, 'y': (f // 2) % 4, 'k': f % 2}


def moved(place, dim, step):
    new = dict(place)
    new[dim] = 1 - place['k'] if dim == 'k' else (place[dim] + step) % 4
    return new


def device(place):
    return {'tp': place['x'], 'fsdp': (place['z'] * 4 + place['y']) * 2 + place['k']}


EPS = 1e-6
TOK, TPAD = 49, 56
IMG = 8
ROWS, XROWS = IMG * TOK, IMG * TPAD
CHUNKS = ((0, 112), (112, 112), (224, 112), (336, 56))
CH, TOKH, CHH = 1024, 512, 4096
BLK = 512
NBLK = CHH // BLK
GELU_C, GELU_A = 0.7978845608028654, 0.044715


def dot_nn(a, b):
    return lax.dot_general(a, b, (((1,), (0,)), ((), ())), preferred_element_type=f32)


def dot_nt(a, b):
    return lax.dot_general(a, b, (((1,), (1,)), ((), ())), preferred_element_type=f32)


def dot_tn(a, b):
    return lax.dot_general(a, b, (((0,), (0,)), ((), ())), preferred_element_type=f32)


def gelu_both(x):
    sq = x * x
    half = 0.5 * jnp.tanh(x * (GELU_C + (GELU_C * GELU_A) * sq))
    rise = 0.5 + half
    value = x * rise
    return value, rise + value * (0.5 - half) * (2.0 * GELU_C + (6.0 * GELU_C * GELU_A) * sq)


def standardize(x):
    mean = jnp.mean(x, axis=-1, keepdims=True)
    cent = x - mean
    inv = lax.rsqrt(jnp.mean(cent * cent, axis=-1, keepdims=True) + EPS)
    return cent * inv, inv


def norm_grad(d, gain, std, inv):
    gs = d * gain
    m0 = jnp.mean(gs, axis=-1, keepdims=True)
    m1 = jnp.mean(gs * std, axis=-1, keepdims=True)
    return inv * (gs - m0 - std * m1)


def row_mask(rows=TPAD):
    return lax.broadcasted_iota(jnp.int32, (rows, 1), 0) < TOK


def image(b):
    return pl.ds(b, TPAD, stride=IMG)


def get(ref, rows):
    return jnp.concatenate([ref[n, rows, :] for n in range(CH // 128)], axis=1)


def put(ref, rows, value):
    for n in range(CH // 128):
        ref[n, rows, :] = value[:, 128 * n:128 * (n + 1)]


class Stream:
    def __init__(self, sem, copies, count):
        self.sem, self.copies, self.count = sem, copies, count

    def make(self, i, slot):
        return [pltpu.make_async_copy(src, dst, self.sem.at[slot, n]) for n, (src, dst) in enumerate(self.copies(i, slot))]

    def start(self, i, slot):
        for copy in self.make(i, slot):
            copy.start()

    def wait(self, i, slot):
        for copy in self.make(i, slot):
            copy.wait()


def for_blocks(stream, body, out=None):
    n = stream.count
    stream.start(0, 0)

    @pl.loop(0, n)
    def _(i):
        slot = i % 2
        stream.wait(i, slot)

        @pl.when(i + 1 < n)
        def _():
            stream.start(i + 1, 1 - slot)
        if out is not None:
            @pl.when(i >= 2)
            def _():
                out.wait(i - 2, slot)
        body(i, slot)
        if out is not None:
            out.start(i, slot)
    if out is not None:
        out.wait(n - 2, n % 2)
        out.wait(n - 1, 1 - n % 2)


TOK_CUTS = 4
FRONT_COPIES = 270
EARLY = [('stem', c) for c in range(3)] + [('ch', c, p) for p in 'ab' for c in range(3)] + [('head', 2)]
PARTS = {'a': pl.ds(0, 2), 'b': pl.ds(2, 2)}
LATE = [('stem', c, None) for c in range(3)] + [('ch', c, g) for g in range(N_CH) for c in range(3)] + [('head', 2, None)]
UNIT_GROUP = {('stem', None): 0, ('ch', 0): 1, ('ch', 1): 2, ('ch', 2): 3, ('ch', 3): 4, ('head', None): 5}
EVERY = pl.ds(0, 4)
FRONT_ORDER = (
    ('prep', (('M0', ('sm',)), ('M0', ('tk',)), ('A0', ('stem', 0)), ('A0', ('stem', 1)), ('A0', ('stem', 2)),
        ('A0', ('ch', 0, 'a')), ('A0', ('ch', 0, 'b')), ('A0', ('ch', 1, 'a')), ('A0', ('ch', 1, 'b')),
        ('A0', ('ch', 2, 'a')), ('A0', ('ch', 2, 'b')), ('A0', ('head', 2)),)),
    ('unpack', (('M1', ('sm',)), ('M1', ('tk',)), ('A', ('stem', 0)), ('A', ('stem', 1)), ('A', ('stem', 2)),
        ('A', ('ch', 0, 'a')), ('A', ('ch', 1, 'a')), ('A', ('ch', 2, 'a')), ('A', ('ch', 0, 'b')), ('A', ('ch', 2, 'b')),
        ('A', ('head', 2)), ('A', ('ch', 1, 'b')), ('B', ('stem', 0)), ('M2', ('sm',)), ('B', ('stem', 1)),
        ('B', ('ch', 0, 'a')), ('B', ('ch', 1, 'a')), ('B', ('ch', 0, 'b')), ('B', ('ch', 1, 'b')), ('M2', ('tk',)),
        ('B', ('stem', 2)), ('B', ('head', 2)), ('C', ('stem', 0)), ('B', ('ch', 2, 'a')), ('B', ('ch', 2, 'b')),
        ('M3', ('sm',)), ('C', ('stem', 2)), ('C', ('stem', 1)), ('C', ('head', 2)),)),
    ('stem0', (('D', ('stem', 0, None)), ('C', ('ch', 0, 'a')), ('C', ('ch', 1, 'a')), ('C', ('ch', 2, 'a')),
        ('D', ('stem', 2, None)), ('D', ('stem', 1, None)), ('D', ('ch', 2, 0)), ('D', ('ch', 2, 1)), ('D', ('ch', 0, 0)),
        ('D', ('ch', 0, 1)), ('E', ('stem', 0, None)), ('E', ('stem', 2, None)), ('E', ('stem', 1, None)),
        ('D', ('ch', 1, 0)), ('D', ('ch', 1, 1)), ('F', ('stem', 1, None)), ('E', ('ch', 2, 0)), ('E', ('ch', 0, 0)),
        ('E', ('ch', 2, 1)), ('F', ('stem', 2, None)), ('C', ('ch', 0, 'b')), ('C', ('ch', 1, 'b')), ('C', ('ch', 2, 'b')),
        ('D', ('head', 2, None)), ('E', ('ch', 1, 0)), ('F', ('ch', 2, 0)), ('E', ('ch', 0, 1)), ('F', ('stem', 0, None)),
        ('F', ('ch', 2, 1)), ('D', ('ch', 0, 2)), ('D', ('ch', 0, 3)),)),
    ('stem1', (('E', ('ch', 1, 1)),)),
    ('stem2', (('F', ('ch', 0, 0)), ('D', ('ch', 2, 2)), ('D', ('ch', 2, 3)),)),
    ('tok0_0', (('D', ('ch', 1, 2)), ('D', ('ch', 1, 3)), ('E', ('head', 2, None)),)),
    ('tok0_1', (('F', ('ch', 1, 0)),)),
    ('tok0_3', (('F', ('ch', 0, 1)),)),
    ('tok0_5', (('F', ('ch', 1, 1)), ('E', ('ch', 2, 2)),)),
    ('ch0_1', (('E', ('ch', 0, 2)), ('E', ('ch', 2, 3)),)),
    ('ch0_2', (('E', ('ch', 1, 2)), ('F', ('head', 2, None)),)),
    ('ch0_4', (('F', ('ch', 2, 2)),)),
    ('ch0_5', (('E', ('ch', 0, 3)), ('F', ('ch', 2, 3)),)),
    ('ch0_7', (('E', ('ch', 1, 3)),)),
    ('tok1_0', (('F', ('ch', 0, 2)),)),
    ('tok1_1', (('F', ('ch', 1, 2)),)),
    ('tok1_3', (('F', ('ch', 0, 3)),)),
    ('tok1_5', (('F', ('ch', 1, 3)),)),
)


class Net:
    def __init__(self, send_sems, recv_sems):
        self.send_sems, self.recv_sems, self.names, self.builds, self.done = send_sems, recv_sems, {}, [], set()

    def copy(self, name):
        n = self.names[name]
        src, dst, target = self.builds[n]()
        return pltpu.make_async_remote_copy(src_ref=src, dst_ref=dst, send_sem=self.send_sems.at[n],
                                            recv_sem=self.recv_sems.at[n], device_id=target, device_id_type=MESH)

    def start(self, name, build):
        self.names[name] = len(self.builds)
        self.builds.append(build)
        self.copy(name).start()

    def arrived(self, *names):
        for name in names:
            self.copy(name).wait_recv()

    def finish(self):
        for name in self.names:
            if name not in self.done:
                self.copy(name).wait_send()


def core_first(size, cols, each):
    half = cols // 2
    row = lax.broadcasted_iota(jnp.int32, (size, size), 0)
    col = lax.broadcasted_iota(jnp.int32, (size, size), 1)
    source = col % half // each * (2 * each) + col // half * each + col % each
    return jnp.where(row == source, 1.0, 0.0).astype(bf16)


def three_parts(x):
    hi = x.astype(bf16)
    rest = x - hi.astype(f32)
    mid = rest.astype(bf16)
    return hi, mid, (rest - mid.astype(f32)).astype(bf16)


def with_bias_rows(a):
    row = lax.broadcasted_iota(jnp.int32, (TPAD, 1), 0)
    return jnp.where(row < TOK, a, jnp.where(row < TOK + 3, 1.0, 0.0)).astype(bf16)


def front_kernel(labels, patches, w_stem, w_ch1, w_ch2, w_head, w_tok1, w_tok2, b_tok1, b_ch1, b_head, b_stem, ln1_g, ln1_b,
                 ln2_g, ln2_b, b_ch2, lnf_g, lnf_b,
                 wc, pat_out, xin, xmid, vout, pre_out, act_out, hl, hr, dx0, hstat, gbh, vec, wt, wt_t,
                 pc, ps, ph, tk_f, tk_p, sm_p, bh_p, ws, wh, tk_v, sm_v, sm_2, bh_v, bch1,
                 turn, p_v, pk_v, x_v, v_v, w1_v, w2_v, pre_v, act_v, g_v,
                 send_sems, recv_sems, sem, sem_w, sem_o, sem_x):
    me = my_place()
    other = moved(me, 'k', 1)
    load_p = pltpu.make_async_copy(patches.at[:, pl.ds(pl.multiple_of(me['x'] * IMG, IMG), IMG)], p_v, sem.at[0])
    load_p.start()

    barrier = pltpu.get_barrier_semaphore()
    for dim in 'xyz':
        for step in (1, 2, 3):
            pl.semaphore_signal(barrier, inc=1, device_id=device(moved(me, dim, step)), device_id_type=MESH)
    pl.semaphore_signal(barrier, inc=1, device_id=device(other), device_id_type=MESH)

    stem = dot_nn(w_stem[...].astype(bf16), core_first(256, 256, 32)).astype(bf16)
    ps[0], ps[1] = stem[:, 0:128], stem[:, 128:256]
    pick = core_first(1024, 1024, 32)
    for l in range(2):
        pc[2 * l] = dot_nn(w_ch1[l].astype(bf16), pick).astype(bf16)
        pc[2 * l + 1] = dot_nn(w_ch2[l].astype(bf16), pick).astype(bf16)
    ph[...] = jnp.zeros_like(ph)
    ph[:, pl.ds(0, 250)] = w_head[...].astype(bf16)
    turn[...] = jnp.zeros_like(turn)
    for n, ref in ((0, b_stem), (11, lnf_g), (12, lnf_b)):
        turn[n, pl.ds(0, 8)] = ref[...]
    for n, ref in enumerate((ln1_g, ln1_b, ln2_g, ln2_b, b_ch2)):
        for l in range(2):
            turn[pl.ds(1 + 5 * l + n, 1), pl.ds(0, 8)] = ref[pl.ds(l, 1), :]
    turn[pl.ds(16, 2), pl.ds(0, 16)] = b_tok1[...]
    turned = turn[...].T
    tk_f[...] = jnp.zeros_like(tk_f)
    for l in range(2):
        tk_f[l, :, pl.ds(0, TOK)] = w_tok1[l]
        tk_f[2 + l, :, pl.ds(0, TOK)] = w_tok2[l]
        for n, part in enumerate(three_parts(turned[0:16, 16 + l:17 + l])):
            tk_f[l, :, pl.ds(TOK + n, 1)] = part.astype(f32)
    tk_p[...] = tk_f[...].astype(bf16)
    sm_p[...] = jnp.zeros_like(sm_p)
    sm_p[:, pl.ds(0, 16)] = turned[0:8, 0:16]
    sm_p[pl.ds(0, 2), pl.ds(32, 32)] = b_ch1[...]
    bh_p[...] = jnp.full_like(bh_p, -1e30)
    bh_p[0, pl.ds(0, 250)] = b_head[...]

    net = Net(send_sems, recv_sems)
    core = me['k']
    ring = {d: [moved(me, d, n)[d] for n in range(4)] for d in 'xyz'}
    columns = [pl.ds(pl.multiple_of(x * 256, 256), 256) for x in ring['x']]
    stem_columns = [pl.ds(pl.multiple_of(x * 128, 128), 128) for x in ring['x']]
    peers = {(d, n): device(moved(me, d, n)) for d in 'xyz' for n in (1, 2, 3)}
    partner = device(other)
    here = {'x': 0, 'y': 0, 'z': 0}

    def view(unit, block, half=None):
        kind, colour = unit[:2]
        x, z, y = (EVERY if block[d] is None else ring[d][block[d]] for d in 'xzy')
        r0, rn = (0, 32) if half is None else (16 * half, 16)
        if kind == 'ch':
            c0, cn = COLS[colour]
            g = PARTS.get(unit[2], unit[2])
            return wc.at[g, x, core, z, y, pl.ds(r0, rn), pl.ds(c0, cn)]
        if kind == 'stem':
            cols = pl.ds(0, 512) if x is EVERY else stem_columns[block['x']]
            return ws.at[:, z, y, core, pl.ds(32 * colour + r0, rn), cols]
        cols = pl.ds(0, CH) if x is EVERY else columns[block['x']]
        return wh.at[core, z, y, pl.ds(r0, rn), cols]

    def piece(unit):
        kind, colour = unit[:2]
        if kind == 'ch':
            return pc.at[PARTS[unit[2]], :, pl.ds(*COLS[colour])]
        return ps.at[:, pl.ds(32 * colour, 32), :] if kind == 'stem' else ph.at[:, :]

    def exchange(unit, tag, dim, block):
        for side, step in (('l', 1), ('r', 3)):
            def build(step=step):
                part = view(unit, block)
                return (piece(unit) if tag == '1' else part), part, peers[dim, step]
            net.start((unit, tag, side), build)

    def forward_half(unit, tag, dim, block):
        for half, (origin, target, side) in enumerate(((3, 1, 'l'), (1, 3, 'r'))):
            def build(half=half, origin=origin, target=target):
                part = view(unit, {**block, dim: origin}, half)
                return part, part, peers[dim, target]
            net.start((unit, tag, side), build)

    def swap(unit, tag, block):
        def build():
            part = view(unit, block)
            return part, part, partner
        net.start((unit, tag), build)

    own = pltpu.make_async_copy(pc, wc.at[:, me['x'], me['k'], me['z'], me['y']], sem.at[1])
    own.start()
    mine = pl.ds(pl.multiple_of(me['x'] * 256, 256), 256)
    for n in range(2):
        ws[n, me['z'], me['y'], me['k'], :, stem_columns[0]] = ps[n]
    wh[me['k'], me['z'], me['y'], :, mine] = ph[...]
    sm_v[me['x'], me['z'], me['y'], me['k']] = sm_p[...]
    tk_v[:, me['z'], me['y'], me['k']] = tk_p[...]
    bh_v[:, mine] = bh_p[...]
    own.wait()
    pl.semaphore_wait(barrier, 10)

    def small(kind, n):
        dims = 'xyz' if kind == 'sm' else 'yz'
        at = {d: EVERY if d in dims[:n] else ring[d][0] for d in 'xyz'}

        def part():
            if kind == 'sm':
                return sm_v.at[at['x'], at['z'], at['y'], core]
            return tk_v.at[:, at['z'], at['y'], core]
        if n > 0:
            net.arrived(*[(kind, n - 1, s) for s in (1, 2, 3)])
        if n < len(dims):
            for s in (1, 2, 3):
                net.start((kind, n, s), lambda s=s: (part(), part(), peers[dims[n], s]))
            if kind == 'sm' and n == 0:
                def head_bias():
                    return bh_v.at[:, columns[0]]
                for s in (1, 2, 3):
                    net.start(('bh', s), lambda s=s: (head_bias(), head_bias(), peers['x', s]))
        else:
            net.start((kind, 'k'), lambda: (part(), part(), partner))

    def step(name, unit):
        if name[0] == 'M':
            small(unit[0], int(name[1]))
            return
        d1, d2, d3 = ORDERS[unit[1]]
        early = unit[:2] if unit[0] != 'ch' or unit[2] in PARTS else ('ch', unit[1], 'a' if unit[2] < 2 else 'b')
        plane = {**here, d1: None, d2: None}
        if name == 'A0':
            exchange(unit, '1', d1, here)
        elif name == 'A':
            net.arrived((unit, '1', 'l'), (unit, '1', 'r'))
            forward_half(unit, '1h', d1, here)
        elif name == 'B':
            net.arrived((unit, '1h', 'l'), (unit, '1h', 'r'))
            exchange(unit, '2', d2, {**here, d1: None})
        elif name == 'C':
            net.arrived((unit, '2', 'l'), (unit, '2', 'r'))
            forward_half(unit, '2h', d2, {**here, d1: None})
        elif name == 'D':
            if early not in planes:
                planes.add(early)
                net.arrived((early, '2h', 'l'), (early, '2h', 'r'))
            exchange(unit, '3', d3, plane)
            swap(unit, 'k0', plane)
        elif name == 'E':
            net.arrived((unit, '3', 'l'), (unit, '3', 'r'))
            forward_half(unit, '3h', d3, plane)
            for n in (1, 3):
                swap(unit, f'k{n}', {**plane, d3: n})
        else:
            net.arrived((unit, '3h', 'l'), (unit, '3h', 'r'))
            swap(unit, 'k2', {**plane, d3: 2})

    planes = set()
    awaited = set()

    def need(group):
        for u in LATE:
            if UNIT_GROUP[u[0], u[2]] <= group and u not in awaited:
                awaited.add(u)
                net.arrived(*[(u, f'k{n}') for n in range(4)])

    bursts = {name: steps for name, steps in FRONT_ORDER}

    def burst(name):
        for s in bursts.get(name, ()):
            step(*s)

    def during(name, count):
        def run(i):
            for n in range(1, count):
                if bursts.get(f'{name}{n}'):
                    pl.when(i == n)(functools.partial(burst, f'{name}{n}'))
        return run

    burst('prep')
    load_p.wait()
    pick = core_first(768, 768, 96)
    for g in range(4):
        part = dot_nn(p_v[:, :, pl.ds(768 * g, 768)].reshape(ROWS, 768), pick).astype(bf16)
        for n in range(2):
            pk_v[n, :, pl.ds(384 * g, 384)] = part[:, 384 * n:384 * n + 384]
    keep_p = pltpu.make_async_copy(pk_v, pat_out, sem.at[0])
    keep_p.start()

    burst('unpack')
    net.arrived(('sm', 'k'), ('tk', 'k'), ('bh', 1), ('bh', 2), ('bh', 3))
    sm_2[...] = sm_v[...].reshape(1024, 128)
    for n in range(8):
        tile = jnp.concatenate([sm_2[pl.ds((n % 4 * 4 + i) * 64 + n // 4 * 32, 32), :] for i in range(4)], axis=0)
        vec[:, pl.ds(128 * n, 128)] = tile.T[0:16, :]
    wt[...] = tk_v[...].reshape(4, TOKH, 128)
    for n in range(4):
        wt_t[n] = wt[n].astype(f32).T[0:TPAD].astype(bf16)
    for l in range(2):
        rows = jnp.concatenate(three_parts(sm_2[pl.ds(l, 128, stride=8), :]), axis=0)

        @pl.loop(0, 8)
        def _(n):
            lane = lax.broadcasted_iota(jnp.int32, (128, 512), 0)
            col = lax.broadcasted_iota(jnp.int32, (128, 512), 1)
            pick = jnp.where(lane == 32 + col % 32, 1.0, 0.0).astype(bf16)
            spread = dot_nn(rows, pick)
            value = spread[0:128] + spread[128:256] + spread[256:384]
            mine = lane == n // 2 * 32 + col // 32 * 2 + n % 2
            bch1[l:l + 1, pl.ds(pl.multiple_of(n * 512, 512), 512)] = jnp.sum(jnp.where(mine, value, 0.0), axis=0, keepdims=True)

    burst('stem0')
    need(0)
    run = during('stem', 4)
    put(x_v, pl.ds(ROWS, XROWS - ROWS), jnp.zeros((XROWS - ROWS, CH), f32))

    @pl.loop(0, 4)
    def _(i):
        run(i)
        cols = pl.ds(pl.multiple_of(i * 256, 256), 256)
        w = ws[i // 2, :, :, :, :, pl.ds(pl.multiple_of(i % 2 * 256, 256), 256)].reshape(3072, 256)
        value = dot_nn(p_v[...].reshape(ROWS, 3072), w) + vec[0:1, cols]
        for n in range(2):
            x_v[2 * i + n, pl.ds(0, ROWS), :] = value[:, 128 * n:128 * (n + 1)]

    wc_all = wc

    def add_rows(value):
        for n in range(CH // 128):
            x_v[n, pl.ds(0, ROWS), :] += value[:, 128 * n:128 * (n + 1)]

    for l in range(2):
        r = 1 + 5 * l
        burst(f'tok{l}_0')
        run = during(f'tok{l}_', IMG)
        save_in = pltpu.make_async_copy(x_v.at[:, pl.ds(0, ROWS)], xin.at[l], sem_x.at[0])
        save_in.start()
        save_in.wait()

        @pl.loop(0, IMG)
        def _(b):
            run(b)
            x = get(x_v, image(b))
            std, _ = standardize(x)
            a = with_bias_rows(std * vec[r:r + 1, :] + vec[r + 1:r + 2, :])
            g_v[...] = gelu_both(dot_nn(wt[l, :, 0:TPAD], a))[0].astype(bf16)
            put(x_v, image(b), x + dot_nn(wt_t[2 + l], g_v[...]))
        save_mid = pltpu.make_async_copy(x_v.at[:, pl.ds(0, ROWS)], xmid.at[l], sem_x.at[0])
        save_mid.start()
        burst(f'ln{l}')

        for at, size in CHUNKS:
            std, _ = standardize(get(x_v, pl.ds(at, size)))
            v_v[pl.ds(at, size), :] = (std * vec[r + 2:r + 3, :] + vec[r + 3:r + 4, :]).astype(bf16)
        save_v = [pltpu.make_async_copy(v_v.at[:, pl.ds(512 * n, 512)], vout.at[l, n], sem_x.at[1 + n]) for n in range(2)]
        for copy in save_v:
            copy.start()
        burst(f'ch{l}_0')
        need(2 + 2 * l)
        save_mid.wait()

        def blocks(i, slot):
            t, h = i // 2, i % 2
            part = pl.ds(pl.multiple_of(h * BLK, BLK), BLK)
            return [(wc_all.at[2 * l, t, :, :, :, :, part], w1_v.at[slot]), (wc_all.at[2 * l + 1, t, h], w2_v.at[slot])]

        def outs(i, slot):
            part = pl.ds(pl.multiple_of(i * BLK, BLK), BLK)
            half = pl.ds(pl.multiple_of(i // 2 * BLK, BLK), BLK)
            return [(pre_v.at[slot], pre_out.at[l, :, part]), (act_v.at[slot], act_out.at[l, i % 2, :, half])]
        run = during(f'ch{l}_', NBLK)

        def channel(i, slot):
            run(i)
            part = pl.ds(pl.multiple_of(i * BLK, BLK), BLK)
            h = dot_nn(v_v[...], w1_v[slot].reshape(CH, BLK)) + bch1[l:l + 1, part]
            value, pre_v[slot] = gelu_both(h)
            act_v[slot] = value.astype(bf16)
            add_rows(dot_nn(act_v[slot], w2_v[slot].reshape(BLK, CH)))
        for_blocks(Stream(sem_w, blocks, NBLK), channel, Stream(sem_o, outs, NBLK))
        add_rows(jnp.broadcast_to(vec[r + 4:r + 5, :], (ROWS, CH)))
        for copy in save_v:
            copy.wait()

    burst('head')
    need(5)
    keep_p.wait()
    last = 11
    pooled = jnp.sum(get(x_v, pl.ds(0, ROWS)).reshape(TOK, IMG, CH), axis=0) * (1.0 / TOK)
    std, inv = standardize(pooled)
    head_in = (std * vec[last:last + 1, :] + vec[last + 1:last + 2, :]).astype(bf16)
    hl[...] = head_in
    w_h = wh[...].reshape(CH, CH)
    logits = dot_nn(head_in, w_h) + bh_v[0:1, :]
    row = lax.broadcasted_iota(jnp.int32, (IMG, 1), 0)
    label = jnp.zeros((IMG, 1), jnp.int32)
    for b in range(IMG):
        value = labels[me['x'] * IMG + b]
        label = jnp.where(row == b, value, label)
    label = label + 6 * sum(jnp.where(label >= edge, 1, 0) for edge in (250, 500, 750))
    is_label = lax.broadcasted_iota(jnp.int32, logits.shape, 1) == label
    top = jnp.max(logits, axis=-1, keepdims=True)
    ex = jnp.exp(logits - top)
    es = jnp.sum(ex, axis=-1, keepdims=True)
    nll = top + jnp.log(es) - jnp.sum(jnp.where(is_label, logits, 0.0), axis=-1, keepdims=True)
    d_logits = (ex / es - jnp.where(is_label, 1.0, 0.0)) * (1.0 / 1024)
    gbh[...] = jnp.sum(d_logits, axis=0, keepdims=True)
    d_bf = d_logits.astype(bf16)
    hr[...] = d_bf
    d_in = dot_nt(d_bf, w_h)
    hstat[0:1, :] = jnp.sum(d_in * std, axis=0, keepdims=True)
    hstat[1:2, :] = jnp.sum(d_in, axis=0, keepdims=True)
    hstat[2:3, :] = jnp.broadcast_to(jnp.sum(nll, axis=0, keepdims=True), (1, CH))
    dx0[...] = norm_grad(d_in, vec[last:last + 1, :], std, inv) * (1.0 / TOK)
    burst('end')
    net.finish()
    assert len(net.builds) <= FRONT_COPIES, len(net.builds)


def front(*operands):
    a, v = pl.BlockSpec(memory_space=pl.ANY), pl.BlockSpec(memory_space=pltpu.VMEM)
    S, V, DMA = jax.ShapeDtypeStruct, pltpu.VMEM, pltpu.SemaphoreType.DMA
    return pl.pallas_call(
        front_kernel, name='front',
        in_specs=[pl.BlockSpec(memory_space=pltpu.SMEM), a] + [v] * 17,
        out_specs=[a] * 7 + [v] * 8,
        out_shape=[S((N_CH, 4, 2, 4, 4, 32, 1024), bf16), S((2, ROWS, 1536), bf16), S((2, CH // 128, ROWS, 128), f32),
                   S((2, CH // 128, ROWS, 128), f32),
                   S((2, 2, ROWS, 512), bf16), S((2, ROWS, CHH), f32), S((2, 2, ROWS, 2048), bf16), S((IMG, CH), bf16),
                   S((IMG, CH), bf16), S((IMG, CH), f32), S((8, CH), f32), S((1, CH), f32), S((16, CH), f32),
                   S((4, TOKH, 128), bf16), S((4, TPAD, TOKH), bf16)],
        scratch_shapes=[V((N_CH, 32, 1024), bf16), V((2, 96, 128), bf16), V((32, 256), bf16), V((4, 16, 128), f32),
                        V((4, 16, 128), bf16), V((8, 128), f32), V((8, 256), f32), V((2, 4, 4, 2, 96, 512), bf16),
                        V((2, 4, 4, 32, CH), bf16), V((4, 4, 4, 2, 16, 128), bf16), V((4, 4, 4, 2, 8, 128), f32),
                        V((1024, 128), f32), V((8, CH), f32), V((2, CHH), f32),
                        V((128, 128), f32), V((TOK, IMG, 3072), bf16), V((2, ROWS, 1536), bf16), V((CH // 128, XROWS, 128), f32),
                        V((ROWS, CH), bf16), V((2, 2, 4, 4, 32, BLK), bf16), V((2, 4, 4, 32, CH), bf16),
                        V((2, ROWS, BLK), f32), V((2, ROWS, BLK), bf16), V((TOKH, CH), bf16),
                        DMA((FRONT_COPIES,)), DMA((FRONT_COPIES,)), DMA((2,)), DMA((2, 2)), DMA((2, 2)), DMA((3,))],
        compiler_params=pltpu.CompilerParams(collective_id=0, has_side_effects=True, vmem_limit_bytes=62 * 1024 * 1024),
        cost_estimate=pl.CostEstimate(flops=90_000_000_000, bytes_accessed=180_000_000, transcendentals=0),
    )(*operands)


GROUPS = (3, 2, 1, HEAD, 0, STEM)
UNITS = tuple((g, c) for g in GROUPS for c in (2, 0, 1) if g != HEAD or c == 2)
BACK_COPIES = 18 * len(UNITS) + 40
NEEDS = {3: ('act1', 'dout1'), 2: ('vin1',), 1: ('act0', 'dout0'), 0: ('vin0',), STEM: ('pat', 'dres'),
         HEAD: ('hl', 'hr')}
BACK_ORDER = (
    ('c1_7', ((3, 'L'),)),
    ('t1_7', ((0, 0), (0, 1), (1, 0), (1, 1),)),
    ('d0', ((0, 2),)),
    ('c0_3', ((1, 2), (0, 3),)),
    ('l0', ((1, 3), (0, 4),)),
    ('t0_1', ((1, 4), (0, 5),)),
    ('t0_3', ((1, 5), (0, 6),)),
    ('t0_4', ((2, 0), (2, 'L'), (2, 1), (1, 6), (0, 7),)),
    ('t0_5', ((3, 0), (3, 1), (1, 7), (4, 0), (4, 1), (2, 2),)),
    ('t0_6', ((3, 2), (5, 0), (1, 'L'), (5, 1),)),
    ('t0_7', ((4, 2), (2, 3), (3, 3),)),
    ('fin', ((6, 0), (6, 1), (5, 2), (2, 4), (7, 0), (7, 1), (4, 3), (3, 4), (8, 0), (0, 'L'), (8, 1), (6, 2), (4, 4),
        (2, 5), (5, 3), (9, 0), (9, 1), (7, 2),)),
    ('end', ((8, 2), (5, 4), (3, 5), (6, 3), (2, 6), (10, 0), (10, 1), (9, 2), (11, 0), (11, 1), (6, 4), (4, 5), (7, 3),
        (5, 5), (2, 7), (12, 0), (4, 'L'), (12, 1), (8, 3), (7, 4), (10, 2), (3, 6), (11, 2), (4, 6), (8, 4), (6, 5),
        (12, 2), (9, 3), (5, 6), (13, 0), (13, 1), (9, 4), (7, 5), (11, 3), (8, 5), (6, 6), (3, 7), (4, 7), (5, 7), (14, 0),
        (14, 1), (15, 0), (15, 1), (9, 5), (10, 3), (12, 3), (8, 6), (11, 4), (13, 2), (6, 7), (14, 2), (7, 6), (15, 2),
        (12, 4), (10, 4), (8, 7), (9, 6), (11, 5), (7, 7), (14, 3), (12, 5), (10, 5), (13, 3), (15, 3), (11, 6), (9, 7),
        (12, 6), (14, 4), (13, 4), (10, 6), (15, 4), (11, 7), (12, 7), (14, 5), (10, 7), (13, 5), (15, 5), (14, 6), (13, 6),
        (15, 6), (14, 7), (13, 7), (15, 7),)),
)
SMALL = dict(sm=((4, 4, 4, 8, 128), (3, 4, 4, 8, 128), (3, 4, 8, 128), (3, 8, 128)),
             tk=((4, 4, 4, 16, 128), (3, 4, 4, 16, 128), (3, 4, 16, 128), (3, 4, 16, 128)))


def reduce_scratch():
    per = []
    for c in range(3):
        n = COLS[c][1]
        many = sum(1 for u in UNITS if u[1] == c)
        lead = ((4, 4), (4,), ())
        b = {'C': pltpu.VMEM((2, 4, 4, 4, 32, n), bf16), 'S1': pltpu.VMEM((4, 4, 32, n), f32), 'S2': pltpu.VMEM((2, 4, 32, n), f32)}
        for ph in range(3):
            if ph:
                b[f'opp{ph}'] = pltpu.VMEM(lead[ph] + (32, n), bf16)
                b[f'pr{ph}'] = pltpu.VMEM(lead[ph] + (16, n), bf16)
                b[f'pl{ph}'] = pltpu.VMEM(lead[ph] + (16, n), bf16)
            for name in ('rig', 'lef'):
                b[f'{name}{ph}'] = pltpu.VMEM(lead[ph] + (16, n), bf16)
            for name in ('half0', 'half1'):
                b[f'{name}{ph}'] = pltpu.VMEM((many,) + lead[ph] + (16, n), bf16)
            for name in ('froml', 'fromr'):
                b[f'{name}{ph}'] = pltpu.VMEM((many,) + lead[ph] + (32, n), bf16)
        per.append(b)
    return per


def small_scratch():
    b = {f'{kind}{n + 1}': pltpu.VMEM(shape, f32) for kind, shapes in SMALL.items() for n, shape in enumerate(shapes)}
    b.update(sm=pltpu.VMEM((4, 4, 4, 2, 8, 128), f32), tk=pltpu.VMEM((4, 4, 4, 2, 16, 128), f32),
             sm_s1=pltpu.VMEM((4, 4, 8, 128), f32), sm_s2=pltpu.VMEM((4, 8, 128), f32),
             tk_s1=pltpu.VMEM((4, 4, 16, 128), f32), tk_s2=pltpu.VMEM((4, 16, 128), f32))
    return b


def small_pack(b, flat, turn, gvec, hstat, gbch1, gbh):
    for n in range(8):
        cols = pl.ds(128 * n, 128)
        turn[n, pl.ds(0, 128), :] = jnp.zeros((128, 128), f32)
        turn[n, pl.ds(0, 16), :] = gvec[:, cols]
        turn[n, pl.ds(11, 2), :] = hstat[pl.ds(0, 2), cols]
    for n in range(8):
        tile = turn[n, pl.ds(0, 128), :].T
        for i in range(4):
            a = n % 4 * 4 + i
            flat[a // 2, pl.ds(a % 2 * 64 + n // 4 * 32, 32), :] = tile[32 * i:32 * i + 32]
    for l in range(2):
        def gather(n, total):
            lane = lax.broadcasted_iota(jnp.int32, (128, 512), 0)
            col = lax.broadcasted_iota(jnp.int32, (128, 512), 1)
            sums = gbch1[l:l + 1, pl.ds(pl.multiple_of(512 * n, 512), 512)]
            mine = jnp.where(lane == n // 2 * 32 + col // 32 * 2 + n % 2, sums, 0.0)
            pick = jnp.where(lane == 32 + col % 32, 1.0, 0.0).astype(bf16)
            return total + dot_nt(jnp.concatenate(three_parts(mine), axis=0), pick)
        total = lax.fori_loop(0, 8, gather, jnp.zeros((384, 128), f32))
        total = total[0:128] + total[128:256] + total[256:384]
        for n in range(8):
            flat[n, pl.ds(l, 16, stride=8), :] += total[16 * n:16 * n + 16]
    lane = lax.broadcasted_iota(jnp.int32, (1, 128), 1)
    for t in range(4):
        for q in range(4):
            tile = gbh[0:1, t * 256 + q // 2 * 128:t * 256 + q // 2 * 128 + 128]
            if q % 2 == 0:
                tile = jnp.concatenate([tile[:, 64:], tile[:, :64]], axis=1)
            tile = jnp.where(lane >= 64, tile, 0.0)
            for n in (2 * t, 2 * t + 1):
                flat[n, pl.ds(2 + q, 16, stride=8), :] += tile
    for n in range(8):
        flat[n, pl.ds(6, 16, stride=8), :] += jnp.where(lane == 64, hstat[2:3, 0:128], 0.0)
        b['sm'][n // 2, pl.ds(n % 2 * 2, 2)] = flat[n, pl.ds(0, 128), :].reshape(2, 4, 2, 8, 128)


def back_kernel(*refs):
    xin, xmid, pre_in, wc, act, vin, pat = refs[:7]
    hl, hr, dx0, hstat, gbh, wt, wt_t, vec = refs[7:15]
    out_c, out_s, out_h, sm_own, tk_own = refs[15:20]
    dpre, dout, dres, x_act, x_vin, x_pat, x_dpre, x_dout, x_dres = refs[20:29]
    (per, b, big, little, x_hl, x_hr, gvec, gbch1, x_v, d_v, dv_v, do_v, w1_v, w2_v, pre_v, dp_v,
     send_sems, recv_sems, load_sems, sem, sem_w, sem_o, ship_sent, ship_got) = refs[29:]
    me = my_place()
    other = moved(me, 'k', 1)
    k, k2 = me['k'], 1 - me['k']
    barrier = pltpu.get_barrier_semaphore()
    for dim in 'xyz':
        for step in (1, 2, 3):
            pl.semaphore_signal(barrier, inc=1, device_id=device(moved(me, dim, step)), device_id_type=MESH)
    pl.semaphore_signal(barrier, inc=1, device_id=device(other), device_id_type=MESH)
    net = Net(send_sems, recv_sems)
    ring = {d: [moved(me, d, n)[d] for n in range(4)] for d in 'xyz'}
    peers = {(d, n): device(moved(me, d, n)) for d in 'xyz' for n in (1, 2, 3)}
    partner = device(other)
    half_at = pl.ds(pl.multiple_of(k * 512, 512), 512)
    half_to = pl.ds(pl.multiple_of(k2 * 512, 512), 512)
    swaps = {'act1': (act.at[1, k2], x_act.at[1]), 'act0': (act.at[0, k2], x_act.at[0]), 'vin1': (vin.at[1, k2], x_vin.at[1]),
             'vin0': (vin.at[0, k2], x_vin.at[0]), 'pat': (pat.at[k2], x_pat), 'dout1': (do_v, x_dout.at[1]), 'dout0': (do_v, x_dout.at[0]), 'dres': (do_v, x_dres),
             'hl': (hl.at[:, half_to], x_hl), 'hr': (hr, x_hr)}

    def swap(*names):
        for name in names:
            net.start(name, lambda name=name: (*swaps[name], partner))
    busy = {}

    def free(key):
        for name in busy.pop(key, ()):
            net.copy(name).wait_send()
            net.done.add(name)

    def ship(l, i, slot):
        part = pl.ds(pl.multiple_of(i * BLK, BLK), BLK)
        return pltpu.make_async_remote_copy(src_ref=dp_v.at[slot], dst_ref=x_dpre.at[l, :, part], send_sem=ship_sent.at[slot],
                                            recv_sem=ship_got.at[l], device_id=partner, device_id_type=MESH)

    def shipped(l):
        pltpu.make_async_remote_copy(src_ref=dpre.at[l], dst_ref=x_dpre.at[l], send_sem=ship_sent.at[0],
                                     recv_sem=ship_got.at[l], device_id=partner, device_id_type=MESH).wait_recv()

    def loads(g):
        l = g // 2
        if g == STEM:
            wide, tall = (pat.at[k], x_pat, 1536), (dres, x_dres, CH)
        elif g % 2:
            wide, tall = (act.at[l, k], x_act.at[l], 2048), (dout.at[l], x_dout.at[l], CH)
        else:
            wide, tall = (dpre.at[l], x_dpre.at[l], CHH), (vin.at[l, k], x_vin.at[l], 512)
        out = []
        for n, (buf, (own, far, cols)) in enumerate(((big, wide), (little, tall))):
            out += [pltpu.make_async_copy(own, buf.at[0, :, pl.ds(0, cols)], load_sems.at[2 * n]),
                    pltpu.make_async_copy(far, buf.at[1, :, pl.ds(0, cols)], load_sems.at[2 * n + 1])]
        return out

    def product(u):
        g, c, slot = u.g, u.c, u.slot
        first = c == 2
        if first and g != HEAD:
            for copy in loads(g):
                copy.wait()
        if g == STEM and not first:
            return
        for v in (units if g == STEM else (u,)):
            if v.g == g:
                free(('C', v.c, v.slot))
        if g == HEAD:
            net.arrived(*NEEDS[g])
            for t in range(4):
                cols = pl.ds(256 * t, 256)
                prod = dot_tn(hl[:, half_at], hr[:, cols]) + dot_tn(x_hl[...], x_hr[:, cols])
                per[c]['C'][slot, t] = prod.astype(bf16).reshape(4, 4, 32, 256)
        elif g == STEM:
            slots = {v.c: v.slot for v in units if v.g == STEM}

            @pl.loop(0, 4)
            def _(z):
                rows = pl.ds(pl.multiple_of(z * 384, 384), 384)
                for t in range(4):
                    def right(s):
                        return jnp.concatenate([little[s, :, 128 * t:128 * t + 128], little[s, :, 512 + 128 * t:640 + 128 * t]], axis=1)
                    prod = dot_tn(big[0, :, rows], right(0)) + dot_tn(big[1, :, rows], right(1))
                    prod = prod.astype(bf16).reshape(4, 3, 32, 256)
                    for d in range(3):
                        per[d]['C'][slots[d], t, z, :, :, pl.ds(0, 256)] = prod[:, d]
        else:
            c0, n = COLS[c]

            @pl.loop(0, 4)
            def _(t):
                for h in range(2):
                    if g % 2:
                        left = pl.ds(pl.multiple_of(t * 512 + h * 256, 256), 256)
                        prod = dot_tn(big[0, :, left], little[0, :, c0:c0 + n]) + dot_tn(big[1, :, left], little[1, :, c0:c0 + n])
                    else:
                        right = pl.ds(pl.multiple_of(t * 1024 + c0, 128), n)
                        rows = slice(256 * h, 256 * h + 256)
                        prod = dot_tn(little[0, :, rows], big[0, :, right]) + dot_tn(little[1, :, rows], big[1, :, right])
                    per[c]['C'][slot, t, 2 * h:2 * h + 2] = prod.astype(bf16).reshape(2, 4, 32, n)

    class Unit:
        def __init__(self, g, c):
            self.g, self.c = g, c
            self.index = [u for u in UNITS if u[1] == c].index((g, c))
            self.slot = self.index % 2
            self.n = COLS[c][1] if g < N_CH else 256
            self.cols = pl.ds(0, self.n)
            self.buf = per[c]
            self.dims = ORDERS[c]
            self.rest = [d for d in 'xzy' if d != self.dims[0]]

        def cut(self, name, *at, rows=slice(None)):
            ref = self.buf[name]
            inner = [slice(None)] * (len(ref.shape) - len(at) - 2)
            return ref.at[(*at, *inner, rows, self.cols)]

        def block(self, p, rows):
            at = {d: EVERY for d in 'xzy'}
            at[self.dims[0]] = p
            return self.buf['C'].at[self.slot, at['x'], at['z'], at['y'], rows, self.cols]

        def share(self, phase, p, e, rows):
            if phase == 0:
                at = dict(zip(self.rest, e))
                at[self.dims[0]] = p
                return self.buf['C'][self.slot, at['x'], at['z'], at['y'], rows, self.cols].astype(f32)
            if phase == 1:
                at = (p, e[0]) if self.dims[1] == self.rest[0] else (e[0], p)
                return self.buf['S1'][(*at, rows, self.cols)]
            return self.buf['S2'][self.slot, p, rows, self.cols]

        def each(self, phase, body):
            if phase == 2:
                body(())
            elif phase == 1:
                pl.loop(0, 4)(lambda i: body((i,)))
            else:
                @pl.loop(0, 4)
                def _(i):
                    pl.loop(0, 4)(lambda j: body((i, j)))

        def send(self, tag, phase, src, dst, step):
            name = (self.g, self.c, tag, phase)
            net.start(name, lambda: (src(), dst(), peers[self.dims[phase], step]))
            return name

        def arrived(self, phase, *tags):
            net.arrived(*[(self.g, self.c, tag, phase) for tag in tags])

        def opposite(self, phase):
            places = ring[self.dims[phase]]
            low, high = pl.ds(0, 16), pl.ds(16, 16)
            if phase == 0:
                sources = [lambda: self.block(places[2], low), lambda: self.block(places[2], high),
                           lambda: self.block(places[1], high), lambda: self.block(places[3], low)]
            else:
                names = (f'opp{phase}', f'pr{phase}', f'pl{phase}')
                for name in names:
                    free((name, self.c))
                opp, right, left = (self.buf[name] for name in names)

                def body(e):
                    opp[(*e, slice(None), self.cols)] = self.share(phase, places[2], e, pl.ds(0, 32)).astype(bf16)
                    right[(*e, slice(None), self.cols)] = self.share(phase, places[1], e, high).astype(bf16)
                    left[(*e, slice(None), self.cols)] = self.share(phase, places[3], e, low).astype(bf16)
                self.each(phase, body)
                sources = [lambda: self.cut(names[0], rows=low), lambda: self.cut(names[0], rows=high),
                           lambda: self.cut(names[1]), lambda: self.cut(names[2])]
            targets = [lambda: self.cut(f'half0{phase}', self.index), lambda: self.cut(f'half1{phase}', self.index),
                       lambda: self.cut(f'froml{phase}', self.index, rows=high),
                       lambda: self.cut(f'fromr{phase}', self.index, rows=low)]
            sent = [self.send(tag, phase, src, dst, step)
                    for tag, src, dst, step in zip(('h0', 'h1', 'p0', 'p1'), sources, targets, (1, 3, 1, 3))]
            if phase == 0:
                busy['C', self.c, self.slot] = sent
            else:
                busy[names[0], self.c] = sent[:2]
                busy[names[1], self.c] = sent[2:3]
                busy[names[2], self.c] = sent[3:]

        def beside(self, phase):
            places = ring[self.dims[phase]]
            for half, step, name, dst in ((0, 1, 'rig', 'froml'), (1, 3, 'lef', 'fromr')):
                self.arrived(phase, f'h{half}')
                key = f'{name}{phase}'
                free((key, self.c))
                out, got = self.buf[key], self.buf[f'half{half}{phase}']
                rows = pl.ds(16 * half, 16)

                def body(e):
                    value = self.share(phase, places[step], e, rows) + got[(self.index, *e, slice(None), self.cols)].astype(f32)
                    out[(*e, slice(None), self.cols)] = value.astype(bf16)
                self.each(phase, body)
                busy[key, self.c] = [self.send(f'f{half}', phase, lambda key=key: self.cut(key),
                                               lambda dst=dst, rows=rows: self.cut(f'{dst}{phase}', self.index, rows=rows), step)]

        def total(self, phase):
            self.arrived(phase, 'p0', 'p1', 'f0', 'f1')
            p = ring[self.dims[phase]][0]

            def body(e):
                got = [self.buf[f'{name}{phase}'][(self.index, *e, slice(None), self.cols)].astype(f32)
                       for name in ('froml', 'fromr')]
                value = self.share(phase, p, e, pl.ds(0, 32)) + got[0] + got[1]
                if phase == 0:
                    self.buf['S1'][(*e, slice(None), self.cols)] = value
                elif phase == 1:
                    self.buf['S2'][(self.slot, *e, slice(None), self.cols)] = value
                elif self.g == STEM:
                    out_s[pl.ds(32 * self.c, 32), :] = value
                elif self.g == HEAD:
                    out_h[...] = value
                else:
                    out_c[self.g, :, pl.ds(*COLS[self.c])] = value
            self.each(phase, body)

        def run(self, stage):
            if stage == 0:
                product(self)
            elif stage == 7:
                self.total(2)
            elif stage % 2 == 0:
                self.beside(stage // 2 - 1)
            else:
                if stage > 1:
                    self.total(stage // 2 - 1)
                self.opposite(stage // 2)

    units = [Unit(g, c) for g, c in UNITS]
    bursts = dict(BACK_ORDER)

    def step(which, stage):
        if stage == 'L':
            net.arrived(*NEEDS[which])
            if which in (0, 2):
                shipped(which // 2)
            for copy in loads(which):
                copy.start()
        else:
            units[which].run(stage)

    def burst(name):
        for s in bursts.get(name, ()):
            step(*s)

    def during(name, count):
        def run(i):
            for n in range(1, count):
                if bursts.get(f'{name}{n}'):
                    pl.when(i == n)(functools.partial(burst, f'{name}{n}'))
        return run

    load = pltpu.make_async_copy(xmid.at[1], x_v.at[:, pl.ds(0, ROWS)], sem.at[0])
    load.start()
    mask = row_mask()
    rest = pl.ds(ROWS, XROWS - ROWS)
    put(d_v, rest, jnp.zeros((XROWS - ROWS, CH), f32))
    put(x_v, rest, jnp.zeros((XROWS - ROWS, CH), f32))
    gvec[...] = jnp.zeros_like(gvec)
    tk = b['tk']
    tk[...] = jnp.zeros_like(tk)

    @pl.loop(0, TOK)
    def _(s):
        put(d_v, pl.ds(pl.multiple_of(s * IMG, IMG), IMG), dx0[...])

    def add(row, value):
        gvec[row:row + 1, :] += jnp.sum(value, axis=0, keepdims=True)

    def add_token(n, value, start=0):
        tk[n, :, :, :, :, pl.ds(start, value.shape[1])] += value.reshape(4, 4, 2, 16, value.shape[1])

    for l in (1, 0):
        r = 1 + 5 * l
        free('do')
        for at, size in CHUNKS:
            d = get(d_v, pl.ds(at, size))
            add(r + 4, d)
            do_v[pl.ds(at, size), :] = d.astype(bf16)
        keep = pltpu.make_async_copy(do_v, dout.at[l], sem.at[1])
        keep.start()
        if l == 1:
            pl.semaphore_wait(barrier, 10)
            swap('dout1', 'act1', 'hl', 'hr', 'vin1', 'act0', 'vin0', 'pat')
        else:
            swap('dout0')
        busy['do'] = [f'dout{l}']
        keep.wait()
        burst(f'c{l}_0')
        run = during(f'c{l}_', NBLK)

        def blocks(i, slot):
            t, h = i // 2, i % 2
            part = pl.ds(pl.multiple_of(h * BLK, BLK), BLK)
            whole = pl.ds(pl.multiple_of(i * BLK, BLK), BLK)
            return [(wc.at[2 * l, t, :, :, :, :, part], w1_v.at[slot]), (wc.at[2 * l + 1, t, h], w2_v.at[slot]),
                    (pre_in.at[l, :, whole], pre_v.at[slot])]

        def outs(i, slot):
            return [(dp_v.at[slot], dpre.at[l, :, pl.ds(pl.multiple_of(i * BLK, BLK), BLK)])]

        def channel(i, slot):
            run(i)

            @pl.when(i >= 2)
            def _():
                ship(l, i - 2, slot).wait_send()
            for n in range(2):
                cols = slice(256 * n, 256 * n + 256)
                d = dot_nt(do_v[...], w2_v[slot, 2 * n:2 * n + 2].reshape(256, CH)) * pre_v[slot, :, cols]
                gbch1[l:l + 1, pl.ds(pl.multiple_of(i * BLK + 256 * n, 256), 256)] = jnp.sum(d, axis=0, keepdims=True)
                dp_v[slot, :, cols] = d.astype(bf16)
            ship(l, i, slot).start()

            @pl.when(i == 0)
            def _():
                dv_v[...] = jnp.zeros_like(dv_v)
            for n in range(2):
                cols = slice(512 * n, 512 * n + 512)
                dv_v[:, cols] += dot_nt(dp_v[slot], w1_v[slot, n].reshape(512, BLK))
        for_blocks(Stream(sem_w, blocks, NBLK), channel, Stream(sem_o, outs, NBLK))
        for slot in range(2):
            ship(l, NBLK - 2 + slot, slot).wait_send()
        burst(f'l{l}')
        load.wait()

        @pl.loop(0, ROWS // TPAD)
        def _(n):
            rows = pl.ds(pl.multiple_of(n * TPAD, TPAD), TPAD)
            std, inv = standardize(get(x_v, rows))
            d = dv_v[rows, :]
            add(r + 2, d * std)
            add(r + 3, d)
            put(d_v, rows, get(d_v, rows) + norm_grad(d, vec[r + 2:r + 3, :], std, inv))
        load = pltpu.make_async_copy(xin.at[l], x_v.at[:, pl.ds(0, ROWS)], sem.at[0])
        load.start()
        burst(f't{l}_0')
        load.wait()
        run = during(f't{l}_', IMG)

        @pl.loop(0, IMG)
        def _(m):
            run(m)
            std, inv = standardize(get(x_v, image(m)))
            a = with_bias_rows(std * vec[r:r + 1, :] + vec[r + 1:r + 2, :])
            d_mid = get(d_v, image(m))
            dm = d_mid.astype(bf16)
            parts = []
            for n in range(TOK_CUTS):
                cols = slice(CH // TOK_CUTS * n, CH // TOK_CUTS * (n + 1))
                value, slope = gelu_both(dot_nn(wt[l, :, 0:TPAD], a[:, cols]))
                add_token(2 + l, dot_nt(value.astype(bf16), dm[:, cols]))
                dh = dot_nn(wt[2 + l, :, 0:TPAD], dm[:, cols]) * slope
                add_token(l, jnp.sum(dh, axis=-1, keepdims=True), 64)
                dh = dh.astype(bf16)
                add_token(l, dot_nt(dh, a[:, cols]))
                parts.append(dot_nn(wt_t[l], dh))
            d = jnp.where(mask, jnp.concatenate(parts, axis=1), 0.0)
            add(r, d * std)
            add(r + 1, d)
            put(d_v, image(m), d_mid + norm_grad(d, vec[r:r + 1, :], std, inv))
        if l == 1:
            load = pltpu.make_async_copy(xmid.at[0], x_v.at[:, pl.ds(0, ROWS)], sem.at[0])
            load.start()
            burst('d0')

    burst('fin')
    free('do')
    for at, size in CHUNKS:
        d = get(d_v, pl.ds(at, size))
        add(0, d)
        do_v[pl.ds(at, size), :] = d.astype(bf16)
    keep = pltpu.make_async_copy(do_v, dres, sem.at[1])
    keep.start()
    swap('dres')
    keep.wait()
    small_pack(b, x_v, d_v, gvec, hstat, gbch1, gbh)

    last = []

    def put_small(name, src, dst, target):
        last.append(name)
        net.start(name, lambda: (src, dst, target))

    def small(n):
        x, z, y = (ring[d][0] for d in 'xzy')
        net.arrived(*last)
        last.clear()
        if n == 0:
            put_small(('sm', 0), b['sm'].at[:, :, :, k2], b['sm1'], partner)
            put_small(('tk', 0), b['tk'].at[:, :, :, k2], b['tk1'], partner)
        elif n == 1:
            b['sm1'][...] += b['sm'][:, :, :, k]
            b['tk1'][...] += b['tk'][:, :, :, k]
            for s in (1, 2, 3):
                put_small(('sm', 1, s), b['sm1'].at[ring['x'][s]], b['sm2'].at[s - 1], peers['x', s])
                put_small(('tk', 1, s), b['tk1'].at[:, ring['z'][s]], b['tk2'].at[s - 1], peers['z', s])
        elif n == 2:
            b['sm_s1'][...] = b['sm1'][x] + b['sm2'][0] + b['sm2'][1] + b['sm2'][2]
            b['tk_s1'][...] = b['tk1'][:, z] + b['tk2'][0] + b['tk2'][1] + b['tk2'][2]
            for s in (1, 2, 3):
                put_small(('sm', 2, s), b['sm_s1'].at[ring['z'][s]], b['sm3'].at[s - 1], peers['z', s])
                put_small(('tk', 2, s), b['tk_s1'].at[:, ring['y'][s]], b['tk3'].at[s - 1], peers['y', s])
        elif n == 3:
            b['sm_s2'][...] = b['sm_s1'][z] + b['sm3'][0] + b['sm3'][1] + b['sm3'][2]
            b['tk_s2'][...] = b['tk_s1'][:, y] + b['tk3'][0] + b['tk3'][1] + b['tk3'][2]
            for s in (1, 2, 3):
                put_small(('sm', 3, s), b['sm_s2'].at[ring['y'][s]], b['sm4'].at[s - 1], peers['y', s])
                put_small(('tk', 3, s), b['tk_s2'], b['tk4'].at[s - 1], peers['x', s])
        else:
            sm_own[...] = b['sm_s2'][y] + b['sm4'][0] + b['sm4'][1] + b['sm4'][2]
            ordered = []
            for place in range(4):
                value = b['tk_s2'][...]
                for s in (1, 2, 3):
                    value = jnp.where(ring['x'][4 - s] == place, b['tk4'][s - 1], value)
                ordered.append(value)
            tk_own[...] = (ordered[0] + ordered[1]) + (ordered[2] + ordered[3])

    tail = bursts.get('end', ())
    small(0)
    for n, s in enumerate(tail):
        step(*s)
        if n in (8, 18, 28, 38):
            small(1 + (8, 18, 28, 38).index(n))
    net.finish()
    assert len(net.builds) <= BACK_COPIES, len(net.builds)


def back(*operands):
    a, v = pl.BlockSpec(memory_space=pl.ANY), pl.BlockSpec(memory_space=pltpu.VMEM)
    S, V, DMA = jax.ShapeDtypeStruct, pltpu.VMEM, pltpu.SemaphoreType.DMA
    return pl.pallas_call(
        back_kernel, name='back',
        in_specs=[a] * 7 + [v] * 8, out_specs=[v] * 5 + [a] * 9,
        out_shape=[S((N_CH, 32, 1024), f32), S((96, 256), f32), S((32, 256), f32), S((8, 128), f32), S((4, 16, 128), f32),
                   S((2, ROWS, CHH), bf16), S((2, ROWS, CH), bf16), S((ROWS, CH), bf16), S((2, ROWS, 2048), bf16),
                   S((2, ROWS, 512), bf16), S((ROWS, 1536), bf16), S((2, ROWS, CHH), bf16), S((2, ROWS, CH), bf16),
                   S((ROWS, CH), bf16)],
        scratch_shapes=[reduce_scratch(), small_scratch(), V((2, ROWS, CHH), bf16), V((2, ROWS, CH), bf16), V((IMG, 512), bf16),
                        V((IMG, CH), bf16), V((16, CH), f32), V((2, CHH), f32), V((CH // 128, XROWS, 128), f32),
                        V((CH // 128, XROWS, 128), f32), V((ROWS, CH), f32), V((ROWS, CH), bf16), V((2, 2, 4, 4, 32, BLK), bf16),
                        V((2, 4, 4, 32, CH), bf16), V((2, ROWS, BLK), f32), V((2, ROWS, BLK), bf16), DMA((BACK_COPIES,)), DMA((BACK_COPIES,)), DMA((4,)), DMA((2,)), DMA((2, 3)),
                        DMA((2, 1)), DMA((2,)), DMA((2,))],
        compiler_params=pltpu.CompilerParams(collective_id=1, has_side_effects=True, vmem_limit_bytes=64 * 1024 * 1024 - 65536),
        cost_estimate=pl.CostEstimate(flops=120_000_000_000, bytes_accessed=200_000_000, transcendentals=0),
    )(*operands)


def finish_kernel(c, stem, head, sm, tk, loss, o_stem, o_bstem, o_ln1g, o_ln1b, o_wt1, o_bt1, o_wt2, o_ln2g, o_ln2b, o_ch1,
                  o_bch1, o_ch2, o_bch2, o_lnfg, o_lnfb, o_head, o_bhead):
    def core_last(value, pick):
        got = dot_nt(jnp.concatenate(three_parts(value), axis=0), pick)
        n = value.shape[0]
        return got[0:n] + got[n:2 * n] + got[2 * n:3 * n]
    pick = core_first(1024, 1024, 32)
    for l in range(2):
        o_ch1[l] = core_last(c[2 * l], pick)
        o_ch2[l] = core_last(c[2 * l + 1], pick)
    o_stem[...] = core_last(stem[...], core_first(256, 256, 32))
    o_head[...] = head[:, 0:250]
    own = sm[...]
    turned = jnp.concatenate([own, jnp.zeros((120, 128), f32)], axis=0).T
    for ref, n in ((o_bstem, 0), (o_lnfg, 11), (o_lnfb, 12)):
        ref[...] = turned[n, 0:8]
    for n, ref in enumerate((o_ln1g, o_ln1b, o_ln2g, o_ln2b, o_bch2)):
        for l in range(2):
            ref[pl.ds(l, 1), :] = turned[1 + 5 * l + n:2 + 5 * l + n, 0:8]
    o_bch1[...] = own[0:2, 32:64]
    classes = jnp.concatenate([own[2 + q:3 + q, 64:128] for q in range(4)], axis=1)
    o_bhead[...] = classes[0, 0:250]
    loss[...] = own[6:7, 64:65] * (1.0 / 1024)
    for l in range(2):
        o_wt1[l] = tk[l, :, 0:TOK]
        o_wt2[l] = tk[2 + l, :, 0:TOK]
        tall = jnp.concatenate([tk[l], jnp.zeros((112, 128), f32)], axis=0).T
        o_bt1[pl.ds(l, 1), :] = tall[64:65, 0:16]


def finish(*operands):
    S = jax.ShapeDtypeStruct
    v = pl.BlockSpec(memory_space=pltpu.VMEM)
    return pl.pallas_call(
        finish_kernel, name='finish', in_specs=[v] * 5, out_specs=[v] * 18,
        out_shape=[S((1, 1), f32), S((96, 256), f32), S((8,), f32), S((2, 8), f32), S((2, 8), f32), S((2, 16, TOK), f32),
                   S((2, 16), f32), S((2, 16, TOK), f32), S((2, 8), f32), S((2, 8), f32), S((2, 32, 1024), f32), S((2, 32), f32),
                   S((2, 32, 1024), f32), S((2, 8), f32), S((8,), f32), S((8,), f32), S((32, 250), f32), S((250,), f32)],
    )(*operands)

CHANNEL_AXES = ('tp', 'fsdp')


def weight_specs():
    vec_spec = P(CHANNEL_AXES)
    layer_vec = P(None, CHANNEL_AXES)
    return (P('fsdp', 'tp'), vec_spec, layer_vec, layer_vec, P(None, None, 'fsdp'), P(None, 'fsdp'),
            P(None, 'fsdp', None), layer_vec, layer_vec, P(None, 'fsdp', 'tp'), layer_vec,
            P(None, CHANNEL_AXES, None), layer_vec, vec_spec, vec_spec, P('fsdp', 'tp'), P('tp'))


def solution(mesh):
    def step(patches, labels, w_stem, b_stem, ln1_g, ln1_b, w_tok1, b_tok1, w_tok2,
             ln2_g, ln2_b, w_ch1, b_ch1, w_ch2, b_ch2, lnf_g, lnf_b, w_head, b_head):
        wc, pat, xin, xmid, vin, pre, act, hl, hr, dx0, hstat, gbh, vec, wt, wt_t = front(
            labels, patches.transpose(1, 0, 2), w_stem, w_ch1, w_ch2, w_head, w_tok1.transpose(0, 2, 1), w_tok2, b_tok1, b_ch1,
            b_head, b_stem, ln1_g, ln1_b, ln2_g, ln2_b, b_ch2, lnf_g, lnf_b)
        sums = back(xin, xmid, pre, wc, act, vin, pat, hl, hr, dx0, hstat, gbh, wt, wt_t, vec)[:5]
        loss, g_s, g_bs, g_1g, g_1b, g_t1, g_bt, g_t2, g_2g, g_2b, g_c1, g_b1, g_c2, g_b2, g_fg, g_fb, g_h, g_bh = finish(*sums)
        return (loss.reshape(()), g_s, g_bs, g_1g, g_1b, g_t1.transpose(0, 2, 1), g_bt, g_t2, g_2g, g_2b, g_c1, g_b1, g_c2, g_b2,
                g_fg, g_fb, g_h, g_bh)

    specs = weight_specs()
    return jax.shard_map(step, mesh=mesh, in_specs=(P('fsdp', None, None), P('fsdp')) + specs,
                         out_specs=(P(),) + specs, check_vma=False)
```

```python
import functools

import jax
import jax.numpy as jnp
from jax import lax
from jax.experimental import pallas as pl
from jax.experimental.pallas import tpu as pltpu
from jax.sharding import PartitionSpec as P

MESH = pl.DeviceIdType.MESH
ORDERS = (('x', 'y', 'z'), ('y', 'z', 'x'), ('z', 'x', 'y'))
COLS = ((0, 384), (384, 384), (768, 256))
N_CH = 4
STEM, HEAD = 4, 5
bf16, f32 = jnp.bfloat16, jnp.float32


def my_place():
    f = lax.axis_index('fsdp')
    return {'x': lax.axis_index('tp'), 'z': f // 8, 'y': (f // 2) % 4, 'k': f % 2}


def moved(place, dim, step):
    new = dict(place)
    new[dim] = 1 - place['k'] if dim == 'k' else (place[dim] + step) % 4
    return new


def device(place):
    return {'tp': place['x'], 'fsdp': (place['z'] * 4 + place['y']) * 2 + place['k']}


EPS = 1e-6
TOK, TPAD = 49, 56
IMG = 8
ROWS, XROWS = IMG * TOK, IMG * TPAD
CHUNKS = ((0, 112), (112, 112), (224, 112), (336, 56))
CH, TOKH, CHH = 1024, 512, 4096
BLK = 512
NBLK = CHH // BLK
GELU_C, GELU_A = 0.7978845608028654, 0.044715


def dot_nn(a, b):
    return lax.dot_general(a, b, (((1,), (0,)), ((), ())), preferred_element_type=f32)


def dot_nt(a, b):
    return lax.dot_general(a, b, (((1,), (1,)), ((), ())), preferred_element_type=f32)


def dot_tn(a, b):
    return lax.dot_general(a, b, (((0,), (0,)), ((), ())), preferred_element_type=f32)


def gelu_both(x):
    sq = x * x
    half = 0.5 * jnp.tanh(x * (GELU_C + (GELU_C * GELU_A) * sq))
    rise = 0.5 + half
    value = x * rise
    return value, rise + value * (0.5 - half) * (2.0 * GELU_C + (6.0 * GELU_C * GELU_A) * sq)


def standardize(x):
    mean = jnp.mean(x, axis=-1, keepdims=True)
    cent = x - mean
    inv = lax.rsqrt(jnp.mean(cent * cent, axis=-1, keepdims=True) + EPS)
    return cent * inv, inv


def norm_grad(d, gain, std, inv):
    gs = d * gain
    m0 = jnp.mean(gs, axis=-1, keepdims=True)
    m1 = jnp.mean(gs * std, axis=-1, keepdims=True)
    return inv * (gs - m0 - std * m1)


def row_mask(rows=TPAD):
    return lax.broadcasted_iota(jnp.int32, (rows, 1), 0) < TOK


def image(b):
    return pl.ds(b, TPAD, stride=IMG)


def get(ref, rows):
    return jnp.concatenate([ref[n, rows, :] for n in range(CH // 128)], axis=1)


def put(ref, rows, value):
    for n in range(CH // 128):
        ref[n, rows, :] = value[:, 128 * n:128 * (n + 1)]


class Stream:
    def __init__(self, sem, copies, count):
        self.sem, self.copies, self.count = sem, copies, count

    def make(self, i, slot):
        return [pltpu.make_async_copy(src, dst, self.sem.at[slot, n]) for n, (src, dst) in enumerate(self.copies(i, slot))]

    def start(self, i, slot):
        for copy in self.make(i, slot):
            copy.start()

    def wait(self, i, slot):
        for copy in self.make(i, slot):
            copy.wait()


def for_blocks(stream, body, out=None):
    n = stream.count
    stream.start(0, 0)

    @pl.loop(0, n)
    def _(i):
        slot = i % 2
        stream.wait(i, slot)

        @pl.when(i + 1 < n)
        def _():
            stream.start(i + 1, 1 - slot)
        if out is not None:
            @pl.when(i >= 2)
            def _():
                out.wait(i - 2, slot)
        body(i, slot)
        if out is not None:
            out.start(i, slot)
    if out is not None:
        out.wait(n - 2, n % 2)
        out.wait(n - 1, 1 - n % 2)


TOK_CUTS = 4
FRONT_COPIES = 270
EARLY = [('stem', c) for c in range(3)] + [('ch', c, p) for p in 'ab' for c in range(3)] + [('head', 2)]
PARTS = {'a': pl.ds(0, 2), 'b': pl.ds(2, 2)}
LATE = [('stem', c, None) for c in range(3)] + [('ch', c, g) for g in range(N_CH) for c in range(3)] + [('head', 2, None)]
UNIT_GROUP = {('stem', None): 0, ('ch', 0): 1, ('ch', 1): 2, ('ch', 2): 3, ('ch', 3): 4, ('head', None): 5}
EVERY = pl.ds(0, 4)
FRONT_ORDER = (
    ('prep', (('M0', ('sm',)), ('M0', ('tk',)), ('A0', ('stem', 0)), ('A0', ('stem', 1)), ('A0', ('stem', 2)),
        ('A0', ('ch', 0, 'a')), ('A0', ('ch', 0, 'b')), ('A0', ('ch', 1, 'a')), ('A0', ('ch', 1, 'b')),
        ('A0', ('ch', 2, 'a')), ('A0', ('ch', 2, 'b')),)),
    ('unpack', (('M1', ('sm',)), ('M1', ('tk',)), ('A', ('stem', 0)), ('A', ('stem', 1)), ('A', ('stem', 2)),
        ('A', ('ch', 0, 'a')), ('A', ('ch', 1, 'a')), ('A', ('ch', 2, 'a')), ('B', ('stem', 0)), ('M2', ('sm',)),
        ('B', ('stem', 1)), ('B', ('ch', 0, 'a')), ('B', ('ch', 1, 'a')), ('M2', ('tk',)), ('B', ('stem', 2)),
        ('C', ('stem', 0)), ('B', ('ch', 2, 'a')), ('M3', ('sm',)), ('C', ('stem', 2)), ('C', ('stem', 1)),)),
    ('stem0', (('D', ('stem', 0, None)), ('D', ('stem', 1, None)), ('D', ('stem', 2, None)), ('C', ('ch', 0, 'a')),
        ('C', ('ch', 1, 'a')), ('C', ('ch', 2, 'a')), ('A', ('ch', 0, 'b')), ('A', ('ch', 1, 'b')), ('A', ('ch', 2, 'b')),
        ('E', ('stem', 0, None)), ('E', ('stem', 1, None)), ('E', ('stem', 2, None)), ('D', ('ch', 2, 0)),
        ('B', ('ch', 0, 'b')), ('D', ('ch', 1, 0)), ('D', ('ch', 0, 0)), ('B', ('ch', 2, 'b')), ('B', ('ch', 1, 'b')),
        ('F', ('stem', 0, None)), ('F', ('stem', 1, None)), ('A0', ('head', 2)), ('F', ('stem', 2, None)),)),
    ('stem1', (('E', ('ch', 2, 0)), ('D', ('ch', 0, 1)), ('D', ('ch', 1, 1)), ('D', ('ch', 2, 1)),)),
    ('stem3', (('E', ('ch', 0, 0)), ('E', ('ch', 1, 0)),)),
    ('tok0_2', (('F', ('ch', 2, 0)), ('A', ('head', 2)),)),
    ('tok0_7', (('E', ('ch', 2, 1)), ('C', ('ch', 0, 'b')), ('C', ('ch', 1, 'b')), ('C', ('ch', 2, 'b')),)),
    ('ln0', (('E', ('ch', 1, 1)),)),
    ('ch0_0', (('E', ('ch', 0, 1)), ('F', ('ch', 1, 0)), ('B', ('head', 2)), ('F', ('ch', 2, 1)), ('D', ('ch', 2, 2)),
        ('D', ('ch', 2, 3)), ('F', ('ch', 0, 0)), ('D', ('ch', 0, 2)), ('D', ('ch', 0, 3)), ('D', ('ch', 1, 2)),
        ('D', ('ch', 1, 3)), ('F', ('ch', 1, 1)), ('C', ('head', 2)),)),
    ('ch0_1', (('F', ('ch', 0, 1)),)),
    ('ch0_2', (('E', ('ch', 2, 2)),)),
    ('ch0_7', (('E', ('ch', 1, 2)), ('E', ('ch', 2, 3)),)),
    ('cb0_0', (('E', ('ch', 0, 2)),)),
    ('cb0_1', (('F', ('ch', 2, 2)),)),
    ('tok1_1', (('F', ('ch', 2, 3)),)),
    ('tok1_2', (('D', ('head', 2, None)), ('E', ('ch', 1, 3)),)),
    ('tok1_3', (('E', ('ch', 0, 3)),)),
    ('tok1_6', (('F', ('ch', 1, 2)), ('F', ('ch', 0, 2)),)),
    ('ch1_0', (('E', ('head', 2, None)), ('F', ('ch', 1, 3)), ('F', ('ch', 0, 3)),)),
    ('ch1_4', (('F', ('head', 2, None)),)),
)


class Net:
    def __init__(self, send_sems, recv_sems):
        self.send_sems, self.recv_sems, self.names, self.builds, self.done = send_sems, recv_sems, {}, [], set()

    def copy(self, name):
        n = self.names[name]
        src, dst, target = self.builds[n]()
        return pltpu.make_async_remote_copy(src_ref=src, dst_ref=dst, send_sem=self.send_sems.at[n],
                                            recv_sem=self.recv_sems.at[n], device_id=target, device_id_type=MESH)

    def start(self, name, build):
        self.names[name] = len(self.builds)
        self.builds.append(build)
        self.copy(name).start()

    def arrived(self, *names):
        for name in names:
            self.copy(name).wait_recv()

    def finish(self):
        for name in self.names:
            if name not in self.done:
                self.copy(name).wait_send()


def core_first(size, cols, each):
    half = cols // 2
    row = lax.broadcasted_iota(jnp.int32, (size, size), 0)
    col = lax.broadcasted_iota(jnp.int32, (size, size), 1)
    source = col % half // each * (2 * each) + col // half * each + col % each
    return jnp.where(row == source, 1.0, 0.0).astype(bf16)


def three_parts(x):
    hi = x.astype(bf16)
    rest = x - hi.astype(f32)
    mid = rest.astype(bf16)
    return hi, mid, (rest - mid.astype(f32)).astype(bf16)


def with_bias_rows(a):
    row = lax.broadcasted_iota(jnp.int32, (TPAD, 1), 0)
    return jnp.where(row < TOK, a, jnp.where(row < TOK + 3, 1.0, 0.0)).astype(bf16)


def front_kernel(labels, patches, w_stem, w_ch1, w_ch2, w_head, w_tok1, w_tok2, b_tok1, b_ch1, b_head, b_stem, ln1_g, ln1_b,
                 ln2_g, ln2_b, b_ch2, lnf_g, lnf_b,
                 wc, pat_out, xin, xmid, vout, pre_out, act_out, hl, hr, dx0, hstat, gbh, vec, wt, wt_t,
                 pc, ps, ph, tk_f, tk_p, sm_p, bh_p, ws, wh, tk_v, sm_v, sm_2, bh_v, bch1,
                 turn, p_v, pk_v, x_v, v_v, w1_v, w2_v, pre_v, act_v, g_v,
                 send_sems, recv_sems, sem, sem_w, sem_o, sem_x):
    me = my_place()
    other = moved(me, 'k', 1)
    load_p = pltpu.make_async_copy(patches.at[:, pl.ds(pl.multiple_of(me['x'] * IMG, IMG), IMG)], p_v, sem.at[0])
    load_p.start()

    barrier = pltpu.get_barrier_semaphore()
    for dim in 'xyz':
        for step in (1, 2, 3):
            pl.semaphore_signal(barrier, inc=1, device_id=device(moved(me, dim, step)), device_id_type=MESH)
    pl.semaphore_signal(barrier, inc=1, device_id=device(other), device_id_type=MESH)

    stem = dot_nn(w_stem[...].astype(bf16), core_first(256, 256, 32)).astype(bf16)
    ps[0], ps[1] = stem[:, 0:128], stem[:, 128:256]
    pick = core_first(1024, 1024, 32)
    for l in range(2):
        pc[2 * l] = dot_nn(w_ch1[l].astype(bf16), pick).astype(bf16)
        pc[2 * l + 1] = dot_nn(w_ch2[l].astype(bf16), pick).astype(bf16)
    ph[...] = jnp.zeros_like(ph)
    ph[:, pl.ds(0, 250)] = w_head[...].astype(bf16)
    turn[...] = jnp.zeros_like(turn)
    for n, ref in ((0, b_stem), (11, lnf_g), (12, lnf_b)):
        turn[n, pl.ds(0, 8)] = ref[...]
    for n, ref in enumerate((ln1_g, ln1_b, ln2_g, ln2_b, b_ch2)):
        for l in range(2):
            turn[pl.ds(1 + 5 * l + n, 1), pl.ds(0, 8)] = ref[pl.ds(l, 1), :]
    turn[pl.ds(16, 2), pl.ds(0, 16)] = b_tok1[...]
    turned = turn[...].T
    tk_f[...] = jnp.zeros_like(tk_f)
    for l in range(2):
        tk_f[l, :, pl.ds(0, TOK)] = w_tok1[l]
        tk_f[2 + l, :, pl.ds(0, TOK)] = w_tok2[l]
        for n, part in enumerate(three_parts(turned[0:16, 16 + l:17 + l])):
            tk_f[l, :, pl.ds(TOK + n, 1)] = part.astype(f32)
    tk_p[...] = tk_f[...].astype(bf16)
    sm_p[...] = jnp.zeros_like(sm_p)
    sm_p[:, pl.ds(0, 16)] = turned[0:8, 0:16]
    sm_p[pl.ds(0, 2), pl.ds(32, 32)] = b_ch1[...]
    bh_p[...] = jnp.full_like(bh_p, -1e30)
    bh_p[0, pl.ds(0, 250)] = b_head[...]

    net = Net(send_sems, recv_sems)
    core = me['k']
    ring = {d: [moved(me, d, n)[d] for n in range(4)] for d in 'xyz'}
    columns = [pl.ds(pl.multiple_of(x * 256, 256), 256) for x in ring['x']]
    stem_columns = [pl.ds(pl.multiple_of(x * 128, 128), 128) for x in ring['x']]
    peers = {(d, n): device(moved(me, d, n)) for d in 'xyz' for n in (1, 2, 3)}
    partner = device(other)
    here = {'x': 0, 'y': 0, 'z': 0}

    def view(unit, block, half=None):
        kind, colour = unit[:2]
        x, z, y = (EVERY if block[d] is None else ring[d][block[d]] for d in 'xzy')
        r0, rn = (0, 32) if half is None else (16 * half, 16)
        if kind == 'ch':
            c0, cn = COLS[colour]
            g = PARTS.get(unit[2], unit[2])
            return wc.at[g, x, core, z, y, pl.ds(r0, rn), pl.ds(c0, cn)]
        if kind == 'stem':
            cols = pl.ds(0, 512) if x is EVERY else stem_columns[block['x']]
            return ws.at[:, z, y, core, pl.ds(32 * colour + r0, rn), cols]
        cols = pl.ds(0, CH) if x is EVERY else columns[block['x']]
        return wh.at[core, z, y, pl.ds(r0, rn), cols]

    def piece(unit):
        kind, colour = unit[:2]
        if kind == 'ch':
            return pc.at[PARTS[unit[2]], :, pl.ds(*COLS[colour])]
        return ps.at[:, pl.ds(32 * colour, 32), :] if kind == 'stem' else ph.at[:, :]

    def exchange(unit, tag, dim, block):
        for side, step in (('l', 1), ('r', 3)):
            def build(step=step):
                part = view(unit, block)
                return (piece(unit) if tag == '1' else part), part, peers[dim, step]
            net.start((unit, tag, side), build)

    def forward_half(unit, tag, dim, block):
        for half, (origin, target, side) in enumerate(((3, 1, 'l'), (1, 3, 'r'))):
            def build(half=half, origin=origin, target=target):
                part = view(unit, {**block, dim: origin}, half)
                return part, part, peers[dim, target]
            net.start((unit, tag, side), build)

    def swap(unit, tag, block):
        def build():
            part = view(unit, block)
            return part, part, partner
        net.start((unit, tag), build)

    own = pltpu.make_async_copy(pc, wc.at[:, me['x'], me['k'], me['z'], me['y']], sem.at[1])
    own.start()
    mine = pl.ds(pl.multiple_of(me['x'] * 256, 256), 256)
    for n in range(2):
        ws[n, me['z'], me['y'], me['k'], :, stem_columns[0]] = ps[n]
    wh[me['k'], me['z'], me['y'], :, mine] = ph[...]
    sm_v[me['x'], me['z'], me['y'], me['k']] = sm_p[...]
    tk_v[:, me['z'], me['y'], me['k']] = tk_p[...]
    bh_v[:, mine] = bh_p[...]
    own.wait()
    pl.semaphore_wait(barrier, 10)

    def small(kind, n):
        dims = 'xyz' if kind == 'sm' else 'yz'
        at = {d: EVERY if d in dims[:n] else ring[d][0] for d in 'xyz'}

        def part():
            if kind == 'sm':
                return sm_v.at[at['x'], at['z'], at['y'], core]
            return tk_v.at[:, at['z'], at['y'], core]
        if n > 0:
            net.arrived(*[(kind, n - 1, s) for s in (1, 2, 3)])
        if n < len(dims):
            for s in (1, 2, 3):
                net.start((kind, n, s), lambda s=s: (part(), part(), peers[dims[n], s]))
            if kind == 'sm' and n == 0:
                def head_bias():
                    return bh_v.at[:, columns[0]]
                for s in (1, 2, 3):
                    net.start(('bh', s), lambda s=s: (head_bias(), head_bias(), peers['x', s]))
        else:
            net.start((kind, 'k'), lambda: (part(), part(), partner))

    def step(name, unit):
        if name[0] == 'M':
            small(unit[0], int(name[1]))
            return
        d1, d2, d3 = ORDERS[unit[1]]
        early = unit[:2] if unit[0] != 'ch' or unit[2] in PARTS else ('ch', unit[1], 'a' if unit[2] < 2 else 'b')
        plane = {**here, d1: None, d2: None}
        if name == 'A0':
            exchange(unit, '1', d1, here)
        elif name == 'A':
            net.arrived((unit, '1', 'l'), (unit, '1', 'r'))
            forward_half(unit, '1h', d1, here)
        elif name == 'B':
            net.arrived((unit, '1h', 'l'), (unit, '1h', 'r'))
            exchange(unit, '2', d2, {**here, d1: None})
        elif name == 'C':
            net.arrived((unit, '2', 'l'), (unit, '2', 'r'))
            forward_half(unit, '2h', d2, {**here, d1: None})
        elif name == 'D':
            if early not in planes:
                planes.add(early)
                net.arrived((early, '2h', 'l'), (early, '2h', 'r'))
            exchange(unit, '3', d3, plane)
            swap(unit, 'k0', plane)
        elif name == 'E':
            net.arrived((unit, '3', 'l'), (unit, '3', 'r'))
            forward_half(unit, '3h', d3, plane)
            for n in (1, 3):
                swap(unit, f'k{n}', {**plane, d3: n})
        else:
            net.arrived((unit, '3h', 'l'), (unit, '3h', 'r'))
            swap(unit, 'k2', {**plane, d3: 2})

    planes = set()
    awaited = set()

    def need(group):
        for u in LATE:
            if UNIT_GROUP[u[0], u[2]] <= group and u not in awaited:
                awaited.add(u)
                net.arrived(*[(u, f'k{n}') for n in range(4)])

    bursts = {name: steps for name, steps in FRONT_ORDER}

    def burst(name):
        for s in bursts.get(name, ()):
            step(*s)

    def during(name, count):
        def run(i):
            for n in range(1, count):
                if bursts.get(f'{name}{n}'):
                    pl.when(i == n)(functools.partial(burst, f'{name}{n}'))
        return run

    burst('prep')
    load_p.wait()
    pick = core_first(768, 768, 96)
    for g in range(4):
        part = dot_nn(p_v[:, :, pl.ds(768 * g, 768)].reshape(ROWS, 768), pick).astype(bf16)
        for n in range(2):
            pk_v[n, :, pl.ds(384 * g, 384)] = part[:, 384 * n:384 * n + 384]
    keep_p = pltpu.make_async_copy(pk_v, pat_out, sem.at[0])
    keep_p.start()

    burst('unpack')
    net.arrived(('sm', 'k'), ('tk', 'k'), ('bh', 1), ('bh', 2), ('bh', 3))
    sm_2[...] = sm_v[...].reshape(1024, 128)
    for n in range(8):
        tile = jnp.concatenate([sm_2[pl.ds((n % 4 * 4 + i) * 64 + n // 4 * 32, 32), :] for i in range(4)], axis=0)
        vec[:, pl.ds(128 * n, 128)] = tile.T[0:16, :]
    wt[...] = tk_v[...].reshape(4, TOKH, 128)
    for n in range(4):
        wt_t[n] = wt[n].astype(f32).T[0:TPAD].astype(bf16)
    for l in range(2):
        rows = jnp.concatenate(three_parts(sm_2[pl.ds(l, 128, stride=8), :]), axis=0)

        @pl.loop(0, 8)
        def _(n):
            lane = lax.broadcasted_iota(jnp.int32, (128, 512), 0)
            col = lax.broadcasted_iota(jnp.int32, (128, 512), 1)
            pick = jnp.where(lane == 32 + col % 32, 1.0, 0.0).astype(bf16)
            spread = dot_nn(rows, pick)
            value = spread[0:128] + spread[128:256] + spread[256:384]
            mine = lane == n // 2 * 32 + col // 32 * 2 + n % 2
            bch1[l:l + 1, pl.ds(pl.multiple_of(n * 512, 512), 512)] = jnp.sum(jnp.where(mine, value, 0.0), axis=0, keepdims=True)

    burst('stem0')
    need(0)
    run = during('stem', 4)
    put(x_v, pl.ds(ROWS, XROWS - ROWS), jnp.zeros((XROWS - ROWS, CH), f32))

    @pl.loop(0, 4)
    def _(i):
        run(i)
        cols = pl.ds(pl.multiple_of(i * 256, 256), 256)
        w = ws[i // 2, :, :, :, :, pl.ds(pl.multiple_of(i % 2 * 256, 256), 256)].reshape(3072, 256)
        value = dot_nn(p_v[...].reshape(ROWS, 3072), w) + vec[0:1, cols]
        for n in range(2):
            x_v[2 * i + n, pl.ds(0, ROWS), :] = value[:, 128 * n:128 * (n + 1)]

    wc_all = wc

    def add_rows(value):
        for n in range(CH // 128):
            x_v[n, pl.ds(0, ROWS), :] += value[:, 128 * n:128 * (n + 1)]

    for l in range(2):
        r = 1 + 5 * l
        burst(f'tok{l}_0')
        run = during(f'tok{l}_', IMG)
        save_in = pltpu.make_async_copy(x_v.at[:, pl.ds(0, ROWS)], xin.at[l], sem_x.at[0])
        save_in.start()
        save_in.wait()

        @pl.loop(0, IMG)
        def _(b):
            run(b)
            x = get(x_v, image(b))
            std, _ = standardize(x)
            a = with_bias_rows(std * vec[r:r + 1, :] + vec[r + 1:r + 2, :])
            g_v[...] = gelu_both(dot_nn(wt[l, :, 0:TPAD], a))[0].astype(bf16)
            put(x_v, image(b), x + dot_nn(wt_t[2 + l], g_v[...]))
        save_mid = pltpu.make_async_copy(x_v.at[:, pl.ds(0, ROWS)], xmid.at[l], sem_x.at[0])
        save_mid.start()
        burst(f'ln{l}')

        for at, size in CHUNKS:
            std, _ = standardize(get(x_v, pl.ds(at, size)))
            v_v[pl.ds(at, size), :] = (std * vec[r + 2:r + 3, :] + vec[r + 3:r + 4, :]).astype(bf16)
        save_v = [pltpu.make_async_copy(v_v.at[:, pl.ds(512 * n, 512)], vout.at[l, n], sem_x.at[1 + n]) for n in range(2)]
        for copy in save_v:
            copy.start()
        burst(f'ch{l}_0')
        need(1 + 2 * l)
        save_mid.wait()

        def blocks(i, slot):
            part = pl.ds(pl.multiple_of(i % 2 * BLK, BLK), BLK)
            return [(wc_all.at[2 * l, i // 2, :, :, :, :, part], w1_v.at[slot])]

        def outs(i, slot):
            part = pl.ds(pl.multiple_of(i * BLK, BLK), BLK)
            half = pl.ds(pl.multiple_of(i // 2 * BLK, BLK), BLK)
            return [(pre_v.at[slot], pre_out.at[l, :, part]), (act_v.at[:, part], act_out.at[l, i % 2, :, half])]
        run_a = during(f'ch{l}_', NBLK)

        def channel(i, slot):
            run_a(i)
            part = pl.ds(pl.multiple_of(i * BLK, BLK), BLK)
            h = dot_nn(v_v[...], w1_v[slot].reshape(CH, BLK)) + bch1[l:l + 1, part]
            value, pre_v[slot] = gelu_both(h)
            act_v[:, part] = value.astype(bf16)
        for_blocks(Stream(sem_w, blocks, NBLK), channel, Stream(sem_o, outs, NBLK))
        burst(f'cb{l}_0')
        need(2 + 2 * l)
        run_b = during(f'cb{l}_', 4)

        def second(t, slot):
            run_b(t)
            add_rows(dot_nn(act_v[:, pl.ds(pl.multiple_of(t * CH, CH), CH)], w2_v[slot].reshape(CH, CH)))
        for_blocks(Stream(sem_w, lambda t, slot: [(wc_all.at[2 * l + 1, t], w2_v.at[slot])], 4), second)
        add_rows(jnp.broadcast_to(vec[r + 4:r + 5, :], (ROWS, CH)))
        for copy in save_v:
            copy.wait()

    burst('head')
    need(5)
    keep_p.wait()
    last = 11
    pooled = jnp.sum(get(x_v, pl.ds(0, ROWS)).reshape(TOK, IMG, CH), axis=0) * (1.0 / TOK)
    std, inv = standardize(pooled)
    head_in = (std * vec[last:last + 1, :] + vec[last + 1:last + 2, :]).astype(bf16)
    hl[...] = head_in
    w_h = wh[...].reshape(CH, CH)
    logits = dot_nn(head_in, w_h) + bh_v[0:1, :]
    row = lax.broadcasted_iota(jnp.int32, (IMG, 1), 0)
    label = jnp.zeros((IMG, 1), jnp.int32)
    for b in range(IMG):
        value = labels[me['x'] * IMG + b]
        label = jnp.where(row == b, value, label)
    label = label + 6 * sum(jnp.where(label >= edge, 1, 0) for edge in (250, 500, 750))
    is_label = lax.broadcasted_iota(jnp.int32, logits.shape, 1) == label
    top = jnp.max(logits, axis=-1, keepdims=True)
    ex = jnp.exp(logits - top)
    es = jnp.sum(ex, axis=-1, keepdims=True)
    nll = top + jnp.log(es) - jnp.sum(jnp.where(is_label, logits, 0.0), axis=-1, keepdims=True)
    d_logits = (ex / es - jnp.where(is_label, 1.0, 0.0)) * (1.0 / 1024)
    gbh[...] = jnp.sum(d_logits, axis=0, keepdims=True)
    d_bf = d_logits.astype(bf16)
    hr[...] = d_bf
    d_in = dot_nt(d_bf, w_h)
    hstat[0:1, :] = jnp.sum(d_in * std, axis=0, keepdims=True)
    hstat[1:2, :] = jnp.sum(d_in, axis=0, keepdims=True)
    hstat[2:3, :] = jnp.broadcast_to(jnp.sum(nll, axis=0, keepdims=True), (1, CH))
    dx0[...] = norm_grad(d_in, vec[last:last + 1, :], std, inv) * (1.0 / TOK)
    burst('end')
    net.finish()
    assert len(net.builds) <= FRONT_COPIES, len(net.builds)


def front(*operands):
    a, v = pl.BlockSpec(memory_space=pl.ANY), pl.BlockSpec(memory_space=pltpu.VMEM)
    S, V, DMA = jax.ShapeDtypeStruct, pltpu.VMEM, pltpu.SemaphoreType.DMA
    return pl.pallas_call(
        front_kernel, name='front',
        in_specs=[pl.BlockSpec(memory_space=pltpu.SMEM), a] + [v] * 17,
        out_specs=[a] * 7 + [v] * 8,
        out_shape=[S((N_CH, 4, 2, 4, 4, 32, 1024), bf16), S((2, ROWS, 1536), bf16), S((2, CH // 128, ROWS, 128), f32),
                   S((2, CH // 128, ROWS, 128), f32),
                   S((2, 2, ROWS, 512), bf16), S((2, ROWS, CHH), f32), S((2, 2, ROWS, 2048), bf16), S((IMG, CH), bf16),
                   S((IMG, CH), bf16), S((IMG, CH), f32), S((8, CH), f32), S((1, CH), f32), S((16, CH), f32),
                   S((4, TOKH, 128), bf16), S((4, TPAD, TOKH), bf16)],
        scratch_shapes=[V((N_CH, 32, 1024), bf16), V((2, 96, 128), bf16), V((32, 256), bf16), V((4, 16, 128), f32),
                        V((4, 16, 128), bf16), V((8, 128), f32), V((8, 256), f32), V((2, 4, 4, 2, 96, 512), bf16),
                        V((2, 4, 4, 32, CH), bf16), V((4, 4, 4, 2, 16, 128), bf16), V((4, 4, 4, 2, 8, 128), f32),
                        V((1024, 128), f32), V((8, CH), f32), V((2, CHH), f32),
                        V((128, 128), f32), V((TOK, IMG, 3072), bf16), V((2, ROWS, 1536), bf16), V((CH // 128, XROWS, 128), f32),
                        V((ROWS, CH), bf16), V((2, 2, 4, 4, 32, BLK), bf16), V((2, 2, 4, 4, 32, CH), bf16),
                        V((2, ROWS, BLK), f32), V((ROWS, CHH), bf16), V((TOKH, CH), bf16),
                        DMA((FRONT_COPIES,)), DMA((FRONT_COPIES,)), DMA((2,)), DMA((2, 2)), DMA((2, 2)), DMA((3,))],
        compiler_params=pltpu.CompilerParams(collective_id=0, has_side_effects=True, vmem_limit_bytes=62 * 1024 * 1024),
        cost_estimate=pl.CostEstimate(flops=90_000_000_000, bytes_accessed=180_000_000, transcendentals=0),
    )(*operands)


GROUPS = (3, 2, 1, HEAD, 0, STEM)
UNITS = tuple((g, c) for g in GROUPS for c in (2, 0, 1) if g != HEAD or c == 2)
BACK_COPIES = 18 * len(UNITS) + 40
NEEDS = {3: ('act1', 'dout1'), 2: ('vin1', 'dpre1'), 1: ('act0', 'dout0'), 0: ('vin0', 'dpre0'), STEM: ('pat', 'dres'),
         HEAD: ('hl', 'hr')}
BACK_ORDER = (
    ('c1_7', ((3, 'L'),)),
    ('t1_0', ((0, 0), (0, 1), (1, 0), (1, 1), (2, 0), (2, 1), (0, 2),)),
    ('t1_2', ((1, 2),)),
    ('t1_3', ((0, 3), (2, 2),)),
    ('t1_4', ((2, 'L'),)),
    ('t1_6', ((1, 3), (0, 4), (3, 0), (3, 1), (2, 3), (4, 0), (4, 1), (1, 4), (0, 5), (5, 0), (5, 1), (3, 2), (1, 5), (0, 6),)),
    ('t1_7', ((2, 4),)),
    ('d0', ((4, 2),)),
    ('c0_1', ((5, 2), (3, 3), (2, 5), (1, 6),)),
    ('c0_3', ((1, 'L'), (1, 7),)),
    ('c0_4', ((4, 3), (3, 4), (0, 7), (6, 0), (6, 1), (2, 6), (7, 0), (7, 1), (5, 3), (4, 4), (3, 5), (2, 7), (8, 0), (8, 1),
        (6, 2), (4, 5), (3, 6), (9, 0), (9, 1),)),
    ('c0_5', ((7, 2), (5, 4),)),
    ('c0_7', ((6, 3), (8, 2), (4, 6),)),
    ('t0_0', ((9, 2),)),
    ('t0_1', ((7, 3), (6, 4), (3, 7),)),
    ('t0_2', ((5, 5), (4, 7),)),
    ('t0_3', ((8, 3), (7, 4), (6, 5), (9, 3), (5, 6),)),
    ('t0_4', ((0, 'L'),)),
    ('t0_5', ((8, 4), (9, 4), (7, 5), (6, 6), (5, 7), (10, 0), (10, 1), (11, 0), (11, 1), (8, 5), (9, 5), (7, 6), (6, 7),
        (12, 0), (12, 1), (10, 2), (9, 6),)),
    ('t0_6', ((7, 7),)),
    ('t0_7', ((11, 2),)),
    ('fin', ((12, 2), (10, 3),)),
    ('end', ((8, 6), (9, 7), (11, 3), (10, 4), (8, 7), (4, 'L'), (12, 3), (10, 5), (11, 4), (13, 0), (13, 1), (12, 4),
        (11, 5), (10, 6), (14, 0), (14, 1), (15, 0), (15, 1), (10, 7), (13, 2), (14, 2), (15, 2), (12, 5), (11, 6), (14, 3),
        (15, 3), (12, 6), (13, 3), (11, 7), (14, 4), (12, 7), (15, 4), (13, 4), (14, 5), (15, 5), (13, 5), (14, 6), (15, 6),
        (13, 6), (14, 7), (15, 7), (13, 7),)),
)
SMALL = dict(sm=((4, 4, 4, 8, 128), (3, 4, 4, 8, 128), (3, 4, 8, 128), (3, 8, 128)),
             tk=((4, 4, 4, 16, 128), (3, 4, 4, 16, 128), (3, 4, 16, 128), (3, 4, 16, 128)))


def reduce_scratch():
    per = []
    for c in range(3):
        n = COLS[c][1]
        many = sum(1 for u in UNITS if u[1] == c)
        lead = ((4, 4), (4,), ())
        b = {'C': pltpu.VMEM((2, 4, 4, 4, 32, n), bf16), 'S1': pltpu.VMEM((4, 4, 32, n), f32), 'S2': pltpu.VMEM((2, 4, 32, n), f32)}
        for ph in range(3):
            if ph:
                b[f'opp{ph}'] = pltpu.VMEM(lead[ph] + (32, n), bf16)
                b[f'pr{ph}'] = pltpu.VMEM(lead[ph] + (16, n), bf16)
                b[f'pl{ph}'] = pltpu.VMEM(lead[ph] + (16, n), bf16)
            for name in ('rig', 'lef'):
                b[f'{name}{ph}'] = pltpu.VMEM(lead[ph] + (16, n), bf16)
            for name in ('half0', 'half1'):
                b[f'{name}{ph}'] = pltpu.VMEM((many,) + lead[ph] + (16, n), bf16)
            for name in ('froml', 'fromr'):
                b[f'{name}{ph}'] = pltpu.VMEM((many,) + lead[ph] + (32, n), bf16)
        per.append(b)
    return per


def small_scratch():
    b = {f'{kind}{n + 1}': pltpu.VMEM(shape, f32) for kind, shapes in SMALL.items() for n, shape in enumerate(shapes)}
    b.update(sm=pltpu.VMEM((4, 4, 4, 2, 8, 128), f32), tk=pltpu.VMEM((4, 4, 4, 2, 16, 128), f32),
             sm_s1=pltpu.VMEM((4, 4, 8, 128), f32), sm_s2=pltpu.VMEM((4, 8, 128), f32),
             tk_s1=pltpu.VMEM((4, 4, 16, 128), f32), tk_s2=pltpu.VMEM((4, 16, 128), f32))
    return b


def small_pack(b, flat, turn, gvec, hstat, gbch1, gbh):
    for n in range(8):
        cols = pl.ds(128 * n, 128)
        turn[n, pl.ds(0, 128), :] = jnp.zeros((128, 128), f32)
        turn[n, pl.ds(0, 16), :] = gvec[:, cols]
        turn[n, pl.ds(11, 2), :] = hstat[pl.ds(0, 2), cols]
    for n in range(8):
        tile = turn[n, pl.ds(0, 128), :].T
        for i in range(4):
            a = n % 4 * 4 + i
            flat[a // 2, pl.ds(a % 2 * 64 + n // 4 * 32, 32), :] = tile[32 * i:32 * i + 32]
    for l in range(2):
        def gather(n, total):
            lane = lax.broadcasted_iota(jnp.int32, (128, 512), 0)
            col = lax.broadcasted_iota(jnp.int32, (128, 512), 1)
            sums = gbch1[l:l + 1, pl.ds(pl.multiple_of(512 * n, 512), 512)]
            mine = jnp.where(lane == n // 2 * 32 + col // 32 * 2 + n % 2, sums, 0.0)
            pick = jnp.where(lane == 32 + col % 32, 1.0, 0.0).astype(bf16)
            return total + dot_nt(jnp.concatenate(three_parts(mine), axis=0), pick)
        total = lax.fori_loop(0, 8, gather, jnp.zeros((384, 128), f32))
        total = total[0:128] + total[128:256] + total[256:384]
        for n in range(8):
            flat[n, pl.ds(l, 16, stride=8), :] += total[16 * n:16 * n + 16]
    lane = lax.broadcasted_iota(jnp.int32, (1, 128), 1)
    for t in range(4):
        for q in range(4):
            tile = gbh[0:1, t * 256 + q // 2 * 128:t * 256 + q // 2 * 128 + 128]
            if q % 2 == 0:
                tile = jnp.concatenate([tile[:, 64:], tile[:, :64]], axis=1)
            tile = jnp.where(lane >= 64, tile, 0.0)
            for n in (2 * t, 2 * t + 1):
                flat[n, pl.ds(2 + q, 16, stride=8), :] += tile
    for n in range(8):
        flat[n, pl.ds(6, 16, stride=8), :] += jnp.where(lane == 64, hstat[2:3, 0:128], 0.0)
        b['sm'][n // 2, pl.ds(n % 2 * 2, 2)] = flat[n, pl.ds(0, 128), :].reshape(2, 4, 2, 8, 128)


def back_kernel(*refs):
    xin, xmid, pre_in, wc, act, vin, pat = refs[:7]
    hl, hr, dx0, hstat, gbh, wt, wt_t, vec = refs[7:15]
    out_c, out_s, out_h, sm_own, tk_own = refs[15:20]
    dpre, dout, dres, x_act, x_vin, x_pat, x_dpre, x_dout, x_dres = refs[20:29]
    (per, b, big, little, x_hl, x_hr, gvec, gbch1, x_v, d_v, dv_v, do_v, w1_v, w2_v, pre_v, dp_v,
     send_sems, recv_sems, load_sems, sem, sem_w, sem_o) = refs[29:]
    me = my_place()
    other = moved(me, 'k', 1)
    k, k2 = me['k'], 1 - me['k']
    barrier = pltpu.get_barrier_semaphore()
    for dim in 'xyz':
        for step in (1, 2, 3):
            pl.semaphore_signal(barrier, inc=1, device_id=device(moved(me, dim, step)), device_id_type=MESH)
    pl.semaphore_signal(barrier, inc=1, device_id=device(other), device_id_type=MESH)
    net = Net(send_sems, recv_sems)
    ring = {d: [moved(me, d, n)[d] for n in range(4)] for d in 'xyz'}
    peers = {(d, n): device(moved(me, d, n)) for d in 'xyz' for n in (1, 2, 3)}
    partner = device(other)
    half_at = pl.ds(pl.multiple_of(k * 512, 512), 512)
    half_to = pl.ds(pl.multiple_of(k2 * 512, 512), 512)
    swaps = {'act1': (act.at[1, k2], x_act.at[1]), 'act0': (act.at[0, k2], x_act.at[0]), 'vin1': (vin.at[1, k2], x_vin.at[1]),
             'vin0': (vin.at[0, k2], x_vin.at[0]), 'pat': (pat.at[k2], x_pat), 'dpre1': (dpre.at[1], x_dpre.at[1]), 'dpre0': (dpre.at[0], x_dpre.at[0]),
             'dout1': (do_v, x_dout.at[1]), 'dout0': (do_v, x_dout.at[0]), 'dres': (do_v, x_dres),
             'hl': (hl.at[:, half_to], x_hl), 'hr': (hr, x_hr)}

    def swap(*names):
        for name in names:
            net.start(name, lambda name=name: (*swaps[name], partner))
    busy = {}

    def free(key):
        for name in busy.pop(key, ()):
            net.copy(name).wait_send()
            net.done.add(name)

    def loads(g):
        l = g // 2
        if g == STEM:
            wide, tall = (pat.at[k], x_pat, 1536), (dres, x_dres, CH)
        elif g % 2:
            wide, tall = (act.at[l, k], x_act.at[l], 2048), (dout.at[l], x_dout.at[l], CH)
        else:
            wide, tall = (dpre.at[l], x_dpre.at[l], CHH), (vin.at[l, k], x_vin.at[l], 512)
        out = []
        for n, (buf, (own, far, cols)) in enumerate(((big, wide), (little, tall))):
            out += [pltpu.make_async_copy(own, buf.at[0, :, pl.ds(0, cols)], load_sems.at[2 * n]),
                    pltpu.make_async_copy(far, buf.at[1, :, pl.ds(0, cols)], load_sems.at[2 * n + 1])]
        return out

    def product(u):
        g, c, slot = u.g, u.c, u.slot
        first = c == 2
        if first and g != HEAD:
            for copy in loads(g):
                copy.wait()
        if g == STEM and not first:
            return
        for v in (units if g == STEM else (u,)):
            if v.g == g:
                free(('C', v.c, v.slot))
        if g == HEAD:
            net.arrived(*NEEDS[g])
            for t in range(4):
                cols = pl.ds(256 * t, 256)
                prod = dot_tn(hl[:, half_at], hr[:, cols]) + dot_tn(x_hl[...], x_hr[:, cols])
                per[c]['C'][slot, t] = prod.astype(bf16).reshape(4, 4, 32, 256)
        elif g == STEM:
            slots = {v.c: v.slot for v in units if v.g == STEM}

            @pl.loop(0, 4)
            def _(z):
                rows = pl.ds(pl.multiple_of(z * 384, 384), 384)
                for t in range(4):
                    def right(s):
                        return jnp.concatenate([little[s, :, 128 * t:128 * t + 128], little[s, :, 512 + 128 * t:640 + 128 * t]], axis=1)
                    prod = dot_tn(big[0, :, rows], right(0)) + dot_tn(big[1, :, rows], right(1))
                    prod = prod.astype(bf16).reshape(4, 3, 32, 256)
                    for d in range(3):
                        per[d]['C'][slots[d], t, z, :, :, pl.ds(0, 256)] = prod[:, d]
        else:
            c0, n = COLS[c]

            @pl.loop(0, 4)
            def _(t):
                for h in range(2):
                    if g % 2:
                        left = pl.ds(pl.multiple_of(t * 512 + h * 256, 256), 256)
                        prod = dot_tn(big[0, :, left], little[0, :, c0:c0 + n]) + dot_tn(big[1, :, left], little[1, :, c0:c0 + n])
                    else:
                        right = pl.ds(pl.multiple_of(t * 1024 + c0, 128), n)
                        rows = slice(256 * h, 256 * h + 256)
                        prod = dot_tn(little[0, :, rows], big[0, :, right]) + dot_tn(little[1, :, rows], big[1, :, right])
                    per[c]['C'][slot, t, 2 * h:2 * h + 2] = prod.astype(bf16).reshape(2, 4, 32, n)

    class Unit:
        def __init__(self, g, c):
            self.g, self.c = g, c
            self.index = [u for u in UNITS if u[1] == c].index((g, c))
            self.slot = self.index % 2
            self.n = COLS[c][1] if g < N_CH else 256
            self.cols = pl.ds(0, self.n)
            self.buf = per[c]
            self.dims = ORDERS[c]
            self.rest = [d for d in 'xzy' if d != self.dims[0]]

        def cut(self, name, *at, rows=slice(None)):
            ref = self.buf[name]
            inner = [slice(None)] * (len(ref.shape) - len(at) - 2)
            return ref.at[(*at, *inner, rows, self.cols)]

        def block(self, p, rows):
            at = {d: EVERY for d in 'xzy'}
            at[self.dims[0]] = p
            return self.buf['C'].at[self.slot, at['x'], at['z'], at['y'], rows, self.cols]

        def share(self, phase, p, e, rows):
            if phase == 0:
                at = dict(zip(self.rest, e))
                at[self.dims[0]] = p
                return self.buf['C'][self.slot, at['x'], at['z'], at['y'], rows, self.cols].astype(f32)
            if phase == 1:
                at = (p, e[0]) if self.dims[1] == self.rest[0] else (e[0], p)
                return self.buf['S1'][(*at, rows, self.cols)]
            return self.buf['S2'][self.slot, p, rows, self.cols]

        def each(self, phase, body):
            if phase == 2:
                body(())
            elif phase == 1:
                pl.loop(0, 4)(lambda i: body((i,)))
            else:
                @pl.loop(0, 4)
                def _(i):
                    pl.loop(0, 4)(lambda j: body((i, j)))

        def send(self, tag, phase, src, dst, step):
            name = (self.g, self.c, tag, phase)
            net.start(name, lambda: (src(), dst(), peers[self.dims[phase], step]))
            return name

        def arrived(self, phase, *tags):
            net.arrived(*[(self.g, self.c, tag, phase) for tag in tags])

        def opposite(self, phase):
            places = ring[self.dims[phase]]
            low, high = pl.ds(0, 16), pl.ds(16, 16)
            if phase == 0:
                sources = [lambda: self.block(places[2], low), lambda: self.block(places[2], high),
                           lambda: self.block(places[1], high), lambda: self.block(places[3], low)]
            else:
                names = (f'opp{phase}', f'pr{phase}', f'pl{phase}')
                for name in names:
                    free((name, self.c))
                opp, right, left = (self.buf[name] for name in names)

                def body(e):
                    opp[(*e, slice(None), self.cols)] = self.share(phase, places[2], e, pl.ds(0, 32)).astype(bf16)
                    right[(*e, slice(None), self.cols)] = self.share(phase, places[1], e, high).astype(bf16)
                    left[(*e, slice(None), self.cols)] = self.share(phase, places[3], e, low).astype(bf16)
                self.each(phase, body)
                sources = [lambda: self.cut(names[0], rows=low), lambda: self.cut(names[0], rows=high),
                           lambda: self.cut(names[1]), lambda: self.cut(names[2])]
            targets = [lambda: self.cut(f'half0{phase}', self.index), lambda: self.cut(f'half1{phase}', self.index),
                       lambda: self.cut(f'froml{phase}', self.index, rows=high),
                       lambda: self.cut(f'fromr{phase}', self.index, rows=low)]
            sent = [self.send(tag, phase, src, dst, step)
                    for tag, src, dst, step in zip(('h0', 'h1', 'p0', 'p1'), sources, targets, (1, 3, 1, 3))]
            if phase == 0:
                busy['C', self.c, self.slot] = sent
            else:
                busy[names[0], self.c] = sent[:2]
                busy[names[1], self.c] = sent[2:3]
                busy[names[2], self.c] = sent[3:]

        def beside(self, phase):
            places = ring[self.dims[phase]]
            for half, step, name, dst in ((0, 1, 'rig', 'froml'), (1, 3, 'lef', 'fromr')):
                self.arrived(phase, f'h{half}')
                key = f'{name}{phase}'
                free((key, self.c))
                out, got = self.buf[key], self.buf[f'half{half}{phase}']
                rows = pl.ds(16 * half, 16)

                def body(e):
                    value = self.share(phase, places[step], e, rows) + got[(self.index, *e, slice(None), self.cols)].astype(f32)
                    out[(*e, slice(None), self.cols)] = value.astype(bf16)
                self.each(phase, body)
                busy[key, self.c] = [self.send(f'f{half}', phase, lambda key=key: self.cut(key),
                                               lambda dst=dst, rows=rows: self.cut(f'{dst}{phase}', self.index, rows=rows), step)]

        def total(self, phase):
            self.arrived(phase, 'p0', 'p1', 'f0', 'f1')
            p = ring[self.dims[phase]][0]

            def body(e):
                got = [self.buf[f'{name}{phase}'][(self.index, *e, slice(None), self.cols)].astype(f32)
                       for name in ('froml', 'fromr')]
                value = self.share(phase, p, e, pl.ds(0, 32)) + got[0] + got[1]
                if phase == 0:
                    self.buf['S1'][(*e, slice(None), self.cols)] = value
                elif phase == 1:
                    self.buf['S2'][(self.slot, *e, slice(None), self.cols)] = value
                elif self.g == STEM:
                    out_s[pl.ds(32 * self.c, 32), :] = value
                elif self.g == HEAD:
                    out_h[...] = value
                else:
                    out_c[self.g, :, pl.ds(*COLS[self.c])] = value
            self.each(phase, body)

        def run(self, stage):
            if stage == 0:
                product(self)
            elif stage == 7:
                self.total(2)
            elif stage % 2 == 0:
                self.beside(stage // 2 - 1)
            else:
                if stage > 1:
                    self.total(stage // 2 - 1)
                self.opposite(stage // 2)

    units = [Unit(g, c) for g, c in UNITS]
    bursts = dict(BACK_ORDER)

    def step(which, stage):
        if stage == 'L':
            net.arrived(*NEEDS[which])
            for copy in loads(which):
                copy.start()
        else:
            units[which].run(stage)

    def burst(name):
        for s in bursts.get(name, ()):
            step(*s)

    def during(name, count):
        def run(i):
            for n in range(1, count):
                if bursts.get(f'{name}{n}'):
                    pl.when(i == n)(functools.partial(burst, f'{name}{n}'))
        return run

    load = pltpu.make_async_copy(xmid.at[1], x_v.at[:, pl.ds(0, ROWS)], sem.at[0])
    load.start()
    mask = row_mask()
    rest = pl.ds(ROWS, XROWS - ROWS)
    put(d_v, rest, jnp.zeros((XROWS - ROWS, CH), f32))
    put(x_v, rest, jnp.zeros((XROWS - ROWS, CH), f32))
    gvec[...] = jnp.zeros_like(gvec)
    tk = b['tk']
    tk[...] = jnp.zeros_like(tk)

    @pl.loop(0, TOK)
    def _(s):
        put(d_v, pl.ds(pl.multiple_of(s * IMG, IMG), IMG), dx0[...])

    def add(row, value):
        gvec[row:row + 1, :] += jnp.sum(value, axis=0, keepdims=True)

    def add_token(n, value, start=0):
        tk[n, :, :, :, :, pl.ds(start, value.shape[1])] += value.reshape(4, 4, 2, 16, value.shape[1])

    for l in (1, 0):
        r = 1 + 5 * l
        free('do')
        for at, size in CHUNKS:
            d = get(d_v, pl.ds(at, size))
            add(r + 4, d)
            do_v[pl.ds(at, size), :] = d.astype(bf16)
        keep = pltpu.make_async_copy(do_v, dout.at[l], sem.at[1])
        keep.start()
        if l == 1:
            pl.semaphore_wait(barrier, 10)
            swap('dout1', 'act1', 'hl', 'hr', 'vin1', 'act0', 'vin0', 'pat')
        else:
            swap('dout0')
        busy['do'] = [f'dout{l}']
        keep.wait()
        burst(f'c{l}_0')
        run = during(f'c{l}_', NBLK)

        def blocks(i, slot):
            t, h = i // 2, i % 2
            part = pl.ds(pl.multiple_of(h * BLK, BLK), BLK)
            whole = pl.ds(pl.multiple_of(i * BLK, BLK), BLK)
            return [(wc.at[2 * l, t, :, :, :, :, part], w1_v.at[slot]), (wc.at[2 * l + 1, t, h], w2_v.at[slot]),
                    (pre_in.at[l, :, whole], pre_v.at[slot])]

        def outs(i, slot):
            return [(dp_v.at[slot], dpre.at[l, :, pl.ds(pl.multiple_of(i * BLK, BLK), BLK)])]

        def channel(i, slot):
            run(i)

            for n in range(2):
                cols = slice(256 * n, 256 * n + 256)
                d = dot_nt(do_v[...], w2_v[slot, 2 * n:2 * n + 2].reshape(256, CH)) * pre_v[slot, :, cols]
                gbch1[l:l + 1, pl.ds(pl.multiple_of(i * BLK + 256 * n, 256), 256)] = jnp.sum(d, axis=0, keepdims=True)
                dp_v[slot, :, cols] = d.astype(bf16)

            @pl.when(i == 0)
            def _():
                dv_v[...] = jnp.zeros_like(dv_v)
            for n in range(2):
                cols = slice(512 * n, 512 * n + 512)
                dv_v[:, cols] += dot_nt(dp_v[slot], w1_v[slot, n].reshape(512, BLK))
        for_blocks(Stream(sem_w, blocks, NBLK), channel, Stream(sem_o, outs, NBLK))
        swap(f'dpre{l}')
        burst(f'l{l}')
        load.wait()

        @pl.loop(0, ROWS // TPAD)
        def _(n):
            rows = pl.ds(pl.multiple_of(n * TPAD, TPAD), TPAD)
            std, inv = standardize(get(x_v, rows))
            d = dv_v[rows, :]
            add(r + 2, d * std)
            add(r + 3, d)
            put(d_v, rows, get(d_v, rows) + norm_grad(d, vec[r + 2:r + 3, :], std, inv))
        load = pltpu.make_async_copy(xin.at[l], x_v.at[:, pl.ds(0, ROWS)], sem.at[0])
        load.start()
        burst(f't{l}_0')
        load.wait()
        run = during(f't{l}_', IMG)

        @pl.loop(0, IMG)
        def _(m):
            run(m)
            std, inv = standardize(get(x_v, image(m)))
            a = with_bias_rows(std * vec[r:r + 1, :] + vec[r + 1:r + 2, :])
            d_mid = get(d_v, image(m))
            dm = d_mid.astype(bf16)
            parts = []
            for n in range(TOK_CUTS):
                cols = slice(CH // TOK_CUTS * n, CH // TOK_CUTS * (n + 1))
                value, slope = gelu_both(dot_nn(wt[l, :, 0:TPAD], a[:, cols]))
                add_token(2 + l, dot_nt(value.astype(bf16), dm[:, cols]))
                dh = dot_nn(wt[2 + l, :, 0:TPAD], dm[:, cols]) * slope
                add_token(l, jnp.sum(dh, axis=-1, keepdims=True), 64)
                dh = dh.astype(bf16)
                add_token(l, dot_nt(dh, a[:, cols]))
                parts.append(dot_nn(wt_t[l], dh))
            d = jnp.where(mask, jnp.concatenate(parts, axis=1), 0.0)
            add(r, d * std)
            add(r + 1, d)
            put(d_v, image(m), d_mid + norm_grad(d, vec[r:r + 1, :], std, inv))
        if l == 1:
            load = pltpu.make_async_copy(xmid.at[0], x_v.at[:, pl.ds(0, ROWS)], sem.at[0])
            load.start()
            burst('d0')

    burst('fin')
    free('do')
    for at, size in CHUNKS:
        d = get(d_v, pl.ds(at, size))
        add(0, d)
        do_v[pl.ds(at, size), :] = d.astype(bf16)
    keep = pltpu.make_async_copy(do_v, dres, sem.at[1])
    keep.start()
    swap('dres')
    keep.wait()
    small_pack(b, x_v, d_v, gvec, hstat, gbch1, gbh)

    last = []

    def put_small(name, src, dst, target):
        last.append(name)
        net.start(name, lambda: (src, dst, target))

    def small(n):
        x, z, y = (ring[d][0] for d in 'xzy')
        net.arrived(*last)
        last.clear()
        if n == 0:
            put_small(('sm', 0), b['sm'].at[:, :, :, k2], b['sm1'], partner)
            put_small(('tk', 0), b['tk'].at[:, :, :, k2], b['tk1'], partner)
        elif n == 1:
            b['sm1'][...] += b['sm'][:, :, :, k]
            b['tk1'][...] += b['tk'][:, :, :, k]
            for s in (1, 2, 3):
                put_small(('sm', 1, s), b['sm1'].at[ring['x'][s]], b['sm2'].at[s - 1], peers['x', s])
                put_small(('tk', 1, s), b['tk1'].at[:, ring['z'][s]], b['tk2'].at[s - 1], peers['z', s])
        elif n == 2:
            b['sm_s1'][...] = b['sm1'][x] + b['sm2'][0] + b['sm2'][1] + b['sm2'][2]
            b['tk_s1'][...] = b['tk1'][:, z] + b['tk2'][0] + b['tk2'][1] + b['tk2'][2]
            for s in (1, 2, 3):
                put_small(('sm', 2, s), b['sm_s1'].at[ring['z'][s]], b['sm3'].at[s - 1], peers['z', s])
                put_small(('tk', 2, s), b['tk_s1'].at[:, ring['y'][s]], b['tk3'].at[s - 1], peers['y', s])
        elif n == 3:
            b['sm_s2'][...] = b['sm_s1'][z] + b['sm3'][0] + b['sm3'][1] + b['sm3'][2]
            b['tk_s2'][...] = b['tk_s1'][:, y] + b['tk3'][0] + b['tk3'][1] + b['tk3'][2]
            for s in (1, 2, 3):
                put_small(('sm', 3, s), b['sm_s2'].at[ring['y'][s]], b['sm4'].at[s - 1], peers['y', s])
                put_small(('tk', 3, s), b['tk_s2'], b['tk4'].at[s - 1], peers['x', s])
        else:
            sm_own[...] = b['sm_s2'][y] + b['sm4'][0] + b['sm4'][1] + b['sm4'][2]
            ordered = []
            for place in range(4):
                value = b['tk_s2'][...]
                for s in (1, 2, 3):
                    value = jnp.where(ring['x'][4 - s] == place, b['tk4'][s - 1], value)
                ordered.append(value)
            tk_own[...] = (ordered[0] + ordered[1]) + (ordered[2] + ordered[3])

    tail = bursts.get('end', ())
    small(0)
    for n, s in enumerate(tail):
        step(*s)
        if n in (8, 18, 28, 38):
            small(1 + (8, 18, 28, 38).index(n))
    net.finish()
    assert len(net.builds) <= BACK_COPIES, len(net.builds)


def back(*operands):
    a, v = pl.BlockSpec(memory_space=pl.ANY), pl.BlockSpec(memory_space=pltpu.VMEM)
    S, V, DMA = jax.ShapeDtypeStruct, pltpu.VMEM, pltpu.SemaphoreType.DMA
    return pl.pallas_call(
        back_kernel, name='back',
        in_specs=[a] * 7 + [v] * 8, out_specs=[v] * 5 + [a] * 9,
        out_shape=[S((N_CH, 32, 1024), f32), S((96, 256), f32), S((32, 256), f32), S((8, 128), f32), S((4, 16, 128), f32),
                   S((2, ROWS, CHH), bf16), S((2, ROWS, CH), bf16), S((ROWS, CH), bf16), S((2, ROWS, 2048), bf16),
                   S((2, ROWS, 512), bf16), S((ROWS, 1536), bf16), S((2, ROWS, CHH), bf16), S((2, ROWS, CH), bf16),
                   S((ROWS, CH), bf16)],
        scratch_shapes=[reduce_scratch(), small_scratch(), V((2, ROWS, CHH), bf16), V((2, ROWS, CH), bf16), V((IMG, 512), bf16),
                        V((IMG, CH), bf16), V((16, CH), f32), V((2, CHH), f32), V((CH // 128, XROWS, 128), f32),
                        V((CH // 128, XROWS, 128), f32), V((ROWS, CH), f32), V((ROWS, CH), bf16), V((2, 2, 4, 4, 32, BLK), bf16),
                        V((2, 4, 4, 32, CH), bf16), V((2, ROWS, BLK), f32), V((2, ROWS, BLK), bf16), DMA((BACK_COPIES,)), DMA((BACK_COPIES,)), DMA((4,)), DMA((2,)), DMA((2, 3)),
                        DMA((2, 1))],
        compiler_params=pltpu.CompilerParams(collective_id=1, has_side_effects=True, vmem_limit_bytes=64 * 1024 * 1024 - 65536),
        cost_estimate=pl.CostEstimate(flops=120_000_000_000, bytes_accessed=200_000_000, transcendentals=0),
    )(*operands)


def finish_kernel(c, stem, head, sm, tk, loss, o_stem, o_bstem, o_ln1g, o_ln1b, o_wt1, o_bt1, o_wt2, o_ln2g, o_ln2b, o_ch1,
                  o_bch1, o_ch2, o_bch2, o_lnfg, o_lnfb, o_head, o_bhead):
    def core_last(value, pick):
        got = dot_nt(jnp.concatenate(three_parts(value), axis=0), pick)
        n = value.shape[0]
        return got[0:n] + got[n:2 * n] + got[2 * n:3 * n]
    pick = core_first(1024, 1024, 32)
    for l in range(2):
        o_ch1[l] = core_last(c[2 * l], pick)
        o_ch2[l] = core_last(c[2 * l + 1], pick)
    o_stem[...] = core_last(stem[...], core_first(256, 256, 32))
    o_head[...] = head[:, 0:250]
    own = sm[...]
    turned = jnp.concatenate([own, jnp.zeros((120, 128), f32)], axis=0).T
    for ref, n in ((o_bstem, 0), (o_lnfg, 11), (o_lnfb, 12)):
        ref[...] = turned[n, 0:8]
    for n, ref in enumerate((o_ln1g, o_ln1b, o_ln2g, o_ln2b, o_bch2)):
        for l in range(2):
            ref[pl.ds(l, 1), :] = turned[1 + 5 * l + n:2 + 5 * l + n, 0:8]
    o_bch1[...] = own[0:2, 32:64]
    classes = jnp.concatenate([own[2 + q:3 + q, 64:128] for q in range(4)], axis=1)
    o_bhead[...] = classes[0, 0:250]
    loss[...] = own[6:7, 64:65] * (1.0 / 1024)
    for l in range(2):
        o_wt1[l] = tk[l, :, 0:TOK]
        o_wt2[l] = tk[2 + l, :, 0:TOK]
        tall = jnp.concatenate([tk[l], jnp.zeros((112, 128), f32)], axis=0).T
        o_bt1[pl.ds(l, 1), :] = tall[64:65, 0:16]


def finish(*operands):
    S = jax.ShapeDtypeStruct
    v = pl.BlockSpec(memory_space=pltpu.VMEM)
    return pl.pallas_call(
        finish_kernel, name='finish', in_specs=[v] * 5, out_specs=[v] * 18,
        out_shape=[S((1, 1), f32), S((96, 256), f32), S((8,), f32), S((2, 8), f32), S((2, 8), f32), S((2, 16, TOK), f32),
                   S((2, 16), f32), S((2, 16, TOK), f32), S((2, 8), f32), S((2, 8), f32), S((2, 32, 1024), f32), S((2, 32), f32),
                   S((2, 32, 1024), f32), S((2, 8), f32), S((8,), f32), S((8,), f32), S((32, 250), f32), S((250,), f32)],
    )(*operands)

CHANNEL_AXES = ('tp', 'fsdp')


def weight_specs():
    vec_spec = P(CHANNEL_AXES)
    layer_vec = P(None, CHANNEL_AXES)
    return (P('fsdp', 'tp'), vec_spec, layer_vec, layer_vec, P(None, None, 'fsdp'), P(None, 'fsdp'),
            P(None, 'fsdp', None), layer_vec, layer_vec, P(None, 'fsdp', 'tp'), layer_vec,
            P(None, CHANNEL_AXES, None), layer_vec, vec_spec, vec_spec, P('fsdp', 'tp'), P('tp'))


def solution(mesh):
    def step(patches, labels, w_stem, b_stem, ln1_g, ln1_b, w_tok1, b_tok1, w_tok2,
             ln2_g, ln2_b, w_ch1, b_ch1, w_ch2, b_ch2, lnf_g, lnf_b, w_head, b_head):
        wc, pat, xin, xmid, vin, pre, act, hl, hr, dx0, hstat, gbh, vec, wt, wt_t = front(
            labels, patches.transpose(1, 0, 2), w_stem, w_ch1, w_ch2, w_head, w_tok1.transpose(0, 2, 1), w_tok2, b_tok1, b_ch1,
            b_head, b_stem, ln1_g, ln1_b, ln2_g, ln2_b, b_ch2, lnf_g, lnf_b)
        sums = back(xin, xmid, pre, wc, act, vin, pat, hl, hr, dx0, hstat, gbh, wt, wt_t, vec)[:5]
        loss, g_s, g_bs, g_1g, g_1b, g_t1, g_bt, g_t2, g_2g, g_2b, g_c1, g_b1, g_c2, g_b2, g_fg, g_fb, g_h, g_bh = finish(*sums)
        return (loss.reshape(()), g_s, g_bs, g_1g, g_1b, g_t1.transpose(0, 2, 1), g_bt, g_t2, g_2g, g_2b, g_c1, g_b1, g_c2, g_b2,
                g_fg, g_fb, g_h, g_bh)

    specs = weight_specs()
    return jax.shard_map(step, mesh=mesh, in_specs=(P('fsdp', None, None), P('fsdp')) + specs,
                         out_specs=(P(),) + specs, check_vma=False)
```

```python
import functools

import jax
import jax.numpy as jnp
from jax import lax
from jax.experimental import pallas as pl
from jax.experimental.pallas import tpu as pltpu
from jax.sharding import PartitionSpec as P

MESH = pl.DeviceIdType.MESH
ORDERS = (('x', 'y', 'z'), ('y', 'z', 'x'), ('z', 'x', 'y'))
COLS = ((0, 384), (384, 384), (768, 256))
N_CH = 4
STEM, HEAD = 4, 5
bf16, f32 = jnp.bfloat16, jnp.float32


def my_place():
    f = lax.axis_index('fsdp')
    return {'x': lax.axis_index('tp'), 'z': f // 8, 'y': (f // 2) % 4, 'k': f % 2}


def moved(place, dim, step):
    new = dict(place)
    new[dim] = 1 - place['k'] if dim == 'k' else (place[dim] + step) % 4
    return new


def device(place):
    return {'tp': place['x'], 'fsdp': (place['z'] * 4 + place['y']) * 2 + place['k']}


EPS = 1e-6
TOK, TPAD = 49, 56
IMG = 8
ROWS, XROWS = IMG * TOK, IMG * TPAD
CHUNKS = ((0, 112), (112, 112), (224, 112), (336, 56))
CH, TOKH, CHH = 1024, 512, 4096
BLK = 512
NBLK = CHH // BLK
GELU_C, GELU_A = 0.7978845608028654, 0.044715


def dot_nn(a, b):
    return lax.dot_general(a, b, (((1,), (0,)), ((), ())), preferred_element_type=f32)


def dot_nt(a, b):
    return lax.dot_general(a, b, (((1,), (1,)), ((), ())), preferred_element_type=f32)


def dot_tn(a, b):
    return lax.dot_general(a, b, (((0,), (0,)), ((), ())), preferred_element_type=f32)


def gelu_both(x):
    sq = x * x
    half = 0.5 * jnp.tanh(x * (GELU_C + (GELU_C * GELU_A) * sq))
    rise = 0.5 + half
    value = x * rise
    return value, rise + value * (0.5 - half) * (2.0 * GELU_C + (6.0 * GELU_C * GELU_A) * sq)


def standardize(x):
    mean = jnp.mean(x, axis=-1, keepdims=True)
    cent = x - mean
    inv = lax.rsqrt(jnp.mean(cent * cent, axis=-1, keepdims=True) + EPS)
    return cent * inv, inv


def norm_grad(d, gain, std, inv):
    gs = d * gain
    m0 = jnp.mean(gs, axis=-1, keepdims=True)
    m1 = jnp.mean(gs * std, axis=-1, keepdims=True)
    return inv * (gs - m0 - std * m1)


def row_mask(rows=TPAD):
    return lax.broadcasted_iota(jnp.int32, (rows, 1), 0) < TOK


def image(b):
    return pl.ds(b, TPAD, stride=IMG)


def get(ref, rows):
    return jnp.concatenate([ref[n, rows, :] for n in range(CH // 128)], axis=1)


def put(ref, rows, value):
    for n in range(CH // 128):
        ref[n, rows, :] = value[:, 128 * n:128 * (n + 1)]


class Stream:
    def __init__(self, sem, copies, count):
        self.sem, self.copies, self.count = sem, copies, count

    def make(self, i, slot):
        return [pltpu.make_async_copy(src, dst, self.sem.at[slot, n]) for n, (src, dst) in enumerate(self.copies(i, slot))]

    def start(self, i, slot):
        for copy in self.make(i, slot):
            copy.start()

    def wait(self, i, slot):
        for copy in self.make(i, slot):
            copy.wait()


def for_blocks(stream, body, out=None):
    n = stream.count
    stream.start(0, 0)

    @pl.loop(0, n)
    def _(i):
        slot = i % 2
        stream.wait(i, slot)

        @pl.when(i + 1 < n)
        def _():
            stream.start(i + 1, 1 - slot)
        if out is not None:
            @pl.when(i >= 2)
            def _():
                out.wait(i - 2, slot)
        body(i, slot)
        if out is not None:
            out.start(i, slot)
    if out is not None:
        out.wait(n - 2, n % 2)
        out.wait(n - 1, 1 - n % 2)


TOK_CUTS = 4
FRONT_COPIES = 270
EARLY = [('stem', c) for c in range(3)] + [('ch', c, p) for p in 'ab' for c in range(3)] + [('head', 2)]
PARTS = {'a': pl.ds(0, 2), 'b': pl.ds(2, 2)}
LATE = [('stem', c, None) for c in range(3)] + [('ch', c, g) for g in range(N_CH) for c in range(3)] + [('head', 2, None)]
UNIT_GROUP = {('stem', None): 0, ('ch', 0): 1, ('ch', 1): 2, ('ch', 2): 3, ('ch', 3): 4, ('head', None): 5}
EVERY = pl.ds(0, 4)
FRONT_ORDER = (
    ('prep', (('M0', ('sm',)), ('M0', ('tk',)), ('A0', ('stem', 0)), ('A0', ('stem', 1)), ('A0', ('stem', 2)),
        ('A0', ('ch', 0, 'a')), ('A0', ('ch', 0, 'b')), ('A0', ('ch', 1, 'a')), ('A0', ('ch', 1, 'b')),
        ('A0', ('ch', 2, 'a')), ('A0', ('ch', 2, 'b')), ('A0', ('head', 2)),)),
    ('unpack', (('M1', ('sm',)), ('M1', ('tk',)), ('A', ('stem', 0)), ('A', ('stem', 1)), ('A', ('stem', 2)),
        ('A', ('ch', 0, 'a')), ('A', ('ch', 1, 'a')), ('A', ('ch', 2, 'a')), ('A', ('ch', 0, 'b')), ('A', ('ch', 2, 'b')),
        ('A', ('head', 2)), ('A', ('ch', 1, 'b')), ('B', ('stem', 0)), ('M2', ('sm',)), ('B', ('stem', 1)),
        ('B', ('ch', 0, 'a')), ('B', ('ch', 1, 'a')), ('B', ('ch', 0, 'b')), ('B', ('ch', 1, 'b')), ('M2', ('tk',)),
        ('B', ('stem', 2)), ('B', ('head', 2)), ('C', ('stem', 0)), ('B', ('ch', 2, 'a')), ('B', ('ch', 2, 'b')),
        ('M3', ('sm',)), ('C', ('stem', 2)), ('C', ('stem', 1)), ('C', ('head', 2)),)),
    ('stem0', (('D', ('stem', 0, None)), ('C', ('ch', 0, 'a')), ('C', ('ch', 1, 'a')), ('C', ('ch', 2, 'a')),
        ('D', ('stem', 2, None)), ('D', ('stem', 1, None)), ('D', ('ch', 2, 0)), ('D', ('ch', 2, 1)), ('D', ('ch', 0, 0)),
        ('D', ('ch', 0, 1)), ('E', ('stem', 0, None)), ('E', ('stem', 2, None)), ('E', ('stem', 1, None)),
        ('D', ('ch', 1, 0)), ('D', ('ch', 1, 1)), ('F', ('stem', 1, None)), ('E', ('ch', 2, 0)), ('E', ('ch', 0, 0)),
        ('E', ('ch', 2, 1)), ('F', ('stem', 2, None)), ('C', ('ch', 0, 'b')), ('C', ('ch', 1, 'b')), ('C', ('ch', 2, 'b')),
        ('D', ('head', 2, None)), ('E', ('ch', 1, 0)), ('F', ('ch', 2, 0)), ('E', ('ch', 0, 1)), ('F', ('stem', 0, None)),
        ('F', ('ch', 2, 1)), ('D', ('ch', 0, 2)), ('D', ('ch', 0, 3)),)),
    ('stem1', (('E', ('ch', 1, 1)),)),
    ('stem2', (('F', ('ch', 0, 0)), ('D', ('ch', 2, 2)), ('D', ('ch', 2, 3)),)),
    ('tok0_0', (('D', ('ch', 1, 2)), ('D', ('ch', 1, 3)), ('E', ('head', 2, None)),)),
    ('tok0_1', (('F', ('ch', 1, 0)),)),
    ('tok0_3', (('F', ('ch', 0, 1)),)),
    ('tok0_5', (('F', ('ch', 1, 1)), ('E', ('ch', 2, 2)),)),
    ('ch0_1', (('E', ('ch', 0, 2)), ('E', ('ch', 2, 3)),)),
    ('ch0_2', (('E', ('ch', 1, 2)), ('F', ('head', 2, None)),)),
    ('ch0_4', (('F', ('ch', 2, 2)),)),
    ('ch0_5', (('E', ('ch', 0, 3)), ('F', ('ch', 2, 3)),)),
    ('ch0_7', (('E', ('ch', 1, 3)),)),
    ('tok1_0', (('F', ('ch', 0, 2)),)),
    ('tok1_1', (('F', ('ch', 1, 2)),)),
    ('tok1_3', (('F', ('ch', 0, 3)),)),
    ('tok1_5', (('F', ('ch', 1, 3)),)),
)


class Net:
    def __init__(self, send_sems, recv_sems):
        self.send_sems, self.recv_sems, self.names, self.builds, self.done = send_sems, recv_sems, {}, [], set()

    def copy(self, name):
        n = self.names[name]
        src, dst, target = self.builds[n]()
        return pltpu.make_async_remote_copy(src_ref=src, dst_ref=dst, send_sem=self.send_sems.at[n],
                                            recv_sem=self.recv_sems.at[n], device_id=target, device_id_type=MESH)

    def start(self, name, build):
        self.names[name] = len(self.builds)
        self.builds.append(build)
        self.copy(name).start()

    def arrived(self, *names):
        for name in names:
            self.copy(name).wait_recv()

    def finish(self):
        for name in self.names:
            if name not in self.done:
                self.copy(name).wait_send()


def core_first(size, cols, each):
    half = cols // 2
    row = lax.broadcasted_iota(jnp.int32, (size, size), 0)
    col = lax.broadcasted_iota(jnp.int32, (1, size), 1)
    source = col % half // each * (2 * each) + col // half * each + col % each
    return jnp.where(row == source, 1.0, 0.0).astype(bf16)


def three_parts(x):
    hi = x.astype(bf16)
    rest = x - hi.astype(f32)
    mid = rest.astype(bf16)
    return hi, mid, (rest - mid.astype(f32)).astype(bf16)


def with_bias_rows(a):
    row = lax.broadcasted_iota(jnp.int32, (TPAD, 1), 0)
    return jnp.where(row < TOK, a, jnp.where(row < TOK + 3, 1.0, 0.0)).astype(bf16)


def front_kernel(labels, patches, w_stem, w_ch1, w_ch2, w_head, w_tok1, w_tok2, b_tok1, b_ch1, b_head, b_stem, ln1_g, ln1_b,
                 ln2_g, ln2_b, b_ch2, lnf_g, lnf_b,
                 wc, pat_out, xin, xmid, vout, pre_out, act_out, hl, hr, dx0, hstat, gbh, vec, wt, wt_t,
                 pc, ps, ph, tk_f, tk_p, sm_p, bh_p, ws, wh, tk_v, sm_v, sm_2, bh_v, bch1,
                 turn, p_v, pk_v, x_a, x_b, v_v, w1_v, w2_v, pre_v, act_v, g_v,
                 send_sems, recv_sems, sem, sem_w, sem_o, sem_x):
    me = my_place()
    other = moved(me, 'k', 1)
    load_p = pltpu.make_async_copy(patches.at[:, pl.ds(pl.multiple_of(me['x'] * IMG, IMG), IMG)], p_v, sem.at[0])
    load_p.start()

    barrier = pltpu.get_barrier_semaphore()
    for dim in 'xyz':
        for step in (1, 2, 3):
            pl.semaphore_signal(barrier, inc=1, device_id=device(moved(me, dim, step)), device_id_type=MESH)
    pl.semaphore_signal(barrier, inc=1, device_id=device(other), device_id_type=MESH)

    stem = dot_nn(w_stem[...].astype(bf16), core_first(256, 256, 32)).astype(bf16)
    ps[0], ps[1] = stem[:, 0:128], stem[:, 128:256]
    pick = core_first(1024, 1024, 32)
    for l in range(2):
        pc[2 * l] = dot_nn(w_ch1[l].astype(bf16), pick).astype(bf16)
        pc[2 * l + 1] = dot_nn(w_ch2[l].astype(bf16), pick).astype(bf16)
    ph[...] = jnp.zeros_like(ph)
    ph[:, pl.ds(0, 250)] = w_head[...].astype(bf16)
    turn[...] = jnp.zeros_like(turn)
    for n, ref in ((0, b_stem), (11, lnf_g), (12, lnf_b)):
        turn[n, pl.ds(0, 8)] = ref[...]
    for n, ref in enumerate((ln1_g, ln1_b, ln2_g, ln2_b, b_ch2)):
        for l in range(2):
            turn[pl.ds(1 + 5 * l + n, 1), pl.ds(0, 8)] = ref[pl.ds(l, 1), :]
    turn[pl.ds(16, 2), pl.ds(0, 16)] = b_tok1[...]
    turned = turn[...].T
    tk_f[...] = jnp.zeros_like(tk_f)
    for l in range(2):
        tk_f[l, :, pl.ds(0, TOK)] = w_tok1[l]
        tk_f[2 + l, :, pl.ds(0, TOK)] = w_tok2[l]
        for n, part in enumerate(three_parts(turned[0:16, 16 + l:17 + l])):
            tk_f[l, :, pl.ds(TOK + n, 1)] = part.astype(f32)
    tk_p[...] = tk_f[...].astype(bf16)
    sm_p[...] = jnp.zeros_like(sm_p)
    sm_p[:, pl.ds(0, 16)] = turned[0:8, 0:16]
    sm_p[pl.ds(0, 2), pl.ds(32, 32)] = b_ch1[...]
    bh_p[...] = jnp.full_like(bh_p, -1e30)
    bh_p[0, pl.ds(0, 250)] = b_head[...]

    net = Net(send_sems, recv_sems)
    core = me['k']
    ring = {d: [moved(me, d, n)[d] for n in range(4)] for d in 'xyz'}
    columns = [pl.ds(pl.multiple_of(x * 256, 256), 256) for x in ring['x']]
    stem_columns = [pl.ds(pl.multiple_of(x * 128, 128), 128) for x in ring['x']]
    peers = {(d, n): device(moved(me, d, n)) for d in 'xyz' for n in (1, 2, 3)}
    partner = device(other)
    here = {'x': 0, 'y': 0, 'z': 0}

    def view(unit, block, half=None):
        kind, colour = unit[:2]
        x, z, y = (EVERY if block[d] is None else ring[d][block[d]] for d in 'xzy')
        r0, rn = (0, 32) if half is None else (16 * half, 16)
        if kind == 'ch':
            c0, cn = COLS[colour]
            g = PARTS.get(unit[2], unit[2])
            return wc.at[g, x, core, z, y, pl.ds(r0, rn), pl.ds(c0, cn)]
        if kind == 'stem':
            cols = pl.ds(0, 512) if x is EVERY else stem_columns[block['x']]
            return ws.at[:, z, y, core, pl.ds(32 * colour + r0, rn), cols]
        cols = pl.ds(0, CH) if x is EVERY else columns[block['x']]
        return wh.at[core, z, y, pl.ds(r0, rn), cols]

    def piece(unit):
        kind, colour = unit[:2]
        if kind == 'ch':
            return pc.at[PARTS[unit[2]], :, pl.ds(*COLS[colour])]
        return ps.at[:, pl.ds(32 * colour, 32), :] if kind == 'stem' else ph.at[:, :]

    def exchange(unit, tag, dim, block):
        for side, step in (('l', 1), ('r', 3)):
            def build(step=step):
                part = view(unit, block)
                return (piece(unit) if tag == '1' else part), part, peers[dim, step]
            net.start((unit, tag, side), build)

    def forward_half(unit, tag, dim, block):
        for half, (origin, target, side) in enumerate(((3, 1, 'l'), (1, 3, 'r'))):
            def build(half=half, origin=origin, target=target):
                part = view(unit, {**block, dim: origin}, half)
                return part, part, peers[dim, target]
            net.start((unit, tag, side), build)

    def swap(unit, tag, block):
        def build():
            part = view(unit, block)
            return part, part, partner
        net.start((unit, tag), build)

    own = pltpu.make_async_copy(pc, wc.at[:, me['x'], me['k'], me['z'], me['y']], sem.at[1])
    own.start()
    mine = pl.ds(pl.multiple_of(me['x'] * 256, 256), 256)
    for n in range(2):
        ws[n, me['z'], me['y'], me['k'], :, stem_columns[0]] = ps[n]
    wh[me['k'], me['z'], me['y'], :, mine] = ph[...]
    sm_v[me['x'], me['z'], me['y'], me['k']] = sm_p[...]
    tk_v[:, me['z'], me['y'], me['k']] = tk_p[...]
    bh_v[:, mine] = bh_p[...]
    own.wait()
    pl.semaphore_wait(barrier, 10)

    def small(kind, n):
        dims = 'xyz' if kind == 'sm' else 'yz'
        at = {d: EVERY if d in dims[:n] else ring[d][0] for d in 'xyz'}

        def part():
            if kind == 'sm':
                return sm_v.at[at['x'], at['z'], at['y'], core]
            return tk_v.at[:, at['z'], at['y'], core]
        if n > 0:
            net.arrived(*[(kind, n - 1, s) for s in (1, 2, 3)])
        if n < len(dims):
            for s in (1, 2, 3):
                net.start((kind, n, s), lambda s=s: (part(), part(), peers[dims[n], s]))
            if kind == 'sm' and n == 0:
                def head_bias():
                    return bh_v.at[:, columns[0]]
                for s in (1, 2, 3):
                    net.start(('bh', s), lambda s=s: (head_bias(), head_bias(), peers['x', s]))
        else:
            net.start((kind, 'k'), lambda: (part(), part(), partner))

    def step(name, unit):
        if name[0] == 'M':
            small(unit[0], int(name[1]))
            return
        d1, d2, d3 = ORDERS[unit[1]]
        early = unit[:2] if unit[0] != 'ch' or unit[2] in PARTS else ('ch', unit[1], 'a' if unit[2] < 2 else 'b')
        plane = {**here, d1: None, d2: None}
        if name == 'A0':
            exchange(unit, '1', d1, here)
        elif name == 'A':
            net.arrived((unit, '1', 'l'), (unit, '1', 'r'))
            forward_half(unit, '1h', d1, here)
        elif name == 'B':
            net.arrived((unit, '1h', 'l'), (unit, '1h', 'r'))
            exchange(unit, '2', d2, {**here, d1: None})
        elif name == 'C':
            net.arrived((unit, '2', 'l'), (unit, '2', 'r'))
            forward_half(unit, '2h', d2, {**here, d1: None})
        elif name == 'D':
            if early not in planes:
                planes.add(early)
                net.arrived((early, '2h', 'l'), (early, '2h', 'r'))
            exchange(unit, '3', d3, plane)
            swap(unit, 'k0', plane)
        elif name == 'E':
            net.arrived((unit, '3', 'l'), (unit, '3', 'r'))
            forward_half(unit, '3h', d3, plane)
            for n in (1, 3):
                swap(unit, f'k{n}', {**plane, d3: n})
        else:
            net.arrived((unit, '3h', 'l'), (unit, '3h', 'r'))
            swap(unit, 'k2', {**plane, d3: 2})

    planes = set()
    awaited = set()

    def need(group):
        for u in LATE:
            if UNIT_GROUP[u[0], u[2]] <= group and u not in awaited:
                awaited.add(u)
                net.arrived(*[(u, f'k{n}') for n in range(4)])

    bursts = {name: steps for name, steps in FRONT_ORDER}

    def burst(name):
        for s in bursts.get(name, ()):
            step(*s)

    def during(name, count):
        def run(i):
            for n in range(1, count):
                if bursts.get(f'{name}{n}'):
                    pl.when(i == n)(functools.partial(burst, f'{name}{n}'))
        return run

    burst('prep')
    load_p.wait()
    pick = core_first(768, 768, 96)
    for g in range(4):
        part = dot_nn(p_v[:, :, pl.ds(768 * g, 768)].reshape(ROWS, 768), pick).astype(bf16)
        for n in range(2):
            pk_v[n, :, pl.ds(384 * g, 384)] = part[:, 384 * n:384 * n + 384]
    keep_p = pltpu.make_async_copy(pk_v, pat_out, sem.at[0])
    keep_p.start()

    burst('unpack')
    net.arrived(('sm', 'k'), ('tk', 'k'), ('bh', 1), ('bh', 2), ('bh', 3))
    sm_2[...] = sm_v[...].reshape(1024, 128)
    for n in range(8):
        tile = jnp.concatenate([sm_2[pl.ds((n % 4 * 4 + i) * 64 + n // 4 * 32, 32), :] for i in range(4)], axis=0)
        vec[:, pl.ds(128 * n, 128)] = tile.T[0:16, :]
    wt[...] = tk_v[...].reshape(4, TOKH, 128)
    for n in range(4):
        wt_t[n] = wt[n].astype(f32).T[0:TPAD].astype(bf16)
    for l in range(2):
        rows = jnp.concatenate(three_parts(sm_2[pl.ds(l, 128, stride=8), :]), axis=0)

        @pl.loop(0, 8)
        def _(n):
            lane = lax.broadcasted_iota(jnp.int32, (128, 512), 0)
            col = lax.broadcasted_iota(jnp.int32, (128, 512), 1)
            pick = jnp.where(lane == 32 + col % 32, 1.0, 0.0).astype(bf16)
            spread = dot_nn(rows, pick)
            value = spread[0:128] + spread[128:256] + spread[256:384]
            mine = lane == n // 2 * 32 + col // 32 * 2 + n % 2
            bch1[l:l + 1, pl.ds(pl.multiple_of(n * 512, 512), 512)] = jnp.sum(jnp.where(mine, value, 0.0), axis=0, keepdims=True)

    burst('stem0')
    need(0)
    run = during('stem', 4)
    put(x_a, pl.ds(ROWS, XROWS - ROWS), jnp.zeros((XROWS - ROWS, CH), f32))

    @pl.loop(0, 4)
    def _(i):
        run(i)
        cols = pl.ds(pl.multiple_of(i * 256, 256), 256)
        w = ws[i // 2, :, :, :, :, pl.ds(pl.multiple_of(i % 2 * 256, 256), 256)].reshape(3072, 256)
        value = dot_nn(p_v[...].reshape(ROWS, 3072), w) + vec[0:1, cols]
        for n in range(2):
            x_a[2 * i + n, pl.ds(0, ROWS), :] = value[:, 128 * n:128 * (n + 1)]

    wc_all = wc

    def add_rows(x_v, value):
        for n in range(CH // 128):
            x_v[n, pl.ds(0, ROWS), :] += value[:, 128 * n:128 * (n + 1)]

    for l in range(2):
        r = 1 + 5 * l
        x_old, x_v = ((x_a, x_b), (x_b, x_a))[l]
        burst(f'tok{l}_0')
        run = during(f'tok{l}_', IMG)
        save_in = pltpu.make_async_copy(x_old.at[:, pl.ds(0, ROWS)], xin.at[l], sem_x.at[3])
        save_in.start()

        @pl.loop(0, IMG)
        def _(b):
            run(b)
            x = get(x_old, image(b))
            std, _ = standardize(x)
            a = with_bias_rows(std * vec[r:r + 1, :] + vec[r + 1:r + 2, :])
            g_v[...] = gelu_both(dot_nn(wt[l, :, 0:TPAD], a))[0].astype(bf16)
            put(x_v, image(b), x + dot_nn(wt_t[2 + l], g_v[...]))
        save_mid = pltpu.make_async_copy(x_v.at[:, pl.ds(0, ROWS)], xmid.at[l], sem_x.at[0])
        save_mid.start()
        burst(f'ln{l}')

        for at, size in CHUNKS:
            std, _ = standardize(get(x_v, pl.ds(at, size)))
            v_v[pl.ds(at, size), :] = (std * vec[r + 2:r + 3, :] + vec[r + 3:r + 4, :]).astype(bf16)
        save_v = [pltpu.make_async_copy(v_v.at[:, pl.ds(512 * n, 512)], vout.at[l, n], sem_x.at[1 + n]) for n in range(2)]
        for copy in save_v:
            copy.start()
        burst(f'ch{l}_0')
        need(2 + 2 * l)
        save_mid.wait()

        def blocks(i, slot):
            t, h = i // 2, i % 2
            part = pl.ds(pl.multiple_of(h * BLK, BLK), BLK)
            return [(wc_all.at[2 * l, t, :, :, :, :, part], w1_v.at[slot]), (wc_all.at[2 * l + 1, t, h], w2_v.at[slot])]

        def outs(i, slot):
            part = pl.ds(pl.multiple_of(i * BLK, BLK), BLK)
            half = pl.ds(pl.multiple_of(i // 2 * BLK, BLK), BLK)
            return [(pre_v.at[slot], pre_out.at[l, :, part]), (act_v.at[slot], act_out.at[l, i % 2, :, half])]
        run = during(f'ch{l}_', NBLK)

        def channel(i, slot):
            run(i)
            part = pl.ds(pl.multiple_of(i * BLK, BLK), BLK)
            h = dot_nn(v_v[...], w1_v[slot].reshape(CH, BLK)) + bch1[l:l + 1, part]
            value, pre_v[slot] = gelu_both(h)
            act_v[slot] = value.astype(bf16)
            add_rows(x_v, dot_nn(act_v[slot], w2_v[slot].reshape(BLK, CH)))
        for_blocks(Stream(sem_w, blocks, NBLK), channel, Stream(sem_o, outs, NBLK))
        add_rows(x_v, jnp.broadcast_to(vec[r + 4:r + 5, :], (ROWS, CH)))
        for copy in (save_in, *save_v):
            copy.wait()

    burst('head')
    need(5)
    keep_p.wait()
    last = 11
    pooled = jnp.sum(get(x_a, pl.ds(0, ROWS)).reshape(TOK, IMG, CH), axis=0) * (1.0 / TOK)
    std, inv = standardize(pooled)
    head_in = (std * vec[last:last + 1, :] + vec[last + 1:last + 2, :]).astype(bf16)
    hl[...] = head_in
    w_h = wh[...].reshape(CH, CH)
    logits = dot_nn(head_in, w_h) + bh_v[0:1, :]
    row = lax.broadcasted_iota(jnp.int32, (IMG, 1), 0)
    label = jnp.zeros((IMG, 1), jnp.int32)
    for b in range(IMG):
        value = labels[me['x'] * IMG + b]
        label = jnp.where(row == b, value, label)
    label = label + 6 * sum(jnp.where(label >= edge, 1, 0) for edge in (250, 500, 750))
    is_label = lax.broadcasted_iota(jnp.int32, logits.shape, 1) == label
    top = jnp.max(logits, axis=-1, keepdims=True)
    ex = jnp.exp(logits - top)
    es = jnp.sum(ex, axis=-1, keepdims=True)
    nll = top + jnp.log(es) - jnp.sum(jnp.where(is_label, logits, 0.0), axis=-1, keepdims=True)
    d_logits = (ex / es - jnp.where(is_label, 1.0, 0.0)) * (1.0 / 1024)
    gbh[...] = jnp.sum(d_logits, axis=0, keepdims=True)
    d_bf = d_logits.astype(bf16)
    hr[...] = d_bf
    d_in = dot_nt(d_bf, w_h)
    hstat[0:1, :] = jnp.sum(d_in * std, axis=0, keepdims=True)
    hstat[1:2, :] = jnp.sum(d_in, axis=0, keepdims=True)
    hstat[2:3, :] = jnp.broadcast_to(jnp.sum(nll, axis=0, keepdims=True), (1, CH))
    dx0[...] = norm_grad(d_in, vec[last:last + 1, :], std, inv) * (1.0 / TOK)
    burst('end')
    net.finish()
    assert len(net.builds) <= FRONT_COPIES, len(net.builds)


def front(*operands):
    a, v = pl.BlockSpec(memory_space=pl.ANY), pl.BlockSpec(memory_space=pltpu.VMEM)
    S, V, DMA = jax.ShapeDtypeStruct, pltpu.VMEM, pltpu.SemaphoreType.DMA
    return pl.pallas_call(
        front_kernel, name='front',
        in_specs=[pl.BlockSpec(memory_space=pltpu.SMEM), a] + [v] * 17,
        out_specs=[a] * 7 + [v] * 8,
        out_shape=[S((N_CH, 4, 2, 4, 4, 32, 1024), bf16), S((2, ROWS, 1536), bf16), S((2, CH // 128, ROWS, 128), f32),
                   S((2, CH // 128, ROWS, 128), f32),
                   S((2, 2, ROWS, 512), bf16), S((2, ROWS, CHH), f32), S((2, 2, ROWS, 2048), bf16), S((IMG, CH), bf16),
                   S((IMG, CH), bf16), S((IMG, CH), f32), S((8, CH), f32), S((1, CH), f32), S((16, CH), f32),
                   S((4, TOKH, 128), bf16), S((4, TPAD, TOKH), bf16)],
        scratch_shapes=[V((N_CH, 32, 1024), bf16), V((2, 96, 128), bf16), V((32, 256), bf16), V((4, 16, 128), f32),
                        V((4, 16, 128), bf16), V((8, 128), f32), V((8, 256), f32), V((2, 4, 4, 2, 96, 512), bf16),
                        V((2, 4, 4, 32, CH), bf16), V((4, 4, 4, 2, 16, 128), bf16), V((4, 4, 4, 2, 8, 128), f32),
                        V((1024, 128), f32), V((8, CH), f32), V((2, CHH), f32),
                        V((128, 128), f32), V((TOK, IMG, 3072), bf16), V((2, ROWS, 1536), bf16), V((CH // 128, XROWS, 128), f32),
                        V((CH // 128, XROWS, 128), f32),
                        V((ROWS, CH), bf16), V((2, 2, 4, 4, 32, BLK), bf16), V((2, 4, 4, 32, CH), bf16),
                        V((2, ROWS, BLK), f32), V((2, ROWS, BLK), bf16), V((TOKH, CH), bf16),
                        DMA((FRONT_COPIES,)), DMA((FRONT_COPIES,)), DMA((2,)), DMA((2, 2)), DMA((2, 2)), DMA((4,))],
        compiler_params=pltpu.CompilerParams(collective_id=0, has_side_effects=True, vmem_limit_bytes=62 * 1024 * 1024),
        cost_estimate=pl.CostEstimate(flops=90_000_000_000, bytes_accessed=180_000_000, transcendentals=0),
    )(*operands)


GROUPS = (3, 2, 1, HEAD, 0, STEM)
UNITS = tuple((g, c) for g in GROUPS for c in (2, 0, 1) if g != HEAD or c == 2)
BACK_COPIES = 18 * len(UNITS) + 40
NEEDS = {3: ('act1', 'dout1'), 2: ('vin1', 'dpre1'), 1: ('act0', 'dout0'), 0: ('vin0', 'dpre0'), STEM: ('pat', 'dres'),
         HEAD: ('hl', 'hr')}
BACK_ORDER = (
    ('c1_7', ((3, 'L'),)),
    ('t1_0', ((0, 0), (0, 1), (1, 0), (1, 1), (2, 0), (2, 1), (0, 2),)),
    ('t1_2', ((1, 2),)),
    ('t1_3', ((0, 3), (2, 2),)),
    ('t1_4', ((2, 'L'),)),
    ('t1_6', ((1, 3), (0, 4), (3, 0), (3, 1), (2, 3), (4, 0), (4, 1), (1, 4), (0, 5), (5, 0), (5, 1), (3, 2), (1, 5), (0, 6),)),
    ('t1_7', ((2, 4),)),
    ('d0', ((4, 2),)),
    ('c0_1', ((5, 2), (3, 3), (2, 5), (1, 6),)),
    ('c0_3', ((1, 'L'), (1, 7),)),
    ('c0_4', ((4, 3), (3, 4), (0, 7), (6, 0), (6, 1), (2, 6), (7, 0), (7, 1), (5, 3), (4, 4), (3, 5), (2, 7), (8, 0), (8, 1),
        (6, 2), (4, 5), (3, 6), (9, 0), (9, 1),)),
    ('c0_5', ((7, 2), (5, 4),)),
    ('c0_7', ((6, 3), (8, 2), (4, 6),)),
    ('t0_0', ((9, 2),)),
    ('t0_1', ((7, 3), (6, 4), (3, 7),)),
    ('t0_2', ((5, 5), (4, 7),)),
    ('t0_3', ((8, 3), (7, 4), (6, 5), (9, 3), (5, 6),)),
    ('t0_4', ((0, 'L'),)),
    ('t0_5', ((8, 4), (9, 4), (7, 5), (6, 6), (5, 7), (10, 0), (10, 1), (11, 0), (11, 1), (8, 5), (9, 5), (7, 6), (6, 7),
        (12, 0), (12, 1), (10, 2), (9, 6),)),
    ('t0_6', ((7, 7),)),
    ('t0_7', ((11, 2),)),
    ('fin', ((12, 2), (10, 3),)),
    ('end', ((8, 6), (9, 7), (11, 3), (10, 4), (8, 7), (4, 'L'), (12, 3), (10, 5), (11, 4), (13, 0), (13, 1), (12, 4),
        (11, 5), (10, 6), (14, 0), (14, 1), (15, 0), (15, 1), (10, 7), (13, 2), (14, 2), (15, 2), (12, 5), (11, 6), (14, 3),
        (15, 3), (12, 6), (13, 3), (11, 7), (14, 4), (12, 7), (15, 4), (13, 4), (14, 5), (15, 5), (13, 5), (14, 6), (15, 6),
        (13, 6), (14, 7), (15, 7), (13, 7),)),
)
SMALL = dict(sm=((4, 4, 4, 8, 128), (3, 4, 4, 8, 128), (3, 4, 8, 128), (3, 8, 128)),
             tk=((4, 4, 4, 16, 128), (3, 4, 4, 16, 128), (3, 4, 16, 128), (3, 4, 16, 128)))


def reduce_scratch():
    per = []
    for c in range(3):
        n = COLS[c][1]
        many = sum(1 for u in UNITS if u[1] == c)
        lead = ((4, 4), (4,), ())
        b = {'C': pltpu.VMEM((2, 4, 4, 4, 32, n), bf16), 'S1': pltpu.VMEM((4, 4, 32, n), f32), 'S2': pltpu.VMEM((2, 4, 32, n), f32)}
        for ph in range(3):
            if ph:
                b[f'opp{ph}'] = pltpu.VMEM(lead[ph] + (32, n), bf16)
                b[f'pr{ph}'] = pltpu.VMEM(lead[ph] + (16, n), bf16)
                b[f'pl{ph}'] = pltpu.VMEM(lead[ph] + (16, n), bf16)
            for name in ('rig', 'lef'):
                b[f'{name}{ph}'] = pltpu.VMEM(lead[ph] + (16, n), bf16)
            for name in ('half0', 'half1'):
                b[f'{name}{ph}'] = pltpu.VMEM((many,) + lead[ph] + (16, n), bf16)
            for name in ('froml', 'fromr'):
                b[f'{name}{ph}'] = pltpu.VMEM((many,) + lead[ph] + (32, n), bf16)
        per.append(b)
    return per


def small_scratch():
    b = {f'{kind}{n + 1}': pltpu.VMEM(shape, f32) for kind, shapes in SMALL.items() for n, shape in enumerate(shapes)}
    b.update(sm=pltpu.VMEM((4, 4, 4, 2, 8, 128), f32), tk=pltpu.VMEM((4, 4, 4, 2, 16, 128), f32),
             sm_s1=pltpu.VMEM((4, 4, 8, 128), f32), sm_s2=pltpu.VMEM((4, 8, 128), f32),
             tk_s1=pltpu.VMEM((4, 4, 16, 128), f32), tk_s2=pltpu.VMEM((4, 16, 128), f32))
    return b


def small_pack(b, flat, turn, gvec, hstat, gbch1, gbh):
    for n in range(8):
        cols = pl.ds(128 * n, 128)
        turn[n, pl.ds(0, 128), :] = jnp.zeros((128, 128), f32)
        turn[n, pl.ds(0, 16), :] = gvec[:, cols]
        turn[n, pl.ds(11, 2), :] = hstat[pl.ds(0, 2), cols]
    for n in range(8):
        tile = turn[n, pl.ds(0, 128), :].T
        for i in range(4):
            a = n % 4 * 4 + i
            flat[a // 2, pl.ds(a % 2 * 64 + n // 4 * 32, 32), :] = tile[32 * i:32 * i + 32]
    for l in range(2):
        def gather(n, total):
            lane = lax.broadcasted_iota(jnp.int32, (128, 512), 0)
            col = lax.broadcasted_iota(jnp.int32, (128, 512), 1)
            sums = gbch1[l:l + 1, pl.ds(pl.multiple_of(512 * n, 512), 512)]
            mine = jnp.where(lane == n // 2 * 32 + col // 32 * 2 + n % 2, sums, 0.0)
            pick = jnp.where(lane == 32 + col % 32, 1.0, 0.0).astype(bf16)
            return total + dot_nt(jnp.concatenate(three_parts(mine), axis=0), pick)
        total = lax.fori_loop(0, 8, gather, jnp.zeros((384, 128), f32))
        total = total[0:128] + total[128:256] + total[256:384]
        for n in range(8):
            flat[n, pl.ds(l, 16, stride=8), :] += total[16 * n:16 * n + 16]
    lane = lax.broadcasted_iota(jnp.int32, (1, 128), 1)
    for t in range(4):
        for q in range(4):
            tile = gbh[0:1, t * 256 + q // 2 * 128:t * 256 + q // 2 * 128 + 128]
            if q % 2 == 0:
                tile = jnp.concatenate([tile[:, 64:], tile[:, :64]], axis=1)
            tile = jnp.where(lane >= 64, tile, 0.0)
            for n in (2 * t, 2 * t + 1):
                flat[n, pl.ds(2 + q, 16, stride=8), :] += tile
    for n in range(8):
        flat[n, pl.ds(6, 16, stride=8), :] += jnp.where(lane == 64, hstat[2:3, 0:128], 0.0)
        b['sm'][n // 2, pl.ds(n % 2 * 2, 2)] = flat[n, pl.ds(0, 128), :].reshape(2, 4, 2, 8, 128)


def back_kernel(*refs):
    xin, xmid, pre_in, wc, act, vin, pat = refs[:7]
    hl, hr, dx0, hstat, gbh, wt, wt_t, vec = refs[7:15]
    out_c, out_s, out_h, sm_own, tk_own = refs[15:20]
    dpre, dout, dres, x_act, x_vin, x_pat, x_dpre, x_dout, x_dres = refs[20:29]
    (per, b, big, little, x_hl, x_hr, gvec, gbch1, x_v, d_v, dv_v, do_v, w1_v, w2_v, pre_v, dp_v,
     send_sems, recv_sems, load_sems, sem, sem_w, sem_o) = refs[29:]
    me = my_place()
    other = moved(me, 'k', 1)
    k, k2 = me['k'], 1 - me['k']
    barrier = pltpu.get_barrier_semaphore()
    for dim in 'xyz':
        for step in (1, 2, 3):
            pl.semaphore_signal(barrier, inc=1, device_id=device(moved(me, dim, step)), device_id_type=MESH)
    pl.semaphore_signal(barrier, inc=1, device_id=device(other), device_id_type=MESH)
    net = Net(send_sems, recv_sems)
    ring = {d: [moved(me, d, n)[d] for n in range(4)] for d in 'xyz'}
    peers = {(d, n): device(moved(me, d, n)) for d in 'xyz' for n in (1, 2, 3)}
    partner = device(other)
    half_at = pl.ds(pl.multiple_of(k * 512, 512), 512)
    half_to = pl.ds(pl.multiple_of(k2 * 512, 512), 512)
    swaps = {'act1': (act.at[1, k2], x_act.at[1]), 'act0': (act.at[0, k2], x_act.at[0]), 'vin1': (vin.at[1, k2], x_vin.at[1]),
             'vin0': (vin.at[0, k2], x_vin.at[0]), 'pat': (pat.at[k2], x_pat), 'dpre1': (dpre.at[1], x_dpre.at[1]), 'dpre0': (dpre.at[0], x_dpre.at[0]),
             'dout1': (do_v, x_dout.at[1]), 'dout0': (do_v, x_dout.at[0]), 'dres': (do_v, x_dres),
             'hl': (hl.at[:, half_to], x_hl), 'hr': (hr, x_hr)}

    def swap(*names):
        for name in names:
            net.start(name, lambda name=name: (*swaps[name], partner))
    busy = {}

    def free(key):
        for name in busy.pop(key, ()):
            net.copy(name).wait_send()
            net.done.add(name)

    def loads(g):
        l = g // 2
        if g == STEM:
            wide, tall = (pat.at[k], x_pat, 1536), (dres, x_dres, CH)
        elif g % 2:
            wide, tall = (act.at[l, k], x_act.at[l], 2048), (dout.at[l], x_dout.at[l], CH)
        else:
            wide, tall = (dpre.at[l], x_dpre.at[l], CHH), (vin.at[l, k], x_vin.at[l], 512)
        out = []
        for n, (buf, (own, far, cols)) in enumerate(((big, wide), (little, tall))):
            out += [pltpu.make_async_copy(own, buf.at[0, :, pl.ds(0, cols)], load_sems.at[2 * n]),
                    pltpu.make_async_copy(far, buf.at[1, :, pl.ds(0, cols)], load_sems.at[2 * n + 1])]
        return out

    def product(u):
        g, c, slot = u.g, u.c, u.slot
        first = c == 2
        if first and g != HEAD:
            for copy in loads(g):
                copy.wait()
        if g == STEM and not first:
            return
        for v in (units if g == STEM else (u,)):
            if v.g == g:
                free(('C', v.c, v.slot))
        if g == HEAD:
            net.arrived(*NEEDS[g])
            for t in range(4):
                cols = pl.ds(256 * t, 256)
                prod = dot_tn(hl[:, half_at], hr[:, cols]) + dot_tn(x_hl[...], x_hr[:, cols])
                per[c]['C'][slot, t] = prod.astype(bf16).reshape(4, 4, 32, 256)
        elif g == STEM:
            slots = {v.c: v.slot for v in units if v.g == STEM}

            @pl.loop(0, 4)
            def _(z):
                rows = pl.ds(pl.multiple_of(z * 384, 384), 384)
                for t in range(4):
                    def right(s):
                        return jnp.concatenate([little[s, :, 128 * t:128 * t + 128], little[s, :, 512 + 128 * t:640 + 128 * t]], axis=1)
                    prod = dot_tn(big[0, :, rows], right(0)) + dot_tn(big[1, :, rows], right(1))
                    prod = prod.astype(bf16).reshape(4, 3, 32, 256)
                    for d in range(3):
                        per[d]['C'][slots[d], t, z, :, :, pl.ds(0, 256)] = prod[:, d]
        else:
            c0, n = COLS[c]

            @pl.loop(0, 4)
            def _(t):
                for h in range(2):
                    if g % 2:
                        left = pl.ds(pl.multiple_of(t * 512 + h * 256, 256), 256)
                        prod = dot_tn(big[0, :, left], little[0, :, c0:c0 + n]) + dot_tn(big[1, :, left], little[1, :, c0:c0 + n])
                    else:
                        right = pl.ds(pl.multiple_of(t * 1024 + c0, 128), n)
                        rows = slice(256 * h, 256 * h + 256)
                        prod = dot_tn(little[0, :, rows], big[0, :, right]) + dot_tn(little[1, :, rows], big[1, :, right])
                    per[c]['C'][slot, t, 2 * h:2 * h + 2] = prod.astype(bf16).reshape(2, 4, 32, n)

    class Unit:
        def __init__(self, g, c):
            self.g, self.c = g, c
            self.index = [u for u in UNITS if u[1] == c].index((g, c))
            self.slot = self.index % 2
            self.n = COLS[c][1] if g < N_CH else 256
            self.cols = pl.ds(0, self.n)
            self.buf = per[c]
            self.dims = ORDERS[c]
            self.rest = [d for d in 'xzy' if d != self.dims[0]]

        def cut(self, name, *at, rows=slice(None)):
            ref = self.buf[name]
            inner = [slice(None)] * (len(ref.shape) - len(at) - 2)
            return ref.at[(*at, *inner, rows, self.cols)]

        def block(self, p, rows):
            at = {d: EVERY for d in 'xzy'}
            at[self.dims[0]] = p
            return self.buf['C'].at[self.slot, at['x'], at['z'], at['y'], rows, self.cols]

        def share(self, phase, p, e, rows):
            if phase == 0:
                at = dict(zip(self.rest, e))
                at[self.dims[0]] = p
                return self.buf['C'][self.slot, at['x'], at['z'], at['y'], rows, self.cols].astype(f32)
            if phase == 1:
                at = (p, e[0]) if self.dims[1] == self.rest[0] else (e[0], p)
                return self.buf['S1'][(*at, rows, self.cols)]
            return self.buf['S2'][self.slot, p, rows, self.cols]

        def each(self, phase, body):
            if phase == 2:
                body(())
            elif phase == 1:
                pl.loop(0, 4)(lambda i: body((i,)))
            else:
                @pl.loop(0, 4)
                def _(i):
                    pl.loop(0, 4)(lambda j: body((i, j)))

        def send(self, tag, phase, src, dst, step):
            name = (self.g, self.c, tag, phase)
            net.start(name, lambda: (src(), dst(), peers[self.dims[phase], step]))
            return name

        def arrived(self, phase, *tags):
            net.arrived(*[(self.g, self.c, tag, phase) for tag in tags])

        def opposite(self, phase):
            places = ring[self.dims[phase]]
            low, high = pl.ds(0, 16), pl.ds(16, 16)
            if phase == 0:
                sources = [lambda: self.block(places[2], low), lambda: self.block(places[2], high),
                           lambda: self.block(places[1], high), lambda: self.block(places[3], low)]
            else:
                names = (f'opp{phase}', f'pr{phase}', f'pl{phase}')
                for name in names:
                    free((name, self.c))
                opp, right, left = (self.buf[name] for name in names)

                def body(e):
                    opp[(*e, slice(None), self.cols)] = self.share(phase, places[2], e, pl.ds(0, 32)).astype(bf16)
                    right[(*e, slice(None), self.cols)] = self.share(phase, places[1], e, high).astype(bf16)
                    left[(*e, slice(None), self.cols)] = self.share(phase, places[3], e, low).astype(bf16)
                self.each(phase, body)
                sources = [lambda: self.cut(names[0], rows=low), lambda: self.cut(names[0], rows=high),
                           lambda: self.cut(names[1]), lambda: self.cut(names[2])]
            targets = [lambda: self.cut(f'half0{phase}', self.index), lambda: self.cut(f'half1{phase}', self.index),
                       lambda: self.cut(f'froml{phase}', self.index, rows=high),
                       lambda: self.cut(f'fromr{phase}', self.index, rows=low)]
            sent = [self.send(tag, phase, src, dst, step)
                    for tag, src, dst, step in zip(('h0', 'h1', 'p0', 'p1'), sources, targets, (1, 3, 1, 3))]
            if phase == 0:
                busy['C', self.c, self.slot] = sent
            else:
                busy[names[0], self.c] = sent[:2]
                busy[names[1], self.c] = sent[2:3]
                busy[names[2], self.c] = sent[3:]

        def beside(self, phase):
            places = ring[self.dims[phase]]
            for half, step, name, dst in ((0, 1, 'rig', 'froml'), (1, 3, 'lef', 'fromr')):
                self.arrived(phase, f'h{half}')
                key = f'{name}{phase}'
                free((key, self.c))
                out, got = self.buf[key], self.buf[f'half{half}{phase}']
                rows = pl.ds(16 * half, 16)

                def body(e):
                    value = self.share(phase, places[step], e, rows) + got[(self.index, *e, slice(None), self.cols)].astype(f32)
                    out[(*e, slice(None), self.cols)] = value.astype(bf16)
                self.each(phase, body)
                busy[key, self.c] = [self.send(f'f{half}', phase, lambda key=key: self.cut(key),
                                               lambda dst=dst, rows=rows: self.cut(f'{dst}{phase}', self.index, rows=rows), step)]

        def total(self, phase):
            self.arrived(phase, 'p0', 'p1', 'f0', 'f1')
            p = ring[self.dims[phase]][0]

            def body(e):
                got = [self.buf[f'{name}{phase}'][(self.index, *e, slice(None), self.cols)].astype(f32)
                       for name in ('froml', 'fromr')]
                value = self.share(phase, p, e, pl.ds(0, 32)) + got[0] + got[1]
                if phase == 0:
                    self.buf['S1'][(*e, slice(None), self.cols)] = value
                elif phase == 1:
                    self.buf['S2'][(self.slot, *e, slice(None), self.cols)] = value
                elif self.g == STEM:
                    out_s[pl.ds(32 * self.c, 32), :] = value
                elif self.g == HEAD:
                    out_h[...] = value
                else:
                    out_c[self.g, :, pl.ds(*COLS[self.c])] = value
            self.each(phase, body)

        def run(self, stage):
            if stage == 0:
                product(self)
            elif stage == 7:
                self.total(2)
            elif stage % 2 == 0:
                self.beside(stage // 2 - 1)
            else:
                if stage > 1:
                    self.total(stage // 2 - 1)
                self.opposite(stage // 2)

    units = [Unit(g, c) for g, c in UNITS]
    bursts = dict(BACK_ORDER)

    def step(which, stage):
        if stage == 'L':
            net.arrived(*NEEDS[which])
            for copy in loads(which):
                copy.start()
        else:
            units[which].run(stage)

    def burst(name):
        for s in bursts.get(name, ()):
            step(*s)

    def during(name, count):
        def run(i):
            for n in range(1, count):
                if bursts.get(f'{name}{n}'):
                    pl.when(i == n)(functools.partial(burst, f'{name}{n}'))
        return run

    load = pltpu.make_async_copy(xmid.at[1], x_v.at[:, pl.ds(0, ROWS)], sem.at[0])
    load.start()
    mask = row_mask()
    rest = pl.ds(ROWS, XROWS - ROWS)
    put(d_v, rest, jnp.zeros((XROWS - ROWS, CH), f32))
    put(x_v, rest, jnp.zeros((XROWS - ROWS, CH), f32))
    gvec[...] = jnp.zeros_like(gvec)
    tk = b['tk']
    tk[...] = jnp.zeros_like(tk)

    @pl.loop(0, TOK)
    def _(s):
        put(d_v, pl.ds(pl.multiple_of(s * IMG, IMG), IMG), dx0[...])

    def add(row, value):
        gvec[row:row + 1, :] += jnp.sum(value, axis=0, keepdims=True)

    def add_token(n, value, start=0):
        tk[n, :, :, :, :, pl.ds(start, value.shape[1])] += value.reshape(4, 4, 2, 16, value.shape[1])

    for l in (1, 0):
        r = 1 + 5 * l
        free('do')
        for at, size in CHUNKS:
            d = get(d_v, pl.ds(at, size))
            add(r + 4, d)
            do_v[pl.ds(at, size), :] = d.astype(bf16)
        keep = pltpu.make_async_copy(do_v, dout.at[l], sem.at[1])
        keep.start()
        if l == 1:
            pl.semaphore_wait(barrier, 10)
            swap('dout1', 'act1', 'hl', 'hr', 'vin1', 'act0', 'vin0', 'pat')
        else:
            swap('dout0')
        busy['do'] = [f'dout{l}']
        keep.wait()
        burst(f'c{l}_0')
        run = during(f'c{l}_', NBLK)

        def blocks(i, slot):
            t, h = i // 2, i % 2
            part = pl.ds(pl.multiple_of(h * BLK, BLK), BLK)
            whole = pl.ds(pl.multiple_of(i * BLK, BLK), BLK)
            return [(wc.at[2 * l, t, :, :, :, :, part], w1_v.at[slot]), (wc.at[2 * l + 1, t, h], w2_v.at[slot]),
                    (pre_in.at[l, :, whole], pre_v.at[slot])]

        def outs(i, slot):
            return [(dp_v.at[slot], dpre.at[l, :, pl.ds(pl.multiple_of(i * BLK, BLK), BLK)])]

        def channel(i, slot):
            run(i)

            for n in range(2):
                cols = slice(256 * n, 256 * n + 256)
                d = dot_nt(do_v[...], w2_v[slot, 2 * n:2 * n + 2].reshape(256, CH)) * pre_v[slot, :, cols]
                gbch1[l:l + 1, pl.ds(pl.multiple_of(i * BLK + 256 * n, 256), 256)] = jnp.sum(d, axis=0, keepdims=True)
                dp_v[slot, :, cols] = d.astype(bf16)

            @pl.when(i == 0)
            def _():
                dv_v[...] = jnp.zeros_like(dv_v)
            for n in range(2):
                cols = slice(512 * n, 512 * n + 512)
                dv_v[:, cols] += dot_nt(dp_v[slot], w1_v[slot, n].reshape(512, BLK))
        for_blocks(Stream(sem_w, blocks, NBLK), channel, Stream(sem_o, outs, NBLK))
        swap(f'dpre{l}')
        burst(f'l{l}')
        load.wait()

        @pl.loop(0, ROWS // TPAD)
        def _(n):
            rows = pl.ds(pl.multiple_of(n * TPAD, TPAD), TPAD)
            std, inv = standardize(get(x_v, rows))
            d = dv_v[rows, :]
            add(r + 2, d * std)
            add(r + 3, d)
            put(d_v, rows, get(d_v, rows) + norm_grad(d, vec[r + 2:r + 3, :], std, inv))
        load = pltpu.make_async_copy(xin.at[l], x_v.at[:, pl.ds(0, ROWS)], sem.at[0])
        load.start()
        burst(f't{l}_0')
        load.wait()
        run = during(f't{l}_', IMG)

        @pl.loop(0, IMG)
        def _(m):
            run(m)
            std, inv = standardize(get(x_v, image(m)))
            a = with_bias_rows(std * vec[r:r + 1, :] + vec[r + 1:r + 2, :])
            d_mid = get(d_v, image(m))
            dm = d_mid.astype(bf16)
            parts = []
            for n in range(TOK_CUTS):
                cols = slice(CH // TOK_CUTS * n, CH // TOK_CUTS * (n + 1))
                value, slope = gelu_both(dot_nn(wt[l, :, 0:TPAD], a[:, cols]))
                add_token(2 + l, dot_nt(value.astype(bf16), dm[:, cols]))
                dh = dot_nn(wt[2 + l, :, 0:TPAD], dm[:, cols]) * slope
                add_token(l, jnp.sum(dh, axis=-1, keepdims=True), 64)
                dh = dh.astype(bf16)
                add_token(l, dot_nt(dh, a[:, cols]))
                parts.append(dot_nn(wt_t[l], dh))
            d = jnp.where(mask, jnp.concatenate(parts, axis=1), 0.0)
            add(r, d * std)
            add(r + 1, d)
            put(d_v, image(m), d_mid + norm_grad(d, vec[r:r + 1, :], std, inv))
        if l == 1:
            load = pltpu.make_async_copy(xmid.at[0], x_v.at[:, pl.ds(0, ROWS)], sem.at[0])
            load.start()
            burst('d0')

    burst('fin')
    free('do')
    for at, size in CHUNKS:
        d = get(d_v, pl.ds(at, size))
        add(0, d)
        do_v[pl.ds(at, size), :] = d.astype(bf16)
    keep = pltpu.make_async_copy(do_v, dres, sem.at[1])
    keep.start()
    swap('dres')
    keep.wait()
    small_pack(b, x_v, d_v, gvec, hstat, gbch1, gbh)

    last = []

    def put_small(name, src, dst, target):
        last.append(name)
        net.start(name, lambda: (src, dst, target))

    def small(n):
        x, z, y = (ring[d][0] for d in 'xzy')
        net.arrived(*last)
        last.clear()
        if n == 0:
            put_small(('sm', 0), b['sm'].at[:, :, :, k2], b['sm1'], partner)
            put_small(('tk', 0), b['tk'].at[:, :, :, k2], b['tk1'], partner)
        elif n == 1:
            b['sm1'][...] += b['sm'][:, :, :, k]
            b['tk1'][...] += b['tk'][:, :, :, k]
            for s in (1, 2, 3):
                put_small(('sm', 1, s), b['sm1'].at[ring['x'][s]], b['sm2'].at[s - 1], peers['x', s])
                put_small(('tk', 1, s), b['tk1'].at[:, ring['z'][s]], b['tk2'].at[s - 1], peers['z', s])
        elif n == 2:
            b['sm_s1'][...] = b['sm1'][x] + b['sm2'][0] + b['sm2'][1] + b['sm2'][2]
            b['tk_s1'][...] = b['tk1'][:, z] + b['tk2'][0] + b['tk2'][1] + b['tk2'][2]
            for s in (1, 2, 3):
                put_small(('sm', 2, s), b['sm_s1'].at[ring['z'][s]], b['sm3'].at[s - 1], peers['z', s])
                put_small(('tk', 2, s), b['tk_s1'].at[:, ring['y'][s]], b['tk3'].at[s - 1], peers['y', s])
        elif n == 3:
            b['sm_s2'][...] = b['sm_s1'][z] + b['sm3'][0] + b['sm3'][1] + b['sm3'][2]
            b['tk_s2'][...] = b['tk_s1'][:, y] + b['tk3'][0] + b['tk3'][1] + b['tk3'][2]
            for s in (1, 2, 3):
                put_small(('sm', 3, s), b['sm_s2'].at[ring['y'][s]], b['sm4'].at[s - 1], peers['y', s])
                put_small(('tk', 3, s), b['tk_s2'], b['tk4'].at[s - 1], peers['x', s])
        else:
            sm_own[...] = b['sm_s2'][y] + b['sm4'][0] + b['sm4'][1] + b['sm4'][2]
            ordered = []
            for place in range(4):
                value = b['tk_s2'][...]
                for s in (1, 2, 3):
                    value = jnp.where(ring['x'][4 - s] == place, b['tk4'][s - 1], value)
                ordered.append(value)
            tk_own[...] = (ordered[0] + ordered[1]) + (ordered[2] + ordered[3])

    tail = bursts.get('end', ())
    small(0)
    for n, s in enumerate(tail):
        step(*s)
        if n in (8, 18, 28, 38):
            small(1 + (8, 18, 28, 38).index(n))
    net.finish()
    assert len(net.builds) <= BACK_COPIES, len(net.builds)


def back(*operands):
    a, v = pl.BlockSpec(memory_space=pl.ANY), pl.BlockSpec(memory_space=pltpu.VMEM)
    S, V, DMA = jax.ShapeDtypeStruct, pltpu.VMEM, pltpu.SemaphoreType.DMA
    return pl.pallas_call(
        back_kernel, name='back',
        in_specs=[a] * 7 + [v] * 8, out_specs=[v] * 5 + [a] * 9,
        out_shape=[S((N_CH, 32, 1024), f32), S((96, 256), f32), S((32, 256), f32), S((8, 128), f32), S((4, 16, 128), f32),
                   S((2, ROWS, CHH), bf16), S((2, ROWS, CH), bf16), S((ROWS, CH), bf16), S((2, ROWS, 2048), bf16),
                   S((2, ROWS, 512), bf16), S((ROWS, 1536), bf16), S((2, ROWS, CHH), bf16), S((2, ROWS, CH), bf16),
                   S((ROWS, CH), bf16)],
        scratch_shapes=[reduce_scratch(), small_scratch(), V((2, ROWS, CHH), bf16), V((2, ROWS, CH), bf16), V((IMG, 512), bf16),
                        V((IMG, CH), bf16), V((16, CH), f32), V((2, CHH), f32), V((CH // 128, XROWS, 128), f32),
                        V((CH // 128, XROWS, 128), f32), V((ROWS, CH), f32), V((ROWS, CH), bf16), V((2, 2, 4, 4, 32, BLK), bf16),
                        V((2, 4, 4, 32, CH), bf16), V((2, ROWS, BLK), f32), V((2, ROWS, BLK), bf16), DMA((BACK_COPIES,)), DMA((BACK_COPIES,)), DMA((4,)), DMA((2,)), DMA((2, 3)),
                        DMA((2, 1))],
        compiler_params=pltpu.CompilerParams(collective_id=1, has_side_effects=True, vmem_limit_bytes=64 * 1024 * 1024 - 65536),
        cost_estimate=pl.CostEstimate(flops=120_000_000_000, bytes_accessed=200_000_000, transcendentals=0),
    )(*operands)


def finish_kernel(c, stem, head, sm, tk, loss, o_stem, o_bstem, o_ln1g, o_ln1b, o_wt1, o_bt1, o_wt2, o_ln2g, o_ln2b, o_ch1,
                  o_bch1, o_ch2, o_bch2, o_lnfg, o_lnfb, o_head, o_bhead):
    def core_last(value, pick):
        got = dot_nt(jnp.concatenate(three_parts(value), axis=0), pick)
        n = value.shape[0]
        return got[0:n] + got[n:2 * n] + got[2 * n:3 * n]
    pick = core_first(1024, 1024, 32)
    for l in range(2):
        o_ch1[l] = core_last(c[2 * l], pick)
        o_ch2[l] = core_last(c[2 * l + 1], pick)
    o_stem[...] = core_last(stem[...], core_first(256, 256, 32))
    o_head[...] = head[:, 0:250]
    own = sm[...]
    turned = jnp.concatenate([own, jnp.zeros((120, 128), f32)], axis=0).T
    for ref, n in ((o_bstem, 0), (o_lnfg, 11), (o_lnfb, 12)):
        ref[...] = turned[n, 0:8]
    for n, ref in enumerate((o_ln1g, o_ln1b, o_ln2g, o_ln2b, o_bch2)):
        for l in range(2):
            ref[pl.ds(l, 1), :] = turned[1 + 5 * l + n:2 + 5 * l + n, 0:8]
    o_bch1[...] = own[0:2, 32:64]
    classes = jnp.concatenate([own[2 + q:3 + q, 64:128] for q in range(4)], axis=1)
    o_bhead[...] = classes[0, 0:250]
    loss[...] = own[6:7, 64:65] * (1.0 / 1024)
    for l in range(2):
        o_wt1[l] = tk[l, :, 0:TOK]
        o_wt2[l] = tk[2 + l, :, 0:TOK]
        tall = jnp.concatenate([tk[l], jnp.zeros((112, 128), f32)], axis=0).T
        o_bt1[pl.ds(l, 1), :] = tall[64:65, 0:16]


def finish(*operands):
    S = jax.ShapeDtypeStruct
    v = pl.BlockSpec(memory_space=pltpu.VMEM)
    return pl.pallas_call(
        finish_kernel, name='finish', in_specs=[v] * 5, out_specs=[v] * 18,
        out_shape=[S((1, 1), f32), S((96, 256), f32), S((8,), f32), S((2, 8), f32), S((2, 8), f32), S((2, 16, TOK), f32),
                   S((2, 16), f32), S((2, 16, TOK), f32), S((2, 8), f32), S((2, 8), f32), S((2, 32, 1024), f32), S((2, 32), f32),
                   S((2, 32, 1024), f32), S((2, 8), f32), S((8,), f32), S((8,), f32), S((32, 250), f32), S((250,), f32)],
    )(*operands)

CHANNEL_AXES = ('tp', 'fsdp')


def weight_specs():
    vec_spec = P(CHANNEL_AXES)
    layer_vec = P(None, CHANNEL_AXES)
    return (P('fsdp', 'tp'), vec_spec, layer_vec, layer_vec, P(None, None, 'fsdp'), P(None, 'fsdp'),
            P(None, 'fsdp', None), layer_vec, layer_vec, P(None, 'fsdp', 'tp'), layer_vec,
            P(None, CHANNEL_AXES, None), layer_vec, vec_spec, vec_spec, P('fsdp', 'tp'), P('tp'))


def solution(mesh):
    def step(patches, labels, w_stem, b_stem, ln1_g, ln1_b, w_tok1, b_tok1, w_tok2,
             ln2_g, ln2_b, w_ch1, b_ch1, w_ch2, b_ch2, lnf_g, lnf_b, w_head, b_head):
        wc, pat, xin, xmid, vin, pre, act, hl, hr, dx0, hstat, gbh, vec, wt, wt_t = front(
            labels, patches.transpose(1, 0, 2), w_stem, w_ch1, w_ch2, w_head, w_tok1.transpose(0, 2, 1), w_tok2, b_tok1, b_ch1,
            b_head, b_stem, ln1_g, ln1_b, ln2_g, ln2_b, b_ch2, lnf_g, lnf_b)
        sums = back(xin, xmid, pre, wc, act, vin, pat, hl, hr, dx0, hstat, gbh, wt, wt_t, vec)[:5]
        loss, g_s, g_bs, g_1g, g_1b, g_t1, g_bt, g_t2, g_2g, g_2b, g_c1, g_b1, g_c2, g_b2, g_fg, g_fb, g_h, g_bh = finish(*sums)
        return (loss.reshape(()), g_s, g_bs, g_1g, g_1b, g_t1.transpose(0, 2, 1), g_bt, g_t2, g_2g, g_2b, g_c1, g_b1, g_c2, g_b2,
                g_fg, g_fb, g_h, g_bh)

    specs = weight_specs()
    return jax.shard_map(step, mesh=mesh, in_specs=(P('fsdp', None, None), P('fsdp')) + specs,
                         out_specs=(P(),) + specs, check_vma=False)
```

```python
import functools

import jax
import jax.numpy as jnp
from jax import lax
from jax.experimental import pallas as pl
from jax.experimental.pallas import tpu as pltpu
from jax.sharding import PartitionSpec as P

MESH = pl.DeviceIdType.MESH
ORDERS = (('x', 'y', 'z'), ('y', 'z', 'x'), ('z', 'x', 'y'))
COLS = ((0, 384), (384, 384), (768, 256))
N_CH = 4
STEM, HEAD = 4, 5
bf16, f32 = jnp.bfloat16, jnp.float32


def my_place():
    f = lax.axis_index('fsdp')
    return {'x': lax.axis_index('tp'), 'z': f // 8, 'y': (f // 2) % 4, 'k': f % 2}


def moved(place, dim, step):
    new = dict(place)
    new[dim] = 1 - place['k'] if dim == 'k' else (place[dim] + step) % 4
    return new


def device(place):
    return {'tp': place['x'], 'fsdp': (place['z'] * 4 + place['y']) * 2 + place['k']}


EPS = 1e-6
TOK, TPAD = 49, 56
IMG = 8
ROWS, XROWS = IMG * TOK, IMG * TPAD
CH, TOKH, CHH = 1024, 512, 4096
BLK = 512
NBLK = CHH // BLK
GELU_C, GELU_A = 0.7978845608028654, 0.044715


def dot_nn(a, b):
    return lax.dot_general(a, b, (((1,), (0,)), ((), ())), preferred_element_type=f32)


def dot_nt(a, b):
    return lax.dot_general(a, b, (((1,), (1,)), ((), ())), preferred_element_type=f32)


def dot_tn(a, b):
    return lax.dot_general(a, b, (((0,), (0,)), ((), ())), preferred_element_type=f32)


def gelu_both(x):
    sq = x * x
    half = 0.5 * jnp.tanh(x * (GELU_C + (GELU_C * GELU_A) * sq))
    rise = 0.5 + half
    value = x * rise
    return value, rise + value * (0.5 - half) * (2.0 * GELU_C + (6.0 * GELU_C * GELU_A) * sq)


def standardize(x):
    mean = jnp.mean(x, axis=-1, keepdims=True)
    cent = x - mean
    inv = lax.rsqrt(jnp.mean(cent * cent, axis=-1, keepdims=True) + EPS)
    return cent * inv, inv


def norm_grad(d, gain, std, inv):
    gs = d * gain
    m0 = jnp.mean(gs, axis=-1, keepdims=True)
    m1 = jnp.mean(gs * std, axis=-1, keepdims=True)
    return inv * (gs - m0 - std * m1)


def row_mask(rows=TPAD):
    return lax.broadcasted_iota(jnp.int32, (rows, 1), 0) < TOK


def image(b):
    return pl.ds(b, TPAD, stride=IMG)


def get(ref, rows):
    return jnp.concatenate([ref[n, rows, :] for n in range(CH // 128)], axis=1)


def put(ref, rows, value):
    for n in range(CH // 128):
        ref[n, rows, :] = value[:, 128 * n:128 * (n + 1)]


class Stream:
    def __init__(self, sem, copies, count):
        self.sem, self.copies, self.count = sem, copies, count

    def make(self, i, slot):
        return [pltpu.make_async_copy(src, dst, self.sem.at[slot, n]) for n, (src, dst) in enumerate(self.copies(i, slot))]

    def start(self, i, slot):
        for copy in self.make(i, slot):
            copy.start()

    def wait(self, i, slot):
        for copy in self.make(i, slot):
            copy.wait()


def for_blocks(stream, body, out=None):
    n = stream.count
    stream.start(0, 0)

    @pl.loop(0, n)
    def _(i):
        slot = i % 2
        stream.wait(i, slot)

        @pl.when(i + 1 < n)
        def _():
            stream.start(i + 1, 1 - slot)
        if out is not None:
            @pl.when(i >= 2)
            def _():
                out.wait(i - 2, slot)
        body(i, slot)
        if out is not None:
            out.start(i, slot)
    if out is not None:
        out.wait(n - 2, n % 2)
        out.wait(n - 1, 1 - n % 2)


TOK_CUTS = 4
FRONT_COPIES = 270
EARLY = [('stem', c) for c in range(3)] + [('ch', c, p) for p in 'ab' for c in range(3)] + [('head', 2)]
PARTS = {'a': pl.ds(0, 2), 'b': pl.ds(2, 2)}
LATE = [('stem', c, None) for c in range(3)] + [('ch', c, g) for g in range(N_CH) for c in range(3)] + [('head', 2, None)]
UNIT_GROUP = {('stem', None): 0, ('ch', 0): 1, ('ch', 1): 2, ('ch', 2): 3, ('ch', 3): 4, ('head', None): 5}
EVERY = pl.ds(0, 4)
FRONT_ORDER = (
    ('prep', (('M0', ('sm',)), ('M0', ('tk',)), ('A0', ('stem', 0)), ('A0', ('stem', 1)), ('A0', ('stem', 2)),
        ('A0', ('ch', 0, 'a')), ('A0', ('ch', 0, 'b')), ('A0', ('ch', 1, 'a')), ('A0', ('ch', 1, 'b')),
        ('A0', ('ch', 2, 'a')), ('A0', ('ch', 2, 'b')), ('A0', ('head', 2)),)),
    ('unpack', (('M1', ('sm',)), ('M1', ('tk',)), ('A', ('stem', 0)), ('A', ('stem', 1)), ('A', ('stem', 2)),
        ('A', ('ch', 0, 'a')), ('A', ('ch', 1, 'a')), ('A', ('ch', 2, 'a')), ('A', ('ch', 0, 'b')), ('A', ('ch', 2, 'b')),
        ('A', ('head', 2)), ('A', ('ch', 1, 'b')), ('B', ('stem', 0)), ('M2', ('sm',)), ('B', ('stem', 1)),
        ('B', ('ch', 0, 'a')), ('B', ('ch', 1, 'a')), ('B', ('ch', 0, 'b')), ('B', ('ch', 1, 'b')), ('M2', ('tk',)),
        ('B', ('stem', 2)), ('B', ('head', 2)), ('C', ('stem', 0)), ('B', ('ch', 2, 'a')), ('B', ('ch', 2, 'b')),
        ('M3', ('sm',)), ('C', ('stem', 2)), ('C', ('stem', 1)), ('C', ('head', 2)),)),
    ('stem0', (('D', ('stem', 0, None)), ('C', ('ch', 0, 'a')), ('C', ('ch', 1, 'a')), ('C', ('ch', 2, 'a')),
        ('D', ('stem', 2, None)), ('D', ('stem', 1, None)), ('D', ('ch', 2, 0)), ('D', ('ch', 2, 1)), ('D', ('ch', 0, 0)),
        ('D', ('ch', 0, 1)), ('E', ('stem', 0, None)), ('E', ('stem', 2, None)), ('E', ('stem', 1, None)),
        ('D', ('ch', 1, 0)), ('D', ('ch', 1, 1)), ('F', ('stem', 1, None)), ('E', ('ch', 2, 0)), ('E', ('ch', 0, 0)),
        ('E', ('ch', 2, 1)), ('F', ('stem', 2, None)), ('C', ('ch', 0, 'b')), ('C', ('ch', 1, 'b')), ('C', ('ch', 2, 'b')),
        ('D', ('head', 2, None)), ('E', ('ch', 1, 0)), ('F', ('ch', 2, 0)), ('E', ('ch', 0, 1)), ('F', ('stem', 0, None)),
        ('F', ('ch', 2, 1)), ('D', ('ch', 0, 2)), ('D', ('ch', 0, 3)),)),
    ('stem1', (('E', ('ch', 1, 1)),)),
    ('stem2', (('F', ('ch', 0, 0)), ('D', ('ch', 2, 2)), ('D', ('ch', 2, 3)),)),
    ('tok0_0', (('D', ('ch', 1, 2)), ('D', ('ch', 1, 3)), ('E', ('head', 2, None)),)),
    ('tok0_1', (('F', ('ch', 1, 0)),)),
    ('tok0_3', (('F', ('ch', 0, 1)),)),
    ('tok0_5', (('F', ('ch', 1, 1)), ('E', ('ch', 2, 2)),)),
    ('ch0_1', (('E', ('ch', 0, 2)), ('E', ('ch', 2, 3)),)),
    ('ch0_2', (('E', ('ch', 1, 2)), ('F', ('head', 2, None)),)),
    ('ch0_4', (('F', ('ch', 2, 2)),)),
    ('ch0_5', (('E', ('ch', 0, 3)), ('F', ('ch', 2, 3)),)),
    ('ch0_7', (('E', ('ch', 1, 3)),)),
    ('tok1_0', (('F', ('ch', 0, 2)),)),
    ('tok1_1', (('F', ('ch', 1, 2)),)),
    ('tok1_3', (('F', ('ch', 0, 3)),)),
    ('tok1_5', (('F', ('ch', 1, 3)),)),
)


class Net:
    def __init__(self, send_sems, recv_sems):
        self.send_sems, self.recv_sems, self.names, self.builds, self.done = send_sems, recv_sems, {}, [], set()

    def copy(self, name):
        n = self.names[name]
        src, dst, target = self.builds[n]()
        return pltpu.make_async_remote_copy(src_ref=src, dst_ref=dst, send_sem=self.send_sems.at[n],
                                            recv_sem=self.recv_sems.at[n], device_id=target, device_id_type=MESH)

    def start(self, name, build):
        self.names[name] = len(self.builds)
        self.builds.append(build)
        self.copy(name).start()

    def arrived(self, *names):
        for name in names:
            self.copy(name).wait_recv()

    def finish(self):
        for name in self.names:
            if name not in self.done:
                self.copy(name).wait_send()


def core_first(size, cols, each):
    half = cols // 2
    row = lax.broadcasted_iota(jnp.int32, (size, size), 0)
    col = lax.broadcasted_iota(jnp.int32, (1, size), 1)
    source = col % half // each * (2 * each) + col // half * each + col % each
    return jnp.where(row == source, 1.0, 0.0).astype(bf16)


def three_parts(x):
    hi = x.astype(bf16)
    rest = x - hi.astype(f32)
    mid = rest.astype(bf16)
    return hi, mid, (rest - mid.astype(f32)).astype(bf16)


def with_bias_rows(a):
    row = lax.broadcasted_iota(jnp.int32, (TPAD, 1), 0)
    return jnp.where(row < TOK, a, jnp.where(row < TOK + 3, 1.0, 0.0)).astype(bf16)


def front_kernel(labels, patches, w_stem, w_ch1, w_ch2, w_head, w_tok1, w_tok2, b_tok1, b_ch1, b_head, b_stem, ln1_g, ln1_b,
                 ln2_g, ln2_b, b_ch2, lnf_g, lnf_b,
                 wc, pat_out, xin, xmid, vout, pre_out, act_out, hl, hr, dx0, hstat, gbh, vec, wt, wt_t,
                 pc, ps, ph, tk_f, tk_p, sm_p, bh_p, ws, wh, tk_v, sm_v, sm_2, bh_v, bch1,
                 turn, p_v, pk_v, x_a, x_b, v_v, w1_v, w2_v, pre_v, act_v, g_v,
                 send_sems, recv_sems, sem, sem_w, sem_o, sem_x):
    me = my_place()
    other = moved(me, 'k', 1)
    load_p = pltpu.make_async_copy(patches.at[:, pl.ds(pl.multiple_of(me['x'] * IMG, IMG), IMG)], p_v, sem.at[0])
    load_p.start()

    barrier = pltpu.get_barrier_semaphore()
    for dim in 'xyz':
        for step in (1, 2, 3):
            pl.semaphore_signal(barrier, inc=1, device_id=device(moved(me, dim, step)), device_id_type=MESH)
    pl.semaphore_signal(barrier, inc=1, device_id=device(other), device_id_type=MESH)

    stem = dot_nn(w_stem[...].astype(bf16), core_first(256, 256, 32)).astype(bf16)
    ps[0], ps[1] = stem[:, 0:128], stem[:, 128:256]
    pick = core_first(1024, 1024, 32)
    for l in range(2):
        pc[2 * l] = dot_nn(w_ch1[l].astype(bf16), pick).astype(bf16)
        pc[2 * l + 1] = dot_nn(w_ch2[l].astype(bf16), pick).astype(bf16)
    ph[...] = jnp.zeros_like(ph)
    ph[:, pl.ds(0, 250)] = w_head[...].astype(bf16)
    turn[...] = jnp.zeros_like(turn)
    for n, ref in ((0, b_stem), (11, lnf_g), (12, lnf_b)):
        turn[n, pl.ds(0, 8)] = ref[...]
    for n, ref in enumerate((ln1_g, ln1_b, ln2_g, ln2_b, b_ch2)):
        for l in range(2):
            turn[pl.ds(1 + 5 * l + n, 1), pl.ds(0, 8)] = ref[pl.ds(l, 1), :]
    turn[pl.ds(16, 2), pl.ds(0, 16)] = b_tok1[...]
    turned = turn[...].T
    tk_f[...] = jnp.zeros_like(tk_f)
    for l in range(2):
        tk_f[l, :, pl.ds(0, TOK)] = w_tok1[l]
        tk_f[2 + l, :, pl.ds(0, TOK)] = w_tok2[l]
        for n, part in enumerate(three_parts(turned[0:16, 16 + l:17 + l])):
            tk_f[l, :, pl.ds(TOK + n, 1)] = part.astype(f32)
    tk_p[...] = tk_f[...].astype(bf16)
    sm_p[...] = jnp.zeros_like(sm_p)
    sm_p[:, pl.ds(0, 16)] = turned[0:8, 0:16]
    sm_p[pl.ds(0, 2), pl.ds(32, 32)] = b_ch1[...]
    bh_p[...] = jnp.full_like(bh_p, -1e30)
    bh_p[0, pl.ds(0, 250)] = b_head[...]

    net = Net(send_sems, recv_sems)
    core = me['k']
    ring = {d: [moved(me, d, n)[d] for n in range(4)] for d in 'xyz'}
    columns = [pl.ds(pl.multiple_of(x * 256, 256), 256) for x in ring['x']]
    stem_columns = [pl.ds(pl.multiple_of(x * 128, 128), 128) for x in ring['x']]
    peers = {(d, n): device(moved(me, d, n)) for d in 'xyz' for n in (1, 2, 3)}
    partner = device(other)
    here = {'x': 0, 'y': 0, 'z': 0}

    def view(unit, block, half=None):
        kind, colour = unit[:2]
        x, z, y = (EVERY if block[d] is None else ring[d][block[d]] for d in 'xzy')
        r0, rn = (0, 32) if half is None else (16 * half, 16)
        if kind == 'ch':
            c0, cn = COLS[colour]
            g = PARTS.get(unit[2], unit[2])
            return wc.at[g, x, core, z, y, pl.ds(r0, rn), pl.ds(c0, cn)]
        if kind == 'stem':
            cols = pl.ds(0, 512) if x is EVERY else stem_columns[block['x']]
            return ws.at[:, z, y, core, pl.ds(32 * colour + r0, rn), cols]
        cols = pl.ds(0, CH) if x is EVERY else columns[block['x']]
        return wh.at[core, z, y, pl.ds(r0, rn), cols]

    def piece(unit):
        kind, colour = unit[:2]
        if kind == 'ch':
            return pc.at[PARTS[unit[2]], :, pl.ds(*COLS[colour])]
        return ps.at[:, pl.ds(32 * colour, 32), :] if kind == 'stem' else ph.at[:, :]

    def exchange(unit, tag, dim, block):
        for side, step in (('l', 1), ('r', 3)):
            def build(step=step):
                part = view(unit, block)
                return (piece(unit) if tag == '1' else part), part, peers[dim, step]
            net.start((unit, tag, side), build)

    def forward_half(unit, tag, dim, block):
        for half, (origin, target, side) in enumerate(((3, 1, 'l'), (1, 3, 'r'))):
            def build(half=half, origin=origin, target=target):
                part = view(unit, {**block, dim: origin}, half)
                return part, part, peers[dim, target]
            net.start((unit, tag, side), build)

    def swap(unit, tag, block):
        def build():
            part = view(unit, block)
            return part, part, partner
        net.start((unit, tag), build)

    own = pltpu.make_async_copy(pc, wc.at[:, me['x'], me['k'], me['z'], me['y']], sem.at[1])
    own.start()
    mine = pl.ds(pl.multiple_of(me['x'] * 256, 256), 256)
    for n in range(2):
        ws[n, me['z'], me['y'], me['k'], :, stem_columns[0]] = ps[n]
    wh[me['k'], me['z'], me['y'], :, mine] = ph[...]
    sm_v[me['x'], me['z'], me['y'], me['k']] = sm_p[...]
    tk_v[:, me['z'], me['y'], me['k']] = tk_p[...]
    bh_v[:, mine] = bh_p[...]
    own.wait()
    pl.semaphore_wait(barrier, 10)

    def small(kind, n):
        dims = 'xyz' if kind == 'sm' else 'yz'
        at = {d: EVERY if d in dims[:n] else ring[d][0] for d in 'xyz'}

        def part():
            if kind == 'sm':
                return sm_v.at[at['x'], at['z'], at['y'], core]
            return tk_v.at[:, at['z'], at['y'], core]
        if n > 0:
            net.arrived(*[(kind, n - 1, s) for s in (1, 2, 3)])
        if n < len(dims):
            for s in (1, 2, 3):
                net.start((kind, n, s), lambda s=s: (part(), part(), peers[dims[n], s]))
            if kind == 'sm' and n == 0:
                def head_bias():
                    return bh_v.at[:, columns[0]]
                for s in (1, 2, 3):
                    net.start(('bh', s), lambda s=s: (head_bias(), head_bias(), peers['x', s]))
        else:
            net.start((kind, 'k'), lambda: (part(), part(), partner))

    def step(name, unit):
        if name[0] == 'M':
            small(unit[0], int(name[1]))
            return
        d1, d2, d3 = ORDERS[unit[1]]
        early = unit[:2] if unit[0] != 'ch' or unit[2] in PARTS else ('ch', unit[1], 'a' if unit[2] < 2 else 'b')
        plane = {**here, d1: None, d2: None}
        if name == 'A0':
            exchange(unit, '1', d1, here)
        elif name == 'A':
            net.arrived((unit, '1', 'l'), (unit, '1', 'r'))
            forward_half(unit, '1h', d1, here)
        elif name == 'B':
            net.arrived((unit, '1h', 'l'), (unit, '1h', 'r'))
            exchange(unit, '2', d2, {**here, d1: None})
        elif name == 'C':
            net.arrived((unit, '2', 'l'), (unit, '2', 'r'))
            forward_half(unit, '2h', d2, {**here, d1: None})
        elif name == 'D':
            if early not in planes:
                planes.add(early)
                net.arrived((early, '2h', 'l'), (early, '2h', 'r'))
            exchange(unit, '3', d3, plane)
            swap(unit, 'k0', plane)
        elif name == 'E':
            net.arrived((unit, '3', 'l'), (unit, '3', 'r'))
            forward_half(unit, '3h', d3, plane)
            for n in (1, 3):
                swap(unit, f'k{n}', {**plane, d3: n})
        else:
            net.arrived((unit, '3h', 'l'), (unit, '3h', 'r'))
            swap(unit, 'k2', {**plane, d3: 2})

    planes = set()
    awaited = set()

    def need(group):
        for u in LATE:
            if UNIT_GROUP[u[0], u[2]] <= group and u not in awaited:
                awaited.add(u)
                net.arrived(*[(u, f'k{n}') for n in range(4)])

    bursts = {name: steps for name, steps in FRONT_ORDER}

    def burst(name):
        for s in bursts.get(name, ()):
            step(*s)

    def during(name, count):
        def run(i):
            for n in range(1, count):
                if bursts.get(f'{name}{n}'):
                    pl.when(i == n)(functools.partial(burst, f'{name}{n}'))
        return run

    burst('prep')
    load_p.wait()
    pick = core_first(768, 768, 96)
    for g in range(4):
        part = dot_nn(p_v[:, :, pl.ds(768 * g, 768)].reshape(ROWS, 768), pick).astype(bf16)
        for n in range(2):
            pk_v[n, :, pl.ds(384 * g, 384)] = part[:, 384 * n:384 * n + 384]
    keep_p = pltpu.make_async_copy(pk_v, pat_out, sem.at[0])
    keep_p.start()

    burst('unpack')
    net.arrived(('sm', 'k'), ('tk', 'k'), ('bh', 1), ('bh', 2), ('bh', 3))
    sm_2[...] = sm_v[...].reshape(1024, 128)
    for n in range(8):
        tile = jnp.concatenate([sm_2[pl.ds((n % 4 * 4 + i) * 64 + n // 4 * 32, 32), :] for i in range(4)], axis=0)
        vec[:, pl.ds(128 * n, 128)] = tile.T[0:16, :]
    wt[...] = tk_v[...].reshape(4, TOKH, 128)
    for n in range(4):
        wt_t[n] = wt[n].astype(f32).T[0:TPAD].astype(bf16)
    for l in range(2):
        rows = jnp.concatenate(three_parts(sm_2[pl.ds(l, 128, stride=8), :]), axis=0)

        @pl.loop(0, 8)
        def _(n):
            lane = lax.broadcasted_iota(jnp.int32, (128, 512), 0)
            col = lax.broadcasted_iota(jnp.int32, (128, 512), 1)
            pick = jnp.where(lane == 32 + col % 32, 1.0, 0.0).astype(bf16)
            spread = dot_nn(rows, pick)
            value = spread[0:128] + spread[128:256] + spread[256:384]
            mine = lane == n // 2 * 32 + col // 32 * 2 + n % 2
            bch1[l:l + 1, pl.ds(pl.multiple_of(n * 512, 512), 512)] = jnp.sum(jnp.where(mine, value, 0.0), axis=0, keepdims=True)

    burst('stem0')
    need(0)
    run = during('stem', 4)
    put(x_a, pl.ds(ROWS, XROWS - ROWS), jnp.zeros((XROWS - ROWS, CH), f32))

    @pl.loop(0, 4)
    def _(i):
        run(i)
        cols = pl.ds(pl.multiple_of(i * 256, 256), 256)
        w = ws[i // 2, :, :, :, :, pl.ds(pl.multiple_of(i % 2 * 256, 256), 256)].reshape(3072, 256)
        value = dot_nn(p_v[...].reshape(ROWS, 3072), w) + vec[0:1, cols]
        for n in range(2):
            x_a[2 * i + n, pl.ds(0, ROWS), :] = value[:, 128 * n:128 * (n + 1)]

    wc_all = wc

    def add_rows(x_v, value):
        for n in range(CH // 128):
            x_v[n, pl.ds(0, ROWS), :] += value[:, 128 * n:128 * (n + 1)]

    for l in range(2):
        r = 1 + 5 * l
        x_old, x_v = ((x_a, x_b), (x_b, x_a))[l]
        burst(f'tok{l}_0')
        run = during(f'tok{l}_', IMG)
        save_in = pltpu.make_async_copy(x_old.at[:, pl.ds(0, ROWS)], xin.at[l], sem_x.at[3])
        save_in.start()

        @pl.loop(0, IMG)
        def _(b):
            run(b)
            x = get(x_old, image(b))
            std, _ = standardize(x)
            a = with_bias_rows(std * vec[r:r + 1, :] + vec[r + 1:r + 2, :])
            g_v[...] = gelu_both(dot_nn(wt[l, :, 0:TPAD], a))[0].astype(bf16)
            put(x_v, image(b), x + dot_nn(wt_t[2 + l], g_v[...]))
        save_mid = pltpu.make_async_copy(x_v.at[:, pl.ds(0, ROWS)], xmid.at[l], sem_x.at[0])
        save_mid.start()
        burst(f'ln{l}')

        @pl.loop(0, ROWS // TPAD)
        def _(n):
            rows = pl.ds(pl.multiple_of(n * TPAD, 8), TPAD)
            std, _ = standardize(get(x_v, rows))
            v_v[rows, :] = (std * vec[r + 2:r + 3, :] + vec[r + 3:r + 4, :]).astype(bf16)
        save_v = [pltpu.make_async_copy(v_v.at[:, pl.ds(512 * n, 512)], vout.at[l, n], sem_x.at[1 + n]) for n in range(2)]
        for copy in save_v:
            copy.start()
        burst(f'ch{l}_0')
        need(2 + 2 * l)
        save_mid.wait()

        def blocks(i, slot):
            t, h = i // 2, i % 2
            part = pl.ds(pl.multiple_of(h * BLK, BLK), BLK)
            return [(wc_all.at[2 * l, t, :, :, :, :, part], w1_v.at[slot]), (wc_all.at[2 * l + 1, t, h], w2_v.at[slot])]

        def outs(i, slot):
            part = pl.ds(pl.multiple_of(i * BLK, BLK), BLK)
            half = pl.ds(pl.multiple_of(i // 2 * BLK, BLK), BLK)
            return [(pre_v.at[slot], pre_out.at[l, :, part]), (act_v.at[slot], act_out.at[l, i % 2, :, half])]
        run = during(f'ch{l}_', NBLK)

        def channel(i, slot):
            run(i)
            part = pl.ds(pl.multiple_of(i * BLK, BLK), BLK)
            h = dot_nn(v_v[...], w1_v[slot].reshape(CH, BLK)) + bch1[l:l + 1, part]
            value, pre_v[slot] = gelu_both(h)
            act_v[slot] = value.astype(bf16)
            add_rows(x_v, dot_nn(act_v[slot], w2_v[slot].reshape(BLK, CH)))
        for_blocks(Stream(sem_w, blocks, NBLK), channel, Stream(sem_o, outs, NBLK))
        add_rows(x_v, jnp.broadcast_to(vec[r + 4:r + 5, :], (ROWS, CH)))
        for copy in (save_in, *save_v):
            copy.wait()

    burst('head')
    need(5)
    keep_p.wait()
    last = 11
    pooled = jnp.sum(get(x_a, pl.ds(0, ROWS)).reshape(TOK, IMG, CH), axis=0) * (1.0 / TOK)
    std, inv = standardize(pooled)
    head_in = (std * vec[last:last + 1, :] + vec[last + 1:last + 2, :]).astype(bf16)
    hl[...] = head_in
    w_h = wh[...].reshape(CH, CH)
    logits = dot_nn(head_in, w_h) + bh_v[0:1, :]
    row = lax.broadcasted_iota(jnp.int32, (IMG, 1), 0)
    label = jnp.zeros((IMG, 1), jnp.int32)
    for b in range(IMG):
        value = labels[me['x'] * IMG + b]
        label = jnp.where(row == b, value, label)
    label = label + 6 * sum(jnp.where(label >= edge, 1, 0) for edge in (250, 500, 750))
    is_label = lax.broadcasted_iota(jnp.int32, logits.shape, 1) == label
    top = jnp.max(logits, axis=-1, keepdims=True)
    ex = jnp.exp(logits - top)
    es = jnp.sum(ex, axis=-1, keepdims=True)
    nll = top + jnp.log(es) - jnp.sum(jnp.where(is_label, logits, 0.0), axis=-1, keepdims=True)
    d_logits = (ex / es - jnp.where(is_label, 1.0, 0.0)) * (1.0 / 1024)
    gbh[...] = jnp.sum(d_logits, axis=0, keepdims=True)
    d_bf = d_logits.astype(bf16)
    hr[...] = d_bf
    d_in = dot_nt(d_bf, w_h)
    hstat[0:1, :] = jnp.sum(d_in * std, axis=0, keepdims=True)
    hstat[1:2, :] = jnp.sum(d_in, axis=0, keepdims=True)
    hstat[2:3, :] = jnp.broadcast_to(jnp.sum(nll, axis=0, keepdims=True), (1, CH))
    dx0[...] = norm_grad(d_in, vec[last:last + 1, :], std, inv) * (1.0 / TOK)
    burst('end')
    net.finish()
    assert len(net.builds) <= FRONT_COPIES, len(net.builds)


def front(*operands):
    a, v = pl.BlockSpec(memory_space=pl.ANY), pl.BlockSpec(memory_space=pltpu.VMEM)
    S, V, DMA = jax.ShapeDtypeStruct, pltpu.VMEM, pltpu.SemaphoreType.DMA
    return pl.pallas_call(
        front_kernel, name='front',
        in_specs=[pl.BlockSpec(memory_space=pltpu.SMEM), a] + [v] * 17,
        out_specs=[a] * 7 + [v] * 8,
        out_shape=[S((N_CH, 4, 2, 4, 4, 32, 1024), bf16), S((2, ROWS, 1536), bf16), S((2, CH // 128, ROWS, 128), f32),
                   S((2, CH // 128, ROWS, 128), f32),
                   S((2, 2, ROWS, 512), bf16), S((2, ROWS, CHH), f32), S((2, 2, ROWS, 2048), bf16), S((IMG, CH), bf16),
                   S((IMG, CH), bf16), S((IMG, CH), f32), S((8, CH), f32), S((1, CH), f32), S((16, CH), f32),
                   S((4, TOKH, 128), bf16), S((4, TPAD, TOKH), bf16)],
        scratch_shapes=[V((N_CH, 32, 1024), bf16), V((2, 96, 128), bf16), V((32, 256), bf16), V((4, 16, 128), f32),
                        V((4, 16, 128), bf16), V((8, 128), f32), V((8, 256), f32), V((2, 4, 4, 2, 96, 512), bf16),
                        V((2, 4, 4, 32, CH), bf16), V((4, 4, 4, 2, 16, 128), bf16), V((4, 4, 4, 2, 8, 128), f32),
                        V((1024, 128), f32), V((8, CH), f32), V((2, CHH), f32),
                        V((128, 128), f32), V((TOK, IMG, 3072), bf16), V((2, ROWS, 1536), bf16), V((CH // 128, XROWS, 128), f32),
                        V((CH // 128, XROWS, 128), f32),
                        V((ROWS, CH), bf16), V((2, 2, 4, 4, 32, BLK), bf16), V((2, 4, 4, 32, CH), bf16),
                        V((2, ROWS, BLK), f32), V((2, ROWS, BLK), bf16), V((TOKH, CH), bf16),
                        DMA((FRONT_COPIES,)), DMA((FRONT_COPIES,)), DMA((2,)), DMA((2, 2)), DMA((2, 2)), DMA((4,))],
        compiler_params=pltpu.CompilerParams(collective_id=0, has_side_effects=True, vmem_limit_bytes=62 * 1024 * 1024),
        cost_estimate=pl.CostEstimate(flops=90_000_000_000, bytes_accessed=180_000_000, transcendentals=0),
    )(*operands)


GROUPS = (3, 2, 1, HEAD, 0, STEM)
UNITS = tuple((g, c) for g in GROUPS for c in (2, 0, 1) if g != HEAD or c == 2)
BACK_COPIES = 18 * len(UNITS) + 40
NEEDS = {3: ('act1', 'dout1'), 2: ('vin1', 'dpre1'), 1: ('act0', 'dout0'), 0: ('vin0', 'dpre0'), STEM: ('pat', 'dres'),
         HEAD: ('hl', 'hr')}
BACK_ORDER = (
    ('c1_7', ((3, 'L'),)),
    ('t1_0', ((0, 0), (0, 1), (1, 0), (1, 1), (2, 0), (2, 1), (0, 2),)),
    ('t1_2', ((1, 2),)),
    ('t1_3', ((0, 3), (2, 2),)),
    ('t1_4', ((2, 'L'),)),
    ('t1_6', ((1, 3), (0, 4), (3, 0), (3, 1), (2, 3), (4, 0), (4, 1), (1, 4), (0, 5), (5, 0), (5, 1), (3, 2), (1, 5), (0, 6),)),
    ('t1_7', ((2, 4),)),
    ('d0', ((4, 2),)),
    ('c0_1', ((5, 2), (3, 3), (2, 5), (1, 6),)),
    ('c0_3', ((1, 'L'), (1, 7),)),
    ('c0_4', ((4, 3), (3, 4), (0, 7), (6, 0), (6, 1), (2, 6), (7, 0), (7, 1), (5, 3), (4, 4), (3, 5), (2, 7), (8, 0), (8, 1),
        (6, 2), (4, 5), (3, 6), (9, 0), (9, 1),)),
    ('c0_5', ((7, 2), (5, 4),)),
    ('c0_7', ((6, 3), (8, 2), (4, 6),)),
    ('t0_0', ((9, 2),)),
    ('t0_1', ((7, 3), (6, 4), (3, 7),)),
    ('t0_2', ((5, 5), (4, 7),)),
    ('t0_3', ((8, 3), (7, 4), (6, 5), (9, 3), (5, 6),)),
    ('t0_4', ((0, 'L'),)),
    ('t0_5', ((8, 4), (9, 4), (7, 5), (6, 6), (5, 7), (10, 0), (10, 1), (11, 0), (11, 1), (8, 5), (9, 5), (7, 6), (6, 7),
        (12, 0), (12, 1), (10, 2), (9, 6),)),
    ('t0_6', ((7, 7),)),
    ('t0_7', ((11, 2),)),
    ('fin', ((12, 2), (10, 3),)),
    ('end', ((8, 6), (9, 7), (11, 3), (10, 4), (8, 7), (4, 'L'), (12, 3), (10, 5), (11, 4), (13, 0), (13, 1), (12, 4),
        (11, 5), (10, 6), (14, 0), (14, 1), (15, 0), (15, 1), (10, 7), (13, 2), (14, 2), (15, 2), (12, 5), (11, 6), (14, 3),
        (15, 3), (12, 6), (13, 3), (11, 7), (14, 4), (12, 7), (15, 4), (13, 4), (14, 5), (15, 5), (13, 5), (14, 6), (15, 6),
        (13, 6), (14, 7), (15, 7), (13, 7),)),
)
SMALL = dict(sm=((4, 4, 4, 8, 128), (3, 4, 4, 8, 128), (3, 4, 8, 128), (3, 8, 128)),
             tk=((4, 4, 4, 16, 128), (3, 4, 4, 16, 128), (3, 4, 16, 128), (3, 4, 16, 128)))


def reduce_scratch():
    per = []
    for c in range(3):
        n = COLS[c][1]
        many = sum(1 for u in UNITS if u[1] == c)
        lead = ((4, 4), (4,), ())
        b = {'C': pltpu.VMEM((2, 4, 4, 4, 32, n), bf16), 'S1': pltpu.VMEM((4, 4, 32, n), f32), 'S2': pltpu.VMEM((2, 4, 32, n), f32)}
        for ph in range(3):
            if ph:
                b[f'opp{ph}'] = pltpu.VMEM(lead[ph] + (32, n), bf16)
                b[f'pr{ph}'] = pltpu.VMEM(lead[ph] + (16, n), bf16)
                b[f'pl{ph}'] = pltpu.VMEM(lead[ph] + (16, n), bf16)
            for name in ('rig', 'lef'):
                b[f'{name}{ph}'] = pltpu.VMEM(lead[ph] + (16, n), bf16)
            for name in ('half0', 'half1'):
                b[f'{name}{ph}'] = pltpu.VMEM((many,) + lead[ph] + (16, n), bf16)
            for name in ('froml', 'fromr'):
                b[f'{name}{ph}'] = pltpu.VMEM((many,) + lead[ph] + (32, n), bf16)
        per.append(b)
    return per


def small_scratch():
    b = {f'{kind}{n + 1}': pltpu.VMEM(shape, f32) for kind, shapes in SMALL.items() for n, shape in enumerate(shapes)}
    b.update(sm=pltpu.VMEM((4, 4, 4, 2, 8, 128), f32), tk=pltpu.VMEM((4, 4, 4, 2, 16, 128), f32),
             sm_s1=pltpu.VMEM((4, 4, 8, 128), f32), sm_s2=pltpu.VMEM((4, 8, 128), f32),
             tk_s1=pltpu.VMEM((4, 4, 16, 128), f32), tk_s2=pltpu.VMEM((4, 16, 128), f32))
    return b


def small_pack(b, flat, turn, gvec, hstat, gbch1, gbh):
    for n in range(8):
        cols = pl.ds(128 * n, 128)
        turn[n, pl.ds(0, 128), :] = jnp.zeros((128, 128), f32)
        turn[n, pl.ds(0, 16), :] = gvec[:, cols]
        turn[n, pl.ds(11, 2), :] = hstat[pl.ds(0, 2), cols]
    for n in range(8):
        tile = turn[n, pl.ds(0, 128), :].T
        for i in range(4):
            a = n % 4 * 4 + i
            flat[a // 2, pl.ds(a % 2 * 64 + n // 4 * 32, 32), :] = tile[32 * i:32 * i + 32]
    for l in range(2):
        def gather(n, total):
            lane = lax.broadcasted_iota(jnp.int32, (128, 512), 0)
            col = lax.broadcasted_iota(jnp.int32, (128, 512), 1)
            sums = gbch1[l:l + 1, pl.ds(pl.multiple_of(512 * n, 512), 512)]
            mine = jnp.where(lane == n // 2 * 32 + col // 32 * 2 + n % 2, sums, 0.0)
            pick = jnp.where(lane == 32 + col % 32, 1.0, 0.0).astype(bf16)
            return total + dot_nt(jnp.concatenate(three_parts(mine), axis=0), pick)
        total = lax.fori_loop(0, 8, gather, jnp.zeros((384, 128), f32))
        total = total[0:128] + total[128:256] + total[256:384]
        for n in range(8):
            flat[n, pl.ds(l, 16, stride=8), :] += total[16 * n:16 * n + 16]
    lane = lax.broadcasted_iota(jnp.int32, (1, 128), 1)
    for t in range(4):
        for q in range(4):
            tile = gbh[0:1, t * 256 + q // 2 * 128:t * 256 + q // 2 * 128 + 128]
            if q % 2 == 0:
                tile = jnp.concatenate([tile[:, 64:], tile[:, :64]], axis=1)
            tile = jnp.where(lane >= 64, tile, 0.0)
            for n in (2 * t, 2 * t + 1):
                flat[n, pl.ds(2 + q, 16, stride=8), :] += tile
    for n in range(8):
        flat[n, pl.ds(6, 16, stride=8), :] += jnp.where(lane == 64, hstat[2:3, 0:128], 0.0)
        b['sm'][n // 2, pl.ds(n % 2 * 2, 2)] = flat[n, pl.ds(0, 128), :].reshape(2, 4, 2, 8, 128)


def back_kernel(*refs):
    xin, xmid, pre_in, wc, act, vin, pat = refs[:7]
    hl, hr, dx0, hstat, gbh, wt, wt_t, vec = refs[7:15]
    out_c, out_s, out_h, sm_own, tk_own = refs[15:20]
    dpre, dout, dres, x_act, x_vin, x_pat, x_dpre, x_dout, x_dres = refs[20:29]
    (per, b, big, little, x_hl, x_hr, gvec, gbch1, x_v, d_v, dv_v, do_v, w1_v, w2_v, pre_v, dp_v,
     send_sems, recv_sems, load_sems, sem, sem_w, sem_o) = refs[29:]
    me = my_place()
    other = moved(me, 'k', 1)
    k, k2 = me['k'], 1 - me['k']
    barrier = pltpu.get_barrier_semaphore()
    for dim in 'xyz':
        for step in (1, 2, 3):
            pl.semaphore_signal(barrier, inc=1, device_id=device(moved(me, dim, step)), device_id_type=MESH)
    pl.semaphore_signal(barrier, inc=1, device_id=device(other), device_id_type=MESH)
    net = Net(send_sems, recv_sems)
    ring = {d: [moved(me, d, n)[d] for n in range(4)] for d in 'xyz'}
    peers = {(d, n): device(moved(me, d, n)) for d in 'xyz' for n in (1, 2, 3)}
    partner = device(other)
    half_at = pl.ds(pl.multiple_of(k * 512, 512), 512)
    half_to = pl.ds(pl.multiple_of(k2 * 512, 512), 512)
    swaps = {'act1': (act.at[1, k2], x_act.at[1]), 'act0': (act.at[0, k2], x_act.at[0]), 'vin1': (vin.at[1, k2], x_vin.at[1]),
             'vin0': (vin.at[0, k2], x_vin.at[0]), 'pat': (pat.at[k2], x_pat), 'dpre1': (dpre.at[1], x_dpre.at[1]), 'dpre0': (dpre.at[0], x_dpre.at[0]),
             'dout1': (do_v, x_dout.at[1]), 'dout0': (do_v, x_dout.at[0]), 'dres': (do_v, x_dres),
             'hl': (hl.at[:, half_to], x_hl), 'hr': (hr, x_hr)}

    def swap(*names):
        for name in names:
            net.start(name, lambda name=name: (*swaps[name], partner))
    busy = {}

    def free(key):
        for name in busy.pop(key, ()):
            net.copy(name).wait_send()
            net.done.add(name)

    def loads(g):
        l = g // 2
        if g == STEM:
            wide, tall = (pat.at[k], x_pat, 1536), (dres, x_dres, CH)
        elif g % 2:
            wide, tall = (act.at[l, k], x_act.at[l], 2048), (dout.at[l], x_dout.at[l], CH)
        else:
            wide, tall = (dpre.at[l], x_dpre.at[l], CHH), (vin.at[l, k], x_vin.at[l], 512)
        out = []
        for n, (buf, (own, far, cols)) in enumerate(((big, wide), (little, tall))):
            out += [pltpu.make_async_copy(own, buf.at[0, :, pl.ds(0, cols)], load_sems.at[2 * n]),
                    pltpu.make_async_copy(far, buf.at[1, :, pl.ds(0, cols)], load_sems.at[2 * n + 1])]
        return out

    def shares(g, t, h, c0, n):
        if g % 2:
            rows, cols = pl.ds(pl.multiple_of(t * 512 + h * 256, 256), 256), slice(c0, c0 + n)
            prod = sum(dot_tn(big[s, :, rows], little[s, :, cols]) for s in range(2))
        else:
            rows, cols = slice(256 * h, 256 * h + 256), pl.ds(pl.multiple_of(t * 1024 + c0, 128), n)
            prod = sum(dot_tn(little[s, :, rows], big[s, :, cols]) for s in range(2))
        return prod.astype(bf16).reshape(2, 4, 32, n)

    def product(u):
        g, c, slot = u.g, u.c, u.slot
        first = c == 2
        if first and g != HEAD:
            for copy in loads(g):
                copy.wait()
        if g == STEM and not first or g < N_CH and c == 1:
            return
        slot1 = 0
        for v in units:
            if v.g == g and (v is u or g == STEM or c == 0):
                if v.c < 2 or v is u or g == STEM:
                    free(('C', v.c, v.slot))
                if v.c == 1:
                    slot1 = v.slot
        if g == HEAD:
            net.arrived(*NEEDS[g])
            for t in range(4):
                cols = pl.ds(256 * t, 256)
                prod = dot_tn(hl[:, half_at], hr[:, cols]) + dot_tn(x_hl[...], x_hr[:, cols])
                per[c]['C'][slot, t] = prod.astype(bf16).reshape(4, 4, 32, 256)
        elif g == STEM:
            slots = {v.c: v.slot for v in units if v.g == STEM}

            @pl.loop(0, 4)
            def _(z):
                rows = pl.ds(pl.multiple_of(z * 384, 384), 384)
                for t in range(4):
                    def right(s):
                        return jnp.concatenate([little[s, :, 128 * t:128 * t + 128], little[s, :, 512 + 128 * t:640 + 128 * t]], axis=1)
                    prod = dot_tn(big[0, :, rows], right(0)) + dot_tn(big[1, :, rows], right(1))
                    prod = prod.astype(bf16).reshape(4, 3, 32, 256)
                    for d in range(3):
                        per[d]['C'][slots[d], t, z, :, :, pl.ds(0, 256)] = prod[:, d]
        elif c == 2:
            c0, n = COLS[c]

            @pl.loop(0, 4)
            def _(t):
                for h in range(2):
                    per[c]['C'][slot, t, 2 * h:2 * h + 2] = shares(g, t, h, c0, n)
        elif c == 0:

            @pl.loop(0, 4)
            def _(t):
                for h in range(2):
                    at = slice(2 * h, 2 * h + 2)
                    prods = [shares(g, t, h, 256 * m, 256) for m in range(3)]
                    left, right = per[0]['C'], per[1]['C']
                    left[slot, t, at, :, :, pl.ds(0, 256)] = prods[0]
                    left[slot, t, at, :, :, pl.ds(256, 128)] = prods[1][..., 0:128]
                    right[slot1, t, at, :, :, pl.ds(0, 128)] = prods[1][..., 128:256]
                    right[slot1, t, at, :, :, pl.ds(128, 256)] = prods[2]

    class Unit:
        def __init__(self, g, c):
            self.g, self.c = g, c
            self.index = [u for u in UNITS if u[1] == c].index((g, c))
            self.slot = self.index % 2
            self.n = COLS[c][1] if g < N_CH else 256
            self.cols = pl.ds(0, self.n)
            self.buf = per[c]
            self.dims = ORDERS[c]
            self.rest = [d for d in 'xzy' if d != self.dims[0]]

        def cut(self, name, *at, rows=slice(None)):
            ref = self.buf[name]
            inner = [slice(None)] * (len(ref.shape) - len(at) - 2)
            return ref.at[(*at, *inner, rows, self.cols)]

        def block(self, p, rows):
            at = {d: EVERY for d in 'xzy'}
            at[self.dims[0]] = p
            return self.buf['C'].at[self.slot, at['x'], at['z'], at['y'], rows, self.cols]

        def share(self, phase, p, e, rows):
            if phase == 0:
                at = dict(zip(self.rest, e))
                at[self.dims[0]] = p
                return self.buf['C'][self.slot, at['x'], at['z'], at['y'], rows, self.cols].astype(f32)
            if phase == 1:
                at = (p, e[0]) if self.dims[1] == self.rest[0] else (e[0], p)
                return self.buf['S1'][(*at, rows, self.cols)]
            return self.buf['S2'][self.slot, p, rows, self.cols]

        def each(self, phase, body):
            if phase == 2:
                body(())
            elif phase == 1:
                pl.loop(0, 4)(lambda i: body((i,)))
            else:
                @pl.loop(0, 4)
                def _(i):
                    pl.loop(0, 4)(lambda j: body((i, j)))

        def send(self, tag, phase, src, dst, step):
            name = (self.g, self.c, tag, phase)
            net.start(name, lambda: (src(), dst(), peers[self.dims[phase], step]))
            return name

        def arrived(self, phase, *tags):
            net.arrived(*[(self.g, self.c, tag, phase) for tag in tags])

        def opposite(self, phase):
            places = ring[self.dims[phase]]
            low, high = pl.ds(0, 16), pl.ds(16, 16)
            if phase == 0:
                sources = [lambda: self.block(places[2], low), lambda: self.block(places[2], high),
                           lambda: self.block(places[1], high), lambda: self.block(places[3], low)]
            else:
                names = (f'opp{phase}', f'pr{phase}', f'pl{phase}')
                for name in names:
                    free((name, self.c))
                opp, right, left = (self.buf[name] for name in names)

                def body(e):
                    opp[(*e, slice(None), self.cols)] = self.share(phase, places[2], e, pl.ds(0, 32)).astype(bf16)
                    right[(*e, slice(None), self.cols)] = self.share(phase, places[1], e, high).astype(bf16)
                    left[(*e, slice(None), self.cols)] = self.share(phase, places[3], e, low).astype(bf16)
                self.each(phase, body)
                sources = [lambda: self.cut(names[0], rows=low), lambda: self.cut(names[0], rows=high),
                           lambda: self.cut(names[1]), lambda: self.cut(names[2])]
            targets = [lambda: self.cut(f'half0{phase}', self.index), lambda: self.cut(f'half1{phase}', self.index),
                       lambda: self.cut(f'froml{phase}', self.index, rows=high),
                       lambda: self.cut(f'fromr{phase}', self.index, rows=low)]
            sent = [self.send(tag, phase, src, dst, step)
                    for tag, src, dst, step in zip(('h0', 'h1', 'p0', 'p1'), sources, targets, (1, 3, 1, 3))]
            if phase == 0:
                busy['C', self.c, self.slot] = sent
            else:
                busy[names[0], self.c] = sent[:2]
                busy[names[1], self.c] = sent[2:3]
                busy[names[2], self.c] = sent[3:]

        def beside(self, phase):
            places = ring[self.dims[phase]]
            for half, step, name, dst in ((0, 1, 'rig', 'froml'), (1, 3, 'lef', 'fromr')):
                self.arrived(phase, f'h{half}')
                key = f'{name}{phase}'
                free((key, self.c))
                out, got = self.buf[key], self.buf[f'half{half}{phase}']
                rows = pl.ds(16 * half, 16)

                def body(e):
                    value = self.share(phase, places[step], e, rows) + got[(self.index, *e, slice(None), self.cols)].astype(f32)
                    out[(*e, slice(None), self.cols)] = value.astype(bf16)
                self.each(phase, body)
                busy[key, self.c] = [self.send(f'f{half}', phase, lambda key=key: self.cut(key),
                                               lambda dst=dst, rows=rows: self.cut(f'{dst}{phase}', self.index, rows=rows), step)]

        def total(self, phase):
            self.arrived(phase, 'p0', 'p1', 'f0', 'f1')
            p = ring[self.dims[phase]][0]

            def body(e):
                got = [self.buf[f'{name}{phase}'][(self.index, *e, slice(None), self.cols)].astype(f32)
                       for name in ('froml', 'fromr')]
                value = self.share(phase, p, e, pl.ds(0, 32)) + got[0] + got[1]
                if phase == 0:
                    self.buf['S1'][(*e, slice(None), self.cols)] = value
                elif phase == 1:
                    self.buf['S2'][(self.slot, *e, slice(None), self.cols)] = value
                elif self.g == STEM:
                    out_s[pl.ds(32 * self.c, 32), :] = value
                elif self.g == HEAD:
                    out_h[...] = value
                else:
                    out_c[self.g, :, pl.ds(*COLS[self.c])] = value
            self.each(phase, body)

        def run(self, stage):
            if stage == 0:
                product(self)
            elif stage == 7:
                self.total(2)
            elif stage % 2 == 0:
                self.beside(stage // 2 - 1)
            else:
                if stage > 1:
                    self.total(stage // 2 - 1)
                self.opposite(stage // 2)

    units = [Unit(g, c) for g, c in UNITS]
    bursts = dict(BACK_ORDER)

    def step(which, stage):
        if stage == 'L':
            net.arrived(*NEEDS[which])
            for copy in loads(which):
                copy.start()
        else:
            units[which].run(stage)

    def burst(name):
        for s in bursts.get(name, ()):
            step(*s)

    def during(name, count):
        def run(i):
            for n in range(1, count):
                if bursts.get(f'{name}{n}'):
                    pl.when(i == n)(functools.partial(burst, f'{name}{n}'))
        return run

    load = pltpu.make_async_copy(xmid.at[1], x_v.at[:, pl.ds(0, ROWS)], sem.at[0])
    load.start()
    mask = row_mask()
    rest = pl.ds(ROWS, XROWS - ROWS)
    put(d_v, rest, jnp.zeros((XROWS - ROWS, CH), f32))
    put(x_v, rest, jnp.zeros((XROWS - ROWS, CH), f32))
    gvec[...] = jnp.zeros_like(gvec)
    tk = b['tk']
    tk[...] = jnp.zeros_like(tk)

    @pl.loop(0, TOK)
    def _(s):
        put(d_v, pl.ds(pl.multiple_of(s * IMG, IMG), IMG), dx0[...])

    def add(row, value):
        gvec[row:row + 1, :] += jnp.sum(value, axis=0, keepdims=True)

    def cast_out(row):
        @pl.loop(0, ROWS // TPAD)
        def _(n):
            rows = pl.ds(pl.multiple_of(n * TPAD, 8), TPAD)
            d = get(d_v, rows)
            add(row, d)
            do_v[rows, :] = d.astype(bf16)

    def add_token(n, value, start=0):
        tk[n, :, :, :, :, pl.ds(start, value.shape[1])] += value.reshape(4, 4, 2, 16, value.shape[1])

    for l in (1, 0):
        r = 1 + 5 * l
        free('do')
        cast_out(r + 4)
        keep = pltpu.make_async_copy(do_v, dout.at[l], sem.at[1])
        keep.start()
        if l == 1:
            pl.semaphore_wait(barrier, 10)
            swap('dout1', 'act1', 'hl', 'hr', 'vin1', 'act0', 'vin0', 'pat')
        else:
            swap('dout0')
        busy['do'] = [f'dout{l}']
        keep.wait()
        burst(f'c{l}_0')
        run = during(f'c{l}_', NBLK)

        def blocks(i, slot):
            t, h = i // 2, i % 2
            part = pl.ds(pl.multiple_of(h * BLK, BLK), BLK)
            whole = pl.ds(pl.multiple_of(i * BLK, BLK), BLK)
            return [(wc.at[2 * l, t, :, :, :, :, part], w1_v.at[slot]), (wc.at[2 * l + 1, t, h], w2_v.at[slot]),
                    (pre_in.at[l, :, whole], pre_v.at[slot])]

        def outs(i, slot):
            return [(dp_v.at[slot], dpre.at[l, :, pl.ds(pl.multiple_of(i * BLK, BLK), BLK)])]

        def channel(i, slot):
            run(i)

            for n in range(2):
                cols = slice(256 * n, 256 * n + 256)
                d = dot_nt(do_v[...], w2_v[slot, 2 * n:2 * n + 2].reshape(256, CH)) * pre_v[slot, :, cols]
                gbch1[l:l + 1, pl.ds(pl.multiple_of(i * BLK + 256 * n, 256), 256)] = jnp.sum(d, axis=0, keepdims=True)
                dp_v[slot, :, cols] = d.astype(bf16)

            @pl.when(i == 0)
            def _():
                dv_v[...] = jnp.zeros_like(dv_v)
            for n in range(2):
                cols = slice(512 * n, 512 * n + 512)
                dv_v[:, cols] += dot_nt(dp_v[slot], w1_v[slot, n].reshape(512, BLK))
        for_blocks(Stream(sem_w, blocks, NBLK), channel, Stream(sem_o, outs, NBLK))
        swap(f'dpre{l}')
        burst(f'l{l}')
        load.wait()

        @pl.loop(0, ROWS // TPAD)
        def _(n):
            rows = pl.ds(pl.multiple_of(n * TPAD, TPAD), TPAD)
            std, inv = standardize(get(x_v, rows))
            d = dv_v[rows, :]
            add(r + 2, d * std)
            add(r + 3, d)
            put(d_v, rows, get(d_v, rows) + norm_grad(d, vec[r + 2:r + 3, :], std, inv))
        load = pltpu.make_async_copy(xin.at[l], x_v.at[:, pl.ds(0, ROWS)], sem.at[0])
        load.start()
        burst(f't{l}_0')
        load.wait()
        run = during(f't{l}_', IMG)

        @pl.loop(0, IMG)
        def _(m):
            run(m)
            std, inv = standardize(get(x_v, image(m)))
            a = with_bias_rows(std * vec[r:r + 1, :] + vec[r + 1:r + 2, :])
            d_mid = get(d_v, image(m))
            dm = d_mid.astype(bf16)
            parts = []
            for n in range(TOK_CUTS):
                cols = slice(CH // TOK_CUTS * n, CH // TOK_CUTS * (n + 1))
                value, slope = gelu_both(dot_nn(wt[l, :, 0:TPAD], a[:, cols]))
                add_token(2 + l, dot_nt(value.astype(bf16), dm[:, cols]))
                dh = dot_nn(wt[2 + l, :, 0:TPAD], dm[:, cols]) * slope
                add_token(l, jnp.sum(dh, axis=-1, keepdims=True), 64)
                dh = dh.astype(bf16)
                add_token(l, dot_nt(dh, a[:, cols]))
                parts.append(dot_nn(wt_t[l], dh))
            d = jnp.where(mask, jnp.concatenate(parts, axis=1), 0.0)
            add(r, d * std)
            add(r + 1, d)
            put(d_v, image(m), d_mid + norm_grad(d, vec[r:r + 1, :], std, inv))
        if l == 1:
            load = pltpu.make_async_copy(xmid.at[0], x_v.at[:, pl.ds(0, ROWS)], sem.at[0])
            load.start()
            burst('d0')

    burst('fin')
    free('do')
    cast_out(0)
    keep = pltpu.make_async_copy(do_v, dres, sem.at[1])
    keep.start()
    swap('dres')
    keep.wait()
    small_pack(b, x_v, d_v, gvec, hstat, gbch1, gbh)

    last = []

    def put_small(name, src, dst, target):
        last.append(name)
        net.start(name, lambda: (src, dst, target))

    def small(n):
        x, z, y = (ring[d][0] for d in 'xzy')
        net.arrived(*last)
        last.clear()
        if n == 0:
            put_small(('sm', 0), b['sm'].at[:, :, :, k2], b['sm1'], partner)
            put_small(('tk', 0), b['tk'].at[:, :, :, k2], b['tk1'], partner)
        elif n == 1:
            @pl.loop(0, 4)
            def _(i):
                b['sm1'][i] += b['sm'][i, :, :, k]
                b['tk1'][i] += b['tk'][i, :, :, k]
            for s in (1, 2, 3):
                put_small(('sm', 1, s), b['sm1'].at[ring['x'][s]], b['sm2'].at[s - 1], peers['x', s])
                put_small(('tk', 1, s), b['tk1'].at[:, ring['z'][s]], b['tk2'].at[s - 1], peers['z', s])
        elif n == 2:
            b['sm_s1'][...] = b['sm1'][x] + b['sm2'][0] + b['sm2'][1] + b['sm2'][2]

            @pl.loop(0, 4)
            def _(i):
                b['tk_s1'][i] = b['tk1'][i, z] + b['tk2'][0, i] + b['tk2'][1, i] + b['tk2'][2, i]
            for s in (1, 2, 3):
                put_small(('sm', 2, s), b['sm_s1'].at[ring['z'][s]], b['sm3'].at[s - 1], peers['z', s])
                put_small(('tk', 2, s), b['tk_s1'].at[:, ring['y'][s]], b['tk3'].at[s - 1], peers['y', s])
        elif n == 3:
            b['sm_s2'][...] = b['sm_s1'][z] + b['sm3'][0] + b['sm3'][1] + b['sm3'][2]
            b['tk_s2'][...] = b['tk_s1'][:, y] + b['tk3'][0] + b['tk3'][1] + b['tk3'][2]
            for s in (1, 2, 3):
                put_small(('sm', 3, s), b['sm_s2'].at[ring['y'][s]], b['sm4'].at[s - 1], peers['y', s])
                put_small(('tk', 3, s), b['tk_s2'], b['tk4'].at[s - 1], peers['x', s])
        else:
            sm_own[...] = b['sm_s2'][y] + b['sm4'][0] + b['sm4'][1] + b['sm4'][2]
            ordered = []
            for place in range(4):
                value = b['tk_s2'][...]
                for s in (1, 2, 3):
                    value = jnp.where(ring['x'][4 - s] == place, b['tk4'][s - 1], value)
                ordered.append(value)
            tk_own[...] = (ordered[0] + ordered[1]) + (ordered[2] + ordered[3])

    tail = bursts.get('end', ())
    small(0)
    for n, s in enumerate(tail):
        step(*s)
        if n in (8, 18, 28, 38):
            small(1 + (8, 18, 28, 38).index(n))
    net.finish()
    assert len(net.builds) <= BACK_COPIES, len(net.builds)


def back(*operands):
    a, v = pl.BlockSpec(memory_space=pl.ANY), pl.BlockSpec(memory_space=pltpu.VMEM)
    S, V, DMA = jax.ShapeDtypeStruct, pltpu.VMEM, pltpu.SemaphoreType.DMA
    return pl.pallas_call(
        back_kernel, name='back',
        in_specs=[a] * 7 + [v] * 8, out_specs=[v] * 5 + [a] * 9,
        out_shape=[S((N_CH, 32, 1024), f32), S((96, 256), f32), S((32, 256), f32), S((8, 128), f32), S((4, 16, 128), f32),
                   S((2, ROWS, CHH), bf16), S((2, ROWS, CH), bf16), S((ROWS, CH), bf16), S((2, ROWS, 2048), bf16),
                   S((2, ROWS, 512), bf16), S((ROWS, 1536), bf16), S((2, ROWS, CHH), bf16), S((2, ROWS, CH), bf16),
                   S((ROWS, CH), bf16)],
        scratch_shapes=[reduce_scratch(), small_scratch(), V((2, ROWS, CHH), bf16), V((2, ROWS, CH), bf16), V((IMG, 512), bf16),
                        V((IMG, CH), bf16), V((16, CH), f32), V((2, CHH), f32), V((CH // 128, XROWS, 128), f32),
                        V((CH // 128, XROWS, 128), f32), V((ROWS, CH), f32), V((ROWS, CH), bf16), V((2, 2, 4, 4, 32, BLK), bf16),
                        V((2, 4, 4, 32, CH), bf16), V((2, ROWS, BLK), f32), V((2, ROWS, BLK), bf16), DMA((BACK_COPIES,)), DMA((BACK_COPIES,)), DMA((4,)), DMA((2,)), DMA((2, 3)),
                        DMA((2, 1))],
        compiler_params=pltpu.CompilerParams(collective_id=1, has_side_effects=True, vmem_limit_bytes=64 * 1024 * 1024 - 65536),
        cost_estimate=pl.CostEstimate(flops=120_000_000_000, bytes_accessed=200_000_000, transcendentals=0),
    )(*operands)


def finish_kernel(c, stem, head, sm, tk, loss, o_stem, o_bstem, o_ln1g, o_ln1b, o_wt1, o_bt1, o_wt2, o_ln2g, o_ln2b, o_ch1,
                  o_bch1, o_ch2, o_bch2, o_lnfg, o_lnfb, o_head, o_bhead):
    def core_last(value):
        half = value.shape[1] // 2
        return jnp.concatenate([value[:, k * half + a:k * half + a + 32] for a in range(0, half, 32) for k in range(2)], axis=1)
    for l in range(2):
        o_ch1[l] = core_last(c[2 * l])
        o_ch2[l] = core_last(c[2 * l + 1])
    o_stem[...] = core_last(stem[...])
    o_head[...] = head[:, 0:250]
    own = sm[...]
    turned = jnp.concatenate([own, jnp.zeros((120, 128), f32)], axis=0).T
    for ref, n in ((o_bstem, 0), (o_lnfg, 11), (o_lnfb, 12)):
        ref[...] = turned[n, 0:8]
    for n, ref in enumerate((o_ln1g, o_ln1b, o_ln2g, o_ln2b, o_bch2)):
        for l in range(2):
            ref[pl.ds(l, 1), :] = turned[1 + 5 * l + n:2 + 5 * l + n, 0:8]
    o_bch1[...] = own[0:2, 32:64]
    classes = jnp.concatenate([own[2 + q:3 + q, 64:128] for q in range(4)], axis=1)
    o_bhead[...] = classes[0, 0:250]
    loss[...] = own[6:7, 64:65] * (1.0 / 1024)
    for l in range(2):
        o_wt1[l] = tk[l, :, 0:TOK]
        o_wt2[l] = tk[2 + l, :, 0:TOK]
        tall = jnp.concatenate([tk[l], jnp.zeros((112, 128), f32)], axis=0).T
        o_bt1[pl.ds(l, 1), :] = tall[64:65, 0:16]


def finish(*operands):
    S = jax.ShapeDtypeStruct
    v = pl.BlockSpec(memory_space=pltpu.VMEM)
    return pl.pallas_call(
        finish_kernel, name='finish', in_specs=[v] * 5, out_specs=[v] * 18,
        out_shape=[S((1, 1), f32), S((96, 256), f32), S((8,), f32), S((2, 8), f32), S((2, 8), f32), S((2, 16, TOK), f32),
                   S((2, 16), f32), S((2, 16, TOK), f32), S((2, 8), f32), S((2, 8), f32), S((2, 32, 1024), f32), S((2, 32), f32),
                   S((2, 32, 1024), f32), S((2, 8), f32), S((8,), f32), S((8,), f32), S((32, 250), f32), S((250,), f32)],
    )(*operands)

CHANNEL_AXES = ('tp', 'fsdp')


def weight_specs():
    vec_spec = P(CHANNEL_AXES)
    layer_vec = P(None, CHANNEL_AXES)
    return (P('fsdp', 'tp'), vec_spec, layer_vec, layer_vec, P(None, None, 'fsdp'), P(None, 'fsdp'),
            P(None, 'fsdp', None), layer_vec, layer_vec, P(None, 'fsdp', 'tp'), layer_vec,
            P(None, CHANNEL_AXES, None), layer_vec, vec_spec, vec_spec, P('fsdp', 'tp'), P('tp'))


def solution(mesh):
    def step(patches, labels, w_stem, b_stem, ln1_g, ln1_b, w_tok1, b_tok1, w_tok2,
             ln2_g, ln2_b, w_ch1, b_ch1, w_ch2, b_ch2, lnf_g, lnf_b, w_head, b_head):
        wc, pat, xin, xmid, vin, pre, act, hl, hr, dx0, hstat, gbh, vec, wt, wt_t = front(
            labels, patches.transpose(1, 0, 2), w_stem, w_ch1, w_ch2, w_head, w_tok1.transpose(0, 2, 1), w_tok2, b_tok1, b_ch1,
            b_head, b_stem, ln1_g, ln1_b, ln2_g, ln2_b, b_ch2, lnf_g, lnf_b)
        sums = back(xin, xmid, pre, wc, act, vin, pat, hl, hr, dx0, hstat, gbh, wt, wt_t, vec)[:5]
        loss, g_s, g_bs, g_1g, g_1b, g_t1, g_bt, g_t2, g_2g, g_2b, g_c1, g_b1, g_c2, g_b2, g_fg, g_fb, g_h, g_bh = finish(*sums)
        return (loss.reshape(()), g_s, g_bs, g_1g, g_1b, g_t1.transpose(0, 2, 1), g_bt, g_t2, g_2g, g_2b, g_c1, g_b1, g_c2, g_b2,
                g_fg, g_fb, g_h, g_bh)

    specs = weight_specs()
    return jax.shard_map(step, mesh=mesh, in_specs=(P('fsdp', None, None), P('fsdp')) + specs,
                         out_specs=(P(),) + specs, check_vma=False)
```

```python
import functools

import jax
import jax.numpy as jnp
from jax import lax
from jax.experimental import pallas as pl
from jax.experimental.pallas import tpu as pltpu
from jax.sharding import PartitionSpec as P

MESH = pl.DeviceIdType.MESH
ORDERS = (('x', 'y', 'z'), ('y', 'z', 'x'), ('z', 'x', 'y'))
COLS = ((0, 384), (384, 384), (768, 256))
N_CH = 4
STEM, HEAD = 4, 5
bf16, f32 = jnp.bfloat16, jnp.float32


def my_place():
    f = lax.axis_index('fsdp')
    return {'x': lax.axis_index('tp'), 'z': f // 8, 'y': (f // 2) % 4, 'k': f % 2}


def moved(place, dim, step):
    new = dict(place)
    new[dim] = 1 - place['k'] if dim == 'k' else (place[dim] + step) % 4
    return new


def device(place):
    return {'tp': place['x'], 'fsdp': (place['z'] * 4 + place['y']) * 2 + place['k']}


EPS = 1e-6
TOK, TPAD = 49, 56
IMG = 8
ROWS, XROWS = IMG * TOK, IMG * TPAD
CH, TOKH, CHH = 1024, 512, 4096
BLK = 512
NBLK = CHH // BLK
GELU_C, GELU_A = 0.7978845608028654, 0.044715


def dot_nn(a, b):
    return lax.dot_general(a, b, (((1,), (0,)), ((), ())), preferred_element_type=f32)


def dot_nt(a, b):
    return lax.dot_general(a, b, (((1,), (1,)), ((), ())), preferred_element_type=f32)


def dot_tn(a, b):
    return lax.dot_general(a, b, (((0,), (0,)), ((), ())), preferred_element_type=f32)


def gelu_both(x):
    sq = x * x
    half = 0.5 * jnp.tanh(x * (GELU_C + (GELU_C * GELU_A) * sq))
    rise = 0.5 + half
    value = x * rise
    return value, rise + value * (0.5 - half) * (2.0 * GELU_C + (6.0 * GELU_C * GELU_A) * sq)


def standardize(x):
    mean = jnp.mean(x, axis=-1, keepdims=True)
    cent = x - mean
    inv = lax.rsqrt(jnp.mean(cent * cent, axis=-1, keepdims=True) + EPS)
    return cent * inv, inv


def norm_grad(d, gain, std, inv):
    gs = d * gain
    m0 = jnp.mean(gs, axis=-1, keepdims=True)
    m1 = jnp.mean(gs * std, axis=-1, keepdims=True)
    return inv * (gs - m0 - std * m1)


def row_mask(rows=TPAD):
    return lax.broadcasted_iota(jnp.int32, (rows, 1), 0) < TOK


def image(b):
    return pl.ds(b, TPAD, stride=IMG)


def get(ref, rows):
    return jnp.concatenate([ref[n, rows, :] for n in range(CH // 128)], axis=1)


def put(ref, rows, value):
    for n in range(CH // 128):
        ref[n, rows, :] = value[:, 128 * n:128 * (n + 1)]


class Stream:
    def __init__(self, sem, copies, count):
        self.sem, self.copies, self.count = sem, copies, count

    def make(self, i, slot):
        return [pltpu.make_async_copy(src, dst, self.sem.at[slot, n]) for n, (src, dst) in enumerate(self.copies(i, slot))]

    def start(self, i, slot):
        for copy in self.make(i, slot):
            copy.start()

    def wait(self, i, slot):
        for copy in self.make(i, slot):
            copy.wait()


def for_blocks(stream, body, out=None):
    n = stream.count
    stream.start(0, 0)

    @pl.loop(0, n)
    def _(i):
        slot = i % 2
        stream.wait(i, slot)

        @pl.when(i + 1 < n)
        def _():
            stream.start(i + 1, 1 - slot)
        if out is not None:
            @pl.when(i >= 2)
            def _():
                out.wait(i - 2, slot)
        body(i, slot)
        if out is not None:
            out.start(i, slot)
    if out is not None:
        out.wait(n - 2, n % 2)
        out.wait(n - 1, 1 - n % 2)


TOK_CUTS = 4
FRONT_COPIES = 270
EARLY = [('stem', c) for c in range(3)] + [('ch', c, p) for p in 'ab' for c in range(3)] + [('head', 2)]
PARTS = {'a': pl.ds(0, 2), 'b': pl.ds(2, 2)}
LATE = [('stem', c, None) for c in range(3)] + [('ch', c, g) for g in range(N_CH) for c in range(3)] + [('head', 2, None)]
UNIT_GROUP = {('stem', None): 0, ('ch', 0): 1, ('ch', 1): 2, ('ch', 2): 3, ('ch', 3): 4, ('head', None): 5}
EVERY = pl.ds(0, 4)
FRONT_ORDER = (
    ('prep', (('M0', ('sm',)), ('M0', ('tk',)), ('A0', ('stem', 0)), ('A0', ('stem', 1)), ('A0', ('stem', 2)),
        ('A0', ('ch', 0, 'a')), ('A0', ('ch', 0, 'b')), ('A0', ('ch', 1, 'a')), ('A0', ('ch', 1, 'b')),
        ('A0', ('ch', 2, 'a')), ('A0', ('ch', 2, 'b')), ('A0', ('head', 2)),)),
    ('unpack', (('M1', ('sm',)), ('M1', ('tk',)), ('A', ('stem', 0)), ('A', ('stem', 1)), ('A', ('stem', 2)),
        ('A', ('ch', 0, 'a')), ('A', ('ch', 1, 'a')), ('A', ('ch', 2, 'a')), ('A', ('ch', 0, 'b')), ('A', ('ch', 2, 'b')),
        ('A', ('head', 2)), ('A', ('ch', 1, 'b')), ('B', ('stem', 0)), ('M2', ('sm',)), ('B', ('stem', 1)),
        ('B', ('ch', 0, 'a')), ('B', ('ch', 1, 'a')), ('B', ('ch', 0, 'b')), ('B', ('ch', 1, 'b')), ('M2', ('tk',)),
        ('B', ('stem', 2)), ('B', ('head', 2)), ('C', ('stem', 0)), ('B', ('ch', 2, 'a')), ('B', ('ch', 2, 'b')),
        ('M3', ('sm',)), ('C', ('stem', 2)), ('C', ('stem', 1)), ('C', ('head', 2)),)),
    ('stem0', (('D', ('stem', 0, None)), ('C', ('ch', 0, 'a')), ('C', ('ch', 1, 'a')), ('C', ('ch', 2, 'a')),
        ('D', ('stem', 2, None)), ('D', ('stem', 1, None)), ('D', ('ch', 2, 0)), ('D', ('ch', 2, 1)), ('D', ('ch', 0, 0)),
        ('D', ('ch', 0, 1)), ('E', ('stem', 0, None)), ('E', ('stem', 2, None)), ('E', ('stem', 1, None)),
        ('D', ('ch', 1, 0)), ('D', ('ch', 1, 1)), ('F', ('stem', 1, None)), ('E', ('ch', 2, 0)), ('E', ('ch', 0, 0)),
        ('E', ('ch', 2, 1)), ('F', ('stem', 2, None)), ('C', ('ch', 0, 'b')), ('C', ('ch', 1, 'b')), ('C', ('ch', 2, 'b')),
        ('D', ('head', 2, None)), ('E', ('ch', 1, 0)), ('F', ('ch', 2, 0)), ('E', ('ch', 0, 1)), ('F', ('stem', 0, None)),
        ('F', ('ch', 2, 1)), ('D', ('ch', 0, 2)), ('D', ('ch', 0, 3)),)),
    ('stem1', (('E', ('ch', 1, 1)),)),
    ('stem2', (('F', ('ch', 0, 0)), ('D', ('ch', 2, 2)), ('D', ('ch', 2, 3)),)),
    ('tok0_0', (('D', ('ch', 1, 2)), ('D', ('ch', 1, 3)), ('E', ('head', 2, None)),)),
    ('tok0_1', (('F', ('ch', 1, 0)),)),
    ('tok0_3', (('F', ('ch', 0, 1)),)),
    ('tok0_5', (('F', ('ch', 1, 1)), ('E', ('ch', 2, 2)),)),
    ('ch0_1', (('E', ('ch', 0, 2)), ('E', ('ch', 2, 3)),)),
    ('ch0_2', (('E', ('ch', 1, 2)), ('F', ('head', 2, None)),)),
    ('ch0_4', (('F', ('ch', 2, 2)),)),
    ('ch0_5', (('E', ('ch', 0, 3)), ('F', ('ch', 2, 3)),)),
    ('ch0_7', (('E', ('ch', 1, 3)),)),
    ('tok1_0', (('F', ('ch', 0, 2)),)),
    ('tok1_1', (('F', ('ch', 1, 2)),)),
    ('tok1_3', (('F', ('ch', 0, 3)),)),
    ('tok1_5', (('F', ('ch', 1, 3)),)),
)


class Net:
    def __init__(self, send_sems, recv_sems):
        self.send_sems, self.recv_sems, self.names, self.builds, self.done = send_sems, recv_sems, {}, [], set()

    def copy(self, name):
        n = self.names[name]
        src, dst, target = self.builds[n]()
        return pltpu.make_async_remote_copy(src_ref=src, dst_ref=dst, send_sem=self.send_sems.at[n],
                                            recv_sem=self.recv_sems.at[n], device_id=target, device_id_type=MESH)

    def start(self, name, build):
        self.names[name] = len(self.builds)
        self.builds.append(build)
        self.copy(name).start()

    def arrived(self, *names):
        for name in names:
            self.copy(name).wait_recv()

    def finish(self):
        for name in self.names:
            if name not in self.done:
                self.copy(name).wait_send()


def core_first(size, cols, each):
    half = cols // 2
    row = lax.broadcasted_iota(jnp.int32, (size, size), 0)
    col = lax.broadcasted_iota(jnp.int32, (1, size), 1)
    source = col % half // each * (2 * each) + col // half * each + col % each
    return jnp.where(row == source, 1.0, 0.0).astype(bf16)


def three_parts(x):
    hi = x.astype(bf16)
    rest = x - hi.astype(f32)
    mid = rest.astype(bf16)
    return hi, mid, (rest - mid.astype(f32)).astype(bf16)


def with_bias_rows(a):
    row = lax.broadcasted_iota(jnp.int32, (TPAD, 1), 0)
    return jnp.where(row < TOK, a, jnp.where(row < TOK + 3, 1.0, 0.0)).astype(bf16)


def front_kernel(labels, patches, w_stem, w_ch1, w_ch2, w_head, w_tok1, w_tok2, b_tok1, b_ch1, b_head, b_stem, ln1_g, ln1_b,
                 ln2_g, ln2_b, b_ch2, lnf_g, lnf_b,
                 wc, pat_out, xin, xmid, vout, pre_out, act_out, hl, hr, dx0, hstat, gbh, vec, wt, wt_t,
                 pc, ps, ph, tk_f, tk_p, sm_p, bh_p, ws, wh, tk_v, sm_v, sm_2, bh_v, bch1,
                 turn, p_v, pk_v, x_a, x_b, v_v, w1_v, w2_v, pre_v, act_v, g_v,
                 send_sems, recv_sems, sem, sem_w, sem_o, sem_x):
    me = my_place()
    other = moved(me, 'k', 1)
    load_p = pltpu.make_async_copy(patches.at[:, pl.ds(pl.multiple_of(me['x'] * IMG, IMG), IMG)], p_v, sem.at[0])
    load_p.start()

    barrier = pltpu.get_barrier_semaphore()
    for dim in 'xyz':
        for step in (1, 2, 3):
            pl.semaphore_signal(barrier, inc=1, device_id=device(moved(me, dim, step)), device_id_type=MESH)
    pl.semaphore_signal(barrier, inc=1, device_id=device(other), device_id_type=MESH)

    stem = dot_nn(w_stem[...].astype(bf16), core_first(256, 256, 32)).astype(bf16)
    ps[0], ps[1] = stem[:, 0:128], stem[:, 128:256]
    pick = core_first(1024, 1024, 32)
    for l in range(2):
        pc[2 * l] = dot_nn(w_ch1[l].astype(bf16), pick).astype(bf16)
        pc[2 * l + 1] = dot_nn(w_ch2[l].astype(bf16), pick).astype(bf16)
    ph[...] = jnp.zeros_like(ph)
    ph[:, pl.ds(0, 250)] = w_head[...].astype(bf16)
    turn[...] = jnp.zeros_like(turn)
    for n, ref in ((0, b_stem), (11, lnf_g), (12, lnf_b)):
        turn[n, pl.ds(0, 8)] = ref[...]
    for n, ref in enumerate((ln1_g, ln1_b, ln2_g, ln2_b, b_ch2)):
        for l in range(2):
            turn[pl.ds(1 + 5 * l + n, 1), pl.ds(0, 8)] = ref[pl.ds(l, 1), :]
    turn[pl.ds(16, 2), pl.ds(0, 16)] = b_tok1[...]
    turned = turn[...].T
    tk_f[...] = jnp.zeros_like(tk_f)
    for l in range(2):
        tk_f[l, :, pl.ds(0, TOK)] = w_tok1[l]
        tk_f[2 + l, :, pl.ds(0, TOK)] = w_tok2[l]
        for n, part in enumerate(three_parts(turned[0:16, 16 + l:17 + l])):
            tk_f[l, :, pl.ds(TOK + n, 1)] = part.astype(f32)
    tk_p[...] = tk_f[...].astype(bf16)
    sm_p[...] = jnp.zeros_like(sm_p)
    sm_p[:, pl.ds(0, 16)] = turned[0:8, 0:16]
    sm_p[pl.ds(0, 2), pl.ds(32, 32)] = b_ch1[...]
    bh_p[...] = jnp.full_like(bh_p, -1e30)
    bh_p[0, pl.ds(0, 250)] = b_head[...]

    net = Net(send_sems, recv_sems)
    core = me['k']
    ring = {d: [moved(me, d, n)[d] for n in range(4)] for d in 'xyz'}
    columns = [pl.ds(pl.multiple_of(x * 256, 256), 256) for x in ring['x']]
    stem_columns = [pl.ds(pl.multiple_of(x * 128, 128), 128) for x in ring['x']]
    peers = {(d, n): device(moved(me, d, n)) for d in 'xyz' for n in (1, 2, 3)}
    partner = device(other)
    here = {'x': 0, 'y': 0, 'z': 0}

    def view(unit, block, half=None):
        kind, colour = unit[:2]
        x, z, y = (EVERY if block[d] is None else ring[d][block[d]] for d in 'xzy')
        r0, rn = (0, 32) if half is None else (16 * half, 16)
        if kind == 'ch':
            c0, cn = COLS[colour]
            g = PARTS.get(unit[2], unit[2])
            return wc.at[g, x, core, z, y, pl.ds(r0, rn), pl.ds(c0, cn)]
        if kind == 'stem':
            cols = pl.ds(0, 512) if x is EVERY else stem_columns[block['x']]
            return ws.at[:, z, y, core, pl.ds(32 * colour + r0, rn), cols]
        cols = pl.ds(0, CH) if x is EVERY else columns[block['x']]
        return wh.at[core, z, y, pl.ds(r0, rn), cols]

    def piece(unit):
        kind, colour = unit[:2]
        if kind == 'ch':
            return pc.at[PARTS[unit[2]], :, pl.ds(*COLS[colour])]
        return ps.at[:, pl.ds(32 * colour, 32), :] if kind == 'stem' else ph.at[:, :]

    def exchange(unit, tag, dim, block):
        for side, step in (('l', 1), ('r', 3)):
            def build(step=step):
                part = view(unit, block)
                return (piece(unit) if tag == '1' else part), part, peers[dim, step]
            net.start((unit, tag, side), build)

    def forward_half(unit, tag, dim, block):
        for half, (origin, target, side) in enumerate(((3, 1, 'l'), (1, 3, 'r'))):
            def build(half=half, origin=origin, target=target):
                part = view(unit, {**block, dim: origin}, half)
                return part, part, peers[dim, target]
            net.start((unit, tag, side), build)

    def swap(unit, tag, block):
        def build():
            part = view(unit, block)
            return part, part, partner
        net.start((unit, tag), build)

    own = pltpu.make_async_copy(pc, wc.at[:, me['x'], me['k'], me['z'], me['y']], sem.at[1])
    own.start()
    mine = pl.ds(pl.multiple_of(me['x'] * 256, 256), 256)
    for n in range(2):
        ws[n, me['z'], me['y'], me['k'], :, stem_columns[0]] = ps[n]
    wh[me['k'], me['z'], me['y'], :, mine] = ph[...]
    sm_v[me['x'], me['z'], me['y'], me['k']] = sm_p[...]
    tk_v[:, me['z'], me['y'], me['k']] = tk_p[...]
    bh_v[:, mine] = bh_p[...]
    own.wait()
    pl.semaphore_wait(barrier, 10)

    def small(kind, n):
        dims = 'xyz' if kind == 'sm' else 'yz'
        at = {d: EVERY if d in dims[:n] else ring[d][0] for d in 'xyz'}

        def part():
            if kind == 'sm':
                return sm_v.at[at['x'], at['z'], at['y'], core]
            return tk_v.at[:, at['z'], at['y'], core]
        if n > 0:
            net.arrived(*[(kind, n - 1, s) for s in (1, 2, 3)])
        if n < len(dims):
            for s in (1, 2, 3):
                net.start((kind, n, s), lambda s=s: (part(), part(), peers[dims[n], s]))
            if kind == 'sm' and n == 0:
                def head_bias():
                    return bh_v.at[:, columns[0]]
                for s in (1, 2, 3):
                    net.start(('bh', s), lambda s=s: (head_bias(), head_bias(), peers['x', s]))
        else:
            net.start((kind, 'k'), lambda: (part(), part(), partner))

    def step(name, unit):
        if name[0] == 'M':
            small(unit[0], int(name[1]))
            return
        d1, d2, d3 = ORDERS[unit[1]]
        early = unit[:2] if unit[0] != 'ch' or unit[2] in PARTS else ('ch', unit[1], 'a' if unit[2] < 2 else 'b')
        plane = {**here, d1: None, d2: None}
        if name == 'A0':
            exchange(unit, '1', d1, here)
        elif name == 'A':
            net.arrived((unit, '1', 'l'), (unit, '1', 'r'))
            forward_half(unit, '1h', d1, here)
        elif name == 'B':
            net.arrived((unit, '1h', 'l'), (unit, '1h', 'r'))
            exchange(unit, '2', d2, {**here, d1: None})
        elif name == 'C':
            net.arrived((unit, '2', 'l'), (unit, '2', 'r'))
            forward_half(unit, '2h', d2, {**here, d1: None})
        elif name == 'D':
            if early not in planes:
                planes.add(early)
                net.arrived((early, '2h', 'l'), (early, '2h', 'r'))
            exchange(unit, '3', d3, plane)
            swap(unit, 'k0', plane)
        elif name == 'E':
            net.arrived((unit, '3', 'l'), (unit, '3', 'r'))
            forward_half(unit, '3h', d3, plane)
            for n in (1, 3):
                swap(unit, f'k{n}', {**plane, d3: n})
        else:
            net.arrived((unit, '3h', 'l'), (unit, '3h', 'r'))
            swap(unit, 'k2', {**plane, d3: 2})

    planes = set()
    awaited = set()

    def need(group):
        for u in LATE:
            if UNIT_GROUP[u[0], u[2]] <= group and u not in awaited:
                awaited.add(u)
                net.arrived(*[(u, f'k{n}') for n in range(4)])

    bursts = {name: steps for name, steps in FRONT_ORDER}

    def burst(name):
        for s in bursts.get(name, ()):
            step(*s)

    def during(name, count):
        def run(i):
            for n in range(1, count):
                if bursts.get(f'{name}{n}'):
                    pl.when(i == n)(functools.partial(burst, f'{name}{n}'))
        return run

    burst('prep')
    load_p.wait()
    pick = core_first(768, 768, 96)
    for g in range(4):
        part = dot_nn(p_v[:, :, pl.ds(768 * g, 768)].reshape(ROWS, 768), pick).astype(bf16)
        for n in range(2):
            pk_v[n, :, pl.ds(384 * g, 384)] = part[:, 384 * n:384 * n + 384]
    keep_p = pltpu.make_async_copy(pk_v, pat_out, sem.at[0])
    keep_p.start()

    burst('unpack')
    net.arrived(('sm', 'k'), ('tk', 'k'), ('bh', 1), ('bh', 2), ('bh', 3))
    sm_2[...] = sm_v[...].reshape(1024, 128)
    for n in range(8):
        tile = jnp.concatenate([sm_2[pl.ds((n % 4 * 4 + i) * 64 + n // 4 * 32, 32), :] for i in range(4)], axis=0)
        vec[:, pl.ds(128 * n, 128)] = tile.T[0:16, :]
    wt[...] = tk_v[...].reshape(4, TOKH, 128)
    for n in range(4):
        wt_t[n] = wt[n].astype(f32).T[0:TPAD].astype(bf16)
    for l in range(2):
        rows = jnp.concatenate(three_parts(sm_2[pl.ds(l, 128, stride=8), :]), axis=0)

        @pl.loop(0, 8)
        def _(n):
            lane = lax.broadcasted_iota(jnp.int32, (128, 512), 0)
            col = lax.broadcasted_iota(jnp.int32, (128, 512), 1)
            pick = jnp.where(lane == 32 + col % 32, 1.0, 0.0).astype(bf16)
            spread = dot_nn(rows, pick)
            value = spread[0:128] + spread[128:256] + spread[256:384]
            mine = lane == n // 2 * 32 + col // 32 * 2 + n % 2
            bch1[l:l + 1, pl.ds(pl.multiple_of(n * 512, 512), 512)] = jnp.sum(jnp.where(mine, value, 0.0), axis=0, keepdims=True)

    burst('stem0')
    need(0)
    run = during('stem', 4)
    put(x_a, pl.ds(ROWS, XROWS - ROWS), jnp.zeros((XROWS - ROWS, CH), f32))

    @pl.loop(0, 4)
    def _(i):
        run(i)
        cols = pl.ds(pl.multiple_of(i * 256, 256), 256)
        w = ws[i // 2, :, :, :, :, pl.ds(pl.multiple_of(i % 2 * 256, 256), 256)].reshape(3072, 256)
        value = dot_nn(p_v[...].reshape(ROWS, 3072), w) + vec[0:1, cols]
        for n in range(2):
            x_a[2 * i + n, pl.ds(0, ROWS), :] = value[:, 128 * n:128 * (n + 1)]

    wc_all = wc

    def add_rows(x_v, value):
        for n in range(CH // 128):
            x_v[n, pl.ds(0, ROWS), :] += value[:, 128 * n:128 * (n + 1)]

    for l in range(2):
        r = 1 + 5 * l
        x_old, x_v = ((x_a, x_b), (x_b, x_a))[l]
        burst(f'tok{l}_0')
        run = during(f'tok{l}_', IMG)
        save_in = pltpu.make_async_copy(x_old.at[:, pl.ds(0, ROWS)], xin.at[l], sem_x.at[3])
        save_in.start()

        @pl.loop(0, IMG)
        def _(b):
            run(b)
            x = get(x_old, image(b))
            std, _ = standardize(x)
            a = with_bias_rows(std * vec[r:r + 1, :] + vec[r + 1:r + 2, :])
            g_v[...] = gelu_both(dot_nn(wt[l, :, 0:TPAD], a))[0].astype(bf16)
            put(x_v, image(b), x + dot_nn(wt_t[2 + l], g_v[...]))
        save_mid = pltpu.make_async_copy(x_v.at[:, pl.ds(0, ROWS)], xmid.at[l], sem_x.at[0])
        save_mid.start()
        burst(f'ln{l}')

        def norm_rows(rows):
            std, _ = standardize(get(x_v, rows))
            v_v[rows, :] = (std * vec[r + 2:r + 3, :] + vec[r + 3:r + 4, :]).astype(bf16)

        @pl.loop(0, ROWS // (2 * TPAD))
        def _(n):
            norm_rows(pl.ds(pl.multiple_of(n * 2 * TPAD, 16), 2 * TPAD))
        norm_rows(pl.ds(ROWS // (2 * TPAD) * 2 * TPAD, TPAD))
        save_v = [pltpu.make_async_copy(v_v.at[:, pl.ds(512 * n, 512)], vout.at[l, n], sem_x.at[1 + n]) for n in range(2)]
        for copy in save_v:
            copy.start()
        burst(f'ch{l}_0')
        need(2 + 2 * l)
        save_mid.wait()

        def blocks(i, slot):
            t, h = i // 2, i % 2
            part = pl.ds(pl.multiple_of(h * BLK, BLK), BLK)
            return [(wc_all.at[2 * l, t, :, :, :, :, part], w1_v.at[slot]), (wc_all.at[2 * l + 1, t, h], w2_v.at[slot])]

        def outs(i, slot):
            part = pl.ds(pl.multiple_of(i * BLK, BLK), BLK)
            half = pl.ds(pl.multiple_of(i // 2 * BLK, BLK), BLK)
            return [(pre_v.at[slot], pre_out.at[l, :, part]), (act_v.at[slot], act_out.at[l, i % 2, :, half])]
        run = during(f'ch{l}_', NBLK)

        def channel(i, slot):
            run(i)
            part = pl.ds(pl.multiple_of(i * BLK, BLK), BLK)
            h = dot_nn(v_v[...], w1_v[slot].reshape(CH, BLK)) + bch1[l:l + 1, part]
            value, pre_v[slot] = gelu_both(h)
            act_v[slot] = value.astype(bf16)
            add_rows(x_v, dot_nn(act_v[slot], w2_v[slot].reshape(BLK, CH)))
        for_blocks(Stream(sem_w, blocks, NBLK), channel, Stream(sem_o, outs, NBLK))

        @pl.loop(0, CH // 128)
        def _(n):
            x_v[n, pl.ds(0, ROWS), :] += vec[r + 4:r + 5, pl.ds(pl.multiple_of(128 * n, 128), 128)]
        for copy in (save_in, *save_v):
            copy.wait()

    burst('head')
    need(5)
    keep_p.wait()
    last = 11
    pooled = jnp.sum(get(x_a, pl.ds(0, ROWS)).reshape(TOK, IMG, CH), axis=0) * (1.0 / TOK)
    std, inv = standardize(pooled)
    head_in = (std * vec[last:last + 1, :] + vec[last + 1:last + 2, :]).astype(bf16)
    hl[...] = head_in
    w_h = wh[...].reshape(CH, CH)
    logits = dot_nn(head_in, w_h) + bh_v[0:1, :]
    row = lax.broadcasted_iota(jnp.int32, (IMG, 1), 0)
    label = jnp.zeros((IMG, 1), jnp.int32)
    for b in range(IMG):
        value = labels[me['x'] * IMG + b]
        label = jnp.where(row == b, value, label)
    label = label + 6 * sum(jnp.where(label >= edge, 1, 0) for edge in (250, 500, 750))
    is_label = lax.broadcasted_iota(jnp.int32, logits.shape, 1) == label
    top = jnp.max(logits, axis=-1, keepdims=True)
    ex = jnp.exp(logits - top)
    es = jnp.sum(ex, axis=-1, keepdims=True)
    nll = top + jnp.log(es) - jnp.sum(jnp.where(is_label, logits, 0.0), axis=-1, keepdims=True)
    d_logits = (ex / es - jnp.where(is_label, 1.0, 0.0)) * (1.0 / 1024)
    gbh[...] = jnp.sum(d_logits, axis=0, keepdims=True)
    d_bf = d_logits.astype(bf16)
    hr[...] = d_bf
    d_in = dot_nt(d_bf, w_h)
    hstat[0:1, :] = jnp.sum(d_in * std, axis=0, keepdims=True)
    hstat[1:2, :] = jnp.sum(d_in, axis=0, keepdims=True)
    hstat[2:3, :] = jnp.broadcast_to(jnp.sum(nll, axis=0, keepdims=True), (1, CH))
    dx0[...] = norm_grad(d_in, vec[last:last + 1, :], std, inv) * (1.0 / TOK)
    burst('end')
    net.finish()
    assert len(net.builds) <= FRONT_COPIES, len(net.builds)


def front(*operands):
    a, v = pl.BlockSpec(memory_space=pl.ANY), pl.BlockSpec(memory_space=pltpu.VMEM)
    S, V, DMA = jax.ShapeDtypeStruct, pltpu.VMEM, pltpu.SemaphoreType.DMA
    return pl.pallas_call(
        front_kernel, name='front',
        in_specs=[pl.BlockSpec(memory_space=pltpu.SMEM), a] + [v] * 17,
        out_specs=[a] * 7 + [v] * 8,
        out_shape=[S((N_CH, 4, 2, 4, 4, 32, 1024), bf16), S((2, ROWS, 1536), bf16), S((2, CH // 128, ROWS, 128), f32),
                   S((2, CH // 128, ROWS, 128), f32),
                   S((2, 2, ROWS, 512), bf16), S((2, ROWS, CHH), f32), S((2, 2, ROWS, 2048), bf16), S((IMG, CH), bf16),
                   S((IMG, CH), bf16), S((IMG, CH), f32), S((8, CH), f32), S((1, CH), f32), S((16, CH), f32),
                   S((4, TOKH, 128), bf16), S((4, TPAD, TOKH), bf16)],
        scratch_shapes=[V((N_CH, 32, 1024), bf16), V((2, 96, 128), bf16), V((32, 256), bf16), V((4, 16, 128), f32),
                        V((4, 16, 128), bf16), V((8, 128), f32), V((8, 256), f32), V((2, 4, 4, 2, 96, 512), bf16),
                        V((2, 4, 4, 32, CH), bf16), V((4, 4, 4, 2, 16, 128), bf16), V((4, 4, 4, 2, 8, 128), f32),
                        V((1024, 128), f32), V((8, CH), f32), V((2, CHH), f32),
                        V((128, 128), f32), V((TOK, IMG, 3072), bf16), V((2, ROWS, 1536), bf16), V((CH // 128, XROWS, 128), f32),
                        V((CH // 128, XROWS, 128), f32),
                        V((ROWS, CH), bf16), V((2, 2, 4, 4, 32, BLK), bf16), V((2, 4, 4, 32, CH), bf16),
                        V((2, ROWS, BLK), f32), V((2, ROWS, BLK), bf16), V((TOKH, CH), bf16),
                        DMA((FRONT_COPIES,)), DMA((FRONT_COPIES,)), DMA((2,)), DMA((2, 2)), DMA((2, 2)), DMA((4,))],
        compiler_params=pltpu.CompilerParams(collective_id=0, has_side_effects=True, vmem_limit_bytes=62 * 1024 * 1024),
        cost_estimate=pl.CostEstimate(flops=90_000_000_000, bytes_accessed=180_000_000, transcendentals=0),
    )(*operands)


GROUPS = (3, 2, 1, HEAD, 0, STEM)
UNITS = tuple((g, c) for g in GROUPS for c in (2, 0, 1) if g != HEAD or c == 2)
BACK_COPIES = 18 * len(UNITS) + 40
NEEDS = {3: ('act1', 'dout1'), 2: ('vin1', 'dpre1'), 1: ('act0', 'dout0'), 0: ('vin0', 'dpre0'), STEM: ('pat', 'dres'),
         HEAD: ('hl', 'hr')}
BACK_ORDER = (
    ('c1_7', ((3, 'L'),)),
    ('t1_0', ((0, 0), (0, 1), (1, 0), (1, 1), (2, 0), (2, 1), (0, 2),)),
    ('t1_2', ((1, 2),)),
    ('t1_3', ((0, 3), (2, 2),)),
    ('t1_4', ((2, 'L'),)),
    ('t1_6', ((1, 3), (0, 4), (3, 0), (3, 1), (2, 3), (4, 0), (4, 1), (1, 4), (0, 5), (5, 0), (5, 1), (3, 2), (1, 5), (0, 6),)),
    ('t1_7', ((2, 4),)),
    ('d0', ((4, 2),)),
    ('c0_1', ((5, 2), (3, 3), (2, 5), (1, 6),)),
    ('c0_3', ((1, 'L'), (1, 7),)),
    ('c0_4', ((4, 3), (3, 4), (0, 7), (6, 0), (6, 1), (2, 6), (7, 0), (7, 1), (5, 3), (4, 4), (3, 5), (2, 7), (8, 0), (8, 1),
        (6, 2), (4, 5), (3, 6), (9, 0), (9, 1),)),
    ('c0_5', ((7, 2), (5, 4),)),
    ('c0_7', ((6, 3), (8, 2), (4, 6),)),
    ('t0_0', ((9, 2),)),
    ('t0_1', ((7, 3), (6, 4), (3, 7),)),
    ('t0_2', ((5, 5), (4, 7),)),
    ('t0_3', ((8, 3), (7, 4), (6, 5), (9, 3), (5, 6),)),
    ('t0_4', ((0, 'L'),)),
    ('t0_5', ((8, 4), (9, 4), (7, 5), (6, 6), (5, 7), (10, 0), (10, 1), (11, 0), (11, 1), (8, 5), (9, 5), (7, 6), (6, 7),
        (12, 0), (12, 1), (10, 2), (9, 6),)),
    ('t0_6', ((7, 7),)),
    ('t0_7', ((11, 2),)),
    ('fin', ((12, 2), (10, 3),)),
    ('end', ((8, 6), (9, 7), (11, 3), (10, 4), (8, 7), (4, 'L'), (12, 3), (10, 5), (11, 4), (13, 0), (13, 1), (12, 4),
        (11, 5), (10, 6), (14, 0), (14, 1), (15, 0), (15, 1), (10, 7), (13, 2), (14, 2), (15, 2), (12, 5), (11, 6), (14, 3),
        (15, 3), (12, 6), (13, 3), (11, 7), (14, 4), (12, 7), (15, 4), (13, 4), (14, 5), (15, 5), (13, 5), (14, 6), (15, 6),
        (13, 6), (14, 7), (15, 7), (13, 7),)),
)
SMALL = dict(sm=((4, 4, 4, 8, 128), (3, 4, 4, 8, 128), (3, 4, 8, 128), (3, 8, 128)),
             tk=((4, 4, 4, 16, 128), (3, 4, 4, 16, 128), (3, 4, 16, 128), (3, 4, 16, 128)))


def reduce_scratch():
    per = []
    for c in range(3):
        n = COLS[c][1]
        many = sum(1 for u in UNITS if u[1] == c)
        lead = ((4, 4), (4,), ())
        b = {'C': pltpu.VMEM((2, 4, 4, 4, 32, n), bf16), 'S1': pltpu.VMEM((4, 4, 32, n), f32), 'S2': pltpu.VMEM((2, 4, 32, n), f32)}
        for ph in range(3):
            if ph:
                b[f'opp{ph}'] = pltpu.VMEM(lead[ph] + (32, n), bf16)
                b[f'pr{ph}'] = pltpu.VMEM(lead[ph] + (16, n), bf16)
                b[f'pl{ph}'] = pltpu.VMEM(lead[ph] + (16, n), bf16)
            for name in ('rig', 'lef'):
                b[f'{name}{ph}'] = pltpu.VMEM(lead[ph] + (16, n), bf16)
            for name in ('half0', 'half1'):
                b[f'{name}{ph}'] = pltpu.VMEM((many,) + lead[ph] + (16, n), bf16)
            for name in ('froml', 'fromr'):
                b[f'{name}{ph}'] = pltpu.VMEM((many,) + lead[ph] + (32, n), bf16)
        per.append(b)
    return per


def small_scratch():
    b = {f'{kind}{n + 1}': pltpu.VMEM(shape, f32) for kind, shapes in SMALL.items() for n, shape in enumerate(shapes)}
    b.update(sm=pltpu.VMEM((4, 4, 4, 2, 8, 128), f32), tk=pltpu.VMEM((4, 4, 4, 2, 16, 128), f32),
             sm_s1=pltpu.VMEM((4, 4, 8, 128), f32), sm_s2=pltpu.VMEM((4, 8, 128), f32),
             tk_s1=pltpu.VMEM((4, 4, 16, 128), f32), tk_s2=pltpu.VMEM((4, 16, 128), f32))
    return b


def small_pack(b, flat, turn, gvec, hstat, gbch1, gbh):
    @pl.loop(0, 8)
    def _(n):
        cols = pl.ds(pl.multiple_of(128 * n, 128), 128)
        turn[n, pl.ds(0, 128), :] = jnp.zeros((128, 128), f32)
        turn[n, pl.ds(0, 16), :] = gvec[:, cols]
        turn[n, pl.ds(11, 2), :] = hstat[pl.ds(0, 2), cols]
        tile = turn[n, pl.ds(0, 128), :].T
        for i in range(4):
            row = pl.multiple_of(i % 2 * 64 + n // 4 * 32, 32)
            flat[n % 4 * 2 + i // 2, pl.ds(row, 32), :] = tile[32 * i:32 * i + 32]
    for l in range(2):
        def gather(n, total):
            lane = lax.broadcasted_iota(jnp.int32, (128, 512), 0)
            col = lax.broadcasted_iota(jnp.int32, (128, 512), 1)
            sums = gbch1[l:l + 1, pl.ds(pl.multiple_of(512 * n, 512), 512)]
            mine = jnp.where(lane == n // 2 * 32 + col // 32 * 2 + n % 2, sums, 0.0)
            pick = jnp.where(lane == 32 + col % 32, 1.0, 0.0).astype(bf16)
            return total + dot_nt(jnp.concatenate(three_parts(mine), axis=0), pick)
        total = lax.fori_loop(0, 8, gather, jnp.zeros((384, 128), f32))
        total = total[0:128] + total[128:256] + total[256:384]
        for n in range(8):
            flat[n, pl.ds(l, 16, stride=8), :] += total[16 * n:16 * n + 16]
    lane = lax.broadcasted_iota(jnp.int32, (1, 128), 1)
    for t in range(4):
        for q in range(4):
            tile = gbh[0:1, t * 256 + q // 2 * 128:t * 256 + q // 2 * 128 + 128]
            if q % 2 == 0:
                tile = jnp.concatenate([tile[:, 64:], tile[:, :64]], axis=1)
            tile = jnp.where(lane >= 64, tile, 0.0)
            for n in (2 * t, 2 * t + 1):
                flat[n, pl.ds(2 + q, 16, stride=8), :] += tile
    for n in range(8):
        flat[n, pl.ds(6, 16, stride=8), :] += jnp.where(lane == 64, hstat[2:3, 0:128], 0.0)
        b['sm'][n // 2, pl.ds(n % 2 * 2, 2)] = flat[n, pl.ds(0, 128), :].reshape(2, 4, 2, 8, 128)


def back_kernel(*refs):
    xin, xmid, pre_in, wc, act, vin, pat = refs[:7]
    hl, hr, dx0, hstat, gbh, wt, wt_t, vec = refs[7:15]
    out_c, out_s, out_h, sm_own, tk_own = refs[15:20]
    dpre, dout, dres, x_act, x_vin, x_pat, x_dpre, x_dout, x_dres = refs[20:29]
    (per, b, big, little, x_hl, x_hr, gvec, gbch1, x_v, d_v, dv_v, do_v, w1_v, w2_v, pre_v, dp_v,
     send_sems, recv_sems, load_sems, sem, sem_w, sem_o) = refs[29:]
    me = my_place()
    other = moved(me, 'k', 1)
    k, k2 = me['k'], 1 - me['k']
    barrier = pltpu.get_barrier_semaphore()
    for dim in 'xyz':
        for step in (1, 2, 3):
            pl.semaphore_signal(barrier, inc=1, device_id=device(moved(me, dim, step)), device_id_type=MESH)
    pl.semaphore_signal(barrier, inc=1, device_id=device(other), device_id_type=MESH)
    net = Net(send_sems, recv_sems)
    ring = {d: [moved(me, d, n)[d] for n in range(4)] for d in 'xyz'}
    peers = {(d, n): device(moved(me, d, n)) for d in 'xyz' for n in (1, 2, 3)}
    partner = device(other)
    half_at = pl.ds(pl.multiple_of(k * 512, 512), 512)
    half_to = pl.ds(pl.multiple_of(k2 * 512, 512), 512)
    swaps = {'act1': (act.at[1, k2], x_act.at[1]), 'act0': (act.at[0, k2], x_act.at[0]), 'vin1': (vin.at[1, k2], x_vin.at[1]),
             'vin0': (vin.at[0, k2], x_vin.at[0]), 'pat': (pat.at[k2], x_pat), 'dpre1': (dpre.at[1], x_dpre.at[1]), 'dpre0': (dpre.at[0], x_dpre.at[0]),
             'dout1': (do_v, x_dout.at[1]), 'dout0': (do_v, x_dout.at[0]), 'dres': (do_v, x_dres),
             'hl': (hl.at[:, half_to], x_hl), 'hr': (hr, x_hr)}

    def swap(*names):
        for name in names:
            net.start(name, lambda name=name: (*swaps[name], partner))
    busy = {}

    def free(key):
        for name in busy.pop(key, ()):
            net.copy(name).wait_send()
            net.done.add(name)

    def loads(g):
        l = g // 2
        if g == STEM:
            wide, tall = (pat.at[k], x_pat, 1536), (dres, x_dres, CH)
        elif g % 2:
            wide, tall = (act.at[l, k], x_act.at[l], 2048), (dout.at[l], x_dout.at[l], CH)
        else:
            wide, tall = (dpre.at[l], x_dpre.at[l], CHH), (vin.at[l, k], x_vin.at[l], 512)
        out = []
        for n, (buf, (own, far, cols)) in enumerate(((big, wide), (little, tall))):
            out += [pltpu.make_async_copy(own, buf.at[0, :, pl.ds(0, cols)], load_sems.at[2 * n]),
                    pltpu.make_async_copy(far, buf.at[1, :, pl.ds(0, cols)], load_sems.at[2 * n + 1])]
        return out

    def product(u):
        g, c, slot = u.g, u.c, u.slot
        first = c == 2
        if first and g != HEAD:
            for copy in loads(g):
                copy.wait()
        if g == STEM and not first:
            return
        for v in (units if g == STEM else (u,)):
            if v.g == g:
                free(('C', v.c, v.slot))
        if g == HEAD:
            net.arrived(*NEEDS[g])
            for t in range(4):
                cols = pl.ds(256 * t, 256)
                prod = dot_tn(hl[:, half_at], hr[:, cols]) + dot_tn(x_hl[...], x_hr[:, cols])
                per[c]['C'][slot, t] = prod.astype(bf16).reshape(4, 4, 32, 256)
        elif g == STEM:
            slots = {v.c: v.slot for v in units if v.g == STEM}

            @pl.loop(0, 4)
            def _(z):
                rows = pl.ds(pl.multiple_of(z * 384, 384), 384)
                for t in range(4):
                    def right(s):
                        return jnp.concatenate([little[s, :, 128 * t:128 * t + 128], little[s, :, 512 + 128 * t:640 + 128 * t]], axis=1)
                    prod = dot_tn(big[0, :, rows], right(0)) + dot_tn(big[1, :, rows], right(1))
                    prod = prod.astype(bf16).reshape(4, 3, 32, 256)
                    for d in range(3):
                        per[d]['C'][slots[d], t, z, :, :, pl.ds(0, 256)] = prod[:, d]
        else:
            c0, n = COLS[c]

            @pl.loop(0, 4)
            def _(t):
                for h in range(2):
                    if g % 2:
                        left = pl.ds(pl.multiple_of(t * 512 + h * 256, 256), 256)
                        prod = dot_tn(big[0, :, left], little[0, :, c0:c0 + n]) + dot_tn(big[1, :, left], little[1, :, c0:c0 + n])
                    else:
                        right = pl.ds(pl.multiple_of(t * 1024 + c0, 128), n)
                        rows = slice(256 * h, 256 * h + 256)
                        prod = dot_tn(little[0, :, rows], big[0, :, right]) + dot_tn(little[1, :, rows], big[1, :, right])
                    per[c]['C'][slot, t, 2 * h:2 * h + 2] = prod.astype(bf16).reshape(2, 4, 32, n)

    class Unit:
        def __init__(self, g, c):
            self.g, self.c = g, c
            self.index = [u for u in UNITS if u[1] == c].index((g, c))
            self.slot = self.index % 2
            self.n = COLS[c][1] if g < N_CH else 256
            self.cols = pl.ds(0, self.n)
            self.buf = per[c]
            self.dims = ORDERS[c]
            self.rest = [d for d in 'xzy' if d != self.dims[0]]

        def cut(self, name, *at, rows=slice(None)):
            ref = self.buf[name]
            inner = [slice(None)] * (len(ref.shape) - len(at) - 2)
            return ref.at[(*at, *inner, rows, self.cols)]

        def block(self, p, rows):
            at = {d: EVERY for d in 'xzy'}
            at[self.dims[0]] = p
            return self.buf['C'].at[self.slot, at['x'], at['z'], at['y'], rows, self.cols]

        def share(self, phase, p, e, rows):
            if phase == 0:
                at = dict(zip(self.rest, e))
                at[self.dims[0]] = p
                return self.buf['C'][self.slot, at['x'], at['z'], at['y'], rows, self.cols].astype(f32)
            if phase == 1:
                at = (p, e[0]) if self.dims[1] == self.rest[0] else (e[0], p)
                return self.buf['S1'][(*at, rows, self.cols)]
            return self.buf['S2'][self.slot, p, rows, self.cols]

        def each(self, phase, body):
            if phase == 2:
                body(())
            elif phase == 1:
                pl.loop(0, 4)(lambda i: body((i,)))
            else:
                @pl.loop(0, 4)
                def _(i):
                    pl.loop(0, 4)(lambda j: body((i, j)))

        def send(self, tag, phase, src, dst, step):
            name = (self.g, self.c, tag, phase)
            net.start(name, lambda: (src(), dst(), peers[self.dims[phase], step]))
            return name

        def arrived(self, phase, *tags):
            net.arrived(*[(self.g, self.c, tag, phase) for tag in tags])

        def opposite(self, phase):
            places = ring[self.dims[phase]]
            low, high = pl.ds(0, 16), pl.ds(16, 16)
            if phase == 0:
                sources = [lambda: self.block(places[2], low), lambda: self.block(places[2], high),
                           lambda: self.block(places[1], high), lambda: self.block(places[3], low)]
            else:
                names = (f'opp{phase}', f'pr{phase}', f'pl{phase}')
                for name in names:
                    free((name, self.c))
                opp, right, left = (self.buf[name] for name in names)

                def body(e):
                    opp[(*e, slice(None), self.cols)] = self.share(phase, places[2], e, pl.ds(0, 32)).astype(bf16)
                    right[(*e, slice(None), self.cols)] = self.share(phase, places[1], e, high).astype(bf16)
                    left[(*e, slice(None), self.cols)] = self.share(phase, places[3], e, low).astype(bf16)
                self.each(phase, body)
                sources = [lambda: self.cut(names[0], rows=low), lambda: self.cut(names[0], rows=high),
                           lambda: self.cut(names[1]), lambda: self.cut(names[2])]
            targets = [lambda: self.cut(f'half0{phase}', self.index), lambda: self.cut(f'half1{phase}', self.index),
                       lambda: self.cut(f'froml{phase}', self.index, rows=high),
                       lambda: self.cut(f'fromr{phase}', self.index, rows=low)]
            sent = [self.send(tag, phase, src, dst, step)
                    for tag, src, dst, step in zip(('h0', 'h1', 'p0', 'p1'), sources, targets, (1, 3, 1, 3))]
            if phase == 0:
                busy['C', self.c, self.slot] = sent
            else:
                busy[names[0], self.c] = sent[:2]
                busy[names[1], self.c] = sent[2:3]
                busy[names[2], self.c] = sent[3:]

        def beside(self, phase):
            places = ring[self.dims[phase]]
            for half, step, name, dst in ((0, 1, 'rig', 'froml'), (1, 3, 'lef', 'fromr')):
                self.arrived(phase, f'h{half}')
                key = f'{name}{phase}'
                free((key, self.c))
                out, got = self.buf[key], self.buf[f'half{half}{phase}']
                rows = pl.ds(16 * half, 16)

                def body(e):
                    value = self.share(phase, places[step], e, rows) + got[(self.index, *e, slice(None), self.cols)].astype(f32)
                    out[(*e, slice(None), self.cols)] = value.astype(bf16)
                self.each(phase, body)
                busy[key, self.c] = [self.send(f'f{half}', phase, lambda key=key: self.cut(key),
                                               lambda dst=dst, rows=rows: self.cut(f'{dst}{phase}', self.index, rows=rows), step)]

        def total(self, phase):
            self.arrived(phase, 'p0', 'p1', 'f0', 'f1')
            p = ring[self.dims[phase]][0]

            def body(e):
                got = [self.buf[f'{name}{phase}'][(self.index, *e, slice(None), self.cols)].astype(f32)
                       for name in ('froml', 'fromr')]
                value = self.share(phase, p, e, pl.ds(0, 32)) + got[0] + got[1]
                if phase == 0:
                    self.buf['S1'][(*e, slice(None), self.cols)] = value
                elif phase == 1:
                    self.buf['S2'][(self.slot, *e, slice(None), self.cols)] = value
                elif self.g == STEM:
                    out_s[pl.ds(32 * self.c, 32), :] = value
                elif self.g == HEAD:
                    out_h[...] = value
                else:
                    out_c[self.g, :, pl.ds(*COLS[self.c])] = value
            self.each(phase, body)

        def run(self, stage):
            if stage == 0:
                product(self)
            elif stage == 7:
                self.total(2)
            elif stage % 2 == 0:
                self.beside(stage // 2 - 1)
            else:
                if stage > 1:
                    self.total(stage // 2 - 1)
                self.opposite(stage // 2)

    units = [Unit(g, c) for g, c in UNITS]
    bursts = dict(BACK_ORDER)

    def step(which, stage):
        if stage == 'L':
            net.arrived(*NEEDS[which])
            for copy in loads(which):
                copy.start()
        else:
            units[which].run(stage)

    def burst(name):
        for s in bursts.get(name, ()):
            step(*s)

    def during(name, count):
        def run(i):
            for n in range(1, count):
                if bursts.get(f'{name}{n}'):
                    pl.when(i == n)(functools.partial(burst, f'{name}{n}'))
        return run

    load = pltpu.make_async_copy(xmid.at[1], x_v.at[:, pl.ds(0, ROWS)], sem.at[0])
    load.start()
    mask = row_mask()
    rest = pl.ds(ROWS, XROWS - ROWS)
    put(d_v, rest, jnp.zeros((XROWS - ROWS, CH), f32))
    put(x_v, rest, jnp.zeros((XROWS - ROWS, CH), f32))
    gvec[...] = jnp.zeros_like(gvec)
    tk = b['tk']
    tk[...] = jnp.zeros_like(tk)

    @pl.loop(0, TOK)
    def _(s):
        put(d_v, pl.ds(pl.multiple_of(s * IMG, IMG), IMG), dx0[...])

    def add(row, value):
        gvec[row:row + 1, :] += jnp.sum(value, axis=0, keepdims=True)

    def cast_out(row):
        @pl.loop(0, ROWS // TPAD)
        def _(n):
            rows = pl.ds(pl.multiple_of(n * TPAD, 8), TPAD)
            d = get(d_v, rows)
            add(row, d)
            do_v[rows, :] = d.astype(bf16)

    def add_token(n, value, start=0):
        tk[n, :, :, :, :, pl.ds(start, value.shape[1])] += value.reshape(4, 4, 2, 16, value.shape[1])

    for l in (1, 0):
        r = 1 + 5 * l
        free('do')
        cast_out(r + 4)
        keep = pltpu.make_async_copy(do_v, dout.at[l], sem.at[1])
        keep.start()
        if l == 1:
            pl.semaphore_wait(barrier, 10)
            swap('dout1', 'act1', 'hl', 'hr', 'vin1', 'act0', 'vin0', 'pat')
        else:
            swap('dout0')
        busy['do'] = [f'dout{l}']
        keep.wait()
        burst(f'c{l}_0')
        run = during(f'c{l}_', NBLK)

        def blocks(i, slot):
            t, h = i // 2, i % 2
            part = pl.ds(pl.multiple_of(h * BLK, BLK), BLK)
            whole = pl.ds(pl.multiple_of(i * BLK, BLK), BLK)
            return [(wc.at[2 * l, t, :, :, :, :, part], w1_v.at[slot]), (wc.at[2 * l + 1, t, h], w2_v.at[slot]),
                    (pre_in.at[l, :, whole], pre_v.at[slot])]

        def outs(i, slot):
            return [(dp_v.at[slot], dpre.at[l, :, pl.ds(pl.multiple_of(i * BLK, BLK), BLK)])]

        def channel(i, slot):
            run(i)

            for n in range(2):
                cols = slice(256 * n, 256 * n + 256)
                d = dot_nt(do_v[...], w2_v[slot, 2 * n:2 * n + 2].reshape(256, CH)) * pre_v[slot, :, cols]
                gbch1[l:l + 1, pl.ds(pl.multiple_of(i * BLK + 256 * n, 256), 256)] = jnp.sum(d, axis=0, keepdims=True)
                dp_v[slot, :, cols] = d.astype(bf16)

            @pl.when(i == 0)
            def _():
                dv_v[...] = jnp.zeros_like(dv_v)
            for n in range(2):
                cols = slice(512 * n, 512 * n + 512)
                dv_v[:, cols] += dot_nt(dp_v[slot], w1_v[slot, n].reshape(512, BLK))
        for_blocks(Stream(sem_w, blocks, NBLK), channel, Stream(sem_o, outs, NBLK))
        swap(f'dpre{l}')
        burst(f'l{l}')
        load.wait()

        @pl.loop(0, ROWS // TPAD)
        def _(n):
            rows = pl.ds(pl.multiple_of(n * TPAD, TPAD), TPAD)
            std, inv = standardize(get(x_v, rows))
            d = dv_v[rows, :]
            add(r + 2, d * std)
            add(r + 3, d)
            put(d_v, rows, get(d_v, rows) + norm_grad(d, vec[r + 2:r + 3, :], std, inv))
        load = pltpu.make_async_copy(xin.at[l], x_v.at[:, pl.ds(0, ROWS)], sem.at[0])
        load.start()
        burst(f't{l}_0')
        load.wait()
        run = during(f't{l}_', IMG)

        @pl.loop(0, IMG)
        def _(m):
            run(m)
            std, inv = standardize(get(x_v, image(m)))
            a = with_bias_rows(std * vec[r:r + 1, :] + vec[r + 1:r + 2, :])
            d_mid = get(d_v, image(m))
            dm = d_mid.astype(bf16)
            parts = []
            for n in range(TOK_CUTS):
                cols = slice(CH // TOK_CUTS * n, CH // TOK_CUTS * (n + 1))
                value, slope = gelu_both(dot_nn(wt[l, :, 0:TPAD], a[:, cols]))
                add_token(2 + l, dot_nt(value.astype(bf16), dm[:, cols]))
                dh = dot_nn(wt[2 + l, :, 0:TPAD], dm[:, cols]) * slope
                add_token(l, jnp.sum(dh, axis=-1, keepdims=True), 64)
                dh = dh.astype(bf16)
                add_token(l, dot_nt(dh, a[:, cols]))
                parts.append(dot_nn(wt_t[l], dh))
            d = jnp.where(mask, jnp.concatenate(parts, axis=1), 0.0)
            add(r, d * std)
            add(r + 1, d)
            put(d_v, image(m), d_mid + norm_grad(d, vec[r:r + 1, :], std, inv))
        if l == 1:
            load = pltpu.make_async_copy(xmid.at[0], x_v.at[:, pl.ds(0, ROWS)], sem.at[0])
            load.start()
            burst('d0')

    burst('fin')
    free('do')
    cast_out(0)
    keep = pltpu.make_async_copy(do_v, dres, sem.at[1])
    keep.start()
    swap('dres')
    keep.wait()
    small_pack(b, x_v, d_v, gvec, hstat, gbch1, gbh)

    last = []

    def put_small(name, src, dst, target):
        last.append(name)
        net.start(name, lambda: (src, dst, target))

    def small(n):
        x, z, y = (ring[d][0] for d in 'xzy')
        net.arrived(*last)
        last.clear()
        if n == 0:
            put_small(('sm', 0), b['sm'].at[:, :, :, k2], b['sm1'], partner)
            put_small(('tk', 0), b['tk'].at[:, :, :, k2], b['tk1'], partner)
        elif n == 1:
            @pl.loop(0, 4)
            def _(i):
                b['sm1'][i] += b['sm'][i, :, :, k]
                b['tk1'][i] += b['tk'][i, :, :, k]
            for s in (1, 2, 3):
                put_small(('sm', 1, s), b['sm1'].at[ring['x'][s]], b['sm2'].at[s - 1], peers['x', s])
                put_small(('tk', 1, s), b['tk1'].at[:, ring['z'][s]], b['tk2'].at[s - 1], peers['z', s])
        elif n == 2:
            b['sm_s1'][...] = b['sm1'][x] + b['sm2'][0] + b['sm2'][1] + b['sm2'][2]

            @pl.loop(0, 4)
            def _(i):
                b['tk_s1'][i] = b['tk1'][i, z] + b['tk2'][0, i] + b['tk2'][1, i] + b['tk2'][2, i]
            for s in (1, 2, 3):
                put_small(('sm', 2, s), b['sm_s1'].at[ring['z'][s]], b['sm3'].at[s - 1], peers['z', s])
                put_small(('tk', 2, s), b['tk_s1'].at[:, ring['y'][s]], b['tk3'].at[s - 1], peers['y', s])
        elif n == 3:
            b['sm_s2'][...] = b['sm_s1'][z] + b['sm3'][0] + b['sm3'][1] + b['sm3'][2]
            b['tk_s2'][...] = b['tk_s1'][:, y] + b['tk3'][0] + b['tk3'][1] + b['tk3'][2]
            for s in (1, 2, 3):
                put_small(('sm', 3, s), b['sm_s2'].at[ring['y'][s]], b['sm4'].at[s - 1], peers['y', s])
                put_small(('tk', 3, s), b['tk_s2'], b['tk4'].at[s - 1], peers['x', s])
        else:
            sm_own[...] = b['sm_s2'][y] + b['sm4'][0] + b['sm4'][1] + b['sm4'][2]
            ordered = []
            for place in range(4):
                value = b['tk_s2'][...]
                for s in (1, 2, 3):
                    value = jnp.where(ring['x'][4 - s] == place, b['tk4'][s - 1], value)
                ordered.append(value)
            tk_own[...] = (ordered[0] + ordered[1]) + (ordered[2] + ordered[3])

    tail = bursts.get('end', ())
    small(0)
    for n, s in enumerate(tail):
        step(*s)
        if n in (8, 18, 28, 38):
            small(1 + (8, 18, 28, 38).index(n))
    net.finish()
    assert len(net.builds) <= BACK_COPIES, len(net.builds)


def back(*operands):
    a, v = pl.BlockSpec(memory_space=pl.ANY), pl.BlockSpec(memory_space=pltpu.VMEM)
    S, V, DMA = jax.ShapeDtypeStruct, pltpu.VMEM, pltpu.SemaphoreType.DMA
    return pl.pallas_call(
        back_kernel, name='back',
        in_specs=[a] * 7 + [v] * 8, out_specs=[v] * 5 + [a] * 9,
        out_shape=[S((N_CH, 32, 1024), f32), S((96, 256), f32), S((32, 256), f32), S((8, 128), f32), S((4, 16, 128), f32),
                   S((2, ROWS, CHH), bf16), S((2, ROWS, CH), bf16), S((ROWS, CH), bf16), S((2, ROWS, 2048), bf16),
                   S((2, ROWS, 512), bf16), S((ROWS, 1536), bf16), S((2, ROWS, CHH), bf16), S((2, ROWS, CH), bf16),
                   S((ROWS, CH), bf16)],
        scratch_shapes=[reduce_scratch(), small_scratch(), V((2, ROWS, CHH), bf16), V((2, ROWS, CH), bf16), V((IMG, 512), bf16),
                        V((IMG, CH), bf16), V((16, CH), f32), V((2, CHH), f32), V((CH // 128, XROWS, 128), f32),
                        V((CH // 128, XROWS, 128), f32), V((ROWS, CH), f32), V((ROWS, CH), bf16), V((2, 2, 4, 4, 32, BLK), bf16),
                        V((2, 4, 4, 32, CH), bf16), V((2, ROWS, BLK), f32), V((2, ROWS, BLK), bf16), DMA((BACK_COPIES,)), DMA((BACK_COPIES,)), DMA((4,)), DMA((2,)), DMA((2, 3)),
                        DMA((2, 1))],
        compiler_params=pltpu.CompilerParams(collective_id=1, has_side_effects=True, vmem_limit_bytes=64 * 1024 * 1024 - 65536),
        cost_estimate=pl.CostEstimate(flops=120_000_000_000, bytes_accessed=200_000_000, transcendentals=0),
    )(*operands)


def finish_kernel(c, stem, head, sm, tk, loss, o_stem, o_bstem, o_ln1g, o_ln1b, o_wt1, o_bt1, o_wt2, o_ln2g, o_ln2b, o_ch1,
                  o_bch1, o_ch2, o_bch2, o_lnfg, o_lnfb, o_head, o_bhead):
    def core_last(value):
        half = value.shape[1] // 2
        return jnp.concatenate([value[:, k * half + a:k * half + a + 32] for a in range(0, half, 32) for k in range(2)], axis=1)
    for l in range(2):
        o_ch1[l] = core_last(c[2 * l])
        o_ch2[l] = core_last(c[2 * l + 1])
    o_stem[...] = core_last(stem[...])
    o_head[...] = head[:, 0:250]
    own = sm[...]
    turned = jnp.concatenate([own, jnp.zeros((120, 128), f32)], axis=0).T
    for ref, n in ((o_bstem, 0), (o_lnfg, 11), (o_lnfb, 12)):
        ref[...] = turned[n, 0:8]
    for n, ref in enumerate((o_ln1g, o_ln1b, o_ln2g, o_ln2b, o_bch2)):
        for l in range(2):
            ref[pl.ds(l, 1), :] = turned[1 + 5 * l + n:2 + 5 * l + n, 0:8]
    o_bch1[...] = own[0:2, 32:64]
    classes = jnp.concatenate([own[2 + q:3 + q, 64:128] for q in range(4)], axis=1)
    o_bhead[...] = classes[0, 0:250]
    loss[...] = own[6:7, 64:65] * (1.0 / 1024)
    for l in range(2):
        o_wt1[l] = tk[l, :, 0:TOK]
        o_wt2[l] = tk[2 + l, :, 0:TOK]
        tall = jnp.concatenate([tk[l], jnp.zeros((112, 128), f32)], axis=0).T
        o_bt1[pl.ds(l, 1), :] = tall[64:65, 0:16]


def finish(*operands):
    S = jax.ShapeDtypeStruct
    v = pl.BlockSpec(memory_space=pltpu.VMEM)
    return pl.pallas_call(
        finish_kernel, name='finish', in_specs=[v] * 5, out_specs=[v] * 18,
        out_shape=[S((1, 1), f32), S((96, 256), f32), S((8,), f32), S((2, 8), f32), S((2, 8), f32), S((2, 16, TOK), f32),
                   S((2, 16), f32), S((2, 16, TOK), f32), S((2, 8), f32), S((2, 8), f32), S((2, 32, 1024), f32), S((2, 32), f32),
                   S((2, 32, 1024), f32), S((2, 8), f32), S((8,), f32), S((8,), f32), S((32, 250), f32), S((250,), f32)],
    )(*operands)

CHANNEL_AXES = ('tp', 'fsdp')


def weight_specs():
    vec_spec = P(CHANNEL_AXES)
    layer_vec = P(None, CHANNEL_AXES)
    return (P('fsdp', 'tp'), vec_spec, layer_vec, layer_vec, P(None, None, 'fsdp'), P(None, 'fsdp'),
            P(None, 'fsdp', None), layer_vec, layer_vec, P(None, 'fsdp', 'tp'), layer_vec,
            P(None, CHANNEL_AXES, None), layer_vec, vec_spec, vec_spec, P('fsdp', 'tp'), P('tp'))


def solution(mesh):
    def step(patches, labels, w_stem, b_stem, ln1_g, ln1_b, w_tok1, b_tok1, w_tok2,
             ln2_g, ln2_b, w_ch1, b_ch1, w_ch2, b_ch2, lnf_g, lnf_b, w_head, b_head):
        wc, pat, xin, xmid, vin, pre, act, hl, hr, dx0, hstat, gbh, vec, wt, wt_t = front(
            labels, patches.transpose(1, 0, 2), w_stem, w_ch1, w_ch2, w_head, w_tok1.transpose(0, 2, 1), w_tok2, b_tok1, b_ch1,
            b_head, b_stem, ln1_g, ln1_b, ln2_g, ln2_b, b_ch2, lnf_g, lnf_b)
        sums = back(xin, xmid, pre, wc, act, vin, pat, hl, hr, dx0, hstat, gbh, wt, wt_t, vec)[:5]
        loss, g_s, g_bs, g_1g, g_1b, g_t1, g_bt, g_t2, g_2g, g_2b, g_c1, g_b1, g_c2, g_b2, g_fg, g_fb, g_h, g_bh = finish(*sums)
        return (loss.reshape(()), g_s, g_bs, g_1g, g_1b, g_t1.transpose(0, 2, 1), g_bt, g_t2, g_2g, g_2b, g_c1, g_b1, g_c2, g_b2,
                g_fg, g_fb, g_h, g_bh)

    specs = weight_specs()
    return jax.shard_map(step, mesh=mesh, in_specs=(P('fsdp', None, None), P('fsdp')) + specs,
                         out_specs=(P(),) + specs, check_vma=False)
```
